32 devices in a mesh: rep: 4 (over x, core), fsdp: 8 (over z, y).
Axes of the slice: x: 2, y: 2, z: 4, core: 2. Of those that a mesh axis runs over, the one named last changes fastest.
Arguments:
- layer_input: bfloat16 [2, 24576, 768], P(None, ('rep', 'fsdp')), may hold values from -6 to 6
- cotangent: bfloat16 [2, 24576, 768], P(None, ('rep', 'fsdp')), may hold values from -6 to 6
- lengths: int32 [2, 384], P(None, ('rep', 'fsdp')), may hold values from 0 to 320, as said below
- attn_gain: bfloat16 [768], P('fsdp'), may hold values from 0.5 to 1.5
- global_gain: bfloat16 [768], P('fsdp'), may hold values from 0.5 to 1.5
- query_weight: bfloat16 [768, 768], P('fsdp'), may hold values from -0.0546875 to 0.0546875
- key_weight: bfloat16 [768, 768], P('fsdp'), may hold values from -0.21875 to 0.21875
- value_weight: bfloat16 [768, 768], P('fsdp'), may hold values from -0.21875 to 0.21875
- out_weight: bfloat16 [768, 768], P('fsdp'), may hold values from -0.875 to 0.875
- ffn_gain: bfloat16 [768], P('fsdp'), may hold values from 0.5 to 1.5
- gate_weight: bfloat16 [768, 2048], P('fsdp'), may hold values from -0.21875 to 0.21875
- up_weight: bfloat16 [768, 2048], P('fsdp'), may hold values from -0.21875 to 0.21875
- down_weight: bfloat16 [2048, 768], P('fsdp'), may hold values from -0.125 to 0.125
Outputs:
- layer_output: bfloat16 [2, 24576, 768], P(None, ('rep', 'fsdp'))
- in_grad: bfloat16 [2, 24576, 768], P(None, ('rep', 'fsdp'))
- attn_gain_grad: float32 [768], P('fsdp')
- global_gain_grad: float32 [768], P('fsdp')
- query_grad: float32 [768, 768], P('fsdp')
- key_grad: float32 [768, 768], P('fsdp')
- value_grad: float32 [768, 768], P('fsdp')
- out_weight_grad: float32 [768, 768], P('fsdp')
- ffn_gain_grad: float32 [768], P('fsdp')
- gate_grad: float32 [768, 2048], P('fsdp')
- up_grad: float32 [768, 2048], P('fsdp')
- down_grad: float32 [2048, 768], P('fsdp')
The draws below stay inside these ranges and needn't reach their ends.
Inputs may be any that keep to these rules, and one draw needn't show every extreme that they name: `lengths`: entry b of the 12 entries that one device holds for one micro-batch is 0 or the length of a sequence whose first token is in block b; a sequence of n tokens fills its first block and the next ceil(n / 64) - 1 blocks of the same device, ending before the next nonzero entry. A device's filled blocks come first. On the 4 devices of one fsdp index, sequences fill exactly 16 blocks of each micro-batch. Some sequence of every draw has 320 tokens.
All inputs are finite; a program needn't handle non-finite values.
Results may differ from the reference program's by a relative error of at most 0.03.
Values may be sent and summed in bfloat16 or wider, within the bound.
A program may use at most 256 MiB of HBM per device.

```python
import jax
import jax.numpy as jnp
from jax import lax

D = 768
H = 12
DH = 64
FF = 2048
RADIUS = 127
GBLK = 16
BLK = 64
MICRO = 2
AVG_BLOCKS = 4
HD = 768
SRC_BLOCKS = 12
QB = 256
KPAD = 128
TOK_ALL = 24576
N_REP = 4
N_FSDP = 8


def tile_marks(base_key, begin, length, longest, positions):
    steps = jax.random.randint(base_key, (positions,), 1, longest + 1)
    marks = begin + jnp.cumsum(steps) - steps
    spots = jnp.arange(positions)
    hits = (spots[:, None] == marks[None, :]) & (marks[None, :] < begin + length)
    return jnp.any(hits, axis=1)


def group_lengths(base_key):
    positions = AVG_BLOCKS * N_REP
    longest = AVG_BLOCKS + 1
    keys_list = jax.random.split(base_key, 6)
    which = jax.random.randint(keys_list[0], (), 0, N_REP - 1)
    left_edge = which * AVG_BLOCKS
    forced = left_edge + AVG_BLOCKS - 1
    after = forced + longest
    spots = jnp.arange(positions)
    starts = tile_marks(keys_list[1], 0, left_edge, longest, positions)
    starts = starts | tile_marks(keys_list[2], left_edge, AVG_BLOCKS - 1, longest, positions)
    starts = starts | tile_marks(keys_list[3], after, positions - after, longest, positions)
    starts = starts | (spots == left_edge) | (spots == forced)
    later = jnp.where(starts[None, :] & (spots[None, :] > spots[:, None]), spots[None, :], positions)
    next_start = jnp.min(later, axis=1)
    blocks = next_start - spots
    tails = jax.random.randint(keys_list[4], (positions,), 1, BLK + 1)
    tokens = jnp.where(spots == forced, longest * BLK, (blocks - 1) * BLK + tails)
    tokens = jnp.where(starts, tokens, 0)
    candidate = starts & (spots >= positions - SRC_BLOCKS) & (spots <= SRC_BLOCKS)

    def pick(pick_key):
        scores = jax.random.randint(pick_key, (positions,), 0, 1 << 20) * positions + spots
        scores = jnp.where(candidate, scores, -1)
        return lax.top_k(scores, 1)[1][0].astype(jnp.int32)
    picks = jnp.sort(jax.vmap(pick)(jax.random.split(keys_list[5], N_REP - 1)))
    bounds = jnp.concatenate([jnp.zeros((1,), jnp.int32), picks, jnp.full((1,), positions, jnp.int32)])
    local_spots = jnp.arange(SRC_BLOCKS)
    source = bounds[:-1, None] + local_spots[None, :]
    inside = source < bounds[1:, None]
    return jnp.where(inside, tokens[jnp.minimum(source, positions - 1)], 0)


def draw_lengths(key, part):
    group_keys = jax.random.split(key, MICRO * N_FSDP)
    table = jax.vmap(group_lengths)(group_keys)
    table = table.reshape(MICRO, N_FSDP, N_REP, SRC_BLOCKS)
    table = jnp.transpose(table, (0, 2, 1, 3))
    return table.reshape(MICRO, N_REP * N_FSDP * SRC_BLOCKS).astype(jnp.int32)


def shard_levels(rng, shape, cuts, least, top_value):
    loudness, own = 1.0, jax.random.fold_in(rng, 6)
    for position, blocks in cuts:
        draws = jnp.exp(jax.random.uniform(jax.random.fold_in(own, position), (blocks,), jnp.float32, least / len(cuts), top_value / len(cuts)))
        loudness = loudness * jnp.repeat(draws, shape[position] // blocks).reshape([-1 if axis == position else 1 for axis in range(len(shape))])
    return loudness


def noise(rng, dims, deviation, bound, cuts=(), held_as=jnp.bfloat16):
    values = deviation * jax.random.normal(rng, dims, jnp.float32)
    if cuts:
        values = values * shard_levels(rng, dims, cuts, -0.22, 0.18)
    return jnp.clip(values, -bound, bound).astype(held_as)


def setup_inputs(seed: int = 0) -> dict:
    key_list = jax.random.split(jax.random.key(seed), 14)
    layer_input = noise(key_list[0], (MICRO, TOK_ALL, D), 1.0, 6.0, ((1, 32),))
    cotangent = noise(key_list[1], (MICRO, TOK_ALL, D), 1.0, 6.0, ((1, 32),))
    lengths = draw_lengths(jax.random.fold_in(key_list[13], 71), 0)
    attn_gain = jnp.clip(1.0 + 0.1 * jax.random.normal(key_list[3], (D,), jnp.float32), 0.5, 1.5).astype(jnp.bfloat16)
    global_gain = jnp.clip(1.0 + 0.1 * jax.random.normal(key_list[4], (D,), jnp.float32), 0.5, 1.5).astype(jnp.bfloat16)
    query_weight = noise(key_list[5], (D, HD), (16 * D) ** -0.5, 0.0546875, ((0, 8),))
    key_weight = noise(key_list[6], (D, HD), D ** -0.5, 0.21875, ((0, 8),))
    value_weight = noise(key_list[7], (D, HD), D ** -0.5, 0.21875, ((0, 8),))
    out_weight = noise(key_list[8], (HD, D), (HD // 16) ** -0.5, 0.875, ((0, 8),))
    ffn_gain = jnp.clip(1.0 + 0.1 * jax.random.normal(key_list[9], (D,), jnp.float32), 0.5, 1.5).astype(jnp.bfloat16)
    gate_weight = noise(key_list[10], (D, FF), D ** -0.5, 0.21875, ((0, 8),))
    up_weight = noise(key_list[11], (D, FF), D ** -0.5, 0.21875, ((0, 8),))
    down_weight = noise(key_list[12], (FF, D), FF ** -0.5, 0.125, ((0, 8),))
    return dict(layer_input=layer_input, cotangent=cotangent, lengths=lengths, attn_gain=attn_gain, global_gain=global_gain, query_weight=query_weight, key_weight=key_weight, value_weight=value_weight, out_weight=out_weight, ffn_gain=ffn_gain, gate_weight=gate_weight, up_weight=up_weight, down_weight=down_weight)


EPSILON = 1e-06
MASKED_SCORE = -1e+30
HIGHEST_PRECISION = lax.Precision.HIGHEST

@jax.custom_vjp
def low(v):
    return lax.optimization_barrier(v.astype(jnp.bfloat16)).astype(jnp.float32)

@jax.custom_vjp
def low_back(v):
    return v

def low_keep(v):
    return (low(v), None)

def low_pass(kept, grad):
    return (grad,)

def back_keep(v):
    return (v, None)

def back_low(kept, grad):
    return (low(grad),)
low.defvjp(low_keep, low_pass)
low_back.defvjp(back_keep, back_low)

def matmul(left_op, right_op):
    return jnp.dot(left_op, right_op, precision=HIGHEST_PRECISION)

def rms_norm(row_data, gain_vec):
    return row_data * lax.rsqrt(lax.optimization_barrier(jnp.mean(row_data * row_data, axis=-1, keepdims=True)) + EPSILON) * gain_vec

def layout(block_lens):
    block_count = block_lens.shape[0]
    block_index = jnp.arange(block_count, dtype=jnp.int32)
    first_start = lax.cummax(jnp.where(block_lens > 0, block_index, -1), axis=0)
    safe_first = jnp.maximum(first_start, 0)
    owner_len = lax.optimization_barrier(jnp.sum(jnp.where(block_index[None, :] == safe_first[:, None], block_lens[None, :], 0), axis=1))
    offset = (block_index - first_start)[:, None] * BLK + jnp.arange(BLK, dtype=jnp.int32)[None, :]
    valid_tok = (first_start[:, None] >= 0) & (offset < owner_len[:, None])
    seg_tok = jnp.broadcast_to(first_start[:, None], (block_count, BLK))
    return (seg_tok.reshape(-1), valid_tok.reshape(-1))

def forward(inputs_f, block_lens, attn_gain, global_gain, query_weight, key_weight, value_weight, out_weight, ffn_gain, gate_weight, up_weight, down_weight):
    row_count = inputs_f.shape[0]
    slot_count = row_count // GBLK
    seg_tok, valid_tok = layout(block_lens)
    valid_col = valid_tok.astype(jnp.float32)[:, None]
    normed = low(rms_norm(inputs_f, attn_gain))
    side_sum = lax.optimization_barrier(jnp.sum((normed * valid_col).reshape(slot_count, GBLK, D), axis=1))
    side_normed = low(rms_norm(side_sum, global_gain))
    queries = low_back(low(matmul(normed, query_weight)))
    keys_all = low_back(low(matmul(normed, key_weight)))
    values_all = low_back(low(matmul(normed, value_weight)))
    global_keys = low_back(low(matmul(side_normed, key_weight))).reshape(slot_count, H, DH)
    global_values = low_back(low(matmul(side_normed, value_weight))).reshape(slot_count, H, DH)
    seg_key = jnp.where(valid_tok, seg_tok, -2)
    seg_global = seg_key[::GBLK]
    keys_pad = jnp.pad(keys_all, ((KPAD, KPAD), (0, 0)))
    values_pad = jnp.pad(values_all, ((KPAD, KPAD), (0, 0)))
    seg_key_pad = jnp.pad(seg_key, (KPAD, KPAD), constant_values=-3)
    key_width = QB + 2 * KPAD
    band = jnp.abs(jnp.arange(QB, dtype=jnp.int32)[:, None] + KPAD - jnp.arange(key_width, dtype=jnp.int32)[None, :]) <= RADIUS

    def attend_one(row_start):
        query_blk = lax.dynamic_slice_in_dim(queries, row_start, QB, 0).reshape(QB, H, DH)
        key_win = lax.dynamic_slice_in_dim(keys_pad, row_start, key_width, 0).reshape(key_width, H, DH)
        value_win = lax.dynamic_slice_in_dim(values_pad, row_start, key_width, 0).reshape(key_width, H, DH)
        seg_rows = lax.dynamic_slice_in_dim(seg_tok, row_start, QB, 0)
        seg_window = lax.dynamic_slice_in_dim(seg_key_pad, row_start, key_width, 0)
        local_scores = jnp.einsum('qhd,khd->hqk', query_blk, key_win, precision=HIGHEST_PRECISION)
        global_scores = jnp.einsum('qhd,ghd->hqg', query_blk, global_keys, precision=HIGHEST_PRECISION)
        scores = low_back(jnp.concatenate([local_scores, global_scores], axis=-1))
        allow_local = band & (seg_rows[:, None] == seg_window[None, :])
        allow_global = seg_rows[:, None] == seg_global[None, :]
        allowed = jnp.concatenate([allow_local, allow_global], axis=-1)
        masked = jnp.where(allowed[None], scores, MASKED_SCORE)
        row_peak = lax.optimization_barrier(jnp.max(masked, axis=-1, keepdims=True))
        weights_exp = jnp.exp(masked - row_peak)
        probs = low(weights_exp / lax.optimization_barrier(jnp.sum(weights_exp, axis=-1, keepdims=True)))
        mixed_rows = jnp.einsum('hqk,khd->qhd', probs[..., :key_width], value_win, precision=HIGHEST_PRECISION)
        mixed_rows = mixed_rows + jnp.einsum('hqg,ghd->qhd', probs[..., key_width:], global_values, precision=HIGHEST_PRECISION)
        return mixed_rows.reshape(QB, H * DH)
    starts = jnp.arange(row_count // QB, dtype=jnp.int32) * QB
    attended = lax.map(jax.checkpoint(attend_one), starts).reshape(row_count, H * DH)
    attended = low_back(low(attended))
    hidden_one = inputs_f + low_back(matmul(attended, out_weight))
    normed_two = low(rms_norm(hidden_one, ffn_gain))
    gate_pre = low_back(matmul(normed_two, gate_weight))
    up_pre = low_back(matmul(normed_two, up_weight))
    hidden_two = low(jax.nn.gelu(gate_pre, approximate=True) * up_pre)
    return valid_col * (hidden_one + matmul(hidden_two, down_weight))

def reference(layer_input, cotangent, lengths, attn_gain, global_gain, query_weight, key_weight, value_weight, out_weight, ffn_gain, gate_weight, up_weight, down_weight):
    params = tuple((weight_arr.astype(jnp.float32) for weight_arr in (attn_gain, global_gain, query_weight, key_weight, value_weight, out_weight, ffn_gain, gate_weight, up_weight, down_weight)))
    span_rows = SRC_BLOCKS * BLK
    buffers = MICRO * N_REP * N_FSDP
    row_data = layer_input.reshape(buffers, span_rows, D).astype(jnp.float32)
    cot_data = cotangent.reshape(buffers, span_rows, D).astype(jnp.float32)
    lens_data = lengths.reshape(buffers, SRC_BLOCKS)

    def step(totals, inputs):
        rows_one, cot_one, lens_one = inputs

        def apply(inputs_f, gain_attn, gain_global, weight_query, weight_key, weight_value, weight_out, gain_ffn, weight_gate, weight_up, weight_down):
            return forward(inputs_f, lens_one, gain_attn, gain_global, weight_query, weight_key, weight_value, weight_out, gain_ffn, weight_gate, weight_up, weight_down)
        result, pullback = jax.vjp(apply, rows_one, params[0], params[1], params[2], params[3], params[4], params[5], params[6], params[7], params[8], params[9])
        grads = pullback(cot_one)
        totals = tuple((total_old + term_new for total_old, term_new in zip(totals, grads[1:])))
        return (totals, (result.astype(jnp.bfloat16), grads[0].astype(jnp.bfloat16)))
    initial = tuple((jnp.zeros(weight_arr.shape, jnp.float32) for weight_arr in params))
    totals, (outputs, input_grads) = lax.scan(step, initial, (row_data, cot_data, lens_data))
    layer_output = outputs.reshape(MICRO, TOK_ALL, D)
    in_grad = input_grads.reshape(MICRO, TOK_ALL, D)
    return (layer_output, in_grad, totals[0], totals[1], totals[2], totals[3], totals[4], totals[5], totals[6], totals[7], totals[8], totals[9])
```

```python
from functools import partial

import jax
import jax.numpy as jnp
from jax import lax
from jax.experimental import pallas as pl
from jax.experimental.pallas import tpu as pltpu
from jax.sharding import PartitionSpec as P

H = 12
DH = 64
RADIUS = 127
GBLK = 16
BLK = 64
SLOTS = 10
MAX_SEQ_BLOCKS = 5
EPSILON = 1e-06
MASKED_SCORE = -1e30
MESH = pl.DeviceIdType.MESH
VMEM_LIMIT = 60 * 1024 * 1024
SEG_AT, LEN_AT, DEST_AT, TABLE_SIZE = 40, 80, 120, 256

ANY = pl.BlockSpec(memory_space=pl.ANY)
VMEM = pl.BlockSpec(memory_space=pltpu.VMEM)
SMEM = pl.BlockSpec(memory_space=pltpu.SMEM)


def grid_of(count):
    inner = 2 if count <= 8 else 4
    return count // inner, inner


def core_of(rank):
    return rank + 1 - 2 * (rank % 2)


def across_of(rank):
    return (rank + 2) % 4


def lens_kernel(lens_ref, all_ref, send_sem, recv_sem):
    rank = lax.axis_index("rep")
    barrier = pltpu.get_barrier_semaphore()
    for step in range(1, 4):
        pl.semaphore_signal(
            barrier, inc=1, device_id={"rep": (rank + step) % 4}, device_id_type=MESH
        )
    pl.semaphore_wait(barrier, 3)
    copies = []
    for step in range(1, 4):
        copy = pltpu.make_async_remote_copy(
            src_ref=lens_ref,
            dst_ref=all_ref.at[rank],
            send_sem=send_sem.at[step - 1],
            recv_sem=recv_sem.at[step - 1],
            device_id={"rep": (rank + step) % 4},
            device_id_type=MESH,
        )
        copy.start()
        copies.append(copy)
    all_ref[rank] = lens_ref[...]
    for copy in copies:
        copy.wait()


def table_kernel(micro, per_dev, lens_ref, tab_ref, order_ref, count_ref, load_ref):
    total = 4 * micro * per_dev

    def length_at(spot):
        return lens_ref[spot // (micro * per_dev), (spot // per_dev) % micro, spot % per_dev]

    def blocks_of(length):
        return (length + (BLK - 1)) // BLK

    def clear(spot, carry):
        tab_ref[spot] = -1
        return carry

    lax.fori_loop(0, TABLE_SIZE, clear, 0)
    for spot in range(4 * SLOTS):
        tab_ref[LEN_AT + spot] = 0
    for size in range(8):
        count_ref[size] = 0
    for dev in range(4):
        load_ref[dev] = 0

    def tally(spot, carry):
        length = length_at(spot)

        @pl.when(length > 0)
        def _():
            size = blocks_of(length)
            count_ref[size] = count_ref[size] + 1

        return carry

    lax.fori_loop(0, total, tally, 0)
    begin = 0
    for size in range(MAX_SEQ_BLOCKS, 0, -1):
        amount = count_ref[size]
        count_ref[size] = begin
        begin = begin + amount

    def place(spot, carry):
        length = length_at(spot)

        @pl.when(length > 0)
        def _():
            size = blocks_of(length)
            where = count_ref[size]
            order_ref[where] = spot
            count_ref[size] = where + 1

        return carry

    lax.fori_loop(0, total, place, 0)

    def assign(number, carry):
        spot = order_ref[number]
        length = length_at(spot)
        size = blocks_of(length)
        best = jnp.int32(0)
        low = load_ref[0]
        for dev in range(1, 4):
            here = load_ref[dev]
            best = jnp.where(here < low, dev, best)
            low = jnp.minimum(here, low)
        load_ref[best] = low + size

        def put(step, inner):
            slot = best * SLOTS + low + step
            tab_ref[slot] = spot + step
            tab_ref[SEG_AT + slot] = low
            tab_ref[LEN_AT + slot] = jnp.minimum(length - BLK * step, BLK)
            tab_ref[DEST_AT + spot + step] = slot
            return inner

        lax.fori_loop(0, size, put, 0)
        return carry

    lax.fori_loop(0, begin, assign, 0)


def deal_table(lengths):
    micro, per_dev = lengths.shape
    padded = jnp.pad(lengths, ((0, 8 - micro), (0, 128 - per_dev)))
    everyone = pl.pallas_call(
        lens_kernel,
        out_shape=jax.ShapeDtypeStruct((4, 8, 128), jnp.int32),
        in_specs=[VMEM],
        out_specs=VMEM,
        scratch_shapes=[pltpu.SemaphoreType.DMA((3,)), pltpu.SemaphoreType.DMA((3,))],
        compiler_params=pltpu.CompilerParams(collective_id=0, has_side_effects=True),
        name="lens_exchange",
    )(padded)
    return pl.pallas_call(
        partial(table_kernel, micro, per_dev),
        out_shape=jax.ShapeDtypeStruct((TABLE_SIZE,), jnp.int32),
        in_specs=[SMEM],
        out_specs=SMEM,
        scratch_shapes=[
            pltpu.SMEM((4 * micro * per_dev,), jnp.int32),
            pltpu.SMEM((8,), jnp.int32),
            pltpu.SMEM((4,), jnp.int32),
        ],
        name="deal_table",
    )(everyone)


def gather_kernel(
    outer, inner, splits, tab_ref, rows_ref, cots_ref, wa_ref, wb_ref, wc_ref,
    ga_ref, gb_ref, gc_ref, rows_out, cots_out,
    psend, precv, xsend, xrecv,
    z_send, z_recv, y_send, y_recv, c_send, c_recv, own_sem,
    p_send, p_recv, x_send, x_recv,
):
    rank = lax.axis_index("rep")
    spot = lax.axis_index("fsdp")
    core = rank % 2
    row, col = spot // inner, spot % inner
    count = outer * inner
    mate, across = core_of(rank), across_of(rank)
    pieces = [(wa_ref, ga_ref, start, width // 2) for start, width in splits]
    pieces.append((wb_ref, gb_ref, 0, wb_ref.shape[1] // 2))
    pieces.append((wc_ref, gc_ref, 0, None))
    halved = [number for number, piece in enumerate(pieces) if piece[3] is not None]

    barrier = pltpu.get_barrier_semaphore()
    neighbours = (
        (row + 1 < outer, {"fsdp": spot + inner}),
        (row > 0, {"fsdp": spot - inner}),
        (col + 1 < inner, {"fsdp": spot + 1}),
        (col > 0, {"fsdp": spot - 1}),
    )
    amount = jnp.int32(2)
    for there, device in neighbours:
        amount = amount + there.astype(jnp.int32)

        @pl.when(there)
        def _():
            pl.semaphore_signal(barrier, inc=1, device_id=device, device_id_type=MESH)

    for device in (mate, across):
        pl.semaphore_signal(barrier, inc=1, device_id={"rep": device}, device_id_type=MESH)
    pl.semaphore_wait(barrier, amount)

    def cut(ref, number):
        _, _, start, half = pieces[number]
        if half is None:
            return ref
        return ref.at[:, pl.ds(pl.multiple_of(start + core * half, 128), half)]

    def landed(number, shard):
        return cut(pieces[number][1].at[shard], number)

    late = []

    def send(there, src, dst, ssem, rsem, device):
        def describe():
            return pltpu.make_async_remote_copy(
                src_ref=src, dst_ref=dst, send_sem=ssem, recv_sem=rsem,
                device_id=device, device_id_type=MESH,
            )

        if there is None:
            describe().start()
            late.append((None, lambda: describe().wait_send()))
        else:
            @pl.when(there)
            def _():
                describe().start()

            late.append((there, lambda: describe().wait_send()))

    def arrive(number, shard, rsem):
        pltpu.make_async_remote_copy(
            src_ref=landed(number, shard), dst_ref=landed(number, shard),
            send_sem=own_sem.at[0], recv_sem=rsem,
            device_id={"rep": mate}, device_id_type=MESH,
        ).wait_recv()

    def both(first, second):
        return second if first is None else jnp.logical_and(first, second)

    def to_mate(there, number, shard):
        if number not in halved:
            return
        place = landed(number, shard)
        send(there, place, place, c_send.at[number, shard], c_recv.at[number, shard], {"rep": mate})

    def along_row(there, number, line, src):
        shard = line * inner + col
        place = landed(number, shard)
        src = place if src is None else src
        send(both(there, col + 1 < inner), src, place,
             y_send.at[0, 0, line, number], y_recv.at[0, 0, line, number], {"fsdp": spot + 1})
        send(both(there, col > 0), src, place,
             y_send.at[1, 0, line, number], y_recv.at[1, 0, line, number], {"fsdp": spot - 1})

    def from_row(there, number, line):
        for step in range(inner - 1):
            for way, source, onward, target in (
                (0, col - 1 - step, col + 1 < inner, spot + 1),
                (1, col + 1 + step, col > 0, spot - 1),
            ):
                here = jnp.logical_and(source >= 0, source < inner)
                here = both(there, here)
                shard = line * inner + source

                @pl.when(here)
                def _():
                    arrive(number, shard, y_recv.at[way, step, line, number])

                if step + 1 < inner - 1:
                    place = landed(number, shard)
                    send(both(here, onward), place, place,
                         y_send.at[way, step + 1, line, number],
                         y_recv.at[way, step + 1, line, number], {"fsdp": target})
                to_mate(here, number, shard)

    for number, piece in enumerate(pieces):
        src, place = cut(piece[0], number), landed(number, spot)
        send(row + 1 < outer, src, place, z_send.at[0, 0, number], z_recv.at[0, 0, number],
             {"fsdp": spot + inner})
        send(row > 0, src, place, z_send.at[1, 0, number], z_recv.at[1, 0, number],
             {"fsdp": spot - inner})
        along_row(None, number, row, src)
    own = [
        pltpu.make_async_copy(wa_ref, ga_ref.at[spot], own_sem.at[0]),
        pltpu.make_async_copy(wb_ref, gb_ref.at[spot], own_sem.at[1]),
        pltpu.make_async_copy(wc_ref, gc_ref.at[spot], own_sem.at[2]),
    ]
    for copy in own:
        copy.start()

    sources = (rows_ref, cots_ref)
    per_rank = rows_ref.shape[0]

    def picked(kind, target, slot):
        index = tab_ref[target * SLOTS + slot] - rank * per_rank
        mine = jnp.logical_and(index >= 0, index < per_rank)
        value = sources[kind][jnp.clip(index, 0, per_rank - 1)]
        return mine, value

    def mate_copy(kind, part):
        return pltpu.make_async_remote_copy(
            src_ref=psend.at[kind, part], dst_ref=precv.at[kind, part],
            send_sem=p_send.at[kind, part], recv_sem=p_recv.at[kind, part],
            device_id={"rep": mate}, device_id_type=MESH,
        )

    def across_copy(kind):
        return pltpu.make_async_remote_copy(
            src_ref=xsend.at[kind], dst_ref=xrecv.at[kind],
            send_sem=x_send.at[kind], recv_sem=x_recv.at[kind],
            device_id={"rep": across}, device_id_type=MESH,
        )

    for kind, part in ((0, 1), (1, 1), (0, 0), (1, 0)):
        target = mate if part == 0 else across_of(mate)

        def pack(slot, carry):
            mine, value = picked(kind, target, slot)
            psend[kind, part, slot] = jnp.where(mine, value, jnp.zeros_like(value))
            return carry

        lax.fori_loop(0, SLOTS, pack, 0)
        mate_copy(kind, part).start()
    for kind in range(2):
        mate_copy(kind, 1).wait_recv()

        def merge(slot, carry):
            mine, value = picked(kind, across, slot)
            xsend[kind, slot] = jnp.where(mine, value, precv[kind, 1, slot])
            return carry

        lax.fori_loop(0, SLOTS, merge, 0)
        across_copy(kind).start()

    def lines(step):
        return ((row - 1 - step >= 0, row - 1 - step, 0, row + 1 < outer, spot + inner),
                (row + 1 + step < outer, row + 1 + step, 1, row > 0, spot - inner))

    for step in range(outer - 1):
        for number in range(len(pieces)):
            for here, line, way, onward, target in lines(step):
                shard = line * inner + col

                @pl.when(here)
                def _():
                    arrive(number, shard, z_recv.at[way, step, number])

                if step + 1 < outer - 1:
                    place = landed(number, shard)
                    send(jnp.logical_and(here, onward), place, place,
                         z_send.at[way, step + 1, number], z_recv.at[way, step + 1, number],
                         {"fsdp": target})
                along_row(here, number, line, None)
                to_mate(here, number, shard)
        for number in range(len(pieces)):
            if step == 0:
                from_row(None, number, row)
            else:
                for here, line, *_ in lines(step - 1):
                    from_row(here, number, line)
    for number in range(len(pieces)):
        for here, line, *_ in lines(outer - 2):
            from_row(here, number, line)

    outs = (rows_out, cots_out)
    for kind in range(2):
        mate_copy(kind, 0).wait_recv()
        across_copy(kind).wait_recv()

        def finish(slot, carry):
            mine, value = picked(kind, rank, slot)
            outs[kind][slot] = jnp.where(mine, value, precv[kind, 0, slot] + xrecv[kind, slot])
            return carry

        lax.fori_loop(0, SLOTS, finish, 0)

    for shard in range(count):
        @pl.when(shard != spot)
        def _():
            for number in halved:
                other = pieces[number]
                view = other[1].at[shard].at[:, pl.ds(0, other[3])]
                pltpu.make_async_remote_copy(
                    src_ref=view, dst_ref=view, send_sem=own_sem.at[0],
                    recv_sem=c_recv.at[number, shard],
                    device_id={"rep": mate}, device_id_type=MESH,
                ).wait_recv()
    for there, finish_send in late:
        if there is None:
            finish_send()
        else:
            pl.when(there)(finish_send)
    for kind in range(2):
        for part in range(2):
            mate_copy(kind, part).wait_send()
        across_copy(kind).wait_send()
    for copy in own:
        copy.wait()


def gather_weights(count, splits, table, rows, cots, wa, wb, wc):
    outer, inner = grid_of(count)
    block = rows.shape[1:]
    kinds = len(splits) + 2
    dma = pltpu.SemaphoreType.DMA
    bf16 = jnp.bfloat16
    return pl.pallas_call(
        partial(gather_kernel, outer, inner, splits),
        out_shape=(
            jax.ShapeDtypeStruct((count,) + wa.shape, bf16),
            jax.ShapeDtypeStruct((count,) + wb.shape, bf16),
            jax.ShapeDtypeStruct((count,) + wc.shape, bf16),
            jax.ShapeDtypeStruct((SLOTS,) + block, bf16),
            jax.ShapeDtypeStruct((SLOTS,) + block, bf16),
        ),
        in_specs=[SMEM, VMEM, VMEM, VMEM, VMEM, VMEM],
        out_specs=(ANY, ANY, ANY, VMEM, VMEM),
        scratch_shapes=[
            pltpu.VMEM((2, 2, SLOTS) + block, bf16),
            pltpu.VMEM((2, 2, SLOTS) + block, bf16),
            pltpu.VMEM((2, SLOTS) + block, bf16),
            pltpu.VMEM((2, SLOTS) + block, bf16),
            dma((2, outer - 1, kinds)), dma((2, outer - 1, kinds)),
            dma((2, inner - 1, outer, kinds)), dma((2, inner - 1, outer, kinds)),
            dma((kinds, count)), dma((kinds, count)), dma((3,)),
            dma((2, 2)), dma((2, 2)), dma((2,)), dma((2,)),
        ],
        compiler_params=pltpu.CompilerParams(
            collective_id=1, has_side_effects=True, vmem_limit_bytes=VMEM_LIMIT
        ),
        name="gather_and_deal",
    )(table, rows, cots, wa, wb, wc)


def reduce_kernel(
    outer, inner, splits, ga_ref, gb_ref, gc_ref, y_ref, g_ref,
    oa_ref, ob_ref, oc_ref, ry_ref, rg_ref, *scratch,
):
    kinds = len(splits) + 2
    mines, crecvs, yrecvs, zrecvs, xrecvs = (
        scratch[kinds * i : kinds * (i + 1)] for i in range(5)
    )
    (c_send, c_recv, m_sem, y_send, y_recv, z_send, z_recv, x_send, x_recv, f_send, f_recv,
     r_send, r_recv, q_sem) = scratch[5 * kinds :]
    rank = lax.axis_index("rep")
    spot = lax.axis_index("fsdp")
    core = rank % 2
    row, col = spot // inner, spot % inner
    mate, across = core_of(rank), across_of(rank)
    pieces = [(ga_ref, oa_ref, start, width // 2) for start, width in splits]
    pieces.append((gb_ref, ob_ref, 0, gb_ref.shape[3] // 2))
    pieces.append((gc_ref, oc_ref, 0, None))

    barrier = pltpu.get_barrier_semaphore()
    neighbours = (
        (row + 1 < outer, {"fsdp": spot + inner}),
        (row > 0, {"fsdp": spot - inner}),
        (col + 1 < inner, {"fsdp": spot + 1}),
        (col > 0, {"fsdp": spot - 1}),
    )
    amount = jnp.int32(2)
    for there, device in neighbours:
        amount = amount + there.astype(jnp.int32)

        @pl.when(there)
        def _():
            pl.semaphore_signal(barrier, inc=1, device_id=device, device_id_type=MESH)

    for device in (mate, across):
        pl.semaphore_signal(barrier, inc=1, device_id={"rep": device}, device_id_type=MESH)
    pl.semaphore_wait(barrier, amount)

    late = []

    def send(there, src, dst, ssem, rsem, device):
        def describe():
            return pltpu.make_async_remote_copy(
                src_ref=src, dst_ref=dst, send_sem=ssem, recv_sem=rsem,
                device_id=device, device_id_type=MESH,
            )

        if there is None:
            describe().start()
            late.append((None, lambda: describe().wait_send()))
        else:
            @pl.when(there)
            def _():
                describe().start()

            late.append((there, lambda: describe().wait_send()))

    def arrive(place, rsem):
        pltpu.make_async_remote_copy(
            src_ref=place, dst_ref=place, send_sem=q_sem.at[0], recv_sem=rsem,
            device_id={"rep": mate}, device_id_type=MESH,
        ).wait_recv()

    def columns(ref, number, which):
        _, _, start, half = pieces[number]
        if half is None:
            return ref
        cols = pl.ds(pl.multiple_of(start + which * half, 128), half)
        return ref.at[:, :, :, cols] if len(ref.shape) == 4 else ref.at[:, cols]

    order = list(range(kinds))
    loads = []
    for number in order:
        src = columns(pieces[number][0], number, 1 - core)
        send(None, src, crecvs[number], c_send.at[number], c_recv.at[number], {"rep": mate})
        load = pltpu.make_async_copy(
            columns(pieces[number][0], number, core), mines[number], m_sem.at[number]
        )
        load.start()
        loads.append(load)

    for kind, (src, dst) in enumerate(((y_ref, ry_ref), (g_ref, rg_ref))):
        send(None, src, dst.at[rank], r_send.at[kind, 0], r_recv.at[kind, 0], {"rep": across})
        send(None, src, dst.at[rank], r_send.at[kind, 1], r_recv.at[kind, 1], {"rep": mate})
        pltpu.make_async_copy(src, dst.at[rank], q_sem.at[kind + 1]).start()

    def slot_of(way, size, place, dest):
        if size == 2:
            return 0
        return dest - place if way == 0 else size - place + dest

    def line_sum(number, size, place, stride, buffer, view, ssem, rsem):
        for far in range(size - 1, 0, -1):
            for way in range(2):
                dest = far if way == 0 else size - 1 - far
                step = 1 if way == 0 else -1
                passes = place < dest if way == 0 else place > dest
                first = place == 0 if way == 0 else place == size - 1
                mine = view(dest)
                got = slot_of(way, size, place, dest)

                @pl.when(jnp.logical_and(passes, jnp.logical_not(first)))
                def _():
                    arrive(buffer.at[got], rsem.at[got, number])
                    mine[...] = mine[...] + buffer[got]

                put = slot_of(way, size, place + step, dest)
                send(passes, mine, buffer.at[put], ssem.at[way, dest, number], rsem.at[put, number],
                     {"fsdp": spot + step * stride})
        for way in range(2):
            has = place > 0 if way == 0 else place < size - 1
            got = slot_of(way, size, place, place)
            mine = view(place)

            @pl.when(has)
            def _():
                arrive(buffer.at[got], rsem.at[got, number])
                mine[...] = mine[...] + buffer[got]

    for number in order:
        loads[number].wait()
        arrive(crecvs[number], c_recv.at[number])
        mine, other = mines[number], crecvs[number]

        def add(index, carry):
            mine[index // inner, index % inner] = (
                mine[index // inner, index % inner] + other[index // inner, index % inner]
            )
            return carry

        lax.fori_loop(0, outer * inner, add, 0)
        if inner == 2:
            send(None, mine.at[:, 1 - col], yrecvs[number].at[0], y_send.at[0, 0, number],
                 y_recv.at[0, number], {"fsdp": spot + 1 - 2 * col})
    for kind, dst in enumerate((ry_ref, rg_ref)):
        place = dst.at[across]
        arrive(place, r_recv.at[kind, 0])
        send(None, place, place, r_send.at[kind, 2], r_recv.at[kind, 2], {"rep": mate})
    for number in order:
        mine = mines[number]
        if inner == 2:
            arrive(yrecvs[number].at[0], y_recv.at[0, number])
            buffer = yrecvs[number]

            def add(index, carry):
                mine[index, col] = mine[index, col] + buffer[0, index]
                return carry

            lax.fori_loop(0, outer, add, 0)
        else:
            line_sum(number, inner, col, 1, yrecvs[number], lambda dest: mine.at[:, dest],
                     y_send, y_recv)
        line_sum(number, outer, row, inner, zrecvs[number], lambda dest: mine.at[dest, col],
                 z_send, z_recv)
        send(None, mine.at[row, col], xrecvs[number], x_send.at[number], x_recv.at[number],
             {"rep": across})
    for number in order:
        arrive(xrecvs[number], x_recv.at[number])
        total = mines[number][row, col].astype(jnp.float32) + xrecvs[number][...].astype(jnp.float32)
        out, half = pieces[number][1], pieces[number][3]
        place = columns(out, number, core)
        place[...] = total
        if half is not None:
            send(None, place, place, f_send.at[number], f_recv.at[number], {"rep": mate})
    for number in order:
        if pieces[number][3] is not None:
            arrive(columns(pieces[number][1], number, 1 - core), f_recv.at[number])
    for kind, dst in enumerate((ry_ref, rg_ref)):
        arrive(dst.at[mate], r_recv.at[kind, 1])
        arrive(dst.at[across_of(mate)], r_recv.at[kind, 2])
        src = y_ref if kind == 0 else g_ref
        pltpu.make_async_copy(src, dst.at[rank], q_sem.at[kind + 1]).wait()
    for there, finish_send in late:
        if there is None:
            finish_send()
        else:
            pl.when(there)(finish_send)


def reduce_grads(count, splits, ga, gb, gc, y_rows, g_rows):
    outer, inner = grid_of(count)
    kinds = len(splits) + 2
    rows_a, rows_b, rows_c = ga.shape[1], gb.shape[1], gc.shape[1]
    shapes = [(rows_a, width // 2, ga.dtype) for _, width in splits]
    shapes.append((rows_b, gb.shape[2] // 2, gb.dtype))
    shapes.append((rows_c, gc.shape[2], gc.dtype))
    dma = pltpu.SemaphoreType.DMA
    y_slots = 1 if inner == 2 else inner + 1
    z_slots = 1 if outer == 2 else outer + 1
    scratch = []
    for lead in ((outer, inner), (outer, inner), (y_slots, outer), (z_slots,), ()):
        scratch += [pltpu.VMEM(lead + (a, b), dtype) for a, b, dtype in shapes]
    scratch += [
        dma((kinds,)), dma((kinds,)), dma((kinds,)),
        dma((2, inner, kinds)), dma((y_slots, kinds)),
        dma((2, outer, kinds)), dma((z_slots, kinds)),
        dma((kinds,)), dma((kinds,)), dma((kinds,)), dma((kinds,)),
        dma((2, 3)), dma((2, 3)), dma((3,)),
    ]
    f32 = jnp.float32
    return pl.pallas_call(
        partial(reduce_kernel, outer, inner, splits),
        out_shape=(
            jax.ShapeDtypeStruct((rows_a, ga.shape[2]), f32),
            jax.ShapeDtypeStruct((rows_b, gb.shape[2]), f32),
            jax.ShapeDtypeStruct((rows_c, gc.shape[2]), f32),
            jax.ShapeDtypeStruct((4,) + y_rows.shape, y_rows.dtype),
            jax.ShapeDtypeStruct((4,) + g_rows.shape, g_rows.dtype),
        ),
        in_specs=[ANY] * 5,
        out_specs=(VMEM, VMEM, VMEM, ANY, ANY),
        scratch_shapes=scratch,
        compiler_params=pltpu.CompilerParams(
            collective_id=2, has_side_effects=True, vmem_limit_bytes=VMEM_LIMIT
        ),
        name="reduce_and_return",
    )(
        ga.reshape((outer, inner) + ga.shape[1:]),
        gb.reshape((outer, inner) + gb.shape[1:]),
        gc.reshape((outer, inner) + gc.shape[1:]),
        y_rows, g_rows,
    )


def home_kernel(tab_ref, ry_ref, rg_ref, y_ref, g_ref):
    base = lax.axis_index("rep") * y_ref.shape[0]

    def fetch(block, carry):
        index = tab_ref[DEST_AT + base + block]
        safe = jnp.maximum(index, 0)
        for src, dst in ((ry_ref, y_ref), (rg_ref, g_ref)):
            value = src[safe // SLOTS, safe % SLOTS]
            dst[block] = jnp.where(index >= 0, value, jnp.zeros_like(value))
        return carry

    lax.fori_loop(0, y_ref.shape[0], fetch, 0)


def bring_home(table, ry, rg, blocks):
    shape = jax.ShapeDtypeStruct((blocks,) + ry.shape[2:], ry.dtype)
    return pl.pallas_call(
        home_kernel,
        out_shape=(shape, shape),
        in_specs=[SMEM, VMEM, VMEM],
        out_specs=(VMEM, VMEM),
        compiler_params=pltpu.CompilerParams(vmem_limit_bytes=VMEM_LIMIT),
        name="place_rows",
    )(table, ry, rg)


def contract_rows(left_op, right_op):
    return lax.dot_general(
        left_op, right_op, (((0,), (0,)), ((), ())), preferred_element_type=jnp.float32
    )


def contract_cols(left_op, right_op):
    return lax.dot_general(
        left_op, right_op, (((1,), (1,)), ((), ())), preferred_element_type=jnp.float32
    )


def rms_norm(row_data, gain_vec):
    return (
        row_data
        * lax.rsqrt(jnp.mean(row_data * row_data, axis=-1, keepdims=True) + EPSILON)
        * gain_vec
    )


QB = 128
KPAD = 128


def band_table():
    query_pos = jnp.arange(QB, dtype=jnp.int32)[:, None] + KPAD
    key_pos = jnp.arange(QB + 2 * KPAD, dtype=jnp.int32)[None, :]
    return jnp.abs(query_pos - key_pos) <= RADIUS


def block_terms(row_start, queries, keys_pad, values_pad, global_keys, seg_query, seg_key_pad, seg_global):
    key_width = QB + 2 * KPAD
    query_blk = queries[row_start : row_start + QB].reshape(QB, H, DH)
    key_win = keys_pad[row_start : row_start + key_width]
    value_win = values_pad[row_start : row_start + key_width]
    local_scores = jnp.einsum("qhd,khd->hqk", query_blk, key_win, preferred_element_type=jnp.float32)
    global_scores = jnp.einsum("qhd,ghd->hqg", query_blk, global_keys, preferred_element_type=jnp.float32)
    seg_rows = seg_query[row_start : row_start + QB]
    allow_local = band_table() & (
        seg_rows[:, None] == seg_key_pad[row_start : row_start + key_width][None, :]
    )
    allow_global = seg_rows[:, None] == seg_global[None, :]
    masked_local = jnp.where(allow_local[None], local_scores, MASKED_SCORE)
    masked_global = jnp.where(allow_global[None], global_scores, MASKED_SCORE)
    return (query_blk, key_win, value_win, masked_local, masked_global)


def attend_forward(queries, keys_pad, values_pad, global_keys, global_values, seg_query, seg_key_pad, seg_global):
    mixed_blocks, kept = [], []
    for row_start in range(0, queries.shape[0], QB):
        query_blk, key_win, value_win, masked_local, masked_global = block_terms(
            row_start, queries, keys_pad, values_pad, global_keys, seg_query, seg_key_pad, seg_global
        )
        row_peak = jnp.maximum(
            jnp.max(masked_local, axis=-1, keepdims=True), jnp.max(masked_global, axis=-1, keepdims=True)
        )
        local_exp = jnp.exp(masked_local - row_peak)
        global_exp = jnp.exp(masked_global - row_peak)
        denominator = jnp.sum(local_exp, axis=-1, keepdims=True) + jnp.sum(global_exp, axis=-1, keepdims=True)
        local_low = (local_exp / denominator).astype(jnp.bfloat16)
        global_low = (global_exp / denominator).astype(jnp.bfloat16)
        mixed_rows = jnp.einsum("hqk,khd->qhd", local_low, value_win, preferred_element_type=jnp.float32)
        mixed_rows = mixed_rows + jnp.einsum(
            "hqg,ghd->qhd", global_low, global_values, preferred_element_type=jnp.float32
        )
        mixed_blocks.append(mixed_rows.reshape(QB, H * DH).astype(jnp.bfloat16))
        kept.append((row_peak, denominator))
    return (jnp.concatenate(mixed_blocks, axis=0), kept)


def attend_backward(grad_mixed, kept, queries, keys_pad, values_pad, global_keys, global_values, seg_query, seg_key_pad, seg_global):
    key_width = QB + 2 * KPAD
    row_count = queries.shape[0]
    grad_keys = jnp.zeros(keys_pad.shape, jnp.float32)
    grad_values = jnp.zeros(values_pad.shape, jnp.float32)
    grad_gkeys = jnp.zeros(global_keys.shape, jnp.float32)
    grad_gvalues = jnp.zeros(global_values.shape, jnp.float32)
    grad_query_blocks = []
    for number, row_start in enumerate(range(0, row_count, QB)):
        row_peak, denominator = kept[number]
        query_blk, key_win, value_win, masked_local, masked_global = block_terms(
            row_start, queries, keys_pad, values_pad, global_keys, seg_query, seg_key_pad, seg_global
        )
        local_probs = jnp.exp(masked_local - row_peak) / denominator
        global_probs = jnp.exp(masked_global - row_peak) / denominator
        grad_blk = grad_mixed[row_start : row_start + QB].reshape(QB, H, DH)
        local_dp = jnp.einsum("qhd,khd->hqk", grad_blk, value_win, preferred_element_type=jnp.float32)
        global_dp = jnp.einsum("qhd,ghd->hqg", grad_blk, global_values, preferred_element_type=jnp.float32)
        centre = jnp.sum(local_probs * local_dp, axis=-1, keepdims=True) + jnp.sum(
            global_probs * global_dp, axis=-1, keepdims=True
        )
        local_ds = (local_probs * (local_dp - centre)).astype(jnp.bfloat16)
        global_ds = (global_probs * (global_dp - centre)).astype(jnp.bfloat16)
        grad_query_rows = jnp.einsum("hqk,khd->qhd", local_ds, key_win, preferred_element_type=jnp.float32)
        grad_query_rows = grad_query_rows + jnp.einsum(
            "hqg,ghd->qhd", global_ds, global_keys, preferred_element_type=jnp.float32
        )
        grad_query_blocks.append(grad_query_rows.reshape(QB, H * DH).astype(jnp.bfloat16))
        grad_keys = grad_keys.at[row_start : row_start + key_width].add(
            jnp.einsum("hqk,qhd->khd", local_ds, query_blk, preferred_element_type=jnp.float32)
        )
        grad_values = grad_values.at[row_start : row_start + key_width].add(
            jnp.einsum("hqk,qhd->khd", local_probs.astype(jnp.bfloat16), grad_blk, preferred_element_type=jnp.float32)
        )
        grad_gkeys = grad_gkeys + jnp.einsum("hqg,qhd->ghd", global_ds, query_blk, preferred_element_type=jnp.float32)
        grad_gvalues = grad_gvalues + jnp.einsum(
            "hqg,qhd->ghd", global_probs.astype(jnp.bfloat16), grad_blk, preferred_element_type=jnp.float32
        )
    slot_count = global_keys.shape[0]
    grad_k = grad_keys[KPAD : KPAD + row_count].reshape(row_count, H * DH).astype(jnp.bfloat16)
    grad_v = grad_values[KPAD : KPAD + row_count].reshape(row_count, H * DH).astype(jnp.bfloat16)
    grad_gk = grad_gkeys.reshape(slot_count, H * DH).astype(jnp.bfloat16)
    grad_gv = grad_gvalues.reshape(slot_count, H * DH).astype(jnp.bfloat16)
    return (jnp.concatenate(grad_query_blocks, axis=0), grad_k, grad_v, grad_gk, grad_gv)


def layer_pass(row_data, cot_data, seg_tok, valid_tok, weights):
    (attn_gain, global_gain, query_weight, key_weight, value_weight, out_weight, ffn_gain,
     gate_weight, up_weight, down_weight) = weights
    row_count = row_data.shape[0]
    slot_count = row_count // GBLK
    valid_col = valid_tok.astype(jnp.float32)[:, None]
    inputs_f = row_data.astype(jnp.float32)
    gain_one = attn_gain.astype(jnp.float32)
    gain_side = global_gain.astype(jnp.float32)
    gain_two = ffn_gain.astype(jnp.float32)
    normed_f, norm_back_one = jax.vjp(rms_norm, inputs_f, gain_one)
    normed = normed_f.astype(jnp.bfloat16)
    side_sum = jnp.sum((normed.astype(jnp.float32) * valid_col).reshape(slot_count, GBLK, -1), axis=1)
    side_f, side_back = jax.vjp(rms_norm, side_sum, gain_side)
    side_normed = side_f.astype(jnp.bfloat16)

    def project(left, right):
        return jnp.dot(left, right, preferred_element_type=jnp.float32).astype(jnp.bfloat16)

    queries = project(normed, query_weight)
    keys_all = project(normed, key_weight)
    values_all = project(normed, value_weight)
    global_keys = project(side_normed, key_weight)
    global_values = project(side_normed, value_weight)
    seg_key = jnp.where(valid_tok, seg_tok, -2)
    seg_global = seg_key[::GBLK]
    keys_pad = jnp.pad(keys_all, ((KPAD, KPAD), (0, 0))).reshape(-1, H, DH)
    values_pad = jnp.pad(values_all, ((KPAD, KPAD), (0, 0))).reshape(-1, H, DH)
    seg_key_pad = jnp.pad(seg_key, (KPAD, KPAD), constant_values=-3)
    global_key_heads = global_keys.reshape(slot_count, H, DH)
    global_value_heads = global_values.reshape(slot_count, H, DH)
    attended, kept = attend_forward(
        queries, keys_pad, values_pad, global_key_heads, global_value_heads, seg_tok, seg_key_pad, seg_global
    )
    hidden_one = inputs_f + jnp.dot(attended, out_weight, preferred_element_type=jnp.float32)
    normed_two_f, norm_back_two = jax.vjp(rms_norm, hidden_one, gain_two)
    normed_two = normed_two_f.astype(jnp.bfloat16)
    gate_pre = jnp.dot(normed_two, gate_weight, preferred_element_type=jnp.float32)
    up_pre = jnp.dot(normed_two, up_weight, preferred_element_type=jnp.float32)
    activated, gelu_back = jax.vjp(partial(jax.nn.gelu, approximate=True), gate_pre)
    hidden_two = (activated * up_pre).astype(jnp.bfloat16)
    result = (
        valid_col * (hidden_one + jnp.dot(hidden_two, down_weight, preferred_element_type=jnp.float32))
    ).astype(jnp.bfloat16)
    grad_res = cot_data.astype(jnp.float32) * valid_col
    grad_out = grad_res.astype(jnp.bfloat16)
    grad_hidden = contract_cols(grad_out, down_weight)
    grad_down = contract_rows(hidden_two, grad_out)
    grad_gate = gelu_back(grad_hidden * up_pre)[0].astype(jnp.bfloat16)
    grad_up = (grad_hidden * activated).astype(jnp.bfloat16)
    grad_gate_w = contract_rows(normed_two, grad_gate)
    grad_up_w = contract_rows(normed_two, grad_up)
    grad_normed_two = contract_cols(grad_gate, gate_weight) + contract_cols(grad_up, up_weight)
    grad_norm_part, grad_gain_two = norm_back_two(grad_normed_two)
    grad_hidden_one = grad_res + grad_norm_part
    grad_branch = grad_hidden_one.astype(jnp.bfloat16)
    grad_out_w = contract_rows(attended, grad_branch)
    grad_attended = contract_cols(grad_branch, out_weight).astype(jnp.bfloat16)
    grad_q, grad_k, grad_v, grad_gk, grad_gv = attend_backward(
        grad_attended, kept, queries, keys_pad, values_pad, global_key_heads, global_value_heads,
        seg_tok, seg_key_pad, seg_global,
    )
    grad_query_w = contract_rows(normed, grad_q)
    grad_key_w = contract_rows(normed, grad_k) + contract_rows(side_normed, grad_gk)
    grad_value_w = contract_rows(normed, grad_v) + contract_rows(side_normed, grad_gv)
    grad_normed = (
        contract_cols(grad_q, query_weight) + contract_cols(grad_k, key_weight) + contract_cols(grad_v, value_weight)
    )
    grad_side_normed = contract_cols(grad_gk, key_weight) + contract_cols(grad_gv, value_weight)
    grad_side, grad_gain_side = side_back(grad_side_normed)
    spread_side = grad_side[:, None, :] * valid_col.reshape(slot_count, GBLK, 1)
    grad_normed = grad_normed + spread_side.reshape(row_count, -1)
    grad_inputs, grad_gain_one = norm_back_one(grad_normed)
    grad_rows = (grad_inputs + grad_hidden_one).astype(jnp.bfloat16)
    grads = (grad_gain_one, grad_gain_side, grad_query_w, grad_key_w, grad_value_w, grad_out_w,
             grad_gain_two, grad_gate_w, grad_up_w, grad_down)
    return (result, grad_rows, grads)


def per_device(count, layer_input, cotangent, lengths, attn_gain, global_gain, query_weight, key_weight,
               value_weight, out_weight, ffn_gain, gate_weight, up_weight, down_weight):
    micro, span, width = layer_input.shape
    hidden = gate_weight.shape[1]
    blocks = micro * span // BLK
    rank = lax.axis_index("rep")
    table = deal_table(lengths)
    wa = jnp.concatenate([query_weight, key_weight, value_weight, out_weight, gate_weight, up_weight], axis=1)
    part = attn_gain.shape[0]
    wc = jnp.pad(jnp.stack([attn_gain, global_gain, ffn_gain]), ((0, 13), (0, 128 - part)))
    splits = ((0, 4 * width), (4 * width, 2 * hidden))
    ga, gb, gc, rows, cots = gather_weights(
        count, splits, table,
        layer_input.reshape(blocks, BLK, width), cotangent.reshape(blocks, BLK, width), wa, down_weight, wc,
    )
    full = ga.reshape(width, -1)
    gains = jnp.transpose(gc[:, :3, :part], (1, 0, 2)).reshape(3, width)
    own = lax.dynamic_slice_in_dim(table, SEG_AT + rank * SLOTS, SLOTS)
    lens = lax.dynamic_slice_in_dim(table, LEN_AT + rank * SLOTS, SLOTS)
    seg_tok = jnp.repeat(own, BLK)
    valid_tok = (jnp.arange(BLK, dtype=jnp.int32)[None, :] < lens[:, None]).reshape(-1)
    heads = 4 * width
    weights = (
        gains[0], gains[1], full[:, :width], full[:, width : 2 * width], full[:, 2 * width : 3 * width],
        full[:, 3 * width : heads], gains[2], full[:, heads : heads + hidden],
        full[:, heads + hidden :], gb.reshape(-1, width),
    )
    result, grad_rows, grads = layer_pass(
        rows.reshape(-1, width), cots.reshape(-1, width), seg_tok, valid_tok, weights
    )
    grad_a = jnp.concatenate(
        [grads[2], grads[3], grads[4], grads[5], grads[7], grads[8]], axis=1
    ).astype(jnp.bfloat16).reshape(ga.shape)
    grad_b = grads[9].astype(jnp.bfloat16).reshape(gb.shape)
    grad_c = jnp.transpose(jnp.stack([grads[0], grads[1], grads[6]]).reshape(3, count, part), (1, 0, 2))
    grad_c = jnp.pad(grad_c, ((0, 0), (0, 5), (0, 128 - part)))
    oa, ob, oc, ry, rg = reduce_grads(
        count, splits, grad_a, grad_b, grad_c, result.reshape(SLOTS, BLK, width), grad_rows.reshape(SLOTS, BLK, width)
    )
    y_home, g_home = bring_home(table, ry, rg, blocks)
    return (
        y_home.reshape(layer_input.shape), g_home.reshape(layer_input.shape),
        oc[0, :part], oc[1, :part],
        oa[:, :width], oa[:, width : 2 * width], oa[:, 2 * width : 3 * width], oa[:, 3 * width : heads],
        oc[2, :part], oa[:, heads : heads + hidden], oa[:, heads + hidden :], ob,
    )


def solution(mesh):
    rows = P(None, ("rep", "fsdp"), None)
    vector, matrix = P("fsdp"), P("fsdp", None)
    return jax.shard_map(
        partial(per_device, mesh.shape["fsdp"]),
        mesh=mesh,
        in_specs=(rows, rows, P(None, ("rep", "fsdp")), vector, vector, matrix, matrix, matrix, matrix,
                  vector, matrix, matrix, matrix),
        out_specs=(rows, rows, vector, vector, matrix, matrix, matrix, matrix, vector, matrix, matrix, matrix),
        check_vma=False,
    )
```

```python
from functools import partial

import jax
import jax.numpy as jnp
from jax import lax
from jax.experimental import pallas as pl
from jax.experimental.pallas import tpu as pltpu
from jax.sharding import PartitionSpec as P

H = 12
DH = 64
RADIUS = 127
GBLK = 16
BLK = 64
SLOTS = 10
MAX_SEQ_BLOCKS = 5
EPSILON = 1e-06
MASKED_SCORE = -1e30
MESH = pl.DeviceIdType.MESH
VMEM_LIMIT = 60 * 1024 * 1024
SEG_AT, LEN_AT, DEST_AT, TABLE_SIZE = 40, 80, 120, 256

ANY = pl.BlockSpec(memory_space=pl.ANY)
VMEM = pl.BlockSpec(memory_space=pltpu.VMEM)
SMEM = pl.BlockSpec(memory_space=pltpu.SMEM)


def grid_of(count):
    inner = 2 if count <= 8 else 4
    return count // inner, inner


def core_of(rank):
    return rank + 1 - 2 * (rank % 2)


def across_of(rank):
    return (rank + 2) % 4


def lens_kernel(lens_ref, all_ref, send_sem, recv_sem):
    rank = lax.axis_index("rep")
    barrier = pltpu.get_barrier_semaphore()
    for step in range(1, 4):
        pl.semaphore_signal(
            barrier, inc=1, device_id={"rep": (rank + step) % 4}, device_id_type=MESH
        )
    pl.semaphore_wait(barrier, 3)
    copies = []
    for step in range(1, 4):
        copy = pltpu.make_async_remote_copy(
            src_ref=lens_ref,
            dst_ref=all_ref.at[rank],
            send_sem=send_sem.at[step - 1],
            recv_sem=recv_sem.at[step - 1],
            device_id={"rep": (rank + step) % 4},
            device_id_type=MESH,
        )
        copy.start()
        copies.append(copy)
    all_ref[rank] = lens_ref[...]
    for copy in copies:
        copy.wait()


def table_kernel(micro, per_dev, lens_ref, tab_ref, order_ref, count_ref, load_ref):
    total = 4 * micro * per_dev

    def length_at(spot):
        return lens_ref[spot // (micro * per_dev), (spot // per_dev) % micro, spot % per_dev]

    def blocks_of(length):
        return (length + (BLK - 1)) // BLK

    def clear(spot, carry):
        tab_ref[spot] = -1
        return carry

    lax.fori_loop(0, TABLE_SIZE, clear, 0)
    for spot in range(4 * SLOTS):
        tab_ref[LEN_AT + spot] = 0
    for size in range(8):
        count_ref[size] = 0
    for dev in range(4):
        load_ref[dev] = 0

    def tally(spot, carry):
        length = length_at(spot)

        @pl.when(length > 0)
        def _():
            size = blocks_of(length)
            count_ref[size] = count_ref[size] + 1

        return carry

    lax.fori_loop(0, total, tally, 0)
    begin = 0
    for size in range(MAX_SEQ_BLOCKS, 0, -1):
        amount = count_ref[size]
        count_ref[size] = begin
        begin = begin + amount

    def place(spot, carry):
        length = length_at(spot)

        @pl.when(length > 0)
        def _():
            size = blocks_of(length)
            where = count_ref[size]
            order_ref[where] = spot
            count_ref[size] = where + 1

        return carry

    lax.fori_loop(0, total, place, 0)

    def assign(number, carry):
        spot = order_ref[number]
        length = length_at(spot)
        size = blocks_of(length)
        best = jnp.int32(0)
        low = load_ref[0]
        for dev in range(1, 4):
            here = load_ref[dev]
            best = jnp.where(here < low, dev, best)
            low = jnp.minimum(here, low)
        load_ref[best] = low + size

        def put(step, inner):
            slot = best * SLOTS + low + step
            tab_ref[slot] = spot + step
            tab_ref[SEG_AT + slot] = low
            tab_ref[LEN_AT + slot] = jnp.minimum(length - BLK * step, BLK)
            tab_ref[DEST_AT + spot + step] = slot
            return inner

        lax.fori_loop(0, size, put, 0)
        return carry

    lax.fori_loop(0, begin, assign, 0)


def deal_table(lengths):
    micro, per_dev = lengths.shape
    padded = jnp.pad(lengths, ((0, 8 - micro), (0, 128 - per_dev)))
    everyone = pl.pallas_call(
        lens_kernel,
        out_shape=jax.ShapeDtypeStruct((4, 8, 128), jnp.int32),
        in_specs=[VMEM],
        out_specs=VMEM,
        scratch_shapes=[pltpu.SemaphoreType.DMA((3,)), pltpu.SemaphoreType.DMA((3,))],
        compiler_params=pltpu.CompilerParams(collective_id=0, has_side_effects=True),
        name="lens_exchange",
    )(padded)
    return pl.pallas_call(
        partial(table_kernel, micro, per_dev),
        out_shape=jax.ShapeDtypeStruct((TABLE_SIZE,), jnp.int32),
        in_specs=[SMEM],
        out_specs=SMEM,
        scratch_shapes=[
            pltpu.SMEM((4 * micro * per_dev,), jnp.int32),
            pltpu.SMEM((8,), jnp.int32),
            pltpu.SMEM((4,), jnp.int32),
        ],
        name="deal_table",
    )(everyone)


def gather_kernel(
    outer, inner, splits, tab_ref, rows_ref, cots_ref, wa_ref, wb_ref, wc_ref,
    ga_ref, gb_ref, gc_ref, rows_out, cots_out,
    psend, precv, xsend, xrecv,
    z_send, z_recv, y_send, y_recv, c_send, c_recv, own_sem,
    p_send, p_recv, x_send, x_recv,
):
    rank = lax.axis_index("rep")
    spot = lax.axis_index("fsdp")
    core = rank % 2
    row, col = spot // inner, spot % inner
    count = outer * inner
    mate, across = core_of(rank), across_of(rank)
    pieces = [(wa_ref, ga_ref, start, width // 2) for start, width in splits]
    pieces.append((wb_ref, gb_ref, 0, wb_ref.shape[1] // 2))
    pieces.append((wc_ref, gc_ref, 0, None))
    halved = [number for number, piece in enumerate(pieces) if piece[3] is not None]

    barrier = pltpu.get_barrier_semaphore()
    neighbours = (
        (row + 1 < outer, {"fsdp": spot + inner}),
        (row > 0, {"fsdp": spot - inner}),
        (col + 1 < inner, {"fsdp": spot + 1}),
        (col > 0, {"fsdp": spot - 1}),
    )
    amount = jnp.int32(2)
    for there, device in neighbours:
        amount = amount + there.astype(jnp.int32)

        @pl.when(there)
        def _():
            pl.semaphore_signal(barrier, inc=1, device_id=device, device_id_type=MESH)

    for device in (mate, across):
        pl.semaphore_signal(barrier, inc=1, device_id={"rep": device}, device_id_type=MESH)
    pl.semaphore_wait(barrier, amount)

    def cut(ref, number):
        _, _, start, half = pieces[number]
        if half is None:
            return ref
        return ref.at[:, pl.ds(pl.multiple_of(start + core * half, 128), half)]

    def landed(number, shard):
        return cut(pieces[number][1].at[shard], number)

    late = []

    def send(there, src, dst, ssem, rsem, device):
        def describe():
            return pltpu.make_async_remote_copy(
                src_ref=src, dst_ref=dst, send_sem=ssem, recv_sem=rsem,
                device_id=device, device_id_type=MESH,
            )

        if there is None:
            describe().start()
            late.append((None, lambda: describe().wait_send()))
        else:
            @pl.when(there)
            def _():
                describe().start()

            late.append((there, lambda: describe().wait_send()))

    def arrive(number, shard, rsem):
        pltpu.make_async_remote_copy(
            src_ref=landed(number, shard), dst_ref=landed(number, shard),
            send_sem=own_sem.at[0], recv_sem=rsem,
            device_id={"rep": mate}, device_id_type=MESH,
        ).wait_recv()

    def both(first, second):
        return second if first is None else jnp.logical_and(first, second)

    def to_mate(there, number, shard):
        if number not in halved:
            return
        place = landed(number, shard)
        send(there, place, place, c_send.at[number, shard], c_recv.at[number, shard], {"rep": mate})

    def along_row(there, number, line, src):
        shard = line * inner + col
        place = landed(number, shard)
        src = place if src is None else src
        send(both(there, col + 1 < inner), src, place,
             y_send.at[0, 0, line, number], y_recv.at[0, 0, line, number], {"fsdp": spot + 1})
        send(both(there, col > 0), src, place,
             y_send.at[1, 0, line, number], y_recv.at[1, 0, line, number], {"fsdp": spot - 1})

    def from_row(there, number, line):
        for step in range(inner - 1):
            for way, source, onward, target in (
                (0, col - 1 - step, col + 1 < inner, spot + 1),
                (1, col + 1 + step, col > 0, spot - 1),
            ):
                here = jnp.logical_and(source >= 0, source < inner)
                here = both(there, here)
                shard = line * inner + source

                @pl.when(here)
                def _():
                    arrive(number, shard, y_recv.at[way, step, line, number])

                if step + 1 < inner - 1:
                    place = landed(number, shard)
                    send(both(here, onward), place, place,
                         y_send.at[way, step + 1, line, number],
                         y_recv.at[way, step + 1, line, number], {"fsdp": target})
                to_mate(here, number, shard)

    for number, piece in enumerate(pieces):
        src, place = cut(piece[0], number), landed(number, spot)
        send(row + 1 < outer, src, place, z_send.at[0, 0, number], z_recv.at[0, 0, number],
             {"fsdp": spot + inner})
        send(row > 0, src, place, z_send.at[1, 0, number], z_recv.at[1, 0, number],
             {"fsdp": spot - inner})
        along_row(None, number, row, src)
    own = [
        pltpu.make_async_copy(wa_ref, ga_ref.at[spot], own_sem.at[0]),
        pltpu.make_async_copy(wb_ref, gb_ref.at[spot], own_sem.at[1]),
        pltpu.make_async_copy(wc_ref, gc_ref.at[spot], own_sem.at[2]),
    ]
    for copy in own:
        copy.start()

    sources = (rows_ref, cots_ref)
    per_rank = rows_ref.shape[0]

    def picked(kind, target, slot):
        index = tab_ref[target * SLOTS + slot] - rank * per_rank
        mine = jnp.logical_and(index >= 0, index < per_rank)
        value = sources[kind][jnp.clip(index, 0, per_rank - 1)]
        return mine, value

    def mate_copy(kind, part):
        return pltpu.make_async_remote_copy(
            src_ref=psend.at[kind, part], dst_ref=precv.at[kind, part],
            send_sem=p_send.at[kind, part], recv_sem=p_recv.at[kind, part],
            device_id={"rep": mate}, device_id_type=MESH,
        )

    def across_copy(kind):
        return pltpu.make_async_remote_copy(
            src_ref=xsend.at[kind], dst_ref=xrecv.at[kind],
            send_sem=x_send.at[kind], recv_sem=x_recv.at[kind],
            device_id={"rep": across}, device_id_type=MESH,
        )

    for kind, part in ((0, 1), (1, 1), (0, 0), (1, 0)):
        target = mate if part == 0 else across_of(mate)

        def pack(slot, carry):
            mine, value = picked(kind, target, slot)
            psend[kind, part, slot] = jnp.where(mine, value, jnp.zeros_like(value))
            return carry

        lax.fori_loop(0, SLOTS, pack, 0)
        mate_copy(kind, part).start()
    for kind in range(2):
        mate_copy(kind, 1).wait_recv()

        def merge(slot, carry):
            mine, value = picked(kind, across, slot)
            xsend[kind, slot] = jnp.where(mine, value, precv[kind, 1, slot])
            return carry

        lax.fori_loop(0, SLOTS, merge, 0)
        across_copy(kind).start()

    def lines(step):
        return ((row - 1 - step >= 0, row - 1 - step, 0, row + 1 < outer, spot + inner),
                (row + 1 + step < outer, row + 1 + step, 1, row > 0, spot - inner))

    for step in range(outer - 1):
        for number in range(len(pieces)):
            for here, line, way, onward, target in lines(step):
                shard = line * inner + col

                @pl.when(here)
                def _():
                    arrive(number, shard, z_recv.at[way, step, number])

                if step + 1 < outer - 1:
                    place = landed(number, shard)
                    send(jnp.logical_and(here, onward), place, place,
                         z_send.at[way, step + 1, number], z_recv.at[way, step + 1, number],
                         {"fsdp": target})
                along_row(here, number, line, None)
                to_mate(here, number, shard)
        for number in range(len(pieces)):
            if step == 0:
                from_row(None, number, row)
            else:
                for here, line, *_ in lines(step - 1):
                    from_row(here, number, line)
    for number in range(len(pieces)):
        for here, line, *_ in lines(outer - 2):
            from_row(here, number, line)

    outs = (rows_out, cots_out)
    for kind in range(2):
        mate_copy(kind, 0).wait_recv()
        across_copy(kind).wait_recv()

        def finish(slot, carry):
            mine, value = picked(kind, rank, slot)
            outs[kind][slot] = jnp.where(mine, value, precv[kind, 0, slot] + xrecv[kind, slot])
            return carry

        lax.fori_loop(0, SLOTS, finish, 0)

    for shard in range(count):
        @pl.when(shard != spot)
        def _():
            for number in halved:
                other = pieces[number]
                view = other[1].at[shard].at[:, pl.ds(0, other[3])]
                pltpu.make_async_remote_copy(
                    src_ref=view, dst_ref=view, send_sem=own_sem.at[0],
                    recv_sem=c_recv.at[number, shard],
                    device_id={"rep": mate}, device_id_type=MESH,
                ).wait_recv()
    for there, finish_send in late:
        if there is None:
            finish_send()
        else:
            pl.when(there)(finish_send)
    for kind in range(2):
        for part in range(2):
            mate_copy(kind, part).wait_send()
        across_copy(kind).wait_send()
    for copy in own:
        copy.wait()


def gather_weights(count, splits, table, rows, cots, wa, wb, wc):
    outer, inner = grid_of(count)
    block = rows.shape[1:]
    kinds = len(splits) + 2
    dma = pltpu.SemaphoreType.DMA
    bf16 = jnp.bfloat16
    return pl.pallas_call(
        partial(gather_kernel, outer, inner, splits),
        out_shape=(
            jax.ShapeDtypeStruct((count,) + wa.shape, bf16),
            jax.ShapeDtypeStruct((count,) + wb.shape, bf16),
            jax.ShapeDtypeStruct((count,) + wc.shape, bf16),
            jax.ShapeDtypeStruct((SLOTS,) + block, bf16),
            jax.ShapeDtypeStruct((SLOTS,) + block, bf16),
        ),
        in_specs=[SMEM, VMEM, VMEM, VMEM, VMEM, VMEM],
        out_specs=(ANY, ANY, ANY, VMEM, VMEM),
        scratch_shapes=[
            pltpu.VMEM((2, 2, SLOTS) + block, bf16),
            pltpu.VMEM((2, 2, SLOTS) + block, bf16),
            pltpu.VMEM((2, SLOTS) + block, bf16),
            pltpu.VMEM((2, SLOTS) + block, bf16),
            dma((2, outer - 1, kinds)), dma((2, outer - 1, kinds)),
            dma((2, inner - 1, outer, kinds)), dma((2, inner - 1, outer, kinds)),
            dma((kinds, count)), dma((kinds, count)), dma((3,)),
            dma((2, 2)), dma((2, 2)), dma((2,)), dma((2,)),
        ],
        compiler_params=pltpu.CompilerParams(
            collective_id=1, has_side_effects=True, vmem_limit_bytes=VMEM_LIMIT
        ),
        name="gather_and_deal",
    )(table, rows, cots, wa, wb, wc)


def reduce_kernel(
    outer, inner, kinds, *refs
):
    grads, (y_ref, g_ref) = refs[:kinds], refs[kinds : kinds + 2]
    totals, (ry_ref, rg_ref) = refs[kinds + 2 : 2 * kinds + 2], refs[2 * kinds + 2 : 2 * kinds + 4]
    scratch = refs[2 * kinds + 4 :]
    mines, crecvs, yrecvs, zrecvs, xrecvs = (
        scratch[kinds * i : kinds * (i + 1)] for i in range(5)
    )
    (c_send, c_recv, m_sem, y_send, y_recv, z_send, z_recv, x_send, x_recv, f_send, f_recv,
     r_send, r_recv, q_sem) = scratch[5 * kinds :]
    rank = lax.axis_index("rep")
    spot = lax.axis_index("fsdp")
    core = rank % 2
    row, col = spot // inner, spot % inner
    mate, across = core_of(rank), across_of(rank)
    pieces = [(src, dst, 0, src.shape[3] // 2) for src, dst in zip(grads[:-1], totals)]
    pieces.append((grads[-1], totals[-1], 0, None))

    barrier = pltpu.get_barrier_semaphore()
    neighbours = (
        (row + 1 < outer, {"fsdp": spot + inner}),
        (row > 0, {"fsdp": spot - inner}),
        (col + 1 < inner, {"fsdp": spot + 1}),
        (col > 0, {"fsdp": spot - 1}),
    )
    amount = jnp.int32(2)
    for there, device in neighbours:
        amount = amount + there.astype(jnp.int32)

        @pl.when(there)
        def _():
            pl.semaphore_signal(barrier, inc=1, device_id=device, device_id_type=MESH)

    for device in (mate, across):
        pl.semaphore_signal(barrier, inc=1, device_id={"rep": device}, device_id_type=MESH)
    pl.semaphore_wait(barrier, amount)

    late = []

    def send(there, src, dst, ssem, rsem, device):
        def describe():
            return pltpu.make_async_remote_copy(
                src_ref=src, dst_ref=dst, send_sem=ssem, recv_sem=rsem,
                device_id=device, device_id_type=MESH,
            )

        if there is None:
            describe().start()
            late.append((None, lambda: describe().wait_send()))
        else:
            @pl.when(there)
            def _():
                describe().start()

            late.append((there, lambda: describe().wait_send()))

    def arrive(place, rsem):
        pltpu.make_async_remote_copy(
            src_ref=place, dst_ref=place, send_sem=q_sem.at[0], recv_sem=rsem,
            device_id={"rep": mate}, device_id_type=MESH,
        ).wait_recv()

    def columns(ref, number, which):
        _, _, start, half = pieces[number]
        if half is None:
            return ref
        cols = pl.ds(pl.multiple_of(start + which * half, 128), half)
        return ref.at[:, :, :, cols] if len(ref.shape) == 4 else ref.at[:, cols]

    order = list(range(kinds))
    loads = []
    for number in order:
        src = columns(pieces[number][0], number, 1 - core)
        send(None, src, crecvs[number], c_send.at[number], c_recv.at[number], {"rep": mate})
        load = pltpu.make_async_copy(
            columns(pieces[number][0], number, core), mines[number], m_sem.at[number]
        )
        load.start()
        loads.append(load)

    for kind, (src, dst) in enumerate(((y_ref, ry_ref), (g_ref, rg_ref))):
        send(None, src, dst.at[rank], r_send.at[kind, 0], r_recv.at[kind, 0], {"rep": across})
        send(None, src, dst.at[rank], r_send.at[kind, 1], r_recv.at[kind, 1], {"rep": mate})
        pltpu.make_async_copy(src, dst.at[rank], q_sem.at[kind + 1]).start()

    def slot_of(way, size, place, dest):
        if size == 2:
            return 0
        return dest - place if way == 0 else size - place + dest

    def line_sum(number, size, place, stride, buffer, view, ssem, rsem):
        for far in range(size - 1, 0, -1):
            for way in range(2):
                dest = far if way == 0 else size - 1 - far
                step = 1 if way == 0 else -1
                passes = place < dest if way == 0 else place > dest
                first = place == 0 if way == 0 else place == size - 1
                mine = view(dest)
                got = slot_of(way, size, place, dest)

                @pl.when(jnp.logical_and(passes, jnp.logical_not(first)))
                def _():
                    arrive(buffer.at[got], rsem.at[got, number])
                    mine[...] = mine[...] + buffer[got]

                put = slot_of(way, size, place + step, dest)
                send(passes, mine, buffer.at[put], ssem.at[way, dest, number], rsem.at[put, number],
                     {"fsdp": spot + step * stride})
        for way in range(2):
            has = place > 0 if way == 0 else place < size - 1
            got = slot_of(way, size, place, place)
            mine = view(place)

            @pl.when(has)
            def _():
                arrive(buffer.at[got], rsem.at[got, number])
                mine[...] = mine[...] + buffer[got]

    for number in order:
        loads[number].wait()
        arrive(crecvs[number], c_recv.at[number])
        mine, other = mines[number], crecvs[number]

        def add(index, carry):
            mine[index // inner, index % inner] = (
                mine[index // inner, index % inner] + other[index // inner, index % inner]
            )
            return carry

        lax.fori_loop(0, outer * inner, add, 0)
        if inner == 2:
            send(None, mine.at[:, 1 - col], yrecvs[number].at[0], y_send.at[0, 0, number],
                 y_recv.at[0, number], {"fsdp": spot + 1 - 2 * col})
    for kind, dst in enumerate((ry_ref, rg_ref)):
        place = dst.at[across]
        arrive(place, r_recv.at[kind, 0])
        send(None, place, place, r_send.at[kind, 2], r_recv.at[kind, 2], {"rep": mate})
    for number in order:
        mine = mines[number]
        if inner == 2:
            arrive(yrecvs[number].at[0], y_recv.at[0, number])
            buffer = yrecvs[number]

            def add(index, carry):
                mine[index, col] = mine[index, col] + buffer[0, index]
                return carry

            lax.fori_loop(0, outer, add, 0)
        else:
            line_sum(number, inner, col, 1, yrecvs[number], lambda dest: mine.at[:, dest],
                     y_send, y_recv)
        line_sum(number, outer, row, inner, zrecvs[number], lambda dest: mine.at[dest, col],
                 z_send, z_recv)
        send(None, mine.at[row, col], xrecvs[number], x_send.at[number], x_recv.at[number],
             {"rep": across})
    for number in order:
        arrive(xrecvs[number], x_recv.at[number])
        total = mines[number][row, col].astype(jnp.float32) + xrecvs[number][...].astype(jnp.float32)
        out, half = pieces[number][1], pieces[number][3]
        place = columns(out, number, core)
        place[...] = total
        if half is not None:
            send(None, place, place, f_send.at[number], f_recv.at[number], {"rep": mate})
    for number in order:
        if pieces[number][3] is not None:
            arrive(columns(pieces[number][1], number, 1 - core), f_recv.at[number])
    for kind, dst in enumerate((ry_ref, rg_ref)):
        arrive(dst.at[mate], r_recv.at[kind, 1])
        arrive(dst.at[across_of(mate)], r_recv.at[kind, 2])
        src = y_ref if kind == 0 else g_ref
        pltpu.make_async_copy(src, dst.at[rank], q_sem.at[kind + 1]).wait()
    for there, finish_send in late:
        if there is None:
            finish_send()
        else:
            pl.when(there)(finish_send)


def reduce_grads(count, grads, y_rows, g_rows):
    outer, inner = grid_of(count)
    kinds = len(grads)
    shapes = [(grad.shape[1], grad.shape[2] // 2, grad.dtype) for grad in grads[:-1]]
    shapes.append(grads[-1].shape[1:] + (grads[-1].dtype,))
    dma = pltpu.SemaphoreType.DMA
    y_slots = 1 if inner == 2 else inner + 1
    z_slots = 1 if outer == 2 else outer + 1
    scratch = []
    for lead in ((outer, inner), (outer, inner), (y_slots, outer), (z_slots,), ()):
        scratch += [pltpu.VMEM(lead + (a, b), dtype) for a, b, dtype in shapes]
    scratch += [
        dma((kinds,)), dma((kinds,)), dma((kinds,)),
        dma((2, inner, kinds)), dma((y_slots, kinds)),
        dma((2, outer, kinds)), dma((z_slots, kinds)),
        dma((kinds,)), dma((kinds,)), dma((kinds,)), dma((kinds,)),
        dma((2, 3)), dma((2, 3)), dma((3,)),
    ]
    return pl.pallas_call(
        partial(reduce_kernel, outer, inner, kinds),
        out_shape=tuple(jax.ShapeDtypeStruct(grad.shape[1:], jnp.float32) for grad in grads) + (
            jax.ShapeDtypeStruct((4,) + y_rows.shape, y_rows.dtype),
            jax.ShapeDtypeStruct((4,) + g_rows.shape, g_rows.dtype),
        ),
        in_specs=[ANY] * (kinds + 2),
        out_specs=(VMEM,) * kinds + (ANY, ANY),
        scratch_shapes=scratch,
        compiler_params=pltpu.CompilerParams(
            collective_id=2, has_side_effects=True, vmem_limit_bytes=VMEM_LIMIT
        ),
        name="reduce_and_return",
    )(*(grad.reshape((outer, inner) + grad.shape[1:]) for grad in grads), y_rows, g_rows)


def home_kernel(tab_ref, ry_ref, rg_ref, y_ref, g_ref):
    base = lax.axis_index("rep") * y_ref.shape[0]

    def fetch(block, carry):
        index = tab_ref[DEST_AT + base + block]
        safe = jnp.maximum(index, 0)
        for src, dst in ((ry_ref, y_ref), (rg_ref, g_ref)):
            value = src[safe // SLOTS, safe % SLOTS]
            dst[block] = jnp.where(index >= 0, value, jnp.zeros_like(value))
        return carry

    lax.fori_loop(0, y_ref.shape[0], fetch, 0)


def bring_home(table, ry, rg, blocks):
    shape = jax.ShapeDtypeStruct((blocks,) + ry.shape[2:], ry.dtype)
    return pl.pallas_call(
        home_kernel,
        out_shape=(shape, shape),
        in_specs=[SMEM, VMEM, VMEM],
        out_specs=(VMEM, VMEM),
        compiler_params=pltpu.CompilerParams(vmem_limit_bytes=VMEM_LIMIT),
        name="place_rows",
    )(table, ry, rg)


D = H * DH
ROWS = SLOTS * BLK
SIDES = SLOTS * (BLK // GBLK)
SIDE_ROWS = 48
ALL_ROWS = ROWS + SIDE_ROWS
QT = 128
WIN = 384
TILES = ROWS // QT
QUAD = 256
FF_TILE = 256
GELU_C = 0.7978845608028654
GELU_A = 0.044715
F32, BF16 = jnp.float32, jnp.bfloat16


def mm(left, right):
    return lax.dot_general(left, right, (((1,), (0,)), ((), ())), preferred_element_type=F32)


def mm_cols(left, right):
    return lax.dot_general(left, right, (((1,), (1,)), ((), ())), preferred_element_type=F32)


def mm_rows(left, right):
    return lax.dot_general(left, right, (((0,), (0,)), ((), ())), preferred_element_type=F32)


def iota(shape, axis):
    return lax.broadcasted_iota(jnp.int32, shape, axis)


def pick_by(index, values, other):
    out = jnp.full(index.shape, other, jnp.int32)
    for number, value in enumerate(values):
        out = jnp.where(index == number, value, out)
    return out


def slot_info(tab_ref, rank):
    seg = [tab_ref[SEG_AT + rank * SLOTS + slot] for slot in range(SLOTS)]
    length = [tab_ref[LEN_AT + rank * SLOTS + slot] for slot in range(SLOTS)]
    return seg, length


def valid_column(tab_ref, rank):
    _, length = slot_info(tab_ref, rank)
    row = iota((ROWS, 1), 0)
    return ((row % BLK) < pick_by(row // BLK, length, 0)).astype(F32)


def pooling(tab_ref, rank):
    _, length = slot_info(tab_ref, rank)
    row = iota((1, ROWS), 1)
    block = jnp.where((row % BLK) < pick_by(row // BLK, length, 0), row // GBLK, -1)
    return jnp.where(iota((SIDE_ROWS, ROWS), 0) == block, 1.0, 0.0).astype(BF16)


def key_segments(tab_ref, rank, first_block, index):
    blocks = WIN // BLK
    base = rank * SLOTS + first_block
    seg = [tab_ref[SEG_AT + base + step] for step in range(blocks)]
    length = [tab_ref[LEN_AT + base + step] for step in range(blocks)]
    alive = (index % BLK) < pick_by(index // BLK, length, 0)
    return jnp.where(alive, pick_by(index // BLK, seg, -2), -2)


def side_segments(tab_ref, rank, index):
    seg, length = slot_info(tab_ref, rank)
    per = BLK // GBLK
    alive = (index % per) * GBLK < pick_by(index // per, length, 0)
    return jnp.where(alive, pick_by(index // per, seg, -2), -2)


def tile_bias(tab_ref, rank, tile, first_row, keys_axis):
    qs, ks, gs = ((QT, 1), (1, WIN), (1, SIDE_ROWS)) if keys_axis == 1 else ((1, QT), (WIN, 1), (SIDE_ROWS, 1))
    q_index = iota(qs, 1 - keys_axis)
    k_index = iota(ks, keys_axis)
    g_index = iota(gs, keys_axis)
    base = SEG_AT + rank * SLOTS + tile * (QT // BLK)
    q_seg = pick_by(q_index // BLK, [tab_ref[base + step] for step in range(QT // BLK)], -1)
    k_seg = key_segments(tab_ref, rank, first_row // BLK, k_index)
    g_seg = side_segments(tab_ref, rank, g_index)
    gap = (q_index + tile * QT) - (k_index + first_row)
    local = (jnp.abs(gap) <= RADIUS) & (q_seg == k_seg)
    return jnp.where(local, 0.0, MASKED_SCORE), jnp.where(q_seg == g_seg, 0.0, MASKED_SCORE)


def window_start(tile):
    return pl.multiple_of(jnp.clip(tile - 1, 0, TILES - WIN // QT) * QT, QT)


def head_stack(rows):
    lane = iota(rows.shape, 1) // DH
    zero = jnp.zeros_like(rows)
    return jnp.concatenate([jnp.where(lane == head, rows, zero) for head in range(QUAD // DH)], axis=0)


def head_merge(stacked):
    lane = iota((QT, QUAD), 1) // DH
    out = stacked[:QT]
    for head in range(1, QUAD // DH):
        out = jnp.where(lane == head, stacked[head * QT : (head + 1) * QT], out)
    return out


def gains_of(gc_ref):
    count = gc_ref.shape[0]
    part = D // count
    lane, column = iota((128, D), 0), iota((128, D), 1)
    total = None
    for shard in range(count):
        pick = jnp.where((column == lane + shard * part) & (lane < part), 1.0, 0.0).astype(BF16)
        term = mm(gc_ref[shard], pick)
        total = term if total is None else total + term
    return total


def three_way(value):
    high = value.astype(BF16)
    rest = value - high.astype(F32)
    middle = rest.astype(BF16)
    return high, middle, (rest - middle.astype(F32)).astype(BF16)


def spread_gain_grads(value, dc_ref):
    count = dc_ref.shape[0]
    part = D // count
    column, lane = iota((D, 128), 0), iota((D, 128), 1)
    parts = three_way(value)
    for shard in range(count):
        pick = jnp.where((column == lane + shard * part) & (lane < part), 1.0, 0.0).astype(BF16)
        dc_ref[shard] = mm(parts[0], pick) + mm(parts[1], pick) + mm(parts[2], pick)


def mean_square(value):
    return jnp.mean(value * value, axis=-1, keepdims=True)


def forward_norm(tab_ref, rank, x_ref, gains, n_ref):
    for tile in range(TILES):
        rows = pl.ds(tile * QT, QT)
        value = x_ref[rows, :].astype(F32)
        n_ref[rows, :] = (value * lax.rsqrt(mean_square(value) + EPSILON) * gains[0:1]).astype(BF16)
    side = mm(pooling(tab_ref, rank), n_ref[:ROWS, :])
    n_ref[ROWS:, :] = (side * lax.rsqrt(mean_square(side) + EPSILON) * gains[1:2]).astype(BF16)


def forward_project(n_ref, w_ref, qkv_ref):
    def step(tile, carry):
        cols = pl.ds(pl.multiple_of(tile * QUAD, QUAD), QUAD)
        qkv_ref[:, cols] = mm(n_ref[...], w_ref[:, cols]).astype(BF16)
        return carry

    lax.fori_loop(0, 3 * D // QUAD, step, 0)


def forward_attention(tab_ref, rank, qkv_ref, att_ref, lse_ref):
    def step(tile, carry):
        first = window_start(tile)
        bias, side_bias = tile_bias(tab_ref, rank, tile, first, 1)
        rows = pl.ds(pl.multiple_of(tile * QT, QT), QT)
        window = pl.ds(first, WIN)
        lse = jnp.zeros((QT, 128), F32)
        lane = iota((QT, 128), 1)
        for quad in range(D // QUAD):
            low = quad * QUAD
            query = head_stack(qkv_ref[rows, low : low + QUAD])
            scores = mm_cols(query, qkv_ref[window, D + low : D + low + QUAD])
            side_scores = mm_cols(query, qkv_ref[ROWS:, D + low : D + low + QUAD])
            local, sides, scale = [], [], []
            for head in range(QUAD // DH):
                part = slice(head * QT, (head + 1) * QT)
                one = scores[part] + bias
                two = side_scores[part] + side_bias
                peak = jnp.maximum(
                    jnp.max(one, axis=-1, keepdims=True), jnp.max(two, axis=-1, keepdims=True)
                )
                one, two = jnp.exp(one - peak), jnp.exp(two - peak)
                total = jnp.sum(one, axis=-1, keepdims=True) + jnp.sum(two, axis=-1, keepdims=True)
                local.append(one.astype(BF16))
                sides.append(two.astype(BF16))
                scale.append(1.0 / total)
                lse = jnp.where(lane == quad * (QUAD // DH) + head, peak + jnp.log(total), lse)
            mixed = mm(jnp.concatenate(local, axis=0), qkv_ref[window, 2 * D + low : 2 * D + low + QUAD])
            mixed = mixed + mm(
                jnp.concatenate(sides, axis=0), qkv_ref[ROWS:, 2 * D + low : 2 * D + low + QUAD]
            )
            mixed = mixed * jnp.concatenate(scale, axis=0)
            att_ref[rows, low : low + QUAD] = head_merge(mixed).astype(BF16)
        lse_ref[tile] = jnp.transpose(lse)[:16]
        return carry

    lax.fori_loop(0, TILES, step, 0)


def feed_forward(tab_ref, rank, x_ref, cot_ref, att_ref, gains, w_ref, wb_ref,
                 y_ref, gh_ref, ga_ref, dg_ref, db_ref, do_ref,
                 h1_ref, nt_ref, ntt_ref, gres_ref, h2_ref, gg_ref, gu_ref, gn_ref):
    hidden = wb_ref.shape[0]
    gate_at = 4 * D
    valid = valid_column(tab_ref, rank)
    gain = gains[2:3]
    for tile in range(TILES):
        rows = pl.ds(tile * QT, QT)
        value = x_ref[rows, :].astype(F32) + mm(att_ref[rows, :], w_ref[:, 3 * D : 4 * D])
        h1_ref[rows, :] = value
        normed = (value * lax.rsqrt(mean_square(value) + EPSILON) * gain).astype(BF16)
        nt_ref[rows, :] = normed
        ntt_ref[:, tile * QT : (tile + 1) * QT] = jnp.transpose(normed)
        gres_ref[rows, :] = (cot_ref[rows, :].astype(F32) * valid[tile * QT : (tile + 1) * QT]).astype(BF16)

    def inward(tile, carry):
        at = pl.multiple_of(tile * FF_TILE, FF_TILE)
        cols = pl.ds(at, FF_TILE)
        gate = mm(nt_ref[...], w_ref[:, pl.ds(gate_at + at, FF_TILE)])
        up = mm(nt_ref[...], w_ref[:, pl.ds(gate_at + hidden + at, FF_TILE)])
        back = mm_cols(gres_ref[...], wb_ref[cols, :])
        square = gate * gate
        bend = jnp.tanh(GELU_C * (gate * (1.0 + GELU_A * square)))
        half = 0.5 * (1.0 + bend)
        act = gate * half
        slope = half + (0.5 * GELU_C) * gate * (1.0 - bend * bend) * (1.0 + (3.0 * GELU_A) * square)
        h2_ref[:, cols] = (act * up).astype(BF16)
        gg_ref[:, cols] = (back * up * slope).astype(BF16)
        gu_ref[:, cols] = (back * act).astype(BF16)
        return carry

    lax.fori_loop(0, hidden // FF_TILE, inward, 0)

    def outward(tile, carry):
        cols = pl.ds(pl.multiple_of(tile * QUAD, QUAD), QUAD)
        value = h1_ref[:, cols] + mm(h2_ref[...], wb_ref[:, cols])
        y_ref[:, cols] = (value * valid).astype(BF16)
        gn_ref[:, cols] = mm_cols(gg_ref[...], w_ref[cols, gate_at : gate_at + hidden]) + mm_cols(
            gu_ref[...], w_ref[cols, gate_at + hidden :]
        )
        return carry

    lax.fori_loop(0, D // QUAD, outward, 0)

    def weights(tile, carry):
        at = pl.multiple_of(tile * FF_TILE, FF_TILE)
        cols = pl.ds(at, FF_TILE)
        dg_ref[:, cols] = mm(ntt_ref[...], gg_ref[:, cols]).astype(BF16)
        dg_ref[:, pl.ds(hidden + at, FF_TILE)] = mm(ntt_ref[...], gu_ref[:, cols]).astype(BF16)
        db_ref[cols, :] = mm_rows(h2_ref[:, cols], gres_ref[...]).astype(BF16)
        return carry

    lax.fori_loop(0, hidden // FF_TILE, weights, 0)

    gain_grad = jnp.zeros((1, D), F32)
    for tile in range(TILES):
        rows = pl.ds(tile * QT, QT)
        value, grad = h1_ref[rows, :], gn_ref[rows, :]
        root = lax.rsqrt(mean_square(value) + EPSILON)
        unit = value * root
        gain_grad = gain_grad + jnp.sum(grad * unit, axis=0, keepdims=True)
        grad = grad * gain
        grad = gres_ref[rows, :].astype(F32) + root * (
            grad - unit * jnp.mean(grad * unit, axis=-1, keepdims=True)
        )
        gh_ref[rows, :] = grad
        low = grad.astype(BF16)
        nt_ref[rows, :] = low
        ga_ref[rows, :] = mm_cols(low, w_ref[:, 3 * D : 4 * D]).astype(BF16)

    def out_weight(tile, carry):
        cols = pl.ds(pl.multiple_of(tile * QUAD, QUAD), QUAD)
        do_ref[cols, :] = mm_rows(att_ref[:, cols], nt_ref[...]).astype(BF16)
        return carry

    lax.fori_loop(0, D // QUAD, out_weight, 0)
    return gain_grad


def backward_attention(tab_ref, rank, qkv_ref, att_ref, ga_ref, lse_ref, dqkv_ref, dk_ref, dv_ref):
    dk_ref[...] = jnp.zeros_like(dk_ref)
    dv_ref[...] = jnp.zeros_like(dv_ref)
    heads = QUAD // DH
    marks = jnp.where(iota((16, D), 1) // DH == iota((16, D), 0), 1.0, 0.0).astype(BF16)

    def step(tile, carry):
        first = window_start(tile)
        bias, side_bias = tile_bias(tab_ref, rank, tile, first, 0)
        bias = jnp.concatenate([bias, side_bias], axis=0)
        rows = pl.ds(pl.multiple_of(tile * QT, QT), QT)
        window = pl.ds(first, WIN)
        product = ga_ref[rows, :].astype(F32) * att_ref[rows, :].astype(F32)
        high = product.astype(BF16)
        rest = (product - high.astype(F32)).astype(BF16)
        centre = mm_cols(marks, high) + mm_cols(marks, rest)
        lse = lse_ref[tile]
        for quad in range(D // QUAD):
            low = quad * QUAD
            query = head_stack(qkv_ref[rows, low : low + QUAD])
            grad = head_stack(ga_ref[rows, low : low + QUAD])
            keys = jnp.concatenate(
                [qkv_ref[window, D + low : D + low + QUAD], qkv_ref[ROWS:, D + low : D + low + QUAD]], axis=0
            )
            values = jnp.concatenate(
                [qkv_ref[window, 2 * D + low : 2 * D + low + QUAD],
                 qkv_ref[ROWS:, 2 * D + low : 2 * D + low + QUAD]], axis=0
            )
            scores = mm_cols(keys, query)
            slopes = mm_cols(values, grad)
            probs, grads = [], []
            for head in range(heads):
                part = slice(head * QT, (head + 1) * QT)
                number = quad * heads + head
                prob = jnp.exp(scores[:, part] + bias - lse[number : number + 1])
                probs.append(prob.astype(BF16))
                grads.append((prob * (slopes[:, part] - centre[number : number + 1])).astype(BF16))
            probs = jnp.concatenate(probs, axis=1)
            grads = jnp.concatenate(grads, axis=1)
            dkey = mm(grads, query)
            dvalue = mm(probs, grad)
            cols = slice(low, low + QUAD)
            dk_ref[window, cols] = dk_ref[window, cols] + dkey[:WIN]
            dk_ref[ROWS:, cols] = dk_ref[ROWS:, cols] + dkey[WIN:]
            dv_ref[window, cols] = dv_ref[window, cols] + dvalue[:WIN]
            dv_ref[ROWS:, cols] = dv_ref[ROWS:, cols] + dvalue[WIN:]
            dqkv_ref[rows, cols] = head_merge(mm_rows(grads, keys)).astype(BF16)
        return carry

    lax.fori_loop(0, TILES, step, 0)
    dqkv_ref[ROWS:, :D] = jnp.zeros((SIDE_ROWS, D), BF16)
    dqkv_ref[:, D : 2 * D] = dk_ref[...].astype(BF16)
    dqkv_ref[:, 2 * D :] = dv_ref[...].astype(BF16)


def backward_project(tab_ref, rank, x_ref, gh_ref, gains, n_ref, dqkv_ref, w_ref, gn_ref, g_ref, dw_ref):
    def step(tile, carry):
        cols = pl.ds(pl.multiple_of(tile * QUAD, QUAD), QUAD)
        gn_ref[:, cols] = mm_cols(dqkv_ref[...], w_ref[cols, : 3 * D])
        return carry

    lax.fori_loop(0, D // QUAD, step, 0)

    def weights(tile, carry):
        cols = pl.ds(pl.multiple_of(tile * QUAD, QUAD), QUAD)
        dw_ref[:, cols] = mm_rows(n_ref[...], dqkv_ref[:, cols]).astype(BF16)
        return carry

    lax.fori_loop(0, 3 * D // QUAD, weights, 0)
    pool = pooling(tab_ref, rank)
    side = mm(pool, n_ref[:ROWS, :])
    root = lax.rsqrt(mean_square(side) + EPSILON)
    unit = side * root
    grad = gn_ref[ROWS:, :]
    side_gain = jnp.sum(grad * unit, axis=0, keepdims=True)
    grad = grad * gains[1:2]
    grad = root * (grad - unit * jnp.mean(grad * unit, axis=-1, keepdims=True))
    parts = three_way(grad)
    gain_grad = jnp.zeros((1, D), F32)
    for tile in range(TILES):
        rows = pl.ds(tile * QT, QT)
        spread = pool[:, tile * QT : (tile + 1) * QT]
        total = gn_ref[rows, :] + mm_rows(spread, parts[0]) + mm_rows(spread, parts[1])
        value = x_ref[rows, :].astype(F32)
        root = lax.rsqrt(mean_square(value) + EPSILON)
        unit = value * root
        gain_grad = gain_grad + jnp.sum(total * unit, axis=0, keepdims=True)
        total = total * gains[0:1]
        g_ref[rows, :] = (
            gh_ref[rows, :] + root * (total - unit * jnp.mean(total * unit, axis=-1, keepdims=True))
        ).astype(BF16)
    return gain_grad, side_gain


def first_kernel(tab_ref, x_ref, gc_ref, w_ref, n_ref, qkv_ref, att_ref, lse_ref):
    rank = lax.axis_index("rep")
    gains = gains_of(gc_ref)
    forward_norm(tab_ref, rank, x_ref, gains, n_ref)
    forward_project(n_ref, w_ref, qkv_ref)
    forward_attention(tab_ref, rank, qkv_ref, att_ref, lse_ref)


def second_kernel(tab_ref, x_ref, cot_ref, att_ref, gc_ref, w_ref, wb_ref,
                  y_ref, gh_ref, ga_ref, dg_ref, db_ref, do_ref, gain_ref, *scratch):
    rank = lax.axis_index("rep")
    gain_ref[...] = feed_forward(tab_ref, rank, x_ref, cot_ref, att_ref, gains_of(gc_ref), w_ref, wb_ref,
                                 y_ref, gh_ref, ga_ref, dg_ref, db_ref, do_ref, *scratch)


def third_kernel(tab_ref, x_ref, gh_ref, ga_ref, att_ref, lse_ref, n_ref, qkv_ref, gain_ref, gc_ref, w_ref,
                 g_ref, dw_ref, dc_ref, dqkv_ref, dk_ref, dv_ref, gn_ref):
    rank = lax.axis_index("rep")
    gains = gains_of(gc_ref)
    backward_attention(tab_ref, rank, qkv_ref, att_ref, ga_ref, lse_ref, dqkv_ref, dk_ref, dv_ref)
    one, side = backward_project(
        tab_ref, rank, x_ref, gh_ref, gains, n_ref, dqkv_ref, w_ref, gn_ref, g_ref, dw_ref
    )
    grads = jnp.concatenate([one, side, gain_ref[...], jnp.zeros((5, D), F32)], axis=0)
    spread_gain_grads(grads, dc_ref)


def layer(tab, x, cot, gc, w, wb):
    hidden = wb.shape[0]
    shape = jax.ShapeDtypeStruct
    params = pltpu.CompilerParams(vmem_limit_bytes=VMEM_LIMIT)
    n, qkv, att, lse = pl.pallas_call(
        first_kernel,
        out_shape=(shape((ALL_ROWS, D), BF16), shape((ALL_ROWS, 3 * D), BF16), shape((ROWS, D), BF16),
                   shape((TILES, 16, QT), F32)),
        in_specs=[SMEM, VMEM, VMEM, pl.BlockSpec((D, 3 * D), lambda step: (0, 0))],
        grid=(1,),
        out_specs=(VMEM,) * 4,
        compiler_params=params,
        name="attend",
    )(tab, x, gc, w)
    y, gh, ga, dg, db, do, gain = pl.pallas_call(
        second_kernel,
        out_shape=(shape((ROWS, D), BF16), shape((ROWS, D), F32), shape((ROWS, D), BF16),
                   shape((D, 2 * hidden), BF16), shape((hidden, D), BF16), shape((D, D), BF16), shape((1, D), F32)),
        in_specs=[SMEM] + [VMEM] * 6,
        out_specs=(VMEM,) * 7,
        scratch_shapes=[pltpu.VMEM((ROWS, D), F32), pltpu.VMEM((ROWS, D), BF16), pltpu.VMEM((D, ROWS), BF16),
                        pltpu.VMEM((ROWS, D), BF16), pltpu.VMEM((ROWS, hidden), BF16),
                        pltpu.VMEM((ROWS, hidden), BF16), pltpu.VMEM((ROWS, hidden), BF16),
                        pltpu.VMEM((ROWS, D), F32)],
        compiler_params=params,
        name="feed_forward",
    )(tab, x, cot, att, gc, w, wb)
    g, dw, dc = pl.pallas_call(
        third_kernel,
        out_shape=(shape((ROWS, D), BF16), shape((D, 3 * D), BF16), shape((gc.shape[0], 8, 128), F32)),
        in_specs=[SMEM] + [VMEM] * 9 + [pl.BlockSpec((D, 3 * D), lambda step: (0, 0))],
        grid=(1,),
        out_specs=(VMEM,) * 3,
        scratch_shapes=[pltpu.VMEM((ALL_ROWS, 3 * D), BF16), pltpu.VMEM((ALL_ROWS, D), F32),
                        pltpu.VMEM((ALL_ROWS, D), F32), pltpu.VMEM((ALL_ROWS, D), F32)],
        compiler_params=params,
        name="attend_back",
    )(tab, x, gh, ga, att, lse, n, qkv, gain, gc, w)
    return y, g, dg, db, do, dw, dc


def per_device(count, layer_input, cotangent, lengths, attn_gain, global_gain, query_weight, key_weight,
               value_weight, out_weight, ffn_gain, gate_weight, up_weight, down_weight):
    micro, span, width = layer_input.shape
    hidden = gate_weight.shape[1]
    blocks = micro * span // BLK
    table = deal_table(lengths)
    wa = jnp.concatenate([query_weight, key_weight, value_weight, out_weight, gate_weight, up_weight], axis=1)
    part = attn_gain.shape[0]
    wc = jnp.pad(jnp.stack([attn_gain, global_gain, ffn_gain]), ((0, 13), (0, 128 - part)))
    splits = ((0, 4 * width), (4 * width, 2 * hidden))
    ga, gb, gc, rows, cots = gather_weights(
        count, splits, table,
        layer_input.reshape(blocks, BLK, width), cotangent.reshape(blocks, BLK, width), wa, down_weight, wc,
    )
    y, g, dg, db, do, dw, dc = layer(
        table, rows.reshape(ROWS, width), cots.reshape(ROWS, width), gc, ga.reshape(width, -1), gb.reshape(-1, width)
    )
    grads = [grad.reshape(count, -1, grad.shape[-1]) for grad in (dg, db, do, dw, dc)]
    og, ob, oo, ow, oc, ry, rg = reduce_grads(
        count, grads, y.reshape(SLOTS, BLK, width), g.reshape(SLOTS, BLK, width)
    )
    y_home, g_home = bring_home(table, ry, rg, blocks)
    return (
        y_home.reshape(layer_input.shape), g_home.reshape(layer_input.shape),
        oc[0, :part], oc[1, :part], ow[:, :width], ow[:, width : 2 * width], ow[:, 2 * width :], oo,
        oc[2, :part], og[:, :hidden], og[:, hidden:], ob,
    )


def solution(mesh):
    rows = P(None, ("rep", "fsdp"), None)
    vector, matrix = P("fsdp"), P("fsdp", None)
    return jax.shard_map(
        partial(per_device, mesh.shape["fsdp"]),
        mesh=mesh,
        in_specs=(rows, rows, P(None, ("rep", "fsdp")), vector, vector, matrix, matrix, matrix, matrix,
                  vector, matrix, matrix, matrix),
        out_specs=(rows, rows, vector, vector, matrix, matrix, matrix, matrix, vector, matrix, matrix, matrix),
        check_vma=False,
    )
```

```python
from functools import partial

import jax
import jax.numpy as jnp
from jax import lax
from jax.experimental import pallas as pl
from jax.experimental.pallas import tpu as pltpu
from jax.sharding import PartitionSpec as P

H = 12
DH = 64
RADIUS = 127
GBLK = 16
BLK = 64
SLOTS = 10
MAX_SEQ_BLOCKS = 5
EPSILON = 1e-06
MASKED_SCORE = -1e30
MESH = pl.DeviceIdType.MESH
VMEM_LIMIT = 60 * 1024 * 1024
SEG_AT, LEN_AT, DEST_AT, TABLE_SIZE = 40, 80, 120, 256

ANY = pl.BlockSpec(memory_space=pl.ANY)
VMEM = pl.BlockSpec(memory_space=pltpu.VMEM)
SMEM = pl.BlockSpec(memory_space=pltpu.SMEM)


def grid_of(count):
    inner = 2 if count <= 8 else 4
    return count // inner, inner


def core_of(rank):
    return rank + 1 - 2 * (rank % 2)


def across_of(rank):
    return (rank + 2) % 4


def lens_kernel(lens_ref, all_ref, send_sem, recv_sem):
    rank = lax.axis_index("rep")
    barrier = pltpu.get_barrier_semaphore()
    for step in range(1, 4):
        pl.semaphore_signal(
            barrier, inc=1, device_id={"rep": (rank + step) % 4}, device_id_type=MESH
        )
    pl.semaphore_wait(barrier, 3)
    copies = []
    for step in range(1, 4):
        copy = pltpu.make_async_remote_copy(
            src_ref=lens_ref,
            dst_ref=all_ref.at[rank],
            send_sem=send_sem.at[step - 1],
            recv_sem=recv_sem.at[step - 1],
            device_id={"rep": (rank + step) % 4},
            device_id_type=MESH,
        )
        copy.start()
        copies.append(copy)
    all_ref[rank] = lens_ref[...]
    for copy in copies:
        copy.wait()


def table_kernel(micro, per_dev, lens_ref, tab_ref, order_ref, count_ref, load_ref):
    total = 4 * micro * per_dev

    def length_at(spot):
        return lens_ref[spot // (micro * per_dev), (spot // per_dev) % micro, spot % per_dev]

    def blocks_of(length):
        return (length + (BLK - 1)) // BLK

    def clear(spot, carry):
        tab_ref[spot] = -1
        return carry

    lax.fori_loop(0, TABLE_SIZE, clear, 0)
    for spot in range(4 * SLOTS):
        tab_ref[LEN_AT + spot] = 0
    for size in range(8):
        count_ref[size] = 0
    for dev in range(4):
        load_ref[dev] = 0

    def tally(spot, carry):
        length = length_at(spot)

        @pl.when(length > 0)
        def _():
            size = blocks_of(length)
            count_ref[size] = count_ref[size] + 1

        return carry

    lax.fori_loop(0, total, tally, 0)
    begin = 0
    for size in range(MAX_SEQ_BLOCKS, 0, -1):
        amount = count_ref[size]
        count_ref[size] = begin
        begin = begin + amount

    def place(spot, carry):
        length = length_at(spot)

        @pl.when(length > 0)
        def _():
            size = blocks_of(length)
            where = count_ref[size]
            order_ref[where] = spot
            count_ref[size] = where + 1

        return carry

    lax.fori_loop(0, total, place, 0)

    def assign(number, carry):
        spot = order_ref[number]
        length = length_at(spot)
        size = blocks_of(length)
        best = jnp.int32(0)
        low = load_ref[0]
        for dev in range(1, 4):
            here = load_ref[dev]
            best = jnp.where(here < low, dev, best)
            low = jnp.minimum(here, low)
        load_ref[best] = low + size

        def put(step, inner):
            slot = best * SLOTS + low + step
            tab_ref[slot] = spot + step
            tab_ref[SEG_AT + slot] = low
            tab_ref[LEN_AT + slot] = jnp.minimum(length - BLK * step, BLK)
            tab_ref[DEST_AT + spot + step] = slot
            return inner

        lax.fori_loop(0, size, put, 0)
        return carry

    lax.fori_loop(0, begin, assign, 0)


def deal_table(lengths):
    micro, per_dev = lengths.shape
    padded = jnp.pad(lengths, ((0, 8 - micro), (0, 128 - per_dev)))
    everyone = pl.pallas_call(
        lens_kernel,
        out_shape=jax.ShapeDtypeStruct((4, 8, 128), jnp.int32),
        in_specs=[VMEM],
        out_specs=VMEM,
        scratch_shapes=[pltpu.SemaphoreType.DMA((3,)), pltpu.SemaphoreType.DMA((3,))],
        compiler_params=pltpu.CompilerParams(collective_id=0, has_side_effects=True),
        name="lens_exchange",
    )(padded)
    return pl.pallas_call(
        partial(table_kernel, micro, per_dev),
        out_shape=jax.ShapeDtypeStruct((TABLE_SIZE,), jnp.int32),
        in_specs=[SMEM],
        out_specs=SMEM,
        scratch_shapes=[
            pltpu.SMEM((4 * micro * per_dev,), jnp.int32),
            pltpu.SMEM((8,), jnp.int32),
            pltpu.SMEM((4,), jnp.int32),
        ],
        name="deal_table",
    )(everyone)


def gather_kernel(
    outer, inner, splits, tab_ref, rows_ref, cots_ref, wa_ref, wb_ref, wc_ref,
    ga_ref, gb_ref, gc_ref, rows_out, cots_out,
    psend, precv, xsend, xrecv,
    z_send, z_recv, y_send, y_recv, c_send, c_recv, own_sem,
    p_send, p_recv, x_send, x_recv,
):
    rank = lax.axis_index("rep")
    spot = lax.axis_index("fsdp")
    core = rank % 2
    row, col = spot // inner, spot % inner
    count = outer * inner
    mate, across = core_of(rank), across_of(rank)
    pieces = [(wa_ref, ga_ref, start, width // 2) for start, width in splits]
    pieces.append((wb_ref, gb_ref, 0, wb_ref.shape[1] // 2))
    pieces.append((wc_ref, gc_ref, 0, None))
    halved = [number for number, piece in enumerate(pieces) if piece[3] is not None]

    barrier = pltpu.get_barrier_semaphore()
    neighbours = (
        (row + 1 < outer, {"fsdp": spot + inner}),
        (row > 0, {"fsdp": spot - inner}),
        (col + 1 < inner, {"fsdp": spot + 1}),
        (col > 0, {"fsdp": spot - 1}),
    )
    amount = jnp.int32(2)
    for there, device in neighbours:
        amount = amount + there.astype(jnp.int32)

        @pl.when(there)
        def _():
            pl.semaphore_signal(barrier, inc=1, device_id=device, device_id_type=MESH)

    for device in (mate, across):
        pl.semaphore_signal(barrier, inc=1, device_id={"rep": device}, device_id_type=MESH)
    pl.semaphore_wait(barrier, amount)

    def cut(ref, number):
        _, _, start, half = pieces[number]
        if half is None:
            return ref
        return ref.at[:, pl.ds(pl.multiple_of(start + core * half, 128), half)]

    def landed(number, shard):
        return cut(pieces[number][1].at[shard], number)

    late = []

    def send(there, src, dst, ssem, rsem, device):
        def describe():
            return pltpu.make_async_remote_copy(
                src_ref=src, dst_ref=dst, send_sem=ssem, recv_sem=rsem,
                device_id=device, device_id_type=MESH,
            )

        if there is None:
            describe().start()
            late.append((None, lambda: describe().wait_send()))
        else:
            @pl.when(there)
            def _():
                describe().start()

            late.append((there, lambda: describe().wait_send()))

    def arrive(number, shard, rsem):
        pltpu.make_async_remote_copy(
            src_ref=landed(number, shard), dst_ref=landed(number, shard),
            send_sem=own_sem.at[0], recv_sem=rsem,
            device_id={"rep": mate}, device_id_type=MESH,
        ).wait_recv()

    def both(first, second):
        return second if first is None else jnp.logical_and(first, second)

    def to_mate(there, number, shard):
        if number not in halved:
            return
        place = landed(number, shard)
        send(there, place, place, c_send.at[number, shard], c_recv.at[number, shard], {"rep": mate})

    def along_row(there, number, line, src):
        shard = line * inner + col
        place = landed(number, shard)
        src = place if src is None else src
        send(both(there, col + 1 < inner), src, place,
             y_send.at[0, 0, line, number], y_recv.at[0, 0, line, number], {"fsdp": spot + 1})
        send(both(there, col > 0), src, place,
             y_send.at[1, 0, line, number], y_recv.at[1, 0, line, number], {"fsdp": spot - 1})

    def from_row(there, number, line):
        for step in range(inner - 1):
            for way, source, onward, target in (
                (0, col - 1 - step, col + 1 < inner, spot + 1),
                (1, col + 1 + step, col > 0, spot - 1),
            ):
                here = jnp.logical_and(source >= 0, source < inner)
                here = both(there, here)
                shard = line * inner + source

                @pl.when(here)
                def _():
                    arrive(number, shard, y_recv.at[way, step, line, number])

                if step + 1 < inner - 1:
                    place = landed(number, shard)
                    send(both(here, onward), place, place,
                         y_send.at[way, step + 1, line, number],
                         y_recv.at[way, step + 1, line, number], {"fsdp": target})
                to_mate(here, number, shard)

    for number, piece in enumerate(pieces):
        src, place = cut(piece[0], number), landed(number, spot)
        send(row + 1 < outer, src, place, z_send.at[0, 0, number], z_recv.at[0, 0, number],
             {"fsdp": spot + inner})
        send(row > 0, src, place, z_send.at[1, 0, number], z_recv.at[1, 0, number],
             {"fsdp": spot - inner})
        along_row(None, number, row, src)
    own = [
        pltpu.make_async_copy(wa_ref, ga_ref.at[spot], own_sem.at[0]),
        pltpu.make_async_copy(wb_ref, gb_ref.at[spot], own_sem.at[1]),
        pltpu.make_async_copy(wc_ref, gc_ref.at[spot], own_sem.at[2]),
    ]
    for copy in own:
        copy.start()

    sources = (rows_ref, cots_ref)
    per_rank = rows_ref.shape[0]

    def picked(kind, target, slot):
        index = tab_ref[target * SLOTS + slot] - rank * per_rank
        mine = jnp.logical_and(index >= 0, index < per_rank)
        value = sources[kind][jnp.clip(index, 0, per_rank - 1)]
        return mine, value

    def mate_copy(kind, part):
        return pltpu.make_async_remote_copy(
            src_ref=psend.at[kind, part], dst_ref=precv.at[kind, part],
            send_sem=p_send.at[kind, part], recv_sem=p_recv.at[kind, part],
            device_id={"rep": mate}, device_id_type=MESH,
        )

    def across_copy(kind):
        return pltpu.make_async_remote_copy(
            src_ref=xsend.at[kind], dst_ref=xrecv.at[kind],
            send_sem=x_send.at[kind], recv_sem=x_recv.at[kind],
            device_id={"rep": across}, device_id_type=MESH,
        )

    for kind, part in ((0, 1), (1, 1), (0, 0), (1, 0)):
        target = mate if part == 0 else across_of(mate)

        def pack(slot, carry):
            mine, value = picked(kind, target, slot)
            psend[kind, part, slot] = jnp.where(mine, value, jnp.zeros_like(value))
            return carry

        lax.fori_loop(0, SLOTS, pack, 0)
        mate_copy(kind, part).start()
    for kind in range(2):
        mate_copy(kind, 1).wait_recv()

        def merge(slot, carry):
            mine, value = picked(kind, across, slot)
            xsend[kind, slot] = jnp.where(mine, value, precv[kind, 1, slot])
            return carry

        lax.fori_loop(0, SLOTS, merge, 0)
        across_copy(kind).start()

    def lines(step):
        return ((row - 1 - step >= 0, row - 1 - step, 0, row + 1 < outer, spot + inner),
                (row + 1 + step < outer, row + 1 + step, 1, row > 0, spot - inner))

    for step in range(outer - 1):
        for number in range(len(pieces)):
            for here, line, way, onward, target in lines(step):
                shard = line * inner + col

                @pl.when(here)
                def _():
                    arrive(number, shard, z_recv.at[way, step, number])

                if step + 1 < outer - 1:
                    place = landed(number, shard)
                    send(jnp.logical_and(here, onward), place, place,
                         z_send.at[way, step + 1, number], z_recv.at[way, step + 1, number],
                         {"fsdp": target})
                along_row(here, number, line, None)
                to_mate(here, number, shard)
        for number in range(len(pieces)):
            if step == 0:
                from_row(None, number, row)
            else:
                for here, line, *_ in lines(step - 1):
                    from_row(here, number, line)
    for number in range(len(pieces)):
        for here, line, *_ in lines(outer - 2):
            from_row(here, number, line)

    outs = (rows_out, cots_out)
    for kind in range(2):
        mate_copy(kind, 0).wait_recv()
        across_copy(kind).wait_recv()

        def finish(slot, carry):
            mine, value = picked(kind, rank, slot)
            outs[kind][slot] = jnp.where(mine, value, precv[kind, 0, slot] + xrecv[kind, slot])
            return carry

        lax.fori_loop(0, SLOTS, finish, 0)

    for shard in range(count):
        @pl.when(shard != spot)
        def _():
            for number in halved:
                other = pieces[number]
                view = other[1].at[shard].at[:, pl.ds(0, other[3])]
                pltpu.make_async_remote_copy(
                    src_ref=view, dst_ref=view, send_sem=own_sem.at[0],
                    recv_sem=c_recv.at[number, shard],
                    device_id={"rep": mate}, device_id_type=MESH,
                ).wait_recv()
    for there, finish_send in late:
        if there is None:
            finish_send()
        else:
            pl.when(there)(finish_send)
    for kind in range(2):
        for part in range(2):
            mate_copy(kind, part).wait_send()
        across_copy(kind).wait_send()
    for copy in own:
        copy.wait()


def gather_weights(count, splits, table, rows, cots, wa, wb, wc):
    outer, inner = grid_of(count)
    block = rows.shape[1:]
    kinds = len(splits) + 2
    dma = pltpu.SemaphoreType.DMA
    bf16 = jnp.bfloat16
    return pl.pallas_call(
        partial(gather_kernel, outer, inner, splits),
        out_shape=(
            jax.ShapeDtypeStruct((count,) + wa.shape, bf16),
            jax.ShapeDtypeStruct((count,) + wb.shape, bf16),
            jax.ShapeDtypeStruct((count,) + wc.shape, bf16),
            jax.ShapeDtypeStruct((SLOTS,) + block, bf16),
            jax.ShapeDtypeStruct((SLOTS,) + block, bf16),
        ),
        in_specs=[SMEM, VMEM, VMEM, VMEM, VMEM, VMEM],
        out_specs=(ANY, ANY, ANY, VMEM, VMEM),
        scratch_shapes=[
            pltpu.VMEM((2, 2, SLOTS) + block, bf16),
            pltpu.VMEM((2, 2, SLOTS) + block, bf16),
            pltpu.VMEM((2, SLOTS) + block, bf16),
            pltpu.VMEM((2, SLOTS) + block, bf16),
            dma((2, outer - 1, kinds)), dma((2, outer - 1, kinds)),
            dma((2, inner - 1, outer, kinds)), dma((2, inner - 1, outer, kinds)),
            dma((kinds, count)), dma((kinds, count)), dma((3,)),
            dma((2, 2)), dma((2, 2)), dma((2,)), dma((2,)),
        ],
        compiler_params=pltpu.CompilerParams(
            collective_id=1, has_side_effects=True, vmem_limit_bytes=VMEM_LIMIT
        ),
        name="gather_and_deal",
    )(table, rows, cots, wa, wb, wc)


def reduce_kernel(
    outer, inner, kinds, *refs
):
    grads, (y_ref, g_ref) = refs[:kinds], refs[kinds : kinds + 2]
    totals, (ry_ref, rg_ref) = refs[kinds + 2 : 2 * kinds + 2], refs[2 * kinds + 2 : 2 * kinds + 4]
    scratch = refs[2 * kinds + 4 :]
    mines, crecvs, yrecvs, zrecvs, xrecvs = (
        scratch[kinds * i : kinds * (i + 1)] for i in range(5)
    )
    (c_send, c_recv, m_sem, y_send, y_recv, z_send, z_recv, x_send, x_recv, f_send, f_recv,
     r_send, r_recv, q_sem) = scratch[5 * kinds :]
    rank = lax.axis_index("rep")
    spot = lax.axis_index("fsdp")
    core = rank % 2
    row, col = spot // inner, spot % inner
    mate, across = core_of(rank), across_of(rank)
    pieces = [(src, dst, 0, src.shape[3] // 2) for src, dst in zip(grads[:-1], totals)]
    pieces.append((grads[-1], totals[-1], 0, None))

    barrier = pltpu.get_barrier_semaphore()
    neighbours = (
        (row + 1 < outer, {"fsdp": spot + inner}),
        (row > 0, {"fsdp": spot - inner}),
        (col + 1 < inner, {"fsdp": spot + 1}),
        (col > 0, {"fsdp": spot - 1}),
    )
    amount = jnp.int32(2)
    for there, device in neighbours:
        amount = amount + there.astype(jnp.int32)

        @pl.when(there)
        def _():
            pl.semaphore_signal(barrier, inc=1, device_id=device, device_id_type=MESH)

    for device in (mate, across):
        pl.semaphore_signal(barrier, inc=1, device_id={"rep": device}, device_id_type=MESH)
    pl.semaphore_wait(barrier, amount)

    late = []

    def send(there, src, dst, ssem, rsem, device):
        def describe():
            return pltpu.make_async_remote_copy(
                src_ref=src, dst_ref=dst, send_sem=ssem, recv_sem=rsem,
                device_id=device, device_id_type=MESH,
            )

        if there is None:
            describe().start()
            late.append((None, lambda: describe().wait_send()))
        else:
            @pl.when(there)
            def _():
                describe().start()

            late.append((there, lambda: describe().wait_send()))

    def arrive(place, rsem):
        pltpu.make_async_remote_copy(
            src_ref=place, dst_ref=place, send_sem=q_sem.at[0], recv_sem=rsem,
            device_id={"rep": mate}, device_id_type=MESH,
        ).wait_recv()

    def columns(ref, number, which):
        _, _, start, half = pieces[number]
        if half is None:
            return ref
        cols = pl.ds(pl.multiple_of(start + which * half, 128), half)
        return ref.at[:, :, :, cols] if len(ref.shape) == 4 else ref.at[:, cols]

    order = list(range(kinds))
    loads = []
    for number in order:
        src = columns(pieces[number][0], number, 1 - core)
        send(None, src, crecvs[number], c_send.at[number], c_recv.at[number], {"rep": mate})
        load = pltpu.make_async_copy(
            columns(pieces[number][0], number, core), mines[number], m_sem.at[number]
        )
        load.start()
        loads.append(load)

    for kind, (src, dst) in enumerate(((y_ref, ry_ref), (g_ref, rg_ref))):
        send(None, src, dst.at[rank], r_send.at[kind, 0], r_recv.at[kind, 0], {"rep": across})
        send(None, src, dst.at[rank], r_send.at[kind, 1], r_recv.at[kind, 1], {"rep": mate})
        pltpu.make_async_copy(src, dst.at[rank], q_sem.at[kind + 1]).start()

    def slot_of(way, size, place, dest):
        if size == 2:
            return 0
        return dest - place if way == 0 else size - place + dest

    def line_sum(number, size, place, stride, buffer, view, ssem, rsem):
        for far in range(size - 1, 0, -1):
            for way in range(2):
                dest = far if way == 0 else size - 1 - far
                step = 1 if way == 0 else -1
                passes = place < dest if way == 0 else place > dest
                first = place == 0 if way == 0 else place == size - 1
                mine = view(dest)
                got = slot_of(way, size, place, dest)

                @pl.when(jnp.logical_and(passes, jnp.logical_not(first)))
                def _():
                    arrive(buffer.at[got], rsem.at[got, number])
                    mine[...] = mine[...] + buffer[got]

                put = slot_of(way, size, place + step, dest)
                send(passes, mine, buffer.at[put], ssem.at[way, dest, number], rsem.at[put, number],
                     {"fsdp": spot + step * stride})
        for way in range(2):
            has = place > 0 if way == 0 else place < size - 1
            got = slot_of(way, size, place, place)
            mine = view(place)

            @pl.when(has)
            def _():
                arrive(buffer.at[got], rsem.at[got, number])
                mine[...] = mine[...] + buffer[got]

    for number in order:
        loads[number].wait()
        arrive(crecvs[number], c_recv.at[number])
        mine, other = mines[number], crecvs[number]

        def add(index, carry):
            mine[index // inner, index % inner] = (
                mine[index // inner, index % inner] + other[index // inner, index % inner]
            )
            return carry

        lax.fori_loop(0, outer * inner, add, 0)
        if inner == 2:
            send(None, mine.at[:, 1 - col], yrecvs[number].at[0], y_send.at[0, 0, number],
                 y_recv.at[0, number], {"fsdp": spot + 1 - 2 * col})
    for kind, dst in enumerate((ry_ref, rg_ref)):
        place = dst.at[across]
        arrive(place, r_recv.at[kind, 0])
        send(None, place, place, r_send.at[kind, 2], r_recv.at[kind, 2], {"rep": mate})
    for number in order:
        mine = mines[number]
        if inner == 2:
            arrive(yrecvs[number].at[0], y_recv.at[0, number])
            buffer = yrecvs[number]

            def add(index, carry):
                mine[index, col] = mine[index, col] + buffer[0, index]
                return carry

            lax.fori_loop(0, outer, add, 0)
        else:
            line_sum(number, inner, col, 1, yrecvs[number], lambda dest: mine.at[:, dest],
                     y_send, y_recv)
        line_sum(number, outer, row, inner, zrecvs[number], lambda dest: mine.at[dest, col],
                 z_send, z_recv)
        send(None, mine.at[row, col], xrecvs[number], x_send.at[number], x_recv.at[number],
             {"rep": across})
    for number in order:
        arrive(xrecvs[number], x_recv.at[number])
        total = mines[number][row, col].astype(jnp.float32) + xrecvs[number][...].astype(jnp.float32)
        out, half = pieces[number][1], pieces[number][3]
        place = columns(out, number, core)
        place[...] = total
        if half is not None:
            send(None, place, place, f_send.at[number], f_recv.at[number], {"rep": mate})
    for number in order:
        if pieces[number][3] is not None:
            arrive(columns(pieces[number][1], number, 1 - core), f_recv.at[number])
    for kind, dst in enumerate((ry_ref, rg_ref)):
        arrive(dst.at[mate], r_recv.at[kind, 1])
        arrive(dst.at[across_of(mate)], r_recv.at[kind, 2])
        src = y_ref if kind == 0 else g_ref
        pltpu.make_async_copy(src, dst.at[rank], q_sem.at[kind + 1]).wait()
    for there, finish_send in late:
        if there is None:
            finish_send()
        else:
            pl.when(there)(finish_send)


def reduce_grads(count, grads, y_rows, g_rows):
    outer, inner = grid_of(count)
    kinds = len(grads)
    shapes = [(grad.shape[1], grad.shape[2] // 2, grad.dtype) for grad in grads[:-1]]
    shapes.append(grads[-1].shape[1:] + (grads[-1].dtype,))
    dma = pltpu.SemaphoreType.DMA
    y_slots = 1 if inner == 2 else inner + 1
    z_slots = 1 if outer == 2 else outer + 1
    scratch = []
    for lead in ((outer, inner), (outer, inner), (y_slots, outer), (z_slots,), ()):
        scratch += [pltpu.VMEM(lead + (a, b), dtype) for a, b, dtype in shapes]
    scratch += [
        dma((kinds,)), dma((kinds,)), dma((kinds,)),
        dma((2, inner, kinds)), dma((y_slots, kinds)),
        dma((2, outer, kinds)), dma((z_slots, kinds)),
        dma((kinds,)), dma((kinds,)), dma((kinds,)), dma((kinds,)),
        dma((2, 3)), dma((2, 3)), dma((3,)),
    ]
    return pl.pallas_call(
        partial(reduce_kernel, outer, inner, kinds),
        out_shape=tuple(jax.ShapeDtypeStruct(grad.shape[1:], jnp.float32) for grad in grads) + (
            jax.ShapeDtypeStruct((4,) + y_rows.shape, y_rows.dtype),
            jax.ShapeDtypeStruct((4,) + g_rows.shape, g_rows.dtype),
        ),
        in_specs=[ANY] * (kinds + 2),
        out_specs=(VMEM,) * kinds + (ANY, ANY),
        scratch_shapes=scratch,
        compiler_params=pltpu.CompilerParams(
            collective_id=2, has_side_effects=True, vmem_limit_bytes=VMEM_LIMIT
        ),
        name="reduce_and_return",
    )(*(grad.reshape((outer, inner) + grad.shape[1:]) for grad in grads), y_rows, g_rows)


def home_kernel(tab_ref, ry_ref, rg_ref, y_ref, g_ref):
    base = lax.axis_index("rep") * y_ref.shape[0]

    def fetch(block, carry):
        index = tab_ref[DEST_AT + base + block]
        safe = jnp.maximum(index, 0)
        for src, dst in ((ry_ref, y_ref), (rg_ref, g_ref)):
            value = src[safe // SLOTS, safe % SLOTS]
            dst[block] = jnp.where(index >= 0, value, jnp.zeros_like(value))
        return carry

    lax.fori_loop(0, y_ref.shape[0], fetch, 0)


def bring_home(table, ry, rg, blocks):
    shape = jax.ShapeDtypeStruct((blocks,) + ry.shape[2:], ry.dtype)
    return pl.pallas_call(
        home_kernel,
        out_shape=(shape, shape),
        in_specs=[SMEM, VMEM, VMEM],
        out_specs=(VMEM, VMEM),
        compiler_params=pltpu.CompilerParams(vmem_limit_bytes=VMEM_LIMIT),
        name="place_rows",
    )(table, ry, rg)


D = H * DH
ROWS = SLOTS * BLK
SIDES = SLOTS * (BLK // GBLK)
SIDE_ROWS = 48
ALL_ROWS = ROWS + SIDE_ROWS
QT = 128
WIN = 384
TILES = ROWS // QT
QUAD = 256
FF_TILE = 256
GELU_C = 0.7978845608028654
GELU_A = 0.044715
F32, BF16 = jnp.float32, jnp.bfloat16


def mm(left, right):
    return lax.dot_general(left, right, (((1,), (0,)), ((), ())), preferred_element_type=F32)


def mm_cols(left, right):
    return lax.dot_general(left, right, (((1,), (1,)), ((), ())), preferred_element_type=F32)


def mm_rows(left, right):
    return lax.dot_general(left, right, (((0,), (0,)), ((), ())), preferred_element_type=F32)


def iota(shape, axis):
    return lax.broadcasted_iota(jnp.int32, shape, axis)


def pick_by(index, values, other):
    out = jnp.full(index.shape, other, jnp.int32)
    for number, value in enumerate(values):
        out = jnp.where(index == number, value, out)
    return out


def slot_info(tab_ref, rank):
    seg = [tab_ref[SEG_AT + rank * SLOTS + slot] for slot in range(SLOTS)]
    length = [tab_ref[LEN_AT + rank * SLOTS + slot] for slot in range(SLOTS)]
    return seg, length


def valid_column(tab_ref, rank):
    _, length = slot_info(tab_ref, rank)
    row = iota((ROWS, 1), 0)
    return ((row % BLK) < pick_by(row // BLK, length, 0)).astype(F32)


def pooling(tab_ref, rank):
    _, length = slot_info(tab_ref, rank)
    row = iota((1, ROWS), 1)
    block = jnp.where((row % BLK) < pick_by(row // BLK, length, 0), row // GBLK, -1)
    return jnp.where(iota((SIDE_ROWS, ROWS), 0) == block, 1.0, 0.0).astype(BF16)


def key_segments(tab_ref, rank, first_block, index):
    blocks = WIN // BLK
    base = rank * SLOTS + first_block
    seg = [tab_ref[SEG_AT + base + step] for step in range(blocks)]
    length = [tab_ref[LEN_AT + base + step] for step in range(blocks)]
    alive = (index % BLK) < pick_by(index // BLK, length, 0)
    return jnp.where(alive, pick_by(index // BLK, seg, -2), -2)


def side_segments(tab_ref, rank, index):
    seg, length = slot_info(tab_ref, rank)
    per = BLK // GBLK
    alive = (index % per) * GBLK < pick_by(index // per, length, 0)
    return jnp.where(alive, pick_by(index // per, seg, -2), -2)


def tile_bias(tab_ref, rank, tile, first_row, keys_axis):
    qs, ks, gs = ((QT, 1), (1, WIN), (1, SIDE_ROWS)) if keys_axis == 1 else ((1, QT), (WIN, 1), (SIDE_ROWS, 1))
    q_index = iota(qs, 1 - keys_axis)
    k_index = iota(ks, keys_axis)
    g_index = iota(gs, keys_axis)
    base = SEG_AT + rank * SLOTS + tile * (QT // BLK)
    q_seg = pick_by(q_index // BLK, [tab_ref[base + step] for step in range(QT // BLK)], -1)
    k_seg = key_segments(tab_ref, rank, first_row // BLK, k_index)
    g_seg = side_segments(tab_ref, rank, g_index)
    gap = (q_index + tile * QT) - (k_index + first_row)
    local = (jnp.abs(gap) <= RADIUS) & (q_seg == k_seg)
    return jnp.where(local, 0.0, MASKED_SCORE), jnp.where(q_seg == g_seg, 0.0, MASKED_SCORE)


def window_start(tile):
    return pl.multiple_of(jnp.clip(tile - 1, 0, TILES - WIN // QT) * QT, QT)


def head_stack(rows):
    lane = iota(rows.shape, 1) // DH
    zero = jnp.zeros_like(rows)
    return jnp.concatenate([jnp.where(lane == head, rows, zero) for head in range(QUAD // DH)], axis=0)


def head_merge(stacked):
    lane = iota((QT, QUAD), 1) // DH
    out = stacked[:QT]
    for head in range(1, QUAD // DH):
        out = jnp.where(lane == head, stacked[head * QT : (head + 1) * QT], out)
    return out


def gains_of(gc_ref):
    count = gc_ref.shape[0]
    part = D // count
    lane, column = iota((128, D), 0), iota((128, D), 1)
    total = None
    for shard in range(count):
        pick = jnp.where((column == lane + shard * part) & (lane < part), 1.0, 0.0).astype(BF16)
        term = mm(gc_ref[shard], pick)
        total = term if total is None else total + term
    return total


def three_way(value):
    high = value.astype(BF16)
    rest = value - high.astype(F32)
    middle = rest.astype(BF16)
    return high, middle, (rest - middle.astype(F32)).astype(BF16)


def spread_gain_grads(value, dc_ref):
    count = dc_ref.shape[0] if len(dc_ref.shape) == 3 else dc_ref.shape[0] * dc_ref.shape[1]
    part = D // count
    column, lane = iota((D, 128), 0), iota((D, 128), 1)
    parts = three_way(value)
    for shard in range(count):
        pick = jnp.where((column == lane + shard * part) & (lane < part), 1.0, 0.0).astype(BF16)
        place = dc_ref.at[shard] if len(dc_ref.shape) == 3 else dc_ref.at[shard // dc_ref.shape[1], shard % dc_ref.shape[1]]
        place[...] = mm(parts[0], pick) + mm(parts[1], pick) + mm(parts[2], pick)


def mean_square(value):
    return jnp.mean(value * value, axis=-1, keepdims=True)


def forward_norm(tab_ref, rank, x_ref, gains, n_ref):
    for tile in range(TILES):
        rows = pl.ds(tile * QT, QT)
        value = x_ref[rows, :].astype(F32)
        n_ref[rows, :] = (value * lax.rsqrt(mean_square(value) + EPSILON) * gains[0:1]).astype(BF16)
    side = mm(pooling(tab_ref, rank), n_ref[:ROWS, :])
    n_ref[ROWS:, :] = (side * lax.rsqrt(mean_square(side) + EPSILON) * gains[1:2]).astype(BF16)


def forward_project(n_ref, w_ref, qkv_ref):
    def step(tile, carry):
        cols = pl.ds(pl.multiple_of(tile * QUAD, QUAD), QUAD)
        qkv_ref[:, cols] = mm(n_ref[...], w_ref[:, cols]).astype(BF16)
        return carry

    lax.fori_loop(0, 3 * D // QUAD, step, 0)


def forward_attention(tab_ref, rank, qkv_ref, att_ref, lse_ref):
    def step(tile, carry):
        first = window_start(tile)
        bias, side_bias = tile_bias(tab_ref, rank, tile, first, 1)
        rows = pl.ds(pl.multiple_of(tile * QT, QT), QT)
        window = pl.ds(first, WIN)
        lse = jnp.zeros((QT, 128), F32)
        lane = iota((QT, 128), 1)
        for quad in range(D // QUAD):
            low = quad * QUAD
            query = head_stack(qkv_ref[rows, low : low + QUAD])
            scores = mm_cols(query, qkv_ref[window, D + low : D + low + QUAD])
            side_scores = mm_cols(query, qkv_ref[ROWS:, D + low : D + low + QUAD])
            local, sides, scale = [], [], []
            for head in range(QUAD // DH):
                part = slice(head * QT, (head + 1) * QT)
                one = scores[part] + bias
                two = side_scores[part] + side_bias
                peak = jnp.maximum(
                    jnp.max(one, axis=-1, keepdims=True), jnp.max(two, axis=-1, keepdims=True)
                )
                one, two = jnp.exp(one - peak), jnp.exp(two - peak)
                total = jnp.sum(one, axis=-1, keepdims=True) + jnp.sum(two, axis=-1, keepdims=True)
                local.append(one.astype(BF16))
                sides.append(two.astype(BF16))
                scale.append(1.0 / total)
                lse = jnp.where(lane == quad * (QUAD // DH) + head, peak + jnp.log(total), lse)
            mixed = mm(jnp.concatenate(local, axis=0), qkv_ref[window, 2 * D + low : 2 * D + low + QUAD])
            mixed = mixed + mm(
                jnp.concatenate(sides, axis=0), qkv_ref[ROWS:, 2 * D + low : 2 * D + low + QUAD]
            )
            mixed = mixed * jnp.concatenate(scale, axis=0)
            att_ref[rows, low : low + QUAD] = head_merge(mixed).astype(BF16)
        lse_ref[tile] = jnp.transpose(lse)[:16]
        return carry

    lax.fori_loop(0, TILES, step, 0)


def feed_forward(tab_ref, rank, x_ref, cot_ref, att_ref, gains, w_ref, wb_ref,
                 y_ref, gh_ref, ga_ref, dg_ref, du_ref, db_ref, do_ref,
                 h1_ref, nt_ref, ntt_ref, gres_ref, h2_ref, gg_ref, gu_ref, gn_ref):
    hidden = wb_ref.shape[0]
    gate_at = 4 * D
    valid = valid_column(tab_ref, rank)
    gain = gains[2:3]
    for tile in range(TILES):
        rows = pl.ds(tile * QT, QT)
        value = x_ref[rows, :].astype(F32) + mm(att_ref[rows, :], w_ref[:, 3 * D : 4 * D])
        h1_ref[rows, :] = value
        normed = (value * lax.rsqrt(mean_square(value) + EPSILON) * gain).astype(BF16)
        nt_ref[rows, :] = normed
        ntt_ref[:, tile * QT : (tile + 1) * QT] = jnp.transpose(normed)
        gres_ref[rows, :] = (cot_ref[rows, :].astype(F32) * valid[tile * QT : (tile + 1) * QT]).astype(BF16)

    def inward(tile, carry):
        at = pl.multiple_of(tile * FF_TILE, FF_TILE)
        cols = pl.ds(at, FF_TILE)
        gate = mm(nt_ref[...], w_ref[:, pl.ds(gate_at + at, FF_TILE)])
        up = mm(nt_ref[...], w_ref[:, pl.ds(gate_at + hidden + at, FF_TILE)])
        back = mm_cols(gres_ref[...], wb_ref[cols, :])
        square = gate * gate
        bend = jnp.tanh(GELU_C * (gate * (1.0 + GELU_A * square)))
        half = 0.5 * (1.0 + bend)
        act = gate * half
        slope = half + (0.5 * GELU_C) * gate * (1.0 - bend * bend) * (1.0 + (3.0 * GELU_A) * square)
        h2_ref[:, cols] = (act * up).astype(BF16)
        gg_ref[:, cols] = (back * up * slope).astype(BF16)
        gu_ref[:, cols] = (back * act).astype(BF16)
        return carry

    lax.fori_loop(0, hidden // FF_TILE, inward, 0)

    def outward(tile, carry):
        cols = pl.ds(pl.multiple_of(tile * QUAD, QUAD), QUAD)
        value = h1_ref[:, cols] + mm(h2_ref[...], wb_ref[:, cols])
        y_ref[:, cols] = (value * valid).astype(BF16)
        gn_ref[:, cols] = mm_cols(gg_ref[...], w_ref[cols, gate_at : gate_at + hidden]) + mm_cols(
            gu_ref[...], w_ref[cols, gate_at + hidden :]
        )
        return carry

    lax.fori_loop(0, D // QUAD, outward, 0)

    def weights(tile, carry):
        at = pl.multiple_of(tile * FF_TILE, FF_TILE)
        cols = pl.ds(at, FF_TILE)
        dg_ref[:, cols] = mm(ntt_ref[...], gg_ref[:, cols]).astype(BF16)
        du_ref[:, cols] = mm(ntt_ref[...], gu_ref[:, cols]).astype(BF16)
        db_ref[cols, :] = mm_rows(h2_ref[:, cols], gres_ref[...]).astype(BF16)
        return carry

    lax.fori_loop(0, hidden // FF_TILE, weights, 0)

    gain_grad = jnp.zeros((1, D), F32)
    for tile in range(TILES):
        rows = pl.ds(tile * QT, QT)
        value, grad = h1_ref[rows, :], gn_ref[rows, :]
        root = lax.rsqrt(mean_square(value) + EPSILON)
        unit = value * root
        gain_grad = gain_grad + jnp.sum(grad * unit, axis=0, keepdims=True)
        grad = grad * gain
        grad = gres_ref[rows, :].astype(F32) + root * (
            grad - unit * jnp.mean(grad * unit, axis=-1, keepdims=True)
        )
        gh_ref[rows, :] = grad
        low = grad.astype(BF16)
        nt_ref[rows, :] = low
        ga_ref[rows, :] = mm_cols(low, w_ref[:, 3 * D : 4 * D]).astype(BF16)

    def out_weight(tile, carry):
        cols = pl.ds(pl.multiple_of(tile * QUAD, QUAD), QUAD)
        do_ref[cols, :] = mm_rows(att_ref[:, cols], nt_ref[...]).astype(BF16)
        return carry

    lax.fori_loop(0, D // QUAD, out_weight, 0)
    return gain_grad


def backward_attention_start(dk_ref, dv_ref):
    dk_ref[...] = jnp.zeros_like(dk_ref)
    dv_ref[...] = jnp.zeros_like(dv_ref)


def backward_attention_tiles(tab_ref, rank, qkv_ref, att_ref, ga_ref, lse_ref, dqkv_ref, dk_ref, dv_ref, begin, end):
    heads = QUAD // DH
    marks = jnp.where(iota((16, D), 1) // DH == iota((16, D), 0), 1.0, 0.0).astype(BF16)

    def step(tile, carry):
        first = window_start(tile)
        bias, side_bias = tile_bias(tab_ref, rank, tile, first, 0)
        bias = jnp.concatenate([bias, side_bias], axis=0)
        rows = pl.ds(pl.multiple_of(tile * QT, QT), QT)
        window = pl.ds(first, WIN)
        product = ga_ref[rows, :].astype(F32) * att_ref[rows, :].astype(F32)
        high = product.astype(BF16)
        rest = (product - high.astype(F32)).astype(BF16)
        centre = mm_cols(marks, high) + mm_cols(marks, rest)
        lse = lse_ref[tile]
        for quad in range(D // QUAD):
            low = quad * QUAD
            query = head_stack(qkv_ref[rows, low : low + QUAD])
            grad = head_stack(ga_ref[rows, low : low + QUAD])
            keys = jnp.concatenate(
                [qkv_ref[window, D + low : D + low + QUAD], qkv_ref[ROWS:, D + low : D + low + QUAD]], axis=0
            )
            values = jnp.concatenate(
                [qkv_ref[window, 2 * D + low : 2 * D + low + QUAD],
                 qkv_ref[ROWS:, 2 * D + low : 2 * D + low + QUAD]], axis=0
            )
            scores = mm_cols(keys, query)
            slopes = mm_cols(values, grad)
            probs, grads = [], []
            for head in range(heads):
                part = slice(head * QT, (head + 1) * QT)
                number = quad * heads + head
                prob = jnp.exp(scores[:, part] + bias - lse[number : number + 1])
                probs.append(prob.astype(BF16))
                grads.append((prob * (slopes[:, part] - centre[number : number + 1])).astype(BF16))
            probs = jnp.concatenate(probs, axis=1)
            grads = jnp.concatenate(grads, axis=1)
            dkey = mm(grads, query)
            dvalue = mm(probs, grad)
            cols = slice(low, low + QUAD)
            dk_ref[window, cols] = dk_ref[window, cols] + dkey[:WIN]
            dk_ref[ROWS:, cols] = dk_ref[ROWS:, cols] + dkey[WIN:]
            dv_ref[window, cols] = dv_ref[window, cols] + dvalue[:WIN]
            dv_ref[ROWS:, cols] = dv_ref[ROWS:, cols] + dvalue[WIN:]
            dqkv_ref[rows, cols] = head_merge(mm_rows(grads, keys)).astype(BF16)
        return carry

    lax.fori_loop(begin, end, step, 0)


def backward_attention_end(dqkv_ref, dk_ref, dv_ref):
    dqkv_ref[ROWS:, :D] = jnp.zeros((SIDE_ROWS, D), BF16)
    dqkv_ref[:, D : 2 * D] = dk_ref[...].astype(BF16)
    dqkv_ref[:, 2 * D :] = dv_ref[...].astype(BF16)


def weight_grads(n_ref, dqkv_ref, refs):
    for number, ref in enumerate(refs):
        def weights(tile, carry):
            at = pl.multiple_of(tile * QUAD, QUAD)
            value = mm_rows(n_ref[...], dqkv_ref[:, pl.ds(number * D + at, QUAD)]).astype(BF16)
            if len(ref.shape) == 4:
                ref[:, :, :, pl.ds(at, QUAD)] = value.reshape(ref.shape[:3] + (QUAD,))
            else:
                ref[:, pl.ds(at, QUAD)] = value
            return carry

        lax.fori_loop(0, D // QUAD, weights, 0)


def backward_project(tab_ref, rank, x_ref, gh_ref, gains, n_ref, dqkv_ref, w_ref, gn_ref, g_ref):
    def step(tile, carry):
        cols = pl.ds(pl.multiple_of(tile * QUAD, QUAD), QUAD)
        gn_ref[:, cols] = mm_cols(dqkv_ref[...], w_ref[cols, : 3 * D])
        return carry

    lax.fori_loop(0, D // QUAD, step, 0)
    pool = pooling(tab_ref, rank)
    side = mm(pool, n_ref[:ROWS, :])
    root = lax.rsqrt(mean_square(side) + EPSILON)
    unit = side * root
    grad = gn_ref[ROWS:, :]
    side_gain = jnp.sum(grad * unit, axis=0, keepdims=True)
    grad = grad * gains[1:2]
    grad = root * (grad - unit * jnp.mean(grad * unit, axis=-1, keepdims=True))
    parts = three_way(grad)
    gain_grad = jnp.zeros((1, D), F32)
    for tile in range(TILES):
        rows = pl.ds(tile * QT, QT)
        spread = pool[:, tile * QT : (tile + 1) * QT]
        total = gn_ref[rows, :] + mm_rows(spread, parts[0]) + mm_rows(spread, parts[1])
        value = x_ref[rows, :].astype(F32)
        root = lax.rsqrt(mean_square(value) + EPSILON)
        unit = value * root
        gain_grad = gain_grad + jnp.sum(total * unit, axis=0, keepdims=True)
        total = total * gains[0:1]
        value = (
            gh_ref[rows, :] + root * (total - unit * jnp.mean(total * unit, axis=-1, keepdims=True))
        ).astype(BF16)
        if len(g_ref.shape) == 3:
            g_ref[pl.ds(tile * (QT // BLK), QT // BLK)] = value.reshape(QT // BLK, BLK, D)
        else:
            g_ref[rows, :] = value
    return gain_grad, side_gain


def first_kernel(tab_ref, x_ref, gc_ref, w_ref, n_ref, qkv_ref, att_ref, lse_ref):
    rank = lax.axis_index("rep")
    gains = gains_of(gc_ref)
    forward_norm(tab_ref, rank, x_ref, gains, n_ref)
    forward_project(n_ref, w_ref, qkv_ref)
    forward_attention(tab_ref, rank, qkv_ref, att_ref, lse_ref)


def second_kernel(tab_ref, x_ref, cot_ref, att_ref, gc_ref, w_ref, wb_ref,
                  y_ref, gh_ref, ga_ref, dg_ref, du_ref, db_ref, do_ref, gain_ref, *scratch):
    rank = lax.axis_index("rep")
    gain_ref[...] = feed_forward(tab_ref, rank, x_ref, cot_ref, att_ref, gains_of(gc_ref), w_ref, wb_ref,
                                 y_ref, gh_ref, ga_ref, dg_ref, du_ref, db_ref, do_ref, *scratch)


def third_kernel(tab_ref, x_ref, gh_ref, ga_ref, att_ref, lse_ref, n_ref, qkv_ref, gain_ref, gc_ref, w_ref,
                 g_ref, dw_ref, dc_ref, dqkv_ref, dk_ref, dv_ref, gn_ref):
    rank = lax.axis_index("rep")
    gains = gains_of(gc_ref)
    backward_attention_start(dk_ref, dv_ref)
    backward_attention_tiles(tab_ref, rank, qkv_ref, att_ref, ga_ref, lse_ref, dqkv_ref, dk_ref, dv_ref, 0, TILES)
    backward_attention_end(dqkv_ref, dk_ref, dv_ref)
    weight_grads(n_ref, dqkv_ref, [dw_ref.at[:, i * D : (i + 1) * D] for i in range(3)])
    one, side = backward_project(tab_ref, rank, x_ref, gh_ref, gains, n_ref, dqkv_ref, w_ref, gn_ref, g_ref)
    grads = jnp.concatenate([one, side, gain_ref[...], jnp.zeros((5, D), F32)], axis=0)
    spread_gain_grads(grads, dc_ref)


def forward_layer(tab, x, cot, gc, w, wb):
    hidden = wb.shape[0]
    shape = jax.ShapeDtypeStruct
    params = pltpu.CompilerParams(vmem_limit_bytes=VMEM_LIMIT)
    n, qkv, att, lse = pl.pallas_call(
        first_kernel,
        out_shape=(shape((ALL_ROWS, D), BF16), shape((ALL_ROWS, 3 * D), BF16), shape((ROWS, D), BF16),
                   shape((TILES, 16, QT), F32)),
        in_specs=[SMEM, VMEM, VMEM, pl.BlockSpec((D, 3 * D), lambda step: (0, 0))],
        grid=(1,),
        out_specs=(VMEM,) * 4,
        compiler_params=params,
        name="attend",
    )(tab, x, gc, w)
    outs = pl.pallas_call(
        second_kernel,
        out_shape=(shape((ROWS, D), BF16), shape((ROWS, D), F32), shape((ROWS, D), BF16),
                   shape((D, hidden), BF16), shape((D, hidden), BF16), shape((hidden, D), BF16), shape((D, D), BF16),
                   shape((1, D), F32)),
        in_specs=[SMEM] + [VMEM] * 6,
        out_specs=(VMEM,) * 8,
        scratch_shapes=[pltpu.VMEM((ROWS, D), F32), pltpu.VMEM((ROWS, D), BF16), pltpu.VMEM((D, ROWS), BF16),
                        pltpu.VMEM((ROWS, D), BF16), pltpu.VMEM((ROWS, hidden), BF16),
                        pltpu.VMEM((ROWS, hidden), BF16), pltpu.VMEM((ROWS, hidden), BF16),
                        pltpu.VMEM((ROWS, D), F32)],
        compiler_params=params,
        name="feed_forward",
    )(tab, x, cot, att, gc, w, wb)
    return (n, qkv, att, lse) + outs


def backward_layer(tab, x, gh, ga, att, lse, n, qkv, gain, gc, w):
    shape = jax.ShapeDtypeStruct
    return pl.pallas_call(
        third_kernel,
        out_shape=(shape((ROWS, D), BF16), shape((D, 3 * D), BF16), shape((gc.shape[0], 8, 128), F32)),
        in_specs=[SMEM] + [VMEM] * 9 + [pl.BlockSpec((D, 3 * D), lambda step: (0, 0))],
        grid=(1,),
        out_specs=(VMEM,) * 3,
        scratch_shapes=[pltpu.VMEM((ALL_ROWS, 3 * D), BF16), pltpu.VMEM((ALL_ROWS, D), F32),
                        pltpu.VMEM((ALL_ROWS, D), F32), pltpu.VMEM((ALL_ROWS, D), F32)],
        compiler_params=pltpu.CompilerParams(vmem_limit_bytes=VMEM_LIMIT),
        name="attend_back",
    )(tab, x, gh, ga, att, lse, n, qkv, gain, gc, w)


class Links:
    def __init__(self, outer, inner):
        self.outer, self.inner = outer, inner
        self.rank, self.spot = lax.axis_index("rep"), lax.axis_index("fsdp")
        self.core = self.rank % 2
        self.row, self.col = self.spot // inner, self.spot % inner
        self.mate, self.across = core_of(self.rank), across_of(self.rank)
        self.late = []

    def greet(self):
        barrier = pltpu.get_barrier_semaphore()
        neighbours = (
            (self.row + 1 < self.outer, {"fsdp": self.spot + self.inner}),
            (self.row > 0, {"fsdp": self.spot - self.inner}),
            (self.col + 1 < self.inner, {"fsdp": self.spot + 1}),
            (self.col > 0, {"fsdp": self.spot - 1}),
        )
        amount = jnp.int32(2)
        for there, device in neighbours:
            amount = amount + there.astype(jnp.int32)

            @pl.when(there)
            def _():
                pl.semaphore_signal(barrier, inc=1, device_id=device, device_id_type=MESH)

        for device in (self.mate, self.across):
            pl.semaphore_signal(barrier, inc=1, device_id={"rep": device}, device_id_type=MESH)
        pl.semaphore_wait(barrier, amount)

    def send(self, there, src, dst, ssem, rsem, device):
        def describe():
            return pltpu.make_async_remote_copy(
                src_ref=src, dst_ref=dst, send_sem=ssem, recv_sem=rsem,
                device_id=device, device_id_type=MESH,
            )

        if there is None:
            describe().start()
        else:
            @pl.when(there)
            def _():
                describe().start()

        self.late.append((there, lambda: describe().wait_send()))

    def arrive(self, place, rsem, spare):
        pltpu.make_async_remote_copy(
            src_ref=place, dst_ref=place, send_sem=spare, recv_sem=rsem,
            device_id={"rep": self.mate}, device_id_type=MESH,
        ).wait_recv()

    def drain(self):
        for there, finish in self.late:
            if there is None:
                finish()
            else:
                pl.when(there)(finish)


def halves(ref, which):
    half = ref.shape[-1] // 2
    cols = pl.ds(pl.multiple_of(which * half, 128), half)
    return ref.at[:, :, :, cols] if len(ref.shape) == 4 else ref.at[:, cols]


class Reduction:
    def __init__(self, links, source, total, mine, crecv, yrecv, zrecv, xrecv, sems, number):
        self.links, self.source, self.total, self.mine = links, source, total, mine
        self.crecv, self.yrecv, self.zrecv, self.xrecv = crecv, yrecv, zrecv, xrecv
        self.sems, self.number = sems, number
        self.whole = total.shape[-1] % 256 != 0
        self.load = None

    def sem(self, name, *index):
        return self.sems[name].at[index + (self.number,)]

    def begin(self):
        links = self.links
        other = self.source if self.whole else halves(self.source, 1 - links.core)
        links.send(None, other, self.crecv, self.sem("c_send"), self.sem("c_recv"), {"rep": links.mate})
        if self.mine is None:
            self.mine = self.source if self.whole else halves(self.source, links.core)
        else:
            own = self.source if self.whole else halves(self.source, links.core)
            self.load = pltpu.make_async_copy(own, self.mine, self.sem("m_sem"))
            self.load.start()

    def pair(self):
        links = self.links
        if self.load is not None:
            self.load.wait()
        links.arrive(self.crecv, self.sem("c_recv"), self.sems["spare"].at[0])
        inner = links.inner

        def add(index, carry):
            row, col = index // inner, index % inner
            self.mine[row, col] = self.mine[row, col] + self.crecv[row, col]
            return carry

        lax.fori_loop(0, links.outer * inner, add, 0)
        links.send(None, self.mine.at[:, 1 - links.col], self.yrecv, self.sem("y_send"), self.sem("y_recv"),
                   {"fsdp": links.spot + 1 - 2 * links.col})

    def slot(self, way, place, dest):
        return dest - place if way == 0 else self.links.outer - place + dest

    def pass_on(self, way, dest, first):
        links = self.links
        step = 1 if way == 0 else -1
        place, size = links.row, links.outer
        passes = place < dest if way == 0 else place > dest
        start = place == 0 if way == 0 else place == size - 1
        mine = self.mine.at[dest, links.col]
        put = self.slot(way, place + step, dest)
        there = jnp.logical_and(passes, start if first else jnp.logical_not(start))
        if not first:
            got = self.slot(way, place, dest)

            @pl.when(there)
            def _():
                links.arrive(self.zrecv.at[got], self.sem("z_recv", got), self.sems["spare"].at[0])
                mine[...] = mine[...] + self.zrecv[got]

        links.send(there, mine, self.zrecv.at[put], self.sem("z_send", way, dest), self.sem("z_recv", put),
                   {"fsdp": links.spot + step * links.inner})

    def column(self):
        links = self.links
        links.arrive(self.yrecv, self.sem("y_recv"), self.sems["spare"].at[0])

        def add(index, carry):
            self.mine[index, links.col] = self.mine[index, links.col] + self.yrecv[index]
            return carry

        lax.fori_loop(0, links.outer, add, 0)
        for far in range(links.outer - 1, 0, -1):
            self.pass_on(0, far, True)
            self.pass_on(1, links.outer - 1 - far, True)

    def line(self):
        links = self.links
        size, place = links.outer, links.row
        for far in range(size - 1, 0, -1):
            self.pass_on(0, far, False)
            self.pass_on(1, size - 1 - far, False)
        mine = self.mine.at[place, links.col]
        for way in range(2):
            got = self.slot(way, place, place)

            @pl.when(place > 0 if way == 0 else place < size - 1)
            def _():
                links.arrive(self.zrecv.at[got], self.sem("z_recv", got), self.sems["spare"].at[0])
                mine[...] = mine[...] + self.zrecv[got]

        links.send(None, mine, self.xrecv, self.sem("x_send"), self.sem("x_recv"), {"rep": links.across})

    def finish(self):
        links = self.links
        links.arrive(self.xrecv, self.sem("x_recv"), self.sems["spare"].at[0])
        value = self.mine[links.row, links.col].astype(F32) + self.xrecv[...].astype(F32)
        if self.whole:
            self.total[...] = value
            return
        place = halves(self.total, links.core)
        place[...] = value
        links.send(None, place, place, self.sem("f_send"), self.sem("f_recv"), {"rep": links.mate})

    def settle(self):
        if not self.whole:
            self.links.arrive(
                halves(self.total, 1 - self.links.core), self.sem("f_recv"), self.sems["spare"].at[0]
            )


SEM_NAMES = ("c_send", "c_recv", "m_sem", "y_send", "y_recv", "z_send", "z_recv", "x_send", "x_recv",
             "f_send", "f_recv", "r_send", "r_recv", "own", "spare")


class Return:
    def __init__(self, links, source, home, sems, kind):
        self.links, self.source, self.home, self.sems, self.kind = links, source, home, sems, kind

    def begin(self):
        links = self.links
        dst = self.home.at[links.rank]
        for way, device in enumerate((links.across, links.mate)):
            links.send(None, self.source, dst, self.sems["r_send"].at[self.kind, way],
                       self.sems["r_recv"].at[self.kind, way], {"rep": device})
        self.copy = pltpu.make_async_copy(self.source, dst, self.sems["own"].at[self.kind])
        self.copy.start()

    def relay(self):
        links = self.links
        place = self.home.at[links.across]
        links.arrive(place, self.sems["r_recv"].at[self.kind, 0], self.sems["spare"].at[0])
        links.send(None, place, place, self.sems["r_send"].at[self.kind, 2],
                   self.sems["r_recv"].at[self.kind, 2], {"rep": links.mate})

    def settle(self):
        links, sem = self.links, self.sems["r_recv"]
        links.arrive(self.home.at[links.mate], sem.at[self.kind, 1], self.sems["spare"].at[0])
        links.arrive(self.home.at[across_of(links.mate)], sem.at[self.kind, 2], self.sems["spare"].at[0])
        self.copy.wait()


def back_kernel(outer, inner, early, *refs):
    (tab_ref, x_ref, gh_ref, ga_ref, att_ref, lse_ref, n_ref, qkv_ref, gain_ref, gc_ref, w_ref), refs = refs[:11], refs[11:]
    grads, (y_ref,), refs = refs[:early], refs[early : early + 1], refs[early + 1 :]
    kinds = early + 4
    totals, (ry_ref, rg_ref), refs = refs[:kinds], refs[kinds : kinds + 2], refs[kinds + 2 :]
    (dq_ref, dkw_ref, dvw_ref, dc_ref), refs = refs[:4], refs[4:]
    (g_ref, dqkv_ref, dk_ref, dv_ref), refs = refs[:4], refs[4:]
    mines, refs = list(refs[:early]) + [None] * 3 + [refs[early]], refs[early + 1 :]
    crecv, yrecv, zrecv, xrecv = (refs[kinds * i : kinds * (i + 1)] for i in range(4))
    sems = dict(zip(SEM_NAMES, refs[4 * kinds :]))
    links = Links(outer, inner)
    rank = links.rank
    sources = list(grads) + [dq_ref, dkw_ref, dvw_ref, dc_ref]
    tasks = [
        Reduction(links, sources[i], totals[i], mines[i], crecv[i], yrecv[i], zrecv[i], xrecv[i], sems, i)
        for i in range(kinds)
    ]
    rows_y, rows_g = Return(links, y_ref, ry_ref, sems, 0), Return(links, g_ref, rg_ref, sems, 1)

    links.greet()
    for task in tasks[:early]:
        task.begin()
    rows_y.begin()
    gains = gains_of(gc_ref)
    for task in tasks[:early]:
        task.pair()
    backward_attention_start(dk_ref, dv_ref)
    backward_attention_tiles(tab_ref, rank, qkv_ref, att_ref, ga_ref, lse_ref, dqkv_ref, dk_ref, dv_ref, 0, TILES)
    tasks[0].column()
    backward_attention_end(dqkv_ref, dk_ref, dv_ref)
    weight_grads(n_ref, dqkv_ref, (dq_ref, dkw_ref, dvw_ref))
    for task in tasks[early : early + 3]:
        task.begin()
    rows_y.relay()
    one, side = backward_project(tab_ref, rank, x_ref, gh_ref, gains, n_ref, dqkv_ref, w_ref, dk_ref, g_ref)
    spread_gain_grads(jnp.concatenate([one, side, gain_ref[...], jnp.zeros((5, D), F32)], axis=0), dc_ref)
    rows_g.begin()
    tasks[kinds - 1].begin()
    for task in tasks[early:]:
        task.pair()
    for number in range(kinds):
        if number + 1 < kinds:
            tasks[number + 1].column()
        tasks[number].line()
        if number == 2:
            rows_g.relay()
        if number > 0:
            tasks[number - 1].finish()
    tasks[-1].finish()
    rows_y.settle()
    rows_g.settle()
    for task in tasks:
        task.settle()
    links.drain()


def attend_back(count, table, x, gh, ga, att, lse, n, qkv, gain, gc, w, grads, y):
    outer, inner = grid_of(count)
    part = D // count
    early = len(grads)
    kinds = early + 4
    grads = [grad.reshape((outer, inner, -1) + grad.shape[1:]) for grad in grads]
    shapes = [grad.shape[2:] for grad in grads] + [(part, D)] * 3 + [(8, 128)]
    dtypes = [BF16] * (kinds - 1) + [F32]
    halved = [(a, b // 2 if b % 256 == 0 else b) for a, b in shapes]
    dma = pltpu.SemaphoreType.DMA
    scratch = [pltpu.VMEM((outer, inner) + shape, dtype) for shape, dtype in zip(shapes[early:], dtypes[early:])]
    scratch += [pltpu.VMEM((SLOTS, BLK, D), BF16), pltpu.VMEM((ALL_ROWS, 3 * D), BF16),
                pltpu.VMEM((ALL_ROWS, D), F32), pltpu.VMEM((ALL_ROWS, D), F32)]
    scratch += [pltpu.VMEM((outer, inner) + shape, BF16) for shape in halved[:early]]
    scratch += [pltpu.VMEM((outer, inner) + halved[-1], F32)]
    for lead in ((outer, inner), (outer,), (outer + 1,), ()):
        scratch += [pltpu.VMEM(lead + shape, dtype) for shape, dtype in zip(halved, dtypes)]
    one = dma((kinds,))
    scratch += [one, one, one, one, one, dma((2, outer, kinds)), dma((outer + 1, kinds)), one, one, one, one,
                dma((2, 3)), dma((2, 3)), dma((2,)), dma((1,))]
    rows = jax.ShapeDtypeStruct((4, SLOTS, BLK, D), BF16)
    outs = pl.pallas_call(
        partial(back_kernel, outer, inner, early),
        out_shape=tuple(jax.ShapeDtypeStruct(shape, F32) for shape in shapes) + (rows, rows),
        grid=(1,),
        in_specs=[SMEM] + [VMEM] * 9 + [pl.BlockSpec((D, 3 * D), lambda step: (0, 0))] + [ANY] * early + [VMEM],
        out_specs=(VMEM,) * kinds + (ANY, ANY),
        scratch_shapes=scratch,
        compiler_params=pltpu.CompilerParams(
            collective_id=2, has_side_effects=True, vmem_limit_bytes=VMEM_LIMIT
        ),
        name="attend_back_and_reduce",
    )(table, x, gh, ga, att, lse, n, qkv, gain, gc, w, *grads, y.reshape(SLOTS, BLK, D))
    return outs[:kinds], outs[kinds], outs[kinds + 1]


def per_device(count, layer_input, cotangent, lengths, attn_gain, global_gain, query_weight, key_weight,
               value_weight, out_weight, ffn_gain, gate_weight, up_weight, down_weight):
    micro, span, width = layer_input.shape
    hidden = gate_weight.shape[1]
    blocks = micro * span // BLK
    table = deal_table(lengths)
    wa = jnp.concatenate([query_weight, key_weight, value_weight, out_weight, gate_weight, up_weight], axis=1)
    part = attn_gain.shape[0]
    wc = jnp.pad(jnp.stack([attn_gain, global_gain, ffn_gain]), ((0, 13), (0, 128 - part)))
    splits = ((0, 4 * width), (4 * width, 2 * hidden))
    ga, gb, gc, rows, cots = gather_weights(
        count, splits, table,
        layer_input.reshape(blocks, BLK, width), cotangent.reshape(blocks, BLK, width), wa, down_weight, wc,
    )
    x, full = rows.reshape(ROWS, width), ga.reshape(width, -1)
    n, qkv, att, lse, y, gh, gatt, dg, du, db, do, gain = forward_layer(
        table, x, cots.reshape(ROWS, width), gc, full, gb.reshape(-1, width)
    )
    if grid_of(count)[1] == 2 and part % 16 == 0:
        totals, ry, rg = attend_back(count, table, x, gh, gatt, att, lse, n, qkv, gain, gc, full, (dg, du, db, do), y)
        og, ou, ob, oo, oq, ok, ov, oc = totals
    else:
        g, dw, dc = backward_layer(table, x, gh, gatt, att, lse, n, qkv, gain, gc, full)
        grads = [grad.reshape(count, -1, grad.shape[-1]) for grad in (dg, du, db, do, dw, dc)]
        og, ou, ob, oo, ow, oc, ry, rg = reduce_grads(
            count, grads, y.reshape(SLOTS, BLK, width), g.reshape(SLOTS, BLK, width)
        )
        oq, ok, ov = ow[:, :width], ow[:, width : 2 * width], ow[:, 2 * width :]
    y_home, g_home = bring_home(table, ry, rg, blocks)
    return (
        y_home.reshape(layer_input.shape), g_home.reshape(layer_input.shape),
        oc[0, :part], oc[1, :part], oq, ok, ov, oo, oc[2, :part], og, ou, ob,
    )


def solution(mesh):
    rows = P(None, ("rep", "fsdp"), None)
    vector, matrix = P("fsdp"), P("fsdp", None)
    return jax.shard_map(
        partial(per_device, mesh.shape["fsdp"]),
        mesh=mesh,
        in_specs=(rows, rows, P(None, ("rep", "fsdp")), vector, vector, matrix, matrix, matrix, matrix,
                  vector, matrix, matrix, matrix),
        out_specs=(rows, rows, vector, vector, matrix, matrix, matrix, matrix, vector, matrix, matrix, matrix),
        check_vma=False,
    )
```

```python
from functools import partial

import jax
import jax.numpy as jnp
from jax import lax
from jax.experimental import pallas as pl
from jax.experimental.pallas import tpu as pltpu
from jax.sharding import PartitionSpec as P

H = 12
DH = 64
RADIUS = 127
GBLK = 16
BLK = 64
SLOTS = 10
MAX_SEQ_BLOCKS = 5
EPSILON = 1e-06
MASKED_SCORE = -1e30
MESH = pl.DeviceIdType.MESH
VMEM_LIMIT = 60 * 1024 * 1024
SEG_AT, LEN_AT, DEST_AT, TABLE_SIZE = 40, 80, 120, 256

ANY = pl.BlockSpec(memory_space=pl.ANY)
VMEM = pl.BlockSpec(memory_space=pltpu.VMEM)
SMEM = pl.BlockSpec(memory_space=pltpu.SMEM)


def grid_of(count):
    inner = 2 if count <= 8 else 4
    return count // inner, inner


def core_of(rank):
    return rank + 1 - 2 * (rank % 2)


def across_of(rank):
    return (rank + 2) % 4


def lens_kernel(lens_ref, all_ref, send_sem, recv_sem):
    rank = lax.axis_index("rep")
    barrier = pltpu.get_barrier_semaphore()
    for step in range(1, 4):
        pl.semaphore_signal(
            barrier, inc=1, device_id={"rep": (rank + step) % 4}, device_id_type=MESH
        )
    pl.semaphore_wait(barrier, 3)
    copies = []
    for step in range(1, 4):
        copy = pltpu.make_async_remote_copy(
            src_ref=lens_ref,
            dst_ref=all_ref.at[rank],
            send_sem=send_sem.at[step - 1],
            recv_sem=recv_sem.at[step - 1],
            device_id={"rep": (rank + step) % 4},
            device_id_type=MESH,
        )
        copy.start()
        copies.append(copy)
    all_ref[rank] = lens_ref[...]
    for copy in copies:
        copy.wait()


def table_kernel(micro, per_dev, lens_ref, tab_ref, order_ref, count_ref, load_ref):
    total = 4 * micro * per_dev

    def length_at(spot):
        return lens_ref[spot // (micro * per_dev), (spot // per_dev) % micro, spot % per_dev]

    def blocks_of(length):
        return (length + (BLK - 1)) // BLK

    def clear(spot, carry):
        tab_ref[spot] = -1
        return carry

    lax.fori_loop(0, TABLE_SIZE, clear, 0)
    for spot in range(4 * SLOTS):
        tab_ref[LEN_AT + spot] = 0
    for size in range(8):
        count_ref[size] = 0
    for dev in range(4):
        load_ref[dev] = 0

    def tally(spot, carry):
        length = length_at(spot)

        @pl.when(length > 0)
        def _():
            size = blocks_of(length)
            count_ref[size] = count_ref[size] + 1

        return carry

    lax.fori_loop(0, total, tally, 0)
    begin = 0
    for size in range(MAX_SEQ_BLOCKS, 0, -1):
        amount = count_ref[size]
        count_ref[size] = begin
        begin = begin + amount

    def place(spot, carry):
        length = length_at(spot)

        @pl.when(length > 0)
        def _():
            size = blocks_of(length)
            where = count_ref[size]
            order_ref[where] = spot
            count_ref[size] = where + 1

        return carry

    lax.fori_loop(0, total, place, 0)

    def assign(number, carry):
        spot = order_ref[number]
        length = length_at(spot)
        size = blocks_of(length)
        best = jnp.int32(0)
        low = load_ref[0]
        for dev in range(1, 4):
            here = load_ref[dev]
            best = jnp.where(here < low, dev, best)
            low = jnp.minimum(here, low)
        load_ref[best] = low + size

        def put(step, inner):
            slot = best * SLOTS + low + step
            tab_ref[slot] = spot + step
            tab_ref[SEG_AT + slot] = low
            tab_ref[LEN_AT + slot] = jnp.minimum(length - BLK * step, BLK)
            tab_ref[DEST_AT + spot + step] = slot
            return inner

        lax.fori_loop(0, size, put, 0)
        return carry

    lax.fori_loop(0, begin, assign, 0)


def deal_table(lengths):
    micro, per_dev = lengths.shape
    padded = jnp.pad(lengths, ((0, 8 - micro), (0, 128 - per_dev)))
    everyone = pl.pallas_call(
        lens_kernel,
        out_shape=jax.ShapeDtypeStruct((4, 8, 128), jnp.int32),
        in_specs=[VMEM],
        out_specs=VMEM,
        scratch_shapes=[pltpu.SemaphoreType.DMA((3,)), pltpu.SemaphoreType.DMA((3,))],
        compiler_params=pltpu.CompilerParams(collective_id=0, has_side_effects=True),
        name="lens_exchange",
    )(padded)
    return pl.pallas_call(
        partial(table_kernel, micro, per_dev),
        out_shape=jax.ShapeDtypeStruct((TABLE_SIZE,), jnp.int32),
        in_specs=[SMEM],
        out_specs=SMEM,
        scratch_shapes=[
            pltpu.SMEM((4 * micro * per_dev,), jnp.int32),
            pltpu.SMEM((8,), jnp.int32),
            pltpu.SMEM((4,), jnp.int32),
        ],
        name="deal_table",
    )(everyone)


def gather_kernel(
    outer, inner, splits, tab_ref, rows_ref, cots_ref, wa_ref, wb_ref, wc_ref,
    ga_ref, gb_ref, gc_ref, rows_out, cots_out,
    psend, precv, xsend, xrecv,
    z_send, z_recv, y_send, y_recv, c_send, c_recv, own_sem,
    p_send, p_recv, x_send, x_recv,
):
    rank = lax.axis_index("rep")
    spot = lax.axis_index("fsdp")
    core = rank % 2
    row, col = spot // inner, spot % inner
    count = outer * inner
    mate, across = core_of(rank), across_of(rank)
    pieces = [(wa_ref, ga_ref, start, width // 2) for start, width in splits]
    pieces.append((wb_ref, gb_ref, 0, wb_ref.shape[1] // 2))
    pieces.append((wc_ref, gc_ref, 0, None))
    halved = [number for number, piece in enumerate(pieces) if piece[3] is not None]

    barrier = pltpu.get_barrier_semaphore()
    neighbours = (
        (row + 1 < outer, {"fsdp": spot + inner}),
        (row > 0, {"fsdp": spot - inner}),
        (col + 1 < inner, {"fsdp": spot + 1}),
        (col > 0, {"fsdp": spot - 1}),
    )
    amount = jnp.int32(2)
    for there, device in neighbours:
        amount = amount + there.astype(jnp.int32)

        @pl.when(there)
        def _():
            pl.semaphore_signal(barrier, inc=1, device_id=device, device_id_type=MESH)

    for device in (mate, across):
        pl.semaphore_signal(barrier, inc=1, device_id={"rep": device}, device_id_type=MESH)
    pl.semaphore_wait(barrier, amount)

    def cut(ref, number):
        _, _, start, half = pieces[number]
        if half is None:
            return ref
        return ref.at[:, pl.ds(pl.multiple_of(start + core * half, 128), half)]

    def landed(number, shard):
        return cut(pieces[number][1].at[shard], number)

    late = []

    def send(there, src, dst, ssem, rsem, device):
        def describe():
            return pltpu.make_async_remote_copy(
                src_ref=src, dst_ref=dst, send_sem=ssem, recv_sem=rsem,
                device_id=device, device_id_type=MESH,
            )

        if there is None:
            describe().start()
            late.append((None, lambda: describe().wait_send()))
        else:
            @pl.when(there)
            def _():
                describe().start()

            late.append((there, lambda: describe().wait_send()))

    def arrive(number, shard, rsem):
        pltpu.make_async_remote_copy(
            src_ref=landed(number, shard), dst_ref=landed(number, shard),
            send_sem=own_sem.at[0], recv_sem=rsem,
            device_id={"rep": mate}, device_id_type=MESH,
        ).wait_recv()

    def both(first, second):
        return second if first is None else jnp.logical_and(first, second)

    def to_mate(there, number, shard):
        if number not in halved:
            return
        place = landed(number, shard)
        send(there, place, place, c_send.at[number, shard], c_recv.at[number, shard], {"rep": mate})

    def along_row(there, number, line, src):
        shard = line * inner + col
        place = landed(number, shard)
        src = place if src is None else src
        send(both(there, col + 1 < inner), src, place,
             y_send.at[0, 0, line, number], y_recv.at[0, 0, line, number], {"fsdp": spot + 1})
        send(both(there, col > 0), src, place,
             y_send.at[1, 0, line, number], y_recv.at[1, 0, line, number], {"fsdp": spot - 1})

    def from_row(there, number, line):
        for step in range(inner - 1):
            for way, source, onward, target in (
                (0, col - 1 - step, col + 1 < inner, spot + 1),
                (1, col + 1 + step, col > 0, spot - 1),
            ):
                here = jnp.logical_and(source >= 0, source < inner)
                here = both(there, here)
                shard = line * inner + source

                @pl.when(here)
                def _():
                    arrive(number, shard, y_recv.at[way, step, line, number])

                if step + 1 < inner - 1:
                    place = landed(number, shard)
                    send(both(here, onward), place, place,
                         y_send.at[way, step + 1, line, number],
                         y_recv.at[way, step + 1, line, number], {"fsdp": target})
                to_mate(here, number, shard)

    for number, piece in enumerate(pieces):
        src, place = cut(piece[0], number), landed(number, spot)
        send(row + 1 < outer, src, place, z_send.at[0, 0, number], z_recv.at[0, 0, number],
             {"fsdp": spot + inner})
        send(row > 0, src, place, z_send.at[1, 0, number], z_recv.at[1, 0, number],
             {"fsdp": spot - inner})
        along_row(None, number, row, src)
    own = [
        pltpu.make_async_copy(wa_ref, ga_ref.at[spot], own_sem.at[0]),
        pltpu.make_async_copy(wb_ref, gb_ref.at[spot], own_sem.at[1]),
        pltpu.make_async_copy(wc_ref, gc_ref.at[spot], own_sem.at[2]),
    ]
    for copy in own:
        copy.start()

    sources = (rows_ref, cots_ref)
    per_rank = rows_ref.shape[0]

    def picked(kind, target, slot):
        index = tab_ref[target * SLOTS + slot] - rank * per_rank
        mine = jnp.logical_and(index >= 0, index < per_rank)
        value = sources[kind][jnp.clip(index, 0, per_rank - 1)]
        return mine, value

    def mate_copy(kind, part):
        return pltpu.make_async_remote_copy(
            src_ref=psend.at[kind, part], dst_ref=precv.at[kind, part],
            send_sem=p_send.at[kind, part], recv_sem=p_recv.at[kind, part],
            device_id={"rep": mate}, device_id_type=MESH,
        )

    def across_copy(kind):
        return pltpu.make_async_remote_copy(
            src_ref=xsend.at[kind], dst_ref=xrecv.at[kind],
            send_sem=x_send.at[kind], recv_sem=x_recv.at[kind],
            device_id={"rep": across}, device_id_type=MESH,
        )

    for kind, part in ((0, 1), (1, 1), (0, 0), (1, 0)):
        target = mate if part == 0 else across_of(mate)

        def pack(slot, carry):
            mine, value = picked(kind, target, slot)
            psend[kind, part, slot] = jnp.where(mine, value, jnp.zeros_like(value))
            return carry

        lax.fori_loop(0, SLOTS, pack, 0)
        mate_copy(kind, part).start()
    for kind in range(2):
        mate_copy(kind, 1).wait_recv()

        def merge(slot, carry):
            mine, value = picked(kind, across, slot)
            xsend[kind, slot] = jnp.where(mine, value, precv[kind, 1, slot])
            return carry

        lax.fori_loop(0, SLOTS, merge, 0)
        across_copy(kind).start()

    def lines(step):
        return ((row - 1 - step >= 0, row - 1 - step, 0, row + 1 < outer, spot + inner),
                (row + 1 + step < outer, row + 1 + step, 1, row > 0, spot - inner))

    for step in range(outer - 1):
        for number in range(len(pieces)):
            for here, line, way, onward, target in lines(step):
                shard = line * inner + col

                @pl.when(here)
                def _():
                    arrive(number, shard, z_recv.at[way, step, number])

                if step + 1 < outer - 1:
                    place = landed(number, shard)
                    send(jnp.logical_and(here, onward), place, place,
                         z_send.at[way, step + 1, number], z_recv.at[way, step + 1, number],
                         {"fsdp": target})
                along_row(here, number, line, None)
                to_mate(here, number, shard)
        for number in range(len(pieces)):
            if step == 0:
                from_row(None, number, row)
            else:
                for here, line, *_ in lines(step - 1):
                    from_row(here, number, line)
    for number in range(len(pieces)):
        for here, line, *_ in lines(outer - 2):
            from_row(here, number, line)

    outs = (rows_out, cots_out)
    for kind in range(2):
        mate_copy(kind, 0).wait_recv()
        across_copy(kind).wait_recv()

        def finish(slot, carry):
            mine, value = picked(kind, rank, slot)
            outs[kind][slot] = jnp.where(mine, value, precv[kind, 0, slot] + xrecv[kind, slot])
            return carry

        lax.fori_loop(0, SLOTS, finish, 0)

    for shard in range(count):
        @pl.when(shard != spot)
        def _():
            for number in halved:
                other = pieces[number]
                view = other[1].at[shard].at[:, pl.ds(0, other[3])]
                pltpu.make_async_remote_copy(
                    src_ref=view, dst_ref=view, send_sem=own_sem.at[0],
                    recv_sem=c_recv.at[number, shard],
                    device_id={"rep": mate}, device_id_type=MESH,
                ).wait_recv()
    for there, finish_send in late:
        if there is None:
            finish_send()
        else:
            pl.when(there)(finish_send)
    for kind in range(2):
        for part in range(2):
            mate_copy(kind, part).wait_send()
        across_copy(kind).wait_send()
    for copy in own:
        copy.wait()


def gather_weights(count, splits, table, rows, cots, wa, wb, wc):
    outer, inner = grid_of(count)
    block = rows.shape[1:]
    kinds = len(splits) + 2
    dma = pltpu.SemaphoreType.DMA
    bf16 = jnp.bfloat16
    return pl.pallas_call(
        partial(gather_kernel, outer, inner, splits),
        out_shape=(
            jax.ShapeDtypeStruct((count,) + wa.shape, bf16),
            jax.ShapeDtypeStruct((count,) + wb.shape, bf16),
            jax.ShapeDtypeStruct((count,) + wc.shape, bf16),
            jax.ShapeDtypeStruct((SLOTS,) + block, bf16),
            jax.ShapeDtypeStruct((SLOTS,) + block, bf16),
        ),
        in_specs=[SMEM, VMEM, VMEM, VMEM, VMEM, VMEM],
        out_specs=(ANY, ANY, ANY, VMEM, VMEM),
        scratch_shapes=[
            pltpu.VMEM((2, 2, SLOTS) + block, bf16),
            pltpu.VMEM((2, 2, SLOTS) + block, bf16),
            pltpu.VMEM((2, SLOTS) + block, bf16),
            pltpu.VMEM((2, SLOTS) + block, bf16),
            dma((2, outer - 1, kinds)), dma((2, outer - 1, kinds)),
            dma((2, inner - 1, outer, kinds)), dma((2, inner - 1, outer, kinds)),
            dma((kinds, count)), dma((kinds, count)), dma((3,)),
            dma((2, 2)), dma((2, 2)), dma((2,)), dma((2,)),
        ],
        compiler_params=pltpu.CompilerParams(
            collective_id=1, has_side_effects=True, vmem_limit_bytes=VMEM_LIMIT
        ),
        name="gather_and_deal",
    )(table, rows, cots, wa, wb, wc)


def reduce_kernel(
    outer, inner, kinds, *refs
):
    grads, (y_ref, g_ref) = refs[:kinds], refs[kinds : kinds + 2]
    totals, (ry_ref, rg_ref) = refs[kinds + 2 : 2 * kinds + 2], refs[2 * kinds + 2 : 2 * kinds + 4]
    scratch = refs[2 * kinds + 4 :]
    mines, crecvs, yrecvs, zrecvs, xrecvs = (
        scratch[kinds * i : kinds * (i + 1)] for i in range(5)
    )
    (c_send, c_recv, m_sem, y_send, y_recv, z_send, z_recv, x_send, x_recv, f_send, f_recv,
     r_send, r_recv, q_sem) = scratch[5 * kinds :]
    rank = lax.axis_index("rep")
    spot = lax.axis_index("fsdp")
    core = rank % 2
    row, col = spot // inner, spot % inner
    mate, across = core_of(rank), across_of(rank)
    pieces = [(src, dst, 0, src.shape[3] // 2) for src, dst in zip(grads[:-1], totals)]
    pieces.append((grads[-1], totals[-1], 0, None))

    barrier = pltpu.get_barrier_semaphore()
    neighbours = (
        (row + 1 < outer, {"fsdp": spot + inner}),
        (row > 0, {"fsdp": spot - inner}),
        (col + 1 < inner, {"fsdp": spot + 1}),
        (col > 0, {"fsdp": spot - 1}),
    )
    amount = jnp.int32(2)
    for there, device in neighbours:
        amount = amount + there.astype(jnp.int32)

        @pl.when(there)
        def _():
            pl.semaphore_signal(barrier, inc=1, device_id=device, device_id_type=MESH)

    for device in (mate, across):
        pl.semaphore_signal(barrier, inc=1, device_id={"rep": device}, device_id_type=MESH)
    pl.semaphore_wait(barrier, amount)

    late = []

    def send(there, src, dst, ssem, rsem, device):
        def describe():
            return pltpu.make_async_remote_copy(
                src_ref=src, dst_ref=dst, send_sem=ssem, recv_sem=rsem,
                device_id=device, device_id_type=MESH,
            )

        if there is None:
            describe().start()
            late.append((None, lambda: describe().wait_send()))
        else:
            @pl.when(there)
            def _():
                describe().start()

            late.append((there, lambda: describe().wait_send()))

    def arrive(place, rsem):
        pltpu.make_async_remote_copy(
            src_ref=place, dst_ref=place, send_sem=q_sem.at[0], recv_sem=rsem,
            device_id={"rep": mate}, device_id_type=MESH,
        ).wait_recv()

    def columns(ref, number, which):
        _, _, start, half = pieces[number]
        if half is None:
            return ref
        cols = pl.ds(pl.multiple_of(start + which * half, 128), half)
        return ref.at[:, :, :, cols] if len(ref.shape) == 4 else ref.at[:, cols]

    order = list(range(kinds))
    loads = []
    for number in order:
        src = columns(pieces[number][0], number, 1 - core)
        send(None, src, crecvs[number], c_send.at[number], c_recv.at[number], {"rep": mate})
        load = pltpu.make_async_copy(
            columns(pieces[number][0], number, core), mines[number], m_sem.at[number]
        )
        load.start()
        loads.append(load)

    for kind, (src, dst) in enumerate(((y_ref, ry_ref), (g_ref, rg_ref))):
        send(None, src, dst.at[rank], r_send.at[kind, 0], r_recv.at[kind, 0], {"rep": across})
        send(None, src, dst.at[rank], r_send.at[kind, 1], r_recv.at[kind, 1], {"rep": mate})
        pltpu.make_async_copy(src, dst.at[rank], q_sem.at[kind + 1]).start()

    def slot_of(way, size, place, dest):
        if size == 2:
            return 0
        return dest - place if way == 0 else size - place + dest

    def line_sum(number, size, place, stride, buffer, view, ssem, rsem):
        for far in range(size - 1, 0, -1):
            for way in range(2):
                dest = far if way == 0 else size - 1 - far
                step = 1 if way == 0 else -1
                passes = place < dest if way == 0 else place > dest
                first = place == 0 if way == 0 else place == size - 1
                mine = view(dest)
                got = slot_of(way, size, place, dest)

                @pl.when(jnp.logical_and(passes, jnp.logical_not(first)))
                def _():
                    arrive(buffer.at[got], rsem.at[got, number])
                    mine[...] = mine[...] + buffer[got]

                put = slot_of(way, size, place + step, dest)
                send(passes, mine, buffer.at[put], ssem.at[way, dest, number], rsem.at[put, number],
                     {"fsdp": spot + step * stride})
        for way in range(2):
            has = place > 0 if way == 0 else place < size - 1
            got = slot_of(way, size, place, place)
            mine = view(place)

            @pl.when(has)
            def _():
                arrive(buffer.at[got], rsem.at[got, number])
                mine[...] = mine[...] + buffer[got]

    for number in order:
        loads[number].wait()
        arrive(crecvs[number], c_recv.at[number])
        mine, other = mines[number], crecvs[number]

        def add(index, carry):
            mine[index // inner, index % inner] = (
                mine[index // inner, index % inner] + other[index // inner, index % inner]
            )
            return carry

        lax.fori_loop(0, outer * inner, add, 0)
        if inner == 2:
            send(None, mine.at[:, 1 - col], yrecvs[number].at[0], y_send.at[0, 0, number],
                 y_recv.at[0, number], {"fsdp": spot + 1 - 2 * col})
    for kind, dst in enumerate((ry_ref, rg_ref)):
        place = dst.at[across]
        arrive(place, r_recv.at[kind, 0])
        send(None, place, place, r_send.at[kind, 2], r_recv.at[kind, 2], {"rep": mate})
    for number in order:
        mine = mines[number]
        if inner == 2:
            arrive(yrecvs[number].at[0], y_recv.at[0, number])
            buffer = yrecvs[number]

            def add(index, carry):
                mine[index, col] = mine[index, col] + buffer[0, index]
                return carry

            lax.fori_loop(0, outer, add, 0)
        else:
            line_sum(number, inner, col, 1, yrecvs[number], lambda dest: mine.at[:, dest],
                     y_send, y_recv)
        line_sum(number, outer, row, inner, zrecvs[number], lambda dest: mine.at[dest, col],
                 z_send, z_recv)
        send(None, mine.at[row, col], xrecvs[number], x_send.at[number], x_recv.at[number],
             {"rep": across})
    for number in order:
        arrive(xrecvs[number], x_recv.at[number])
        total = mines[number][row, col].astype(jnp.float32) + xrecvs[number][...].astype(jnp.float32)
        out, half = pieces[number][1], pieces[number][3]
        place = columns(out, number, core)
        place[...] = total
        if half is not None:
            send(None, place, place, f_send.at[number], f_recv.at[number], {"rep": mate})
    for number in order:
        if pieces[number][3] is not None:
            arrive(columns(pieces[number][1], number, 1 - core), f_recv.at[number])
    for kind, dst in enumerate((ry_ref, rg_ref)):
        arrive(dst.at[mate], r_recv.at[kind, 1])
        arrive(dst.at[across_of(mate)], r_recv.at[kind, 2])
        src = y_ref if kind == 0 else g_ref
        pltpu.make_async_copy(src, dst.at[rank], q_sem.at[kind + 1]).wait()
    for there, finish_send in late:
        if there is None:
            finish_send()
        else:
            pl.when(there)(finish_send)


def reduce_grads(count, grads, y_rows, g_rows):
    outer, inner = grid_of(count)
    kinds = len(grads)
    shapes = [(grad.shape[1], grad.shape[2] // 2, grad.dtype) for grad in grads[:-1]]
    shapes.append(grads[-1].shape[1:] + (grads[-1].dtype,))
    dma = pltpu.SemaphoreType.DMA
    y_slots = 1 if inner == 2 else inner + 1
    z_slots = 1 if outer == 2 else outer + 1
    scratch = []
    for lead in ((outer, inner), (outer, inner), (y_slots, outer), (z_slots,), ()):
        scratch += [pltpu.VMEM(lead + (a, b), dtype) for a, b, dtype in shapes]
    scratch += [
        dma((kinds,)), dma((kinds,)), dma((kinds,)),
        dma((2, inner, kinds)), dma((y_slots, kinds)),
        dma((2, outer, kinds)), dma((z_slots, kinds)),
        dma((kinds,)), dma((kinds,)), dma((kinds,)), dma((kinds,)),
        dma((2, 3)), dma((2, 3)), dma((3,)),
    ]
    return pl.pallas_call(
        partial(reduce_kernel, outer, inner, kinds),
        out_shape=tuple(jax.ShapeDtypeStruct(grad.shape[1:], jnp.float32) for grad in grads) + (
            jax.ShapeDtypeStruct((4,) + y_rows.shape, y_rows.dtype),
            jax.ShapeDtypeStruct((4,) + g_rows.shape, g_rows.dtype),
        ),
        in_specs=[ANY] * (kinds + 2),
        out_specs=(VMEM,) * kinds + (ANY, ANY),
        scratch_shapes=scratch,
        compiler_params=pltpu.CompilerParams(
            collective_id=2, has_side_effects=True, vmem_limit_bytes=VMEM_LIMIT
        ),
        name="reduce_and_return",
    )(*(grad.reshape((outer, inner) + grad.shape[1:]) for grad in grads), y_rows, g_rows)


def home_kernel(tab_ref, ry_ref, rg_ref, y_ref, g_ref):
    base = lax.axis_index("rep") * y_ref.shape[0]

    def fetch(block, carry):
        index = tab_ref[DEST_AT + base + block]
        safe = jnp.maximum(index, 0)
        for src, dst in ((ry_ref, y_ref), (rg_ref, g_ref)):
            value = src[safe // SLOTS, safe % SLOTS]
            dst[block] = jnp.where(index >= 0, value, jnp.zeros_like(value))
        return carry

    lax.fori_loop(0, y_ref.shape[0], fetch, 0)


def bring_home(table, ry, rg, blocks):
    shape = jax.ShapeDtypeStruct((blocks,) + ry.shape[2:], ry.dtype)
    return pl.pallas_call(
        home_kernel,
        out_shape=(shape, shape),
        in_specs=[SMEM, VMEM, VMEM],
        out_specs=(VMEM, VMEM),
        compiler_params=pltpu.CompilerParams(vmem_limit_bytes=VMEM_LIMIT),
        name="place_rows",
    )(table, ry, rg)


D = H * DH
ROWS = SLOTS * BLK
SIDES = SLOTS * (BLK // GBLK)
SIDE_ROWS = 48
ALL_ROWS = ROWS + SIDE_ROWS
QT = 128
WIN = 384
TILES = ROWS // QT
QUAD = 256
FF_TILE = 256
GELU_C = 0.7978845608028654
GELU_A = 0.044715
F32, BF16 = jnp.float32, jnp.bfloat16


def mm(left, right):
    return lax.dot_general(left, right, (((1,), (0,)), ((), ())), preferred_element_type=F32)


def mm_cols(left, right):
    return lax.dot_general(left, right, (((1,), (1,)), ((), ())), preferred_element_type=F32)


def mm_rows(left, right):
    return lax.dot_general(left, right, (((0,), (0,)), ((), ())), preferred_element_type=F32)


def iota(shape, axis):
    return lax.broadcasted_iota(jnp.int32, shape, axis)


def pick_by(index, values, other):
    out = jnp.full(index.shape, other, jnp.int32)
    for number, value in enumerate(values):
        out = jnp.where(index == number, value, out)
    return out


def slot_info(tab_ref, rank):
    seg = [tab_ref[SEG_AT + rank * SLOTS + slot] for slot in range(SLOTS)]
    length = [tab_ref[LEN_AT + rank * SLOTS + slot] for slot in range(SLOTS)]
    return seg, length


def valid_column(tab_ref, rank):
    _, length = slot_info(tab_ref, rank)
    row = iota((ROWS, 1), 0)
    return ((row % BLK) < pick_by(row // BLK, length, 0)).astype(F32)


def pooling(tab_ref, rank):
    _, length = slot_info(tab_ref, rank)
    row = iota((1, ROWS), 1)
    block = jnp.where((row % BLK) < pick_by(row // BLK, length, 0), row // GBLK, -1)
    return jnp.where(iota((SIDE_ROWS, ROWS), 0) == block, 1.0, 0.0).astype(BF16)


def key_segments(tab_ref, rank, first_block, index):
    blocks = WIN // BLK
    base = rank * SLOTS + first_block
    seg = [tab_ref[SEG_AT + base + step] for step in range(blocks)]
    length = [tab_ref[LEN_AT + base + step] for step in range(blocks)]
    alive = (index % BLK) < pick_by(index // BLK, length, 0)
    return jnp.where(alive, pick_by(index // BLK, seg, -2), -2)


def side_segments(tab_ref, rank, index):
    seg, length = slot_info(tab_ref, rank)
    per = BLK // GBLK
    alive = (index % per) * GBLK < pick_by(index // per, length, 0)
    return jnp.where(alive, pick_by(index // per, seg, -2), -2)


def tile_bias(tab_ref, rank, tile, first_row, keys_axis):
    qs, ks, gs = ((QT, 1), (1, WIN), (1, SIDE_ROWS)) if keys_axis == 1 else ((1, QT), (WIN, 1), (SIDE_ROWS, 1))
    q_index = iota(qs, 1 - keys_axis)
    k_index = iota(ks, keys_axis)
    g_index = iota(gs, keys_axis)
    base = SEG_AT + rank * SLOTS + tile * (QT // BLK)
    q_seg = pick_by(q_index // BLK, [tab_ref[base + step] for step in range(QT // BLK)], -1)
    k_seg = key_segments(tab_ref, rank, first_row // BLK, k_index)
    g_seg = side_segments(tab_ref, rank, g_index)
    gap = (q_index + tile * QT) - (k_index + first_row)
    local = (jnp.abs(gap) <= RADIUS) & (q_seg == k_seg)
    return jnp.where(local, 0.0, MASKED_SCORE), jnp.where(q_seg == g_seg, 0.0, MASKED_SCORE)


def window_start(tile):
    return pl.multiple_of(jnp.clip(tile - 1, 0, TILES - WIN // QT) * QT, QT)


def head_stack(rows):
    lane = iota(rows.shape, 1) // DH
    zero = jnp.zeros_like(rows)
    return jnp.concatenate([jnp.where(lane == head, rows, zero) for head in range(QUAD // DH)], axis=0)


def head_merge(stacked):
    lane = iota((QT, QUAD), 1) // DH
    out = stacked[:QT]
    for head in range(1, QUAD // DH):
        out = jnp.where(lane == head, stacked[head * QT : (head + 1) * QT], out)
    return out


def gains_of(gc_ref):
    count = gc_ref.shape[0]
    part = D // count
    lane, column = iota((128, D), 0), iota((128, D), 1)
    total = None
    for shard in range(count):
        pick = jnp.where((column == lane + shard * part) & (lane < part), 1.0, 0.0).astype(BF16)
        term = mm(gc_ref[shard], pick)
        total = term if total is None else total + term
    return total


def three_way(value):
    high = value.astype(BF16)
    rest = value - high.astype(F32)
    middle = rest.astype(BF16)
    return high, middle, (rest - middle.astype(F32)).astype(BF16)


def spread_gain_grads(value, dc_ref):
    count = dc_ref.shape[0] if len(dc_ref.shape) == 3 else dc_ref.shape[0] * dc_ref.shape[1]
    part = D // count
    column, lane = iota((D, 128), 0), iota((D, 128), 1)
    parts = three_way(value)
    for shard in range(count):
        pick = jnp.where((column == lane + shard * part) & (lane < part), 1.0, 0.0).astype(BF16)
        place = dc_ref.at[shard] if len(dc_ref.shape) == 3 else dc_ref.at[shard // dc_ref.shape[1], shard % dc_ref.shape[1]]
        place[...] = mm(parts[0], pick) + mm(parts[1], pick) + mm(parts[2], pick)


def mean_square(value):
    return jnp.mean(value * value, axis=-1, keepdims=True)


def forward_norm(tab_ref, rank, x_ref, gains, n_ref):
    for tile in range(TILES):
        rows = pl.ds(tile * QT, QT)
        value = x_ref[rows, :].astype(F32)
        n_ref[rows, :] = (value * lax.rsqrt(mean_square(value) + EPSILON) * gains[0:1]).astype(BF16)
    side = mm(pooling(tab_ref, rank), n_ref[:ROWS, :])
    n_ref[ROWS:, :] = (side * lax.rsqrt(mean_square(side) + EPSILON) * gains[1:2]).astype(BF16)


def forward_project(n_ref, w_ref, qkv_ref):
    def step(tile, carry):
        cols = pl.ds(pl.multiple_of(tile * QUAD, QUAD), QUAD)
        qkv_ref[:, cols] = mm(n_ref[...], w_ref[:, cols]).astype(BF16)
        return carry

    lax.fori_loop(0, 3 * D // QUAD, step, 0)


def forward_attention(tab_ref, rank, qkv_ref, att_ref, lse_ref):
    def step(tile, carry):
        first = window_start(tile)
        bias, side_bias = tile_bias(tab_ref, rank, tile, first, 1)
        rows = pl.ds(pl.multiple_of(tile * QT, QT), QT)
        window = pl.ds(first, WIN)
        lse = jnp.zeros((QT, 128), F32)
        lane = iota((QT, 128), 1)
        for quad in range(D // QUAD):
            low = quad * QUAD
            query = head_stack(qkv_ref[rows, low : low + QUAD])
            scores = mm_cols(query, qkv_ref[window, D + low : D + low + QUAD])
            side_scores = mm_cols(query, qkv_ref[ROWS:, D + low : D + low + QUAD])
            local, sides, scale = [], [], []
            for head in range(QUAD // DH):
                part = slice(head * QT, (head + 1) * QT)
                one = scores[part] + bias
                two = side_scores[part] + side_bias
                peak = jnp.maximum(
                    jnp.max(one, axis=-1, keepdims=True), jnp.max(two, axis=-1, keepdims=True)
                )
                one, two = jnp.exp(one - peak), jnp.exp(two - peak)
                total = jnp.sum(one, axis=-1, keepdims=True) + jnp.sum(two, axis=-1, keepdims=True)
                local.append(one.astype(BF16))
                sides.append(two.astype(BF16))
                scale.append(1.0 / total)
                lse = jnp.where(lane == quad * (QUAD // DH) + head, peak + jnp.log(total), lse)
            mixed = mm(jnp.concatenate(local, axis=0), qkv_ref[window, 2 * D + low : 2 * D + low + QUAD])
            mixed = mixed + mm(
                jnp.concatenate(sides, axis=0), qkv_ref[ROWS:, 2 * D + low : 2 * D + low + QUAD]
            )
            mixed = mixed * jnp.concatenate(scale, axis=0)
            att_ref[rows, low : low + QUAD] = head_merge(mixed).astype(BF16)
        lse_ref[tile] = jnp.transpose(lse)[:16]
        return carry

    lax.fori_loop(0, TILES, step, 0)


def feed_forward(tab_ref, rank, x_ref, cot_ref, att_ref, gains, w_ref, wb_ref,
                 y_ref, gh_ref, ga_ref, dg_ref, du_ref, db_ref, do_ref,
                 h1_ref, nt_ref, ntt_ref, gres_ref, h2_ref, gg_ref, gu_ref, gn_ref):
    hidden = wb_ref.shape[0]
    gate_at = 4 * D
    valid = valid_column(tab_ref, rank)
    gain = gains[2:3]
    for tile in range(TILES):
        rows = pl.ds(tile * QT, QT)
        value = x_ref[rows, :].astype(F32) + mm(att_ref[rows, :], w_ref[:, 3 * D : 4 * D])
        h1_ref[rows, :] = value
        normed = (value * lax.rsqrt(mean_square(value) + EPSILON) * gain).astype(BF16)
        nt_ref[rows, :] = normed
        ntt_ref[:, tile * QT : (tile + 1) * QT] = jnp.transpose(normed)
        gres_ref[rows, :] = (cot_ref[rows, :].astype(F32) * valid[tile * QT : (tile + 1) * QT]).astype(BF16)

    def inward(tile, carry):
        at = pl.multiple_of(tile * FF_TILE, FF_TILE)
        cols = pl.ds(at, FF_TILE)
        gate = mm(nt_ref[...], w_ref[:, pl.ds(gate_at + at, FF_TILE)])
        up = mm(nt_ref[...], w_ref[:, pl.ds(gate_at + hidden + at, FF_TILE)])
        back = mm_cols(gres_ref[...], wb_ref[cols, :])
        square = gate * gate
        bend = jnp.tanh(GELU_C * (gate * (1.0 + GELU_A * square)))
        half = 0.5 * (1.0 + bend)
        act = gate * half
        slope = half + (0.5 * GELU_C) * gate * (1.0 - bend * bend) * (1.0 + (3.0 * GELU_A) * square)
        h2_ref[:, cols] = (act * up).astype(BF16)
        gg_ref[:, cols] = (back * up * slope).astype(BF16)
        gu_ref[:, cols] = (back * act).astype(BF16)
        return carry

    lax.fori_loop(0, hidden // FF_TILE, inward, 0)

    def outward(tile, carry):
        cols = pl.ds(pl.multiple_of(tile * QUAD, QUAD), QUAD)
        value = h1_ref[:, cols] + mm(h2_ref[...], wb_ref[:, cols])
        y_ref[:, cols] = (value * valid).astype(BF16)
        gn_ref[:, cols] = mm_cols(gg_ref[...], w_ref[cols, gate_at : gate_at + hidden]) + mm_cols(
            gu_ref[...], w_ref[cols, gate_at + hidden :]
        )
        return carry

    lax.fori_loop(0, D // QUAD, outward, 0)

    def weights(tile, carry):
        at = pl.multiple_of(tile * FF_TILE, FF_TILE)
        cols = pl.ds(at, FF_TILE)
        dg_ref[:, cols] = mm(ntt_ref[...], gg_ref[:, cols]).astype(BF16)
        du_ref[:, cols] = mm(ntt_ref[...], gu_ref[:, cols]).astype(BF16)
        db_ref[cols, :] = mm_rows(h2_ref[:, cols], gres_ref[...]).astype(BF16)
        return carry

    lax.fori_loop(0, hidden // FF_TILE, weights, 0)

    gain_grad = jnp.zeros((1, D), F32)
    for tile in range(TILES):
        rows = pl.ds(tile * QT, QT)
        value, grad = h1_ref[rows, :], gn_ref[rows, :]
        root = lax.rsqrt(mean_square(value) + EPSILON)
        unit = value * root
        gain_grad = gain_grad + jnp.sum(grad * unit, axis=0, keepdims=True)
        grad = grad * gain
        grad = gres_ref[rows, :].astype(F32) + root * (
            grad - unit * jnp.mean(grad * unit, axis=-1, keepdims=True)
        )
        gh_ref[rows, :] = grad
        low = grad.astype(BF16)
        nt_ref[rows, :] = low
        ga_ref[rows, :] = mm_cols(low, w_ref[:, 3 * D : 4 * D]).astype(BF16)

    def out_weight(tile, carry):
        cols = pl.ds(pl.multiple_of(tile * QUAD, QUAD), QUAD)
        do_ref[cols, :] = mm_rows(att_ref[:, cols], nt_ref[...]).astype(BF16)
        return carry

    lax.fori_loop(0, D // QUAD, out_weight, 0)
    return gain_grad


def backward_attention_start(dk_ref, dv_ref):
    dk_ref[...] = jnp.zeros_like(dk_ref)
    dv_ref[...] = jnp.zeros_like(dv_ref)


def backward_attention_tiles(tab_ref, rank, qkv_ref, att_ref, ga_ref, lse_ref, dqkv_ref, dk_ref, dv_ref, begin, end):
    heads = QUAD // DH
    marks = jnp.where(iota((16, D), 1) // DH == iota((16, D), 0), 1.0, 0.0).astype(BF16)

    def step(tile, carry):
        first = window_start(tile)
        bias, side_bias = tile_bias(tab_ref, rank, tile, first, 0)
        bias = jnp.concatenate([bias, side_bias], axis=0)
        rows = pl.ds(pl.multiple_of(tile * QT, QT), QT)
        window = pl.ds(first, WIN)
        product = ga_ref[rows, :].astype(F32) * att_ref[rows, :].astype(F32)
        high = product.astype(BF16)
        rest = (product - high.astype(F32)).astype(BF16)
        centre = mm_cols(marks, high) + mm_cols(marks, rest)
        lse = lse_ref[tile]
        for quad in range(D // QUAD):
            low = quad * QUAD
            query = head_stack(qkv_ref[rows, low : low + QUAD])
            grad = head_stack(ga_ref[rows, low : low + QUAD])
            keys = jnp.concatenate(
                [qkv_ref[window, D + low : D + low + QUAD], qkv_ref[ROWS:, D + low : D + low + QUAD]], axis=0
            )
            values = jnp.concatenate(
                [qkv_ref[window, 2 * D + low : 2 * D + low + QUAD],
                 qkv_ref[ROWS:, 2 * D + low : 2 * D + low + QUAD]], axis=0
            )
            scores = mm_cols(keys, query)
            slopes = mm_cols(values, grad)
            probs, grads = [], []
            for head in range(heads):
                part = slice(head * QT, (head + 1) * QT)
                number = quad * heads + head
                prob = jnp.exp(scores[:, part] + bias - lse[number : number + 1])
                probs.append(prob.astype(BF16))
                grads.append((prob * (slopes[:, part] - centre[number : number + 1])).astype(BF16))
            probs = jnp.concatenate(probs, axis=1)
            grads = jnp.concatenate(grads, axis=1)
            dkey = mm(grads, query)
            dvalue = mm(probs, grad)
            cols = slice(low, low + QUAD)
            dk_ref[window, cols] = dk_ref[window, cols] + dkey[:WIN]
            dk_ref[ROWS:, cols] = dk_ref[ROWS:, cols] + dkey[WIN:]
            dv_ref[window, cols] = dv_ref[window, cols] + dvalue[:WIN]
            dv_ref[ROWS:, cols] = dv_ref[ROWS:, cols] + dvalue[WIN:]
            dqkv_ref[rows, cols] = head_merge(mm_rows(grads, keys)).astype(BF16)
        return carry

    lax.fori_loop(begin, end, step, 0)


def backward_attention_end(dqkv_ref, dk_ref, dv_ref):
    dqkv_ref[ROWS:, :D] = jnp.zeros((SIDE_ROWS, D), BF16)
    dqkv_ref[:, D : 2 * D] = dk_ref[...].astype(BF16)
    dqkv_ref[:, 2 * D :] = dv_ref[...].astype(BF16)


def weight_grads(n_ref, dqkv_ref, refs):
    for number, ref in enumerate(refs):
        def weights(tile, carry):
            at = pl.multiple_of(tile * QUAD, QUAD)
            value = mm_rows(n_ref[...], dqkv_ref[:, pl.ds(number * D + at, QUAD)]).astype(BF16)
            if len(ref.shape) == 4:
                ref[:, :, :, pl.ds(at, QUAD)] = value.reshape(ref.shape[:3] + (QUAD,))
            else:
                ref[:, pl.ds(at, QUAD)] = value
            return carry

        lax.fori_loop(0, D // QUAD, weights, 0)


def backward_project(tab_ref, rank, x_ref, gh_ref, gains, n_ref, dqkv_ref, w_ref, gn_ref, g_ref):
    def step(tile, carry):
        cols = pl.ds(pl.multiple_of(tile * QUAD, QUAD), QUAD)
        gn_ref[:, cols] = mm_cols(dqkv_ref[...], w_ref[cols, : 3 * D])
        return carry

    lax.fori_loop(0, D // QUAD, step, 0)
    pool = pooling(tab_ref, rank)
    side = mm(pool, n_ref[:ROWS, :])
    root = lax.rsqrt(mean_square(side) + EPSILON)
    unit = side * root
    grad = gn_ref[ROWS:, :]
    side_gain = jnp.sum(grad * unit, axis=0, keepdims=True)
    grad = grad * gains[1:2]
    grad = root * (grad - unit * jnp.mean(grad * unit, axis=-1, keepdims=True))
    parts = three_way(grad)
    gain_grad = jnp.zeros((1, D), F32)
    for tile in range(TILES):
        rows = pl.ds(tile * QT, QT)
        spread = pool[:, tile * QT : (tile + 1) * QT]
        total = gn_ref[rows, :] + mm_rows(spread, parts[0]) + mm_rows(spread, parts[1])
        value = x_ref[rows, :].astype(F32)
        root = lax.rsqrt(mean_square(value) + EPSILON)
        unit = value * root
        gain_grad = gain_grad + jnp.sum(total * unit, axis=0, keepdims=True)
        total = total * gains[0:1]
        value = (
            gh_ref[rows, :] + root * (total - unit * jnp.mean(total * unit, axis=-1, keepdims=True))
        ).astype(BF16)
        if len(g_ref.shape) == 3:
            g_ref[pl.ds(tile * (QT // BLK), QT // BLK)] = value.reshape(QT // BLK, BLK, D)
        else:
            g_ref[rows, :] = value
    return gain_grad, side_gain


def first_kernel(tab_ref, x_ref, gc_ref, w_ref, n_ref, qkv_ref, att_ref, lse_ref):
    rank = lax.axis_index("rep")
    gains = gains_of(gc_ref)
    forward_norm(tab_ref, rank, x_ref, gains, n_ref)
    forward_project(n_ref, w_ref, qkv_ref)
    forward_attention(tab_ref, rank, qkv_ref, att_ref, lse_ref)


def second_kernel(tab_ref, x_ref, cot_ref, att_ref, gc_ref, w_ref, wb_ref,
                  y_ref, gh_ref, ga_ref, dg_ref, du_ref, db_ref, do_ref, gain_ref, *scratch):
    rank = lax.axis_index("rep")
    gain_ref[...] = feed_forward(tab_ref, rank, x_ref, cot_ref, att_ref, gains_of(gc_ref), w_ref, wb_ref,
                                 y_ref, gh_ref, ga_ref, dg_ref, du_ref, db_ref, do_ref, *scratch)


def third_kernel(tab_ref, x_ref, gh_ref, ga_ref, att_ref, lse_ref, n_ref, qkv_ref, gain_ref, gc_ref, w_ref,
                 g_ref, dw_ref, dc_ref, dqkv_ref, dk_ref, dv_ref, gn_ref):
    rank = lax.axis_index("rep")
    gains = gains_of(gc_ref)
    backward_attention_start(dk_ref, dv_ref)
    backward_attention_tiles(tab_ref, rank, qkv_ref, att_ref, ga_ref, lse_ref, dqkv_ref, dk_ref, dv_ref, 0, TILES)
    backward_attention_end(dqkv_ref, dk_ref, dv_ref)
    weight_grads(n_ref, dqkv_ref, [dw_ref.at[:, i * D : (i + 1) * D] for i in range(3)])
    one, side = backward_project(tab_ref, rank, x_ref, gh_ref, gains, n_ref, dqkv_ref, w_ref, gn_ref, g_ref)
    grads = jnp.concatenate([one, side, gain_ref[...], jnp.zeros((5, D), F32)], axis=0)
    spread_gain_grads(grads, dc_ref)


def forward_layer(tab, x, cot, gc, w, wb):
    hidden = wb.shape[0]
    shape = jax.ShapeDtypeStruct
    params = pltpu.CompilerParams(vmem_limit_bytes=VMEM_LIMIT)
    n, qkv, att, lse = pl.pallas_call(
        first_kernel,
        out_shape=(shape((ALL_ROWS, D), BF16), shape((ALL_ROWS, 3 * D), BF16), shape((ROWS, D), BF16),
                   shape((TILES, 16, QT), F32)),
        in_specs=[SMEM, VMEM, VMEM, pl.BlockSpec((D, 3 * D), lambda step: (0, 0))],
        grid=(1,),
        out_specs=(VMEM,) * 4,
        compiler_params=params,
        name="attend",
    )(tab, x, gc, w)
    outs = pl.pallas_call(
        second_kernel,
        out_shape=(shape((ROWS, D), BF16), shape((ROWS, D), F32), shape((ROWS, D), BF16),
                   shape((D, hidden), BF16), shape((D, hidden), BF16), shape((hidden, D), BF16), shape((D, D), BF16),
                   shape((1, D), F32)),
        in_specs=[SMEM] + [VMEM] * 6,
        out_specs=(VMEM,) * 8,
        scratch_shapes=[pltpu.VMEM((ROWS, D), F32), pltpu.VMEM((ROWS, D), BF16), pltpu.VMEM((D, ROWS), BF16),
                        pltpu.VMEM((ROWS, D), BF16), pltpu.VMEM((ROWS, hidden), BF16),
                        pltpu.VMEM((ROWS, hidden), BF16), pltpu.VMEM((ROWS, hidden), BF16),
                        pltpu.VMEM((ROWS, D), F32)],
        compiler_params=params,
        name="feed_forward",
    )(tab, x, cot, att, gc, w, wb)
    return (n, qkv, att, lse) + outs


def backward_layer(tab, x, gh, ga, att, lse, n, qkv, gain, gc, w):
    shape = jax.ShapeDtypeStruct
    return pl.pallas_call(
        third_kernel,
        out_shape=(shape((ROWS, D), BF16), shape((D, 3 * D), BF16), shape((gc.shape[0], 8, 128), F32)),
        in_specs=[SMEM] + [VMEM] * 9 + [pl.BlockSpec((D, 3 * D), lambda step: (0, 0))],
        grid=(1,),
        out_specs=(VMEM,) * 3,
        scratch_shapes=[pltpu.VMEM((ALL_ROWS, 3 * D), BF16), pltpu.VMEM((ALL_ROWS, D), F32),
                        pltpu.VMEM((ALL_ROWS, D), F32), pltpu.VMEM((ALL_ROWS, D), F32)],
        compiler_params=pltpu.CompilerParams(vmem_limit_bytes=VMEM_LIMIT),
        name="attend_back",
    )(tab, x, gh, ga, att, lse, n, qkv, gain, gc, w)


class Links:
    def __init__(self, outer, inner):
        self.outer, self.inner = outer, inner
        self.rank, self.spot = lax.axis_index("rep"), lax.axis_index("fsdp")
        self.core = self.rank % 2
        self.row, self.col = self.spot // inner, self.spot % inner
        self.mate, self.across = core_of(self.rank), across_of(self.rank)
        self.late = []

    def greet(self):
        barrier = pltpu.get_barrier_semaphore()
        neighbours = (
            (self.row + 1 < self.outer, {"fsdp": self.spot + self.inner}),
            (self.row > 0, {"fsdp": self.spot - self.inner}),
            (self.col + 1 < self.inner, {"fsdp": self.spot + 1}),
            (self.col > 0, {"fsdp": self.spot - 1}),
        )
        amount = jnp.int32(2)
        for there, device in neighbours:
            amount = amount + there.astype(jnp.int32)

            @pl.when(there)
            def _():
                pl.semaphore_signal(barrier, inc=1, device_id=device, device_id_type=MESH)

        for device in (self.mate, self.across):
            pl.semaphore_signal(barrier, inc=1, device_id={"rep": device}, device_id_type=MESH)
        pl.semaphore_wait(barrier, amount)

    def send(self, there, src, dst, ssem, rsem, device):
        def describe():
            return pltpu.make_async_remote_copy(
                src_ref=src, dst_ref=dst, send_sem=ssem, recv_sem=rsem,
                device_id=device, device_id_type=MESH,
            )

        if there is None:
            describe().start()
        else:
            @pl.when(there)
            def _():
                describe().start()

        self.late.append((there, lambda: describe().wait_send()))

    def arrive(self, place, rsem, spare):
        pltpu.make_async_remote_copy(
            src_ref=place, dst_ref=place, send_sem=spare, recv_sem=rsem,
            device_id={"rep": self.mate}, device_id_type=MESH,
        ).wait_recv()

    def drain(self):
        for there, finish in self.late:
            if there is None:
                finish()
            else:
                pl.when(there)(finish)


def halves(ref, which):
    half = ref.shape[-1] // 2
    cols = pl.ds(pl.multiple_of(which * half, 128), half)
    return ref.at[:, :, :, cols] if len(ref.shape) == 4 else ref.at[:, cols]


class Reduction:
    def __init__(self, links, source, total, mine, crecv, yrecv, zrecv, xrecv, sems, number):
        self.links, self.source, self.total, self.mine = links, source, total, mine
        self.crecv, self.yrecv, self.zrecv, self.xrecv = crecv, yrecv, zrecv, xrecv
        self.sems, self.number = sems, number
        self.whole = total.shape[-1] % 256 != 0
        self.load = None

    def sem(self, name, *index):
        return self.sems[name].at[index + (self.number,)]

    def begin(self):
        links = self.links
        other = self.source if self.whole else halves(self.source, 1 - links.core)
        links.send(None, other, self.crecv, self.sem("c_send"), self.sem("c_recv"), {"rep": links.mate})
        if self.mine is None:
            self.mine = self.source if self.whole else halves(self.source, links.core)
        else:
            own = self.source if self.whole else halves(self.source, links.core)
            self.load = pltpu.make_async_copy(own, self.mine, self.sem("m_sem"))
            self.load.start()

    def pair(self):
        links = self.links
        if self.load is not None:
            self.load.wait()
        links.arrive(self.crecv, self.sem("c_recv"), self.sems["spare"].at[0])
        inner = links.inner

        def add(index, carry):
            row, col = index // inner, index % inner
            self.mine[row, col] = self.mine[row, col] + self.crecv[row, col]
            return carry

        lax.fori_loop(0, links.outer * inner, add, 0)
        links.send(None, self.mine.at[:, 1 - links.col], self.yrecv, self.sem("y_send"), self.sem("y_recv"),
                   {"fsdp": links.spot + 1 - 2 * links.col})

    def slot(self, way, place, dest):
        return dest - place if way == 0 else self.links.outer - place + dest

    def pass_on(self, way, dest, there, first):
        links = self.links
        step = 1 if way == 0 else -1
        mine = self.mine.at[dest, links.col]
        put = self.slot(way, links.row + step, dest)
        if not first:
            got = self.slot(way, links.row, dest)

            @pl.when(there)
            def _():
                links.arrive(self.zrecv.at[got], self.sem("z_recv", got), self.sems["spare"].at[0])
                mine[...] = mine[...] + self.zrecv[got]

        links.send(there, mine, self.zrecv.at[put], self.sem("z_send", way, dest), self.sem("z_recv", put),
                   {"fsdp": links.spot + step * links.inner})

    def column(self):
        links = self.links
        size = links.outer
        links.arrive(self.yrecv, self.sem("y_recv"), self.sems["spare"].at[0])

        def add(index, carry):
            self.mine[index, links.col] = self.mine[index, links.col] + self.yrecv[index]
            return carry

        lax.fori_loop(0, size, add, 0)
        for far in range(size - 1, 0, -1):
            self.pass_on(0, far, links.row == 0, True)
            self.pass_on(1, size - 1 - far, links.row == size - 1, True)

    def hop(self, turn):
        links = self.links
        size = links.outer
        for way in range(2):
            place = turn if way == 0 else size - 1 - turn
            here = links.row == place
            rest = range(size - 1, place, -1) if way == 0 else range(0, place)
            for dest in rest:
                self.pass_on(way, dest, here, False)
            mine = self.mine.at[place, links.col]
            got = self.slot(way, place, place)

            @pl.when(here)
            def _():
                links.arrive(self.zrecv.at[got], self.sem("z_recv", got), self.sems["spare"].at[0])
                mine[...] = mine[...] + self.zrecv[got]

    def cross(self):
        links = self.links
        mine = self.mine.at[links.row, links.col]
        links.send(None, mine, self.xrecv, self.sem("x_send"), self.sem("x_recv"), {"rep": links.across})

    def finish(self):
        links = self.links
        links.arrive(self.xrecv, self.sem("x_recv"), self.sems["spare"].at[0])
        value = self.mine[links.row, links.col].astype(F32) + self.xrecv[...].astype(F32)
        if self.whole:
            self.total[...] = value
            return
        place = halves(self.total, links.core)
        place[...] = value
        links.send(None, place, place, self.sem("f_send"), self.sem("f_recv"), {"rep": links.mate})

    def settle(self):
        if not self.whole:
            self.links.arrive(
                halves(self.total, 1 - self.links.core), self.sem("f_recv"), self.sems["spare"].at[0]
            )


SEM_NAMES = ("c_send", "c_recv", "m_sem", "y_send", "y_recv", "z_send", "z_recv", "x_send", "x_recv",
             "f_send", "f_recv", "r_send", "r_recv", "own", "spare")


class Return:
    def __init__(self, links, source, home, sems, kind):
        self.links, self.source, self.home, self.sems, self.kind = links, source, home, sems, kind

    def begin(self):
        links = self.links
        dst = self.home.at[links.rank]
        for way, device in enumerate((links.across, links.mate)):
            links.send(None, self.source, dst, self.sems["r_send"].at[self.kind, way],
                       self.sems["r_recv"].at[self.kind, way], {"rep": device})
        self.copy = pltpu.make_async_copy(self.source, dst, self.sems["own"].at[self.kind])
        self.copy.start()

    def relay(self):
        links = self.links
        place = self.home.at[links.across]
        links.arrive(place, self.sems["r_recv"].at[self.kind, 0], self.sems["spare"].at[0])
        links.send(None, place, place, self.sems["r_send"].at[self.kind, 2],
                   self.sems["r_recv"].at[self.kind, 2], {"rep": links.mate})

    def settle(self):
        links, sem = self.links, self.sems["r_recv"]
        links.arrive(self.home.at[links.mate], sem.at[self.kind, 1], self.sems["spare"].at[0])
        links.arrive(self.home.at[across_of(links.mate)], sem.at[self.kind, 2], self.sems["spare"].at[0])
        self.copy.wait()


def back_kernel(outer, inner, early, *refs):
    (tab_ref, x_ref, gh_ref, ga_ref, att_ref, lse_ref, n_ref, qkv_ref, gain_ref, gc_ref, w_ref), refs = refs[:11], refs[11:]
    grads, (y_ref,), refs = refs[:early], refs[early : early + 1], refs[early + 1 :]
    kinds = early + 4
    totals, (ry_ref, rg_ref), refs = refs[:kinds], refs[kinds : kinds + 2], refs[kinds + 2 :]
    (dq_ref, dkw_ref, dvw_ref, dc_ref), refs = refs[:4], refs[4:]
    (g_ref, dqkv_ref, dk_ref, dv_ref), refs = refs[:4], refs[4:]
    mines, refs = list(refs[:early]) + [None] * 3 + [refs[early]], refs[early + 1 :]
    crecv, yrecv, zrecv, xrecv = (refs[kinds * i : kinds * (i + 1)] for i in range(4))
    sems = dict(zip(SEM_NAMES, refs[4 * kinds :]))
    links = Links(outer, inner)
    rank = links.rank
    sources = list(grads) + [dq_ref, dkw_ref, dvw_ref, dc_ref]
    tasks = [
        Reduction(links, sources[i], totals[i], mines[i], crecv[i], yrecv[i], zrecv[i], xrecv[i], sems, i)
        for i in range(kinds)
    ]
    rows_y, rows_g = Return(links, y_ref, ry_ref, sems, 0), Return(links, g_ref, rg_ref, sems, 1)

    links.greet()
    for task in tasks[:early]:
        task.begin()
    rows_y.begin()
    gains = gains_of(gc_ref)
    for task in tasks[:early]:
        task.pair()
    backward_attention_start(dk_ref, dv_ref)
    backward_attention_tiles(tab_ref, rank, qkv_ref, att_ref, ga_ref, lse_ref, dqkv_ref, dk_ref, dv_ref, 0, TILES)
    tasks[0].column()
    backward_attention_end(dqkv_ref, dk_ref, dv_ref)
    weight_grads(n_ref, dqkv_ref, (dq_ref, dkw_ref, dvw_ref))
    for task in tasks[early : early + 3]:
        task.begin()
    rows_y.relay()
    one, side = backward_project(tab_ref, rank, x_ref, gh_ref, gains, n_ref, dqkv_ref, w_ref, dk_ref, g_ref)
    spread_gain_grads(jnp.concatenate([one, side, gain_ref[...], jnp.zeros((5, D), F32)], axis=0), dc_ref)
    rows_g.begin()
    tasks[kinds - 1].begin()
    for task in tasks[early:]:
        task.pair()
    for number in range(1, kinds + outer):
        if number < kinds:
            tasks[number].column()
        if number == 2:
            rows_g.relay()
        for turn in range(1, outer):
            if 0 <= number - turn < kinds:
                tasks[number - turn].hop(turn)
        if 0 <= number - outer + 1 < kinds:
            tasks[number - outer + 1].cross()
        if 0 <= number - outer < kinds:
            tasks[number - outer].finish()
    rows_y.settle()
    rows_g.settle()
    for task in tasks:
        task.settle()
    links.drain()


def attend_back(count, table, x, gh, ga, att, lse, n, qkv, gain, gc, w, grads, y):
    outer, inner = grid_of(count)
    part = D // count
    early = len(grads)
    kinds = early + 4
    grads = [grad.reshape((outer, inner, -1) + grad.shape[1:]) for grad in grads]
    shapes = [grad.shape[2:] for grad in grads] + [(part, D)] * 3 + [(8, 128)]
    dtypes = [BF16] * (kinds - 1) + [F32]
    halved = [(a, b // 2 if b % 256 == 0 else b) for a, b in shapes]
    dma = pltpu.SemaphoreType.DMA
    scratch = [pltpu.VMEM((outer, inner) + shape, dtype) for shape, dtype in zip(shapes[early:], dtypes[early:])]
    scratch += [pltpu.VMEM((SLOTS, BLK, D), BF16), pltpu.VMEM((ALL_ROWS, 3 * D), BF16),
                pltpu.VMEM((ALL_ROWS, D), F32), pltpu.VMEM((ALL_ROWS, D), F32)]
    scratch += [pltpu.VMEM((outer, inner) + shape, BF16) for shape in halved[:early]]
    scratch += [pltpu.VMEM((outer, inner) + halved[-1], F32)]
    for lead in ((outer, inner), (outer,), (outer + 1,), ()):
        scratch += [pltpu.VMEM(lead + shape, dtype) for shape, dtype in zip(halved, dtypes)]
    one = dma((kinds,))
    scratch += [one, one, one, one, one, dma((2, outer, kinds)), dma((outer + 1, kinds)), one, one, one, one,
                dma((2, 3)), dma((2, 3)), dma((2,)), dma((1,))]
    rows = jax.ShapeDtypeStruct((4, SLOTS, BLK, D), BF16)
    outs = pl.pallas_call(
        partial(back_kernel, outer, inner, early),
        out_shape=tuple(jax.ShapeDtypeStruct(shape, F32) for shape in shapes) + (rows, rows),
        grid=(1,),
        in_specs=[SMEM] + [VMEM] * 9 + [pl.BlockSpec((D, 3 * D), lambda step: (0, 0))] + [ANY] * early + [VMEM],
        out_specs=(VMEM,) * kinds + (ANY, ANY),
        scratch_shapes=scratch,
        compiler_params=pltpu.CompilerParams(
            collective_id=2, has_side_effects=True, vmem_limit_bytes=VMEM_LIMIT
        ),
        name="attend_back_and_reduce",
    )(table, x, gh, ga, att, lse, n, qkv, gain, gc, w, *grads, y.reshape(SLOTS, BLK, D))
    return outs[:kinds], outs[kinds], outs[kinds + 1]


def per_device(count, layer_input, cotangent, lengths, attn_gain, global_gain, query_weight, key_weight,
               value_weight, out_weight, ffn_gain, gate_weight, up_weight, down_weight):
    micro, span, width = layer_input.shape
    hidden = gate_weight.shape[1]
    blocks = micro * span // BLK
    table = deal_table(lengths)
    wa = jnp.concatenate([query_weight, key_weight, value_weight, out_weight, gate_weight, up_weight], axis=1)
    part = attn_gain.shape[0]
    wc = jnp.pad(jnp.stack([attn_gain, global_gain, ffn_gain]), ((0, 13), (0, 128 - part)))
    splits = ((0, 4 * width), (4 * width, 2 * hidden))
    ga, gb, gc, rows, cots = gather_weights(
        count, splits, table,
        layer_input.reshape(blocks, BLK, width), cotangent.reshape(blocks, BLK, width), wa, down_weight, wc,
    )
    x, full = rows.reshape(ROWS, width), ga.reshape(width, -1)
    n, qkv, att, lse, y, gh, gatt, dg, du, db, do, gain = forward_layer(
        table, x, cots.reshape(ROWS, width), gc, full, gb.reshape(-1, width)
    )
    if grid_of(count)[1] == 2 and part % 16 == 0:
        totals, ry, rg = attend_back(count, table, x, gh, gatt, att, lse, n, qkv, gain, gc, full, (dg, du, db, do), y)
        og, ou, ob, oo, oq, ok, ov, oc = totals
    else:
        g, dw, dc = backward_layer(table, x, gh, gatt, att, lse, n, qkv, gain, gc, full)
        grads = [grad.reshape(count, -1, grad.shape[-1]) for grad in (dg, du, db, do, dw, dc)]
        og, ou, ob, oo, ow, oc, ry, rg = reduce_grads(
            count, grads, y.reshape(SLOTS, BLK, width), g.reshape(SLOTS, BLK, width)
        )
        oq, ok, ov = ow[:, :width], ow[:, width : 2 * width], ow[:, 2 * width :]
    y_home, g_home = bring_home(table, ry, rg, blocks)
    return (
        y_home.reshape(layer_input.shape), g_home.reshape(layer_input.shape),
        oc[0, :part], oc[1, :part], oq, ok, ov, oo, oc[2, :part], og, ou, ob,
    )


def solution(mesh):
    rows = P(None, ("rep", "fsdp"), None)
    vector, matrix = P("fsdp"), P("fsdp", None)
    return jax.shard_map(
        partial(per_device, mesh.shape["fsdp"]),
        mesh=mesh,
        in_specs=(rows, rows, P(None, ("rep", "fsdp")), vector, vector, matrix, matrix, matrix, matrix,
                  vector, matrix, matrix, matrix),
        out_specs=(rows, rows, vector, vector, matrix, matrix, matrix, matrix, vector, matrix, matrix, matrix),
        check_vma=False,
    )
```

```python
from functools import partial

import jax
import jax.numpy as jnp
from jax import lax
from jax.experimental import pallas as pl
from jax.experimental.pallas import tpu as pltpu
from jax.sharding import PartitionSpec as P

H = 12
DH = 64
RADIUS = 127
GBLK = 16
BLK = 64
SLOTS = 10
MAX_SEQ_BLOCKS = 5
EPSILON = 1e-06
MASKED_SCORE = -1e30
MESH = pl.DeviceIdType.MESH
VMEM_LIMIT = 60 * 1024 * 1024
SEG_AT, LEN_AT, DEST_AT, TABLE_SIZE = 40, 80, 120, 256

ANY = pl.BlockSpec(memory_space=pl.ANY)
VMEM = pl.BlockSpec(memory_space=pltpu.VMEM)
SMEM = pl.BlockSpec(memory_space=pltpu.SMEM)


def grid_of(count):
    inner = 2 if count <= 8 else 4
    return count // inner, inner


def core_of(rank):
    return rank + 1 - 2 * (rank % 2)


def across_of(rank):
    return (rank + 2) % 4


def lens_kernel(lens_ref, all_ref, send_sem, recv_sem):
    rank = lax.axis_index("rep")
    barrier = pltpu.get_barrier_semaphore()
    for step in range(1, 4):
        pl.semaphore_signal(
            barrier, inc=1, device_id={"rep": (rank + step) % 4}, device_id_type=MESH
        )
    pl.semaphore_wait(barrier, 3)
    copies = []
    for step in range(1, 4):
        copy = pltpu.make_async_remote_copy(
            src_ref=lens_ref,
            dst_ref=all_ref.at[rank],
            send_sem=send_sem.at[step - 1],
            recv_sem=recv_sem.at[step - 1],
            device_id={"rep": (rank + step) % 4},
            device_id_type=MESH,
        )
        copy.start()
        copies.append(copy)
    all_ref[rank] = lens_ref[...]
    for copy in copies:
        copy.wait()


def table_kernel(micro, per_dev, lens_ref, tab_ref, order_ref, count_ref, load_ref):
    total = 4 * micro * per_dev

    def length_at(spot):
        return lens_ref[spot // (micro * per_dev), (spot // per_dev) % micro, spot % per_dev]

    def blocks_of(length):
        return (length + (BLK - 1)) // BLK

    def clear(spot, carry):
        tab_ref[spot] = -1
        return carry

    lax.fori_loop(0, TABLE_SIZE, clear, 0)
    for spot in range(4 * SLOTS):
        tab_ref[LEN_AT + spot] = 0
    for size in range(8):
        count_ref[size] = 0
    for dev in range(4):
        load_ref[dev] = 0

    def tally(spot, carry):
        length = length_at(spot)

        @pl.when(length > 0)
        def _():
            size = blocks_of(length)
            count_ref[size] = count_ref[size] + 1

        return carry

    lax.fori_loop(0, total, tally, 0)
    begin = 0
    for size in range(MAX_SEQ_BLOCKS, 0, -1):
        amount = count_ref[size]
        count_ref[size] = begin
        begin = begin + amount

    def place(spot, carry):
        length = length_at(spot)

        @pl.when(length > 0)
        def _():
            size = blocks_of(length)
            where = count_ref[size]
            order_ref[where] = spot
            count_ref[size] = where + 1

        return carry

    lax.fori_loop(0, total, place, 0)

    def assign(number, carry):
        spot = order_ref[number]
        length = length_at(spot)
        size = blocks_of(length)
        best = jnp.int32(0)
        low = load_ref[0]
        for dev in range(1, 4):
            here = load_ref[dev]
            best = jnp.where(here < low, dev, best)
            low = jnp.minimum(here, low)
        load_ref[best] = low + size

        def put(step, inner):
            slot = best * SLOTS + low + step
            tab_ref[slot] = spot + step
            tab_ref[SEG_AT + slot] = low
            tab_ref[LEN_AT + slot] = jnp.minimum(length - BLK * step, BLK)
            tab_ref[DEST_AT + spot + step] = slot
            return inner

        lax.fori_loop(0, size, put, 0)
        return carry

    lax.fori_loop(0, begin, assign, 0)


def deal_table(lengths):
    micro, per_dev = lengths.shape
    padded = jnp.pad(lengths, ((0, 8 - micro), (0, 128 - per_dev)))
    everyone = pl.pallas_call(
        lens_kernel,
        out_shape=jax.ShapeDtypeStruct((4, 8, 128), jnp.int32),
        in_specs=[VMEM],
        out_specs=VMEM,
        scratch_shapes=[pltpu.SemaphoreType.DMA((3,)), pltpu.SemaphoreType.DMA((3,))],
        compiler_params=pltpu.CompilerParams(collective_id=0, has_side_effects=True),
        name="lens_exchange",
    )(padded)
    return pl.pallas_call(
        partial(table_kernel, micro, per_dev),
        out_shape=jax.ShapeDtypeStruct((TABLE_SIZE,), jnp.int32),
        in_specs=[SMEM],
        out_specs=SMEM,
        scratch_shapes=[
            pltpu.SMEM((4 * micro * per_dev,), jnp.int32),
            pltpu.SMEM((8,), jnp.int32),
            pltpu.SMEM((4,), jnp.int32),
        ],
        name="deal_table",
    )(everyone)


def gather_kernel(
    outer, inner, splits, tab_ref, rows_ref, cots_ref, wa_ref, wb_ref, wc_ref,
    ga_ref, gb_ref, gc_ref, rows_out, cots_out,
    psend, precv, xsend, xrecv,
    z_send, z_recv, y_send, y_recv, c_send, c_recv, own_sem,
    p_send, p_recv, x_send, x_recv,
):
    rank = lax.axis_index("rep")
    spot = lax.axis_index("fsdp")
    core = rank % 2
    row, col = spot // inner, spot % inner
    count = outer * inner
    mate, across = core_of(rank), across_of(rank)
    pieces = [(wa_ref, ga_ref, start, width // 2) for start, width in splits]
    pieces.append((wb_ref, gb_ref, 0, wb_ref.shape[1] // 2))
    pieces.append((wc_ref, gc_ref, 0, None))
    halved = [number for number, piece in enumerate(pieces) if piece[3] is not None]

    barrier = pltpu.get_barrier_semaphore()
    neighbours = (
        (row + 1 < outer, {"fsdp": spot + inner}),
        (row > 0, {"fsdp": spot - inner}),
        (col + 1 < inner, {"fsdp": spot + 1}),
        (col > 0, {"fsdp": spot - 1}),
    )
    amount = jnp.int32(2)
    for there, device in neighbours:
        amount = amount + there.astype(jnp.int32)

        @pl.when(there)
        def _():
            pl.semaphore_signal(barrier, inc=1, device_id=device, device_id_type=MESH)

    for device in (mate, across):
        pl.semaphore_signal(barrier, inc=1, device_id={"rep": device}, device_id_type=MESH)
    pl.semaphore_wait(barrier, amount)

    def cut(ref, number):
        _, _, start, half = pieces[number]
        if half is None:
            return ref
        return ref.at[:, pl.ds(pl.multiple_of(start + core * half, 128), half)]

    def landed(number, shard):
        return cut(pieces[number][1].at[shard], number)

    late = []

    def send(there, src, dst, ssem, rsem, device):
        def describe():
            return pltpu.make_async_remote_copy(
                src_ref=src, dst_ref=dst, send_sem=ssem, recv_sem=rsem,
                device_id=device, device_id_type=MESH,
            )

        if there is None:
            describe().start()
            late.append((None, lambda: describe().wait_send()))
        else:
            @pl.when(there)
            def _():
                describe().start()

            late.append((there, lambda: describe().wait_send()))

    def arrive(number, shard, rsem):
        pltpu.make_async_remote_copy(
            src_ref=landed(number, shard), dst_ref=landed(number, shard),
            send_sem=own_sem.at[0], recv_sem=rsem,
            device_id={"rep": mate}, device_id_type=MESH,
        ).wait_recv()

    def both(first, second):
        return second if first is None else jnp.logical_and(first, second)

    def to_mate(there, number, shard):
        if number not in halved:
            return
        place = landed(number, shard)
        send(there, place, place, c_send.at[number, shard], c_recv.at[number, shard], {"rep": mate})

    def along_row(there, number, line, src):
        shard = line * inner + col
        place = landed(number, shard)
        src = place if src is None else src
        send(both(there, col + 1 < inner), src, place,
             y_send.at[0, 0, line, number], y_recv.at[0, 0, line, number], {"fsdp": spot + 1})
        send(both(there, col > 0), src, place,
             y_send.at[1, 0, line, number], y_recv.at[1, 0, line, number], {"fsdp": spot - 1})

    def from_row(there, number, line):
        for step in range(inner - 1):
            for way, source, onward, target in (
                (0, col - 1 - step, col + 1 < inner, spot + 1),
                (1, col + 1 + step, col > 0, spot - 1),
            ):
                here = jnp.logical_and(source >= 0, source < inner)
                here = both(there, here)
                shard = line * inner + source

                @pl.when(here)
                def _():
                    arrive(number, shard, y_recv.at[way, step, line, number])

                if step + 1 < inner - 1:
                    place = landed(number, shard)
                    send(both(here, onward), place, place,
                         y_send.at[way, step + 1, line, number],
                         y_recv.at[way, step + 1, line, number], {"fsdp": target})
                to_mate(here, number, shard)

    for number, piece in enumerate(pieces):
        src, place = cut(piece[0], number), landed(number, spot)
        send(row + 1 < outer, src, place, z_send.at[0, 0, number], z_recv.at[0, 0, number],
             {"fsdp": spot + inner})
        send(row > 0, src, place, z_send.at[1, 0, number], z_recv.at[1, 0, number],
             {"fsdp": spot - inner})
        along_row(None, number, row, src)
    own = [
        pltpu.make_async_copy(wa_ref, ga_ref.at[spot], own_sem.at[0]),
        pltpu.make_async_copy(wb_ref, gb_ref.at[spot], own_sem.at[1]),
        pltpu.make_async_copy(wc_ref, gc_ref.at[spot], own_sem.at[2]),
    ]
    for copy in own:
        copy.start()

    sources = (rows_ref, cots_ref)
    per_rank = rows_ref.shape[0]

    def picked(kind, target, slot):
        index = tab_ref[target * SLOTS + slot] - rank * per_rank
        mine = jnp.logical_and(index >= 0, index < per_rank)
        value = sources[kind][jnp.clip(index, 0, per_rank - 1)]
        return mine, value

    def mate_copy(kind, part):
        return pltpu.make_async_remote_copy(
            src_ref=psend.at[kind, part], dst_ref=precv.at[kind, part],
            send_sem=p_send.at[kind, part], recv_sem=p_recv.at[kind, part],
            device_id={"rep": mate}, device_id_type=MESH,
        )

    def across_copy(kind):
        return pltpu.make_async_remote_copy(
            src_ref=xsend.at[kind], dst_ref=xrecv.at[kind],
            send_sem=x_send.at[kind], recv_sem=x_recv.at[kind],
            device_id={"rep": across}, device_id_type=MESH,
        )

    for kind, part in ((0, 1), (1, 1), (0, 0), (1, 0)):
        target = mate if part == 0 else across_of(mate)

        def pack(slot, carry):
            mine, value = picked(kind, target, slot)
            psend[kind, part, slot] = jnp.where(mine, value, jnp.zeros_like(value))
            return carry

        lax.fori_loop(0, SLOTS, pack, 0)
        mate_copy(kind, part).start()
    for kind in range(2):
        mate_copy(kind, 1).wait_recv()

        def merge(slot, carry):
            mine, value = picked(kind, across, slot)
            xsend[kind, slot] = jnp.where(mine, value, precv[kind, 1, slot])
            return carry

        lax.fori_loop(0, SLOTS, merge, 0)
        across_copy(kind).start()

    def lines(step):
        return ((row - 1 - step >= 0, row - 1 - step, 0, row + 1 < outer, spot + inner),
                (row + 1 + step < outer, row + 1 + step, 1, row > 0, spot - inner))

    for step in range(outer - 1):
        for number in range(len(pieces)):
            for here, line, way, onward, target in lines(step):
                shard = line * inner + col

                @pl.when(here)
                def _():
                    arrive(number, shard, z_recv.at[way, step, number])

                if step + 1 < outer - 1:
                    place = landed(number, shard)
                    send(jnp.logical_and(here, onward), place, place,
                         z_send.at[way, step + 1, number], z_recv.at[way, step + 1, number],
                         {"fsdp": target})
                along_row(here, number, line, None)
                to_mate(here, number, shard)
        for number in range(len(pieces)):
            if step == 0:
                from_row(None, number, row)
            else:
                for here, line, *_ in lines(step - 1):
                    from_row(here, number, line)
    for number in range(len(pieces)):
        for here, line, *_ in lines(outer - 2):
            from_row(here, number, line)

    outs = (rows_out, cots_out)
    for kind in range(2):
        mate_copy(kind, 0).wait_recv()
        across_copy(kind).wait_recv()

        def finish(slot, carry):
            mine, value = picked(kind, rank, slot)
            outs[kind][slot] = jnp.where(mine, value, precv[kind, 0, slot] + xrecv[kind, slot])
            return carry

        lax.fori_loop(0, SLOTS, finish, 0)

    for shard in range(count):
        @pl.when(shard != spot)
        def _():
            for number in halved:
                other = pieces[number]
                view = other[1].at[shard].at[:, pl.ds(0, other[3])]
                pltpu.make_async_remote_copy(
                    src_ref=view, dst_ref=view, send_sem=own_sem.at[0],
                    recv_sem=c_recv.at[number, shard],
                    device_id={"rep": mate}, device_id_type=MESH,
                ).wait_recv()
    for there, finish_send in late:
        if there is None:
            finish_send()
        else:
            pl.when(there)(finish_send)
    for kind in range(2):
        for part in range(2):
            mate_copy(kind, part).wait_send()
        across_copy(kind).wait_send()
    for copy in own:
        copy.wait()


def gather_weights(count, splits, table, rows, cots, wa, wb, wc):
    outer, inner = grid_of(count)
    block = rows.shape[1:]
    kinds = len(splits) + 2
    dma = pltpu.SemaphoreType.DMA
    bf16 = jnp.bfloat16
    return pl.pallas_call(
        partial(gather_kernel, outer, inner, splits),
        out_shape=(
            jax.ShapeDtypeStruct((count,) + wa.shape, bf16),
            jax.ShapeDtypeStruct((count,) + wb.shape, bf16),
            jax.ShapeDtypeStruct((count,) + wc.shape, bf16),
            jax.ShapeDtypeStruct((SLOTS,) + block, bf16),
            jax.ShapeDtypeStruct((SLOTS,) + block, bf16),
        ),
        in_specs=[SMEM, VMEM, VMEM, VMEM, VMEM, VMEM],
        out_specs=(ANY, ANY, ANY, VMEM, VMEM),
        scratch_shapes=[
            pltpu.VMEM((2, 2, SLOTS) + block, bf16),
            pltpu.VMEM((2, 2, SLOTS) + block, bf16),
            pltpu.VMEM((2, SLOTS) + block, bf16),
            pltpu.VMEM((2, SLOTS) + block, bf16),
            dma((2, outer - 1, kinds)), dma((2, outer - 1, kinds)),
            dma((2, inner - 1, outer, kinds)), dma((2, inner - 1, outer, kinds)),
            dma((kinds, count)), dma((kinds, count)), dma((3,)),
            dma((2, 2)), dma((2, 2)), dma((2,)), dma((2,)),
        ],
        compiler_params=pltpu.CompilerParams(
            collective_id=1, has_side_effects=True, vmem_limit_bytes=VMEM_LIMIT
        ),
        name="gather_and_deal",
    )(table, rows, cots, wa, wb, wc)


def reduce_kernel(
    outer, inner, kinds, *refs
):
    grads, (y_ref, g_ref) = refs[:kinds], refs[kinds : kinds + 2]
    totals, (ry_ref, rg_ref) = refs[kinds + 2 : 2 * kinds + 2], refs[2 * kinds + 2 : 2 * kinds + 4]
    scratch = refs[2 * kinds + 4 :]
    mines, crecvs, yrecvs, zrecvs, xrecvs = (
        scratch[kinds * i : kinds * (i + 1)] for i in range(5)
    )
    (c_send, c_recv, m_sem, y_send, y_recv, z_send, z_recv, x_send, x_recv, f_send, f_recv,
     r_send, r_recv, q_sem) = scratch[5 * kinds :]
    rank = lax.axis_index("rep")
    spot = lax.axis_index("fsdp")
    core = rank % 2
    row, col = spot // inner, spot % inner
    mate, across = core_of(rank), across_of(rank)
    pieces = [(src, dst, 0, src.shape[3] // 2) for src, dst in zip(grads[:-1], totals)]
    pieces.append((grads[-1], totals[-1], 0, None))

    barrier = pltpu.get_barrier_semaphore()
    neighbours = (
        (row + 1 < outer, {"fsdp": spot + inner}),
        (row > 0, {"fsdp": spot - inner}),
        (col + 1 < inner, {"fsdp": spot + 1}),
        (col > 0, {"fsdp": spot - 1}),
    )
    amount = jnp.int32(2)
    for there, device in neighbours:
        amount = amount + there.astype(jnp.int32)

        @pl.when(there)
        def _():
            pl.semaphore_signal(barrier, inc=1, device_id=device, device_id_type=MESH)

    for device in (mate, across):
        pl.semaphore_signal(barrier, inc=1, device_id={"rep": device}, device_id_type=MESH)
    pl.semaphore_wait(barrier, amount)

    late = []

    def send(there, src, dst, ssem, rsem, device):
        def describe():
            return pltpu.make_async_remote_copy(
                src_ref=src, dst_ref=dst, send_sem=ssem, recv_sem=rsem,
                device_id=device, device_id_type=MESH,
            )

        if there is None:
            describe().start()
            late.append((None, lambda: describe().wait_send()))
        else:
            @pl.when(there)
            def _():
                describe().start()

            late.append((there, lambda: describe().wait_send()))

    def arrive(place, rsem):
        pltpu.make_async_remote_copy(
            src_ref=place, dst_ref=place, send_sem=q_sem.at[0], recv_sem=rsem,
            device_id={"rep": mate}, device_id_type=MESH,
        ).wait_recv()

    def columns(ref, number, which):
        _, _, start, half = pieces[number]
        if half is None:
            return ref
        cols = pl.ds(pl.multiple_of(start + which * half, 128), half)
        return ref.at[:, :, :, cols] if len(ref.shape) == 4 else ref.at[:, cols]

    order = list(range(kinds))
    loads = []
    for number in order:
        src = columns(pieces[number][0], number, 1 - core)
        send(None, src, crecvs[number], c_send.at[number], c_recv.at[number], {"rep": mate})
        load = pltpu.make_async_copy(
            columns(pieces[number][0], number, core), mines[number], m_sem.at[number]
        )
        load.start()
        loads.append(load)

    for kind, (src, dst) in enumerate(((y_ref, ry_ref), (g_ref, rg_ref))):
        send(None, src, dst.at[rank], r_send.at[kind, 0], r_recv.at[kind, 0], {"rep": across})
        send(None, src, dst.at[rank], r_send.at[kind, 1], r_recv.at[kind, 1], {"rep": mate})
        pltpu.make_async_copy(src, dst.at[rank], q_sem.at[kind + 1]).start()

    def slot_of(way, size, place, dest):
        if size == 2:
            return 0
        return dest - place if way == 0 else size - place + dest

    def line_sum(number, size, place, stride, buffer, view, ssem, rsem):
        for far in range(size - 1, 0, -1):
            for way in range(2):
                dest = far if way == 0 else size - 1 - far
                step = 1 if way == 0 else -1
                passes = place < dest if way == 0 else place > dest
                first = place == 0 if way == 0 else place == size - 1
                mine = view(dest)
                got = slot_of(way, size, place, dest)

                @pl.when(jnp.logical_and(passes, jnp.logical_not(first)))
                def _():
                    arrive(buffer.at[got], rsem.at[got, number])
                    mine[...] = mine[...] + buffer[got]

                put = slot_of(way, size, place + step, dest)
                send(passes, mine, buffer.at[put], ssem.at[way, dest, number], rsem.at[put, number],
                     {"fsdp": spot + step * stride})
        for way in range(2):
            has = place > 0 if way == 0 else place < size - 1
            got = slot_of(way, size, place, place)
            mine = view(place)

            @pl.when(has)
            def _():
                arrive(buffer.at[got], rsem.at[got, number])
                mine[...] = mine[...] + buffer[got]

    for number in order:
        loads[number].wait()
        arrive(crecvs[number], c_recv.at[number])
        mine, other = mines[number], crecvs[number]

        def add(index, carry):
            mine[index // inner, index % inner] = (
                mine[index // inner, index % inner] + other[index // inner, index % inner]
            )
            return carry

        lax.fori_loop(0, outer * inner, add, 0)
        if inner == 2:
            send(None, mine.at[:, 1 - col], yrecvs[number].at[0], y_send.at[0, 0, number],
                 y_recv.at[0, number], {"fsdp": spot + 1 - 2 * col})
    for kind, dst in enumerate((ry_ref, rg_ref)):
        place = dst.at[across]
        arrive(place, r_recv.at[kind, 0])
        send(None, place, place, r_send.at[kind, 2], r_recv.at[kind, 2], {"rep": mate})
    for number in order:
        mine = mines[number]
        if inner == 2:
            arrive(yrecvs[number].at[0], y_recv.at[0, number])
            buffer = yrecvs[number]

            def add(index, carry):
                mine[index, col] = mine[index, col] + buffer[0, index]
                return carry

            lax.fori_loop(0, outer, add, 0)
        else:
            line_sum(number, inner, col, 1, yrecvs[number], lambda dest: mine.at[:, dest],
                     y_send, y_recv)
        line_sum(number, outer, row, inner, zrecvs[number], lambda dest: mine.at[dest, col],
                 z_send, z_recv)
        send(None, mine.at[row, col], xrecvs[number], x_send.at[number], x_recv.at[number],
             {"rep": across})
    for number in order:
        arrive(xrecvs[number], x_recv.at[number])
        total = mines[number][row, col].astype(jnp.float32) + xrecvs[number][...].astype(jnp.float32)
        out, half = pieces[number][1], pieces[number][3]
        place = columns(out, number, core)
        place[...] = total
        if half is not None:
            send(None, place, place, f_send.at[number], f_recv.at[number], {"rep": mate})
    for number in order:
        if pieces[number][3] is not None:
            arrive(columns(pieces[number][1], number, 1 - core), f_recv.at[number])
    for kind, dst in enumerate((ry_ref, rg_ref)):
        arrive(dst.at[mate], r_recv.at[kind, 1])
        arrive(dst.at[across_of(mate)], r_recv.at[kind, 2])
        src = y_ref if kind == 0 else g_ref
        pltpu.make_async_copy(src, dst.at[rank], q_sem.at[kind + 1]).wait()
    for there, finish_send in late:
        if there is None:
            finish_send()
        else:
            pl.when(there)(finish_send)


def reduce_grads(count, grads, y_rows, g_rows):
    outer, inner = grid_of(count)
    kinds = len(grads)
    shapes = [(grad.shape[1], grad.shape[2] // 2, grad.dtype) for grad in grads[:-1]]
    shapes.append(grads[-1].shape[1:] + (grads[-1].dtype,))
    dma = pltpu.SemaphoreType.DMA
    y_slots = 1 if inner == 2 else inner + 1
    z_slots = 1 if outer == 2 else outer + 1
    scratch = []
    for lead in ((outer, inner), (outer, inner), (y_slots, outer), (z_slots,), ()):
        scratch += [pltpu.VMEM(lead + (a, b), dtype) for a, b, dtype in shapes]
    scratch += [
        dma((kinds,)), dma((kinds,)), dma((kinds,)),
        dma((2, inner, kinds)), dma((y_slots, kinds)),
        dma((2, outer, kinds)), dma((z_slots, kinds)),
        dma((kinds,)), dma((kinds,)), dma((kinds,)), dma((kinds,)),
        dma((2, 3)), dma((2, 3)), dma((3,)),
    ]
    return pl.pallas_call(
        partial(reduce_kernel, outer, inner, kinds),
        out_shape=tuple(jax.ShapeDtypeStruct(grad.shape[1:], jnp.float32) for grad in grads) + (
            jax.ShapeDtypeStruct((4,) + y_rows.shape, y_rows.dtype),
            jax.ShapeDtypeStruct((4,) + g_rows.shape, g_rows.dtype),
        ),
        in_specs=[ANY] * (kinds + 2),
        out_specs=(VMEM,) * kinds + (ANY, ANY),
        scratch_shapes=scratch,
        compiler_params=pltpu.CompilerParams(
            collective_id=2, has_side_effects=True, vmem_limit_bytes=VMEM_LIMIT
        ),
        name="reduce_and_return",
    )(*(grad.reshape((outer, inner) + grad.shape[1:]) for grad in grads), y_rows, g_rows)


def home_kernel(tab_ref, ry_ref, rg_ref, y_ref, g_ref):
    base = lax.axis_index("rep") * y_ref.shape[0]

    def fetch(block, carry):
        index = tab_ref[DEST_AT + base + block] if len(tab_ref.shape) == 1 else tab_ref[48, base + block]
        safe = jnp.maximum(index, 0)
        for src, dst in ((ry_ref, y_ref), (rg_ref, g_ref)):
            value = src[safe // SLOTS, safe % SLOTS]
            dst[block] = jnp.where(index >= 0, value, jnp.zeros_like(value))
        return carry

    lax.fori_loop(0, y_ref.shape[0], fetch, 0)


def bring_home(table, ry, rg, blocks):
    shape = jax.ShapeDtypeStruct((blocks,) + ry.shape[2:], ry.dtype)
    return pl.pallas_call(
        home_kernel,
        out_shape=(shape, shape),
        in_specs=[SMEM, VMEM, VMEM],
        out_specs=(VMEM, VMEM),
        compiler_params=pltpu.CompilerParams(vmem_limit_bytes=VMEM_LIMIT),
        name="place_rows",
    )(table, ry, rg)


D = H * DH
ROWS = SLOTS * BLK
SIDES = SLOTS * (BLK // GBLK)
SIDE_ROWS = 48
ALL_ROWS = ROWS + SIDE_ROWS
QT = 128
WIN = 384
TILES = ROWS // QT
QUAD = 256
FF_TILE = 256
GELU_C = 0.7978845608028654
GELU_A = 0.044715
F32, BF16 = jnp.float32, jnp.bfloat16


def mm(left, right):
    return lax.dot_general(left, right, (((1,), (0,)), ((), ())), preferred_element_type=F32)


def mm_cols(left, right):
    return lax.dot_general(left, right, (((1,), (1,)), ((), ())), preferred_element_type=F32)


def mm_rows(left, right):
    return lax.dot_general(left, right, (((0,), (0,)), ((), ())), preferred_element_type=F32)


def iota(shape, axis):
    return lax.broadcasted_iota(jnp.int32, shape, axis)


def pick_by(index, values, other):
    out = jnp.full(index.shape, other, jnp.int32)
    for number, value in enumerate(values):
        out = jnp.where(index == number, value, out)
    return out


def block_at(tab_ref, slot):
    return lax.rem(tab_ref[slot, 0], 128) - 1


def seg_at(tab_ref, slot):
    if len(tab_ref.shape) == 1:
        return tab_ref[SEG_AT + slot]
    return lax.div(tab_ref[slot, 0], 16384) - 1


def len_at(tab_ref, slot):
    if len(tab_ref.shape) == 1:
        return tab_ref[LEN_AT + slot]
    return lax.rem(lax.div(tab_ref[slot, 0], 128), 128)


def slot_info(tab_ref, rank):
    seg = [seg_at(tab_ref, rank * SLOTS + slot) for slot in range(SLOTS)]
    length = [len_at(tab_ref, rank * SLOTS + slot) for slot in range(SLOTS)]
    return seg, length


def valid_column(tab_ref, rank):
    _, length = slot_info(tab_ref, rank)
    row = iota((ROWS, 1), 0)
    return ((row % BLK) < pick_by(row // BLK, length, 0)).astype(F32)


def pooling(tab_ref, rank):
    _, length = slot_info(tab_ref, rank)
    row = iota((1, ROWS), 1)
    block = jnp.where((row % BLK) < pick_by(row // BLK, length, 0), row // GBLK, -1)
    return jnp.where(iota((SIDE_ROWS, ROWS), 0) == block, 1.0, 0.0).astype(BF16)


def key_segments(tab_ref, rank, first_block, index):
    blocks = WIN // BLK
    base = rank * SLOTS + first_block
    seg = [seg_at(tab_ref, base + step) for step in range(blocks)]
    length = [len_at(tab_ref, base + step) for step in range(blocks)]
    alive = (index % BLK) < pick_by(index // BLK, length, 0)
    return jnp.where(alive, pick_by(index // BLK, seg, -2), -2)


def side_segments(tab_ref, rank, index):
    seg, length = slot_info(tab_ref, rank)
    per = BLK // GBLK
    alive = (index % per) * GBLK < pick_by(index // per, length, 0)
    return jnp.where(alive, pick_by(index // per, seg, -2), -2)


def tile_bias(tab_ref, rank, tile, first_row, keys_axis):
    qs, ks, gs = ((QT, 1), (1, WIN), (1, SIDE_ROWS)) if keys_axis == 1 else ((1, QT), (WIN, 1), (SIDE_ROWS, 1))
    q_index = iota(qs, 1 - keys_axis)
    k_index = iota(ks, keys_axis)
    g_index = iota(gs, keys_axis)
    base = rank * SLOTS + tile * (QT // BLK)
    q_seg = pick_by(q_index // BLK, [seg_at(tab_ref, base + step) for step in range(QT // BLK)], -1)
    k_seg = key_segments(tab_ref, rank, first_row // BLK, k_index)
    g_seg = side_segments(tab_ref, rank, g_index)
    gap = (q_index + tile * QT) - (k_index + first_row)
    local = (jnp.abs(gap) <= RADIUS) & (q_seg == k_seg)
    return jnp.where(local, 0.0, MASKED_SCORE), jnp.where(q_seg == g_seg, 0.0, MASKED_SCORE)


def window_start(tile):
    return pl.multiple_of(jnp.clip(tile - 1, 0, TILES - WIN // QT) * QT, QT)


def head_stack(rows):
    lane = iota(rows.shape, 1) // DH
    zero = jnp.zeros_like(rows)
    return jnp.concatenate([jnp.where(lane == head, rows, zero) for head in range(QUAD // DH)], axis=0)


def head_merge(stacked):
    lane = iota((QT, QUAD), 1) // DH
    out = stacked[:QT]
    for head in range(1, QUAD // DH):
        out = jnp.where(lane == head, stacked[head * QT : (head + 1) * QT], out)
    return out


def gains_of(gc_ref):
    count = gc_ref.shape[0]
    part = D // count
    lane, column = iota((128, D), 0), iota((128, D), 1)
    total = None
    for shard in range(count):
        pick = jnp.where((column == lane + shard * part) & (lane < part), 1.0, 0.0).astype(BF16)
        term = mm(gc_ref[shard], pick)
        total = term if total is None else total + term
    return total


def three_way(value):
    high = value.astype(BF16)
    rest = value - high.astype(F32)
    middle = rest.astype(BF16)
    return high, middle, (rest - middle.astype(F32)).astype(BF16)


def spread_gain_grads(value, dc_ref):
    count = dc_ref.shape[0] if len(dc_ref.shape) == 3 else dc_ref.shape[0] * dc_ref.shape[1]
    part = D // count
    column, lane = iota((D, 128), 0), iota((D, 128), 1)
    parts = three_way(value)
    for shard in range(count):
        pick = jnp.where((column == lane + shard * part) & (lane < part), 1.0, 0.0).astype(BF16)
        place = dc_ref.at[shard] if len(dc_ref.shape) == 3 else dc_ref.at[shard // dc_ref.shape[1], shard % dc_ref.shape[1]]
        place[...] = mm(parts[0], pick) + mm(parts[1], pick) + mm(parts[2], pick)


def mean_square(value):
    return jnp.mean(value * value, axis=-1, keepdims=True)


def forward_norm(tab_ref, rank, x_ref, gains, n_ref):
    for tile in range(TILES):
        rows = pl.ds(tile * QT, QT)
        value = x_ref[rows, :].astype(F32)
        n_ref[rows, :] = (value * lax.rsqrt(mean_square(value) + EPSILON) * gains[0:1]).astype(BF16)
    side = mm(pooling(tab_ref, rank), n_ref[:ROWS, :])
    n_ref[ROWS:, :] = (side * lax.rsqrt(mean_square(side) + EPSILON) * gains[1:2]).astype(BF16)


def forward_project(n_ref, w_ref, qkv_ref):
    def step(tile, carry):
        cols = pl.ds(pl.multiple_of(tile * QUAD, QUAD), QUAD)
        qkv_ref[:, cols] = mm(n_ref[...], w_ref[:, cols]).astype(BF16)
        return carry

    lax.fori_loop(0, 3 * D // QUAD, step, 0)


def forward_attention(tab_ref, rank, qkv_ref, att_ref, lse_ref, begin, end):
    def step(tile, carry):
        first = window_start(tile)
        bias, side_bias = tile_bias(tab_ref, rank, tile, first, 1)
        rows = pl.ds(pl.multiple_of(tile * QT, QT), QT)
        window = pl.ds(first, WIN)
        lse = jnp.zeros((QT, 128), F32)
        lane = iota((QT, 128), 1)
        for quad in range(D // QUAD):
            low = quad * QUAD
            query = head_stack(qkv_ref[rows, low : low + QUAD])
            scores = mm_cols(query, qkv_ref[window, D + low : D + low + QUAD])
            side_scores = mm_cols(query, qkv_ref[ROWS:, D + low : D + low + QUAD])
            local, sides, scale = [], [], []
            for head in range(QUAD // DH):
                part = slice(head * QT, (head + 1) * QT)
                one = scores[part] + bias
                two = side_scores[part] + side_bias
                peak = jnp.maximum(
                    jnp.max(one, axis=-1, keepdims=True), jnp.max(two, axis=-1, keepdims=True)
                )
                one, two = jnp.exp(one - peak), jnp.exp(two - peak)
                total = jnp.sum(one, axis=-1, keepdims=True) + jnp.sum(two, axis=-1, keepdims=True)
                local.append(one.astype(BF16))
                sides.append(two.astype(BF16))
                scale.append(1.0 / total)
                lse = jnp.where(lane == quad * (QUAD // DH) + head, peak + jnp.log(total), lse)
            mixed = mm(jnp.concatenate(local, axis=0), qkv_ref[window, 2 * D + low : 2 * D + low + QUAD])
            mixed = mixed + mm(
                jnp.concatenate(sides, axis=0), qkv_ref[ROWS:, 2 * D + low : 2 * D + low + QUAD]
            )
            mixed = mixed * jnp.concatenate(scale, axis=0)
            att_ref[rows, low : low + QUAD] = head_merge(mixed).astype(BF16)
        lse_ref[tile] = jnp.transpose(lse)[:16]
        return carry

    lax.fori_loop(begin, end, step, 0)


def feed_forward(tab_ref, rank, x_ref, cot_ref, att_ref, gains, w_ref, wb_ref,
                 y_ref, gh_ref, ga_ref, dg_ref, du_ref, db_ref, do_ref,
                 h1_ref, nt_ref, ntt_ref, gres_ref, h2_ref, gg_ref, gu_ref, gn_ref):
    hidden = wb_ref.shape[0]
    gate_at = w_ref.shape[1] - 2 * hidden
    out_at = gate_at - D
    valid = valid_column(tab_ref, rank)
    gain = gains[2:3]
    for tile in range(TILES):
        rows = pl.ds(tile * QT, QT)
        value = x_ref[rows, :].astype(F32) + mm(att_ref[rows, :], w_ref[:, out_at:gate_at])
        h1_ref[rows, :] = value
        normed = (value * lax.rsqrt(mean_square(value) + EPSILON) * gain).astype(BF16)
        nt_ref[rows, :] = normed
        ntt_ref[:, tile * QT : (tile + 1) * QT] = jnp.transpose(normed)
        gres_ref[rows, :] = (cot_ref[rows, :].astype(F32) * valid[tile * QT : (tile + 1) * QT]).astype(BF16)

    def inward(tile, carry):
        at = pl.multiple_of(tile * FF_TILE, FF_TILE)
        cols = pl.ds(at, FF_TILE)
        gate = mm(nt_ref[...], w_ref[:, pl.ds(gate_at + at, FF_TILE)])
        up = mm(nt_ref[...], w_ref[:, pl.ds(gate_at + hidden + at, FF_TILE)])
        back = mm_cols(gres_ref[...], wb_ref[cols, :])
        square = gate * gate
        bend = jnp.tanh(GELU_C * (gate * (1.0 + GELU_A * square)))
        half = 0.5 * (1.0 + bend)
        act = gate * half
        slope = half + (0.5 * GELU_C) * gate * (1.0 - bend * bend) * (1.0 + (3.0 * GELU_A) * square)
        h2_ref[:, cols] = (act * up).astype(BF16)
        gg_ref[:, cols] = (back * up * slope).astype(BF16)
        gu_ref[:, cols] = (back * act).astype(BF16)
        return carry

    lax.fori_loop(0, hidden // FF_TILE, inward, 0)

    def outward(tile, carry):
        cols = pl.ds(pl.multiple_of(tile * QUAD, QUAD), QUAD)
        value = h1_ref[:, cols] + mm(h2_ref[...], wb_ref[:, cols])
        y_ref[:, cols] = (value * valid).astype(BF16)
        gn_ref[:, cols] = mm_cols(gg_ref[...], w_ref[cols, gate_at : gate_at + hidden]) + mm_cols(
            gu_ref[...], w_ref[cols, gate_at + hidden :]
        )
        return carry

    lax.fori_loop(0, D // QUAD, outward, 0)

    def weights(tile, carry):
        at = pl.multiple_of(tile * FF_TILE, FF_TILE)
        cols = pl.ds(at, FF_TILE)
        dg_ref[:, cols] = mm(ntt_ref[...], gg_ref[:, cols]).astype(BF16)
        du_ref[:, cols] = mm(ntt_ref[...], gu_ref[:, cols]).astype(BF16)
        db_ref[cols, :] = mm_rows(h2_ref[:, cols], gres_ref[...]).astype(BF16)
        return carry

    lax.fori_loop(0, hidden // FF_TILE, weights, 0)

    gain_grad = jnp.zeros((1, D), F32)
    for tile in range(TILES):
        rows = pl.ds(tile * QT, QT)
        value, grad = h1_ref[rows, :], gn_ref[rows, :]
        root = lax.rsqrt(mean_square(value) + EPSILON)
        unit = value * root
        gain_grad = gain_grad + jnp.sum(grad * unit, axis=0, keepdims=True)
        grad = grad * gain
        grad = gres_ref[rows, :].astype(F32) + root * (
            grad - unit * jnp.mean(grad * unit, axis=-1, keepdims=True)
        )
        gh_ref[rows, :] = grad
        low = grad.astype(BF16)
        nt_ref[rows, :] = low
        ga_ref[rows, :] = mm_cols(low, w_ref[:, out_at:gate_at]).astype(BF16)

    def out_weight(tile, carry):
        cols = pl.ds(pl.multiple_of(tile * QUAD, QUAD), QUAD)
        do_ref[cols, :] = mm_rows(att_ref[:, cols], nt_ref[...]).astype(BF16)
        return carry

    lax.fori_loop(0, D // QUAD, out_weight, 0)
    return gain_grad


def backward_attention_start(dk_ref, dv_ref):
    dk_ref[...] = jnp.zeros_like(dk_ref)
    dv_ref[...] = jnp.zeros_like(dv_ref)


def backward_attention_tiles(tab_ref, rank, qkv_ref, att_ref, ga_ref, lse_ref, dqkv_ref, dk_ref, dv_ref, begin, end):
    heads = QUAD // DH
    marks = jnp.where(iota((16, D), 1) // DH == iota((16, D), 0), 1.0, 0.0).astype(BF16)

    def step(tile, carry):
        first = window_start(tile)
        bias, side_bias = tile_bias(tab_ref, rank, tile, first, 0)
        bias = jnp.concatenate([bias, side_bias], axis=0)
        rows = pl.ds(pl.multiple_of(tile * QT, QT), QT)
        window = pl.ds(first, WIN)
        product = ga_ref[rows, :].astype(F32) * att_ref[rows, :].astype(F32)
        high = product.astype(BF16)
        rest = (product - high.astype(F32)).astype(BF16)
        centre = mm_cols(marks, high) + mm_cols(marks, rest)
        lse = lse_ref[tile]
        for quad in range(D // QUAD):
            low = quad * QUAD
            query = head_stack(qkv_ref[rows, low : low + QUAD])
            grad = head_stack(ga_ref[rows, low : low + QUAD])
            keys = jnp.concatenate(
                [qkv_ref[window, D + low : D + low + QUAD], qkv_ref[ROWS:, D + low : D + low + QUAD]], axis=0
            )
            values = jnp.concatenate(
                [qkv_ref[window, 2 * D + low : 2 * D + low + QUAD],
                 qkv_ref[ROWS:, 2 * D + low : 2 * D + low + QUAD]], axis=0
            )
            scores = mm_cols(keys, query)
            slopes = mm_cols(values, grad)
            probs, grads = [], []
            for head in range(heads):
                part = slice(head * QT, (head + 1) * QT)
                number = quad * heads + head
                prob = jnp.exp(scores[:, part] + bias - lse[number : number + 1])
                probs.append(prob.astype(BF16))
                grads.append((prob * (slopes[:, part] - centre[number : number + 1])).astype(BF16))
            probs = jnp.concatenate(probs, axis=1)
            grads = jnp.concatenate(grads, axis=1)
            dkey = mm(grads, query)
            dvalue = mm(probs, grad)
            cols = slice(low, low + QUAD)
            dk_ref[window, cols] = dk_ref[window, cols] + dkey[:WIN]
            dk_ref[ROWS:, cols] = dk_ref[ROWS:, cols] + dkey[WIN:]
            dv_ref[window, cols] = dv_ref[window, cols] + dvalue[:WIN]
            dv_ref[ROWS:, cols] = dv_ref[ROWS:, cols] + dvalue[WIN:]
            dqkv_ref[rows, cols] = head_merge(mm_rows(grads, keys)).astype(BF16)
        return carry

    lax.fori_loop(begin, end, step, 0)


def backward_attention_end(dqkv_ref, dk_ref, dv_ref):
    dqkv_ref[ROWS:, :D] = jnp.zeros((SIDE_ROWS, D), BF16)
    dqkv_ref[:, D : 2 * D] = dk_ref[...].astype(BF16)
    dqkv_ref[:, 2 * D :] = dv_ref[...].astype(BF16)


def weight_grads(n_ref, dqkv_ref, refs):
    for number, ref in enumerate(refs):
        def weights(tile, carry):
            at = pl.multiple_of(tile * QUAD, QUAD)
            value = mm_rows(n_ref[...], dqkv_ref[:, pl.ds(number * D + at, QUAD)]).astype(BF16)
            if len(ref.shape) == 4:
                ref[:, :, :, pl.ds(at, QUAD)] = value.reshape(ref.shape[:3] + (QUAD,))
            else:
                ref[:, pl.ds(at, QUAD)] = value
            return carry

        lax.fori_loop(0, D // QUAD, weights, 0)


def backward_project(tab_ref, rank, x_ref, gh_ref, gains, n_ref, dqkv_ref, w_ref, gn_ref, g_ref):
    def step(tile, carry):
        cols = pl.ds(pl.multiple_of(tile * QUAD, QUAD), QUAD)
        gn_ref[:, cols] = mm_cols(dqkv_ref[...], w_ref[cols, : 3 * D])
        return carry

    lax.fori_loop(0, D // QUAD, step, 0)
    pool = pooling(tab_ref, rank)
    side = mm(pool, n_ref[:ROWS, :])
    root = lax.rsqrt(mean_square(side) + EPSILON)
    unit = side * root
    grad = gn_ref[ROWS:, :]
    side_gain = jnp.sum(grad * unit, axis=0, keepdims=True)
    grad = grad * gains[1:2]
    grad = root * (grad - unit * jnp.mean(grad * unit, axis=-1, keepdims=True))
    parts = three_way(grad)
    gain_grad = jnp.zeros((1, D), F32)
    for tile in range(TILES):
        rows = pl.ds(tile * QT, QT)
        spread = pool[:, tile * QT : (tile + 1) * QT]
        total = gn_ref[rows, :] + mm_rows(spread, parts[0]) + mm_rows(spread, parts[1])
        value = x_ref[rows, :].astype(F32)
        root = lax.rsqrt(mean_square(value) + EPSILON)
        unit = value * root
        gain_grad = gain_grad + jnp.sum(total * unit, axis=0, keepdims=True)
        total = total * gains[0:1]
        value = (
            gh_ref[rows, :] + root * (total - unit * jnp.mean(total * unit, axis=-1, keepdims=True))
        ).astype(BF16)
        if len(g_ref.shape) == 3:
            g_ref[pl.ds(tile * (QT // BLK), QT // BLK)] = value.reshape(QT // BLK, BLK, D)
        else:
            g_ref[rows, :] = value
    return gain_grad, side_gain


def first_kernel(tab_ref, x_ref, gc_ref, w_ref, n_ref, qkv_ref, att_ref, lse_ref):
    rank = lax.axis_index("rep")
    gains = gains_of(gc_ref)
    forward_norm(tab_ref, rank, x_ref, gains, n_ref)
    forward_project(n_ref, w_ref, qkv_ref)
    forward_attention(tab_ref, rank, qkv_ref, att_ref, lse_ref, 0, TILES)


def second_kernel(tab_ref, x_ref, cot_ref, att_ref, gc_ref, w_ref, wb_ref,
                  y_ref, gh_ref, ga_ref, dg_ref, du_ref, db_ref, do_ref, gain_ref, *scratch):
    rank = lax.axis_index("rep")
    gain_ref[...] = feed_forward(tab_ref, rank, x_ref, cot_ref, att_ref, gains_of(gc_ref), w_ref, wb_ref,
                                 y_ref, gh_ref, ga_ref, dg_ref, du_ref, db_ref, do_ref, *scratch)


def third_kernel(tab_ref, x_ref, gh_ref, ga_ref, att_ref, lse_ref, n_ref, qkv_ref, gain_ref, gc_ref, w_ref,
                 g_ref, dw_ref, dc_ref, dqkv_ref, dk_ref, dv_ref, gn_ref):
    rank = lax.axis_index("rep")
    gains = gains_of(gc_ref)
    backward_attention_start(dk_ref, dv_ref)
    backward_attention_tiles(tab_ref, rank, qkv_ref, att_ref, ga_ref, lse_ref, dqkv_ref, dk_ref, dv_ref, 0, TILES)
    backward_attention_end(dqkv_ref, dk_ref, dv_ref)
    weight_grads(n_ref, dqkv_ref, [dw_ref.at[:, i * D : (i + 1) * D] for i in range(3)])
    one, side = backward_project(tab_ref, rank, x_ref, gh_ref, gains, n_ref, dqkv_ref, w_ref, gn_ref, g_ref)
    grads = jnp.concatenate([one, side, gain_ref[...], jnp.zeros((5, D), F32)], axis=0)
    spread_gain_grads(grads, dc_ref)


def attend(tab, x, gc, w):
    shape = jax.ShapeDtypeStruct
    return pl.pallas_call(
        first_kernel,
        out_shape=(shape((ALL_ROWS, D), BF16), shape((ALL_ROWS, 3 * D), BF16), shape((ROWS, D), BF16),
                   shape((TILES, 16, QT), F32)),
        in_specs=[SMEM, VMEM, VMEM, pl.BlockSpec((D, 3 * D), lambda step: (0, 0))],
        grid=(1,),
        out_specs=(VMEM,) * 4,
        compiler_params=pltpu.CompilerParams(vmem_limit_bytes=VMEM_LIMIT),
        name="attend",
    )(tab, x, gc, w)


def feed(tab, x, cot, att, gc, w, wb):
    hidden = wb.shape[0]
    shape = jax.ShapeDtypeStruct
    return pl.pallas_call(
        second_kernel,
        out_shape=(shape((ROWS, D), BF16), shape((ROWS, D), F32), shape((ROWS, D), BF16),
                   shape((D, hidden), BF16), shape((D, hidden), BF16), shape((hidden, D), BF16), shape((D, D), BF16),
                   shape((1, D), F32)),
        in_specs=[SMEM] + [VMEM] * 6,
        out_specs=(VMEM,) * 8,
        scratch_shapes=[pltpu.VMEM((ROWS, D), F32), pltpu.VMEM((ROWS, D), BF16), pltpu.VMEM((D, ROWS), BF16),
                        pltpu.VMEM((ROWS, D), BF16), pltpu.VMEM((ROWS, hidden), BF16),
                        pltpu.VMEM((ROWS, hidden), BF16), pltpu.VMEM((ROWS, hidden), BF16),
                        pltpu.VMEM((ROWS, D), F32)],
        compiler_params=pltpu.CompilerParams(vmem_limit_bytes=VMEM_LIMIT),
        name="feed_forward",
    )(tab, x, cot, att, gc, w, wb)


def backward_layer(tab, x, gh, ga, att, lse, n, qkv, gain, gc, w):
    shape = jax.ShapeDtypeStruct
    return pl.pallas_call(
        third_kernel,
        out_shape=(shape((ROWS, D), BF16), shape((D, 3 * D), BF16), shape((gc.shape[0], 8, 128), F32)),
        in_specs=[SMEM] + [VMEM] * 9 + [pl.BlockSpec((D, 3 * D), lambda step: (0, 0))],
        grid=(1,),
        out_specs=(VMEM,) * 3,
        scratch_shapes=[pltpu.VMEM((ALL_ROWS, 3 * D), BF16), pltpu.VMEM((ALL_ROWS, D), F32),
                        pltpu.VMEM((ALL_ROWS, D), F32), pltpu.VMEM((ALL_ROWS, D), F32)],
        compiler_params=pltpu.CompilerParams(vmem_limit_bytes=VMEM_LIMIT),
        name="attend_back",
    )(tab, x, gh, ga, att, lse, n, qkv, gain, gc, w)


class Links:
    def __init__(self, outer, inner):
        self.outer, self.inner = outer, inner
        self.rank, self.spot = lax.axis_index("rep"), lax.axis_index("fsdp")
        self.core = self.rank % 2
        self.row, self.col = self.spot // inner, self.spot % inner
        self.mate, self.across = core_of(self.rank), across_of(self.rank)
        self.late = []

    def greet(self, everyone=False):
        barrier = pltpu.get_barrier_semaphore()
        neighbours = (
            (self.row + 1 < self.outer, {"fsdp": self.spot + self.inner}),
            (self.row > 0, {"fsdp": self.spot - self.inner}),
            (self.col + 1 < self.inner, {"fsdp": self.spot + 1}),
            (self.col > 0, {"fsdp": self.spot - 1}),
        )
        group = (self.mate, self.across) + ((across_of(self.mate),) if everyone else ())
        amount = jnp.int32(len(group))
        for there, device in neighbours:
            amount = amount + there.astype(jnp.int32)

            @pl.when(there)
            def _():
                pl.semaphore_signal(barrier, inc=1, device_id=device, device_id_type=MESH)

        for device in group:
            pl.semaphore_signal(barrier, inc=1, device_id={"rep": device}, device_id_type=MESH)
        pl.semaphore_wait(barrier, amount)

    def send(self, there, src, dst, ssem, rsem, device):
        def describe():
            return pltpu.make_async_remote_copy(
                src_ref=src, dst_ref=dst, send_sem=ssem, recv_sem=rsem,
                device_id=device, device_id_type=MESH,
            )

        if there is None:
            describe().start()
        else:
            @pl.when(there)
            def _():
                describe().start()

        self.late.append((there, lambda: describe().wait_send()))

    def arrive(self, place, rsem, spare):
        pltpu.make_async_remote_copy(
            src_ref=place, dst_ref=place, send_sem=spare, recv_sem=rsem,
            device_id={"rep": self.mate}, device_id_type=MESH,
        ).wait_recv()

    def drain(self):
        for there, finish in self.late:
            if there is None:
                finish()
            else:
                pl.when(there)(finish)


def halves(ref, which):
    half = ref.shape[-1] // 2
    cols = pl.ds(pl.multiple_of(which * half, 128), half)
    return ref.at[:, :, :, cols] if len(ref.shape) == 4 else ref.at[:, cols]


class Reduction:
    def __init__(self, links, source, total, mine, crecv, yrecv, zrecv, xrecv, sems, number):
        self.links, self.source, self.total, self.mine = links, source, total, mine
        self.crecv, self.yrecv, self.zrecv, self.xrecv = crecv, yrecv, zrecv, xrecv
        self.sems, self.number = sems, number
        self.whole = total.shape[-1] % 256 != 0
        self.load = None

    def sem(self, name, *index):
        return self.sems[name].at[index + (self.number,)]

    def begin(self):
        links = self.links
        other = self.source if self.whole else halves(self.source, 1 - links.core)
        links.send(None, other, self.crecv, self.sem("c_send"), self.sem("c_recv"), {"rep": links.mate})
        if self.mine is None:
            self.mine = self.source if self.whole else halves(self.source, links.core)
        else:
            own = self.source if self.whole else halves(self.source, links.core)
            self.load = pltpu.make_async_copy(own, self.mine, self.sem("m_sem"))
            self.load.start()

    def pair(self):
        links = self.links
        if self.load is not None:
            self.load.wait()
        links.arrive(self.crecv, self.sem("c_recv"), self.sems["spare"].at[0])
        inner = links.inner

        def add(index, carry):
            row, col = index // inner, index % inner
            self.mine[row, col] = self.mine[row, col] + self.crecv[row, col]
            return carry

        lax.fori_loop(0, links.outer * inner, add, 0)
        links.send(None, self.mine.at[:, 1 - links.col], self.yrecv, self.sem("y_send"), self.sem("y_recv"),
                   {"fsdp": links.spot + 1 - 2 * links.col})

    def slot(self, way, place, dest):
        return dest - place if way == 0 else self.links.outer - place + dest

    def pass_on(self, way, dest, there, first):
        links = self.links
        step = 1 if way == 0 else -1
        mine = self.mine.at[dest, links.col]
        put = self.slot(way, links.row + step, dest)
        if not first:
            got = self.slot(way, links.row, dest)

            @pl.when(there)
            def _():
                links.arrive(self.zrecv.at[got], self.sem("z_recv", got), self.sems["spare"].at[0])
                mine[...] = mine[...] + self.zrecv[got]

        links.send(there, mine, self.zrecv.at[put], self.sem("z_send", way, dest), self.sem("z_recv", put),
                   {"fsdp": links.spot + step * links.inner})

    def column(self):
        links = self.links
        size = links.outer
        links.arrive(self.yrecv, self.sem("y_recv"), self.sems["spare"].at[0])

        def add(index, carry):
            self.mine[index, links.col] = self.mine[index, links.col] + self.yrecv[index]
            return carry

        lax.fori_loop(0, size, add, 0)
        for far in range(size - 1, 0, -1):
            self.pass_on(0, far, links.row == 0, True)
            self.pass_on(1, size - 1 - far, links.row == size - 1, True)

    def hop(self, turn):
        links = self.links
        size = links.outer
        for way in range(2):
            place = turn if way == 0 else size - 1 - turn
            here = links.row == place
            rest = range(size - 1, place, -1) if way == 0 else range(0, place)
            for dest in rest:
                self.pass_on(way, dest, here, False)
            mine = self.mine.at[place, links.col]
            got = self.slot(way, place, place)

            @pl.when(here)
            def _():
                links.arrive(self.zrecv.at[got], self.sem("z_recv", got), self.sems["spare"].at[0])
                mine[...] = mine[...] + self.zrecv[got]

    def cross(self):
        links = self.links
        mine = self.mine.at[links.row, links.col]
        links.send(None, mine, self.xrecv, self.sem("x_send"), self.sem("x_recv"), {"rep": links.across})

    def finish(self):
        links = self.links
        links.arrive(self.xrecv, self.sem("x_recv"), self.sems["spare"].at[0])
        value = self.mine[links.row, links.col].astype(F32) + self.xrecv[...].astype(F32)
        if self.whole:
            self.total[...] = value
            return
        place = halves(self.total, links.core)
        place[...] = value
        links.send(None, place, place, self.sem("f_send"), self.sem("f_recv"), {"rep": links.mate})

    def settle(self):
        if not self.whole:
            self.links.arrive(
                halves(self.total, 1 - self.links.core), self.sem("f_recv"), self.sems["spare"].at[0]
            )


SEM_NAMES = ("c_send", "c_recv", "m_sem", "y_send", "y_recv", "z_send", "z_recv", "x_send", "x_recv",
             "f_send", "f_recv", "r_send", "r_recv", "own", "spare")


class Return:
    def __init__(self, links, source, home, sems, kind):
        self.links, self.source, self.home, self.sems, self.kind = links, source, home, sems, kind

    def begin(self):
        links = self.links
        dst = self.home.at[links.rank]
        for way, device in enumerate((links.across, links.mate)):
            links.send(None, self.source, dst, self.sems["r_send"].at[self.kind, way],
                       self.sems["r_recv"].at[self.kind, way], {"rep": device})
        self.copy = pltpu.make_async_copy(self.source, dst, self.sems["own"].at[self.kind])
        self.copy.start()

    def relay(self):
        links = self.links
        place = self.home.at[links.across]
        links.arrive(place, self.sems["r_recv"].at[self.kind, 0], self.sems["spare"].at[0])
        links.send(None, place, place, self.sems["r_send"].at[self.kind, 2],
                   self.sems["r_recv"].at[self.kind, 2], {"rep": links.mate})

    def settle(self):
        links, sem = self.links, self.sems["r_recv"]
        links.arrive(self.home.at[links.mate], sem.at[self.kind, 1], self.sems["spare"].at[0])
        links.arrive(self.home.at[across_of(links.mate)], sem.at[self.kind, 2], self.sems["spare"].at[0])
        self.copy.wait()


def back_kernel(outer, inner, early, *refs):
    (tab_ref, x_ref, gh_ref, ga_ref, att_ref, lse_ref, n_ref, qkv_ref, gain_ref, gc_ref, w_ref), refs = refs[:11], refs[11:]
    grads, (y_ref,), refs = refs[:early], refs[early : early + 1], refs[early + 1 :]
    kinds = early + 4
    totals, (ry_ref, rg_ref), refs = refs[:kinds], refs[kinds : kinds + 2], refs[kinds + 2 :]
    (dq_ref, dkw_ref, dvw_ref, dc_ref), refs = refs[:4], refs[4:]
    (g_ref, dqkv_ref, dk_ref, dv_ref), refs = refs[:4], refs[4:]
    mines, refs = list(refs[:early]) + [None] * 3 + [refs[early]], refs[early + 1 :]
    crecv, yrecv, zrecv, xrecv = (refs[kinds * i : kinds * (i + 1)] for i in range(4))
    sems = dict(zip(SEM_NAMES, refs[4 * kinds :]))
    links = Links(outer, inner)
    rank = links.rank
    sources = list(grads) + [dq_ref, dkw_ref, dvw_ref, dc_ref]
    tasks = [
        Reduction(links, sources[i], totals[i], mines[i], crecv[i], yrecv[i], zrecv[i], xrecv[i], sems, i)
        for i in range(kinds)
    ]
    rows_y, rows_g = Return(links, y_ref, ry_ref, sems, 0), Return(links, g_ref, rg_ref, sems, 1)

    links.greet()
    for task in tasks[:early]:
        task.begin()
    rows_y.begin()
    gains = gains_of(gc_ref)
    for task in tasks[:early]:
        task.pair()
    backward_attention_start(dk_ref, dv_ref)
    backward_attention_tiles(tab_ref, rank, qkv_ref, att_ref, ga_ref, lse_ref, dqkv_ref, dk_ref, dv_ref, 0, TILES)
    tasks[0].column()
    backward_attention_end(dqkv_ref, dk_ref, dv_ref)
    weight_grads(n_ref, dqkv_ref, (dq_ref, dkw_ref, dvw_ref))
    for task in tasks[early : early + 3]:
        task.begin()
    rows_y.relay()
    one, side = backward_project(tab_ref, rank, x_ref, gh_ref, gains, n_ref, dqkv_ref, w_ref, dk_ref, g_ref)
    spread_gain_grads(jnp.concatenate([one, side, gain_ref[...], jnp.zeros((5, D), F32)], axis=0), dc_ref)
    rows_g.begin()
    tasks[kinds - 1].begin()
    for task in tasks[early:]:
        task.pair()
    for number in range(1, kinds + outer):
        if number < kinds:
            tasks[number].column()
        if number == 2:
            rows_g.relay()
        for turn in range(1, outer):
            if 0 <= number - turn < kinds:
                tasks[number - turn].hop(turn)
        if 0 <= number - outer + 1 < kinds:
            tasks[number - outer + 1].cross()
        if 0 <= number - outer < kinds:
            tasks[number - outer].finish()
    rows_y.settle()
    rows_g.settle()
    for task in tasks:
        task.settle()
    links.drain()


def attend_back(count, table, x, gh, ga, att, lse, n, qkv, gain, gc, w, grads, y):
    outer, inner = grid_of(count)
    part = D // count
    early = len(grads)
    kinds = early + 4
    grads = [grad.reshape((outer, inner, -1) + grad.shape[1:]) for grad in grads]
    shapes = [grad.shape[2:] for grad in grads] + [(part, D)] * 3 + [(8, 128)]
    dtypes = [BF16] * (kinds - 1) + [F32]
    halved = [(a, b // 2 if b % 256 == 0 else b) for a, b in shapes]
    dma = pltpu.SemaphoreType.DMA
    scratch = [pltpu.VMEM((outer, inner) + shape, dtype) for shape, dtype in zip(shapes[early:], dtypes[early:])]
    scratch += [pltpu.VMEM((SLOTS, BLK, D), BF16), pltpu.VMEM((ALL_ROWS, 3 * D), BF16),
                pltpu.VMEM((ALL_ROWS, D), F32), pltpu.VMEM((ALL_ROWS, D), F32)]
    scratch += [pltpu.VMEM((outer, inner) + shape, BF16) for shape in halved[:early]]
    scratch += [pltpu.VMEM((outer, inner) + halved[-1], F32)]
    for lead in ((outer, inner), (outer,), (outer + 1,), ()):
        scratch += [pltpu.VMEM(lead + shape, dtype) for shape, dtype in zip(halved, dtypes)]
    one = dma((kinds,))
    scratch += [one, one, one, one, one, dma((2, outer, kinds)), dma((outer + 1, kinds)), one, one, one, one,
                dma((2, 3)), dma((2, 3)), dma((2,)), dma((1,))]
    rows = jax.ShapeDtypeStruct((4, SLOTS, BLK, D), BF16)
    outs = pl.pallas_call(
        partial(back_kernel, outer, inner, early),
        out_shape=tuple(jax.ShapeDtypeStruct(shape, F32) for shape in shapes) + (rows, rows),
        grid=(1,),
        in_specs=[SMEM] + [VMEM] * 9 + [pl.BlockSpec((D, 3 * D), lambda step: (0, 0))] + [ANY] * early + [VMEM],
        out_specs=(VMEM,) * kinds + (ANY, ANY),
        scratch_shapes=scratch,
        compiler_params=pltpu.CompilerParams(
            collective_id=2, has_side_effects=True, vmem_limit_bytes=VMEM_LIMIT
        ),
        name="attend_back_and_reduce",
    )(table, x, gh, ga, att, lse, n, qkv, gain, gc, w, *grads, y.reshape(SLOTS, BLK, D))
    return outs[:kinds], outs[kinds], outs[kinds + 1]


TABLE_ROWS = 56


def packed_table(lens, tabv_ref):
    lane = iota((8, 128), 1)
    blocks = lax.div(lens + (BLK - 1), BLK)
    key = jnp.where(blocks > 0, blocks * 128 + (127 - lane), 0)
    wide = jnp.broadcast_to(key[:1], (128, 128))
    other = jnp.sum(jnp.where(iota((128, 128), 0) == iota((128, 128), 1), wide, 0), axis=1, keepdims=True)
    order = jnp.sum(jnp.where(other > wide, 1, 0), axis=0, keepdims=True)
    order = jnp.broadcast_to(order, (8, 128))
    edges, below = [], jnp.zeros((8, 1), jnp.int32)
    for size in range(MAX_SEQ_BLOCKS, 0, -1):
        below = below + jnp.sum(jnp.where(blocks == size, 1, 0), axis=1, keepdims=True)
        edges.append(jnp.broadcast_to(below, (8, 128)))

    def assign(number, carry):
        loads, slot, first = carry[:4], carry[4], carry[5]
        size = jnp.zeros((8, 128), jnp.int32)
        for step, edge in enumerate(edges):
            size = size + jnp.where(number < edge, 1, 0)
        low = jnp.minimum(jnp.minimum(loads[0], loads[1]), jnp.minimum(loads[2], loads[3]))
        best = jnp.full((8, 128), 3, jnp.int32)
        for dev in (2, 1, 0):
            best = jnp.where(loads[dev] == low, dev, best)
        mine = order == number
        slot = jnp.where(mine, best * SLOTS + low, slot)
        first = jnp.where(mine, low, first)
        loads = tuple(loads[dev] + jnp.where(best == dev, size, 0) for dev in range(4))
        return loads + (slot, first)

    zero = jnp.zeros((8, 128), jnp.int32)
    carry = lax.fori_loop(0, 32, assign, (zero,) * 6)
    slot, first = carry[4], carry[5]
    where, tokens, segment = zero - 1, zero, zero
    for step in range(MAX_SEQ_BLOCKS):
        def shifted(value):
            return value if step == 0 else pltpu.roll(value, step, 1)

        covers = shifted(blocks) > step
        where = jnp.where(covers, shifted(slot) + step, where)
        tokens = jnp.where(covers, jnp.minimum(shifted(lens) - BLK * step, BLK), tokens)
        segment = jnp.where(covers, shifted(first) + 1, segment)
    packed = jnp.where(where >= 0, (lane + 1) + 128 * tokens + 16384 * segment, 0)
    spots = jnp.broadcast_to(where[:1], (48, 128))
    values = jnp.broadcast_to(packed[:1], (48, 128))
    column = jnp.sum(jnp.where(spots == iota((48, 128), 0), values, 0), axis=1, keepdims=True)
    tabv_ref[:48] = jnp.broadcast_to(column, (48, 128))
    tabv_ref[48:] = where


def front_kernel(outer, inner, *refs):
    (lens_ref, rows_ref, cots_ref, *weights), refs = refs[:9], refs[9:]
    (wd_ref, wc_ref), refs = refs[:2], refs[2:]
    (tab_ref, x_ref, cot_ref, n_ref, qkv_ref, att_ref, lse_ref, wqkv_ref, gc_ref, ga_ref, gb_ref), refs = refs[:11], refs[11:]
    (stage, lens_all, tabs, psend, precv, xsend, xrecv), refs = refs[:7], refs[7:]
    (l_send, l_recv, t_sem, w_sem, z_send, z_recv, y_send, y_recv, c_send, c_recv, d_send, d_recv, own_sem,
     p_send, p_recv, x_send, x_recv, spare) = refs
    links = Links(outer, inner)
    rank, spot, core, mate, across = links.rank, links.spot, links.core, links.mate, links.across
    row, col = links.row, links.col
    side = rank // 2
    count = outer * inner
    part = stage.shape[0]
    per_rank = rows_ref.shape[0]
    width = 3 * D
    tall = wd_ref.shape[0]
    hidden = weights[-1].shape[1]
    gate_half, up_half = (D + hidden) // 2, hidden // 2

    at = 0
    loads = []
    for number, ref in enumerate(weights):
        cols = slice(at, at + ref.shape[1])
        loads.append(pltpu.make_async_copy(ref, stage.at[:, cols], w_sem.at[number]))
        loads[-1].start()
        at += ref.shape[1]

    links.greet(True)
    lens_all[rank] = lens_ref[...]
    for step in range(1, 4):
        links.send(None, lens_ref, lens_all.at[rank], l_send.at[step - 1], l_recv.at[step - 1],
                   {"rep": (rank + step) % 4})

    def cols_of(start, half, which):
        return pl.ds(pl.multiple_of(start + which * half, 128), half)

    down_half = D // 2

    def tall_rows(which):
        return pl.ds(pl.multiple_of(which * (tall // 2), 16), tall // 2)

    def source(number):
        return (
            lambda: stage.at[:, cols_of(0, width // 2, core)],
            lambda: stage.at[:, cols_of(width, gate_half, core)],
            lambda: stage.at[:, cols_of(width + 2 * gate_half, up_half, core)],
            lambda: wd_ref.at[tall_rows(side), cols_of(0, down_half, core)],
            lambda: wc_ref,
        )[number]()

    def place(number, shard, which=None):
        which = core if which is None else which
        return (
            lambda: wqkv_ref.at[pl.ds(pl.multiple_of(shard * part, 16), part), cols_of(0, width // 2, which)],
            lambda: ga_ref.at[shard, :, cols_of(0, gate_half, which)],
            lambda: ga_ref.at[shard, :, cols_of(2 * gate_half, up_half, which)],
            lambda: gb_ref.at[shard, tall_rows(side), cols_of(0, down_half, which)],
            lambda: gc_ref.at[shard],
            lambda: gb_ref.at[shard, tall_rows(1 - side), cols_of(0, down_half, which)],
        )[number]()

    nobody = spare.at[0]

    def both(first, second):
        return second if first is None else jnp.logical_and(first, second)

    def guarded(there, action):
        if there is None:
            action()
        else:
            pl.when(there)(action)

    def share(there, number, shard):
        if number == 4:
            return
        here = place(number, shard)
        links.send(there, here, here, c_send.at[number, shard], c_recv.at[number, shard], {"rep": mate})
        if number == 3:
            links.send(there, here, here, d_send.at[shard], d_recv.at[shard], {"rep": across})

    other_column = {"fsdp": spot + 1 - 2 * col}

    def along_row(there, number, line, src):
        here = place(number, line * inner + col)
        links.send(there, here if src is None else src, here, y_send.at[line, number], y_recv.at[line, number],
                   other_column)

    def lines(step):
        return ((row - 1 - step >= 0, row - 1 - step, 0, row + 1 < outer, spot + inner),
                (row + 1 + step < outer, row + 1 + step, 1, row > 0, spot - inner))

    def own(number):
        src, dst = source(number), place(number, spot)
        links.send(row + 1 < outer, src, dst, z_send.at[0, 0, number], z_recv.at[0, 0, number],
                   {"fsdp": spot + inner})
        links.send(row > 0, src, dst, z_send.at[1, 0, number], z_recv.at[1, 0, number], {"fsdp": spot - inner})
        along_row(None, number, row, src)

    def hop(number, step):
        for here, line, way, onward, target in lines(step):
            shard = line * inner + col
            guarded(here, lambda: links.arrive(place(number, shard), z_recv.at[way, step, number], nobody))
            if step + 1 < outer - 1:
                view = place(number, shard)
                links.send(both(here, onward), view, view, z_send.at[way, step + 1, number],
                           z_recv.at[way, step + 1, number], {"fsdp": target})
            along_row(here, number, line, None)
            share(here, number, shard)

    def from_row(number):
        def one(there, line):
            shard = line * inner + 1 - col
            guarded(there, lambda: links.arrive(place(number, shard), y_recv.at[line, number], nobody))
            share(there, number, shard)

        one(None, row)
        for step in range(outer - 1):
            for here, line, *_ in lines(step):
                one(here, line)

    def gathered(*numbers):
        for shard in range(count):
            @pl.when(shard != spot)
            def _():
                for number in numbers:
                    links.arrive(place(number, shard, 1 - core), c_recv.at[number, shard], nobody)

    def from_across():
        for shard in range(count):
            there = shard != spot
            guarded(there, lambda: links.arrive(place(5, shard), d_recv.at[shard], nobody))
            here = place(5, shard)
            links.send(there, here, here, c_send.at[5, shard], c_recv.at[5, shard], {"rep": mate})

    for load in loads:
        load.wait()
    own(0)
    own(4)
    own(1)
    keep = [
        pltpu.make_async_copy(stage.at[:, :width], wqkv_ref.at[pl.ds(pl.multiple_of(spot * part, 16), part)], own_sem.at[0]),
        pltpu.make_async_copy(stage.at[:, width:], ga_ref.at[spot], own_sem.at[1]),
        pltpu.make_async_copy(wd_ref, gb_ref.at[spot], own_sem.at[2]),
        pltpu.make_async_copy(wc_ref, gc_ref.at[spot], own_sem.at[3]),
    ]
    for copy in keep:
        copy.start()

    for step in range(1, 4):
        links.arrive(lens_all.at[(rank + 4 - step) % 4], l_recv.at[step - 1], nobody)
    lens = lens_all[0] + lens_all[1] + lens_all[2] + lens_all[3]
    packed_table(jnp.broadcast_to(lens[:1], (8, 128)), tab_ref)
    to_scalar = pltpu.make_async_copy(tab_ref, tabs, t_sem.at[0])
    to_scalar.start()
    to_scalar.wait()

    sources = (rows_ref, cots_ref)
    outs = (x_ref, cot_ref)

    def picked(kind, target, slot):
        index = block_at(tabs, target * SLOTS + slot) - rank * per_rank
        mine = jnp.logical_and(index >= 0, index < per_rank)
        return mine, sources[kind][jnp.clip(index, 0, per_rank - 1)]

    def mate_copy(kind, piece):
        return pltpu.make_async_remote_copy(
            src_ref=psend.at[kind, piece], dst_ref=precv.at[kind, piece],
            send_sem=p_send.at[kind, piece], recv_sem=p_recv.at[kind, piece],
            device_id={"rep": mate}, device_id_type=MESH,
        )

    def across_copy(kind):
        return pltpu.make_async_remote_copy(
            src_ref=xsend.at[kind], dst_ref=xrecv.at[kind],
            send_sem=x_send.at[kind], recv_sem=x_recv.at[kind],
            device_id={"rep": across}, device_id_type=MESH,
        )

    def pack_rows(kind, piece):
        target = mate if piece == 0 else across_of(mate)

        def pack(slot, carry):
            mine, value = picked(kind, target, slot)
            psend[kind, piece, slot] = jnp.where(mine, value, jnp.zeros_like(value))
            return carry

        lax.fori_loop(0, SLOTS, pack, 0)
        mate_copy(kind, piece).start()

    def cross_rows(kind):
        mate_copy(kind, 1).wait_recv()

        def merge(slot, carry):
            mine, value = picked(kind, across, slot)
            xsend[kind, slot] = jnp.where(mine, value, precv[kind, 1, slot])
            return carry

        lax.fori_loop(0, SLOTS, merge, 0)
        across_copy(kind).start()

    def finish_rows(kind):
        mate_copy(kind, 0).wait_recv()
        across_copy(kind).wait_recv()

        def finish(slot, carry):
            mine, value = picked(kind, rank, slot)
            rows = pl.ds(pl.multiple_of(slot * BLK, BLK), BLK)
            outs[kind][rows, :] = jnp.where(mine, value, precv[kind, 0, slot] + xrecv[kind, slot])
            return carry

        lax.fori_loop(0, SLOTS, finish, 0)

    pack_rows(0, 1)
    pack_rows(1, 1)
    cross_rows(0)
    pack_rows(0, 0)
    cross_rows(1)
    pack_rows(1, 0)
    for step in range(outer - 1):
        hop(0, step)
    for step in range(outer - 1):
        hop(4, step)
    hop(1, 0)
    own(2)
    from_row(0)
    from_row(4)
    for step in range(1, outer - 1):
        hop(1, step)
    keep[3].wait()
    gains = gains_of(gc_ref)
    finish_rows(0)
    forward_norm(tabs, rank, x_ref, gains, n_ref)
    hop(2, 0)
    own(3)
    keep[0].wait()
    gathered(0)
    forward_project(n_ref, wqkv_ref, qkv_ref)
    hop(2, 1)
    forward_attention(tabs, rank, qkv_ref, att_ref, lse_ref, 0, 2)
    from_row(1)
    for step in range(2, outer - 1):
        hop(2, step)
    hop(3, 0)
    forward_attention(tabs, rank, qkv_ref, att_ref, lse_ref, 2, 4)
    from_row(2)
    for step in range(1, outer - 1):
        hop(3, step)
    forward_attention(tabs, rank, qkv_ref, att_ref, lse_ref, 4, TILES)
    from_row(3)
    finish_rows(1)
    from_across()
    gathered(1, 2, 3, 5)
    links.drain()
    for kind in range(2):
        for piece in range(2):
            mate_copy(kind, piece).wait_send()
        across_copy(kind).wait_send()
    for copy in keep[1:3]:
        copy.wait()


def gather_and_attend(count, lens, rows, cots, weights, wd, wc):
    outer, inner = grid_of(count)
    block = rows.shape[1:]
    part, hidden = wd.shape[0], weights[-1].shape[1]
    part = weights[0].shape[0]
    dma, shape = pltpu.SemaphoreType.DMA, jax.ShapeDtypeStruct
    total = sum(weight.shape[1] for weight in weights)
    kinds = 5
    return pl.pallas_call(
        partial(front_kernel, outer, inner),
        out_shape=(
            shape((TABLE_ROWS, 128), jnp.int32), shape((ROWS, D), BF16), shape((ROWS, D), BF16),
            shape((ALL_ROWS, D), BF16), shape((ALL_ROWS, 3 * D), BF16), shape((ROWS, D), BF16),
            shape((TILES, 16, QT), F32), shape((D, 3 * D), BF16), shape((count,) + wc.shape, BF16),
            shape((count, part, total - 3 * D), BF16), shape((count,) + wd.shape, BF16),
        ),
        in_specs=[VMEM] * 3 + [ANY] * 6 + [VMEM] * 2,
        out_specs=(VMEM,) * 9 + (ANY,) * 2,
        scratch_shapes=[
            pltpu.VMEM((part, total), BF16), pltpu.VMEM((4, 8, 128), jnp.int32), pltpu.SMEM((TABLE_ROWS, 128), jnp.int32),
            pltpu.VMEM((2, 2, SLOTS) + block, BF16), pltpu.VMEM((2, 2, SLOTS) + block, BF16),
            pltpu.VMEM((2, SLOTS) + block, BF16), pltpu.VMEM((2, SLOTS) + block, BF16),
            dma((3,)), dma((3,)), dma((1,)), dma((6,)),
            dma((2, outer - 1, kinds)), dma((2, outer - 1, kinds)), dma((outer, kinds)), dma((outer, kinds)),
            dma((kinds + 1, count)), dma((kinds + 1, count)), dma((count,)), dma((count,)), dma((4,)),
            dma((2, 2)), dma((2, 2)), dma((2,)), dma((2,)), dma((1,)),
        ],
        compiler_params=pltpu.CompilerParams(
            collective_id=1, has_side_effects=True, vmem_limit_bytes=VMEM_LIMIT
        ),
        name="gather_and_attend",
    )(lens, rows, cots, *weights, wd, wc)


def per_device(count, layer_input, cotangent, lengths, attn_gain, global_gain, query_weight, key_weight,
               value_weight, out_weight, ffn_gain, gate_weight, up_weight, down_weight):
    micro, span, width = layer_input.shape
    hidden = gate_weight.shape[1]
    blocks = micro * span // BLK
    part = attn_gain.shape[0]
    rows_in = layer_input.reshape(blocks, BLK, width)
    cots_in = cotangent.reshape(blocks, BLK, width)
    weights = (query_weight, key_weight, value_weight, out_weight, gate_weight, up_weight)
    wc = jnp.pad(jnp.stack([attn_gain, global_gain, ffn_gain]), ((0, 13), (0, 128 - part)))
    if grid_of(count)[1] == 2 and part % 16 == 0:
        lens = lax.dynamic_update_slice(
            jnp.zeros((8, 128), jnp.int32), lengths.reshape(1, blocks), (0, lax.axis_index("rep") * blocks)
        )
        table, x, cot, n, qkv, att, lse, wqkv, gc, ga, gb = gather_and_attend(
            count, lens, rows_in, cots_in, weights, down_weight, wc
        )
        y, gh, gatt, dg, du, db, do, gain = feed(
            table, x, cot, att, gc, ga.reshape(width, -1), gb.reshape(-1, width)
        )
        totals, ry, rg = attend_back(count, table, x, gh, gatt, att, lse, n, qkv, gain, gc, wqkv, (dg, du, db, do), y)
        og, ou, ob, oo, oq, ok, ov, oc = totals
    else:
        table = deal_table(lengths)
        splits = ((0, 4 * width), (4 * width, 2 * hidden))
        ga, gb, gc, rows, cots = gather_weights(
            count, splits, table, rows_in, cots_in, jnp.concatenate(weights, axis=1), down_weight, wc
        )
        x, full = rows.reshape(ROWS, width), ga.reshape(width, -1)
        n, qkv, att, lse = attend(table, x, gc, full)
        y, gh, gatt, dg, du, db, do, gain = feed(
            table, x, cots.reshape(ROWS, width), att, gc, full, gb.reshape(-1, width)
        )
        g, dw, dc = backward_layer(table, x, gh, gatt, att, lse, n, qkv, gain, gc, full)
        grads = [grad.reshape(count, -1, grad.shape[-1]) for grad in (dg, du, db, do, dw, dc)]
        og, ou, ob, oo, ow, oc, ry, rg = reduce_grads(
            count, grads, y.reshape(SLOTS, BLK, width), g.reshape(SLOTS, BLK, width)
        )
        oq, ok, ov = ow[:, :width], ow[:, width : 2 * width], ow[:, 2 * width :]
    y_home, g_home = bring_home(table, ry, rg, blocks)
    return (
        y_home.reshape(layer_input.shape), g_home.reshape(layer_input.shape),
        oc[0, :part], oc[1, :part], oq, ok, ov, oo, oc[2, :part], og, ou, ob,
    )


def solution(mesh):
    rows = P(None, ("rep", "fsdp"), None)
    vector, matrix = P("fsdp"), P("fsdp", None)
    return jax.shard_map(
        partial(per_device, mesh.shape["fsdp"]),
        mesh=mesh,
        in_specs=(rows, rows, P(None, ("rep", "fsdp")), vector, vector, matrix, matrix, matrix, matrix,
                  vector, matrix, matrix, matrix),
        out_specs=(rows, rows, vector, vector, matrix, matrix, matrix, matrix, vector, matrix, matrix, matrix),
        check_vma=False,
    )
```

```python
from functools import partial

import jax
import jax.numpy as jnp
from jax import lax
from jax.experimental import pallas as pl
from jax.experimental.pallas import tpu as pltpu
from jax.sharding import PartitionSpec as P

H = 12
DH = 64
RADIUS = 127
GBLK = 16
BLK = 64
SLOTS = 10
MAX_SEQ_BLOCKS = 5
EPSILON = 1e-06
MASKED_SCORE = -1e30
MESH = pl.DeviceIdType.MESH
VMEM_LIMIT = 60 * 1024 * 1024
SEG_AT, LEN_AT, DEST_AT, TABLE_SIZE = 40, 80, 120, 256

ANY = pl.BlockSpec(memory_space=pl.ANY)
VMEM = pl.BlockSpec(memory_space=pltpu.VMEM)
SMEM = pl.BlockSpec(memory_space=pltpu.SMEM)


def grid_of(count):
    inner = 2 if count <= 8 else 4
    return count // inner, inner


def core_of(rank):
    return rank + 1 - 2 * (rank % 2)


def across_of(rank):
    return (rank + 2) % 4


def lens_kernel(lens_ref, all_ref, send_sem, recv_sem):
    rank = lax.axis_index("rep")
    barrier = pltpu.get_barrier_semaphore()
    for step in range(1, 4):
        pl.semaphore_signal(
            barrier, inc=1, device_id={"rep": (rank + step) % 4}, device_id_type=MESH
        )
    pl.semaphore_wait(barrier, 3)
    copies = []
    for step in range(1, 4):
        copy = pltpu.make_async_remote_copy(
            src_ref=lens_ref,
            dst_ref=all_ref.at[rank],
            send_sem=send_sem.at[step - 1],
            recv_sem=recv_sem.at[step - 1],
            device_id={"rep": (rank + step) % 4},
            device_id_type=MESH,
        )
        copy.start()
        copies.append(copy)
    all_ref[rank] = lens_ref[...]
    for copy in copies:
        copy.wait()


def table_kernel(micro, per_dev, lens_ref, tab_ref, order_ref, count_ref, load_ref):
    total = 4 * micro * per_dev

    def length_at(spot):
        return lens_ref[spot // (micro * per_dev), (spot // per_dev) % micro, spot % per_dev]

    def blocks_of(length):
        return (length + (BLK - 1)) // BLK

    def clear(spot, carry):
        tab_ref[spot] = -1
        return carry

    lax.fori_loop(0, TABLE_SIZE, clear, 0)
    for spot in range(4 * SLOTS):
        tab_ref[LEN_AT + spot] = 0
    for size in range(8):
        count_ref[size] = 0
    for dev in range(4):
        load_ref[dev] = 0

    def tally(spot, carry):
        length = length_at(spot)

        @pl.when(length > 0)
        def _():
            size = blocks_of(length)
            count_ref[size] = count_ref[size] + 1

        return carry

    lax.fori_loop(0, total, tally, 0)
    begin = 0
    for size in range(MAX_SEQ_BLOCKS, 0, -1):
        amount = count_ref[size]
        count_ref[size] = begin
        begin = begin + amount

    def place(spot, carry):
        length = length_at(spot)

        @pl.when(length > 0)
        def _():
            size = blocks_of(length)
            where = count_ref[size]
            order_ref[where] = spot
            count_ref[size] = where + 1

        return carry

    lax.fori_loop(0, total, place, 0)

    def assign(number, carry):
        spot = order_ref[number]
        length = length_at(spot)
        size = blocks_of(length)
        best = jnp.int32(0)
        low = load_ref[0]
        for dev in range(1, 4):
            here = load_ref[dev]
            best = jnp.where(here < low, dev, best)
            low = jnp.minimum(here, low)
        load_ref[best] = low + size

        def put(step, inner):
            slot = best * SLOTS + low + step
            tab_ref[slot] = spot + step
            tab_ref[SEG_AT + slot] = low
            tab_ref[LEN_AT + slot] = jnp.minimum(length - BLK * step, BLK)
            tab_ref[DEST_AT + spot + step] = slot
            return inner

        lax.fori_loop(0, size, put, 0)
        return carry

    lax.fori_loop(0, begin, assign, 0)


def deal_table(lengths):
    micro, per_dev = lengths.shape
    padded = jnp.pad(lengths, ((0, 8 - micro), (0, 128 - per_dev)))
    everyone = pl.pallas_call(
        lens_kernel,
        out_shape=jax.ShapeDtypeStruct((4, 8, 128), jnp.int32),
        in_specs=[VMEM],
        out_specs=VMEM,
        scratch_shapes=[pltpu.SemaphoreType.DMA((3,)), pltpu.SemaphoreType.DMA((3,))],
        compiler_params=pltpu.CompilerParams(collective_id=0, has_side_effects=True),
        name="lens_exchange",
    )(padded)
    return pl.pallas_call(
        partial(table_kernel, micro, per_dev),
        out_shape=jax.ShapeDtypeStruct((TABLE_SIZE,), jnp.int32),
        in_specs=[SMEM],
        out_specs=SMEM,
        scratch_shapes=[
            pltpu.SMEM((4 * micro * per_dev,), jnp.int32),
            pltpu.SMEM((8,), jnp.int32),
            pltpu.SMEM((4,), jnp.int32),
        ],
        name="deal_table",
    )(everyone)


def gather_kernel(
    outer, inner, splits, tab_ref, rows_ref, cots_ref, wa_ref, wb_ref, wc_ref,
    ga_ref, gb_ref, gc_ref, rows_out, cots_out,
    psend, precv, xsend, xrecv,
    z_send, z_recv, y_send, y_recv, c_send, c_recv, own_sem,
    p_send, p_recv, x_send, x_recv,
):
    rank = lax.axis_index("rep")
    spot = lax.axis_index("fsdp")
    core = rank % 2
    row, col = spot // inner, spot % inner
    count = outer * inner
    mate, across = core_of(rank), across_of(rank)
    pieces = [(wa_ref, ga_ref, start, width // 2) for start, width in splits]
    pieces.append((wb_ref, gb_ref, 0, wb_ref.shape[1] // 2))
    pieces.append((wc_ref, gc_ref, 0, None))
    halved = [number for number, piece in enumerate(pieces) if piece[3] is not None]

    barrier = pltpu.get_barrier_semaphore()
    neighbours = (
        (row + 1 < outer, {"fsdp": spot + inner}),
        (row > 0, {"fsdp": spot - inner}),
        (col + 1 < inner, {"fsdp": spot + 1}),
        (col > 0, {"fsdp": spot - 1}),
    )
    amount = jnp.int32(2)
    for there, device in neighbours:
        amount = amount + there.astype(jnp.int32)

        @pl.when(there)
        def _():
            pl.semaphore_signal(barrier, inc=1, device_id=device, device_id_type=MESH)

    for device in (mate, across):
        pl.semaphore_signal(barrier, inc=1, device_id={"rep": device}, device_id_type=MESH)
    pl.semaphore_wait(barrier, amount)

    def cut(ref, number):
        _, _, start, half = pieces[number]
        if half is None:
            return ref
        return ref.at[:, pl.ds(pl.multiple_of(start + core * half, 128), half)]

    def landed(number, shard):
        return cut(pieces[number][1].at[shard], number)

    late = []

    def send(there, src, dst, ssem, rsem, device):
        def describe():
            return pltpu.make_async_remote_copy(
                src_ref=src, dst_ref=dst, send_sem=ssem, recv_sem=rsem,
                device_id=device, device_id_type=MESH,
            )

        if there is None:
            describe().start()
            late.append((None, lambda: describe().wait_send()))
        else:
            @pl.when(there)
            def _():
                describe().start()

            late.append((there, lambda: describe().wait_send()))

    def arrive(number, shard, rsem):
        pltpu.make_async_remote_copy(
            src_ref=landed(number, shard), dst_ref=landed(number, shard),
            send_sem=own_sem.at[0], recv_sem=rsem,
            device_id={"rep": mate}, device_id_type=MESH,
        ).wait_recv()

    def both(first, second):
        return second if first is None else jnp.logical_and(first, second)

    def to_mate(there, number, shard):
        if number not in halved:
            return
        place = landed(number, shard)
        send(there, place, place, c_send.at[number, shard], c_recv.at[number, shard], {"rep": mate})

    def along_row(there, number, line, src):
        shard = line * inner + col
        place = landed(number, shard)
        src = place if src is None else src
        send(both(there, col + 1 < inner), src, place,
             y_send.at[0, 0, line, number], y_recv.at[0, 0, line, number], {"fsdp": spot + 1})
        send(both(there, col > 0), src, place,
             y_send.at[1, 0, line, number], y_recv.at[1, 0, line, number], {"fsdp": spot - 1})

    def from_row(there, number, line):
        for step in range(inner - 1):
            for way, source, onward, target in (
                (0, col - 1 - step, col + 1 < inner, spot + 1),
                (1, col + 1 + step, col > 0, spot - 1),
            ):
                here = jnp.logical_and(source >= 0, source < inner)
                here = both(there, here)
                shard = line * inner + source

                @pl.when(here)
                def _():
                    arrive(number, shard, y_recv.at[way, step, line, number])

                if step + 1 < inner - 1:
                    place = landed(number, shard)
                    send(both(here, onward), place, place,
                         y_send.at[way, step + 1, line, number],
                         y_recv.at[way, step + 1, line, number], {"fsdp": target})
                to_mate(here, number, shard)

    for number, piece in enumerate(pieces):
        src, place = cut(piece[0], number), landed(number, spot)
        send(row + 1 < outer, src, place, z_send.at[0, 0, number], z_recv.at[0, 0, number],
             {"fsdp": spot + inner})
        send(row > 0, src, place, z_send.at[1, 0, number], z_recv.at[1, 0, number],
             {"fsdp": spot - inner})
        along_row(None, number, row, src)
    own = [
        pltpu.make_async_copy(wa_ref, ga_ref.at[spot], own_sem.at[0]),
        pltpu.make_async_copy(wb_ref, gb_ref.at[spot], own_sem.at[1]),
        pltpu.make_async_copy(wc_ref, gc_ref.at[spot], own_sem.at[2]),
    ]
    for copy in own:
        copy.start()

    sources = (rows_ref, cots_ref)
    per_rank = rows_ref.shape[0]

    def picked(kind, target, slot):
        index = tab_ref[target * SLOTS + slot] - rank * per_rank
        mine = jnp.logical_and(index >= 0, index < per_rank)
        value = sources[kind][jnp.clip(index, 0, per_rank - 1)]
        return mine, value

    def mate_copy(kind, part):
        return pltpu.make_async_remote_copy(
            src_ref=psend.at[kind, part], dst_ref=precv.at[kind, part],
            send_sem=p_send.at[kind, part], recv_sem=p_recv.at[kind, part],
            device_id={"rep": mate}, device_id_type=MESH,
        )

    def across_copy(kind):
        return pltpu.make_async_remote_copy(
            src_ref=xsend.at[kind], dst_ref=xrecv.at[kind],
            send_sem=x_send.at[kind], recv_sem=x_recv.at[kind],
            device_id={"rep": across}, device_id_type=MESH,
        )

    for kind, part in ((0, 1), (1, 1), (0, 0), (1, 0)):
        target = mate if part == 0 else across_of(mate)

        def pack(slot, carry):
            mine, value = picked(kind, target, slot)
            psend[kind, part, slot] = jnp.where(mine, value, jnp.zeros_like(value))
            return carry

        lax.fori_loop(0, SLOTS, pack, 0)
        mate_copy(kind, part).start()
    for kind in range(2):
        mate_copy(kind, 1).wait_recv()

        def merge(slot, carry):
            mine, value = picked(kind, across, slot)
            xsend[kind, slot] = jnp.where(mine, value, precv[kind, 1, slot])
            return carry

        lax.fori_loop(0, SLOTS, merge, 0)
        across_copy(kind).start()

    def lines(step):
        return ((row - 1 - step >= 0, row - 1 - step, 0, row + 1 < outer, spot + inner),
                (row + 1 + step < outer, row + 1 + step, 1, row > 0, spot - inner))

    for step in range(outer - 1):
        for number in range(len(pieces)):
            for here, line, way, onward, target in lines(step):
                shard = line * inner + col

                @pl.when(here)
                def _():
                    arrive(number, shard, z_recv.at[way, step, number])

                if step + 1 < outer - 1:
                    place = landed(number, shard)
                    send(jnp.logical_and(here, onward), place, place,
                         z_send.at[way, step + 1, number], z_recv.at[way, step + 1, number],
                         {"fsdp": target})
                along_row(here, number, line, None)
                to_mate(here, number, shard)
        for number in range(len(pieces)):
            if step == 0:
                from_row(None, number, row)
            else:
                for here, line, *_ in lines(step - 1):
                    from_row(here, number, line)
    for number in range(len(pieces)):
        for here, line, *_ in lines(outer - 2):
            from_row(here, number, line)

    outs = (rows_out, cots_out)
    for kind in range(2):
        mate_copy(kind, 0).wait_recv()
        across_copy(kind).wait_recv()

        def finish(slot, carry):
            mine, value = picked(kind, rank, slot)
            outs[kind][slot] = jnp.where(mine, value, precv[kind, 0, slot] + xrecv[kind, slot])
            return carry

        lax.fori_loop(0, SLOTS, finish, 0)

    for shard in range(count):
        @pl.when(shard != spot)
        def _():
            for number in halved:
                other = pieces[number]
                view = other[1].at[shard].at[:, pl.ds(0, other[3])]
                pltpu.make_async_remote_copy(
                    src_ref=view, dst_ref=view, send_sem=own_sem.at[0],
                    recv_sem=c_recv.at[number, shard],
                    device_id={"rep": mate}, device_id_type=MESH,
                ).wait_recv()
    for there, finish_send in late:
        if there is None:
            finish_send()
        else:
            pl.when(there)(finish_send)
    for kind in range(2):
        for part in range(2):
            mate_copy(kind, part).wait_send()
        across_copy(kind).wait_send()
    for copy in own:
        copy.wait()


def gather_weights(count, splits, table, rows, cots, wa, wb, wc):
    outer, inner = grid_of(count)
    block = rows.shape[1:]
    kinds = len(splits) + 2
    dma = pltpu.SemaphoreType.DMA
    bf16 = jnp.bfloat16
    return pl.pallas_call(
        partial(gather_kernel, outer, inner, splits),
        out_shape=(
            jax.ShapeDtypeStruct((count,) + wa.shape, bf16),
            jax.ShapeDtypeStruct((count,) + wb.shape, bf16),
            jax.ShapeDtypeStruct((count,) + wc.shape, bf16),
            jax.ShapeDtypeStruct((SLOTS,) + block, bf16),
            jax.ShapeDtypeStruct((SLOTS,) + block, bf16),
        ),
        in_specs=[SMEM, VMEM, VMEM, VMEM, VMEM, VMEM],
        out_specs=(ANY, ANY, ANY, VMEM, VMEM),
        scratch_shapes=[
            pltpu.VMEM((2, 2, SLOTS) + block, bf16),
            pltpu.VMEM((2, 2, SLOTS) + block, bf16),
            pltpu.VMEM((2, SLOTS) + block, bf16),
            pltpu.VMEM((2, SLOTS) + block, bf16),
            dma((2, outer - 1, kinds)), dma((2, outer - 1, kinds)),
            dma((2, inner - 1, outer, kinds)), dma((2, inner - 1, outer, kinds)),
            dma((kinds, count)), dma((kinds, count)), dma((3,)),
            dma((2, 2)), dma((2, 2)), dma((2,)), dma((2,)),
        ],
        compiler_params=pltpu.CompilerParams(
            collective_id=1, has_side_effects=True, vmem_limit_bytes=VMEM_LIMIT
        ),
        name="gather_and_deal",
    )(table, rows, cots, wa, wb, wc)


def reduce_kernel(
    outer, inner, kinds, *refs
):
    grads, (y_ref, g_ref) = refs[:kinds], refs[kinds : kinds + 2]
    totals, (ry_ref, rg_ref) = refs[kinds + 2 : 2 * kinds + 2], refs[2 * kinds + 2 : 2 * kinds + 4]
    scratch = refs[2 * kinds + 4 :]
    mines, crecvs, yrecvs, zrecvs, xrecvs = (
        scratch[kinds * i : kinds * (i + 1)] for i in range(5)
    )
    (c_send, c_recv, m_sem, y_send, y_recv, z_send, z_recv, x_send, x_recv, f_send, f_recv,
     r_send, r_recv, q_sem) = scratch[5 * kinds :]
    rank = lax.axis_index("rep")
    spot = lax.axis_index("fsdp")
    core = rank % 2
    row, col = spot // inner, spot % inner
    mate, across = core_of(rank), across_of(rank)
    pieces = [(src, dst, 0, src.shape[3] // 2) for src, dst in zip(grads[:-1], totals)]
    pieces.append((grads[-1], totals[-1], 0, None))

    barrier = pltpu.get_barrier_semaphore()
    neighbours = (
        (row + 1 < outer, {"fsdp": spot + inner}),
        (row > 0, {"fsdp": spot - inner}),
        (col + 1 < inner, {"fsdp": spot + 1}),
        (col > 0, {"fsdp": spot - 1}),
    )
    amount = jnp.int32(2)
    for there, device in neighbours:
        amount = amount + there.astype(jnp.int32)

        @pl.when(there)
        def _():
            pl.semaphore_signal(barrier, inc=1, device_id=device, device_id_type=MESH)

    for device in (mate, across):
        pl.semaphore_signal(barrier, inc=1, device_id={"rep": device}, device_id_type=MESH)
    pl.semaphore_wait(barrier, amount)

    late = []

    def send(there, src, dst, ssem, rsem, device):
        def describe():
            return pltpu.make_async_remote_copy(
                src_ref=src, dst_ref=dst, send_sem=ssem, recv_sem=rsem,
                device_id=device, device_id_type=MESH,
            )

        if there is None:
            describe().start()
            late.append((None, lambda: describe().wait_send()))
        else:
            @pl.when(there)
            def _():
                describe().start()

            late.append((there, lambda: describe().wait_send()))

    def arrive(place, rsem):
        pltpu.make_async_remote_copy(
            src_ref=place, dst_ref=place, send_sem=q_sem.at[0], recv_sem=rsem,
            device_id={"rep": mate}, device_id_type=MESH,
        ).wait_recv()

    def columns(ref, number, which):
        _, _, start, half = pieces[number]
        if half is None:
            return ref
        cols = pl.ds(pl.multiple_of(start + which * half, 128), half)
        return ref.at[:, :, :, cols] if len(ref.shape) == 4 else ref.at[:, cols]

    order = list(range(kinds))
    loads = []
    for number in order:
        src = columns(pieces[number][0], number, 1 - core)
        send(None, src, crecvs[number], c_send.at[number], c_recv.at[number], {"rep": mate})
        load = pltpu.make_async_copy(
            columns(pieces[number][0], number, core), mines[number], m_sem.at[number]
        )
        load.start()
        loads.append(load)

    for kind, (src, dst) in enumerate(((y_ref, ry_ref), (g_ref, rg_ref))):
        send(None, src, dst.at[rank], r_send.at[kind, 0], r_recv.at[kind, 0], {"rep": across})
        send(None, src, dst.at[rank], r_send.at[kind, 1], r_recv.at[kind, 1], {"rep": mate})
        pltpu.make_async_copy(src, dst.at[rank], q_sem.at[kind + 1]).start()

    def slot_of(way, size, place, dest):
        if size == 2:
            return 0
        return dest - place if way == 0 else size - place + dest

    def line_sum(number, size, place, stride, buffer, view, ssem, rsem):
        for far in range(size - 1, 0, -1):
            for way in range(2):
                dest = far if way == 0 else size - 1 - far
                step = 1 if way == 0 else -1
                passes = place < dest if way == 0 else place > dest
                first = place == 0 if way == 0 else place == size - 1
                mine = view(dest)
                got = slot_of(way, size, place, dest)

                @pl.when(jnp.logical_and(passes, jnp.logical_not(first)))
                def _():
                    arrive(buffer.at[got], rsem.at[got, number])
                    mine[...] = mine[...] + buffer[got]

                put = slot_of(way, size, place + step, dest)
                send(passes, mine, buffer.at[put], ssem.at[way, dest, number], rsem.at[put, number],
                     {"fsdp": spot + step * stride})
        for way in range(2):
            has = place > 0 if way == 0 else place < size - 1
            got = slot_of(way, size, place, place)
            mine = view(place)

            @pl.when(has)
            def _():
                arrive(buffer.at[got], rsem.at[got, number])
                mine[...] = mine[...] + buffer[got]

    for number in order:
        loads[number].wait()
        arrive(crecvs[number], c_recv.at[number])
        mine, other = mines[number], crecvs[number]

        def add(index, carry):
            mine[index // inner, index % inner] = (
                mine[index // inner, index % inner] + other[index // inner, index % inner]
            )
            return carry

        lax.fori_loop(0, outer * inner, add, 0)
        if inner == 2:
            send(None, mine.at[:, 1 - col], yrecvs[number].at[0], y_send.at[0, 0, number],
                 y_recv.at[0, number], {"fsdp": spot + 1 - 2 * col})
    for kind, dst in enumerate((ry_ref, rg_ref)):
        place = dst.at[across]
        arrive(place, r_recv.at[kind, 0])
        send(None, place, place, r_send.at[kind, 2], r_recv.at[kind, 2], {"rep": mate})
    for number in order:
        mine = mines[number]
        if inner == 2:
            arrive(yrecvs[number].at[0], y_recv.at[0, number])
            buffer = yrecvs[number]

            def add(index, carry):
                mine[index, col] = mine[index, col] + buffer[0, index]
                return carry

            lax.fori_loop(0, outer, add, 0)
        else:
            line_sum(number, inner, col, 1, yrecvs[number], lambda dest: mine.at[:, dest],
                     y_send, y_recv)
        line_sum(number, outer, row, inner, zrecvs[number], lambda dest: mine.at[dest, col],
                 z_send, z_recv)
        send(None, mine.at[row, col], xrecvs[number], x_send.at[number], x_recv.at[number],
             {"rep": across})
    for number in order:
        arrive(xrecvs[number], x_recv.at[number])
        total = mines[number][row, col].astype(jnp.float32) + xrecvs[number][...].astype(jnp.float32)
        out, half = pieces[number][1], pieces[number][3]
        place = columns(out, number, core)
        place[...] = total
        if half is not None:
            send(None, place, place, f_send.at[number], f_recv.at[number], {"rep": mate})
    for number in order:
        if pieces[number][3] is not None:
            arrive(columns(pieces[number][1], number, 1 - core), f_recv.at[number])
    for kind, dst in enumerate((ry_ref, rg_ref)):
        arrive(dst.at[mate], r_recv.at[kind, 1])
        arrive(dst.at[across_of(mate)], r_recv.at[kind, 2])
        src = y_ref if kind == 0 else g_ref
        pltpu.make_async_copy(src, dst.at[rank], q_sem.at[kind + 1]).wait()
    for there, finish_send in late:
        if there is None:
            finish_send()
        else:
            pl.when(there)(finish_send)


def reduce_grads(count, grads, y_rows, g_rows):
    outer, inner = grid_of(count)
    kinds = len(grads)
    shapes = [(grad.shape[1], grad.shape[2] // 2, grad.dtype) for grad in grads[:-1]]
    shapes.append(grads[-1].shape[1:] + (grads[-1].dtype,))
    dma = pltpu.SemaphoreType.DMA
    y_slots = 1 if inner == 2 else inner + 1
    z_slots = 1 if outer == 2 else outer + 1
    scratch = []
    for lead in ((outer, inner), (outer, inner), (y_slots, outer), (z_slots,), ()):
        scratch += [pltpu.VMEM(lead + (a, b), dtype) for a, b, dtype in shapes]
    scratch += [
        dma((kinds,)), dma((kinds,)), dma((kinds,)),
        dma((2, inner, kinds)), dma((y_slots, kinds)),
        dma((2, outer, kinds)), dma((z_slots, kinds)),
        dma((kinds,)), dma((kinds,)), dma((kinds,)), dma((kinds,)),
        dma((2, 3)), dma((2, 3)), dma((3,)),
    ]
    return pl.pallas_call(
        partial(reduce_kernel, outer, inner, kinds),
        out_shape=tuple(jax.ShapeDtypeStruct(grad.shape[1:], jnp.float32) for grad in grads) + (
            jax.ShapeDtypeStruct((4,) + y_rows.shape, y_rows.dtype),
            jax.ShapeDtypeStruct((4,) + g_rows.shape, g_rows.dtype),
        ),
        in_specs=[ANY] * (kinds + 2),
        out_specs=(VMEM,) * kinds + (ANY, ANY),
        scratch_shapes=scratch,
        compiler_params=pltpu.CompilerParams(
            collective_id=2, has_side_effects=True, vmem_limit_bytes=VMEM_LIMIT
        ),
        name="reduce_and_return",
    )(*(grad.reshape((outer, inner) + grad.shape[1:]) for grad in grads), y_rows, g_rows)


def home_kernel(tab_ref, ry_ref, rg_ref, y_ref, g_ref):
    base = lax.axis_index("rep") * y_ref.shape[0]

    def fetch(block, carry):
        index = tab_ref[DEST_AT + base + block] if len(tab_ref.shape) == 1 else tab_ref[48, base + block]
        safe = jnp.maximum(index, 0)
        for src, dst in ((ry_ref, y_ref), (rg_ref, g_ref)):
            value = src[safe // SLOTS, safe % SLOTS]
            dst[block] = jnp.where(index >= 0, value, jnp.zeros_like(value))
        return carry

    lax.fori_loop(0, y_ref.shape[0], fetch, 0)


def bring_home(table, ry, rg, blocks):
    shape = jax.ShapeDtypeStruct((blocks,) + ry.shape[2:], ry.dtype)
    return pl.pallas_call(
        home_kernel,
        out_shape=(shape, shape),
        in_specs=[SMEM, VMEM, VMEM],
        out_specs=(VMEM, VMEM),
        compiler_params=pltpu.CompilerParams(vmem_limit_bytes=VMEM_LIMIT),
        name="place_rows",
    )(table, ry, rg)


D = H * DH
ROWS = SLOTS * BLK
SIDES = SLOTS * (BLK // GBLK)
SIDE_ROWS = 48
ALL_ROWS = ROWS + SIDE_ROWS
QT = 128
WIN = 384
TILES = ROWS // QT
QUAD = 256
FF_TILE = 256
GELU_C = 0.7978845608028654
GELU_A = 0.044715
F32, BF16 = jnp.float32, jnp.bfloat16


def mm(left, right):
    return lax.dot_general(left, right, (((1,), (0,)), ((), ())), preferred_element_type=F32)


def mm_cols(left, right):
    return lax.dot_general(left, right, (((1,), (1,)), ((), ())), preferred_element_type=F32)


def mm_rows(left, right):
    return lax.dot_general(left, right, (((0,), (0,)), ((), ())), preferred_element_type=F32)


def iota(shape, axis):
    return lax.broadcasted_iota(jnp.int32, shape, axis)


def pick_by(index, values, other):
    out = jnp.full(index.shape, other, jnp.int32)
    for number, value in enumerate(values):
        out = jnp.where(index == number, value, out)
    return out


def block_at(tab_ref, slot):
    return lax.rem(tab_ref[slot, 0], 128) - 1


def seg_at(tab_ref, slot):
    if len(tab_ref.shape) == 1:
        return tab_ref[SEG_AT + slot]
    return lax.div(tab_ref[slot, 0], 16384) - 1


def len_at(tab_ref, slot):
    if len(tab_ref.shape) == 1:
        return tab_ref[LEN_AT + slot]
    return lax.rem(lax.div(tab_ref[slot, 0], 128), 128)


def slot_info(tab_ref, rank):
    seg = [seg_at(tab_ref, rank * SLOTS + slot) for slot in range(SLOTS)]
    length = [len_at(tab_ref, rank * SLOTS + slot) for slot in range(SLOTS)]
    return seg, length


def valid_column(tab_ref, rank):
    _, length = slot_info(tab_ref, rank)
    row = iota((ROWS, 1), 0)
    return ((row % BLK) < pick_by(row // BLK, length, 0)).astype(F32)


def pooling(tab_ref, rank):
    _, length = slot_info(tab_ref, rank)
    row = iota((1, ROWS), 1)
    block = jnp.where((row % BLK) < pick_by(row // BLK, length, 0), row // GBLK, -1)
    return jnp.where(iota((SIDE_ROWS, ROWS), 0) == block, 1.0, 0.0).astype(BF16)


def key_segments(tab_ref, rank, first_block, index):
    blocks = WIN // BLK
    base = rank * SLOTS + first_block
    seg = [seg_at(tab_ref, base + step) for step in range(blocks)]
    length = [len_at(tab_ref, base + step) for step in range(blocks)]
    alive = (index % BLK) < pick_by(index // BLK, length, 0)
    return jnp.where(alive, pick_by(index // BLK, seg, -2), -2)


def side_segments(tab_ref, rank, index):
    seg, length = slot_info(tab_ref, rank)
    per = BLK // GBLK
    alive = (index % per) * GBLK < pick_by(index // per, length, 0)
    return jnp.where(alive, pick_by(index // per, seg, -2), -2)


def tile_bias(tab_ref, rank, tile, first_row, keys_axis):
    qs, ks, gs = ((QT, 1), (1, WIN), (1, SIDE_ROWS)) if keys_axis == 1 else ((1, QT), (WIN, 1), (SIDE_ROWS, 1))
    q_index = iota(qs, 1 - keys_axis)
    k_index = iota(ks, keys_axis)
    g_index = iota(gs, keys_axis)
    base = rank * SLOTS + tile * (QT // BLK)
    q_seg = pick_by(q_index // BLK, [seg_at(tab_ref, base + step) for step in range(QT // BLK)], -1)
    k_seg = key_segments(tab_ref, rank, first_row // BLK, k_index)
    g_seg = side_segments(tab_ref, rank, g_index)
    gap = (q_index + tile * QT) - (k_index + first_row)
    local = (jnp.abs(gap) <= RADIUS) & (q_seg == k_seg)
    return jnp.where(local, 0.0, MASKED_SCORE), jnp.where(q_seg == g_seg, 0.0, MASKED_SCORE)


def window_start(tile):
    return pl.multiple_of(jnp.clip(tile - 1, 0, TILES - WIN // QT) * QT, QT)


def head_stack(rows):
    lane = iota(rows.shape, 1) // DH
    zero = jnp.zeros_like(rows)
    return jnp.concatenate([jnp.where(lane == head, rows, zero) for head in range(QUAD // DH)], axis=0)


def head_merge(stacked):
    lane = iota((QT, QUAD), 1) // DH
    out = stacked[:QT]
    for head in range(1, QUAD // DH):
        out = jnp.where(lane == head, stacked[head * QT : (head + 1) * QT], out)
    return out


def gains_of(gc_ref):
    count = gc_ref.shape[0]
    part = D // count
    lane, column = iota((128, D), 0), iota((128, D), 1)
    total = None
    for shard in range(count):
        pick = jnp.where((column == lane + shard * part) & (lane < part), 1.0, 0.0).astype(BF16)
        term = mm(gc_ref[shard], pick)
        total = term if total is None else total + term
    return total


def three_way(value):
    high = value.astype(BF16)
    rest = value - high.astype(F32)
    middle = rest.astype(BF16)
    return high, middle, (rest - middle.astype(F32)).astype(BF16)


def spread_gain_grads(value, dc_ref):
    count = dc_ref.shape[0] if len(dc_ref.shape) == 3 else dc_ref.shape[0] * dc_ref.shape[1]
    part = D // count
    column, lane = iota((D, 128), 0), iota((D, 128), 1)
    parts = three_way(value)
    for shard in range(count):
        pick = jnp.where((column == lane + shard * part) & (lane < part), 1.0, 0.0).astype(BF16)
        place = dc_ref.at[shard] if len(dc_ref.shape) == 3 else dc_ref.at[shard // dc_ref.shape[1], shard % dc_ref.shape[1]]
        place[...] = mm(parts[0], pick) + mm(parts[1], pick) + mm(parts[2], pick)


def mean_square(value):
    return jnp.mean(value * value, axis=-1, keepdims=True)


def forward_norm(tab_ref, rank, x_ref, gains, n_ref):
    for tile in range(TILES):
        rows = pl.ds(tile * QT, QT)
        value = x_ref[rows, :].astype(F32)
        n_ref[rows, :] = (value * lax.rsqrt(mean_square(value) + EPSILON) * gains[0:1]).astype(BF16)
    side = mm(pooling(tab_ref, rank), n_ref[:ROWS, :])
    n_ref[ROWS:, :] = (side * lax.rsqrt(mean_square(side) + EPSILON) * gains[1:2]).astype(BF16)


def forward_project(n_ref, w_ref, qkv_ref):
    def step(tile, carry):
        cols = pl.ds(pl.multiple_of(tile * QUAD, QUAD), QUAD)
        qkv_ref[:, cols] = mm(n_ref[...], w_ref[:, cols]).astype(BF16)
        return carry

    lax.fori_loop(0, 3 * D // QUAD, step, 0)


def forward_attention(tab_ref, rank, qkv_ref, att_ref, lse_ref, begin, end):
    def step(tile, carry):
        first = window_start(tile)
        bias, side_bias = tile_bias(tab_ref, rank, tile, first, 1)
        rows = pl.ds(pl.multiple_of(tile * QT, QT), QT)
        window = pl.ds(first, WIN)
        lse = jnp.zeros((QT, 128), F32)
        lane = iota((QT, 128), 1)
        for quad in range(D // QUAD):
            low = quad * QUAD
            query = head_stack(qkv_ref[rows, low : low + QUAD])
            scores = mm_cols(query, qkv_ref[window, D + low : D + low + QUAD])
            side_scores = mm_cols(query, qkv_ref[ROWS:, D + low : D + low + QUAD])
            local, sides, scale = [], [], []
            for head in range(QUAD // DH):
                part = slice(head * QT, (head + 1) * QT)
                one = scores[part] + bias
                two = side_scores[part] + side_bias
                peak = jnp.maximum(
                    jnp.max(one, axis=-1, keepdims=True), jnp.max(two, axis=-1, keepdims=True)
                )
                one, two = jnp.exp(one - peak), jnp.exp(two - peak)
                total = jnp.sum(one, axis=-1, keepdims=True) + jnp.sum(two, axis=-1, keepdims=True)
                local.append(one.astype(BF16))
                sides.append(two.astype(BF16))
                scale.append(1.0 / total)
                lse = jnp.where(lane == quad * (QUAD // DH) + head, peak + jnp.log(total), lse)
            mixed = mm(jnp.concatenate(local, axis=0), qkv_ref[window, 2 * D + low : 2 * D + low + QUAD])
            mixed = mixed + mm(
                jnp.concatenate(sides, axis=0), qkv_ref[ROWS:, 2 * D + low : 2 * D + low + QUAD]
            )
            mixed = mixed * jnp.concatenate(scale, axis=0)
            att_ref[rows, low : low + QUAD] = head_merge(mixed).astype(BF16)
        lse_ref[tile] = jnp.transpose(lse)[:16]
        return carry

    lax.fori_loop(begin, end, step, 0)


def feed_forward(tab_ref, rank, x_ref, cot_ref, att_ref, gains, w_ref, wb_ref,
                 y_ref, gh_ref, ga_ref, dg_ref, du_ref, db_ref, do_ref,
                 h1_ref, nt_ref, ntt_ref, gres_ref, h2_ref, gg_ref, gu_ref, gn_ref):
    hidden = wb_ref.shape[0]
    gate_at = w_ref.shape[1] - 2 * hidden
    out_at = gate_at - D
    valid = valid_column(tab_ref, rank)
    gain = gains[2:3]
    for tile in range(TILES):
        rows = pl.ds(tile * QT, QT)
        value = x_ref[rows, :].astype(F32) + mm(att_ref[rows, :], w_ref[:, out_at:gate_at])
        h1_ref[rows, :] = value
        normed = (value * lax.rsqrt(mean_square(value) + EPSILON) * gain).astype(BF16)
        nt_ref[rows, :] = normed
        ntt_ref[:, tile * QT : (tile + 1) * QT] = jnp.transpose(normed)
        gres_ref[rows, :] = (cot_ref[rows, :].astype(F32) * valid[tile * QT : (tile + 1) * QT]).astype(BF16)

    def inward(tile, carry):
        at = pl.multiple_of(tile * FF_TILE, FF_TILE)
        cols = pl.ds(at, FF_TILE)
        gate = mm(nt_ref[...], w_ref[:, pl.ds(gate_at + at, FF_TILE)])
        up = mm(nt_ref[...], w_ref[:, pl.ds(gate_at + hidden + at, FF_TILE)])
        back = mm_cols(gres_ref[...], wb_ref[cols, :])
        square = gate * gate
        bend = jnp.tanh(GELU_C * (gate * (1.0 + GELU_A * square)))
        half = 0.5 * (1.0 + bend)
        act = gate * half
        slope = half + (0.5 * GELU_C) * gate * (1.0 - bend * bend) * (1.0 + (3.0 * GELU_A) * square)
        h2_ref[:, cols] = (act * up).astype(BF16)
        gg_ref[:, cols] = (back * up * slope).astype(BF16)
        gu_ref[:, cols] = (back * act).astype(BF16)
        return carry

    lax.fori_loop(0, hidden // FF_TILE, inward, 0)

    def outward(tile, carry):
        cols = pl.ds(pl.multiple_of(tile * QUAD, QUAD), QUAD)
        value = h1_ref[:, cols] + mm(h2_ref[...], wb_ref[:, cols])
        y_ref[:, cols] = (value * valid).astype(BF16)
        gn_ref[:, cols] = mm_cols(gg_ref[...], w_ref[cols, gate_at : gate_at + hidden]) + mm_cols(
            gu_ref[...], w_ref[cols, gate_at + hidden :]
        )
        return carry

    lax.fori_loop(0, D // QUAD, outward, 0)

    def weights(tile, carry):
        at = pl.multiple_of(tile * FF_TILE, FF_TILE)
        cols = pl.ds(at, FF_TILE)
        dg_ref[:, cols] = mm(ntt_ref[...], gg_ref[:, cols]).astype(BF16)
        du_ref[:, cols] = mm(ntt_ref[...], gu_ref[:, cols]).astype(BF16)
        db_ref[cols, :] = mm_rows(h2_ref[:, cols], gres_ref[...]).astype(BF16)
        return carry

    lax.fori_loop(0, hidden // FF_TILE, weights, 0)

    gain_grad = jnp.zeros((1, D), F32)
    for tile in range(TILES):
        rows = pl.ds(tile * QT, QT)
        value, grad = h1_ref[rows, :], gn_ref[rows, :]
        root = lax.rsqrt(mean_square(value) + EPSILON)
        unit = value * root
        gain_grad = gain_grad + jnp.sum(grad * unit, axis=0, keepdims=True)
        grad = grad * gain
        grad = gres_ref[rows, :].astype(F32) + root * (
            grad - unit * jnp.mean(grad * unit, axis=-1, keepdims=True)
        )
        gh_ref[rows, :] = grad
        low = grad.astype(BF16)
        nt_ref[rows, :] = low
        ga_ref[rows, :] = mm_cols(low, w_ref[:, out_at:gate_at]).astype(BF16)

    def out_weight(tile, carry):
        cols = pl.ds(pl.multiple_of(tile * QUAD, QUAD), QUAD)
        do_ref[cols, :] = mm_rows(att_ref[:, cols], nt_ref[...]).astype(BF16)
        return carry

    lax.fori_loop(0, D // QUAD, out_weight, 0)
    return gain_grad


def backward_attention_start(dk_ref, dv_ref):
    dk_ref[...] = jnp.zeros_like(dk_ref)
    dv_ref[...] = jnp.zeros_like(dv_ref)


def backward_attention_tiles(tab_ref, rank, qkv_ref, att_ref, ga_ref, lse_ref, dqkv_ref, dk_ref, dv_ref, begin, end):
    heads = QUAD // DH
    marks = jnp.where(iota((16, D), 1) // DH == iota((16, D), 0), 1.0, 0.0).astype(BF16)

    def step(tile, carry):
        first = window_start(tile)
        bias, side_bias = tile_bias(tab_ref, rank, tile, first, 0)
        bias = jnp.concatenate([bias, side_bias], axis=0)
        rows = pl.ds(pl.multiple_of(tile * QT, QT), QT)
        window = pl.ds(first, WIN)
        product = ga_ref[rows, :].astype(F32) * att_ref[rows, :].astype(F32)
        high = product.astype(BF16)
        rest = (product - high.astype(F32)).astype(BF16)
        centre = mm_cols(marks, high) + mm_cols(marks, rest)
        lse = lse_ref[tile]
        for quad in range(D // QUAD):
            low = quad * QUAD
            query = head_stack(qkv_ref[rows, low : low + QUAD])
            grad = head_stack(ga_ref[rows, low : low + QUAD])
            keys = jnp.concatenate(
                [qkv_ref[window, D + low : D + low + QUAD], qkv_ref[ROWS:, D + low : D + low + QUAD]], axis=0
            )
            values = jnp.concatenate(
                [qkv_ref[window, 2 * D + low : 2 * D + low + QUAD],
                 qkv_ref[ROWS:, 2 * D + low : 2 * D + low + QUAD]], axis=0
            )
            scores = mm_cols(keys, query)
            slopes = mm_cols(values, grad)
            probs, grads = [], []
            for head in range(heads):
                part = slice(head * QT, (head + 1) * QT)
                number = quad * heads + head
                prob = jnp.exp(scores[:, part] + bias - lse[number : number + 1])
                probs.append(prob.astype(BF16))
                grads.append((prob * (slopes[:, part] - centre[number : number + 1])).astype(BF16))
            probs = jnp.concatenate(probs, axis=1)
            grads = jnp.concatenate(grads, axis=1)
            dkey = mm(grads, query)
            dvalue = mm(probs, grad)
            cols = slice(low, low + QUAD)
            dk_ref[window, cols] = dk_ref[window, cols] + dkey[:WIN]
            dk_ref[ROWS:, cols] = dk_ref[ROWS:, cols] + dkey[WIN:]
            dv_ref[window, cols] = dv_ref[window, cols] + dvalue[:WIN]
            dv_ref[ROWS:, cols] = dv_ref[ROWS:, cols] + dvalue[WIN:]
            dqkv_ref[rows, cols] = head_merge(mm_rows(grads, keys)).astype(BF16)
        return carry

    lax.fori_loop(begin, end, step, 0)


def backward_attention_end(dqkv_ref, dk_ref, dv_ref):
    dqkv_ref[ROWS:, :D] = jnp.zeros((SIDE_ROWS, D), BF16)
    dqkv_ref[:, D : 2 * D] = dk_ref[...].astype(BF16)
    dqkv_ref[:, 2 * D :] = dv_ref[...].astype(BF16)


def weight_grads(n_ref, dqkv_ref, refs):
    for number, ref in enumerate(refs):
        def weights(tile, carry):
            at = pl.multiple_of(tile * QUAD, QUAD)
            value = mm_rows(n_ref[...], dqkv_ref[:, pl.ds(number * D + at, QUAD)]).astype(BF16)
            if len(ref.shape) == 4:
                ref[:, :, :, pl.ds(at, QUAD)] = value.reshape(ref.shape[:3] + (QUAD,))
            else:
                ref[:, pl.ds(at, QUAD)] = value
            return carry

        lax.fori_loop(0, D // QUAD, weights, 0)


def backward_project(tab_ref, rank, x_ref, gh_ref, gains, n_ref, dqkv_ref, w_ref, gn_ref, g_ref):
    def step(tile, carry):
        cols = pl.ds(pl.multiple_of(tile * QUAD, QUAD), QUAD)
        gn_ref[:, cols] = mm_cols(dqkv_ref[...], w_ref[cols, : 3 * D])
        return carry

    lax.fori_loop(0, D // QUAD, step, 0)
    pool = pooling(tab_ref, rank)
    side = mm(pool, n_ref[:ROWS, :])
    root = lax.rsqrt(mean_square(side) + EPSILON)
    unit = side * root
    grad = gn_ref[ROWS:, :]
    side_gain = jnp.sum(grad * unit, axis=0, keepdims=True)
    grad = grad * gains[1:2]
    grad = root * (grad - unit * jnp.mean(grad * unit, axis=-1, keepdims=True))
    parts = three_way(grad)
    gain_grad = jnp.zeros((1, D), F32)
    for tile in range(TILES):
        rows = pl.ds(tile * QT, QT)
        spread = pool[:, tile * QT : (tile + 1) * QT]
        total = gn_ref[rows, :] + mm_rows(spread, parts[0]) + mm_rows(spread, parts[1])
        value = x_ref[rows, :].astype(F32)
        root = lax.rsqrt(mean_square(value) + EPSILON)
        unit = value * root
        gain_grad = gain_grad + jnp.sum(total * unit, axis=0, keepdims=True)
        total = total * gains[0:1]
        value = (
            gh_ref[rows, :] + root * (total - unit * jnp.mean(total * unit, axis=-1, keepdims=True))
        ).astype(BF16)
        if len(g_ref.shape) == 3:
            g_ref[pl.ds(tile * (QT // BLK), QT // BLK)] = value.reshape(QT // BLK, BLK, D)
        else:
            g_ref[rows, :] = value
    return gain_grad, side_gain


def first_kernel(tab_ref, x_ref, gc_ref, w_ref, n_ref, qkv_ref, att_ref, lse_ref):
    rank = lax.axis_index("rep")
    gains = gains_of(gc_ref)
    forward_norm(tab_ref, rank, x_ref, gains, n_ref)
    forward_project(n_ref, w_ref, qkv_ref)
    forward_attention(tab_ref, rank, qkv_ref, att_ref, lse_ref, 0, TILES)


def second_kernel(tab_ref, x_ref, cot_ref, att_ref, gc_ref, w_ref, wb_ref,
                  y_ref, gh_ref, ga_ref, dg_ref, du_ref, db_ref, do_ref, gain_ref, *scratch):
    rank = lax.axis_index("rep")
    gain_ref[...] = feed_forward(tab_ref, rank, x_ref, cot_ref, att_ref, gains_of(gc_ref), w_ref, wb_ref,
                                 y_ref, gh_ref, ga_ref, dg_ref, du_ref, db_ref, do_ref, *scratch)


def third_kernel(tab_ref, x_ref, gh_ref, ga_ref, att_ref, lse_ref, n_ref, qkv_ref, gain_ref, gc_ref, w_ref,
                 g_ref, dw_ref, dc_ref, dqkv_ref, dk_ref, dv_ref, gn_ref):
    rank = lax.axis_index("rep")
    gains = gains_of(gc_ref)
    backward_attention_start(dk_ref, dv_ref)
    backward_attention_tiles(tab_ref, rank, qkv_ref, att_ref, ga_ref, lse_ref, dqkv_ref, dk_ref, dv_ref, 0, TILES)
    backward_attention_end(dqkv_ref, dk_ref, dv_ref)
    weight_grads(n_ref, dqkv_ref, [dw_ref.at[:, i * D : (i + 1) * D] for i in range(3)])
    one, side = backward_project(tab_ref, rank, x_ref, gh_ref, gains, n_ref, dqkv_ref, w_ref, gn_ref, g_ref)
    grads = jnp.concatenate([one, side, gain_ref[...], jnp.zeros((5, D), F32)], axis=0)
    spread_gain_grads(grads, dc_ref)


def attend(tab, x, gc, w):
    shape = jax.ShapeDtypeStruct
    return pl.pallas_call(
        first_kernel,
        out_shape=(shape((ALL_ROWS, D), BF16), shape((ALL_ROWS, 3 * D), BF16), shape((ROWS, D), BF16),
                   shape((TILES, 16, QT), F32)),
        in_specs=[SMEM, VMEM, VMEM, pl.BlockSpec((D, 3 * D), lambda step: (0, 0))],
        grid=(1,),
        out_specs=(VMEM,) * 4,
        compiler_params=pltpu.CompilerParams(vmem_limit_bytes=VMEM_LIMIT),
        name="attend",
    )(tab, x, gc, w)


def feed(tab, x, cot, att, gc, w, wb):
    hidden = wb.shape[0]
    shape = jax.ShapeDtypeStruct
    return pl.pallas_call(
        second_kernel,
        out_shape=(shape((ROWS, D), BF16), shape((ROWS, D), F32), shape((ROWS, D), BF16),
                   shape((D, hidden), BF16), shape((D, hidden), BF16), shape((hidden, D), BF16), shape((D, D), BF16),
                   shape((1, D), F32)),
        in_specs=[SMEM] + [VMEM] * 6,
        out_specs=(VMEM,) * 8,
        scratch_shapes=[pltpu.VMEM((ROWS, D), F32), pltpu.VMEM((ROWS, D), BF16), pltpu.VMEM((D, ROWS), BF16),
                        pltpu.VMEM((ROWS, D), BF16), pltpu.VMEM((ROWS, hidden), BF16),
                        pltpu.VMEM((ROWS, hidden), BF16), pltpu.VMEM((ROWS, hidden), BF16),
                        pltpu.VMEM((ROWS, D), F32)],
        compiler_params=pltpu.CompilerParams(vmem_limit_bytes=VMEM_LIMIT),
        name="feed_forward",
    )(tab, x, cot, att, gc, w, wb)


def backward_layer(tab, x, gh, ga, att, lse, n, qkv, gain, gc, w):
    shape = jax.ShapeDtypeStruct
    return pl.pallas_call(
        third_kernel,
        out_shape=(shape((ROWS, D), BF16), shape((D, 3 * D), BF16), shape((gc.shape[0], 8, 128), F32)),
        in_specs=[SMEM] + [VMEM] * 9 + [pl.BlockSpec((D, 3 * D), lambda step: (0, 0))],
        grid=(1,),
        out_specs=(VMEM,) * 3,
        scratch_shapes=[pltpu.VMEM((ALL_ROWS, 3 * D), BF16), pltpu.VMEM((ALL_ROWS, D), F32),
                        pltpu.VMEM((ALL_ROWS, D), F32), pltpu.VMEM((ALL_ROWS, D), F32)],
        compiler_params=pltpu.CompilerParams(vmem_limit_bytes=VMEM_LIMIT),
        name="attend_back",
    )(tab, x, gh, ga, att, lse, n, qkv, gain, gc, w)


class Links:
    def __init__(self, outer, inner):
        self.outer, self.inner = outer, inner
        self.rank, self.spot = lax.axis_index("rep"), lax.axis_index("fsdp")
        self.core = self.rank % 2
        self.row, self.col = self.spot // inner, self.spot % inner
        self.mate, self.across = core_of(self.rank), across_of(self.rank)
        self.late = []

    def greet(self, everyone=False):
        barrier = pltpu.get_barrier_semaphore()
        neighbours = (
            (self.row + 1 < self.outer, {"fsdp": self.spot + self.inner}),
            (self.row > 0, {"fsdp": self.spot - self.inner}),
            (self.col + 1 < self.inner, {"fsdp": self.spot + 1}),
            (self.col > 0, {"fsdp": self.spot - 1}),
        )
        group = (self.mate, self.across) + ((across_of(self.mate),) if everyone else ())
        amount = jnp.int32(len(group))
        for there, device in neighbours:
            amount = amount + there.astype(jnp.int32)

            @pl.when(there)
            def _():
                pl.semaphore_signal(barrier, inc=1, device_id=device, device_id_type=MESH)

        for device in group:
            pl.semaphore_signal(barrier, inc=1, device_id={"rep": device}, device_id_type=MESH)
        pl.semaphore_wait(barrier, amount)

    def send(self, there, src, dst, ssem, rsem, device):
        def describe():
            return pltpu.make_async_remote_copy(
                src_ref=src, dst_ref=dst, send_sem=ssem, recv_sem=rsem,
                device_id=device, device_id_type=MESH,
            )

        if there is None:
            describe().start()
        else:
            @pl.when(there)
            def _():
                describe().start()

        self.late.append((there, lambda: describe().wait_send()))

    def arrive(self, place, rsem, spare):
        pltpu.make_async_remote_copy(
            src_ref=place, dst_ref=place, send_sem=spare, recv_sem=rsem,
            device_id={"rep": self.mate}, device_id_type=MESH,
        ).wait_recv()

    def drain(self):
        for there, finish in self.late:
            if there is None:
                finish()
            else:
                pl.when(there)(finish)


def halves(ref, which):
    half = ref.shape[-1] // 2
    cols = pl.ds(pl.multiple_of(which * half, 128), half)
    return ref.at[:, :, :, cols] if len(ref.shape) == 4 else ref.at[:, cols]


class Reduction:
    def __init__(self, links, source, total, mine, crecv, yrecv, zrecv, xrecv, stage, sems, number):
        self.links, self.source, self.total, self.mine, self.stage = links, source, total, mine, stage
        self.crecv, self.yrecv, self.zrecv, self.xrecv = crecv, yrecv, zrecv, xrecv
        self.sems, self.number = sems, number
        self.whole = total.shape[-1] % 256 != 0
        self.load = None

    def sem(self, name, *index):
        return self.sems[name].at[index + (self.number,)]

    def begin(self):
        links = self.links
        other = self.source if self.whole else halves(self.source, 1 - links.core)
        links.send(None, other, self.crecv, self.sem("c_send"), self.sem("c_recv"), {"rep": links.mate})
        if self.mine is None:
            self.mine = self.source if self.whole else halves(self.source, links.core)
        else:
            own = self.source if self.whole else halves(self.source, links.core)
            self.load = pltpu.make_async_copy(own, self.mine, self.sem("m_sem"))
            self.load.start()

    def pair(self):
        links = self.links
        if self.load is not None:
            self.load.wait()
        links.arrive(self.crecv, self.sem("c_recv"), self.sems["spare"].at[0])
        inner = links.inner

        def add(index, carry):
            row, col = index // inner, index % inner
            self.mine[row, col] = self.mine[row, col] + self.crecv[row, col]
            return carry

        lax.fori_loop(0, links.outer * inner, add, 0)
        links.send(None, self.mine.at[:, 1 - links.col], self.yrecv, self.sem("y_send"), self.sem("y_recv"),
                   {"fsdp": links.spot + 1 - 2 * links.col})

    def slot(self, way, place, dest):
        return dest - place if way == 0 else self.links.outer - place + dest

    def pass_on(self, way, dest, there, first):
        links = self.links
        step = 1 if way == 0 else -1
        mine = self.mine.at[dest, links.col]
        put = self.slot(way, links.row + step, dest)
        if not first:
            got = self.slot(way, links.row, dest)

            @pl.when(there)
            def _():
                links.arrive(self.zrecv.at[got], self.sem("z_recv", got), self.sems["spare"].at[0])
                mine[...] = mine[...] + self.zrecv[got]

        links.send(there, mine, self.zrecv.at[put], self.sem("z_send", way, dest), self.sem("z_recv", put),
                   {"fsdp": links.spot + step * links.inner})

    def column(self):
        links = self.links
        size = links.outer
        links.arrive(self.yrecv, self.sem("y_recv"), self.sems["spare"].at[0])

        def add(index, carry):
            self.mine[index, links.col] = self.mine[index, links.col] + self.yrecv[index]
            return carry

        lax.fori_loop(0, size, add, 0)
        for far in range(size - 1, 0, -1):
            self.pass_on(0, far, links.row == 0, True)
            self.pass_on(1, size - 1 - far, links.row == size - 1, True)

    def hop(self, turn):
        links = self.links
        size = links.outer
        for way in range(2):
            place = turn if way == 0 else size - 1 - turn
            here = links.row == place
            rest = range(size - 1, place, -1) if way == 0 else range(0, place)
            for dest in rest:
                self.pass_on(way, dest, here, False)
            mine = self.mine.at[place, links.col]
            got = self.slot(way, place, place)

            @pl.when(here)
            def _():
                links.arrive(self.zrecv.at[got], self.sem("z_recv", got), self.sems["spare"].at[0])
                mine[...] = mine[...] + self.zrecv[got]

    def cross(self):
        links = self.links
        mine = self.mine.at[links.row, links.col]
        links.send(None, mine, self.xrecv, self.sem("x_send"), self.sem("x_recv"), {"rep": links.across})

    def finish(self):
        links = self.links
        links.arrive(self.xrecv, self.sem("x_recv"), self.sems["spare"].at[0])
        self.stage[...] = self.mine[links.row, links.col].astype(F32) + self.xrecv[...].astype(F32)
        place = self.total if self.whole else halves(self.total, links.core)
        self.keep = pltpu.make_async_copy(self.stage, place, self.sem("m_sem"))
        self.keep.start()
        if not self.whole:
            links.send(None, self.stage, place, self.sem("f_send"), self.sem("f_recv"), {"rep": links.mate})

    def settle(self):
        self.keep.wait()
        if not self.whole:
            self.links.arrive(
                halves(self.total, 1 - self.links.core), self.sem("f_recv"), self.sems["spare"].at[0]
            )


SEM_NAMES = ("c_send", "c_recv", "m_sem", "y_send", "y_recv", "z_send", "z_recv", "x_send", "x_recv",
             "f_send", "f_recv", "r_send", "r_recv", "own", "spare")


class Return:
    def __init__(self, links, source, home, sems, kind):
        self.links, self.source, self.home, self.sems, self.kind = links, source, home, sems, kind

    def begin(self):
        links = self.links
        dst = self.home.at[links.rank]
        for way, device in enumerate((links.across, links.mate)):
            links.send(None, self.source, dst, self.sems["r_send"].at[self.kind, way],
                       self.sems["r_recv"].at[self.kind, way], {"rep": device})
        self.copy = pltpu.make_async_copy(self.source, dst, self.sems["own"].at[self.kind])
        self.copy.start()

    def relay(self):
        links = self.links
        place = self.home.at[links.across]
        links.arrive(place, self.sems["r_recv"].at[self.kind, 0], self.sems["spare"].at[0])
        links.send(None, place, place, self.sems["r_send"].at[self.kind, 2],
                   self.sems["r_recv"].at[self.kind, 2], {"rep": links.mate})

    def settle(self):
        links, sem = self.links, self.sems["r_recv"]
        links.arrive(self.home.at[links.mate], sem.at[self.kind, 1], self.sems["spare"].at[0])
        links.arrive(self.home.at[across_of(links.mate)], sem.at[self.kind, 2], self.sems["spare"].at[0])
        self.copy.wait()


TABLE_ROWS = 56


def packed_table(lens, tabv_ref):
    lane = iota((8, 128), 1)
    blocks = lax.div(lens + (BLK - 1), BLK)
    key = jnp.where(blocks > 0, blocks * 128 + (127 - lane), 0)
    wide = jnp.broadcast_to(key[:1], (128, 128))
    other = jnp.sum(jnp.where(iota((128, 128), 0) == iota((128, 128), 1), wide, 0), axis=1, keepdims=True)
    order = jnp.sum(jnp.where(other > wide, 1, 0), axis=0, keepdims=True)
    order = jnp.broadcast_to(order, (8, 128))
    edges, below = [], jnp.zeros((8, 1), jnp.int32)
    for size in range(MAX_SEQ_BLOCKS, 0, -1):
        below = below + jnp.sum(jnp.where(blocks == size, 1, 0), axis=1, keepdims=True)
        edges.append(jnp.broadcast_to(below, (8, 128)))

    def assign(number, carry):
        loads, slot, first = carry[:4], carry[4], carry[5]
        size = jnp.zeros((8, 128), jnp.int32)
        for step, edge in enumerate(edges):
            size = size + jnp.where(number < edge, 1, 0)
        low = jnp.minimum(jnp.minimum(loads[0], loads[1]), jnp.minimum(loads[2], loads[3]))
        best = jnp.full((8, 128), 3, jnp.int32)
        for dev in (2, 1, 0):
            best = jnp.where(loads[dev] == low, dev, best)
        mine = order == number
        slot = jnp.where(mine, best * SLOTS + low, slot)
        first = jnp.where(mine, low, first)
        loads = tuple(loads[dev] + jnp.where(best == dev, size, 0) for dev in range(4))
        return loads + (slot, first)

    zero = jnp.zeros((8, 128), jnp.int32)
    carry = lax.fori_loop(0, 32, assign, (zero,) * 6)
    slot, first = carry[4], carry[5]
    where, tokens, segment = zero - 1, zero, zero
    for step in range(MAX_SEQ_BLOCKS):
        def shifted(value):
            return value if step == 0 else pltpu.roll(value, step, 1)

        covers = shifted(blocks) > step
        where = jnp.where(covers, shifted(slot) + step, where)
        tokens = jnp.where(covers, jnp.minimum(shifted(lens) - BLK * step, BLK), tokens)
        segment = jnp.where(covers, shifted(first) + 1, segment)
    packed = jnp.where(where >= 0, (lane + 1) + 128 * tokens + 16384 * segment, 0)
    spots = jnp.broadcast_to(where[:1], (48, 128))
    values = jnp.broadcast_to(packed[:1], (48, 128))
    column = jnp.sum(jnp.where(spots == iota((48, 128), 0), values, 0), axis=1, keepdims=True)
    tabv_ref[:48] = jnp.broadcast_to(column, (48, 128))
    tabv_ref[48:] = where


def front_kernel(outer, inner, *refs):
    (lens_ref, rows_ref, cots_ref, *weights), refs = refs[:9], refs[9:]
    (wd_ref, wc_ref), refs = refs[:2], refs[2:]
    (tab_ref, x_ref, cot_ref, n_ref, qkv_ref, att_ref, lse_ref, wqkv_ref, gc_ref, ga_ref, gb_ref), refs = refs[:11], refs[11:]
    (stage, lens_all, tabs, psend, precv, xsend, xrecv), refs = refs[:7], refs[7:]
    (l_send, l_recv, t_sem, w_sem, z_send, z_recv, y_send, y_recv, c_send, c_recv, d_send, d_recv, own_sem,
     p_send, p_recv, x_send, x_recv, spare) = refs
    links = Links(outer, inner)
    rank, spot, core, mate, across = links.rank, links.spot, links.core, links.mate, links.across
    row, col = links.row, links.col
    side = rank // 2
    count = outer * inner
    part = stage.shape[0]
    per_rank = rows_ref.shape[0]
    width = 3 * D
    tall = wd_ref.shape[0]
    hidden = weights[-1].shape[1]
    gate_half, up_half = (D + hidden) // 2, hidden // 2

    at = 0
    loads = []
    for number, ref in enumerate(weights):
        cols = slice(at, at + ref.shape[1])
        loads.append(pltpu.make_async_copy(ref, stage.at[:, cols], w_sem.at[number]))
        loads[-1].start()
        at += ref.shape[1]

    links.greet(True)
    lens_all[rank] = lens_ref[...]
    for step in range(1, 4):
        links.send(None, lens_ref, lens_all.at[rank], l_send.at[step - 1], l_recv.at[step - 1],
                   {"rep": (rank + step) % 4})

    def cols_of(start, half, which):
        return pl.ds(pl.multiple_of(start + which * half, 128), half)

    down_half = D // 2

    def tall_rows(which):
        return pl.ds(pl.multiple_of(which * (tall // 2), 16), tall // 2)

    def source(number):
        return (
            lambda: stage.at[:, cols_of(0, width // 2, core)],
            lambda: stage.at[:, cols_of(width, gate_half, core)],
            lambda: stage.at[:, cols_of(width + 2 * gate_half, up_half, core)],
            lambda: wd_ref.at[tall_rows(side), cols_of(0, down_half, core)],
            lambda: wc_ref,
        )[number]()

    def place(number, shard, which=None):
        which = core if which is None else which
        return (
            lambda: wqkv_ref.at[pl.ds(pl.multiple_of(shard * part, 16), part), cols_of(0, width // 2, which)],
            lambda: ga_ref.at[shard, :, cols_of(0, gate_half, which)],
            lambda: ga_ref.at[shard, :, cols_of(2 * gate_half, up_half, which)],
            lambda: gb_ref.at[shard, tall_rows(side), cols_of(0, down_half, which)],
            lambda: gc_ref.at[shard],
            lambda: gb_ref.at[shard, tall_rows(1 - side), cols_of(0, down_half, which)],
        )[number]()

    nobody = spare.at[0]

    def both(first, second):
        return second if first is None else jnp.logical_and(first, second)

    def guarded(there, action):
        if there is None:
            action()
        else:
            pl.when(there)(action)

    def share(there, number, shard):
        if number == 4:
            return
        here = place(number, shard)
        links.send(there, here, here, c_send.at[number, shard], c_recv.at[number, shard], {"rep": mate})
        if number == 3:
            links.send(there, here, here, d_send.at[shard], d_recv.at[shard], {"rep": across})

    other_column = {"fsdp": spot + 1 - 2 * col}

    def along_row(there, number, line, src):
        here = place(number, line * inner + col)
        links.send(there, here if src is None else src, here, y_send.at[line, number], y_recv.at[line, number],
                   other_column)

    def lines(step):
        return ((row - 1 - step >= 0, row - 1 - step, 0, row + 1 < outer, spot + inner),
                (row + 1 + step < outer, row + 1 + step, 1, row > 0, spot - inner))

    def own(number):
        src, dst = source(number), place(number, spot)
        links.send(row + 1 < outer, src, dst, z_send.at[0, 0, number], z_recv.at[0, 0, number],
                   {"fsdp": spot + inner})
        links.send(row > 0, src, dst, z_send.at[1, 0, number], z_recv.at[1, 0, number], {"fsdp": spot - inner})
        along_row(None, number, row, src)

    def hop(number, step):
        for here, line, way, onward, target in lines(step):
            shard = line * inner + col
            guarded(here, lambda: links.arrive(place(number, shard), z_recv.at[way, step, number], nobody))
            if step + 1 < outer - 1:
                view = place(number, shard)
                links.send(both(here, onward), view, view, z_send.at[way, step + 1, number],
                           z_recv.at[way, step + 1, number], {"fsdp": target})
            along_row(here, number, line, None)
            share(here, number, shard)

    def from_row(number):
        def one(there, line):
            shard = line * inner + 1 - col
            guarded(there, lambda: links.arrive(place(number, shard), y_recv.at[line, number], nobody))
            share(there, number, shard)

        one(None, row)
        for step in range(outer - 1):
            for here, line, *_ in lines(step):
                one(here, line)

    def gathered(*numbers):
        for shard in range(count):
            @pl.when(shard != spot)
            def _():
                for number in numbers:
                    links.arrive(place(number, shard, 1 - core), c_recv.at[number, shard], nobody)

    def from_across():
        for shard in range(count):
            there = shard != spot
            guarded(there, lambda: links.arrive(place(5, shard), d_recv.at[shard], nobody))
            here = place(5, shard)
            links.send(there, here, here, c_send.at[5, shard], c_recv.at[5, shard], {"rep": mate})

    for load in loads:
        load.wait()
    own(0)
    own(4)
    own(1)
    keep = [
        pltpu.make_async_copy(stage.at[:, :width], wqkv_ref.at[pl.ds(pl.multiple_of(spot * part, 16), part)], own_sem.at[0]),
        pltpu.make_async_copy(stage.at[:, width:], ga_ref.at[spot], own_sem.at[1]),
        pltpu.make_async_copy(wd_ref, gb_ref.at[spot], own_sem.at[2]),
        pltpu.make_async_copy(wc_ref, gc_ref.at[spot], own_sem.at[3]),
    ]
    for copy in keep:
        copy.start()

    for step in range(1, 4):
        links.arrive(lens_all.at[(rank + 4 - step) % 4], l_recv.at[step - 1], nobody)
    lens = lens_all[0] + lens_all[1] + lens_all[2] + lens_all[3]
    packed_table(jnp.broadcast_to(lens[:1], (8, 128)), tab_ref)
    to_scalar = pltpu.make_async_copy(tab_ref, tabs, t_sem.at[0])
    to_scalar.start()
    to_scalar.wait()

    sources = (rows_ref, cots_ref)
    outs = (x_ref, cot_ref)

    def picked(kind, target, slot):
        index = block_at(tabs, target * SLOTS + slot) - rank * per_rank
        mine = jnp.logical_and(index >= 0, index < per_rank)
        return mine, sources[kind][jnp.clip(index, 0, per_rank - 1)]

    def mate_copy(kind, piece):
        return pltpu.make_async_remote_copy(
            src_ref=psend.at[kind, piece], dst_ref=precv.at[kind, piece],
            send_sem=p_send.at[kind, piece], recv_sem=p_recv.at[kind, piece],
            device_id={"rep": mate}, device_id_type=MESH,
        )

    def across_copy(kind):
        return pltpu.make_async_remote_copy(
            src_ref=xsend.at[kind], dst_ref=xrecv.at[kind],
            send_sem=x_send.at[kind], recv_sem=x_recv.at[kind],
            device_id={"rep": across}, device_id_type=MESH,
        )

    def pack_rows(kind, piece):
        target = mate if piece == 0 else across_of(mate)

        def pack(slot, carry):
            mine, value = picked(kind, target, slot)
            psend[kind, piece, slot] = jnp.where(mine, value, jnp.zeros_like(value))
            return carry

        lax.fori_loop(0, SLOTS, pack, 0)
        mate_copy(kind, piece).start()

    def cross_rows(kind):
        mate_copy(kind, 1).wait_recv()

        def merge(slot, carry):
            mine, value = picked(kind, across, slot)
            xsend[kind, slot] = jnp.where(mine, value, precv[kind, 1, slot])
            return carry

        lax.fori_loop(0, SLOTS, merge, 0)
        across_copy(kind).start()

    def finish_rows(kind):
        mate_copy(kind, 0).wait_recv()
        across_copy(kind).wait_recv()

        def finish(slot, carry):
            mine, value = picked(kind, rank, slot)
            rows = pl.ds(pl.multiple_of(slot * BLK, BLK), BLK)
            outs[kind][rows, :] = jnp.where(mine, value, precv[kind, 0, slot] + xrecv[kind, slot])
            return carry

        lax.fori_loop(0, SLOTS, finish, 0)

    pack_rows(0, 1)
    pack_rows(1, 1)
    cross_rows(0)
    pack_rows(0, 0)
    cross_rows(1)
    pack_rows(1, 0)
    for step in range(outer - 1):
        hop(0, step)
    for step in range(outer - 1):
        hop(4, step)
    hop(1, 0)
    own(2)
    from_row(0)
    from_row(4)
    for step in range(1, outer - 1):
        hop(1, step)
    keep[3].wait()
    gains = gains_of(gc_ref)
    finish_rows(0)
    forward_norm(tabs, rank, x_ref, gains, n_ref)
    hop(2, 0)
    own(3)
    keep[0].wait()
    gathered(0)
    forward_project(n_ref, wqkv_ref, qkv_ref)
    hop(2, 1)
    forward_attention(tabs, rank, qkv_ref, att_ref, lse_ref, 0, 2)
    from_row(1)
    for step in range(2, outer - 1):
        hop(2, step)
    hop(3, 0)
    forward_attention(tabs, rank, qkv_ref, att_ref, lse_ref, 2, 4)
    from_row(2)
    for step in range(1, outer - 1):
        hop(3, step)
    forward_attention(tabs, rank, qkv_ref, att_ref, lse_ref, 4, TILES)
    from_row(3)
    finish_rows(1)
    from_across()
    gathered(1, 2, 3, 5)
    links.drain()
    for kind in range(2):
        for piece in range(2):
            mate_copy(kind, piece).wait_send()
        across_copy(kind).wait_send()
    for copy in keep[1:3]:
        copy.wait()


def gather_and_attend(count, lens, rows, cots, weights, wd, wc):
    outer, inner = grid_of(count)
    block = rows.shape[1:]
    part, hidden = wd.shape[0], weights[-1].shape[1]
    part = weights[0].shape[0]
    dma, shape = pltpu.SemaphoreType.DMA, jax.ShapeDtypeStruct
    total = sum(weight.shape[1] for weight in weights)
    kinds = 5
    return pl.pallas_call(
        partial(front_kernel, outer, inner),
        out_shape=(
            shape((TABLE_ROWS, 128), jnp.int32), shape((ROWS, D), BF16), shape((ROWS, D), BF16),
            shape((ALL_ROWS, D), BF16), shape((ALL_ROWS, 3 * D), BF16), shape((ROWS, D), BF16),
            shape((TILES, 16, QT), F32), shape((D, 3 * D), BF16), shape((count,) + wc.shape, BF16),
            shape((count, part, total - 3 * D), BF16), shape((count,) + wd.shape, BF16),
        ),
        in_specs=[VMEM] * 3 + [ANY] * 6 + [VMEM] * 2,
        out_specs=(VMEM,) * 9 + (ANY,) * 2,
        scratch_shapes=[
            pltpu.VMEM((part, total), BF16), pltpu.VMEM((4, 8, 128), jnp.int32), pltpu.SMEM((TABLE_ROWS, 128), jnp.int32),
            pltpu.VMEM((2, 2, SLOTS) + block, BF16), pltpu.VMEM((2, 2, SLOTS) + block, BF16),
            pltpu.VMEM((2, SLOTS) + block, BF16), pltpu.VMEM((2, SLOTS) + block, BF16),
            dma((3,)), dma((3,)), dma((1,)), dma((6,)),
            dma((2, outer - 1, kinds)), dma((2, outer - 1, kinds)), dma((outer, kinds)), dma((outer, kinds)),
            dma((kinds + 1, count)), dma((kinds + 1, count)), dma((count,)), dma((count,)), dma((4,)),
            dma((2, 2)), dma((2, 2)), dma((2,)), dma((2,)), dma((1,)),
        ],
        compiler_params=pltpu.CompilerParams(
            collective_id=1, has_side_effects=True, vmem_limit_bytes=VMEM_LIMIT
        ),
        name="gather_and_attend",
    )(lens, rows, cots, *weights, wd, wc)


def rear_kernel(outer, inner, *refs):
    (tab_ref, x_ref, att_ref, lse_ref, gc_ref), refs = refs[:5], refs[5:]
    (cot_any, n_any, qkv_any, wqkv_any, wf_any, wd_any), refs = refs[:6], refs[6:]
    kinds = 8
    totals, (ry_ref, rg_ref), refs = refs[:kinds], refs[kinds : kinds + 2], refs[kinds + 2 :]
    (y_ref, gh_ref, fa_ref, dk_ref, b0_ref, b1_ref, b2_ref, n_ref, ntt_ref, gres_ref, ga_ref), refs = refs[:11], refs[11:]
    (wf_ref, wd_ref, dg_ref, du_ref, db_ref, do_ref, dc_ref, mine_ref), refs = refs[:8], refs[8:]
    (gate_recv, up_recv, down_recv, out_recv, gain_recv), refs = refs[:5], refs[5:]
    narrow = D // 2
    crecv = (gate_recv, up_recv, down_recv, out_recv, gate_recv.at[:, :, :, :narrow],
             gate_recv.at[:, :, :, narrow : 2 * narrow], up_recv.at[:, :, :, :narrow], gain_recv)
    yrecv, zrecv, xrecv, stages = (refs[kinds * i : kinds * (i + 1)] for i in range(4))
    sems = dict(zip(SEM_NAMES, refs[4 * kinds :]))
    load_sem, free_sem = refs[4 * kinds + len(SEM_NAMES) :]
    links = Links(outer, inner)
    rank = links.rank
    hidden = wd_ref.shape[0]
    part = wf_ref.shape[2]
    group = 4 * part

    def fetch(number, src, dst):
        copy = pltpu.make_async_copy(src, dst, load_sem.at[number])
        copy.start()
        return copy

    load_cot = fetch(0, cot_any, ga_ref)
    load_out = fetch(1, wf_any.at[:, :, :, :D], wf_ref.at[:, :, :, :D])
    load_in = fetch(2, wf_any.at[:, :, :, D:], wf_ref.at[:, :, :, D:])
    load_down = fetch(3, wd_any, wd_ref)
    links.greet()

    def weight(start, size):
        return wf_ref[:, :, :, pl.ds(start, size)].reshape(D, size)

    grads = [dg_ref, du_ref, db_ref, do_ref] + [wf_ref.at[:, :, :, i * D : (i + 1) * D] for i in range(3)] + [dc_ref]
    tasks = [
        Reduction(links, grads[i], totals[i], mine_ref if i == kinds - 1 else None,
                  crecv[i], yrecv[i], zrecv[i], xrecv[i], stages[i], sems, i)
        for i in range(kinds)
    ]
    rows_y, rows_g = Return(links, y_ref, ry_ref, sems, 0), Return(links, gres_ref, rg_ref, sems, 1)

    gains = gains_of(gc_ref)
    gain = gains[2:3]
    valid = valid_column(tab_ref, rank)
    h1_ref = fa_ref
    load_cot.wait()
    load_out.wait()
    for tile in range(TILES):
        rows = pl.ds(tile * QT, QT)
        value = x_ref[rows, :].astype(F32) + mm(att_ref[rows, :], weight(0, D))
        h1_ref[rows, :] = value
        normed = (value * lax.rsqrt(mean_square(value) + EPSILON) * gain).astype(BF16)
        n_ref[rows, :] = normed
        ntt_ref[:, tile * QT : (tile + 1) * QT] = jnp.transpose(normed)
        gres_ref[rows, :] = (ga_ref[rows, :].astype(F32) * valid[tile * QT : (tile + 1) * QT]).astype(BF16)
    load_in.wait()
    load_down.wait()

    def inward(tile, carry):
        at = pl.multiple_of(tile * FF_TILE, FF_TILE)
        cols = pl.ds(at, FF_TILE)
        normed = n_ref[:ROWS, :]
        gate = mm(normed, weight(D + at, FF_TILE))
        up = mm(normed, weight(D + hidden + at, FF_TILE))
        back = mm_cols(gres_ref[...], wd_ref[cols, :])
        square = gate * gate
        bend = jnp.tanh(GELU_C * (gate * (1.0 + GELU_A * square)))
        half = 0.5 * (1.0 + bend)
        act = gate * half
        slope = half + (0.5 * GELU_C) * gate * (1.0 - bend * bend) * (1.0 + (3.0 * GELU_A) * square)
        b0_ref[:ROWS, cols] = (act * up).astype(BF16)
        b1_ref[:ROWS, cols] = (back * up * slope).astype(BF16)
        b2_ref[:ROWS, cols] = (back * act).astype(BF16)
        return carry

    lax.fori_loop(0, hidden // FF_TILE, inward, 0)

    def outer_products(ref, right_ref):
        def step(tile, carry):
            cols = pl.ds(pl.multiple_of(tile * FF_TILE, FF_TILE), FF_TILE)
            value = mm(ntt_ref[...], right_ref[:ROWS, cols]).astype(BF16)
            ref[:, :, :, cols] = value.reshape(outer, inner, part, FF_TILE)
            return carry

        lax.fori_loop(0, hidden // FF_TILE, step, 0)

    outer_products(dg_ref, b1_ref)
    tasks[0].begin()
    outer_products(du_ref, b2_ref)
    tasks[0].pair()
    tasks[1].begin()

    def down_products(tile, carry):
        cols = pl.ds(pl.multiple_of(tile * FF_TILE, FF_TILE), FF_TILE)
        db_ref[tile // inner, tile % inner] = mm_rows(b0_ref[:ROWS, cols], gres_ref[...]).astype(BF16)
        return carry

    lax.fori_loop(0, hidden // FF_TILE, down_products, 0)
    tasks[1].pair()
    pl.semaphore_signal(free_sem, inc=1, device_id={"rep": links.mate}, device_id_type=MESH)
    tasks[2].begin()

    def outward(tile, carry):
        cols = pl.ds(pl.multiple_of(tile * group, 128), group)
        value = h1_ref[:ROWS, cols] + mm(b0_ref[:ROWS, :hidden], wd_ref[:, cols])
        y_ref[:, cols] = (value * valid).astype(BF16)
        shards = pl.ds(tile * (4 // inner), 4 // inner)
        gh_ref[:, cols] = mm_cols(
            b1_ref[:ROWS, :hidden], wf_ref[shards, :, :, D : D + hidden].reshape(group, hidden)
        ) + mm_cols(b2_ref[:ROWS, :hidden], wf_ref[shards, :, :, D + hidden :].reshape(group, hidden))
        return carry

    lax.fori_loop(0, D // group, outward, 0)
    tasks[2].pair()
    rows_y.begin()
    load_qkv = fetch(4, qkv_any, b1_ref)
    load_wqkv = fetch(5, wqkv_any, b2_ref)

    gain_grad = jnp.zeros((1, D), F32)
    for tile in range(TILES):
        rows = pl.ds(tile * QT, QT)
        value, grad = h1_ref[rows, :], gh_ref[rows, :]
        root = lax.rsqrt(mean_square(value) + EPSILON)
        unit = value * root
        gain_grad = gain_grad + jnp.sum(grad * unit, axis=0, keepdims=True)
        grad = grad * gain
        grad = gres_ref[rows, :].astype(F32) + root * (
            grad - unit * jnp.mean(grad * unit, axis=-1, keepdims=True)
        )
        gh_ref[rows, :] = grad
        low = grad.astype(BF16)
        n_ref[rows, :] = low
        ga_ref[rows, :] = mm_cols(low, weight(0, D)).astype(BF16)

    def out_products(tile, carry):
        cols = pl.ds(pl.multiple_of(tile * QUAD, QUAD), QUAD)
        value = mm_rows(att_ref[...], n_ref[:ROWS, cols]).astype(BF16)
        do_ref[:, :, :, cols] = value.reshape(outer, inner, part, QUAD)
        return carry

    lax.fori_loop(0, D // QUAD, out_products, 0)
    tasks[3].begin()
    load_n = fetch(6, n_any, n_ref)
    dv_ref = fa_ref
    backward_attention_start(dk_ref, dv_ref)
    load_qkv.wait()
    tasks[3].pair()

    def attention(begin, end):
        backward_attention_tiles(tab_ref, rank, b1_ref, att_ref, ga_ref, lse_ref, b0_ref, dk_ref, dv_ref, begin, end)

    def round_of(number):
        if number < kinds:
            tasks[number].column()
        for turn in range(1, outer):
            if 0 <= number - turn < kinds:
                tasks[number - turn].hop(turn)
        if 0 <= number - outer + 1 < kinds:
            tasks[number - outer + 1].cross()
        if 0 <= number - outer < kinds:
            tasks[number - outer].finish()

    attention(0, 3)
    round_of(0)
    attention(3, TILES)
    backward_attention_end(b0_ref, dk_ref, dv_ref)
    load_n.wait()
    load_wqkv.wait()

    def project_products(tile, carry):
        cols = pl.ds(pl.multiple_of(tile * QUAD, QUAD), QUAD)
        value = mm_rows(n_ref[...], b0_ref[:, cols]).astype(BF16)
        wf_ref[:, :, :, cols] = value.reshape(outer, inner, part, QUAD)
        return carry

    lax.fori_loop(0, 3 * D // QUAD, project_products, 0)
    pl.semaphore_wait(free_sem, 1)
    for task in tasks[4:7]:
        task.begin()
    round_of(1)
    rows_y.relay()
    one, side = backward_project(tab_ref, rank, x_ref, gh_ref, gains, n_ref, b0_ref, b2_ref, dk_ref, gres_ref)
    rows_g.begin()
    for task in tasks[4:7]:
        task.pair()
    spread_gain_grads(jnp.concatenate([one, side, gain_grad, jnp.zeros((5, D), F32)], axis=0), dc_ref)
    tasks[7].begin()
    tasks[7].pair()
    for number in range(2, kinds + outer):
        round_of(number)
        if number == 3:
            rows_g.relay()
    rows_y.settle()
    rows_g.settle()
    for task in tasks:
        task.settle()
    links.drain()


def feed_and_reduce(count, table, x, att, lse, gc, cot, n, qkv, wqkv, wf, wd):
    outer, inner = grid_of(count)
    part, tall = D // count, wd.shape[1]
    hidden = count * tall
    wf = wf.reshape((outer, inner) + wf.shape[1:])
    shapes = [(part, hidden), (part, hidden), (tall, D)] + [(part, D)] * 4 + [(8, 128)]
    kinds = len(shapes)
    dtypes = [BF16] * (kinds - 1) + [F32]
    halved = [(a, b // 2 if b % 256 == 0 else b) for a, b in shapes]
    dma, vmem = pltpu.SemaphoreType.DMA, pltpu.VMEM
    scratch = [
        vmem((ROWS, D), BF16), vmem((ROWS, D), F32), vmem((ALL_ROWS, D), F32), vmem((ALL_ROWS, D), F32),
        vmem((ALL_ROWS, 3 * D), BF16), vmem((ALL_ROWS, 3 * D), BF16), vmem((D, 3 * D), BF16),
        vmem((ALL_ROWS, D), BF16), vmem((D, ROWS), BF16), vmem((ROWS, D), BF16), vmem((ROWS, D), BF16),
        vmem(wf.shape, BF16), vmem((hidden, D), BF16),
    ]
    scratch += [vmem((outer, inner) + shape, BF16) for shape in shapes[:4]]
    scratch += [vmem((outer, inner) + shapes[-1], F32)] * 2
    scratch += [vmem((outer, inner) + halved[i], dtypes[i]) for i in (0, 1, 2, 3, 7)]
    for lead in ((outer,), (outer + 1,), ()):
        scratch += [vmem(lead + shape, dtype) for shape, dtype in zip(halved, dtypes)]
    scratch += [vmem(shape, F32) for shape in halved]
    one = dma((kinds,))
    scratch += [one, one, one, one, one, dma((2, outer, kinds)), dma((outer + 1, kinds)), one, one, one, one,
                dma((2, 3)), dma((2, 3)), dma((2,)), dma((1,)), dma((7,)), pltpu.SemaphoreType.REGULAR]
    rows = jax.ShapeDtypeStruct((4, ROWS, D), BF16)
    outs = pl.pallas_call(
        partial(rear_kernel, outer, inner),
        out_shape=tuple(jax.ShapeDtypeStruct(shape, F32) for shape in shapes) + (rows, rows),
        in_specs=[SMEM] + [VMEM] * 4 + [ANY] * 6,
        out_specs=(ANY,) * (kinds + 2),
        scratch_shapes=scratch,
        compiler_params=pltpu.CompilerParams(
            collective_id=2, has_side_effects=True, vmem_limit_bytes=67043328
        ),
        name="feed_and_reduce",
    )(table, x, att, lse, gc, cot, n, qkv, wqkv, wf, wd.reshape(hidden, D))
    return outs[:kinds], outs[kinds], outs[kinds + 1]


def per_device(count, layer_input, cotangent, lengths, attn_gain, global_gain, query_weight, key_weight,
               value_weight, out_weight, ffn_gain, gate_weight, up_weight, down_weight):
    micro, span, width = layer_input.shape
    hidden = gate_weight.shape[1]
    blocks = micro * span // BLK
    part = attn_gain.shape[0]
    rows_in = layer_input.reshape(blocks, BLK, width)
    cots_in = cotangent.reshape(blocks, BLK, width)
    weights = (query_weight, key_weight, value_weight, out_weight, gate_weight, up_weight)
    wc = jnp.pad(jnp.stack([attn_gain, global_gain, ffn_gain]), ((0, 13), (0, 128 - part)))
    if grid_of(count)[1] == 2 and part % 16 == 0:
        lens = lax.dynamic_update_slice(
            jnp.zeros((8, 128), jnp.int32), lengths.reshape(1, blocks), (0, lax.axis_index("rep") * blocks)
        )
        table, x, cot, n, qkv, att, lse, wqkv, gc, ga, gb = gather_and_attend(
            count, lens, rows_in, cots_in, weights, down_weight, wc
        )
        totals, ry, rg = feed_and_reduce(count, table, x, att, lse, gc, cot, n, qkv, wqkv, ga, gb)
        ry, rg = (rows.reshape(4, SLOTS, BLK, width) for rows in (ry, rg))
        og, ou, ob, oo, oq, ok, ov, oc = totals
    else:
        table = deal_table(lengths)
        splits = ((0, 4 * width), (4 * width, 2 * hidden))
        ga, gb, gc, rows, cots = gather_weights(
            count, splits, table, rows_in, cots_in, jnp.concatenate(weights, axis=1), down_weight, wc
        )
        x, full = rows.reshape(ROWS, width), ga.reshape(width, -1)
        n, qkv, att, lse = attend(table, x, gc, full)
        y, gh, gatt, dg, du, db, do, gain = feed(
            table, x, cots.reshape(ROWS, width), att, gc, full, gb.reshape(-1, width)
        )
        g, dw, dc = backward_layer(table, x, gh, gatt, att, lse, n, qkv, gain, gc, full)
        grads = [grad.reshape(count, -1, grad.shape[-1]) for grad in (dg, du, db, do, dw, dc)]
        og, ou, ob, oo, ow, oc, ry, rg = reduce_grads(
            count, grads, y.reshape(SLOTS, BLK, width), g.reshape(SLOTS, BLK, width)
        )
        oq, ok, ov = ow[:, :width], ow[:, width : 2 * width], ow[:, 2 * width :]
    y_home, g_home = bring_home(table, ry, rg, blocks)
    return (
        y_home.reshape(layer_input.shape), g_home.reshape(layer_input.shape),
        oc[0, :part], oc[1, :part], oq, ok, ov, oo, oc[2, :part], og, ou, ob,
    )


def solution(mesh):
    rows = P(None, ("rep", "fsdp"), None)
    vector, matrix = P("fsdp"), P("fsdp", None)
    return jax.shard_map(
        partial(per_device, mesh.shape["fsdp"]),
        mesh=mesh,
        in_specs=(rows, rows, P(None, ("rep", "fsdp")), vector, vector, matrix, matrix, matrix, matrix,
                  vector, matrix, matrix, matrix),
        out_specs=(rows, rows, vector, vector, matrix, matrix, matrix, matrix, vector, matrix, matrix, matrix),
        check_vma=False,
    )
```

```python
from functools import partial

import jax
import jax.numpy as jnp
from jax import lax
from jax.experimental import pallas as pl
from jax.experimental.pallas import tpu as pltpu
from jax.sharding import PartitionSpec as P

H = 12
DH = 64
RADIUS = 127
GBLK = 16
BLK = 64
SLOTS = 10
MAX_SEQ_BLOCKS = 5
EPSILON = 1e-06
MASKED_SCORE = -1e30
MESH = pl.DeviceIdType.MESH
VMEM_LIMIT = 60 * 1024 * 1024
SEG_AT, LEN_AT, DEST_AT, TABLE_SIZE = 40, 80, 120, 256

ANY = pl.BlockSpec(memory_space=pl.ANY)
VMEM = pl.BlockSpec(memory_space=pltpu.VMEM)
SMEM = pl.BlockSpec(memory_space=pltpu.SMEM)


def grid_of(count):
    inner = 2 if count <= 8 else 4
    return count // inner, inner


def core_of(rank):
    return rank + 1 - 2 * (rank % 2)


def across_of(rank):
    return (rank + 2) % 4


def lens_kernel(lens_ref, all_ref, send_sem, recv_sem):
    rank = lax.axis_index("rep")
    barrier = pltpu.get_barrier_semaphore()
    for step in range(1, 4):
        pl.semaphore_signal(
            barrier, inc=1, device_id={"rep": (rank + step) % 4}, device_id_type=MESH
        )
    pl.semaphore_wait(barrier, 3)
    copies = []
    for step in range(1, 4):
        copy = pltpu.make_async_remote_copy(
            src_ref=lens_ref,
            dst_ref=all_ref.at[rank],
            send_sem=send_sem.at[step - 1],
            recv_sem=recv_sem.at[step - 1],
            device_id={"rep": (rank + step) % 4},
            device_id_type=MESH,
        )
        copy.start()
        copies.append(copy)
    all_ref[rank] = lens_ref[...]
    for copy in copies:
        copy.wait()


def table_kernel(micro, per_dev, lens_ref, tab_ref, order_ref, count_ref, load_ref):
    total = 4 * micro * per_dev

    def length_at(spot):
        return lens_ref[spot // (micro * per_dev), (spot // per_dev) % micro, spot % per_dev]

    def blocks_of(length):
        return (length + (BLK - 1)) // BLK

    def clear(spot, carry):
        tab_ref[spot] = -1
        return carry

    lax.fori_loop(0, TABLE_SIZE, clear, 0)
    for spot in range(4 * SLOTS):
        tab_ref[LEN_AT + spot] = 0
    for size in range(8):
        count_ref[size] = 0
    for dev in range(4):
        load_ref[dev] = 0

    def tally(spot, carry):
        length = length_at(spot)

        @pl.when(length > 0)
        def _():
            size = blocks_of(length)
            count_ref[size] = count_ref[size] + 1

        return carry

    lax.fori_loop(0, total, tally, 0)
    begin = 0
    for size in range(MAX_SEQ_BLOCKS, 0, -1):
        amount = count_ref[size]
        count_ref[size] = begin
        begin = begin + amount

    def place(spot, carry):
        length = length_at(spot)

        @pl.when(length > 0)
        def _():
            size = blocks_of(length)
            where = count_ref[size]
            order_ref[where] = spot
            count_ref[size] = where + 1

        return carry

    lax.fori_loop(0, total, place, 0)

    def assign(number, carry):
        spot = order_ref[number]
        length = length_at(spot)
        size = blocks_of(length)
        best = jnp.int32(0)
        low = load_ref[0]
        for dev in range(1, 4):
            here = load_ref[dev]
            best = jnp.where(here < low, dev, best)
            low = jnp.minimum(here, low)
        load_ref[best] = low + size

        def put(step, inner):
            slot = best * SLOTS + low + step
            tab_ref[slot] = spot + step
            tab_ref[SEG_AT + slot] = low
            tab_ref[LEN_AT + slot] = jnp.minimum(length - BLK * step, BLK)
            tab_ref[DEST_AT + spot + step] = slot
            return inner

        lax.fori_loop(0, size, put, 0)
        return carry

    lax.fori_loop(0, begin, assign, 0)


def deal_table(lengths):
    micro, per_dev = lengths.shape
    padded = jnp.pad(lengths, ((0, 8 - micro), (0, 128 - per_dev)))
    everyone = pl.pallas_call(
        lens_kernel,
        out_shape=jax.ShapeDtypeStruct((4, 8, 128), jnp.int32),
        in_specs=[VMEM],
        out_specs=VMEM,
        scratch_shapes=[pltpu.SemaphoreType.DMA((3,)), pltpu.SemaphoreType.DMA((3,))],
        compiler_params=pltpu.CompilerParams(collective_id=0, has_side_effects=True),
        name="lens_exchange",
    )(padded)
    return pl.pallas_call(
        partial(table_kernel, micro, per_dev),
        out_shape=jax.ShapeDtypeStruct((TABLE_SIZE,), jnp.int32),
        in_specs=[SMEM],
        out_specs=SMEM,
        scratch_shapes=[
            pltpu.SMEM((4 * micro * per_dev,), jnp.int32),
            pltpu.SMEM((8,), jnp.int32),
            pltpu.SMEM((4,), jnp.int32),
        ],
        name="deal_table",
    )(everyone)


def gather_kernel(
    outer, inner, splits, tab_ref, rows_ref, cots_ref, wa_ref, wb_ref, wc_ref,
    ga_ref, gb_ref, gc_ref, rows_out, cots_out,
    psend, precv, xsend, xrecv,
    z_send, z_recv, y_send, y_recv, c_send, c_recv, own_sem,
    p_send, p_recv, x_send, x_recv,
):
    rank = lax.axis_index("rep")
    spot = lax.axis_index("fsdp")
    core = rank % 2
    row, col = spot // inner, spot % inner
    count = outer * inner
    mate, across = core_of(rank), across_of(rank)
    pieces = [(wa_ref, ga_ref, start, width // 2) for start, width in splits]
    pieces.append((wb_ref, gb_ref, 0, wb_ref.shape[1] // 2))
    pieces.append((wc_ref, gc_ref, 0, None))
    halved = [number for number, piece in enumerate(pieces) if piece[3] is not None]

    barrier = pltpu.get_barrier_semaphore()
    neighbours = (
        (row + 1 < outer, {"fsdp": spot + inner}),
        (row > 0, {"fsdp": spot - inner}),
        (col + 1 < inner, {"fsdp": spot + 1}),
        (col > 0, {"fsdp": spot - 1}),
    )
    amount = jnp.int32(2)
    for there, device in neighbours:
        amount = amount + there.astype(jnp.int32)

        @pl.when(there)
        def _():
            pl.semaphore_signal(barrier, inc=1, device_id=device, device_id_type=MESH)

    for device in (mate, across):
        pl.semaphore_signal(barrier, inc=1, device_id={"rep": device}, device_id_type=MESH)
    pl.semaphore_wait(barrier, amount)

    def cut(ref, number):
        _, _, start, half = pieces[number]
        if half is None:
            return ref
        return ref.at[:, pl.ds(pl.multiple_of(start + core * half, 128), half)]

    def landed(number, shard):
        return cut(pieces[number][1].at[shard], number)

    late = []

    def send(there, src, dst, ssem, rsem, device):
        def describe():
            return pltpu.make_async_remote_copy(
                src_ref=src, dst_ref=dst, send_sem=ssem, recv_sem=rsem,
                device_id=device, device_id_type=MESH,
            )

        if there is None:
            describe().start()
            late.append((None, lambda: describe().wait_send()))
        else:
            @pl.when(there)
            def _():
                describe().start()

            late.append((there, lambda: describe().wait_send()))

    def arrive(number, shard, rsem):
        pltpu.make_async_remote_copy(
            src_ref=landed(number, shard), dst_ref=landed(number, shard),
            send_sem=own_sem.at[0], recv_sem=rsem,
            device_id={"rep": mate}, device_id_type=MESH,
        ).wait_recv()

    def both(first, second):
        return second if first is None else jnp.logical_and(first, second)

    def to_mate(there, number, shard):
        if number not in halved:
            return
        place = landed(number, shard)
        send(there, place, place, c_send.at[number, shard], c_recv.at[number, shard], {"rep": mate})

    def along_row(there, number, line, src):
        shard = line * inner + col
        place = landed(number, shard)
        src = place if src is None else src
        send(both(there, col + 1 < inner), src, place,
             y_send.at[0, 0, line, number], y_recv.at[0, 0, line, number], {"fsdp": spot + 1})
        send(both(there, col > 0), src, place,
             y_send.at[1, 0, line, number], y_recv.at[1, 0, line, number], {"fsdp": spot - 1})

    def from_row(there, number, line):
        for step in range(inner - 1):
            for way, source, onward, target in (
                (0, col - 1 - step, col + 1 < inner, spot + 1),
                (1, col + 1 + step, col > 0, spot - 1),
            ):
                here = jnp.logical_and(source >= 0, source < inner)
                here = both(there, here)
                shard = line * inner + source

                @pl.when(here)
                def _():
                    arrive(number, shard, y_recv.at[way, step, line, number])

                if step + 1 < inner - 1:
                    place = landed(number, shard)
                    send(both(here, onward), place, place,
                         y_send.at[way, step + 1, line, number],
                         y_recv.at[way, step + 1, line, number], {"fsdp": target})
                to_mate(here, number, shard)

    for number, piece in enumerate(pieces):
        src, place = cut(piece[0], number), landed(number, spot)
        send(row + 1 < outer, src, place, z_send.at[0, 0, number], z_recv.at[0, 0, number],
             {"fsdp": spot + inner})
        send(row > 0, src, place, z_send.at[1, 0, number], z_recv.at[1, 0, number],
             {"fsdp": spot - inner})
        along_row(None, number, row, src)
    own = [
        pltpu.make_async_copy(wa_ref, ga_ref.at[spot], own_sem.at[0]),
        pltpu.make_async_copy(wb_ref, gb_ref.at[spot], own_sem.at[1]),
        pltpu.make_async_copy(wc_ref, gc_ref.at[spot], own_sem.at[2]),
    ]
    for copy in own:
        copy.start()

    sources = (rows_ref, cots_ref)
    per_rank = rows_ref.shape[0]

    def picked(kind, target, slot):
        index = tab_ref[target * SLOTS + slot] - rank * per_rank
        mine = jnp.logical_and(index >= 0, index < per_rank)
        value = sources[kind][jnp.clip(index, 0, per_rank - 1)]
        return mine, value

    def mate_copy(kind, part):
        return pltpu.make_async_remote_copy(
            src_ref=psend.at[kind, part], dst_ref=precv.at[kind, part],
            send_sem=p_send.at[kind, part], recv_sem=p_recv.at[kind, part],
            device_id={"rep": mate}, device_id_type=MESH,
        )

    def across_copy(kind):
        return pltpu.make_async_remote_copy(
            src_ref=xsend.at[kind], dst_ref=xrecv.at[kind],
            send_sem=x_send.at[kind], recv_sem=x_recv.at[kind],
            device_id={"rep": across}, device_id_type=MESH,
        )

    for kind, part in ((0, 1), (1, 1), (0, 0), (1, 0)):
        target = mate if part == 0 else across_of(mate)

        def pack(slot, carry):
            mine, value = picked(kind, target, slot)
            psend[kind, part, slot] = jnp.where(mine, value, jnp.zeros_like(value))
            return carry

        lax.fori_loop(0, SLOTS, pack, 0)
        mate_copy(kind, part).start()
    for kind in range(2):
        mate_copy(kind, 1).wait_recv()

        def merge(slot, carry):
            mine, value = picked(kind, across, slot)
            xsend[kind, slot] = jnp.where(mine, value, precv[kind, 1, slot])
            return carry

        lax.fori_loop(0, SLOTS, merge, 0)
        across_copy(kind).start()

    def lines(step):
        return ((row - 1 - step >= 0, row - 1 - step, 0, row + 1 < outer, spot + inner),
                (row + 1 + step < outer, row + 1 + step, 1, row > 0, spot - inner))

    for step in range(outer - 1):
        for number in range(len(pieces)):
            for here, line, way, onward, target in lines(step):
                shard = line * inner + col

                @pl.when(here)
                def _():
                    arrive(number, shard, z_recv.at[way, step, number])

                if step + 1 < outer - 1:
                    place = landed(number, shard)
                    send(jnp.logical_and(here, onward), place, place,
                         z_send.at[way, step + 1, number], z_recv.at[way, step + 1, number],
                         {"fsdp": target})
                along_row(here, number, line, None)
                to_mate(here, number, shard)
        for number in range(len(pieces)):
            if step == 0:
                from_row(None, number, row)
            else:
                for here, line, *_ in lines(step - 1):
                    from_row(here, number, line)
    for number in range(len(pieces)):
        for here, line, *_ in lines(outer - 2):
            from_row(here, number, line)

    outs = (rows_out, cots_out)
    for kind in range(2):
        mate_copy(kind, 0).wait_recv()
        across_copy(kind).wait_recv()

        def finish(slot, carry):
            mine, value = picked(kind, rank, slot)
            outs[kind][slot] = jnp.where(mine, value, precv[kind, 0, slot] + xrecv[kind, slot])
            return carry

        lax.fori_loop(0, SLOTS, finish, 0)

    for shard in range(count):
        @pl.when(shard != spot)
        def _():
            for number in halved:
                other = pieces[number]
                view = other[1].at[shard].at[:, pl.ds(0, other[3])]
                pltpu.make_async_remote_copy(
                    src_ref=view, dst_ref=view, send_sem=own_sem.at[0],
                    recv_sem=c_recv.at[number, shard],
                    device_id={"rep": mate}, device_id_type=MESH,
                ).wait_recv()
    for there, finish_send in late:
        if there is None:
            finish_send()
        else:
            pl.when(there)(finish_send)
    for kind in range(2):
        for part in range(2):
            mate_copy(kind, part).wait_send()
        across_copy(kind).wait_send()
    for copy in own:
        copy.wait()


def gather_weights(count, splits, table, rows, cots, wa, wb, wc):
    outer, inner = grid_of(count)
    block = rows.shape[1:]
    kinds = len(splits) + 2
    dma = pltpu.SemaphoreType.DMA
    bf16 = jnp.bfloat16
    return pl.pallas_call(
        partial(gather_kernel, outer, inner, splits),
        out_shape=(
            jax.ShapeDtypeStruct((count,) + wa.shape, bf16),
            jax.ShapeDtypeStruct((count,) + wb.shape, bf16),
            jax.ShapeDtypeStruct((count,) + wc.shape, bf16),
            jax.ShapeDtypeStruct((SLOTS,) + block, bf16),
            jax.ShapeDtypeStruct((SLOTS,) + block, bf16),
        ),
        in_specs=[SMEM, VMEM, VMEM, VMEM, VMEM, VMEM],
        out_specs=(ANY, ANY, ANY, VMEM, VMEM),
        scratch_shapes=[
            pltpu.VMEM((2, 2, SLOTS) + block, bf16),
            pltpu.VMEM((2, 2, SLOTS) + block, bf16),
            pltpu.VMEM((2, SLOTS) + block, bf16),
            pltpu.VMEM((2, SLOTS) + block, bf16),
            dma((2, outer - 1, kinds)), dma((2, outer - 1, kinds)),
            dma((2, inner - 1, outer, kinds)), dma((2, inner - 1, outer, kinds)),
            dma((kinds, count)), dma((kinds, count)), dma((3,)),
            dma((2, 2)), dma((2, 2)), dma((2,)), dma((2,)),
        ],
        compiler_params=pltpu.CompilerParams(
            collective_id=1, has_side_effects=True, vmem_limit_bytes=VMEM_LIMIT
        ),
        name="gather_and_deal",
    )(table, rows, cots, wa, wb, wc)


def reduce_kernel(
    outer, inner, kinds, *refs
):
    grads, (y_ref, g_ref) = refs[:kinds], refs[kinds : kinds + 2]
    totals, (ry_ref, rg_ref) = refs[kinds + 2 : 2 * kinds + 2], refs[2 * kinds + 2 : 2 * kinds + 4]
    scratch = refs[2 * kinds + 4 :]
    mines, crecvs, yrecvs, zrecvs, xrecvs = (
        scratch[kinds * i : kinds * (i + 1)] for i in range(5)
    )
    (c_send, c_recv, m_sem, y_send, y_recv, z_send, z_recv, x_send, x_recv, f_send, f_recv,
     r_send, r_recv, q_sem) = scratch[5 * kinds :]
    rank = lax.axis_index("rep")
    spot = lax.axis_index("fsdp")
    core = rank % 2
    row, col = spot // inner, spot % inner
    mate, across = core_of(rank), across_of(rank)
    pieces = [(src, dst, 0, src.shape[3] // 2) for src, dst in zip(grads[:-1], totals)]
    pieces.append((grads[-1], totals[-1], 0, None))

    barrier = pltpu.get_barrier_semaphore()
    neighbours = (
        (row + 1 < outer, {"fsdp": spot + inner}),
        (row > 0, {"fsdp": spot - inner}),
        (col + 1 < inner, {"fsdp": spot + 1}),
        (col > 0, {"fsdp": spot - 1}),
    )
    amount = jnp.int32(2)
    for there, device in neighbours:
        amount = amount + there.astype(jnp.int32)

        @pl.when(there)
        def _():
            pl.semaphore_signal(barrier, inc=1, device_id=device, device_id_type=MESH)

    for device in (mate, across):
        pl.semaphore_signal(barrier, inc=1, device_id={"rep": device}, device_id_type=MESH)
    pl.semaphore_wait(barrier, amount)

    late = []

    def send(there, src, dst, ssem, rsem, device):
        def describe():
            return pltpu.make_async_remote_copy(
                src_ref=src, dst_ref=dst, send_sem=ssem, recv_sem=rsem,
                device_id=device, device_id_type=MESH,
            )

        if there is None:
            describe().start()
            late.append((None, lambda: describe().wait_send()))
        else:
            @pl.when(there)
            def _():
                describe().start()

            late.append((there, lambda: describe().wait_send()))

    def arrive(place, rsem):
        pltpu.make_async_remote_copy(
            src_ref=place, dst_ref=place, send_sem=q_sem.at[0], recv_sem=rsem,
            device_id={"rep": mate}, device_id_type=MESH,
        ).wait_recv()

    def columns(ref, number, which):
        _, _, start, half = pieces[number]
        if half is None:
            return ref
        cols = pl.ds(pl.multiple_of(start + which * half, 128), half)
        return ref.at[:, :, :, cols] if len(ref.shape) == 4 else ref.at[:, cols]

    order = list(range(kinds))
    loads = []
    for number in order:
        src = columns(pieces[number][0], number, 1 - core)
        send(None, src, crecvs[number], c_send.at[number], c_recv.at[number], {"rep": mate})
        load = pltpu.make_async_copy(
            columns(pieces[number][0], number, core), mines[number], m_sem.at[number]
        )
        load.start()
        loads.append(load)

    for kind, (src, dst) in enumerate(((y_ref, ry_ref), (g_ref, rg_ref))):
        send(None, src, dst.at[rank], r_send.at[kind, 0], r_recv.at[kind, 0], {"rep": across})
        send(None, src, dst.at[rank], r_send.at[kind, 1], r_recv.at[kind, 1], {"rep": mate})
        pltpu.make_async_copy(src, dst.at[rank], q_sem.at[kind + 1]).start()

    def slot_of(way, size, place, dest):
        if size == 2:
            return 0
        return dest - place if way == 0 else size - place + dest

    def line_sum(number, size, place, stride, buffer, view, ssem, rsem):
        for far in range(size - 1, 0, -1):
            for way in range(2):
                dest = far if way == 0 else size - 1 - far
                step = 1 if way == 0 else -1
                passes = place < dest if way == 0 else place > dest
                first = place == 0 if way == 0 else place == size - 1
                mine = view(dest)
                got = slot_of(way, size, place, dest)

                @pl.when(jnp.logical_and(passes, jnp.logical_not(first)))
                def _():
                    arrive(buffer.at[got], rsem.at[got, number])
                    mine[...] = mine[...] + buffer[got]

                put = slot_of(way, size, place + step, dest)
                send(passes, mine, buffer.at[put], ssem.at[way, dest, number], rsem.at[put, number],
                     {"fsdp": spot + step * stride})
        for way in range(2):
            has = place > 0 if way == 0 else place < size - 1
            got = slot_of(way, size, place, place)
            mine = view(place)

            @pl.when(has)
            def _():
                arrive(buffer.at[got], rsem.at[got, number])
                mine[...] = mine[...] + buffer[got]

    for number in order:
        loads[number].wait()
        arrive(crecvs[number], c_recv.at[number])
        mine, other = mines[number], crecvs[number]

        def add(index, carry):
            mine[index // inner, index % inner] = (
                mine[index // inner, index % inner] + other[index // inner, index % inner]
            )
            return carry

        lax.fori_loop(0, outer * inner, add, 0)
        if inner == 2:
            send(None, mine.at[:, 1 - col], yrecvs[number].at[0], y_send.at[0, 0, number],
                 y_recv.at[0, number], {"fsdp": spot + 1 - 2 * col})
    for kind, dst in enumerate((ry_ref, rg_ref)):
        place = dst.at[across]
        arrive(place, r_recv.at[kind, 0])
        send(None, place, place, r_send.at[kind, 2], r_recv.at[kind, 2], {"rep": mate})
    for number in order:
        mine = mines[number]
        if inner == 2:
            arrive(yrecvs[number].at[0], y_recv.at[0, number])
            buffer = yrecvs[number]

            def add(index, carry):
                mine[index, col] = mine[index, col] + buffer[0, index]
                return carry

            lax.fori_loop(0, outer, add, 0)
        else:
            line_sum(number, inner, col, 1, yrecvs[number], lambda dest: mine.at[:, dest],
                     y_send, y_recv)
        line_sum(number, outer, row, inner, zrecvs[number], lambda dest: mine.at[dest, col],
                 z_send, z_recv)
        send(None, mine.at[row, col], xrecvs[number], x_send.at[number], x_recv.at[number],
             {"rep": across})
    for number in order:
        arrive(xrecvs[number], x_recv.at[number])
        total = mines[number][row, col].astype(jnp.float32) + xrecvs[number][...].astype(jnp.float32)
        out, half = pieces[number][1], pieces[number][3]
        place = columns(out, number, core)
        place[...] = total
        if half is not None:
            send(None, place, place, f_send.at[number], f_recv.at[number], {"rep": mate})
    for number in order:
        if pieces[number][3] is not None:
            arrive(columns(pieces[number][1], number, 1 - core), f_recv.at[number])
    for kind, dst in enumerate((ry_ref, rg_ref)):
        arrive(dst.at[mate], r_recv.at[kind, 1])
        arrive(dst.at[across_of(mate)], r_recv.at[kind, 2])
        src = y_ref if kind == 0 else g_ref
        pltpu.make_async_copy(src, dst.at[rank], q_sem.at[kind + 1]).wait()
    for there, finish_send in late:
        if there is None:
            finish_send()
        else:
            pl.when(there)(finish_send)


def reduce_grads(count, grads, y_rows, g_rows):
    outer, inner = grid_of(count)
    kinds = len(grads)
    shapes = [(grad.shape[1], grad.shape[2] // 2, grad.dtype) for grad in grads[:-1]]
    shapes.append(grads[-1].shape[1:] + (grads[-1].dtype,))
    dma = pltpu.SemaphoreType.DMA
    y_slots = 1 if inner == 2 else inner + 1
    z_slots = 1 if outer == 2 else outer + 1
    scratch = []
    for lead in ((outer, inner), (outer, inner), (y_slots, outer), (z_slots,), ()):
        scratch += [pltpu.VMEM(lead + (a, b), dtype) for a, b, dtype in shapes]
    scratch += [
        dma((kinds,)), dma((kinds,)), dma((kinds,)),
        dma((2, inner, kinds)), dma((y_slots, kinds)),
        dma((2, outer, kinds)), dma((z_slots, kinds)),
        dma((kinds,)), dma((kinds,)), dma((kinds,)), dma((kinds,)),
        dma((2, 3)), dma((2, 3)), dma((3,)),
    ]
    return pl.pallas_call(
        partial(reduce_kernel, outer, inner, kinds),
        out_shape=tuple(jax.ShapeDtypeStruct(grad.shape[1:], jnp.float32) for grad in grads) + (
            jax.ShapeDtypeStruct((4,) + y_rows.shape, y_rows.dtype),
            jax.ShapeDtypeStruct((4,) + g_rows.shape, g_rows.dtype),
        ),
        in_specs=[ANY] * (kinds + 2),
        out_specs=(VMEM,) * kinds + (ANY, ANY),
        scratch_shapes=scratch,
        compiler_params=pltpu.CompilerParams(
            collective_id=2, has_side_effects=True, vmem_limit_bytes=VMEM_LIMIT
        ),
        name="reduce_and_return",
    )(*(grad.reshape((outer, inner) + grad.shape[1:]) for grad in grads), y_rows, g_rows)


def home_kernel(tab_ref, ry_ref, rg_ref, y_ref, g_ref):
    base = lax.axis_index("rep") * y_ref.shape[0]

    def fetch(block, carry):
        index = tab_ref[DEST_AT + base + block] if len(tab_ref.shape) == 1 else tab_ref[48, base + block]
        safe = jnp.maximum(index, 0)
        for src, dst in ((ry_ref, y_ref), (rg_ref, g_ref)):
            value = src[safe // SLOTS, safe % SLOTS]
            dst[block] = jnp.where(index >= 0, value, jnp.zeros_like(value))
        return carry

    lax.fori_loop(0, y_ref.shape[0], fetch, 0)


def bring_home(table, ry, rg, blocks):
    shape = jax.ShapeDtypeStruct((blocks,) + ry.shape[2:], ry.dtype)
    return pl.pallas_call(
        home_kernel,
        out_shape=(shape, shape),
        in_specs=[SMEM, VMEM, VMEM],
        out_specs=(VMEM, VMEM),
        compiler_params=pltpu.CompilerParams(vmem_limit_bytes=VMEM_LIMIT),
        name="place_rows",
    )(table, ry, rg)


D = H * DH
ROWS = SLOTS * BLK
SIDES = SLOTS * (BLK // GBLK)
SIDE_ROWS = 48
ALL_ROWS = ROWS + SIDE_ROWS
QT = 128
WIN = 384
TILES = ROWS // QT
QUAD = 256
FF_TILE = 256
GELU_C = 0.7978845608028654
GELU_A = 0.044715
F32, BF16 = jnp.float32, jnp.bfloat16


def mm(left, right):
    return lax.dot_general(left, right, (((1,), (0,)), ((), ())), preferred_element_type=F32)


def mm_cols(left, right):
    return lax.dot_general(left, right, (((1,), (1,)), ((), ())), preferred_element_type=F32)


def mm_rows(left, right):
    return lax.dot_general(left, right, (((0,), (0,)), ((), ())), preferred_element_type=F32)


def iota(shape, axis):
    return lax.broadcasted_iota(jnp.int32, shape, axis)


def pick_by(index, values, other):
    out = jnp.full(index.shape, other, jnp.int32)
    for number, value in enumerate(values):
        out = jnp.where(index == number, value, out)
    return out


def block_at(tab_ref, slot):
    return lax.rem(tab_ref[slot, 0], 128) - 1


def seg_at(tab_ref, slot):
    if len(tab_ref.shape) == 1:
        return tab_ref[SEG_AT + slot]
    return lax.div(tab_ref[slot, 0], 16384) - 1


def len_at(tab_ref, slot):
    if len(tab_ref.shape) == 1:
        return tab_ref[LEN_AT + slot]
    return lax.rem(lax.div(tab_ref[slot, 0], 128), 128)


def slot_info(tab_ref, rank):
    seg = [seg_at(tab_ref, rank * SLOTS + slot) for slot in range(SLOTS)]
    length = [len_at(tab_ref, rank * SLOTS + slot) for slot in range(SLOTS)]
    return seg, length


def valid_column(tab_ref, rank):
    _, length = slot_info(tab_ref, rank)
    row = iota((ROWS, 1), 0)
    return ((row % BLK) < pick_by(row // BLK, length, 0)).astype(F32)


def pooling(tab_ref, rank):
    _, length = slot_info(tab_ref, rank)
    row = iota((1, ROWS), 1)
    block = jnp.where((row % BLK) < pick_by(row // BLK, length, 0), row // GBLK, -1)
    return jnp.where(iota((SIDE_ROWS, ROWS), 0) == block, 1.0, 0.0).astype(BF16)


def key_segments(tab_ref, rank, first_block, index):
    blocks = WIN // BLK
    base = rank * SLOTS + first_block
    seg = [seg_at(tab_ref, base + step) for step in range(blocks)]
    length = [len_at(tab_ref, base + step) for step in range(blocks)]
    alive = (index % BLK) < pick_by(index // BLK, length, 0)
    return jnp.where(alive, pick_by(index // BLK, seg, -2), -2)


def side_segments(tab_ref, rank, index):
    seg, length = slot_info(tab_ref, rank)
    per = BLK // GBLK
    alive = (index % per) * GBLK < pick_by(index // per, length, 0)
    return jnp.where(alive, pick_by(index // per, seg, -2), -2)


def tile_bias(tab_ref, rank, tile, first_row, keys_axis):
    qs, ks, gs = ((QT, 1), (1, WIN), (1, SIDE_ROWS)) if keys_axis == 1 else ((1, QT), (WIN, 1), (SIDE_ROWS, 1))
    q_index = iota(qs, 1 - keys_axis)
    k_index = iota(ks, keys_axis)
    g_index = iota(gs, keys_axis)
    base = rank * SLOTS + tile * (QT // BLK)
    q_seg = pick_by(q_index // BLK, [seg_at(tab_ref, base + step) for step in range(QT // BLK)], -1)
    k_seg = key_segments(tab_ref, rank, first_row // BLK, k_index)
    g_seg = side_segments(tab_ref, rank, g_index)
    gap = (q_index + tile * QT) - (k_index + first_row)
    local = (jnp.abs(gap) <= RADIUS) & (q_seg == k_seg)
    return jnp.where(local, 0.0, MASKED_SCORE), jnp.where(q_seg == g_seg, 0.0, MASKED_SCORE)


def window_start(tile):
    return pl.multiple_of(jnp.clip(tile - 1, 0, TILES - WIN // QT) * QT, QT)


def head_stack(rows):
    lane = iota(rows.shape, 1) // DH
    zero = jnp.zeros_like(rows)
    return jnp.concatenate([jnp.where(lane == head, rows, zero) for head in range(QUAD // DH)], axis=0)


def head_merge(stacked):
    lane = iota((QT, QUAD), 1) // DH
    out = stacked[:QT]
    for head in range(1, QUAD // DH):
        out = jnp.where(lane == head, stacked[head * QT : (head + 1) * QT], out)
    return out


def gains_of(gc_ref):
    count = gc_ref.shape[0]
    part = D // count
    lane, column = iota((128, D), 0), iota((128, D), 1)
    total = None
    for shard in range(count):
        pick = jnp.where((column == lane + shard * part) & (lane < part), 1.0, 0.0).astype(BF16)
        term = mm(gc_ref[shard], pick)
        total = term if total is None else total + term
    return total


def three_way(value):
    high = value.astype(BF16)
    rest = value - high.astype(F32)
    middle = rest.astype(BF16)
    return high, middle, (rest - middle.astype(F32)).astype(BF16)


def spread_gain_grads(value, dc_ref):
    count = dc_ref.shape[0] if len(dc_ref.shape) == 3 else dc_ref.shape[0] * dc_ref.shape[1]
    part = D // count
    column, lane = iota((D, 128), 0), iota((D, 128), 1)
    parts = three_way(value)
    for shard in range(count):
        pick = jnp.where((column == lane + shard * part) & (lane < part), 1.0, 0.0).astype(BF16)
        place = dc_ref.at[shard] if len(dc_ref.shape) == 3 else dc_ref.at[shard // dc_ref.shape[1], shard % dc_ref.shape[1]]
        place[...] = mm(parts[0], pick) + mm(parts[1], pick) + mm(parts[2], pick)


def mean_square(value):
    return jnp.mean(value * value, axis=-1, keepdims=True)


def forward_norm(tab_ref, rank, x_ref, gains, n_ref):
    for tile in range(TILES):
        rows = pl.ds(tile * QT, QT)
        value = x_ref[rows, :].astype(F32)
        n_ref[rows, :] = (value * lax.rsqrt(mean_square(value) + EPSILON) * gains[0:1]).astype(BF16)
    side = mm(pooling(tab_ref, rank), n_ref[:ROWS, :])
    n_ref[ROWS:, :] = (side * lax.rsqrt(mean_square(side) + EPSILON) * gains[1:2]).astype(BF16)


def forward_project(n_ref, w_ref, qkv_ref):
    def step(tile, carry):
        cols = pl.ds(pl.multiple_of(tile * QUAD, QUAD), QUAD)
        qkv_ref[:, cols] = mm(n_ref[...], w_ref[:, cols]).astype(BF16)
        return carry

    lax.fori_loop(0, 3 * D // QUAD, step, 0)


def forward_attention(tab_ref, rank, qkv_ref, att_ref, lse_ref, begin, end):
    def step(tile, carry):
        first = window_start(tile)
        bias, side_bias = tile_bias(tab_ref, rank, tile, first, 1)
        rows = pl.ds(pl.multiple_of(tile * QT, QT), QT)
        window = pl.ds(first, WIN)
        lse = jnp.zeros((QT, 128), F32)
        lane = iota((QT, 128), 1)
        for quad in range(D // QUAD):
            low = quad * QUAD
            query = head_stack(qkv_ref[rows, low : low + QUAD])
            scores = mm_cols(query, qkv_ref[window, D + low : D + low + QUAD])
            side_scores = mm_cols(query, qkv_ref[ROWS:, D + low : D + low + QUAD])
            local, sides, scale = [], [], []
            for head in range(QUAD // DH):
                part = slice(head * QT, (head + 1) * QT)
                one = scores[part] + bias
                two = side_scores[part] + side_bias
                peak = jnp.maximum(
                    jnp.max(one, axis=-1, keepdims=True), jnp.max(two, axis=-1, keepdims=True)
                )
                one, two = jnp.exp(one - peak), jnp.exp(two - peak)
                total = jnp.sum(one, axis=-1, keepdims=True) + jnp.sum(two, axis=-1, keepdims=True)
                local.append(one.astype(BF16))
                sides.append(two.astype(BF16))
                scale.append(1.0 / total)
                lse = jnp.where(lane == quad * (QUAD // DH) + head, peak + jnp.log(total), lse)
            mixed = mm(jnp.concatenate(local, axis=0), qkv_ref[window, 2 * D + low : 2 * D + low + QUAD])
            mixed = mixed + mm(
                jnp.concatenate(sides, axis=0), qkv_ref[ROWS:, 2 * D + low : 2 * D + low + QUAD]
            )
            mixed = mixed * jnp.concatenate(scale, axis=0)
            att_ref[rows, low : low + QUAD] = head_merge(mixed).astype(BF16)
        lse_ref[tile] = jnp.transpose(lse)[:16]
        return carry

    lax.fori_loop(begin, end, step, 0)


def feed_forward(tab_ref, rank, x_ref, cot_ref, att_ref, gains, w_ref, wb_ref,
                 y_ref, gh_ref, ga_ref, dg_ref, du_ref, db_ref, do_ref,
                 h1_ref, nt_ref, ntt_ref, gres_ref, h2_ref, gg_ref, gu_ref, gn_ref):
    hidden = wb_ref.shape[0]
    gate_at = w_ref.shape[1] - 2 * hidden
    out_at = gate_at - D
    valid = valid_column(tab_ref, rank)
    gain = gains[2:3]
    for tile in range(TILES):
        rows = pl.ds(tile * QT, QT)
        value = x_ref[rows, :].astype(F32) + mm(att_ref[rows, :], w_ref[:, out_at:gate_at])
        h1_ref[rows, :] = value
        normed = (value * lax.rsqrt(mean_square(value) + EPSILON) * gain).astype(BF16)
        nt_ref[rows, :] = normed
        ntt_ref[:, tile * QT : (tile + 1) * QT] = jnp.transpose(normed)
        gres_ref[rows, :] = (cot_ref[rows, :].astype(F32) * valid[tile * QT : (tile + 1) * QT]).astype(BF16)

    def inward(tile, carry):
        at = pl.multiple_of(tile * FF_TILE, FF_TILE)
        cols = pl.ds(at, FF_TILE)
        gate = mm(nt_ref[...], w_ref[:, pl.ds(gate_at + at, FF_TILE)])
        up = mm(nt_ref[...], w_ref[:, pl.ds(gate_at + hidden + at, FF_TILE)])
        back = mm_cols(gres_ref[...], wb_ref[cols, :])
        square = gate * gate
        bend = jnp.tanh(GELU_C * (gate * (1.0 + GELU_A * square)))
        half = 0.5 * (1.0 + bend)
        act = gate * half
        slope = half + (0.5 * GELU_C) * gate * (1.0 - bend * bend) * (1.0 + (3.0 * GELU_A) * square)
        h2_ref[:, cols] = (act * up).astype(BF16)
        gg_ref[:, cols] = (back * up * slope).astype(BF16)
        gu_ref[:, cols] = (back * act).astype(BF16)
        return carry

    lax.fori_loop(0, hidden // FF_TILE, inward, 0)

    def outward(tile, carry):
        cols = pl.ds(pl.multiple_of(tile * QUAD, QUAD), QUAD)
        value = h1_ref[:, cols] + mm(h2_ref[...], wb_ref[:, cols])
        y_ref[:, cols] = (value * valid).astype(BF16)
        gn_ref[:, cols] = mm_cols(gg_ref[...], w_ref[cols, gate_at : gate_at + hidden]) + mm_cols(
            gu_ref[...], w_ref[cols, gate_at + hidden :]
        )
        return carry

    lax.fori_loop(0, D // QUAD, outward, 0)

    def weights(tile, carry):
        at = pl.multiple_of(tile * FF_TILE, FF_TILE)
        cols = pl.ds(at, FF_TILE)
        dg_ref[:, cols] = mm(ntt_ref[...], gg_ref[:, cols]).astype(BF16)
        du_ref[:, cols] = mm(ntt_ref[...], gu_ref[:, cols]).astype(BF16)
        db_ref[cols, :] = mm_rows(h2_ref[:, cols], gres_ref[...]).astype(BF16)
        return carry

    lax.fori_loop(0, hidden // FF_TILE, weights, 0)

    gain_grad = jnp.zeros((1, D), F32)
    for tile in range(TILES):
        rows = pl.ds(tile * QT, QT)
        value, grad = h1_ref[rows, :], gn_ref[rows, :]
        root = lax.rsqrt(mean_square(value) + EPSILON)
        unit = value * root
        gain_grad = gain_grad + jnp.sum(grad * unit, axis=0, keepdims=True)
        grad = grad * gain
        grad = gres_ref[rows, :].astype(F32) + root * (
            grad - unit * jnp.mean(grad * unit, axis=-1, keepdims=True)
        )
        gh_ref[rows, :] = grad
        low = grad.astype(BF16)
        nt_ref[rows, :] = low
        ga_ref[rows, :] = mm_cols(low, w_ref[:, out_at:gate_at]).astype(BF16)

    def out_weight(tile, carry):
        cols = pl.ds(pl.multiple_of(tile * QUAD, QUAD), QUAD)
        do_ref[cols, :] = mm_rows(att_ref[:, cols], nt_ref[...]).astype(BF16)
        return carry

    lax.fori_loop(0, D // QUAD, out_weight, 0)
    return gain_grad


def backward_attention_start(dk_ref, dv_ref):
    dk_ref[...] = jnp.zeros_like(dk_ref)
    dv_ref[...] = jnp.zeros_like(dv_ref)


def backward_attention_quad(tab_ref, rank, qkv_ref, att_ref, ga_ref, lse_ref, dqkv_ref, dk_ref, dv_ref, quad):
    heads = QUAD // DH
    marks = jnp.where(iota((16, QUAD), 1) // DH == iota((16, QUAD), 0), 1.0, 0.0).astype(BF16)
    low = quad * QUAD
    cols = slice(low, low + QUAD)

    def step(tile, carry):
        first = window_start(tile)
        bias, side_bias = tile_bias(tab_ref, rank, tile, first, 0)
        bias = jnp.concatenate([bias, side_bias], axis=0)
        rows = pl.ds(pl.multiple_of(tile * QT, QT), QT)
        window = pl.ds(first, WIN)
        lse = lse_ref[tile]
        product = ga_ref[rows, cols].astype(F32) * att_ref[rows, cols].astype(F32)
        high = product.astype(BF16)
        rest = (product - high.astype(F32)).astype(BF16)
        centre = mm_cols(marks, high) + mm_cols(marks, rest)
        query = head_stack(qkv_ref[rows, cols])
        grad = head_stack(ga_ref[rows, cols])
        keys = jnp.concatenate(
            [qkv_ref[window, D + low : D + low + QUAD], qkv_ref[ROWS:, D + low : D + low + QUAD]], axis=0
        )
        values = jnp.concatenate(
            [qkv_ref[window, 2 * D + low : 2 * D + low + QUAD],
             qkv_ref[ROWS:, 2 * D + low : 2 * D + low + QUAD]], axis=0
        )
        scores = mm_cols(keys, query)
        slopes = mm_cols(values, grad)
        probs, grads = [], []
        for head in range(heads):
            part = slice(head * QT, (head + 1) * QT)
            number = quad * heads + head
            prob = jnp.exp(scores[:, part] + bias - lse[number : number + 1])
            probs.append(prob.astype(BF16))
            grads.append((prob * (slopes[:, part] - centre[head : head + 1])).astype(BF16))
        probs = jnp.concatenate(probs, axis=1)
        grads = jnp.concatenate(grads, axis=1)
        dkey = mm(grads, query)
        dvalue = mm(probs, grad)
        dk_ref[window, cols] = dk_ref[window, cols] + dkey[:WIN]
        dk_ref[ROWS:, cols] = dk_ref[ROWS:, cols] + dkey[WIN:]
        dv_ref[window, cols] = dv_ref[window, cols] + dvalue[:WIN]
        dv_ref[ROWS:, cols] = dv_ref[ROWS:, cols] + dvalue[WIN:]
        dqkv_ref[rows, cols] = head_merge(mm_rows(grads, keys)).astype(BF16)
        return carry

    lax.fori_loop(0, TILES, step, 0)
    dqkv_ref[ROWS:, cols] = jnp.zeros((SIDE_ROWS, QUAD), BF16)
    dqkv_ref[:, D + low : D + low + QUAD] = dk_ref[:, cols].astype(BF16)
    dqkv_ref[:, 2 * D + low : 2 * D + low + QUAD] = dv_ref[:, cols].astype(BF16)


def weight_grads(n_ref, dqkv_ref, refs):
    for number, ref in enumerate(refs):
        def weights(tile, carry):
            at = pl.multiple_of(tile * QUAD, QUAD)
            value = mm_rows(n_ref[...], dqkv_ref[:, pl.ds(number * D + at, QUAD)]).astype(BF16)
            if len(ref.shape) == 4:
                ref[:, :, :, pl.ds(at, QUAD)] = value.reshape(ref.shape[:3] + (QUAD,))
            else:
                ref[:, pl.ds(at, QUAD)] = value
            return carry

        lax.fori_loop(0, D // QUAD, weights, 0)


def backward_project(tab_ref, rank, x_ref, gh_ref, gains, n_ref, dqkv_ref, w_ref, gn_ref, g_ref):
    def step(tile, carry):
        cols = pl.ds(pl.multiple_of(tile * QUAD, QUAD), QUAD)
        gn_ref[:, cols] = mm_cols(dqkv_ref[...], w_ref[cols, : 3 * D])
        return carry

    lax.fori_loop(0, D // QUAD, step, 0)
    pool = pooling(tab_ref, rank)
    side = mm(pool, n_ref[:ROWS, :])
    root = lax.rsqrt(mean_square(side) + EPSILON)
    unit = side * root
    grad = gn_ref[ROWS:, :]
    side_gain = jnp.sum(grad * unit, axis=0, keepdims=True)
    grad = grad * gains[1:2]
    grad = root * (grad - unit * jnp.mean(grad * unit, axis=-1, keepdims=True))
    parts = three_way(grad)
    gain_grad = jnp.zeros((1, D), F32)
    for tile in range(TILES):
        rows = pl.ds(tile * QT, QT)
        spread = pool[:, tile * QT : (tile + 1) * QT]
        total = gn_ref[rows, :] + mm_rows(spread, parts[0]) + mm_rows(spread, parts[1])
        value = x_ref[rows, :].astype(F32)
        root = lax.rsqrt(mean_square(value) + EPSILON)
        unit = value * root
        gain_grad = gain_grad + jnp.sum(total * unit, axis=0, keepdims=True)
        total = total * gains[0:1]
        value = (
            gh_ref[rows, :] + root * (total - unit * jnp.mean(total * unit, axis=-1, keepdims=True))
        ).astype(BF16)
        if len(g_ref.shape) == 3:
            g_ref[pl.ds(tile * (QT // BLK), QT // BLK)] = value.reshape(QT // BLK, BLK, D)
        else:
            g_ref[rows, :] = value
    return gain_grad, side_gain


def first_kernel(tab_ref, x_ref, gc_ref, w_ref, n_ref, qkv_ref, att_ref, lse_ref):
    rank = lax.axis_index("rep")
    gains = gains_of(gc_ref)
    forward_norm(tab_ref, rank, x_ref, gains, n_ref)
    forward_project(n_ref, w_ref, qkv_ref)
    forward_attention(tab_ref, rank, qkv_ref, att_ref, lse_ref, 0, TILES)


def second_kernel(tab_ref, x_ref, cot_ref, att_ref, gc_ref, w_ref, wb_ref,
                  y_ref, gh_ref, ga_ref, dg_ref, du_ref, db_ref, do_ref, gain_ref, *scratch):
    rank = lax.axis_index("rep")
    gain_ref[...] = feed_forward(tab_ref, rank, x_ref, cot_ref, att_ref, gains_of(gc_ref), w_ref, wb_ref,
                                 y_ref, gh_ref, ga_ref, dg_ref, du_ref, db_ref, do_ref, *scratch)


def third_kernel(tab_ref, x_ref, gh_ref, ga_ref, att_ref, lse_ref, n_ref, qkv_ref, gain_ref, gc_ref, w_ref,
                 g_ref, dw_ref, dc_ref, dqkv_ref, dk_ref, dv_ref, gn_ref):
    rank = lax.axis_index("rep")
    gains = gains_of(gc_ref)
    backward_attention_start(dk_ref, dv_ref)
    for quad in range(D // QUAD):
        backward_attention_quad(tab_ref, rank, qkv_ref, att_ref, ga_ref, lse_ref, dqkv_ref, dk_ref, dv_ref, quad)
    weight_grads(n_ref, dqkv_ref, [dw_ref.at[:, i * D : (i + 1) * D] for i in range(3)])
    one, side = backward_project(tab_ref, rank, x_ref, gh_ref, gains, n_ref, dqkv_ref, w_ref, gn_ref, g_ref)
    grads = jnp.concatenate([one, side, gain_ref[...], jnp.zeros((5, D), F32)], axis=0)
    spread_gain_grads(grads, dc_ref)


def attend(tab, x, gc, w):
    shape = jax.ShapeDtypeStruct
    return pl.pallas_call(
        first_kernel,
        out_shape=(shape((ALL_ROWS, D), BF16), shape((ALL_ROWS, 3 * D), BF16), shape((ROWS, D), BF16),
                   shape((TILES, 16, QT), F32)),
        in_specs=[SMEM, VMEM, VMEM, pl.BlockSpec((D, 3 * D), lambda step: (0, 0))],
        grid=(1,),
        out_specs=(VMEM,) * 4,
        compiler_params=pltpu.CompilerParams(vmem_limit_bytes=VMEM_LIMIT),
        name="attend",
    )(tab, x, gc, w)


def feed(tab, x, cot, att, gc, w, wb):
    hidden = wb.shape[0]
    shape = jax.ShapeDtypeStruct
    return pl.pallas_call(
        second_kernel,
        out_shape=(shape((ROWS, D), BF16), shape((ROWS, D), F32), shape((ROWS, D), BF16),
                   shape((D, hidden), BF16), shape((D, hidden), BF16), shape((hidden, D), BF16), shape((D, D), BF16),
                   shape((1, D), F32)),
        in_specs=[SMEM] + [VMEM] * 6,
        out_specs=(VMEM,) * 8,
        scratch_shapes=[pltpu.VMEM((ROWS, D), F32), pltpu.VMEM((ROWS, D), BF16), pltpu.VMEM((D, ROWS), BF16),
                        pltpu.VMEM((ROWS, D), BF16), pltpu.VMEM((ROWS, hidden), BF16),
                        pltpu.VMEM((ROWS, hidden), BF16), pltpu.VMEM((ROWS, hidden), BF16),
                        pltpu.VMEM((ROWS, D), F32)],
        compiler_params=pltpu.CompilerParams(vmem_limit_bytes=VMEM_LIMIT),
        name="feed_forward",
    )(tab, x, cot, att, gc, w, wb)


def backward_layer(tab, x, gh, ga, att, lse, n, qkv, gain, gc, w):
    shape = jax.ShapeDtypeStruct
    return pl.pallas_call(
        third_kernel,
        out_shape=(shape((ROWS, D), BF16), shape((D, 3 * D), BF16), shape((gc.shape[0], 8, 128), F32)),
        in_specs=[SMEM] + [VMEM] * 9 + [pl.BlockSpec((D, 3 * D), lambda step: (0, 0))],
        grid=(1,),
        out_specs=(VMEM,) * 3,
        scratch_shapes=[pltpu.VMEM((ALL_ROWS, 3 * D), BF16), pltpu.VMEM((ALL_ROWS, D), F32),
                        pltpu.VMEM((ALL_ROWS, D), F32), pltpu.VMEM((ALL_ROWS, D), F32)],
        compiler_params=pltpu.CompilerParams(vmem_limit_bytes=VMEM_LIMIT),
        name="attend_back",
    )(tab, x, gh, ga, att, lse, n, qkv, gain, gc, w)


class Links:
    def __init__(self, outer, inner):
        self.outer, self.inner = outer, inner
        self.rank, self.spot = lax.axis_index("rep"), lax.axis_index("fsdp")
        self.core = self.rank % 2
        self.row, self.col = self.spot // inner, self.spot % inner
        self.mate, self.across = core_of(self.rank), across_of(self.rank)
        self.late = []

    def greet(self, everyone=False):
        barrier = pltpu.get_barrier_semaphore()
        neighbours = (
            (self.row + 1 < self.outer, {"fsdp": self.spot + self.inner}),
            (self.row > 0, {"fsdp": self.spot - self.inner}),
            (self.col + 1 < self.inner, {"fsdp": self.spot + 1}),
            (self.col > 0, {"fsdp": self.spot - 1}),
        )
        group = (self.mate, self.across) + ((across_of(self.mate),) if everyone else ())
        amount = jnp.int32(len(group))
        for there, device in neighbours:
            amount = amount + there.astype(jnp.int32)

            @pl.when(there)
            def _():
                pl.semaphore_signal(barrier, inc=1, device_id=device, device_id_type=MESH)

        for device in group:
            pl.semaphore_signal(barrier, inc=1, device_id={"rep": device}, device_id_type=MESH)
        pl.semaphore_wait(barrier, amount)

    def send(self, there, src, dst, ssem, rsem, device):
        def describe():
            return pltpu.make_async_remote_copy(
                src_ref=src, dst_ref=dst, send_sem=ssem, recv_sem=rsem,
                device_id=device, device_id_type=MESH,
            )

        if there is None:
            describe().start()
        else:
            @pl.when(there)
            def _():
                describe().start()

        self.late.append((there, lambda: describe().wait_send()))

    def arrive(self, place, rsem, spare):
        pltpu.make_async_remote_copy(
            src_ref=place, dst_ref=place, send_sem=spare, recv_sem=rsem,
            device_id={"rep": self.mate}, device_id_type=MESH,
        ).wait_recv()

    def drain(self):
        for there, finish in self.late:
            if there is None:
                finish()
            else:
                pl.when(there)(finish)


def halves(ref, which):
    half = ref.shape[-1] // 2
    cols = pl.ds(pl.multiple_of(which * half, 128), half)
    return ref.at[:, :, :, cols] if len(ref.shape) == 4 else ref.at[:, cols]


class Reduction:
    def __init__(self, links, source, total, mine, crecv, yrecv, zrecv, xrecv, stage, sems, number):
        self.links, self.source, self.total, self.mine, self.stage = links, source, total, mine, stage
        self.crecv, self.yrecv, self.zrecv, self.xrecv = crecv, yrecv, zrecv, xrecv
        self.sems, self.number = sems, number
        self.whole = total.shape[-1] % 256 != 0
        self.load = None

    def sem(self, name, *index):
        return self.sems[name].at[index + (self.number,)]

    def begin(self):
        links = self.links
        other = self.source if self.whole else halves(self.source, 1 - links.core)
        links.send(None, other, self.crecv, self.sem("c_send"), self.sem("c_recv"), {"rep": links.mate})
        if self.mine is None:
            self.mine = self.source if self.whole else halves(self.source, links.core)
        else:
            own = self.source if self.whole else halves(self.source, links.core)
            self.load = pltpu.make_async_copy(own, self.mine, self.sem("m_sem"))
            self.load.start()

    def pair(self):
        links = self.links
        if self.load is not None:
            self.load.wait()
        links.arrive(self.crecv, self.sem("c_recv"), self.sems["spare"].at[0])
        inner = links.inner

        def add(index, carry):
            row, col = index // inner, index % inner
            self.mine[row, col] = self.mine[row, col] + self.crecv[row, col]
            return carry

        lax.fori_loop(0, links.outer * inner, add, 0)
        links.send(None, self.mine.at[:, 1 - links.col], self.yrecv, self.sem("y_send"), self.sem("y_recv"),
                   {"fsdp": links.spot + 1 - 2 * links.col})

    def slot(self, way, place, dest):
        return dest - place if way == 0 else self.links.outer - place + dest

    def pass_on(self, way, dest, there, first):
        links = self.links
        step = 1 if way == 0 else -1
        mine = self.mine.at[dest, links.col]
        put = self.slot(way, links.row + step, dest)
        if not first:
            got = self.slot(way, links.row, dest)

            @pl.when(there)
            def _():
                links.arrive(self.zrecv.at[got], self.sem("z_recv", got), self.sems["spare"].at[0])
                mine[...] = mine[...] + self.zrecv[got]

        links.send(there, mine, self.zrecv.at[put], self.sem("z_send", way, dest), self.sem("z_recv", put),
                   {"fsdp": links.spot + step * links.inner})

    def column(self):
        links = self.links
        size = links.outer
        links.arrive(self.yrecv, self.sem("y_recv"), self.sems["spare"].at[0])

        def add(index, carry):
            self.mine[index, links.col] = self.mine[index, links.col] + self.yrecv[index]
            return carry

        lax.fori_loop(0, size, add, 0)
        for far in range(size - 1, 0, -1):
            self.pass_on(0, far, links.row == 0, True)
            self.pass_on(1, size - 1 - far, links.row == size - 1, True)

    def hop(self, turn):
        links = self.links
        size = links.outer
        for way in range(2):
            place = turn if way == 0 else size - 1 - turn
            here = links.row == place
            rest = range(size - 1, place, -1) if way == 0 else range(0, place)
            for dest in rest:
                self.pass_on(way, dest, here, False)
            mine = self.mine.at[place, links.col]
            got = self.slot(way, place, place)

            @pl.when(here)
            def _():
                links.arrive(self.zrecv.at[got], self.sem("z_recv", got), self.sems["spare"].at[0])
                mine[...] = mine[...] + self.zrecv[got]

    def cross(self):
        links = self.links
        mine = self.mine.at[links.row, links.col]
        links.send(None, mine, self.xrecv, self.sem("x_send"), self.sem("x_recv"), {"rep": links.across})

    def finish(self):
        links = self.links
        links.arrive(self.xrecv, self.sem("x_recv"), self.sems["spare"].at[0])
        self.stage[...] = self.mine[links.row, links.col].astype(F32) + self.xrecv[...].astype(F32)
        place = self.total if self.whole else halves(self.total, links.core)
        self.keep = pltpu.make_async_copy(self.stage, place, self.sem("m_sem"))
        self.keep.start()
        if not self.whole:
            links.send(None, self.stage, place, self.sem("f_send"), self.sem("f_recv"), {"rep": links.mate})

    def settle(self):
        self.keep.wait()
        if not self.whole:
            self.links.arrive(
                halves(self.total, 1 - self.links.core), self.sem("f_recv"), self.sems["spare"].at[0]
            )


class AcrossFirst(Reduction):
    def pair(self):
        links = self.links
        if self.load is not None:
            self.load.wait()
        links.arrive(self.crecv, self.sem("c_recv"), self.sems["spare"].at[0])
        inner = links.inner

        def add(index, carry):
            row, col = index // inner, index % inner
            self.mine[row, col] = self.mine[row, col] + self.crecv[row, col]
            return carry

        lax.fori_loop(0, links.outer * inner, add, 0)
        self.side = links.rank // 2
        links.send(None, self.rows_of(self.mine, 1 - self.side), self.xrecv, self.sem("x_send"), self.sem("x_recv"),
                   {"rep": links.across})

    def rows_of(self, ref, which):
        half = ref.shape[-2] // 2
        rows = pl.ds(pl.multiple_of(which * half, 16), half)
        return ref.at[:, :, rows, :] if len(ref.shape) == 4 else ref.at[rows, :]

    def meet(self):
        links = self.links
        links.arrive(self.xrecv, self.sem("x_recv"), self.sems["spare"].at[0])
        self.mine = self.rows_of(self.mine, self.side)
        inner = links.inner

        def add(index, carry):
            row, col = index // inner, index % inner
            self.mine[row, col] = self.mine[row, col] + self.xrecv[row, col]
            return carry

        lax.fori_loop(0, links.outer * inner, add, 0)
        links.send(None, self.mine.at[:, 1 - links.col], self.yrecv, self.sem("y_send"), self.sem("y_recv"),
                   {"fsdp": links.spot + 1 - 2 * links.col})

    def quarter(self, side, core):
        return halves(self.rows_of(self.total, side), core)

    def spread(self, stage, place, keep, ssem, rsem):
        links = self.links
        self.keeps.append(pltpu.make_async_copy(stage, place, keep))
        self.keeps[-1].start()
        links.send(None, stage, place, ssem, rsem, {"rep": links.mate})

    def cross(self):
        links = self.links
        mine = self.mine.at[links.row, links.col]
        links.send(None, mine, self.third, self.sem("h_send"), self.sem("h_recv"), {"rep": links.across})
        self.stage[...] = mine[...].astype(F32)
        self.keeps = []
        self.spread(self.stage, self.quarter(self.side, links.core), self.sem("m_sem"),
                    self.sem("f_send"), self.sem("f_recv"))

    def finish(self):
        links = self.links
        links.arrive(self.third, self.sem("h_recv"), self.sems["spare"].at[0])
        self.stage_two[...] = self.third[...].astype(F32)
        self.spread(self.stage_two, self.quarter(1 - self.side, links.core), self.sem("k_keep"),
                    self.sem("k_send"), self.sem("k_recv"))

    def settle(self):
        links = self.links
        for keep in self.keeps:
            keep.wait()
        for side, name in ((self.side, "f_recv"), (1 - self.side, "k_recv")):
            links.arrive(self.quarter(side, 1 - links.core), self.sem(name), self.sems["spare"].at[0])


SEM_NAMES = ("c_send", "c_recv", "m_sem", "y_send", "y_recv", "z_send", "z_recv", "x_send", "x_recv",
             "f_send", "f_recv", "h_send", "h_recv", "k_send", "k_recv", "k_keep", "r_send", "r_recv", "own", "spare")


class Return:
    def __init__(self, links, source, home, sems, kind):
        self.links, self.source, self.home, self.sems, self.kind = links, source, home, sems, kind

    def begin(self):
        links = self.links
        dst = self.home.at[links.rank]
        for way, device in enumerate((links.across, links.mate)):
            links.send(None, self.source, dst, self.sems["r_send"].at[self.kind, way],
                       self.sems["r_recv"].at[self.kind, way], {"rep": device})
        self.copy = pltpu.make_async_copy(self.source, dst, self.sems["own"].at[self.kind])
        self.copy.start()

    def relay(self):
        links = self.links
        place = self.home.at[links.across]
        links.arrive(place, self.sems["r_recv"].at[self.kind, 0], self.sems["spare"].at[0])
        links.send(None, place, place, self.sems["r_send"].at[self.kind, 2],
                   self.sems["r_recv"].at[self.kind, 2], {"rep": links.mate})

    def settle(self):
        links, sem = self.links, self.sems["r_recv"]
        links.arrive(self.home.at[links.mate], sem.at[self.kind, 1], self.sems["spare"].at[0])
        links.arrive(self.home.at[across_of(links.mate)], sem.at[self.kind, 2], self.sems["spare"].at[0])
        self.copy.wait()


TABLE_ROWS = 56


def packed_table(lens, tabv_ref):
    lane = iota((8, 128), 1)
    blocks = lax.div(lens + (BLK - 1), BLK)
    key = jnp.where(blocks > 0, blocks * 128 + (127 - lane), 0)
    wide = jnp.broadcast_to(key[:1], (128, 128))
    other = jnp.sum(jnp.where(iota((128, 128), 0) == iota((128, 128), 1), wide, 0), axis=1, keepdims=True)
    order = jnp.sum(jnp.where(other > wide, 1, 0), axis=0, keepdims=True)
    order = jnp.broadcast_to(order, (8, 128))
    edges, below = [], jnp.zeros((8, 1), jnp.int32)
    for size in range(MAX_SEQ_BLOCKS, 0, -1):
        below = below + jnp.sum(jnp.where(blocks == size, 1, 0), axis=1, keepdims=True)
        edges.append(jnp.broadcast_to(below, (8, 128)))

    def assign(number, carry):
        loads, slot, first = carry[:4], carry[4], carry[5]
        size = jnp.zeros((8, 128), jnp.int32)
        for step, edge in enumerate(edges):
            size = size + jnp.where(number < edge, 1, 0)
        low = jnp.minimum(jnp.minimum(loads[0], loads[1]), jnp.minimum(loads[2], loads[3]))
        best = jnp.full((8, 128), 3, jnp.int32)
        for dev in (2, 1, 0):
            best = jnp.where(loads[dev] == low, dev, best)
        mine = order == number
        slot = jnp.where(mine, best * SLOTS + low, slot)
        first = jnp.where(mine, low, first)
        loads = tuple(loads[dev] + jnp.where(best == dev, size, 0) for dev in range(4))
        return loads + (slot, first)

    zero = jnp.zeros((8, 128), jnp.int32)
    carry = lax.fori_loop(0, 32, assign, (zero,) * 6)
    slot, first = carry[4], carry[5]
    where, tokens, segment = zero - 1, zero, zero
    for step in range(MAX_SEQ_BLOCKS):
        def shifted(value):
            return value if step == 0 else pltpu.roll(value, step, 1)

        covers = shifted(blocks) > step
        where = jnp.where(covers, shifted(slot) + step, where)
        tokens = jnp.where(covers, jnp.minimum(shifted(lens) - BLK * step, BLK), tokens)
        segment = jnp.where(covers, shifted(first) + 1, segment)
    packed = jnp.where(where >= 0, (lane + 1) + 128 * tokens + 16384 * segment, 0)
    spots = jnp.broadcast_to(where[:1], (48, 128))
    values = jnp.broadcast_to(packed[:1], (48, 128))
    column = jnp.sum(jnp.where(spots == iota((48, 128), 0), values, 0), axis=1, keepdims=True)
    tabv_ref[:48] = jnp.broadcast_to(column, (48, 128))
    tabv_ref[48:] = where


def front_kernel(outer, inner, *refs):
    (lens_ref, rows_ref, cots_ref, *weights), refs = refs[:9], refs[9:]
    (wd_ref, wc_ref), refs = refs[:2], refs[2:]
    (tab_ref, x_ref, cot_ref, n_ref, qkv_ref, att_ref, lse_ref, wqkv_ref, gc_ref, ga_ref, gb_ref), refs = refs[:11], refs[11:]
    (stage, lens_all, tabs, psend, precv, xsend, xrecv), refs = refs[:7], refs[7:]
    (l_send, l_recv, t_sem, w_sem, z_send, z_recv, y_send, y_recv, c_send, c_recv, d_send, d_recv, own_sem,
     p_send, p_recv, x_send, x_recv, spare) = refs
    links = Links(outer, inner)
    rank, spot, core, mate, across = links.rank, links.spot, links.core, links.mate, links.across
    row, col = links.row, links.col
    side = rank // 2
    count = outer * inner
    part = stage.shape[0]
    per_rank = rows_ref.shape[0]
    width = 3 * D
    tall = wd_ref.shape[0]
    hidden = weights[-1].shape[1]
    gate_half, up_half = (D + hidden) // 2, hidden // 2

    at = 0
    loads = []
    for number, ref in enumerate(weights):
        cols = slice(at, at + ref.shape[1])
        loads.append(pltpu.make_async_copy(ref, stage.at[:, cols], w_sem.at[number]))
        loads[-1].start()
        at += ref.shape[1]

    links.greet(True)
    lens_all[rank] = lens_ref[...]
    for step in range(1, 4):
        links.send(None, lens_ref, lens_all.at[rank], l_send.at[step - 1], l_recv.at[step - 1],
                   {"rep": (rank + step) % 4})

    def cols_of(start, half, which):
        return pl.ds(pl.multiple_of(start + which * half, 128), half)

    down_half = D // 2

    def tall_rows(which):
        return pl.ds(pl.multiple_of(which * (tall // 2), 16), tall // 2)

    def source(number):
        return (
            lambda: stage.at[:, cols_of(0, width // 2, core)],
            lambda: stage.at[:, cols_of(width, gate_half, core)],
            lambda: stage.at[:, cols_of(width + 2 * gate_half, up_half, core)],
            lambda: wd_ref.at[tall_rows(side), cols_of(0, down_half, core)],
            lambda: wc_ref,
        )[number]()

    def place(number, shard, which=None):
        which = core if which is None else which
        return (
            lambda: wqkv_ref.at[pl.ds(pl.multiple_of(shard * part, 16), part), cols_of(0, width // 2, which)],
            lambda: ga_ref.at[shard, :, cols_of(0, gate_half, which)],
            lambda: ga_ref.at[shard, :, cols_of(2 * gate_half, up_half, which)],
            lambda: gb_ref.at[shard, tall_rows(side), cols_of(0, down_half, which)],
            lambda: gc_ref.at[shard],
            lambda: gb_ref.at[shard, tall_rows(1 - side), cols_of(0, down_half, which)],
        )[number]()

    nobody = spare.at[0]

    def both(first, second):
        return second if first is None else jnp.logical_and(first, second)

    def guarded(there, action):
        if there is None:
            action()
        else:
            pl.when(there)(action)

    def share(there, number, shard):
        if number == 4:
            return
        here = place(number, shard)
        links.send(there, here, here, c_send.at[number, shard], c_recv.at[number, shard], {"rep": mate})
        if number == 3:
            links.send(there, here, here, d_send.at[shard], d_recv.at[shard], {"rep": across})

    other_column = {"fsdp": spot + 1 - 2 * col}

    def along_row(there, number, line, src):
        here = place(number, line * inner + col)
        links.send(there, here if src is None else src, here, y_send.at[line, number], y_recv.at[line, number],
                   other_column)

    def lines(step):
        return ((row - 1 - step >= 0, row - 1 - step, 0, row + 1 < outer, spot + inner),
                (row + 1 + step < outer, row + 1 + step, 1, row > 0, spot - inner))

    def own(number):
        src, dst = source(number), place(number, spot)
        links.send(row + 1 < outer, src, dst, z_send.at[0, 0, number], z_recv.at[0, 0, number],
                   {"fsdp": spot + inner})
        links.send(row > 0, src, dst, z_send.at[1, 0, number], z_recv.at[1, 0, number], {"fsdp": spot - inner})
        along_row(None, number, row, src)

    def hop(number, step):
        for here, line, way, onward, target in lines(step):
            shard = line * inner + col
            guarded(here, lambda: links.arrive(place(number, shard), z_recv.at[way, step, number], nobody))
            if step + 1 < outer - 1:
                view = place(number, shard)
                links.send(both(here, onward), view, view, z_send.at[way, step + 1, number],
                           z_recv.at[way, step + 1, number], {"fsdp": target})
            along_row(here, number, line, None)
            share(here, number, shard)

    def from_row(number):
        def one(there, line):
            shard = line * inner + 1 - col
            guarded(there, lambda: links.arrive(place(number, shard), y_recv.at[line, number], nobody))
            share(there, number, shard)

        one(None, row)
        for step in range(outer - 1):
            for here, line, *_ in lines(step):
                one(here, line)

    def gathered(*numbers):
        for shard in range(count):
            @pl.when(shard != spot)
            def _():
                for number in numbers:
                    links.arrive(place(number, shard, 1 - core), c_recv.at[number, shard], nobody)

    def from_across():
        for shard in range(count):
            there = shard != spot
            guarded(there, lambda: links.arrive(place(5, shard), d_recv.at[shard], nobody))
            here = place(5, shard)
            links.send(there, here, here, c_send.at[5, shard], c_recv.at[5, shard], {"rep": mate})

    for load in loads:
        load.wait()
    own(0)
    own(4)
    own(1)
    keep = [
        pltpu.make_async_copy(stage.at[:, :width], wqkv_ref.at[pl.ds(pl.multiple_of(spot * part, 16), part)], own_sem.at[0]),
        pltpu.make_async_copy(stage.at[:, width:], ga_ref.at[spot], own_sem.at[1]),
        pltpu.make_async_copy(wd_ref, gb_ref.at[spot], own_sem.at[2]),
        pltpu.make_async_copy(wc_ref, gc_ref.at[spot], own_sem.at[3]),
    ]
    for copy in keep:
        copy.start()

    for step in range(1, 4):
        links.arrive(lens_all.at[(rank + 4 - step) % 4], l_recv.at[step - 1], nobody)
    lens = lens_all[0] + lens_all[1] + lens_all[2] + lens_all[3]
    packed_table(jnp.broadcast_to(lens[:1], (8, 128)), tab_ref)
    to_scalar = pltpu.make_async_copy(tab_ref, tabs, t_sem.at[0])
    to_scalar.start()
    to_scalar.wait()

    sources = (rows_ref, cots_ref)
    outs = (x_ref, cot_ref)

    def picked(kind, target, slot):
        index = block_at(tabs, target * SLOTS + slot) - rank * per_rank
        mine = jnp.logical_and(index >= 0, index < per_rank)
        return mine, sources[kind][jnp.clip(index, 0, per_rank - 1)]

    def mate_copy(kind, piece):
        return pltpu.make_async_remote_copy(
            src_ref=psend.at[kind, piece], dst_ref=precv.at[kind, piece],
            send_sem=p_send.at[kind, piece], recv_sem=p_recv.at[kind, piece],
            device_id={"rep": mate}, device_id_type=MESH,
        )

    def across_copy(kind):
        return pltpu.make_async_remote_copy(
            src_ref=xsend.at[kind], dst_ref=xrecv.at[kind],
            send_sem=x_send.at[kind], recv_sem=x_recv.at[kind],
            device_id={"rep": across}, device_id_type=MESH,
        )

    def pack_rows(kind, piece):
        target = mate if piece == 0 else across_of(mate)

        def pack(slot, carry):
            mine, value = picked(kind, target, slot)
            psend[kind, piece, slot] = jnp.where(mine, value, jnp.zeros_like(value))
            return carry

        lax.fori_loop(0, SLOTS, pack, 0)
        mate_copy(kind, piece).start()

    def cross_rows(kind):
        mate_copy(kind, 1).wait_recv()

        def merge(slot, carry):
            mine, value = picked(kind, across, slot)
            xsend[kind, slot] = jnp.where(mine, value, precv[kind, 1, slot])
            return carry

        lax.fori_loop(0, SLOTS, merge, 0)
        across_copy(kind).start()

    def finish_rows(kind):
        mate_copy(kind, 0).wait_recv()
        across_copy(kind).wait_recv()

        def finish(slot, carry):
            mine, value = picked(kind, rank, slot)
            rows = pl.ds(pl.multiple_of(slot * BLK, BLK), BLK)
            outs[kind][rows, :] = jnp.where(mine, value, precv[kind, 0, slot] + xrecv[kind, slot])
            return carry

        lax.fori_loop(0, SLOTS, finish, 0)

    pack_rows(0, 1)
    pack_rows(1, 1)
    cross_rows(0)
    pack_rows(0, 0)
    cross_rows(1)
    pack_rows(1, 0)
    for step in range(outer - 1):
        hop(0, step)
    for step in range(outer - 1):
        hop(4, step)
    hop(1, 0)
    own(2)
    from_row(0)
    from_row(4)
    for step in range(1, outer - 1):
        hop(1, step)
    keep[3].wait()
    gains = gains_of(gc_ref)
    finish_rows(0)
    forward_norm(tabs, rank, x_ref, gains, n_ref)
    hop(2, 0)
    own(3)
    keep[0].wait()
    gathered(0)
    forward_project(n_ref, wqkv_ref, qkv_ref)
    hop(2, 1)
    forward_attention(tabs, rank, qkv_ref, att_ref, lse_ref, 0, 2)
    from_row(1)
    for step in range(2, outer - 1):
        hop(2, step)
    hop(3, 0)
    forward_attention(tabs, rank, qkv_ref, att_ref, lse_ref, 2, 4)
    from_row(2)
    for step in range(1, outer - 1):
        hop(3, step)
    forward_attention(tabs, rank, qkv_ref, att_ref, lse_ref, 4, TILES)
    from_row(3)
    finish_rows(1)
    from_across()
    gathered(1, 2, 3, 5)
    links.drain()
    for kind in range(2):
        for piece in range(2):
            mate_copy(kind, piece).wait_send()
        across_copy(kind).wait_send()
    for copy in keep[1:3]:
        copy.wait()


def gather_and_attend(count, lens, rows, cots, weights, wd, wc):
    outer, inner = grid_of(count)
    block = rows.shape[1:]
    part, hidden = wd.shape[0], weights[-1].shape[1]
    part = weights[0].shape[0]
    dma, shape = pltpu.SemaphoreType.DMA, jax.ShapeDtypeStruct
    total = sum(weight.shape[1] for weight in weights)
    kinds = 5
    return pl.pallas_call(
        partial(front_kernel, outer, inner),
        out_shape=(
            shape((TABLE_ROWS, 128), jnp.int32), shape((ROWS, D), BF16), shape((ROWS, D), BF16),
            shape((ALL_ROWS, D), BF16), shape((ALL_ROWS, 3 * D), BF16), shape((ROWS, D), BF16),
            shape((TILES, 16, QT), F32), shape((D, 3 * D), BF16), shape((count,) + wc.shape, BF16),
            shape((count, part, total - 3 * D), BF16), shape((count,) + wd.shape, BF16),
        ),
        in_specs=[VMEM] * 3 + [ANY] * 6 + [VMEM] * 2,
        out_specs=(VMEM,) * 9 + (ANY,) * 2,
        scratch_shapes=[
            pltpu.VMEM((part, total), BF16), pltpu.VMEM((4, 8, 128), jnp.int32), pltpu.SMEM((TABLE_ROWS, 128), jnp.int32),
            pltpu.VMEM((2, 2, SLOTS) + block, BF16), pltpu.VMEM((2, 2, SLOTS) + block, BF16),
            pltpu.VMEM((2, SLOTS) + block, BF16), pltpu.VMEM((2, SLOTS) + block, BF16),
            dma((3,)), dma((3,)), dma((1,)), dma((6,)),
            dma((2, outer - 1, kinds)), dma((2, outer - 1, kinds)), dma((outer, kinds)), dma((outer, kinds)),
            dma((kinds + 1, count)), dma((kinds + 1, count)), dma((count,)), dma((count,)), dma((4,)),
            dma((2, 2)), dma((2, 2)), dma((2,)), dma((2,)), dma((1,)),
        ],
        compiler_params=pltpu.CompilerParams(
            collective_id=1, has_side_effects=True, vmem_limit_bytes=VMEM_LIMIT
        ),
        name="gather_and_attend",
    )(lens, rows, cots, *weights, wd, wc)


ACROSS_FIRST = (2, 3)
REAR_ORDER = (
    ("do", "start"), ("do", "P0"), ("do", "P1a"), ("do", "gA"), ("begin", 0), ("do", "uA"), ("begin", 1),
    ("do", "P1b"), ("pair", 0), ("pair", 1), ("do", "gB"), ("begin", 2), ("do", "uB"), ("begin", 3), ("do", "d"),
    ("begin", 4), ("pair", 2), ("pair", 3), ("do", "out"), ("rows", 0), ("pair", 4), ("col", 0), ("meet", 2),
    ("do", "P4"), ("col", 1), ("do", "P5"), ("begin", 5), ("do", "q0"), ("meet", 3), ("pair", 5), ("hop", 0, 1),
    ("hop", 1, 1), ("do", "p0"), ("begin", 6), ("do", "q1"), ("pair", 6), ("col", 4), ("hop", 0, 2), ("hop", 1, 2),
    ("do", "p1"), ("begin", 7), ("do", "q2"), ("pair", 7), ("col", 2), ("col", 3), ("hop", 0, 3), ("cross", 0),
    ("hop", 1, 3), ("cross", 1), ("do", "bp"), ("rows", 1), ("relay", 0), ("col", 5), ("hop", 4, 1), ("fin", 0),
    ("fin", 1), ("do", "p2"), ("begin", 8), ("hop", 2, 1), ("do", "dc"), ("begin", 9), ("hop", 3, 1), ("pair", 8),
    ("pair", 9), ("col", 6), ("hop", 4, 2), ("hop", 5, 1), ("hop", 2, 2), ("hop", 3, 2), ("hop", 6, 1),
    ("hop", 5, 2), ("hop", 6, 2), ("hop", 4, 3), ("cross", 4), ("col", 7), ("hop", 7, 1), ("hop", 2, 3),
    ("cross", 2), ("hop", 3, 3), ("cross", 3), ("col", 8), ("col", 9), ("hop", 5, 3), ("cross", 5), ("hop", 6, 3),
    ("cross", 6), ("relay", 1), ("hop", 8, 1), ("hop", 9, 1), ("hop", 7, 2), ("hop", 8, 2), ("hop", 9, 2),
    ("fin", 4), ("fin", 2), ("fin", 3), ("hop", 7, 3), ("cross", 7), ("fin", 5), ("hop", 8, 3), ("cross", 8),
    ("hop", 9, 3), ("cross", 9), ("fin", 6), ("fin", 7), ("fin", 8), ("fin", 9),
)


def rear_kernel(outer, inner, *refs):
    (tab_ref, x_ref, att_ref, lse_ref, gc_ref), refs = refs[:5], refs[5:]
    (cot_any, n_any, qkv_any, wqkv_any, wf_any, wd_any), refs = refs[:6], refs[6:]
    kinds = 10
    (og_ref, ou_ref, od_ref, oo_ref, op_ref, oc_ref, ry_ref, rg_ref), refs = refs[:8], refs[8:]
    (y_ref, gh_ref, fa_ref, dk_ref, b0_ref, b1_ref, b2_ref, n_ref, ntt_ref, gres_ref, ga_ref), refs = refs[:11], refs[11:]
    (wf_ref, wd_ref, dg_ref, du_ref, db_ref, do_ref, dc_ref, mine_ref), refs = refs[:8], refs[8:]
    crecv, refs = list(refs[:7]), refs[7:]
    narrow = D // 2
    crecv = crecv[:6] + [crecv[i].at[:, :, :, :narrow] for i in range(3)] + crecv[6:]
    yrecv, zrecv, xrecv, stages = (refs[kinds * i : kinds * (i + 1)] for i in range(4))
    refs = refs[4 * kinds :]
    extra, refs = refs[: 2 * len(ACROSS_FIRST)], refs[2 * len(ACROSS_FIRST) :]
    sems = dict(zip(SEM_NAMES, refs))
    load_sem, free_sem = refs[len(SEM_NAMES) :]
    links = Links(outer, inner)
    rank = links.rank
    hidden = wd_ref.shape[0]
    part = wf_ref.shape[2]
    group = 4 * part

    def fetch(number, src, dst):
        copy = pltpu.make_async_copy(src, dst, load_sem.at[number])
        copy.start()
        return copy

    load_cot = fetch(0, cot_any, ga_ref)
    load_out = fetch(1, wf_any.at[:, :, :, :D], wf_ref.at[:, :, :, :D])
    load_in = fetch(2, wf_any.at[:, :, :, D:], wf_ref.at[:, :, :, D:])
    load_down = fetch(3, wd_any, wd_ref)
    links.greet()

    def weight(start, size):
        return wf_ref[:, :, :, pl.ds(start, size)].reshape(D, size)

    wide = hidden // 2
    first, second = slice(0, wide), slice(wide, hidden)
    grads = [dg_ref.at[:, :, :, first], du_ref.at[:, :, :, first], dg_ref.at[:, :, :, second], du_ref.at[:, :, :, second],
             db_ref, do_ref] + [wf_ref.at[:, :, :, i * D : (i + 1) * D] for i in range(3)] + [dc_ref]
    totals = [og_ref.at[:, first], ou_ref.at[:, first], og_ref.at[:, second], ou_ref.at[:, second],
              od_ref, oo_ref] + [op_ref.at[:, i * D : (i + 1) * D] for i in range(3)] + [oc_ref]
    tasks = [
        (AcrossFirst if i in ACROSS_FIRST else Reduction)(
            links, grads[i], totals[i], mine_ref if i == kinds - 1 else None,
            crecv[i], yrecv[i], zrecv[i], xrecv[i], stages[i], sems, i,
        )
        for i in range(kinds)
    ]
    for number, i in enumerate(ACROSS_FIRST):
        tasks[i].third, tasks[i].stage_two = extra[2 * number], extra[2 * number + 1]
    returns = (Return(links, y_ref, ry_ref, sems, 0), Return(links, gres_ref, rg_ref, sems, 1))
    gains = gains_of(gc_ref)
    gain = gains[2:3]
    valid = valid_column(tab_ref, rank)
    h1_ref, dv_ref = fa_ref, fa_ref
    tiles = hidden // FF_TILE
    kept = {}

    def enter():
        load_cot.wait()
        load_out.wait()
        for tile in range(TILES):
            rows = pl.ds(tile * QT, QT)
            value = x_ref[rows, :].astype(F32) + mm(att_ref[rows, :], weight(0, D))
            h1_ref[rows, :] = value
            normed = (value * lax.rsqrt(mean_square(value) + EPSILON) * gain).astype(BF16)
            n_ref[rows, :] = normed
            ntt_ref[:, tile * QT : (tile + 1) * QT] = jnp.transpose(normed)
            gres_ref[rows, :] = (ga_ref[rows, :].astype(F32) * valid[tile * QT : (tile + 1) * QT]).astype(BF16)
        load_in.wait()
        load_down.wait()

    def inward(begin, end):
        def step(tile, carry):
            at = pl.multiple_of(tile * FF_TILE, FF_TILE)
            cols = pl.ds(at, FF_TILE)
            normed = n_ref[:ROWS, :]
            gate = mm(normed, weight(D + at, FF_TILE))
            up = mm(normed, weight(D + hidden + at, FF_TILE))
            back = mm_cols(gres_ref[...], wd_ref[cols, :])
            square = gate * gate
            bend = jnp.tanh(GELU_C * (gate * (1.0 + GELU_A * square)))
            half = 0.5 * (1.0 + bend)
            act = gate * half
            slope = half + (0.5 * GELU_C) * gate * (1.0 - bend * bend) * (1.0 + (3.0 * GELU_A) * square)
            b0_ref[:ROWS, cols] = (act * up).astype(BF16)
            b1_ref[:ROWS, cols] = (back * up * slope).astype(BF16)
            b2_ref[:ROWS, cols] = (back * act).astype(BF16)
            return carry

        lax.fori_loop(begin, end, step, 0)

    def outer_products(ref, right_ref, begin, end):
        def step(tile, carry):
            cols = pl.ds(pl.multiple_of(tile * FF_TILE, FF_TILE), FF_TILE)
            value = mm(ntt_ref[...], right_ref[:ROWS, cols]).astype(BF16)
            ref[:, :, :, cols] = value.reshape(outer, inner, part, FF_TILE)
            return carry

        lax.fori_loop(begin, end, step, 0)

    def down_products():
        def step(tile, carry):
            cols = pl.ds(pl.multiple_of(tile * FF_TILE, FF_TILE), FF_TILE)
            db_ref[tile // inner, tile % inner] = mm_rows(b0_ref[:ROWS, cols], gres_ref[...]).astype(BF16)
            return carry

        lax.fori_loop(0, tiles, step, 0)

    def outward():
        def step(tile, carry):
            cols = pl.ds(pl.multiple_of(tile * group, 128), group)
            value = h1_ref[:ROWS, cols] + mm(b0_ref[:ROWS, :hidden], wd_ref[:, cols])
            y_ref[:, cols] = (value * valid).astype(BF16)
            shards = pl.ds(tile * (4 // inner), 4 // inner)
            gh_ref[:, cols] = mm_cols(
                b1_ref[:ROWS, :hidden], wf_ref[shards, :, :, D : D + hidden].reshape(group, hidden)
            ) + mm_cols(b2_ref[:ROWS, :hidden], wf_ref[shards, :, :, D + hidden :].reshape(group, hidden))
            return carry

        lax.fori_loop(0, D // group, step, 0)
        kept["qkv"] = fetch(4, qkv_any, b1_ref)
        kept["wqkv"] = fetch(5, wqkv_any, b2_ref)

    def middle():
        gain_grad = jnp.zeros((1, D), F32)
        for tile in range(TILES):
            rows = pl.ds(tile * QT, QT)
            value, grad = h1_ref[rows, :], gh_ref[rows, :]
            root = lax.rsqrt(mean_square(value) + EPSILON)
            unit = value * root
            gain_grad = gain_grad + jnp.sum(grad * unit, axis=0, keepdims=True)
            grad = grad * gain
            grad = gres_ref[rows, :].astype(F32) + root * (
                grad - unit * jnp.mean(grad * unit, axis=-1, keepdims=True)
            )
            gh_ref[rows, :] = grad
            low = grad.astype(BF16)
            n_ref[rows, :] = low
            ga_ref[rows, :] = mm_cols(low, weight(0, D)).astype(BF16)
        kept["gain"] = gain_grad

    def out_products():
        def step(tile, carry):
            cols = pl.ds(pl.multiple_of(tile * QUAD, QUAD), QUAD)
            value = mm_rows(att_ref[...], n_ref[:ROWS, cols]).astype(BF16)
            do_ref[:, :, :, cols] = value.reshape(outer, inner, part, QUAD)
            return carry

        lax.fori_loop(0, D // QUAD, step, 0)
        kept["n"] = fetch(6, n_any, n_ref)

    def attention(quad):
        if quad == 0:
            backward_attention_start(dk_ref, dv_ref)
            kept["qkv"].wait()
        backward_attention_quad(tab_ref, rank, b1_ref, att_ref, ga_ref, lse_ref, b0_ref, dk_ref, dv_ref, quad)

    def project_products(quad):
        if quad == 0:
            kept["n"].wait()
        for number in range(3):
            value = mm_rows(n_ref[...], b0_ref[:, number * D + quad * QUAD : number * D + (quad + 1) * QUAD])
            low = (quad * 3 + number) * QUAD
            wf_ref[:, :, :, low : low + QUAD] = value.astype(BF16).reshape(outer, inner, part, QUAD)

    def input_gradient():
        kept["wqkv"].wait()
        kept["one"], kept["side"] = backward_project(
            tab_ref, rank, x_ref, gh_ref, gains, n_ref, b0_ref, b2_ref, dk_ref, gres_ref
        )

    def gain_pieces():
        rows = jnp.concatenate([kept["one"], kept["side"], kept["gain"], jnp.zeros((5, D), F32)], axis=0)
        spread_gain_grads(rows, dc_ref)

    half = tiles // 2
    work = {
        "start": lambda: None, "P0": enter, "P1a": lambda: inward(0, half), "P1b": lambda: inward(half, tiles),
        "gA": lambda: outer_products(dg_ref, b1_ref, 0, half), "gB": lambda: outer_products(dg_ref, b1_ref, half, tiles),
        "uA": lambda: outer_products(du_ref, b2_ref, 0, half), "uB": lambda: outer_products(du_ref, b2_ref, half, tiles),
        "d": down_products, "out": outward, "P4": middle, "P5": out_products,
        "q0": lambda: attention(0), "q1": lambda: attention(1), "q2": lambda: attention(2),
        "p0": lambda: project_products(0), "p1": lambda: project_products(1), "p2": lambda: project_products(2),
        "bp": input_gradient, "dc": gain_pieces,
    }
    paired = set()
    for action, which, *turn in REAR_ORDER:
        if action == "do":
            work[which]()
        elif action == "begin":
            if which == 6:
                pl.semaphore_wait(free_sem, 1)
            tasks[which].begin()
        elif action == "pair":
            tasks[which].pair()
            paired.add(which)
            if which < 3 and paired >= {0, 1, 2}:
                pl.semaphore_signal(free_sem, inc=1, device_id={"rep": links.mate}, device_id_type=MESH)
        elif action == "meet":
            tasks[which].meet()
        elif action == "col":
            tasks[which].column()
        elif action == "hop":
            tasks[which].hop(turn[0])
        elif action == "cross":
            tasks[which].cross()
        elif action == "fin":
            tasks[which].finish()
        elif action == "rows":
            returns[which].begin()
        else:
            returns[which].relay()
    for one in returns:
        one.settle()
    for task in tasks:
        task.settle()
    links.drain()


def feed_and_reduce(count, table, x, att, lse, gc, cot, n, qkv, wqkv, wf, wd):
    outer, inner = grid_of(count)
    part, tall = D // count, wd.shape[1]
    hidden = count * tall
    wf = wf.reshape((outer, inner) + wf.shape[1:])
    full = [(part, hidden), (part, hidden), (tall, D), (part, D), (part, 3 * D), (8, 128)]
    shapes = [(part, hidden // 2)] * 4 + [(tall, D)] + [(part, D)] * 4 + [(8, 128)]
    kinds = len(shapes)
    dtypes = [BF16] * (kinds - 1) + [F32]
    halved = [(a, b // 2 if b % 256 == 0 else b) for a, b in shapes]
    later = [(a // 2, b) if i in ACROSS_FIRST else (a, b) for i, (a, b) in enumerate(halved)]
    dma, vmem = pltpu.SemaphoreType.DMA, pltpu.VMEM
    scratch = [
        vmem((ROWS, D), BF16), vmem((ROWS, D), F32), vmem((ALL_ROWS, D), F32), vmem((ALL_ROWS, D), F32),
        vmem((ALL_ROWS, 3 * D), BF16), vmem((ALL_ROWS, 3 * D), BF16), vmem((D, 3 * D), BF16),
        vmem((ALL_ROWS, D), BF16), vmem((D, ROWS), BF16), vmem((ROWS, D), BF16), vmem((ROWS, D), BF16),
        vmem(wf.shape, BF16), vmem((hidden, D), BF16),
    ]
    scratch += [vmem((outer, inner) + shape, BF16) for shape in full[:4]]
    scratch += [vmem((outer, inner) + full[-1], F32)] * 2
    scratch += [vmem((outer, inner) + halved[i], dtypes[i]) for i in (0, 1, 2, 3, 4, 5, 9)]
    for lead in ((outer,), (outer + 1,), ()):
        for i in range(kinds):
            across = (outer, inner) if i in ACROSS_FIRST and lead == () else lead
            scratch.append(vmem(across + later[i], dtypes[i]))
    scratch += [vmem(shape, F32) for shape in later]
    for i in ACROSS_FIRST:
        scratch += [vmem(later[i], BF16), vmem(later[i], F32)]
    one = dma((kinds,))
    scratch += [one, one, one, one, one, dma((2, outer, kinds)), dma((outer + 1, kinds))] + [one] * 9
    scratch += [dma((2, 3)), dma((2, 3)), dma((2,)), dma((1,)), dma((7,)), pltpu.SemaphoreType.REGULAR]
    rows = jax.ShapeDtypeStruct((4, ROWS, D), BF16)
    outs = pl.pallas_call(
        partial(rear_kernel, outer, inner),
        out_shape=tuple(jax.ShapeDtypeStruct(shape, F32) for shape in full) + (rows, rows),
        in_specs=[SMEM] + [VMEM] * 4 + [ANY] * 6,
        out_specs=(ANY,) * 8,
        scratch_shapes=scratch,
        compiler_params=pltpu.CompilerParams(
            collective_id=2, has_side_effects=True, vmem_limit_bytes=67043328
        ),
        name="feed_and_reduce",
    )(table, x, att, lse, gc, cot, n, qkv, wqkv, wf, wd.reshape(hidden, D))
    return outs[:6], outs[6], outs[7]


def place_kernel(part, tab_ref, ry_ref, rg_ref, og_ref, ou_ref, od_ref, oo_ref, op_ref, oc_ref, *refs):
    (y_ref, g_ref, q_out, k_out, v_out, o_out, g_out, u_out, d_out, one_out, side_out, two_out), refs = refs[:12], refs[12:]
    (y_buf, g_buf, bg, bu, bd, bo, bp, sem_in, sem_out, sem_rows, sem_home) = refs
    blocks = y_buf.shape[0]
    base = lax.axis_index("rep") * blocks
    tables = ((og_ref, bg), (ou_ref, bu), (od_ref, bd), (oo_ref, bo), (op_ref, bp))
    reads = [pltpu.make_async_copy(src, dst, sem_in.at[i]) for i, (src, dst) in enumerate(tables)]
    rows = ((ry_ref, y_buf, y_ref), (rg_ref, g_buf, g_ref))

    def fetch(block, carry):
        index = tab_ref[48, base + block]
        safe = jnp.maximum(index, 0)
        for kind, (src, buf, _) in enumerate(rows):
            @pl.when(index >= 0)
            def _():
                pltpu.make_async_copy(
                    src.at[lax.div(safe, SLOTS), lax.rem(safe, SLOTS)], buf.at[block], sem_rows.at[kind, block]
                ).start()

            @pl.when(index < 0)
            def _():
                buf[block] = jnp.zeros(buf.shape[1:], buf.dtype)

        return carry

    lax.fori_loop(0, blocks, fetch, 0)
    for read in reads:
        read.start()

    def leave(block, carry):
        index = tab_ref[48, base + block]
        for kind, (src, buf, dst) in enumerate(rows):
            @pl.when(index >= 0)
            def _():
                pltpu.make_async_copy(src.at[0, 0], buf.at[block], sem_rows.at[kind, block]).wait()

            pltpu.make_async_copy(buf.at[block], dst.at[block], sem_home.at[kind, block]).start()
        return carry

    lax.fori_loop(0, blocks, leave, 0)
    for number, out in enumerate((one_out, side_out, two_out)):
        out[...] = oc_ref[number, :part]
    writes = []
    for number, (buf, dst) in enumerate(((bg, g_out), (bu, u_out), (bd, d_out), (bo, o_out))):
        reads[number].wait()
        writes.append(pltpu.make_async_copy(buf, dst, sem_out.at[number]))
        writes[-1].start()
    reads[4].wait()
    for quad in range(D // QUAD):
        for number, dst in enumerate((q_out, k_out, v_out)):
            low = (3 * quad + number) * QUAD
            copy = pltpu.make_async_copy(
                bp.at[:, low : low + QUAD], dst.at[:, quad * QUAD : (quad + 1) * QUAD], sem_out.at[4 + 3 * quad + number]
            )
            copy.start()
            writes.append(copy)
    for write in writes:
        write.wait()

    def rest(block, carry):
        for kind, (_, buf, dst) in enumerate(rows):
            pltpu.make_async_copy(buf.at[block], dst.at[block], sem_home.at[kind, block]).wait()
        return carry

    lax.fori_loop(0, blocks, rest, 0)


def place_all(table, ry, rg, totals, blocks, part, shape):
    out = jax.ShapeDtypeStruct
    og, ou, od, oo, op, oc = totals
    block = (blocks,) + ry.shape[2:]
    dma, vmem = pltpu.SemaphoreType.DMA, pltpu.VMEM
    gain = out((part,), F32)
    y, g, q, k, v, o, gate, up, down, one, side, two = pl.pallas_call(
        partial(place_kernel, part),
        out_shape=(out(block, ry.dtype), out(block, rg.dtype), out(oo.shape, F32), out(oo.shape, F32), out(oo.shape, F32),
                   out(oo.shape, F32), out(og.shape, F32), out(ou.shape, F32), out(od.shape, F32), gain, gain, gain),
        in_specs=[SMEM] + [ANY] * 7 + [VMEM],
        out_specs=(ANY,) * 9 + (VMEM,) * 3,
        scratch_shapes=[vmem(block, ry.dtype), vmem(block, rg.dtype)] + [vmem(t.shape, F32) for t in totals[:5]]
        + [dma((5,)), dma((13,)), dma((2, blocks)), dma((2, blocks))],
        compiler_params=pltpu.CompilerParams(vmem_limit_bytes=VMEM_LIMIT),
        name="place_outputs",
    )(table, ry, rg, og, ou, od, oo, op, oc)
    return (y.reshape(shape), g.reshape(shape), one, side, q, k, v, o, two, gate, up, down)


def per_device(count, layer_input, cotangent, lengths, attn_gain, global_gain, query_weight, key_weight,
               value_weight, out_weight, ffn_gain, gate_weight, up_weight, down_weight):
    micro, span, width = layer_input.shape
    hidden = gate_weight.shape[1]
    blocks = micro * span // BLK
    part = attn_gain.shape[0]
    rows_in = layer_input.reshape(blocks, BLK, width)
    cots_in = cotangent.reshape(blocks, BLK, width)
    weights = (query_weight, key_weight, value_weight, out_weight, gate_weight, up_weight)
    wc = jnp.pad(jnp.stack([attn_gain, global_gain, ffn_gain]), ((0, 13), (0, 128 - part)))
    if grid_of(count)[1] == 2 and part % 16 == 0:
        lens = lax.dynamic_update_slice(
            jnp.zeros((8, 128), jnp.int32), lengths.reshape(1, blocks), (0, lax.axis_index("rep") * blocks)
        )
        table, x, cot, n, qkv, att, lse, wqkv, gc, ga, gb = gather_and_attend(
            count, lens, rows_in, cots_in, weights, down_weight, wc
        )
        totals, ry, rg = feed_and_reduce(count, table, x, att, lse, gc, cot, n, qkv, wqkv, ga, gb)
        ry, rg = (rows.reshape(4, SLOTS, BLK, width) for rows in (ry, rg))
        return place_all(table, ry, rg, totals, blocks, part, layer_input.shape)
    else:
        table = deal_table(lengths)
        splits = ((0, 4 * width), (4 * width, 2 * hidden))
        ga, gb, gc, rows, cots = gather_weights(
            count, splits, table, rows_in, cots_in, jnp.concatenate(weights, axis=1), down_weight, wc
        )
        x, full = rows.reshape(ROWS, width), ga.reshape(width, -1)
        n, qkv, att, lse = attend(table, x, gc, full)
        y, gh, gatt, dg, du, db, do, gain = feed(
            table, x, cots.reshape(ROWS, width), att, gc, full, gb.reshape(-1, width)
        )
        g, dw, dc = backward_layer(table, x, gh, gatt, att, lse, n, qkv, gain, gc, full)
        grads = [grad.reshape(count, -1, grad.shape[-1]) for grad in (dg, du, db, do, dw, dc)]
        og, ou, ob, oo, ow, oc, ry, rg = reduce_grads(
            count, grads, y.reshape(SLOTS, BLK, width), g.reshape(SLOTS, BLK, width)
        )
        oq, ok, ov = ow[:, :width], ow[:, width : 2 * width], ow[:, 2 * width :]
    y_home, g_home = bring_home(table, ry, rg, blocks)
    return (
        y_home.reshape(layer_input.shape), g_home.reshape(layer_input.shape),
        oc[0, :part], oc[1, :part], oq, ok, ov, oo, oc[2, :part], og, ou, ob,
    )


def solution(mesh):
    rows = P(None, ("rep", "fsdp"), None)
    vector, matrix = P("fsdp"), P("fsdp", None)
    return jax.shard_map(
        partial(per_device, mesh.shape["fsdp"]),
        mesh=mesh,
        in_specs=(rows, rows, P(None, ("rep", "fsdp")), vector, vector, matrix, matrix, matrix, matrix,
                  vector, matrix, matrix, matrix),
        out_specs=(rows, rows, vector, vector, matrix, matrix, matrix, matrix, vector, matrix, matrix, matrix),
        check_vma=False,
    )
```

```python
from functools import partial

import jax
import jax.numpy as jnp
from jax import lax
from jax.experimental import pallas as pl
from jax.experimental.pallas import tpu as pltpu
from jax.sharding import PartitionSpec as P

H = 12
DH = 64
RADIUS = 127
GBLK = 16
BLK = 64
SLOTS = 10
MAX_SEQ_BLOCKS = 5
EPSILON = 1e-06
MASKED_SCORE = -1e30
MESH = pl.DeviceIdType.MESH
VMEM_LIMIT = 60 * 1024 * 1024
SEG_AT, LEN_AT, DEST_AT, TABLE_SIZE = 40, 80, 120, 256

ANY = pl.BlockSpec(memory_space=pl.ANY)
VMEM = pl.BlockSpec(memory_space=pltpu.VMEM)
SMEM = pl.BlockSpec(memory_space=pltpu.SMEM)


def grid_of(count):
    inner = 2 if count <= 8 else 4
    return count // inner, inner


def core_of(rank):
    return rank + 1 - 2 * (rank % 2)


def across_of(rank):
    return (rank + 2) % 4


def lens_kernel(lens_ref, all_ref, send_sem, recv_sem):
    rank = lax.axis_index("rep")
    barrier = pltpu.get_barrier_semaphore()
    for step in range(1, 4):
        pl.semaphore_signal(
            barrier, inc=1, device_id={"rep": (rank + step) % 4}, device_id_type=MESH
        )
    pl.semaphore_wait(barrier, 3)
    copies = []
    for step in range(1, 4):
        copy = pltpu.make_async_remote_copy(
            src_ref=lens_ref,
            dst_ref=all_ref.at[rank],
            send_sem=send_sem.at[step - 1],
            recv_sem=recv_sem.at[step - 1],
            device_id={"rep": (rank + step) % 4},
            device_id_type=MESH,
        )
        copy.start()
        copies.append(copy)
    all_ref[rank] = lens_ref[...]
    for copy in copies:
        copy.wait()


def table_kernel(micro, per_dev, lens_ref, tab_ref, order_ref, count_ref, load_ref):
    total = 4 * micro * per_dev

    def length_at(spot):
        return lens_ref[spot // (micro * per_dev), (spot // per_dev) % micro, spot % per_dev]

    def blocks_of(length):
        return (length + (BLK - 1)) // BLK

    def clear(spot, carry):
        tab_ref[spot] = -1
        return carry

    lax.fori_loop(0, TABLE_SIZE, clear, 0)
    for spot in range(4 * SLOTS):
        tab_ref[LEN_AT + spot] = 0
    for size in range(8):
        count_ref[size] = 0
    for dev in range(4):
        load_ref[dev] = 0

    def tally(spot, carry):
        length = length_at(spot)

        @pl.when(length > 0)
        def _():
            size = blocks_of(length)
            count_ref[size] = count_ref[size] + 1

        return carry

    lax.fori_loop(0, total, tally, 0)
    begin = 0
    for size in range(MAX_SEQ_BLOCKS, 0, -1):
        amount = count_ref[size]
        count_ref[size] = begin
        begin = begin + amount

    def place(spot, carry):
        length = length_at(spot)

        @pl.when(length > 0)
        def _():
            size = blocks_of(length)
            where = count_ref[size]
            order_ref[where] = spot
            count_ref[size] = where + 1

        return carry

    lax.fori_loop(0, total, place, 0)

    def assign(number, carry):
        spot = order_ref[number]
        length = length_at(spot)
        size = blocks_of(length)
        best = jnp.int32(0)
        low = load_ref[0]
        for dev in range(1, 4):
            here = load_ref[dev]
            best = jnp.where(here < low, dev, best)
            low = jnp.minimum(here, low)
        load_ref[best] = low + size

        def put(step, inner):
            slot = best * SLOTS + low + step
            tab_ref[slot] = spot + step
            tab_ref[SEG_AT + slot] = low
            tab_ref[LEN_AT + slot] = jnp.minimum(length - BLK * step, BLK)
            tab_ref[DEST_AT + spot + step] = slot
            return inner

        lax.fori_loop(0, size, put, 0)
        return carry

    lax.fori_loop(0, begin, assign, 0)


def deal_table(lengths):
    micro, per_dev = lengths.shape
    padded = jnp.pad(lengths, ((0, 8 - micro), (0, 128 - per_dev)))
    everyone = pl.pallas_call(
        lens_kernel,
        out_shape=jax.ShapeDtypeStruct((4, 8, 128), jnp.int32),
        in_specs=[VMEM],
        out_specs=VMEM,
        scratch_shapes=[pltpu.SemaphoreType.DMA((3,)), pltpu.SemaphoreType.DMA((3,))],
        compiler_params=pltpu.CompilerParams(collective_id=0, has_side_effects=True),
        name="lens_exchange",
    )(padded)
    return pl.pallas_call(
        partial(table_kernel, micro, per_dev),
        out_shape=jax.ShapeDtypeStruct((TABLE_SIZE,), jnp.int32),
        in_specs=[SMEM],
        out_specs=SMEM,
        scratch_shapes=[
            pltpu.SMEM((4 * micro * per_dev,), jnp.int32),
            pltpu.SMEM((8,), jnp.int32),
            pltpu.SMEM((4,), jnp.int32),
        ],
        name="deal_table",
    )(everyone)


def gather_kernel(
    outer, inner, splits, tab_ref, rows_ref, cots_ref, wa_ref, wb_ref, wc_ref,
    ga_ref, gb_ref, gc_ref, rows_out, cots_out,
    psend, precv, xsend, xrecv,
    z_send, z_recv, y_send, y_recv, c_send, c_recv, own_sem,
    p_send, p_recv, x_send, x_recv,
):
    rank = lax.axis_index("rep")
    spot = lax.axis_index("fsdp")
    core = rank % 2
    row, col = spot // inner, spot % inner
    count = outer * inner
    mate, across = core_of(rank), across_of(rank)
    pieces = [(wa_ref, ga_ref, start, width // 2) for start, width in splits]
    pieces.append((wb_ref, gb_ref, 0, wb_ref.shape[1] // 2))
    pieces.append((wc_ref, gc_ref, 0, None))
    halved = [number for number, piece in enumerate(pieces) if piece[3] is not None]

    barrier = pltpu.get_barrier_semaphore()
    neighbours = (
        (row + 1 < outer, {"fsdp": spot + inner}),
        (row > 0, {"fsdp": spot - inner}),
        (col + 1 < inner, {"fsdp": spot + 1}),
        (col > 0, {"fsdp": spot - 1}),
    )
    amount = jnp.int32(2)
    for there, device in neighbours:
        amount = amount + there.astype(jnp.int32)

        @pl.when(there)
        def _():
            pl.semaphore_signal(barrier, inc=1, device_id=device, device_id_type=MESH)

    for device in (mate, across):
        pl.semaphore_signal(barrier, inc=1, device_id={"rep": device}, device_id_type=MESH)
    pl.semaphore_wait(barrier, amount)

    def cut(ref, number):
        _, _, start, half = pieces[number]
        if half is None:
            return ref
        return ref.at[:, pl.ds(pl.multiple_of(start + core * half, 128), half)]

    def landed(number, shard):
        return cut(pieces[number][1].at[shard], number)

    late = []

    def send(there, src, dst, ssem, rsem, device):
        def describe():
            return pltpu.make_async_remote_copy(
                src_ref=src, dst_ref=dst, send_sem=ssem, recv_sem=rsem,
                device_id=device, device_id_type=MESH,
            )

        if there is None:
            describe().start()
            late.append((None, lambda: describe().wait_send()))
        else:
            @pl.when(there)
            def _():
                describe().start()

            late.append((there, lambda: describe().wait_send()))

    def arrive(number, shard, rsem):
        pltpu.make_async_remote_copy(
            src_ref=landed(number, shard), dst_ref=landed(number, shard),
            send_sem=own_sem.at[0], recv_sem=rsem,
            device_id={"rep": mate}, device_id_type=MESH,
        ).wait_recv()

    def both(first, second):
        return second if first is None else jnp.logical_and(first, second)

    def to_mate(there, number, shard):
        if number not in halved:
            return
        place = landed(number, shard)
        send(there, place, place, c_send.at[number, shard], c_recv.at[number, shard], {"rep": mate})

    def along_row(there, number, line, src):
        shard = line * inner + col
        place = landed(number, shard)
        src = place if src is None else src
        send(both(there, col + 1 < inner), src, place,
             y_send.at[0, 0, line, number], y_recv.at[0, 0, line, number], {"fsdp": spot + 1})
        send(both(there, col > 0), src, place,
             y_send.at[1, 0, line, number], y_recv.at[1, 0, line, number], {"fsdp": spot - 1})

    def from_row(there, number, line):
        for step in range(inner - 1):
            for way, source, onward, target in (
                (0, col - 1 - step, col + 1 < inner, spot + 1),
                (1, col + 1 + step, col > 0, spot - 1),
            ):
                here = jnp.logical_and(source >= 0, source < inner)
                here = both(there, here)
                shard = line * inner + source

                @pl.when(here)
                def _():
                    arrive(number, shard, y_recv.at[way, step, line, number])

                if step + 1 < inner - 1:
                    place = landed(number, shard)
                    send(both(here, onward), place, place,
                         y_send.at[way, step + 1, line, number],
                         y_recv.at[way, step + 1, line, number], {"fsdp": target})
                to_mate(here, number, shard)

    for number, piece in enumerate(pieces):
        src, place = cut(piece[0], number), landed(number, spot)
        send(row + 1 < outer, src, place, z_send.at[0, 0, number], z_recv.at[0, 0, number],
             {"fsdp": spot + inner})
        send(row > 0, src, place, z_send.at[1, 0, number], z_recv.at[1, 0, number],
             {"fsdp": spot - inner})
        along_row(None, number, row, src)
    own = [
        pltpu.make_async_copy(wa_ref, ga_ref.at[spot], own_sem.at[0]),
        pltpu.make_async_copy(wb_ref, gb_ref.at[spot], own_sem.at[1]),
        pltpu.make_async_copy(wc_ref, gc_ref.at[spot], own_sem.at[2]),
    ]
    for copy in own:
        copy.start()

    sources = (rows_ref, cots_ref)
    per_rank = rows_ref.shape[0]

    def picked(kind, target, slot):
        index = tab_ref[target * SLOTS + slot] - rank * per_rank
        mine = jnp.logical_and(index >= 0, index < per_rank)
        value = sources[kind][jnp.clip(index, 0, per_rank - 1)]
        return mine, value

    def mate_copy(kind, part):
        return pltpu.make_async_remote_copy(
            src_ref=psend.at[kind, part], dst_ref=precv.at[kind, part],
            send_sem=p_send.at[kind, part], recv_sem=p_recv.at[kind, part],
            device_id={"rep": mate}, device_id_type=MESH,
        )

    def across_copy(kind):
        return pltpu.make_async_remote_copy(
            src_ref=xsend.at[kind], dst_ref=xrecv.at[kind],
            send_sem=x_send.at[kind], recv_sem=x_recv.at[kind],
            device_id={"rep": across}, device_id_type=MESH,
        )

    for kind, part in ((0, 1), (1, 1), (0, 0), (1, 0)):
        target = mate if part == 0 else across_of(mate)

        def pack(slot, carry):
            mine, value = picked(kind, target, slot)
            psend[kind, part, slot] = jnp.where(mine, value, jnp.zeros_like(value))
            return carry

        lax.fori_loop(0, SLOTS, pack, 0)
        mate_copy(kind, part).start()
    for kind in range(2):
        mate_copy(kind, 1).wait_recv()

        def merge(slot, carry):
            mine, value = picked(kind, across, slot)
            xsend[kind, slot] = jnp.where(mine, value, precv[kind, 1, slot])
            return carry

        lax.fori_loop(0, SLOTS, merge, 0)
        across_copy(kind).start()

    def lines(step):
        return ((row - 1 - step >= 0, row - 1 - step, 0, row + 1 < outer, spot + inner),
                (row + 1 + step < outer, row + 1 + step, 1, row > 0, spot - inner))

    for step in range(outer - 1):
        for number in range(len(pieces)):
            for here, line, way, onward, target in lines(step):
                shard = line * inner + col

                @pl.when(here)
                def _():
                    arrive(number, shard, z_recv.at[way, step, number])

                if step + 1 < outer - 1:
                    place = landed(number, shard)
                    send(jnp.logical_and(here, onward), place, place,
                         z_send.at[way, step + 1, number], z_recv.at[way, step + 1, number],
                         {"fsdp": target})
                along_row(here, number, line, None)
                to_mate(here, number, shard)
        for number in range(len(pieces)):
            if step == 0:
                from_row(None, number, row)
            else:
                for here, line, *_ in lines(step - 1):
                    from_row(here, number, line)
    for number in range(len(pieces)):
        for here, line, *_ in lines(outer - 2):
            from_row(here, number, line)

    outs = (rows_out, cots_out)
    for kind in range(2):
        mate_copy(kind, 0).wait_recv()
        across_copy(kind).wait_recv()

        def finish(slot, carry):
            mine, value = picked(kind, rank, slot)
            outs[kind][slot] = jnp.where(mine, value, precv[kind, 0, slot] + xrecv[kind, slot])
            return carry

        lax.fori_loop(0, SLOTS, finish, 0)

    for shard in range(count):
        @pl.when(shard != spot)
        def _():
            for number in halved:
                other = pieces[number]
                view = other[1].at[shard].at[:, pl.ds(0, other[3])]
                pltpu.make_async_remote_copy(
                    src_ref=view, dst_ref=view, send_sem=own_sem.at[0],
                    recv_sem=c_recv.at[number, shard],
                    device_id={"rep": mate}, device_id_type=MESH,
                ).wait_recv()
    for there, finish_send in late:
        if there is None:
            finish_send()
        else:
            pl.when(there)(finish_send)
    for kind in range(2):
        for part in range(2):
            mate_copy(kind, part).wait_send()
        across_copy(kind).wait_send()
    for copy in own:
        copy.wait()


def gather_weights(count, splits, table, rows, cots, wa, wb, wc):
    outer, inner = grid_of(count)
    block = rows.shape[1:]
    kinds = len(splits) + 2
    dma = pltpu.SemaphoreType.DMA
    bf16 = jnp.bfloat16
    return pl.pallas_call(
        partial(gather_kernel, outer, inner, splits),
        out_shape=(
            jax.ShapeDtypeStruct((count,) + wa.shape, bf16),
            jax.ShapeDtypeStruct((count,) + wb.shape, bf16),
            jax.ShapeDtypeStruct((count,) + wc.shape, bf16),
            jax.ShapeDtypeStruct((SLOTS,) + block, bf16),
            jax.ShapeDtypeStruct((SLOTS,) + block, bf16),
        ),
        in_specs=[SMEM, VMEM, VMEM, VMEM, VMEM, VMEM],
        out_specs=(ANY, ANY, ANY, VMEM, VMEM),
        scratch_shapes=[
            pltpu.VMEM((2, 2, SLOTS) + block, bf16),
            pltpu.VMEM((2, 2, SLOTS) + block, bf16),
            pltpu.VMEM((2, SLOTS) + block, bf16),
            pltpu.VMEM((2, SLOTS) + block, bf16),
            dma((2, outer - 1, kinds)), dma((2, outer - 1, kinds)),
            dma((2, inner - 1, outer, kinds)), dma((2, inner - 1, outer, kinds)),
            dma((kinds, count)), dma((kinds, count)), dma((3,)),
            dma((2, 2)), dma((2, 2)), dma((2,)), dma((2,)),
        ],
        compiler_params=pltpu.CompilerParams(
            collective_id=1, has_side_effects=True, vmem_limit_bytes=VMEM_LIMIT
        ),
        name="gather_and_deal",
    )(table, rows, cots, wa, wb, wc)


def reduce_kernel(
    outer, inner, kinds, *refs
):
    grads, (y_ref, g_ref) = refs[:kinds], refs[kinds : kinds + 2]
    totals, (ry_ref, rg_ref) = refs[kinds + 2 : 2 * kinds + 2], refs[2 * kinds + 2 : 2 * kinds + 4]
    scratch = refs[2 * kinds + 4 :]
    mines, crecvs, yrecvs, zrecvs, xrecvs = (
        scratch[kinds * i : kinds * (i + 1)] for i in range(5)
    )
    (c_send, c_recv, m_sem, y_send, y_recv, z_send, z_recv, x_send, x_recv, f_send, f_recv,
     r_send, r_recv, q_sem) = scratch[5 * kinds :]
    rank = lax.axis_index("rep")
    spot = lax.axis_index("fsdp")
    core = rank % 2
    row, col = spot // inner, spot % inner
    mate, across = core_of(rank), across_of(rank)
    pieces = [(src, dst, 0, src.shape[3] // 2) for src, dst in zip(grads[:-1], totals)]
    pieces.append((grads[-1], totals[-1], 0, None))

    barrier = pltpu.get_barrier_semaphore()
    neighbours = (
        (row + 1 < outer, {"fsdp": spot + inner}),
        (row > 0, {"fsdp": spot - inner}),
        (col + 1 < inner, {"fsdp": spot + 1}),
        (col > 0, {"fsdp": spot - 1}),
    )
    amount = jnp.int32(2)
    for there, device in neighbours:
        amount = amount + there.astype(jnp.int32)

        @pl.when(there)
        def _():
            pl.semaphore_signal(barrier, inc=1, device_id=device, device_id_type=MESH)

    for device in (mate, across):
        pl.semaphore_signal(barrier, inc=1, device_id={"rep": device}, device_id_type=MESH)
    pl.semaphore_wait(barrier, amount)

    late = []

    def send(there, src, dst, ssem, rsem, device):
        def describe():
            return pltpu.make_async_remote_copy(
                src_ref=src, dst_ref=dst, send_sem=ssem, recv_sem=rsem,
                device_id=device, device_id_type=MESH,
            )

        if there is None:
            describe().start()
            late.append((None, lambda: describe().wait_send()))
        else:
            @pl.when(there)
            def _():
                describe().start()

            late.append((there, lambda: describe().wait_send()))

    def arrive(place, rsem):
        pltpu.make_async_remote_copy(
            src_ref=place, dst_ref=place, send_sem=q_sem.at[0], recv_sem=rsem,
            device_id={"rep": mate}, device_id_type=MESH,
        ).wait_recv()

    def columns(ref, number, which):
        _, _, start, half = pieces[number]
        if half is None:
            return ref
        cols = pl.ds(pl.multiple_of(start + which * half, 128), half)
        return ref.at[:, :, :, cols] if len(ref.shape) == 4 else ref.at[:, cols]

    order = list(range(kinds))
    loads = []
    for number in order:
        src = columns(pieces[number][0], number, 1 - core)
        send(None, src, crecvs[number], c_send.at[number], c_recv.at[number], {"rep": mate})
        load = pltpu.make_async_copy(
            columns(pieces[number][0], number, core), mines[number], m_sem.at[number]
        )
        load.start()
        loads.append(load)

    for kind, (src, dst) in enumerate(((y_ref, ry_ref), (g_ref, rg_ref))):
        send(None, src, dst.at[rank], r_send.at[kind, 0], r_recv.at[kind, 0], {"rep": across})
        send(None, src, dst.at[rank], r_send.at[kind, 1], r_recv.at[kind, 1], {"rep": mate})
        pltpu.make_async_copy(src, dst.at[rank], q_sem.at[kind + 1]).start()

    def slot_of(way, size, place, dest):
        if size == 2:
            return 0
        return dest - place if way == 0 else size - place + dest

    def line_sum(number, size, place, stride, buffer, view, ssem, rsem):
        for far in range(size - 1, 0, -1):
            for way in range(2):
                dest = far if way == 0 else size - 1 - far
                step = 1 if way == 0 else -1
                passes = place < dest if way == 0 else place > dest
                first = place == 0 if way == 0 else place == size - 1
                mine = view(dest)
                got = slot_of(way, size, place, dest)

                @pl.when(jnp.logical_and(passes, jnp.logical_not(first)))
                def _():
                    arrive(buffer.at[got], rsem.at[got, number])
                    mine[...] = mine[...] + buffer[got]

                put = slot_of(way, size, place + step, dest)
                send(passes, mine, buffer.at[put], ssem.at[way, dest, number], rsem.at[put, number],
                     {"fsdp": spot + step * stride})
        for way in range(2):
            has = place > 0 if way == 0 else place < size - 1
            got = slot_of(way, size, place, place)
            mine = view(place)

            @pl.when(has)
            def _():
                arrive(buffer.at[got], rsem.at[got, number])
                mine[...] = mine[...] + buffer[got]

    for number in order:
        loads[number].wait()
        arrive(crecvs[number], c_recv.at[number])
        mine, other = mines[number], crecvs[number]

        def add(index, carry):
            mine[index // inner, index % inner] = (
                mine[index // inner, index % inner] + other[index // inner, index % inner]
            )
            return carry

        lax.fori_loop(0, outer * inner, add, 0)
        if inner == 2:
            send(None, mine.at[:, 1 - col], yrecvs[number].at[0], y_send.at[0, 0, number],
                 y_recv.at[0, number], {"fsdp": spot + 1 - 2 * col})
    for kind, dst in enumerate((ry_ref, rg_ref)):
        place = dst.at[across]
        arrive(place, r_recv.at[kind, 0])
        send(None, place, place, r_send.at[kind, 2], r_recv.at[kind, 2], {"rep": mate})
    for number in order:
        mine = mines[number]
        if inner == 2:
            arrive(yrecvs[number].at[0], y_recv.at[0, number])
            buffer = yrecvs[number]

            def add(index, carry):
                mine[index, col] = mine[index, col] + buffer[0, index]
                return carry

            lax.fori_loop(0, outer, add, 0)
        else:
            line_sum(number, inner, col, 1, yrecvs[number], lambda dest: mine.at[:, dest],
                     y_send, y_recv)
        line_sum(number, outer, row, inner, zrecvs[number], lambda dest: mine.at[dest, col],
                 z_send, z_recv)
        send(None, mine.at[row, col], xrecvs[number], x_send.at[number], x_recv.at[number],
             {"rep": across})
    for number in order:
        arrive(xrecvs[number], x_recv.at[number])
        total = mines[number][row, col].astype(jnp.float32) + xrecvs[number][...].astype(jnp.float32)
        out, half = pieces[number][1], pieces[number][3]
        place = columns(out, number, core)
        place[...] = total
        if half is not None:
            send(None, place, place, f_send.at[number], f_recv.at[number], {"rep": mate})
    for number in order:
        if pieces[number][3] is not None:
            arrive(columns(pieces[number][1], number, 1 - core), f_recv.at[number])
    for kind, dst in enumerate((ry_ref, rg_ref)):
        arrive(dst.at[mate], r_recv.at[kind, 1])
        arrive(dst.at[across_of(mate)], r_recv.at[kind, 2])
        src = y_ref if kind == 0 else g_ref
        pltpu.make_async_copy(src, dst.at[rank], q_sem.at[kind + 1]).wait()
    for there, finish_send in late:
        if there is None:
            finish_send()
        else:
            pl.when(there)(finish_send)


def reduce_grads(count, grads, y_rows, g_rows):
    outer, inner = grid_of(count)
    kinds = len(grads)
    shapes = [(grad.shape[1], grad.shape[2] // 2, grad.dtype) for grad in grads[:-1]]
    shapes.append(grads[-1].shape[1:] + (grads[-1].dtype,))
    dma = pltpu.SemaphoreType.DMA
    y_slots = 1 if inner == 2 else inner + 1
    z_slots = 1 if outer == 2 else outer + 1
    scratch = []
    for lead in ((outer, inner), (outer, inner), (y_slots, outer), (z_slots,), ()):
        scratch += [pltpu.VMEM(lead + (a, b), dtype) for a, b, dtype in shapes]
    scratch += [
        dma((kinds,)), dma((kinds,)), dma((kinds,)),
        dma((2, inner, kinds)), dma((y_slots, kinds)),
        dma((2, outer, kinds)), dma((z_slots, kinds)),
        dma((kinds,)), dma((kinds,)), dma((kinds,)), dma((kinds,)),
        dma((2, 3)), dma((2, 3)), dma((3,)),
    ]
    return pl.pallas_call(
        partial(reduce_kernel, outer, inner, kinds),
        out_shape=tuple(jax.ShapeDtypeStruct(grad.shape[1:], jnp.float32) for grad in grads) + (
            jax.ShapeDtypeStruct((4,) + y_rows.shape, y_rows.dtype),
            jax.ShapeDtypeStruct((4,) + g_rows.shape, g_rows.dtype),
        ),
        in_specs=[ANY] * (kinds + 2),
        out_specs=(VMEM,) * kinds + (ANY, ANY),
        scratch_shapes=scratch,
        compiler_params=pltpu.CompilerParams(
            collective_id=2, has_side_effects=True, vmem_limit_bytes=VMEM_LIMIT
        ),
        name="reduce_and_return",
    )(*(grad.reshape((outer, inner) + grad.shape[1:]) for grad in grads), y_rows, g_rows)


def home_kernel(tab_ref, ry_ref, rg_ref, y_ref, g_ref):
    base = lax.axis_index("rep") * y_ref.shape[0]

    def fetch(block, carry):
        index = tab_ref[DEST_AT + base + block] if len(tab_ref.shape) == 1 else tab_ref[48, base + block]
        safe = jnp.maximum(index, 0)
        for src, dst in ((ry_ref, y_ref), (rg_ref, g_ref)):
            value = src[safe // SLOTS, safe % SLOTS]
            dst[block] = jnp.where(index >= 0, value, jnp.zeros_like(value))
        return carry

    lax.fori_loop(0, y_ref.shape[0], fetch, 0)


def bring_home(table, ry, rg, blocks):
    shape = jax.ShapeDtypeStruct((blocks,) + ry.shape[2:], ry.dtype)
    return pl.pallas_call(
        home_kernel,
        out_shape=(shape, shape),
        in_specs=[SMEM, VMEM, VMEM],
        out_specs=(VMEM, VMEM),
        compiler_params=pltpu.CompilerParams(vmem_limit_bytes=VMEM_LIMIT),
        name="place_rows",
    )(table, ry, rg)


D = H * DH
ROWS = SLOTS * BLK
SIDES = SLOTS * (BLK // GBLK)
SIDE_ROWS = 48
ALL_ROWS = ROWS + SIDE_ROWS
QT = 128
WIN = 384
TILES = ROWS // QT
QUAD = 256
FF_TILE = 256
GELU_C = 0.7978845608028654
GELU_A = 0.044715
F32, BF16 = jnp.float32, jnp.bfloat16


def mm(left, right):
    return lax.dot_general(left, right, (((1,), (0,)), ((), ())), preferred_element_type=F32)


def mm_cols(left, right):
    return lax.dot_general(left, right, (((1,), (1,)), ((), ())), preferred_element_type=F32)


def mm_rows(left, right):
    return lax.dot_general(left, right, (((0,), (0,)), ((), ())), preferred_element_type=F32)


def iota(shape, axis):
    return lax.broadcasted_iota(jnp.int32, shape, axis)


def pick_by(index, values, other):
    out = jnp.full(index.shape, other, jnp.int32)
    for number, value in enumerate(values):
        out = jnp.where(index == number, value, out)
    return out


def block_at(tab_ref, slot):
    return lax.rem(tab_ref[slot, 0], 128) - 1


def seg_at(tab_ref, slot):
    if len(tab_ref.shape) == 1:
        return tab_ref[SEG_AT + slot]
    return lax.div(tab_ref[slot, 0], 16384) - 1


def len_at(tab_ref, slot):
    if len(tab_ref.shape) == 1:
        return tab_ref[LEN_AT + slot]
    return lax.rem(lax.div(tab_ref[slot, 0], 128), 128)


def slot_info(tab_ref, rank):
    seg = [seg_at(tab_ref, rank * SLOTS + slot) for slot in range(SLOTS)]
    length = [len_at(tab_ref, rank * SLOTS + slot) for slot in range(SLOTS)]
    return seg, length


def valid_column(tab_ref, rank):
    _, length = slot_info(tab_ref, rank)
    row = iota((ROWS, 1), 0)
    return ((row % BLK) < pick_by(row // BLK, length, 0)).astype(F32)


def pooling(tab_ref, rank):
    _, length = slot_info(tab_ref, rank)
    row = iota((1, ROWS), 1)
    block = jnp.where((row % BLK) < pick_by(row // BLK, length, 0), row // GBLK, -1)
    return jnp.where(iota((SIDE_ROWS, ROWS), 0) == block, 1.0, 0.0).astype(BF16)


def key_segments(tab_ref, rank, first_block, index):
    blocks = WIN // BLK
    base = rank * SLOTS + first_block
    seg = [seg_at(tab_ref, base + step) for step in range(blocks)]
    length = [len_at(tab_ref, base + step) for step in range(blocks)]
    alive = (index % BLK) < pick_by(index // BLK, length, 0)
    return jnp.where(alive, pick_by(index // BLK, seg, -2), -2)


def side_segments(tab_ref, rank, index):
    seg, length = slot_info(tab_ref, rank)
    per = BLK // GBLK
    alive = (index % per) * GBLK < pick_by(index // per, length, 0)
    return jnp.where(alive, pick_by(index // per, seg, -2), -2)


def tile_bias(tab_ref, rank, tile, first_row, keys_axis):
    qs, ks, gs = ((QT, 1), (1, WIN), (1, SIDE_ROWS)) if keys_axis == 1 else ((1, QT), (WIN, 1), (SIDE_ROWS, 1))
    q_index = iota(qs, 1 - keys_axis)
    k_index = iota(ks, keys_axis)
    g_index = iota(gs, keys_axis)
    base = rank * SLOTS + tile * (QT // BLK)
    q_seg = pick_by(q_index // BLK, [seg_at(tab_ref, base + step) for step in range(QT // BLK)], -1)
    k_seg = key_segments(tab_ref, rank, first_row // BLK, k_index)
    g_seg = side_segments(tab_ref, rank, g_index)
    gap = (q_index + tile * QT) - (k_index + first_row)
    local = (jnp.abs(gap) <= RADIUS) & (q_seg == k_seg)
    return jnp.where(local, 0.0, MASKED_SCORE), jnp.where(q_seg == g_seg, 0.0, MASKED_SCORE)


def window_start(tile):
    return pl.multiple_of(jnp.clip(tile - 1, 0, TILES - WIN // QT) * QT, QT)


def head_stack(rows):
    lane = iota(rows.shape, 1) // DH
    zero = jnp.zeros_like(rows)
    return jnp.concatenate([jnp.where(lane == head, rows, zero) for head in range(QUAD // DH)], axis=0)


def head_merge(stacked):
    lane = iota((QT, QUAD), 1) // DH
    out = stacked[:QT]
    for head in range(1, QUAD // DH):
        out = jnp.where(lane == head, stacked[head * QT : (head + 1) * QT], out)
    return out


def gains_of(gc_ref):
    count = gc_ref.shape[0]
    part = D // count
    lane, column = iota((128, D), 0), iota((128, D), 1)
    total = None
    for shard in range(count):
        pick = jnp.where((column == lane + shard * part) & (lane < part), 1.0, 0.0).astype(BF16)
        term = mm(gc_ref[shard], pick)
        total = term if total is None else total + term
    return total


def three_way(value):
    high = value.astype(BF16)
    rest = value - high.astype(F32)
    middle = rest.astype(BF16)
    return high, middle, (rest - middle.astype(F32)).astype(BF16)


def spread_gain_grads(value, dc_ref):
    count = dc_ref.shape[0] if len(dc_ref.shape) == 3 else dc_ref.shape[0] * dc_ref.shape[1]
    part = D // count
    column, lane = iota((D, 128), 0), iota((D, 128), 1)
    parts = three_way(value)
    for shard in range(count):
        pick = jnp.where((column == lane + shard * part) & (lane < part), 1.0, 0.0).astype(BF16)
        place = dc_ref.at[shard] if len(dc_ref.shape) == 3 else dc_ref.at[shard // dc_ref.shape[1], shard % dc_ref.shape[1]]
        place[...] = mm(parts[0], pick) + mm(parts[1], pick) + mm(parts[2], pick)


def mean_square(value):
    return jnp.mean(value * value, axis=-1, keepdims=True)


def forward_norm(tab_ref, rank, x_ref, gains, n_ref):
    for tile in range(TILES):
        rows = pl.ds(tile * QT, QT)
        value = x_ref[rows, :].astype(F32)
        n_ref[rows, :] = (value * lax.rsqrt(mean_square(value) + EPSILON) * gains[0:1]).astype(BF16)
    side = mm(pooling(tab_ref, rank), n_ref[:ROWS, :])
    n_ref[ROWS:, :] = (side * lax.rsqrt(mean_square(side) + EPSILON) * gains[1:2]).astype(BF16)


def forward_project(n_ref, w_ref, qkv_ref):
    def step(tile, carry):
        cols = pl.ds(pl.multiple_of(tile * QUAD, QUAD), QUAD)
        qkv_ref[:, cols] = mm(n_ref[...], w_ref[:, cols]).astype(BF16)
        return carry

    lax.fori_loop(0, 3 * D // QUAD, step, 0)


def forward_attention(tab_ref, rank, qkv_ref, att_ref, lse_ref, begin, end):
    heads = QUAD // DH

    def step(tile, carry):
        first = window_start(tile)
        bias, side_bias = tile_bias(tab_ref, rank, tile, first, 1)
        rows = pl.ds(pl.multiple_of(tile * QT, QT), QT)
        window = pl.ds(first, WIN)
        lane = iota((QT, 128), 1)

        def four(quad, lse):
            low = pl.multiple_of(quad * QUAD, QUAD)
            cols, key_cols, value_cols = (pl.ds(low + number * D, QUAD) for number in range(3))
            query = head_stack(qkv_ref[rows, cols])
            scores = mm_cols(query, qkv_ref[window, key_cols])
            side_scores = mm_cols(query, qkv_ref[ROWS:, key_cols])
            local, sides, scale = [], [], []
            for head in range(heads):
                part = slice(head * QT, (head + 1) * QT)
                one = scores[part] + bias
                two = side_scores[part] + side_bias
                peak = jnp.maximum(
                    jnp.max(one, axis=-1, keepdims=True), jnp.max(two, axis=-1, keepdims=True)
                )
                one, two = jnp.exp(one - peak), jnp.exp(two - peak)
                total = jnp.sum(one, axis=-1, keepdims=True) + jnp.sum(two, axis=-1, keepdims=True)
                local.append(one.astype(BF16))
                sides.append(two.astype(BF16))
                scale.append(1.0 / total)
                lse = jnp.where(lane == quad * heads + head, peak + jnp.log(total), lse)
            mixed = mm(jnp.concatenate(local, axis=0), qkv_ref[window, value_cols])
            mixed = mixed + mm(jnp.concatenate(sides, axis=0), qkv_ref[ROWS:, value_cols])
            mixed = mixed * jnp.concatenate(scale, axis=0)
            att_ref[rows, cols] = head_merge(mixed).astype(BF16)
            return lse

        lse = lax.fori_loop(0, D // QUAD, four, jnp.zeros((QT, 128), F32))
        lse_ref[tile] = jnp.transpose(lse)[:16]
        return carry

    lax.fori_loop(begin, end, step, 0)


def feed_forward(tab_ref, rank, x_ref, cot_ref, att_ref, gains, w_ref, wb_ref,
                 y_ref, gh_ref, ga_ref, dg_ref, du_ref, db_ref, do_ref,
                 h1_ref, nt_ref, ntt_ref, gres_ref, h2_ref, gg_ref, gu_ref, gn_ref):
    hidden = wb_ref.shape[0]
    gate_at = w_ref.shape[1] - 2 * hidden
    out_at = gate_at - D
    valid = valid_column(tab_ref, rank)
    gain = gains[2:3]
    for tile in range(TILES):
        rows = pl.ds(tile * QT, QT)
        value = x_ref[rows, :].astype(F32) + mm(att_ref[rows, :], w_ref[:, out_at:gate_at])
        h1_ref[rows, :] = value
        normed = (value * lax.rsqrt(mean_square(value) + EPSILON) * gain).astype(BF16)
        nt_ref[rows, :] = normed
        ntt_ref[:, tile * QT : (tile + 1) * QT] = jnp.transpose(normed)
        gres_ref[rows, :] = (cot_ref[rows, :].astype(F32) * valid[tile * QT : (tile + 1) * QT]).astype(BF16)

    def inward(tile, carry):
        at = pl.multiple_of(tile * FF_TILE, FF_TILE)
        cols = pl.ds(at, FF_TILE)
        gate = mm(nt_ref[...], w_ref[:, pl.ds(gate_at + at, FF_TILE)])
        up = mm(nt_ref[...], w_ref[:, pl.ds(gate_at + hidden + at, FF_TILE)])
        back = mm_cols(gres_ref[...], wb_ref[cols, :])
        square = gate * gate
        bend = jnp.tanh(GELU_C * (gate * (1.0 + GELU_A * square)))
        half = 0.5 * (1.0 + bend)
        act = gate * half
        slope = half + (0.5 * GELU_C) * gate * (1.0 - bend * bend) * (1.0 + (3.0 * GELU_A) * square)
        h2_ref[:, cols] = (act * up).astype(BF16)
        gg_ref[:, cols] = (back * up * slope).astype(BF16)
        gu_ref[:, cols] = (back * act).astype(BF16)
        return carry

    lax.fori_loop(0, hidden // FF_TILE, inward, 0)

    def outward(tile, carry):
        cols = pl.ds(pl.multiple_of(tile * QUAD, QUAD), QUAD)
        value = h1_ref[:, cols] + mm(h2_ref[...], wb_ref[:, cols])
        y_ref[:, cols] = (value * valid).astype(BF16)
        gn_ref[:, cols] = mm_cols(gg_ref[...], w_ref[cols, gate_at : gate_at + hidden]) + mm_cols(
            gu_ref[...], w_ref[cols, gate_at + hidden :]
        )
        return carry

    lax.fori_loop(0, D // QUAD, outward, 0)

    def weights(tile, carry):
        at = pl.multiple_of(tile * FF_TILE, FF_TILE)
        cols = pl.ds(at, FF_TILE)
        dg_ref[:, cols] = mm(ntt_ref[...], gg_ref[:, cols]).astype(BF16)
        du_ref[:, cols] = mm(ntt_ref[...], gu_ref[:, cols]).astype(BF16)
        db_ref[cols, :] = mm_rows(h2_ref[:, cols], gres_ref[...]).astype(BF16)
        return carry

    lax.fori_loop(0, hidden // FF_TILE, weights, 0)

    gain_grad = jnp.zeros((1, D), F32)
    for tile in range(TILES):
        rows = pl.ds(tile * QT, QT)
        value, grad = h1_ref[rows, :], gn_ref[rows, :]
        root = lax.rsqrt(mean_square(value) + EPSILON)
        unit = value * root
        gain_grad = gain_grad + jnp.sum(grad * unit, axis=0, keepdims=True)
        grad = grad * gain
        grad = gres_ref[rows, :].astype(F32) + root * (
            grad - unit * jnp.mean(grad * unit, axis=-1, keepdims=True)
        )
        gh_ref[rows, :] = grad
        low = grad.astype(BF16)
        nt_ref[rows, :] = low
        ga_ref[rows, :] = mm_cols(low, w_ref[:, out_at:gate_at]).astype(BF16)

    def out_weight(tile, carry):
        cols = pl.ds(pl.multiple_of(tile * QUAD, QUAD), QUAD)
        do_ref[cols, :] = mm_rows(att_ref[:, cols], nt_ref[...]).astype(BF16)
        return carry

    lax.fori_loop(0, D // QUAD, out_weight, 0)
    return gain_grad


def backward_attention_start(dk_ref, dv_ref):
    dk_ref[...] = jnp.zeros_like(dk_ref)
    dv_ref[...] = jnp.zeros_like(dv_ref)


def backward_attention_quad(tab_ref, rank, qkv_ref, att_ref, ga_ref, lse_ref, dqkv_ref, dk_ref, dv_ref, quad):
    heads = QUAD // DH
    marks = jnp.where(iota((16, QUAD), 1) // DH == iota((16, QUAD), 0), 1.0, 0.0).astype(BF16)
    low = quad * QUAD
    cols = slice(low, low + QUAD)

    def step(tile, carry):
        first = window_start(tile)
        bias, side_bias = tile_bias(tab_ref, rank, tile, first, 0)
        bias = jnp.concatenate([bias, side_bias], axis=0)
        rows = pl.ds(pl.multiple_of(tile * QT, QT), QT)
        window = pl.ds(first, WIN)
        lse = lse_ref[tile]
        product = ga_ref[rows, cols].astype(F32) * att_ref[rows, cols].astype(F32)
        high = product.astype(BF16)
        rest = (product - high.astype(F32)).astype(BF16)
        centre = mm_cols(marks, high) + mm_cols(marks, rest)
        query = head_stack(qkv_ref[rows, cols])
        grad = head_stack(ga_ref[rows, cols])
        keys = jnp.concatenate(
            [qkv_ref[window, D + low : D + low + QUAD], qkv_ref[ROWS:, D + low : D + low + QUAD]], axis=0
        )
        values = jnp.concatenate(
            [qkv_ref[window, 2 * D + low : 2 * D + low + QUAD],
             qkv_ref[ROWS:, 2 * D + low : 2 * D + low + QUAD]], axis=0
        )
        scores = mm_cols(keys, query)
        slopes = mm_cols(values, grad)
        probs, grads = [], []
        for head in range(heads):
            part = slice(head * QT, (head + 1) * QT)
            number = quad * heads + head
            prob = jnp.exp(scores[:, part] + bias - lse[number : number + 1])
            probs.append(prob.astype(BF16))
            grads.append((prob * (slopes[:, part] - centre[head : head + 1])).astype(BF16))
        probs = jnp.concatenate(probs, axis=1)
        grads = jnp.concatenate(grads, axis=1)
        dkey = mm(grads, query)
        dvalue = mm(probs, grad)
        dk_ref[window, cols] = dk_ref[window, cols] + dkey[:WIN]
        dk_ref[ROWS:, cols] = dk_ref[ROWS:, cols] + dkey[WIN:]
        dv_ref[window, cols] = dv_ref[window, cols] + dvalue[:WIN]
        dv_ref[ROWS:, cols] = dv_ref[ROWS:, cols] + dvalue[WIN:]
        dqkv_ref[rows, cols] = head_merge(mm_rows(grads, keys)).astype(BF16)
        return carry

    lax.fori_loop(0, TILES, step, 0)
    dqkv_ref[ROWS:, cols] = jnp.zeros((SIDE_ROWS, QUAD), BF16)
    dqkv_ref[:, D + low : D + low + QUAD] = dk_ref[:, cols].astype(BF16)
    dqkv_ref[:, 2 * D + low : 2 * D + low + QUAD] = dv_ref[:, cols].astype(BF16)


def weight_grads(n_ref, dqkv_ref, refs):
    for number, ref in enumerate(refs):
        def weights(tile, carry):
            at = pl.multiple_of(tile * QUAD, QUAD)
            value = mm_rows(n_ref[...], dqkv_ref[:, pl.ds(number * D + at, QUAD)]).astype(BF16)
            if len(ref.shape) == 4:
                ref[:, :, :, pl.ds(at, QUAD)] = value.reshape(ref.shape[:3] + (QUAD,))
            else:
                ref[:, pl.ds(at, QUAD)] = value
            return carry

        lax.fori_loop(0, D // QUAD, weights, 0)


def backward_project(tab_ref, rank, x_ref, gh_ref, gains, n_ref, dqkv_ref, w_ref, gn_ref, g_ref):
    def step(tile, carry):
        cols = pl.ds(pl.multiple_of(tile * QUAD, QUAD), QUAD)
        gn_ref[:, cols] = mm_cols(dqkv_ref[...], w_ref[cols, : 3 * D])
        return carry

    lax.fori_loop(0, D // QUAD, step, 0)
    pool = pooling(tab_ref, rank)
    side = mm(pool, n_ref[:ROWS, :])
    root = lax.rsqrt(mean_square(side) + EPSILON)
    unit = side * root
    grad = gn_ref[ROWS:, :]
    side_gain = jnp.sum(grad * unit, axis=0, keepdims=True)
    grad = grad * gains[1:2]
    grad = root * (grad - unit * jnp.mean(grad * unit, axis=-1, keepdims=True))
    parts = three_way(grad)
    gain_grad = jnp.zeros((1, D), F32)
    for tile in range(TILES):
        rows = pl.ds(tile * QT, QT)
        spread = pool[:, tile * QT : (tile + 1) * QT]
        total = gn_ref[rows, :] + mm_rows(spread, parts[0]) + mm_rows(spread, parts[1])
        value = x_ref[rows, :].astype(F32)
        root = lax.rsqrt(mean_square(value) + EPSILON)
        unit = value * root
        gain_grad = gain_grad + jnp.sum(total * unit, axis=0, keepdims=True)
        total = total * gains[0:1]
        value = (
            gh_ref[rows, :] + root * (total - unit * jnp.mean(total * unit, axis=-1, keepdims=True))
        ).astype(BF16)
        if len(g_ref.shape) == 3:
            g_ref[pl.ds(tile * (QT // BLK), QT // BLK)] = value.reshape(QT // BLK, BLK, D)
        else:
            g_ref[rows, :] = value
    return gain_grad, side_gain


def first_kernel(tab_ref, x_ref, gc_ref, w_ref, n_ref, qkv_ref, att_ref, lse_ref):
    rank = lax.axis_index("rep")
    gains = gains_of(gc_ref)
    forward_norm(tab_ref, rank, x_ref, gains, n_ref)
    forward_project(n_ref, w_ref, qkv_ref)
    forward_attention(tab_ref, rank, qkv_ref, att_ref, lse_ref, 0, TILES)


def second_kernel(tab_ref, x_ref, cot_ref, att_ref, gc_ref, w_ref, wb_ref,
                  y_ref, gh_ref, ga_ref, dg_ref, du_ref, db_ref, do_ref, gain_ref, *scratch):
    rank = lax.axis_index("rep")
    gain_ref[...] = feed_forward(tab_ref, rank, x_ref, cot_ref, att_ref, gains_of(gc_ref), w_ref, wb_ref,
                                 y_ref, gh_ref, ga_ref, dg_ref, du_ref, db_ref, do_ref, *scratch)


def third_kernel(tab_ref, x_ref, gh_ref, ga_ref, att_ref, lse_ref, n_ref, qkv_ref, gain_ref, gc_ref, w_ref,
                 g_ref, dw_ref, dc_ref, dqkv_ref, dk_ref, dv_ref, gn_ref):
    rank = lax.axis_index("rep")
    gains = gains_of(gc_ref)
    backward_attention_start(dk_ref, dv_ref)
    for quad in range(D // QUAD):
        backward_attention_quad(tab_ref, rank, qkv_ref, att_ref, ga_ref, lse_ref, dqkv_ref, dk_ref, dv_ref, quad)
    weight_grads(n_ref, dqkv_ref, [dw_ref.at[:, i * D : (i + 1) * D] for i in range(3)])
    one, side = backward_project(tab_ref, rank, x_ref, gh_ref, gains, n_ref, dqkv_ref, w_ref, gn_ref, g_ref)
    grads = jnp.concatenate([one, side, gain_ref[...], jnp.zeros((5, D), F32)], axis=0)
    spread_gain_grads(grads, dc_ref)


def attend(tab, x, gc, w):
    shape = jax.ShapeDtypeStruct
    return pl.pallas_call(
        first_kernel,
        out_shape=(shape((ALL_ROWS, D), BF16), shape((ALL_ROWS, 3 * D), BF16), shape((ROWS, D), BF16),
                   shape((TILES, 16, QT), F32)),
        in_specs=[SMEM, VMEM, VMEM, pl.BlockSpec((D, 3 * D), lambda step: (0, 0))],
        grid=(1,),
        out_specs=(VMEM,) * 4,
        compiler_params=pltpu.CompilerParams(vmem_limit_bytes=VMEM_LIMIT),
        name="attend",
    )(tab, x, gc, w)


def feed(tab, x, cot, att, gc, w, wb):
    hidden = wb.shape[0]
    shape = jax.ShapeDtypeStruct
    return pl.pallas_call(
        second_kernel,
        out_shape=(shape((ROWS, D), BF16), shape((ROWS, D), F32), shape((ROWS, D), BF16),
                   shape((D, hidden), BF16), shape((D, hidden), BF16), shape((hidden, D), BF16), shape((D, D), BF16),
                   shape((1, D), F32)),
        in_specs=[SMEM] + [VMEM] * 6,
        out_specs=(VMEM,) * 8,
        scratch_shapes=[pltpu.VMEM((ROWS, D), F32), pltpu.VMEM((ROWS, D), BF16), pltpu.VMEM((D, ROWS), BF16),
                        pltpu.VMEM((ROWS, D), BF16), pltpu.VMEM((ROWS, hidden), BF16),
                        pltpu.VMEM((ROWS, hidden), BF16), pltpu.VMEM((ROWS, hidden), BF16),
                        pltpu.VMEM((ROWS, D), F32)],
        compiler_params=pltpu.CompilerParams(vmem_limit_bytes=VMEM_LIMIT),
        name="feed_forward",
    )(tab, x, cot, att, gc, w, wb)


def backward_layer(tab, x, gh, ga, att, lse, n, qkv, gain, gc, w):
    shape = jax.ShapeDtypeStruct
    return pl.pallas_call(
        third_kernel,
        out_shape=(shape((ROWS, D), BF16), shape((D, 3 * D), BF16), shape((gc.shape[0], 8, 128), F32)),
        in_specs=[SMEM] + [VMEM] * 9 + [pl.BlockSpec((D, 3 * D), lambda step: (0, 0))],
        grid=(1,),
        out_specs=(VMEM,) * 3,
        scratch_shapes=[pltpu.VMEM((ALL_ROWS, 3 * D), BF16), pltpu.VMEM((ALL_ROWS, D), F32),
                        pltpu.VMEM((ALL_ROWS, D), F32), pltpu.VMEM((ALL_ROWS, D), F32)],
        compiler_params=pltpu.CompilerParams(vmem_limit_bytes=VMEM_LIMIT),
        name="attend_back",
    )(tab, x, gh, ga, att, lse, n, qkv, gain, gc, w)


class Links:
    def __init__(self, outer, inner):
        self.outer, self.inner = outer, inner
        self.rank, self.spot = lax.axis_index("rep"), lax.axis_index("fsdp")
        self.core = self.rank % 2
        self.row, self.col = self.spot // inner, self.spot % inner
        self.mate, self.across = core_of(self.rank), across_of(self.rank)
        self.late = []

    def greet(self, everyone=False):
        barrier = pltpu.get_barrier_semaphore()
        neighbours = (
            (self.row + 1 < self.outer, {"fsdp": self.spot + self.inner}),
            (self.row > 0, {"fsdp": self.spot - self.inner}),
            (self.col + 1 < self.inner, {"fsdp": self.spot + 1}),
            (self.col > 0, {"fsdp": self.spot - 1}),
        )
        group = (self.mate, self.across) + ((across_of(self.mate),) if everyone else ())
        amount = jnp.int32(len(group))
        for there, device in neighbours:
            amount = amount + there.astype(jnp.int32)

            @pl.when(there)
            def _():
                pl.semaphore_signal(barrier, inc=1, device_id=device, device_id_type=MESH)

        for device in group:
            pl.semaphore_signal(barrier, inc=1, device_id={"rep": device}, device_id_type=MESH)
        pl.semaphore_wait(barrier, amount)

    def send(self, there, src, dst, ssem, rsem, device):
        def describe():
            return pltpu.make_async_remote_copy(
                src_ref=src, dst_ref=dst, send_sem=ssem, recv_sem=rsem,
                device_id=device, device_id_type=MESH,
            )

        if there is None:
            describe().start()
        else:
            @pl.when(there)
            def _():
                describe().start()

        self.late.append((there, lambda: describe().wait_send()))

    def arrive(self, place, rsem, spare):
        pltpu.make_async_remote_copy(
            src_ref=place, dst_ref=place, send_sem=spare, recv_sem=rsem,
            device_id={"rep": self.mate}, device_id_type=MESH,
        ).wait_recv()

    def drain(self):
        for there, finish in self.late:
            if there is None:
                finish()
            else:
                pl.when(there)(finish)


def halves(ref, which):
    half = ref.shape[-1] // 2
    cols = pl.ds(pl.multiple_of(which * half, 128), half)
    return ref.at[:, :, :, cols] if len(ref.shape) == 4 else ref.at[:, cols]


class Reduction:
    def __init__(self, links, source, total, mine, crecv, yrecv, zrecv, xrecv, stage, sems, number):
        self.links, self.source, self.total, self.mine, self.stage = links, source, total, mine, stage
        self.crecv, self.yrecv, self.zrecv, self.xrecv = crecv, yrecv, zrecv, xrecv
        self.sems, self.number = sems, number
        self.whole = total.shape[-1] % 256 != 0
        self.load = None

    def sem(self, name, *index):
        return self.sems[name].at[index + (self.number,)]

    def begin(self):
        links = self.links
        other = self.source if self.whole else halves(self.source, 1 - links.core)
        links.send(None, other, self.crecv, self.sem("c_send"), self.sem("c_recv"), {"rep": links.mate})
        if self.mine is None:
            self.mine = self.source if self.whole else halves(self.source, links.core)
        else:
            own = self.source if self.whole else halves(self.source, links.core)
            self.load = pltpu.make_async_copy(own, self.mine, self.sem("m_sem"))
            self.load.start()

    def pair(self):
        links = self.links
        if self.load is not None:
            self.load.wait()
        links.arrive(self.crecv, self.sem("c_recv"), self.sems["spare"].at[0])
        inner = links.inner

        def add(index, carry):
            row, col = index // inner, index % inner
            self.mine[row, col] = self.mine[row, col] + self.crecv[row, col]
            return carry

        lax.fori_loop(0, links.outer * inner, add, 0)
        links.send(None, self.mine.at[:, 1 - links.col], self.yrecv, self.sem("y_send"), self.sem("y_recv"),
                   {"fsdp": links.spot + 1 - 2 * links.col})

    def slot(self, way, place, dest):
        return dest - place if way == 0 else self.links.outer - place + dest

    def pass_on(self, way, dest, there, first):
        links = self.links
        step = 1 if way == 0 else -1
        mine = self.mine.at[dest, links.col]
        put = self.slot(way, links.row + step, dest)
        if not first:
            got = self.slot(way, links.row, dest)

            @pl.when(there)
            def _():
                links.arrive(self.zrecv.at[got], self.sem("z_recv", got), self.sems["spare"].at[0])
                mine[...] = mine[...] + self.zrecv[got]

        links.send(there, mine, self.zrecv.at[put], self.sem("z_send", way, dest), self.sem("z_recv", put),
                   {"fsdp": links.spot + step * links.inner})

    def column(self):
        links = self.links
        size = links.outer
        links.arrive(self.yrecv, self.sem("y_recv"), self.sems["spare"].at[0])

        def add(index, carry):
            self.mine[index, links.col] = self.mine[index, links.col] + self.yrecv[index]
            return carry

        lax.fori_loop(0, size, add, 0)
        for far in range(size - 1, 0, -1):
            self.pass_on(0, far, links.row == 0, True)
            self.pass_on(1, size - 1 - far, links.row == size - 1, True)

    def hop(self, turn):
        links = self.links
        size = links.outer
        for way in range(2):
            place = turn if way == 0 else size - 1 - turn
            here = links.row == place
            rest = range(size - 1, place, -1) if way == 0 else range(0, place)
            for dest in rest:
                self.pass_on(way, dest, here, False)
            mine = self.mine.at[place, links.col]
            got = self.slot(way, place, place)

            @pl.when(here)
            def _():
                links.arrive(self.zrecv.at[got], self.sem("z_recv", got), self.sems["spare"].at[0])
                mine[...] = mine[...] + self.zrecv[got]

    def cross(self):
        links = self.links
        mine = self.mine.at[links.row, links.col]
        links.send(None, mine, self.xrecv, self.sem("x_send"), self.sem("x_recv"), {"rep": links.across})

    def finish(self):
        links = self.links
        links.arrive(self.xrecv, self.sem("x_recv"), self.sems["spare"].at[0])
        self.stage[...] = self.mine[links.row, links.col].astype(F32) + self.xrecv[...].astype(F32)
        place = self.total if self.whole else halves(self.total, links.core)
        self.keep = pltpu.make_async_copy(self.stage, place, self.sem("m_sem"))
        self.keep.start()
        if not self.whole:
            links.send(None, self.stage, place, self.sem("f_send"), self.sem("f_recv"), {"rep": links.mate})

    def settle(self):
        self.keep.wait()
        if not self.whole:
            self.links.arrive(
                halves(self.total, 1 - self.links.core), self.sem("f_recv"), self.sems["spare"].at[0]
            )


class AcrossFirst(Reduction):
    def pair(self):
        links = self.links
        if self.load is not None:
            self.load.wait()
        links.arrive(self.crecv, self.sem("c_recv"), self.sems["spare"].at[0])
        inner = links.inner

        def add(index, carry):
            row, col = index // inner, index % inner
            self.mine[row, col] = self.mine[row, col] + self.crecv[row, col]
            return carry

        lax.fori_loop(0, links.outer * inner, add, 0)
        self.side = links.rank // 2
        links.send(None, self.rows_of(self.mine, 1 - self.side), self.xrecv, self.sem("x_send"), self.sem("x_recv"),
                   {"rep": links.across})

    def rows_of(self, ref, which):
        half = ref.shape[-2] // 2
        rows = pl.ds(pl.multiple_of(which * half, 16), half)
        return ref.at[:, :, rows, :] if len(ref.shape) == 4 else ref.at[rows, :]

    def meet(self):
        links = self.links
        links.arrive(self.xrecv, self.sem("x_recv"), self.sems["spare"].at[0])
        self.mine = self.rows_of(self.mine, self.side)
        inner = links.inner

        def add(index, carry):
            row, col = index // inner, index % inner
            self.mine[row, col] = self.mine[row, col] + self.xrecv[row, col]
            return carry

        lax.fori_loop(0, links.outer * inner, add, 0)
        links.send(None, self.mine.at[:, 1 - links.col], self.yrecv, self.sem("y_send"), self.sem("y_recv"),
                   {"fsdp": links.spot + 1 - 2 * links.col})

    def quarter(self, side, core):
        return halves(self.rows_of(self.total, side), core)

    def spread(self, stage, place, keep, ssem, rsem):
        links = self.links
        self.keeps.append(pltpu.make_async_copy(stage, place, keep))
        self.keeps[-1].start()
        links.send(None, stage, place, ssem, rsem, {"rep": links.mate})

    def cross(self):
        links = self.links
        mine = self.mine.at[links.row, links.col]
        links.send(None, mine, self.third, self.sem("h_send"), self.sem("h_recv"), {"rep": links.across})
        self.stage[...] = mine[...].astype(F32)
        self.keeps = []
        self.spread(self.stage, self.quarter(self.side, links.core), self.sem("m_sem"),
                    self.sem("f_send"), self.sem("f_recv"))

    def finish(self):
        links = self.links
        links.arrive(self.third, self.sem("h_recv"), self.sems["spare"].at[0])
        self.stage_two[...] = self.third[...].astype(F32)
        self.spread(self.stage_two, self.quarter(1 - self.side, links.core), self.sem("k_keep"),
                    self.sem("k_send"), self.sem("k_recv"))

    def settle(self):
        links = self.links
        for keep in self.keeps:
            keep.wait()
        for side, name in ((self.side, "f_recv"), (1 - self.side, "k_recv")):
            links.arrive(self.quarter(side, 1 - links.core), self.sem(name), self.sems["spare"].at[0])


SEM_NAMES = ("c_send", "c_recv", "m_sem", "y_send", "y_recv", "z_send", "z_recv", "x_send", "x_recv",
             "f_send", "f_recv", "h_send", "h_recv", "k_send", "k_recv", "k_keep", "r_send", "r_recv", "own", "spare")


class Return:
    def __init__(self, links, source, home, sems, kind):
        self.links, self.source, self.home, self.sems, self.kind = links, source, home, sems, kind

    def begin(self):
        links = self.links
        dst = self.home.at[links.rank]
        for way, device in enumerate((links.across, links.mate)):
            links.send(None, self.source, dst, self.sems["r_send"].at[self.kind, way],
                       self.sems["r_recv"].at[self.kind, way], {"rep": device})
        self.copy = pltpu.make_async_copy(self.source, dst, self.sems["own"].at[self.kind])
        self.copy.start()

    def relay(self):
        links = self.links
        place = self.home.at[links.across]
        links.arrive(place, self.sems["r_recv"].at[self.kind, 0], self.sems["spare"].at[0])
        links.send(None, place, place, self.sems["r_send"].at[self.kind, 2],
                   self.sems["r_recv"].at[self.kind, 2], {"rep": links.mate})

    def settle(self):
        links, sem = self.links, self.sems["r_recv"]
        links.arrive(self.home.at[links.mate], sem.at[self.kind, 1], self.sems["spare"].at[0])
        links.arrive(self.home.at[across_of(links.mate)], sem.at[self.kind, 2], self.sems["spare"].at[0])
        self.copy.wait()


TABLE_ROWS = 56


def packed_table(lens, tabv_ref):
    lane = iota((8, 128), 1)
    blocks = lax.div(lens + (BLK - 1), BLK)
    key = jnp.where(blocks > 0, blocks * 128 + (127 - lane), 0)
    wide = jnp.broadcast_to(key[:1], (128, 128))
    other = jnp.sum(jnp.where(iota((128, 128), 0) == iota((128, 128), 1), wide, 0), axis=1, keepdims=True)
    order = jnp.sum(jnp.where(other > wide, 1, 0), axis=0, keepdims=True)
    order = jnp.broadcast_to(order, (8, 128))
    edges, below = [], jnp.zeros((8, 1), jnp.int32)
    for size in range(MAX_SEQ_BLOCKS, 0, -1):
        below = below + jnp.sum(jnp.where(blocks == size, 1, 0), axis=1, keepdims=True)
        edges.append(jnp.broadcast_to(below, (8, 128)))

    def assign(number, carry):
        loads, slot, first = carry[:4], carry[4], carry[5]
        size = jnp.zeros((8, 128), jnp.int32)
        for step, edge in enumerate(edges):
            size = size + jnp.where(number < edge, 1, 0)
        low = jnp.minimum(jnp.minimum(loads[0], loads[1]), jnp.minimum(loads[2], loads[3]))
        best = jnp.full((8, 128), 3, jnp.int32)
        for dev in (2, 1, 0):
            best = jnp.where(loads[dev] == low, dev, best)
        mine = order == number
        slot = jnp.where(mine, best * SLOTS + low, slot)
        first = jnp.where(mine, low, first)
        loads = tuple(loads[dev] + jnp.where(best == dev, size, 0) for dev in range(4))
        return loads + (slot, first)

    zero = jnp.zeros((8, 128), jnp.int32)
    carry = lax.fori_loop(0, 32, assign, (zero,) * 6)
    slot, first = carry[4], carry[5]
    where, tokens, segment = zero - 1, zero, zero
    for step in range(MAX_SEQ_BLOCKS):
        def shifted(value):
            return value if step == 0 else pltpu.roll(value, step, 1)

        covers = shifted(blocks) > step
        where = jnp.where(covers, shifted(slot) + step, where)
        tokens = jnp.where(covers, jnp.minimum(shifted(lens) - BLK * step, BLK), tokens)
        segment = jnp.where(covers, shifted(first) + 1, segment)
    packed = jnp.where(where >= 0, (lane + 1) + 128 * tokens + 16384 * segment, 0)
    spots = jnp.broadcast_to(where[:1], (48, 128))
    values = jnp.broadcast_to(packed[:1], (48, 128))
    column = jnp.sum(jnp.where(spots == iota((48, 128), 0), values, 0), axis=1, keepdims=True)
    tabv_ref[:48] = jnp.broadcast_to(column, (48, 128))
    tabv_ref[48:] = where


FRONT_ORDER = (
    ("own", 5), ("own", 0), ("own", 1), ("own", 2), ("do", "table"), ("hop", 5, 0), ("pack", 0, 1), ("pack", 1, 1),
    ("cross", 0), ("pack", 0, 0), ("hop", 0, 0), ("hop", 5, 1), ("cross", 1), ("pack", 1, 0), ("hop", 1, 0),
    ("hop", 2, 0), ("hop", 0, 1), ("hop", 5, 2), ("hop", 1, 1), ("own", 3), ("hop", 2, 1), ("own", 4), ("hop", 0, 2),
    ("hop", 1, 2), ("hop", 3, 0), ("fr", 5), ("rfin", 0), ("do", "norm"), ("hop", 2, 2), ("hop", 4, 0),
    ("hop", 3, 1), ("fr", 0), ("hop", 4, 1), ("got", 0), ("do", "proj"), ("hop", 3, 2), ("fr", 1), ("do", "a0"),
    ("hop", 4, 2), ("fr", 2), ("do", "a1"), ("rfin", 1), ("do", "a2"), ("fr", 3), ("xin", 1), ("fr", 4), ("got", 1),
    ("got", 2), ("got", 3), ("got", 4),
)


def front_kernel(outer, inner, *refs):
    (lens_ref, rows_any, cots_any, *weights), refs = refs[:9], refs[9:]
    (wd_ref, wc_ref), refs = refs[:2], refs[2:]
    tab_ref, outs_any, (ga_ref, gb_ref), refs = refs[0], refs[1:9], refs[9:11], refs[11:]
    (stage, lens_all, tabs, psend, precv, xsend, xrecv, rows_ref, cots_ref), refs = refs[:9], refs[9:]
    held, refs = refs[:8], refs[8:]
    x_ref, cot_ref, n_ref, qkv_ref, att_ref, lse_ref, wqkv_ref, gc_ref = held
    (l_send, l_recv, t_sem, w_sem, z_send, z_recv, y_send, y_recv, c_send, c_recv, d_send, d_recv, own_sem,
     p_send, p_recv, x_send, x_recv, spare, out_sem) = refs
    links = Links(outer, inner)
    rank, spot, core, mate, across = links.rank, links.spot, links.core, links.mate, links.across
    row, col = links.row, links.col
    side = rank // 2
    count = outer * inner
    part = stage.shape[0]
    per_rank = rows_ref.shape[0]
    width = 3 * D
    tall = wd_ref.shape[0]
    hidden = weights[-1].shape[1]
    rest = stage.shape[1] - width
    cuts = [0, 7 * rest // 19, 13 * rest // 19, rest]
    spans = [(cuts[i], (cuts[i + 1] - cuts[i]) // 2) for i in range(3)]

    at = 0
    loads = []
    row_loads = [pltpu.make_async_copy(rows_any, rows_ref, w_sem.at[6]), pltpu.make_async_copy(cots_any, cots_ref, w_sem.at[7])]
    for number, ref in enumerate(weights):
        cols = slice(at, at + ref.shape[1])
        loads.append(pltpu.make_async_copy(ref, stage.at[:, cols], w_sem.at[number]))
        loads[-1].start()
        at += ref.shape[1]
    for load in row_loads:
        load.start()

    links.greet(True)
    lens_all[rank] = lens_ref[...]
    for step in range(1, 4):
        links.send(None, lens_ref, lens_all.at[rank], l_send.at[step - 1], l_recv.at[step - 1],
                   {"rep": (rank + step) % 4})

    def cols_of(start, half, which):
        return pl.ds(pl.multiple_of(start + which * half, 128), half)

    down_half = D // 2

    def tall_rows(which):
        return pl.ds(pl.multiple_of(which * (tall // 2), 16), tall // 2)

    def source(number):
        if number == 0:
            return stage.at[:, cols_of(0, width // 2, core)]
        if number == 1:
            return wd_ref.at[tall_rows(side), cols_of(0, down_half, core)]
        if number == 5:
            return wc_ref
        start, half = spans[number - 2]
        return stage.at[:, cols_of(width + start, half, core)]

    def place(number, shard, which=None):
        which = core if which is None else which
        if number == 0:
            return wqkv_ref.at[pl.ds(pl.multiple_of(shard * part, 16), part), cols_of(0, width // 2, which)]
        if number in (1, 6):
            return gb_ref.at[shard, tall_rows(side if number == 1 else 1 - side), cols_of(0, down_half, which)]
        if number == 5:
            return gc_ref.at[shard]
        start, half = spans[number - 2]
        return ga_ref.at[shard, :, cols_of(start, half, which)]

    nobody = spare.at[0]

    def both(first, second):
        return second if first is None else jnp.logical_and(first, second)

    def guarded(there, action):
        if there is None:
            action()
        else:
            pl.when(there)(action)

    def share(there, number, shard):
        if number == 5:
            return
        here = place(number, shard)
        links.send(there, here, here, c_send.at[number, shard], c_recv.at[number, shard], {"rep": mate})
        if number == 1:
            links.send(there, here, here, d_send.at[shard], d_recv.at[shard], {"rep": across})

    other_column = {"fsdp": spot + 1 - 2 * col}

    def along_row(there, number, line, src):
        here = place(number, line * inner + col)
        links.send(there, here if src is None else src, here, y_send.at[line, number], y_recv.at[line, number],
                   other_column)

    def lines(step):
        return ((row - 1 - step >= 0, row - 1 - step, 0, row + 1 < outer, spot + inner),
                (row + 1 + step < outer, row + 1 + step, 1, row > 0, spot - inner))

    def own(number):
        src, dst = source(number), place(number, spot)
        links.send(row + 1 < outer, src, dst, z_send.at[0, 0, number], z_recv.at[0, 0, number],
                   {"fsdp": spot + inner})
        links.send(row > 0, src, dst, z_send.at[1, 0, number], z_recv.at[1, 0, number], {"fsdp": spot - inner})
        along_row(None, number, row, src)

    def hop(number, step):
        for here, line, way, onward, target in lines(step):
            shard = line * inner + col
            guarded(here, lambda: links.arrive(place(number, shard), z_recv.at[way, step, number], nobody))
            if step + 1 < outer - 1:
                view = place(number, shard)
                links.send(both(here, onward), view, view, z_send.at[way, step + 1, number],
                           z_recv.at[way, step + 1, number], {"fsdp": target})
            along_row(here, number, line, None)
            share(here, number, shard)

    def from_row(number):
        def one(there, line):
            shard = line * inner + 1 - col
            guarded(there, lambda: links.arrive(place(number, shard), y_recv.at[line, number], nobody))
            share(there, number, shard)

        one(None, row)
        for step in range(outer - 1):
            for here, line, *_ in lines(step):
                one(here, line)

    def gathered(*numbers):
        def wait(shard, carry):
            @pl.when(shard != spot)
            def _():
                for number in numbers:
                    links.arrive(place(number, shard, 1 - core), c_recv.at[number, shard], nobody)

            return carry

        lax.fori_loop(0, count, wait, 0)

    def from_across():
        def relay(shard, carry):
            here = place(6, shard)

            @pl.when(shard != spot)
            def _():
                links.arrive(here, d_recv.at[shard], nobody)
                pltpu.make_async_remote_copy(
                    src_ref=here, dst_ref=here, send_sem=c_send.at[6, shard], recv_sem=c_recv.at[6, shard],
                    device_id={"rep": mate}, device_id_type=MESH,
                ).start()

            return carry

        lax.fori_loop(0, count, relay, 0)

    for load in loads:
        load.wait()
    keep = [
        pltpu.make_async_copy(stage.at[:, :width], wqkv_ref.at[pl.ds(pl.multiple_of(spot * part, 16), part)], own_sem.at[0]),
        pltpu.make_async_copy(stage.at[:, width:], ga_ref.at[spot], own_sem.at[1]),
        pltpu.make_async_copy(wd_ref, gb_ref.at[spot], own_sem.at[2]),
        pltpu.make_async_copy(wc_ref, gc_ref.at[spot], own_sem.at[3]),
    ]
    for copy in keep:
        copy.start()
    leaving = []

    def leave(*numbers):
        for number in numbers:
            leaving.append(pltpu.make_async_copy(held[number], outs_any[number], out_sem.at[number]))
            leaving[-1].start()

    def make_table():
        for step in range(1, 4):
            links.arrive(lens_all.at[(rank + 4 - step) % 4], l_recv.at[step - 1], nobody)
        lens = lens_all[0] + lens_all[1] + lens_all[2] + lens_all[3]
        packed_table(jnp.broadcast_to(lens[:1], (8, 128)), tab_ref)
        to_scalar = pltpu.make_async_copy(tab_ref, tabs, t_sem.at[0])
        to_scalar.start()
        to_scalar.wait()
        for load in row_loads:
            load.wait()

    sources = (rows_ref, cots_ref)
    outs = (x_ref, cot_ref)

    def picked(kind, target, slot):
        index = block_at(tabs, target * SLOTS + slot) - rank * per_rank
        mine = jnp.logical_and(index >= 0, index < per_rank)
        return mine, sources[kind][jnp.clip(index, 0, per_rank - 1)]

    def mate_copy(kind, piece):
        return pltpu.make_async_remote_copy(
            src_ref=psend.at[kind, piece], dst_ref=precv.at[kind, piece],
            send_sem=p_send.at[kind, piece], recv_sem=p_recv.at[kind, piece],
            device_id={"rep": mate}, device_id_type=MESH,
        )

    def across_copy(kind):
        return pltpu.make_async_remote_copy(
            src_ref=xsend.at[kind], dst_ref=xrecv.at[kind],
            send_sem=x_send.at[kind], recv_sem=x_recv.at[kind],
            device_id={"rep": across}, device_id_type=MESH,
        )

    def pack_rows(kind, piece):
        target = mate if piece == 0 else across_of(mate)

        def pack(slot, carry):
            mine, value = picked(kind, target, slot)
            psend[kind, piece, slot] = jnp.where(mine, value, jnp.zeros_like(value))
            return carry

        lax.fori_loop(0, SLOTS, pack, 0)
        mate_copy(kind, piece).start()

    def cross_rows(kind):
        mate_copy(kind, 1).wait_recv()

        def merge(slot, carry):
            mine, value = picked(kind, across, slot)
            xsend[kind, slot] = jnp.where(mine, value, precv[kind, 1, slot])
            return carry

        lax.fori_loop(0, SLOTS, merge, 0)
        across_copy(kind).start()

    def finish_rows(kind):
        mate_copy(kind, 0).wait_recv()
        across_copy(kind).wait_recv()

        def finish(slot, carry):
            mine, value = picked(kind, rank, slot)
            rows = pl.ds(pl.multiple_of(slot * BLK, BLK), BLK)
            outs[kind][rows, :] = jnp.where(mine, value, precv[kind, 0, slot] + xrecv[kind, slot])
            return carry

        lax.fori_loop(0, SLOTS, finish, 0)

    def norm():
        keep[3].wait()
        forward_norm(tabs, rank, x_ref, gains_of(gc_ref), n_ref)
        leave(2, 7)

    def project():
        keep[0].wait()
        forward_project(n_ref, wqkv_ref, qkv_ref)
        leave(3, 6)

    def attend_tiles(begin, end):
        forward_attention(tabs, rank, qkv_ref, att_ref, lse_ref, begin, end)
        if end == TILES:
            leave(4, 5)

    work = {"table": make_table, "norm": norm, "proj": project, "a0": lambda: attend_tiles(0, 2),
            "a1": lambda: attend_tiles(2, 4), "a2": lambda: attend_tiles(4, TILES)}
    tail = []
    for action, which, *more in FRONT_ORDER:
        if action == "do":
            work[which]()
        elif action == "own":
            own(which)
        elif action == "hop":
            hop(which, more[0])
        elif action == "fr":
            from_row(which)
        elif action == "xin":
            from_across()
        elif action == "got" and which == 0:
            gathered(0)
        elif action == "got":
            tail.append(which)
        elif action == "pack":
            pack_rows(which, more[0])
        elif action == "cross":
            cross_rows(which)
        else:
            finish_rows(which)
            leave(which)
    gathered(*tail, 6)

    def sent(shard, carry):
        @pl.when(shard != spot)
        def _():
            pltpu.make_async_remote_copy(
                src_ref=place(6, shard), dst_ref=place(6, shard), send_sem=c_send.at[6, shard], recv_sem=c_recv.at[6, shard],
                device_id={"rep": mate}, device_id_type=MESH,
            ).wait_send()

        return carry

    lax.fori_loop(0, count, sent, 0)
    links.drain()
    for kind in range(2):
        for piece in range(2):
            mate_copy(kind, piece).wait_send()
        across_copy(kind).wait_send()
    for copy in keep[1:3] + leaving:
        copy.wait()


def gather_and_attend(count, lens, rows, cots, weights, wd, wc):
    outer, inner = grid_of(count)
    block = rows.shape[1:]
    part, hidden = wd.shape[0], weights[-1].shape[1]
    part = weights[0].shape[0]
    dma, shape = pltpu.SemaphoreType.DMA, jax.ShapeDtypeStruct
    total = sum(weight.shape[1] for weight in weights)
    kinds = 6
    held = (shape((ROWS, D), BF16), shape((ROWS, D), BF16), shape((ALL_ROWS, D), BF16), shape((ALL_ROWS, 3 * D), BF16),
            shape((ROWS, D), BF16), shape((TILES, 16, QT), F32), shape((D, 3 * D), BF16), shape((count,) + wc.shape, BF16))
    return pl.pallas_call(
        partial(front_kernel, outer, inner),
        out_shape=(shape((TABLE_ROWS, 128), jnp.int32),) + held + (
            shape((count, part, total - 3 * D), BF16), shape((count,) + wd.shape, BF16),
        ),
        in_specs=[VMEM] + [ANY] * 8 + [VMEM] * 2,
        out_specs=(VMEM,) + (ANY,) * 10,
        scratch_shapes=[
            pltpu.VMEM((part, total), BF16), pltpu.VMEM((4, 8, 128), jnp.int32), pltpu.SMEM((TABLE_ROWS, 128), jnp.int32),
            pltpu.VMEM((2, 2, SLOTS) + block, BF16), pltpu.VMEM((2, 2, SLOTS) + block, BF16),
            pltpu.VMEM((2, SLOTS) + block, BF16), pltpu.VMEM((2, SLOTS) + block, BF16),
            pltpu.VMEM(rows.shape, BF16), pltpu.VMEM(cots.shape, BF16),
            *(pltpu.VMEM(one.shape, one.dtype) for one in held),
            dma((3,)), dma((3,)), dma((1,)), dma((8,)),
            dma((2, outer - 1, kinds)), dma((2, outer - 1, kinds)), dma((outer, kinds)), dma((outer, kinds)),
            dma((kinds + 1, count)), dma((kinds + 1, count)), dma((count,)), dma((count,)), dma((4,)),
            dma((2, 2)), dma((2, 2)), dma((2,)), dma((2,)), dma((1,)), dma((8,)),
        ],
        compiler_params=pltpu.CompilerParams(
            collective_id=1, has_side_effects=True, vmem_limit_bytes=VMEM_LIMIT
        ),
        name="gather_and_attend",
    )(lens, rows, cots, *weights, wd, wc)


ACROSS_FIRST = (2, 3)
REAR_ORDER = (
    ("do", "start"), ("do", "P0"), ("do", "P1a"), ("do", "gA"), ("begin", 0), ("do", "uA"), ("begin", 1),
    ("do", "P1b"), ("pair", 0), ("pair", 1), ("do", "gB"), ("begin", 2), ("do", "uB"), ("begin", 3), ("do", "d"),
    ("begin", 4), ("pair", 2), ("pair", 3), ("do", "out"), ("rows", 0), ("pair", 4), ("col", 0), ("meet", 2),
    ("do", "P4"), ("col", 1), ("do", "P5"), ("begin", 5), ("do", "q0"), ("meet", 3), ("pair", 5), ("hop", 0, 1),
    ("hop", 1, 1), ("do", "p0"), ("begin", 6), ("do", "q1"), ("pair", 6), ("col", 4), ("hop", 0, 2), ("hop", 1, 2),
    ("do", "p1"), ("begin", 7), ("do", "q2"), ("pair", 7), ("col", 2), ("col", 3), ("hop", 0, 3), ("cross", 0),
    ("hop", 1, 3), ("cross", 1), ("do", "bp"), ("rows", 1), ("relay", 0), ("col", 5), ("hop", 4, 1), ("fin", 0),
    ("fin", 1), ("do", "p2"), ("begin", 8), ("hop", 2, 1), ("do", "dc"), ("begin", 9), ("hop", 3, 1), ("pair", 8),
    ("pair", 9), ("col", 6), ("hop", 4, 2), ("hop", 5, 1), ("hop", 2, 2), ("hop", 3, 2), ("hop", 6, 1),
    ("hop", 5, 2), ("hop", 6, 2), ("hop", 4, 3), ("cross", 4), ("col", 7), ("hop", 7, 1), ("hop", 2, 3),
    ("cross", 2), ("hop", 3, 3), ("cross", 3), ("col", 8), ("col", 9), ("hop", 5, 3), ("cross", 5), ("hop", 6, 3),
    ("cross", 6), ("relay", 1), ("hop", 8, 1), ("hop", 9, 1), ("hop", 7, 2), ("hop", 8, 2), ("hop", 9, 2),
    ("fin", 4), ("fin", 2), ("fin", 3), ("hop", 7, 3), ("cross", 7), ("fin", 5), ("hop", 8, 3), ("cross", 8),
    ("hop", 9, 3), ("cross", 9), ("fin", 6), ("fin", 7), ("fin", 8), ("fin", 9),
)


def rear_kernel(outer, inner, *refs):
    (tab_ref, x_ref, att_ref, lse_ref, gc_ref), refs = refs[:5], refs[5:]
    (cot_any, n_any, qkv_any, wqkv_any, wf_any, wd_any), refs = refs[:6], refs[6:]
    kinds = 10
    (og_ref, ou_ref, od_ref, oo_ref, op_ref, oc_ref, ry_ref, rg_ref), refs = refs[:8], refs[8:]
    (y_ref, gh_ref, fa_ref, dk_ref, b0_ref, b1_ref, b2_ref, n_ref, ntt_ref, gres_ref, ga_ref), refs = refs[:11], refs[11:]
    (wf_ref, wd_ref, dg_ref, du_ref, db_ref, do_ref, dc_ref, mine_ref), refs = refs[:8], refs[8:]
    crecv, refs = list(refs[:7]), refs[7:]
    narrow = D // 2
    crecv = crecv[:6] + [crecv[i].at[:, :, :, :narrow] for i in range(3)] + crecv[6:]
    yrecv, zrecv, xrecv, stages = (refs[kinds * i : kinds * (i + 1)] for i in range(4))
    refs = refs[4 * kinds :]
    extra, refs = refs[: 2 * len(ACROSS_FIRST)], refs[2 * len(ACROSS_FIRST) :]
    sems = dict(zip(SEM_NAMES, refs))
    load_sem, free_sem = refs[len(SEM_NAMES) :]
    links = Links(outer, inner)
    rank = links.rank
    hidden = wd_ref.shape[0]
    part = wf_ref.shape[2]
    group = 4 * part

    def fetch(number, src, dst):
        copy = pltpu.make_async_copy(src, dst, load_sem.at[number])
        copy.start()
        return copy

    load_cot = fetch(0, cot_any, ga_ref)
    load_out = fetch(1, wf_any.at[:, :, :, :D], wf_ref.at[:, :, :, :D])
    load_in = fetch(2, wf_any.at[:, :, :, D:], wf_ref.at[:, :, :, D:])
    load_down = fetch(3, wd_any, wd_ref)
    links.greet()

    def weight(start, size):
        return wf_ref[:, :, :, pl.ds(start, size)].reshape(D, size)

    wide = hidden // 2
    first, second = slice(0, wide), slice(wide, hidden)
    grads = [dg_ref.at[:, :, :, first], du_ref.at[:, :, :, first], dg_ref.at[:, :, :, second], du_ref.at[:, :, :, second],
             db_ref, do_ref] + [wf_ref.at[:, :, :, i * D : (i + 1) * D] for i in range(3)] + [dc_ref]
    totals = [og_ref.at[:, first], ou_ref.at[:, first], og_ref.at[:, second], ou_ref.at[:, second],
              od_ref, oo_ref] + [op_ref.at[:, i * D : (i + 1) * D] for i in range(3)] + [oc_ref]
    tasks = [
        (AcrossFirst if i in ACROSS_FIRST else Reduction)(
            links, grads[i], totals[i], mine_ref if i == kinds - 1 else None,
            crecv[i], yrecv[i], zrecv[i], xrecv[i], stages[i], sems, i,
        )
        for i in range(kinds)
    ]
    for number, i in enumerate(ACROSS_FIRST):
        tasks[i].third, tasks[i].stage_two = extra[2 * number], extra[2 * number + 1]
    returns = (Return(links, y_ref, ry_ref, sems, 0), Return(links, gres_ref, rg_ref, sems, 1))
    gains = gains_of(gc_ref)
    gain = gains[2:3]
    valid = valid_column(tab_ref, rank)
    h1_ref, dv_ref = fa_ref, fa_ref
    tiles = hidden // FF_TILE
    kept = {}

    def enter():
        load_cot.wait()
        load_out.wait()
        for tile in range(TILES):
            rows = pl.ds(tile * QT, QT)
            value = x_ref[rows, :].astype(F32) + mm(att_ref[rows, :], weight(0, D))
            h1_ref[rows, :] = value
            normed = (value * lax.rsqrt(mean_square(value) + EPSILON) * gain).astype(BF16)
            n_ref[rows, :] = normed
            ntt_ref[:, tile * QT : (tile + 1) * QT] = jnp.transpose(normed)
            gres_ref[rows, :] = (ga_ref[rows, :].astype(F32) * valid[tile * QT : (tile + 1) * QT]).astype(BF16)
        load_in.wait()
        load_down.wait()

    def inward(begin, end):
        def step(tile, carry):
            at = pl.multiple_of(tile * FF_TILE, FF_TILE)
            cols = pl.ds(at, FF_TILE)
            normed = n_ref[:ROWS, :]
            gate = mm(normed, weight(D + at, FF_TILE))
            up = mm(normed, weight(D + hidden + at, FF_TILE))
            back = mm_cols(gres_ref[...], wd_ref[cols, :])
            square = gate * gate
            bend = jnp.tanh(GELU_C * (gate * (1.0 + GELU_A * square)))
            half = 0.5 * (1.0 + bend)
            act = gate * half
            slope = half + (0.5 * GELU_C) * gate * (1.0 - bend * bend) * (1.0 + (3.0 * GELU_A) * square)
            b0_ref[:ROWS, cols] = (act * up).astype(BF16)
            b1_ref[:ROWS, cols] = (back * up * slope).astype(BF16)
            b2_ref[:ROWS, cols] = (back * act).astype(BF16)
            return carry

        lax.fori_loop(begin, end, step, 0)

    def outer_products(ref, right_ref, begin, end):
        def step(tile, carry):
            cols = pl.ds(pl.multiple_of(tile * FF_TILE, FF_TILE), FF_TILE)
            value = mm(ntt_ref[...], right_ref[:ROWS, cols]).astype(BF16)
            ref[:, :, :, cols] = value.reshape(outer, inner, part, FF_TILE)
            return carry

        lax.fori_loop(begin, end, step, 0)

    def down_products():
        def step(tile, carry):
            cols = pl.ds(pl.multiple_of(tile * FF_TILE, FF_TILE), FF_TILE)
            db_ref[tile // inner, tile % inner] = mm_rows(b0_ref[:ROWS, cols], gres_ref[...]).astype(BF16)
            return carry

        lax.fori_loop(0, tiles, step, 0)

    def outward():
        def step(tile, carry):
            cols = pl.ds(pl.multiple_of(tile * group, 128), group)
            value = h1_ref[:ROWS, cols] + mm(b0_ref[:ROWS, :hidden], wd_ref[:, cols])
            y_ref[:, cols] = (value * valid).astype(BF16)
            shards = pl.ds(tile * (4 // inner), 4 // inner)
            gh_ref[:, cols] = mm_cols(
                b1_ref[:ROWS, :hidden], wf_ref[shards, :, :, D : D + hidden].reshape(group, hidden)
            ) + mm_cols(b2_ref[:ROWS, :hidden], wf_ref[shards, :, :, D + hidden :].reshape(group, hidden))
            return carry

        lax.fori_loop(0, D // group, step, 0)
        kept["qkv"] = fetch(4, qkv_any, b1_ref)
        kept["wqkv"] = fetch(5, wqkv_any, b2_ref)

    def middle():
        gain_grad = jnp.zeros((1, D), F32)
        for tile in range(TILES):
            rows = pl.ds(tile * QT, QT)
            value, grad = h1_ref[rows, :], gh_ref[rows, :]
            root = lax.rsqrt(mean_square(value) + EPSILON)
            unit = value * root
            gain_grad = gain_grad + jnp.sum(grad * unit, axis=0, keepdims=True)
            grad = grad * gain
            grad = gres_ref[rows, :].astype(F32) + root * (
                grad - unit * jnp.mean(grad * unit, axis=-1, keepdims=True)
            )
            gh_ref[rows, :] = grad
            low = grad.astype(BF16)
            n_ref[rows, :] = low
            ga_ref[rows, :] = mm_cols(low, weight(0, D)).astype(BF16)
        kept["gain"] = gain_grad

    def out_products():
        def step(tile, carry):
            cols = pl.ds(pl.multiple_of(tile * QUAD, QUAD), QUAD)
            value = mm_rows(att_ref[...], n_ref[:ROWS, cols]).astype(BF16)
            do_ref[:, :, :, cols] = value.reshape(outer, inner, part, QUAD)
            return carry

        lax.fori_loop(0, D // QUAD, step, 0)
        kept["n"] = fetch(6, n_any, n_ref)

    def attention(quad):
        if quad == 0:
            backward_attention_start(dk_ref, dv_ref)
            kept["qkv"].wait()
        backward_attention_quad(tab_ref, rank, b1_ref, att_ref, ga_ref, lse_ref, b0_ref, dk_ref, dv_ref, quad)

    def project_products(quad):
        if quad == 0:
            kept["n"].wait()
        for number in range(3):
            value = mm_rows(n_ref[...], b0_ref[:, number * D + quad * QUAD : number * D + (quad + 1) * QUAD])
            low = (quad * 3 + number) * QUAD
            wf_ref[:, :, :, low : low + QUAD] = value.astype(BF16).reshape(outer, inner, part, QUAD)

    def input_gradient():
        kept["wqkv"].wait()
        kept["one"], kept["side"] = backward_project(
            tab_ref, rank, x_ref, gh_ref, gains, n_ref, b0_ref, b2_ref, dk_ref, gres_ref
        )

    def gain_pieces():
        rows = jnp.concatenate([kept["one"], kept["side"], kept["gain"], jnp.zeros((5, D), F32)], axis=0)
        spread_gain_grads(rows, dc_ref)

    half = tiles // 2
    work = {
        "start": lambda: None, "P0": enter, "P1a": lambda: inward(0, half), "P1b": lambda: inward(half, tiles),
        "gA": lambda: outer_products(dg_ref, b1_ref, 0, half), "gB": lambda: outer_products(dg_ref, b1_ref, half, tiles),
        "uA": lambda: outer_products(du_ref, b2_ref, 0, half), "uB": lambda: outer_products(du_ref, b2_ref, half, tiles),
        "d": down_products, "out": outward, "P4": middle, "P5": out_products,
        "q0": lambda: attention(0), "q1": lambda: attention(1), "q2": lambda: attention(2),
        "p0": lambda: project_products(0), "p1": lambda: project_products(1), "p2": lambda: project_products(2),
        "bp": input_gradient, "dc": gain_pieces,
    }
    paired = set()
    for action, which, *turn in REAR_ORDER:
        if action == "do":
            work[which]()
        elif action == "begin":
            if which == 6:
                pl.semaphore_wait(free_sem, 1)
            tasks[which].begin()
        elif action == "pair":
            tasks[which].pair()
            paired.add(which)
            if which < 3 and paired >= {0, 1, 2}:
                pl.semaphore_signal(free_sem, inc=1, device_id={"rep": links.mate}, device_id_type=MESH)
        elif action == "meet":
            tasks[which].meet()
        elif action == "col":
            tasks[which].column()
        elif action == "hop":
            tasks[which].hop(turn[0])
        elif action == "cross":
            tasks[which].cross()
        elif action == "fin":
            tasks[which].finish()
        elif action == "rows":
            returns[which].begin()
        else:
            returns[which].relay()
    for one in returns:
        one.settle()
    for task in tasks:
        task.settle()
    links.drain()


def feed_and_reduce(count, table, x, att, lse, gc, cot, n, qkv, wqkv, wf, wd):
    outer, inner = grid_of(count)
    part, tall = D // count, wd.shape[1]
    hidden = count * tall
    wf = wf.reshape((outer, inner) + wf.shape[1:])
    full = [(part, hidden), (part, hidden), (tall, D), (part, D), (part, 3 * D), (8, 128)]
    shapes = [(part, hidden // 2)] * 4 + [(tall, D)] + [(part, D)] * 4 + [(8, 128)]
    kinds = len(shapes)
    dtypes = [BF16] * (kinds - 1) + [F32]
    halved = [(a, b // 2 if b % 256 == 0 else b) for a, b in shapes]
    later = [(a // 2, b) if i in ACROSS_FIRST else (a, b) for i, (a, b) in enumerate(halved)]
    dma, vmem = pltpu.SemaphoreType.DMA, pltpu.VMEM
    scratch = [
        vmem((ROWS, D), BF16), vmem((ROWS, D), F32), vmem((ALL_ROWS, D), F32), vmem((ALL_ROWS, D), F32),
        vmem((ALL_ROWS, 3 * D), BF16), vmem((ALL_ROWS, 3 * D), BF16), vmem((D, 3 * D), BF16),
        vmem((ALL_ROWS, D), BF16), vmem((D, ROWS), BF16), vmem((ROWS, D), BF16), vmem((ROWS, D), BF16),
        vmem(wf.shape, BF16), vmem((hidden, D), BF16),
    ]
    scratch += [vmem((outer, inner) + shape, BF16) for shape in full[:4]]
    scratch += [vmem((outer, inner) + full[-1], F32)] * 2
    scratch += [vmem((outer, inner) + halved[i], dtypes[i]) for i in (0, 1, 2, 3, 4, 5, 9)]
    for lead in ((outer,), (outer + 1,), ()):
        for i in range(kinds):
            across = (outer, inner) if i in ACROSS_FIRST and lead == () else lead
            scratch.append(vmem(across + later[i], dtypes[i]))
    scratch += [vmem(shape, F32) for shape in later]
    for i in ACROSS_FIRST:
        scratch += [vmem(later[i], BF16), vmem(later[i], F32)]
    one = dma((kinds,))
    scratch += [one, one, one, one, one, dma((2, outer, kinds)), dma((outer + 1, kinds))] + [one] * 9
    scratch += [dma((2, 3)), dma((2, 3)), dma((2,)), dma((1,)), dma((7,)), pltpu.SemaphoreType.REGULAR]
    rows = jax.ShapeDtypeStruct((4, ROWS, D), BF16)
    outs = pl.pallas_call(
        partial(rear_kernel, outer, inner),
        out_shape=tuple(jax.ShapeDtypeStruct(shape, F32) for shape in full) + (rows, rows),
        in_specs=[SMEM] + [VMEM] * 4 + [ANY] * 6,
        out_specs=(ANY,) * 8,
        scratch_shapes=scratch,
        compiler_params=pltpu.CompilerParams(
            collective_id=2, has_side_effects=True, vmem_limit_bytes=67043328
        ),
        name="feed_and_reduce",
    )(table, x, att, lse, gc, cot, n, qkv, wqkv, wf, wd.reshape(hidden, D))
    return outs[:6], outs[6], outs[7]


def place_kernel(part, tab_ref, ry_ref, rg_ref, og_ref, ou_ref, od_ref, oo_ref, op_ref, oc_ref, *refs):
    (y_ref, g_ref, q_out, k_out, v_out, o_out, g_out, u_out, d_out, one_out, side_out, two_out), refs = refs[:12], refs[12:]
    (y_buf, g_buf, bg, bu, bd, bo, bp, sem_in, sem_out, sem_rows, sem_home) = refs
    blocks = y_buf.shape[0]
    base = lax.axis_index("rep") * blocks
    tables = ((og_ref, bg), (ou_ref, bu), (od_ref, bd), (oo_ref, bo), (op_ref, bp))
    reads = [pltpu.make_async_copy(src, dst, sem_in.at[i]) for i, (src, dst) in enumerate(tables)]
    rows = ((ry_ref, y_buf, y_ref), (rg_ref, g_buf, g_ref))

    def fetch(block, carry):
        index = tab_ref[48, base + block]
        safe = jnp.maximum(index, 0)
        for kind, (src, buf, _) in enumerate(rows):
            @pl.when(index >= 0)
            def _():
                pltpu.make_async_copy(
                    src.at[lax.div(safe, SLOTS), lax.rem(safe, SLOTS)], buf.at[block], sem_rows.at[kind, block]
                ).start()

            @pl.when(index < 0)
            def _():
                buf[block] = jnp.zeros(buf.shape[1:], buf.dtype)

        return carry

    lax.fori_loop(0, blocks, fetch, 0)
    for read in reads:
        read.start()

    def leave(block, carry):
        index = tab_ref[48, base + block]
        for kind, (src, buf, dst) in enumerate(rows):
            @pl.when(index >= 0)
            def _():
                pltpu.make_async_copy(src.at[0, 0], buf.at[block], sem_rows.at[kind, block]).wait()

            pltpu.make_async_copy(buf.at[block], dst.at[block], sem_home.at[kind, block]).start()
        return carry

    lax.fori_loop(0, blocks, leave, 0)
    for number, out in enumerate((one_out, side_out, two_out)):
        out[...] = oc_ref[number, :part]
    writes = []
    for number, (buf, dst) in enumerate(((bg, g_out), (bu, u_out), (bd, d_out), (bo, o_out))):
        reads[number].wait()
        writes.append(pltpu.make_async_copy(buf, dst, sem_out.at[number]))
        writes[-1].start()
    reads[4].wait()
    for quad in range(D // QUAD):
        for number, dst in enumerate((q_out, k_out, v_out)):
            low = (3 * quad + number) * QUAD
            copy = pltpu.make_async_copy(
                bp.at[:, low : low + QUAD], dst.at[:, quad * QUAD : (quad + 1) * QUAD], sem_out.at[4 + 3 * quad + number]
            )
            copy.start()
            writes.append(copy)
    for write in writes:
        write.wait()

    def rest(block, carry):
        for kind, (_, buf, dst) in enumerate(rows):
            pltpu.make_async_copy(buf.at[block], dst.at[block], sem_home.at[kind, block]).wait()
        return carry

    lax.fori_loop(0, blocks, rest, 0)


def place_all(table, ry, rg, totals, blocks, part, shape):
    out = jax.ShapeDtypeStruct
    og, ou, od, oo, op, oc = totals
    block = (blocks,) + ry.shape[2:]
    dma, vmem = pltpu.SemaphoreType.DMA, pltpu.VMEM
    gain = out((part,), F32)
    y, g, q, k, v, o, gate, up, down, one, side, two = pl.pallas_call(
        partial(place_kernel, part),
        out_shape=(out(block, ry.dtype), out(block, rg.dtype), out(oo.shape, F32), out(oo.shape, F32), out(oo.shape, F32),
                   out(oo.shape, F32), out(og.shape, F32), out(ou.shape, F32), out(od.shape, F32), gain, gain, gain),
        in_specs=[SMEM] + [ANY] * 7 + [VMEM],
        out_specs=(ANY,) * 9 + (VMEM,) * 3,
        scratch_shapes=[vmem(block, ry.dtype), vmem(block, rg.dtype)] + [vmem(t.shape, F32) for t in totals[:5]]
        + [dma((5,)), dma((13,)), dma((2, blocks)), dma((2, blocks))],
        compiler_params=pltpu.CompilerParams(vmem_limit_bytes=VMEM_LIMIT),
        name="place_outputs",
    )(table, ry, rg, og, ou, od, oo, op, oc)
    return (y.reshape(shape), g.reshape(shape), one, side, q, k, v, o, two, gate, up, down)


def per_device(count, layer_input, cotangent, lengths, attn_gain, global_gain, query_weight, key_weight,
               value_weight, out_weight, ffn_gain, gate_weight, up_weight, down_weight):
    micro, span, width = layer_input.shape
    hidden = gate_weight.shape[1]
    blocks = micro * span // BLK
    part = attn_gain.shape[0]
    rows_in = layer_input.reshape(blocks, BLK, width)
    cots_in = cotangent.reshape(blocks, BLK, width)
    weights = (query_weight, key_weight, value_weight, out_weight, gate_weight, up_weight)
    wc = jnp.pad(jnp.stack([attn_gain, global_gain, ffn_gain]), ((0, 13), (0, 128 - part)))
    if grid_of(count)[1] == 2 and part % 16 == 0:
        lens = lax.dynamic_update_slice(
            jnp.zeros((8, 128), jnp.int32), lengths.reshape(1, blocks), (0, lax.axis_index("rep") * blocks)
        )
        table, x, cot, n, qkv, att, lse, wqkv, gc, ga, gb = gather_and_attend(
            count, lens, rows_in, cots_in, weights, down_weight, wc
        )
        totals, ry, rg = feed_and_reduce(count, table, x, att, lse, gc, cot, n, qkv, wqkv, ga, gb)
        ry, rg = (rows.reshape(4, SLOTS, BLK, width) for rows in (ry, rg))
        return place_all(table, ry, rg, totals, blocks, part, layer_input.shape)
    else:
        table = deal_table(lengths)
        splits = ((0, 4 * width), (4 * width, 2 * hidden))
        ga, gb, gc, rows, cots = gather_weights(
            count, splits, table, rows_in, cots_in, jnp.concatenate(weights, axis=1), down_weight, wc
        )
        x, full = rows.reshape(ROWS, width), ga.reshape(width, -1)
        n, qkv, att, lse = attend(table, x, gc, full)
        y, gh, gatt, dg, du, db, do, gain = feed(
            table, x, cots.reshape(ROWS, width), att, gc, full, gb.reshape(-1, width)
        )
        g, dw, dc = backward_layer(table, x, gh, gatt, att, lse, n, qkv, gain, gc, full)
        grads = [grad.reshape(count, -1, grad.shape[-1]) for grad in (dg, du, db, do, dw, dc)]
        og, ou, ob, oo, ow, oc, ry, rg = reduce_grads(
            count, grads, y.reshape(SLOTS, BLK, width), g.reshape(SLOTS, BLK, width)
        )
        oq, ok, ov = ow[:, :width], ow[:, width : 2 * width], ow[:, 2 * width :]
    y_home, g_home = bring_home(table, ry, rg, blocks)
    return (
        y_home.reshape(layer_input.shape), g_home.reshape(layer_input.shape),
        oc[0, :part], oc[1, :part], oq, ok, ov, oo, oc[2, :part], og, ou, ob,
    )


def solution(mesh):
    rows = P(None, ("rep", "fsdp"), None)
    vector, matrix = P("fsdp"), P("fsdp", None)
    return jax.shard_map(
        partial(per_device, mesh.shape["fsdp"]),
        mesh=mesh,
        in_specs=(rows, rows, P(None, ("rep", "fsdp")), vector, vector, matrix, matrix, matrix, matrix,
                  vector, matrix, matrix, matrix),
        out_specs=(rows, rows, vector, vector, matrix, matrix, matrix, matrix, vector, matrix, matrix, matrix),
        check_vma=False,
    )
```

```python
from functools import partial

import jax
import jax.numpy as jnp
from jax import lax
from jax.experimental import pallas as pl
from jax.experimental.pallas import tpu as pltpu
from jax.sharding import PartitionSpec as P

H = 12
DH = 64
RADIUS = 127
GBLK = 16
BLK = 64
SLOTS = 10
MAX_SEQ_BLOCKS = 5
EPSILON = 1e-06
MASKED_SCORE = -1e30
MESH = pl.DeviceIdType.MESH
VMEM_LIMIT = 60 * 1024 * 1024
SEG_AT, LEN_AT, DEST_AT, TABLE_SIZE = 40, 80, 120, 256

ANY = pl.BlockSpec(memory_space=pl.ANY)
VMEM = pl.BlockSpec(memory_space=pltpu.VMEM)
SMEM = pl.BlockSpec(memory_space=pltpu.SMEM)


def grid_of(count):
    inner = 2 if count <= 8 else 4
    return count // inner, inner


def core_of(rank):
    return rank + 1 - 2 * (rank % 2)


def across_of(rank):
    return (rank + 2) % 4


def lens_kernel(lens_ref, all_ref, send_sem, recv_sem):
    rank = lax.axis_index("rep")
    barrier = pltpu.get_barrier_semaphore()
    for step in range(1, 4):
        pl.semaphore_signal(
            barrier, inc=1, device_id={"rep": (rank + step) % 4}, device_id_type=MESH
        )
    pl.semaphore_wait(barrier, 3)
    copies = []
    for step in range(1, 4):
        copy = pltpu.make_async_remote_copy(
            src_ref=lens_ref,
            dst_ref=all_ref.at[rank],
            send_sem=send_sem.at[step - 1],
            recv_sem=recv_sem.at[step - 1],
            device_id={"rep": (rank + step) % 4},
            device_id_type=MESH,
        )
        copy.start()
        copies.append(copy)
    all_ref[rank] = lens_ref[...]
    for copy in copies:
        copy.wait()


def table_kernel(micro, per_dev, lens_ref, tab_ref, order_ref, count_ref, load_ref):
    total = 4 * micro * per_dev

    def length_at(spot):
        return lens_ref[spot // (micro * per_dev), (spot // per_dev) % micro, spot % per_dev]

    def blocks_of(length):
        return (length + (BLK - 1)) // BLK

    def clear(spot, carry):
        tab_ref[spot] = -1
        return carry

    lax.fori_loop(0, TABLE_SIZE, clear, 0)
    for spot in range(4 * SLOTS):
        tab_ref[LEN_AT + spot] = 0
    for size in range(8):
        count_ref[size] = 0
    for dev in range(4):
        load_ref[dev] = 0

    def tally(spot, carry):
        length = length_at(spot)

        @pl.when(length > 0)
        def _():
            size = blocks_of(length)
            count_ref[size] = count_ref[size] + 1

        return carry

    lax.fori_loop(0, total, tally, 0)
    begin = 0
    for size in range(MAX_SEQ_BLOCKS, 0, -1):
        amount = count_ref[size]
        count_ref[size] = begin
        begin = begin + amount

    def place(spot, carry):
        length = length_at(spot)

        @pl.when(length > 0)
        def _():
            size = blocks_of(length)
            where = count_ref[size]
            order_ref[where] = spot
            count_ref[size] = where + 1

        return carry

    lax.fori_loop(0, total, place, 0)

    def assign(number, carry):
        spot = order_ref[number]
        length = length_at(spot)
        size = blocks_of(length)
        best = jnp.int32(0)
        low = load_ref[0]
        for dev in range(1, 4):
            here = load_ref[dev]
            best = jnp.where(here < low, dev, best)
            low = jnp.minimum(here, low)
        load_ref[best] = low + size

        def put(step, inner):
            slot = best * SLOTS + low + step
            tab_ref[slot] = spot + step
            tab_ref[SEG_AT + slot] = low
            tab_ref[LEN_AT + slot] = jnp.minimum(length - BLK * step, BLK)
            tab_ref[DEST_AT + spot + step] = slot
            return inner

        lax.fori_loop(0, size, put, 0)
        return carry

    lax.fori_loop(0, begin, assign, 0)


def deal_table(lengths):
    micro, per_dev = lengths.shape
    padded = jnp.pad(lengths, ((0, 8 - micro), (0, 128 - per_dev)))
    everyone = pl.pallas_call(
        lens_kernel,
        out_shape=jax.ShapeDtypeStruct((4, 8, 128), jnp.int32),
        in_specs=[VMEM],
        out_specs=VMEM,
        scratch_shapes=[pltpu.SemaphoreType.DMA((3,)), pltpu.SemaphoreType.DMA((3,))],
        compiler_params=pltpu.CompilerParams(collective_id=0, has_side_effects=True),
        name="lens_exchange",
    )(padded)
    return pl.pallas_call(
        partial(table_kernel, micro, per_dev),
        out_shape=jax.ShapeDtypeStruct((TABLE_SIZE,), jnp.int32),
        in_specs=[SMEM],
        out_specs=SMEM,
        scratch_shapes=[
            pltpu.SMEM((4 * micro * per_dev,), jnp.int32),
            pltpu.SMEM((8,), jnp.int32),
            pltpu.SMEM((4,), jnp.int32),
        ],
        name="deal_table",
    )(everyone)


def gather_kernel(
    outer, inner, splits, tab_ref, rows_ref, cots_ref, wa_ref, wb_ref, wc_ref,
    ga_ref, gb_ref, gc_ref, rows_out, cots_out,
    psend, precv, xsend, xrecv,
    z_send, z_recv, y_send, y_recv, c_send, c_recv, own_sem,
    p_send, p_recv, x_send, x_recv,
):
    rank = lax.axis_index("rep")
    spot = lax.axis_index("fsdp")
    core = rank % 2
    row, col = spot // inner, spot % inner
    count = outer * inner
    mate, across = core_of(rank), across_of(rank)
    pieces = [(wa_ref, ga_ref, start, width // 2) for start, width in splits]
    pieces.append((wb_ref, gb_ref, 0, wb_ref.shape[1] // 2))
    pieces.append((wc_ref, gc_ref, 0, None))
    halved = [number for number, piece in enumerate(pieces) if piece[3] is not None]

    barrier = pltpu.get_barrier_semaphore()
    neighbours = (
        (row + 1 < outer, {"fsdp": spot + inner}),
        (row > 0, {"fsdp": spot - inner}),
        (col + 1 < inner, {"fsdp": spot + 1}),
        (col > 0, {"fsdp": spot - 1}),
    )
    amount = jnp.int32(2)
    for there, device in neighbours:
        amount = amount + there.astype(jnp.int32)

        @pl.when(there)
        def _():
            pl.semaphore_signal(barrier, inc=1, device_id=device, device_id_type=MESH)

    for device in (mate, across):
        pl.semaphore_signal(barrier, inc=1, device_id={"rep": device}, device_id_type=MESH)
    pl.semaphore_wait(barrier, amount)

    def cut(ref, number):
        _, _, start, half = pieces[number]
        if half is None:
            return ref
        return ref.at[:, pl.ds(pl.multiple_of(start + core * half, 128), half)]

    def landed(number, shard):
        return cut(pieces[number][1].at[shard], number)

    late = []

    def send(there, src, dst, ssem, rsem, device):
        def describe():
            return pltpu.make_async_remote_copy(
                src_ref=src, dst_ref=dst, send_sem=ssem, recv_sem=rsem,
                device_id=device, device_id_type=MESH,
            )

        if there is None:
            describe().start()
            late.append((None, lambda: describe().wait_send()))
        else:
            @pl.when(there)
            def _():
                describe().start()

            late.append((there, lambda: describe().wait_send()))

    def arrive(number, shard, rsem):
        pltpu.make_async_remote_copy(
            src_ref=landed(number, shard), dst_ref=landed(number, shard),
            send_sem=own_sem.at[0], recv_sem=rsem,
            device_id={"rep": mate}, device_id_type=MESH,
        ).wait_recv()

    def both(first, second):
        return second if first is None else jnp.logical_and(first, second)

    def to_mate(there, number, shard):
        if number not in halved:
            return
        place = landed(number, shard)
        send(there, place, place, c_send.at[number, shard], c_recv.at[number, shard], {"rep": mate})

    def along_row(there, number, line, src):
        shard = line * inner + col
        place = landed(number, shard)
        src = place if src is None else src
        send(both(there, col + 1 < inner), src, place,
             y_send.at[0, 0, line, number], y_recv.at[0, 0, line, number], {"fsdp": spot + 1})
        send(both(there, col > 0), src, place,
             y_send.at[1, 0, line, number], y_recv.at[1, 0, line, number], {"fsdp": spot - 1})

    def from_row(there, number, line):
        for step in range(inner - 1):
            for way, source, onward, target in (
                (0, col - 1 - step, col + 1 < inner, spot + 1),
                (1, col + 1 + step, col > 0, spot - 1),
            ):
                here = jnp.logical_and(source >= 0, source < inner)
                here = both(there, here)
                shard = line * inner + source

                @pl.when(here)
                def _():
                    arrive(number, shard, y_recv.at[way, step, line, number])

                if step + 1 < inner - 1:
                    place = landed(number, shard)
                    send(both(here, onward), place, place,
                         y_send.at[way, step + 1, line, number],
                         y_recv.at[way, step + 1, line, number], {"fsdp": target})
                to_mate(here, number, shard)

    for number, piece in enumerate(pieces):
        src, place = cut(piece[0], number), landed(number, spot)
        send(row + 1 < outer, src, place, z_send.at[0, 0, number], z_recv.at[0, 0, number],
             {"fsdp": spot + inner})
        send(row > 0, src, place, z_send.at[1, 0, number], z_recv.at[1, 0, number],
             {"fsdp": spot - inner})
        along_row(None, number, row, src)
    own = [
        pltpu.make_async_copy(wa_ref, ga_ref.at[spot], own_sem.at[0]),
        pltpu.make_async_copy(wb_ref, gb_ref.at[spot], own_sem.at[1]),
        pltpu.make_async_copy(wc_ref, gc_ref.at[spot], own_sem.at[2]),
    ]
    for copy in own:
        copy.start()

    sources = (rows_ref, cots_ref)
    per_rank = rows_ref.shape[0]

    def picked(kind, target, slot):
        index = tab_ref[target * SLOTS + slot] - rank * per_rank
        mine = jnp.logical_and(index >= 0, index < per_rank)
        value = sources[kind][jnp.clip(index, 0, per_rank - 1)]
        return mine, value

    def mate_copy(kind, part):
        return pltpu.make_async_remote_copy(
            src_ref=psend.at[kind, part], dst_ref=precv.at[kind, part],
            send_sem=p_send.at[kind, part], recv_sem=p_recv.at[kind, part],
            device_id={"rep": mate}, device_id_type=MESH,
        )

    def across_copy(kind):
        return pltpu.make_async_remote_copy(
            src_ref=xsend.at[kind], dst_ref=xrecv.at[kind],
            send_sem=x_send.at[kind], recv_sem=x_recv.at[kind],
            device_id={"rep": across}, device_id_type=MESH,
        )

    for kind, part in ((0, 1), (1, 1), (0, 0), (1, 0)):
        target = mate if part == 0 else across_of(mate)

        def pack(slot, carry):
            mine, value = picked(kind, target, slot)
            psend[kind, part, slot] = jnp.where(mine, value, jnp.zeros_like(value))
            return carry

        lax.fori_loop(0, SLOTS, pack, 0)
        mate_copy(kind, part).start()
    for kind in range(2):
        mate_copy(kind, 1).wait_recv()

        def merge(slot, carry):
            mine, value = picked(kind, across, slot)
            xsend[kind, slot] = jnp.where(mine, value, precv[kind, 1, slot])
            return carry

        lax.fori_loop(0, SLOTS, merge, 0)
        across_copy(kind).start()

    def lines(step):
        return ((row - 1 - step >= 0, row - 1 - step, 0, row + 1 < outer, spot + inner),
                (row + 1 + step < outer, row + 1 + step, 1, row > 0, spot - inner))

    for step in range(outer - 1):
        for number in range(len(pieces)):
            for here, line, way, onward, target in lines(step):
                shard = line * inner + col

                @pl.when(here)
                def _():
                    arrive(number, shard, z_recv.at[way, step, number])

                if step + 1 < outer - 1:
                    place = landed(number, shard)
                    send(jnp.logical_and(here, onward), place, place,
                         z_send.at[way, step + 1, number], z_recv.at[way, step + 1, number],
                         {"fsdp": target})
                along_row(here, number, line, None)
                to_mate(here, number, shard)
        for number in range(len(pieces)):
            if step == 0:
                from_row(None, number, row)
            else:
                for here, line, *_ in lines(step - 1):
                    from_row(here, number, line)
    for number in range(len(pieces)):
        for here, line, *_ in lines(outer - 2):
            from_row(here, number, line)

    outs = (rows_out, cots_out)
    for kind in range(2):
        mate_copy(kind, 0).wait_recv()
        across_copy(kind).wait_recv()

        def finish(slot, carry):
            mine, value = picked(kind, rank, slot)
            outs[kind][slot] = jnp.where(mine, value, precv[kind, 0, slot] + xrecv[kind, slot])
            return carry

        lax.fori_loop(0, SLOTS, finish, 0)

    for shard in range(count):
        @pl.when(shard != spot)
        def _():
            for number in halved:
                other = pieces[number]
                view = other[1].at[shard].at[:, pl.ds(0, other[3])]
                pltpu.make_async_remote_copy(
                    src_ref=view, dst_ref=view, send_sem=own_sem.at[0],
                    recv_sem=c_recv.at[number, shard],
                    device_id={"rep": mate}, device_id_type=MESH,
                ).wait_recv()
    for there, finish_send in late:
        if there is None:
            finish_send()
        else:
            pl.when(there)(finish_send)
    for kind in range(2):
        for part in range(2):
            mate_copy(kind, part).wait_send()
        across_copy(kind).wait_send()
    for copy in own:
        copy.wait()


def gather_weights(count, splits, table, rows, cots, wa, wb, wc):
    outer, inner = grid_of(count)
    block = rows.shape[1:]
    kinds = len(splits) + 2
    dma = pltpu.SemaphoreType.DMA
    bf16 = jnp.bfloat16
    return pl.pallas_call(
        partial(gather_kernel, outer, inner, splits),
        out_shape=(
            jax.ShapeDtypeStruct((count,) + wa.shape, bf16),
            jax.ShapeDtypeStruct((count,) + wb.shape, bf16),
            jax.ShapeDtypeStruct((count,) + wc.shape, bf16),
            jax.ShapeDtypeStruct((SLOTS,) + block, bf16),
            jax.ShapeDtypeStruct((SLOTS,) + block, bf16),
        ),
        in_specs=[SMEM, VMEM, VMEM, VMEM, VMEM, VMEM],
        out_specs=(ANY, ANY, ANY, VMEM, VMEM),
        scratch_shapes=[
            pltpu.VMEM((2, 2, SLOTS) + block, bf16),
            pltpu.VMEM((2, 2, SLOTS) + block, bf16),
            pltpu.VMEM((2, SLOTS) + block, bf16),
            pltpu.VMEM((2, SLOTS) + block, bf16),
            dma((2, outer - 1, kinds)), dma((2, outer - 1, kinds)),
            dma((2, inner - 1, outer, kinds)), dma((2, inner - 1, outer, kinds)),
            dma((kinds, count)), dma((kinds, count)), dma((3,)),
            dma((2, 2)), dma((2, 2)), dma((2,)), dma((2,)),
        ],
        compiler_params=pltpu.CompilerParams(
            collective_id=1, has_side_effects=True, vmem_limit_bytes=VMEM_LIMIT
        ),
        name="gather_and_deal",
    )(table, rows, cots, wa, wb, wc)


def reduce_kernel(
    outer, inner, kinds, *refs
):
    grads, (y_ref, g_ref) = refs[:kinds], refs[kinds : kinds + 2]
    totals, (ry_ref, rg_ref) = refs[kinds + 2 : 2 * kinds + 2], refs[2 * kinds + 2 : 2 * kinds + 4]
    scratch = refs[2 * kinds + 4 :]
    mines, crecvs, yrecvs, zrecvs, xrecvs = (
        scratch[kinds * i : kinds * (i + 1)] for i in range(5)
    )
    (c_send, c_recv, m_sem, y_send, y_recv, z_send, z_recv, x_send, x_recv, f_send, f_recv,
     r_send, r_recv, q_sem) = scratch[5 * kinds :]
    rank = lax.axis_index("rep")
    spot = lax.axis_index("fsdp")
    core = rank % 2
    row, col = spot // inner, spot % inner
    mate, across = core_of(rank), across_of(rank)
    pieces = [(src, dst, 0, src.shape[3] // 2) for src, dst in zip(grads[:-1], totals)]
    pieces.append((grads[-1], totals[-1], 0, None))

    barrier = pltpu.get_barrier_semaphore()
    neighbours = (
        (row + 1 < outer, {"fsdp": spot + inner}),
        (row > 0, {"fsdp": spot - inner}),
        (col + 1 < inner, {"fsdp": spot + 1}),
        (col > 0, {"fsdp": spot - 1}),
    )
    amount = jnp.int32(2)
    for there, device in neighbours:
        amount = amount + there.astype(jnp.int32)

        @pl.when(there)
        def _():
            pl.semaphore_signal(barrier, inc=1, device_id=device, device_id_type=MESH)

    for device in (mate, across):
        pl.semaphore_signal(barrier, inc=1, device_id={"rep": device}, device_id_type=MESH)
    pl.semaphore_wait(barrier, amount)

    late = []

    def send(there, src, dst, ssem, rsem, device):
        def describe():
            return pltpu.make_async_remote_copy(
                src_ref=src, dst_ref=dst, send_sem=ssem, recv_sem=rsem,
                device_id=device, device_id_type=MESH,
            )

        if there is None:
            describe().start()
            late.append((None, lambda: describe().wait_send()))
        else:
            @pl.when(there)
            def _():
                describe().start()

            late.append((there, lambda: describe().wait_send()))

    def arrive(place, rsem):
        pltpu.make_async_remote_copy(
            src_ref=place, dst_ref=place, send_sem=q_sem.at[0], recv_sem=rsem,
            device_id={"rep": mate}, device_id_type=MESH,
        ).wait_recv()

    def columns(ref, number, which):
        _, _, start, half = pieces[number]
        if half is None:
            return ref
        cols = pl.ds(pl.multiple_of(start + which * half, 128), half)
        return ref.at[:, :, :, cols] if len(ref.shape) == 4 else ref.at[:, cols]

    order = list(range(kinds))
    loads = []
    for number in order:
        src = columns(pieces[number][0], number, 1 - core)
        send(None, src, crecvs[number], c_send.at[number], c_recv.at[number], {"rep": mate})
        load = pltpu.make_async_copy(
            columns(pieces[number][0], number, core), mines[number], m_sem.at[number]
        )
        load.start()
        loads.append(load)

    for kind, (src, dst) in enumerate(((y_ref, ry_ref), (g_ref, rg_ref))):
        send(None, src, dst.at[rank], r_send.at[kind, 0], r_recv.at[kind, 0], {"rep": across})
        send(None, src, dst.at[rank], r_send.at[kind, 1], r_recv.at[kind, 1], {"rep": mate})
        pltpu.make_async_copy(src, dst.at[rank], q_sem.at[kind + 1]).start()

    def slot_of(way, size, place, dest):
        if size == 2:
            return 0
        return dest - place if way == 0 else size - place + dest

    def line_sum(number, size, place, stride, buffer, view, ssem, rsem):
        for far in range(size - 1, 0, -1):
            for way in range(2):
                dest = far if way == 0 else size - 1 - far
                step = 1 if way == 0 else -1
                passes = place < dest if way == 0 else place > dest
                first = place == 0 if way == 0 else place == size - 1
                mine = view(dest)
                got = slot_of(way, size, place, dest)

                @pl.when(jnp.logical_and(passes, jnp.logical_not(first)))
                def _():
                    arrive(buffer.at[got], rsem.at[got, number])
                    mine[...] = mine[...] + buffer[got]

                put = slot_of(way, size, place + step, dest)
                send(passes, mine, buffer.at[put], ssem.at[way, dest, number], rsem.at[put, number],
                     {"fsdp": spot + step * stride})
        for way in range(2):
            has = place > 0 if way == 0 else place < size - 1
            got = slot_of(way, size, place, place)
            mine = view(place)

            @pl.when(has)
            def _():
                arrive(buffer.at[got], rsem.at[got, number])
                mine[...] = mine[...] + buffer[got]

    for number in order:
        loads[number].wait()
        arrive(crecvs[number], c_recv.at[number])
        mine, other = mines[number], crecvs[number]

        def add(index, carry):
            mine[index // inner, index % inner] = (
                mine[index // inner, index % inner] + other[index // inner, index % inner]
            )
            return carry

        lax.fori_loop(0, outer * inner, add, 0)
        if inner == 2:
            send(None, mine.at[:, 1 - col], yrecvs[number].at[0], y_send.at[0, 0, number],
                 y_recv.at[0, number], {"fsdp": spot + 1 - 2 * col})
    for kind, dst in enumerate((ry_ref, rg_ref)):
        place = dst.at[across]
        arrive(place, r_recv.at[kind, 0])
        send(None, place, place, r_send.at[kind, 2], r_recv.at[kind, 2], {"rep": mate})
    for number in order:
        mine = mines[number]
        if inner == 2:
            arrive(yrecvs[number].at[0], y_recv.at[0, number])
            buffer = yrecvs[number]

            def add(index, carry):
                mine[index, col] = mine[index, col] + buffer[0, index]
                return carry

            lax.fori_loop(0, outer, add, 0)
        else:
            line_sum(number, inner, col, 1, yrecvs[number], lambda dest: mine.at[:, dest],
                     y_send, y_recv)
        line_sum(number, outer, row, inner, zrecvs[number], lambda dest: mine.at[dest, col],
                 z_send, z_recv)
        send(None, mine.at[row, col], xrecvs[number], x_send.at[number], x_recv.at[number],
             {"rep": across})
    for number in order:
        arrive(xrecvs[number], x_recv.at[number])
        total = mines[number][row, col].astype(jnp.float32) + xrecvs[number][...].astype(jnp.float32)
        out, half = pieces[number][1], pieces[number][3]
        place = columns(out, number, core)
        place[...] = total
        if half is not None:
            send(None, place, place, f_send.at[number], f_recv.at[number], {"rep": mate})
    for number in order:
        if pieces[number][3] is not None:
            arrive(columns(pieces[number][1], number, 1 - core), f_recv.at[number])
    for kind, dst in enumerate((ry_ref, rg_ref)):
        arrive(dst.at[mate], r_recv.at[kind, 1])
        arrive(dst.at[across_of(mate)], r_recv.at[kind, 2])
        src = y_ref if kind == 0 else g_ref
        pltpu.make_async_copy(src, dst.at[rank], q_sem.at[kind + 1]).wait()
    for there, finish_send in late:
        if there is None:
            finish_send()
        else:
            pl.when(there)(finish_send)


def reduce_grads(count, grads, y_rows, g_rows):
    outer, inner = grid_of(count)
    kinds = len(grads)
    shapes = [(grad.shape[1], grad.shape[2] // 2, grad.dtype) for grad in grads[:-1]]
    shapes.append(grads[-1].shape[1:] + (grads[-1].dtype,))
    dma = pltpu.SemaphoreType.DMA
    y_slots = 1 if inner == 2 else inner + 1
    z_slots = 1 if outer == 2 else outer + 1
    scratch = []
    for lead in ((outer, inner), (outer, inner), (y_slots, outer), (z_slots,), ()):
        scratch += [pltpu.VMEM(lead + (a, b), dtype) for a, b, dtype in shapes]
    scratch += [
        dma((kinds,)), dma((kinds,)), dma((kinds,)),
        dma((2, inner, kinds)), dma((y_slots, kinds)),
        dma((2, outer, kinds)), dma((z_slots, kinds)),
        dma((kinds,)), dma((kinds,)), dma((kinds,)), dma((kinds,)),
        dma((2, 3)), dma((2, 3)), dma((3,)),
    ]
    return pl.pallas_call(
        partial(reduce_kernel, outer, inner, kinds),
        out_shape=tuple(jax.ShapeDtypeStruct(grad.shape[1:], jnp.float32) for grad in grads) + (
            jax.ShapeDtypeStruct((4,) + y_rows.shape, y_rows.dtype),
            jax.ShapeDtypeStruct((4,) + g_rows.shape, g_rows.dtype),
        ),
        in_specs=[ANY] * (kinds + 2),
        out_specs=(VMEM,) * kinds + (ANY, ANY),
        scratch_shapes=scratch,
        compiler_params=pltpu.CompilerParams(
            collective_id=2, has_side_effects=True, vmem_limit_bytes=VMEM_LIMIT
        ),
        name="reduce_and_return",
    )(*(grad.reshape((outer, inner) + grad.shape[1:]) for grad in grads), y_rows, g_rows)


def home_kernel(tab_ref, ry_ref, rg_ref, y_ref, g_ref):
    base = lax.axis_index("rep") * y_ref.shape[0]

    def fetch(block, carry):
        index = tab_ref[DEST_AT + base + block] if len(tab_ref.shape) == 1 else tab_ref[48, base + block]
        safe = jnp.maximum(index, 0)
        for src, dst in ((ry_ref, y_ref), (rg_ref, g_ref)):
            value = src[safe // SLOTS, safe % SLOTS]
            dst[block] = jnp.where(index >= 0, value, jnp.zeros_like(value))
        return carry

    lax.fori_loop(0, y_ref.shape[0], fetch, 0)


def bring_home(table, ry, rg, blocks):
    shape = jax.ShapeDtypeStruct((blocks,) + ry.shape[2:], ry.dtype)
    return pl.pallas_call(
        home_kernel,
        out_shape=(shape, shape),
        in_specs=[SMEM, VMEM, VMEM],
        out_specs=(VMEM, VMEM),
        compiler_params=pltpu.CompilerParams(vmem_limit_bytes=VMEM_LIMIT),
        name="place_rows",
    )(table, ry, rg)


D = H * DH
ROWS = SLOTS * BLK
SIDES = SLOTS * (BLK // GBLK)
SIDE_ROWS = 48
ALL_ROWS = ROWS + SIDE_ROWS
QT = 128
WIN = 384
TILES = ROWS // QT
QUAD = 256
FF_TILE = 256
GELU_C = 0.7978845608028654
GELU_A = 0.044715
F32, BF16 = jnp.float32, jnp.bfloat16


def mm(left, right):
    return lax.dot_general(left, right, (((1,), (0,)), ((), ())), preferred_element_type=F32)


def mm_cols(left, right):
    return lax.dot_general(left, right, (((1,), (1,)), ((), ())), preferred_element_type=F32)


def mm_rows(left, right):
    return lax.dot_general(left, right, (((0,), (0,)), ((), ())), preferred_element_type=F32)


def iota(shape, axis):
    return lax.broadcasted_iota(jnp.int32, shape, axis)


def pick_by(index, values, other):
    out = jnp.full(index.shape, other, jnp.int32)
    for number, value in enumerate(values):
        out = jnp.where(index == number, value, out)
    return out


def block_at(tab_ref, slot):
    return lax.rem(tab_ref[slot, 0], 128) - 1


def seg_at(tab_ref, slot):
    if len(tab_ref.shape) == 1:
        return tab_ref[SEG_AT + slot]
    return lax.div(tab_ref[slot, 0], 16384) - 1


def len_at(tab_ref, slot):
    if len(tab_ref.shape) == 1:
        return tab_ref[LEN_AT + slot]
    return lax.rem(lax.div(tab_ref[slot, 0], 128), 128)


def slot_info(tab_ref, rank):
    seg = [seg_at(tab_ref, rank * SLOTS + slot) for slot in range(SLOTS)]
    length = [len_at(tab_ref, rank * SLOTS + slot) for slot in range(SLOTS)]
    return seg, length


def valid_column(tab_ref, rank):
    _, length = slot_info(tab_ref, rank)
    row = iota((ROWS, 1), 0)
    return ((row % BLK) < pick_by(row // BLK, length, 0)).astype(F32)


def pooling(tab_ref, rank):
    _, length = slot_info(tab_ref, rank)
    row = iota((1, ROWS), 1)
    block = jnp.where((row % BLK) < pick_by(row // BLK, length, 0), row // GBLK, -1)
    return jnp.where(iota((SIDE_ROWS, ROWS), 0) == block, 1.0, 0.0).astype(BF16)


def key_segments(tab_ref, rank, first_block, index):
    blocks = WIN // BLK
    base = rank * SLOTS + first_block
    seg = [seg_at(tab_ref, base + step) for step in range(blocks)]
    length = [len_at(tab_ref, base + step) for step in range(blocks)]
    alive = (index % BLK) < pick_by(index // BLK, length, 0)
    return jnp.where(alive, pick_by(index // BLK, seg, -2), -2)


def side_segments(tab_ref, rank, index):
    seg, length = slot_info(tab_ref, rank)
    per = BLK // GBLK
    alive = (index % per) * GBLK < pick_by(index // per, length, 0)
    return jnp.where(alive, pick_by(index // per, seg, -2), -2)


def tile_bias(tab_ref, rank, tile, first_row, keys_axis):
    qs, ks, gs = ((QT, 1), (1, WIN), (1, SIDE_ROWS)) if keys_axis == 1 else ((1, QT), (WIN, 1), (SIDE_ROWS, 1))
    q_index = iota(qs, 1 - keys_axis)
    k_index = iota(ks, keys_axis)
    g_index = iota(gs, keys_axis)
    base = rank * SLOTS + tile * (QT // BLK)
    q_seg = pick_by(q_index // BLK, [seg_at(tab_ref, base + step) for step in range(QT // BLK)], -1)
    k_seg = key_segments(tab_ref, rank, first_row // BLK, k_index)
    g_seg = side_segments(tab_ref, rank, g_index)
    gap = (q_index + tile * QT) - (k_index + first_row)
    local = (jnp.abs(gap) <= RADIUS) & (q_seg == k_seg)
    return jnp.where(local, 0.0, MASKED_SCORE), jnp.where(q_seg == g_seg, 0.0, MASKED_SCORE)


def window_start(tile):
    return pl.multiple_of(jnp.clip(tile - 1, 0, TILES - WIN // QT) * QT, QT)


def head_stack(rows):
    lane = iota(rows.shape, 1) // DH
    zero = jnp.zeros_like(rows)
    return jnp.concatenate([jnp.where(lane == head, rows, zero) for head in range(QUAD // DH)], axis=0)


def head_merge(stacked):
    lane = iota((QT, QUAD), 1) // DH
    out = stacked[:QT]
    for head in range(1, QUAD // DH):
        out = jnp.where(lane == head, stacked[head * QT : (head + 1) * QT], out)
    return out


def gains_of(gc_ref):
    count = gc_ref.shape[0]
    part = D // count
    lane, column = iota((128, D), 0), iota((128, D), 1)
    total = None
    for shard in range(count):
        pick = jnp.where((column == lane + shard * part) & (lane < part), 1.0, 0.0).astype(BF16)
        term = mm(gc_ref[shard], pick)
        total = term if total is None else total + term
    return total


def three_way(value):
    high = value.astype(BF16)
    rest = value - high.astype(F32)
    middle = rest.astype(BF16)
    return high, middle, (rest - middle.astype(F32)).astype(BF16)


def spread_gain_grads(value, dc_ref):
    count = dc_ref.shape[0] if len(dc_ref.shape) == 3 else dc_ref.shape[0] * dc_ref.shape[1]
    part = D // count
    column, lane = iota((D, 128), 0), iota((D, 128), 1)
    parts = three_way(value)
    for shard in range(count):
        pick = jnp.where((column == lane + shard * part) & (lane < part), 1.0, 0.0).astype(BF16)
        place = dc_ref.at[shard] if len(dc_ref.shape) == 3 else dc_ref.at[shard // dc_ref.shape[1], shard % dc_ref.shape[1]]
        place[...] = mm(parts[0], pick) + mm(parts[1], pick) + mm(parts[2], pick)


def mean_square(value):
    return jnp.mean(value * value, axis=-1, keepdims=True)


def forward_norm(tab_ref, rank, x_ref, gains, n_ref):
    for tile in range(TILES):
        rows = pl.ds(tile * QT, QT)
        value = x_ref[rows, :].astype(F32)
        n_ref[rows, :] = (value * lax.rsqrt(mean_square(value) + EPSILON) * gains[0:1]).astype(BF16)
    side = mm(pooling(tab_ref, rank), n_ref[:ROWS, :])
    n_ref[ROWS:, :] = (side * lax.rsqrt(mean_square(side) + EPSILON) * gains[1:2]).astype(BF16)


def forward_project(n_ref, w_ref, qkv_ref):
    def step(tile, carry):
        cols = pl.ds(pl.multiple_of(tile * QUAD, QUAD), QUAD)
        qkv_ref[:, cols] = mm(n_ref[...], w_ref[:, cols]).astype(BF16)
        return carry

    lax.fori_loop(0, 3 * D // QUAD, step, 0)


def forward_attention(tab_ref, rank, qkv_ref, att_ref, lse_ref, begin, end):
    heads = QUAD // DH

    def step(tile, carry):
        first = window_start(tile)
        bias, side_bias = tile_bias(tab_ref, rank, tile, first, 1)
        rows = pl.ds(pl.multiple_of(tile * QT, QT), QT)
        window = pl.ds(first, WIN)
        lane = iota((QT, 128), 1)

        def four(quad, lse):
            low = pl.multiple_of(quad * QUAD, QUAD)
            cols, key_cols, value_cols = (pl.ds(low + number * D, QUAD) for number in range(3))
            query = head_stack(qkv_ref[rows, cols])
            scores = mm_cols(query, qkv_ref[window, key_cols])
            side_scores = mm_cols(query, qkv_ref[ROWS:, key_cols])
            local, sides, scale = [], [], []
            for head in range(heads):
                part = slice(head * QT, (head + 1) * QT)
                one = scores[part] + bias
                two = side_scores[part] + side_bias
                peak = jnp.maximum(
                    jnp.max(one, axis=-1, keepdims=True), jnp.max(two, axis=-1, keepdims=True)
                )
                one, two = jnp.exp(one - peak), jnp.exp(two - peak)
                total = jnp.sum(one, axis=-1, keepdims=True) + jnp.sum(two, axis=-1, keepdims=True)
                local.append(one.astype(BF16))
                sides.append(two.astype(BF16))
                scale.append(1.0 / total)
                lse = jnp.where(lane == quad * heads + head, peak + jnp.log(total), lse)
            mixed = mm(jnp.concatenate(local, axis=0), qkv_ref[window, value_cols])
            mixed = mixed + mm(jnp.concatenate(sides, axis=0), qkv_ref[ROWS:, value_cols])
            mixed = mixed * jnp.concatenate(scale, axis=0)
            att_ref[rows, cols] = head_merge(mixed).astype(BF16)
            return lse

        lse = lax.fori_loop(0, D // QUAD, four, jnp.zeros((QT, 128), F32))
        lse_ref[tile] = jnp.transpose(lse)[:16]
        return carry

    lax.fori_loop(begin, end, step, 0)


def feed_forward(tab_ref, rank, x_ref, cot_ref, att_ref, gains, w_ref, wb_ref,
                 y_ref, gh_ref, ga_ref, dg_ref, du_ref, db_ref, do_ref,
                 h1_ref, nt_ref, ntt_ref, gres_ref, h2_ref, gg_ref, gu_ref, gn_ref):
    hidden = wb_ref.shape[0]
    gate_at = w_ref.shape[1] - 2 * hidden
    out_at = gate_at - D
    valid = valid_column(tab_ref, rank)
    gain = gains[2:3]
    for tile in range(TILES):
        rows = pl.ds(tile * QT, QT)
        value = x_ref[rows, :].astype(F32) + mm(att_ref[rows, :], w_ref[:, out_at:gate_at])
        h1_ref[rows, :] = value
        normed = (value * lax.rsqrt(mean_square(value) + EPSILON) * gain).astype(BF16)
        nt_ref[rows, :] = normed
        ntt_ref[:, tile * QT : (tile + 1) * QT] = jnp.transpose(normed)
        gres_ref[rows, :] = (cot_ref[rows, :].astype(F32) * valid[tile * QT : (tile + 1) * QT]).astype(BF16)

    def inward(tile, carry):
        at = pl.multiple_of(tile * FF_TILE, FF_TILE)
        cols = pl.ds(at, FF_TILE)
        gate = mm(nt_ref[...], w_ref[:, pl.ds(gate_at + at, FF_TILE)])
        up = mm(nt_ref[...], w_ref[:, pl.ds(gate_at + hidden + at, FF_TILE)])
        back = mm_cols(gres_ref[...], wb_ref[cols, :])
        square = gate * gate
        bend = jnp.tanh(GELU_C * (gate * (1.0 + GELU_A * square)))
        half = 0.5 * (1.0 + bend)
        act = gate * half
        slope = half + (0.5 * GELU_C) * gate * (1.0 - bend * bend) * (1.0 + (3.0 * GELU_A) * square)
        h2_ref[:, cols] = (act * up).astype(BF16)
        gg_ref[:, cols] = (back * up * slope).astype(BF16)
        gu_ref[:, cols] = (back * act).astype(BF16)
        return carry

    lax.fori_loop(0, hidden // FF_TILE, inward, 0)

    def outward(tile, carry):
        cols = pl.ds(pl.multiple_of(tile * QUAD, QUAD), QUAD)
        value = h1_ref[:, cols] + mm(h2_ref[...], wb_ref[:, cols])
        y_ref[:, cols] = (value * valid).astype(BF16)
        gn_ref[:, cols] = mm_cols(gg_ref[...], w_ref[cols, gate_at : gate_at + hidden]) + mm_cols(
            gu_ref[...], w_ref[cols, gate_at + hidden :]
        )
        return carry

    lax.fori_loop(0, D // QUAD, outward, 0)

    def weights(tile, carry):
        at = pl.multiple_of(tile * FF_TILE, FF_TILE)
        cols = pl.ds(at, FF_TILE)
        dg_ref[:, cols] = mm(ntt_ref[...], gg_ref[:, cols]).astype(BF16)
        du_ref[:, cols] = mm(ntt_ref[...], gu_ref[:, cols]).astype(BF16)
        db_ref[cols, :] = mm_rows(h2_ref[:, cols], gres_ref[...]).astype(BF16)
        return carry

    lax.fori_loop(0, hidden // FF_TILE, weights, 0)

    gain_grad = jnp.zeros((1, D), F32)
    for tile in range(TILES):
        rows = pl.ds(tile * QT, QT)
        value, grad = h1_ref[rows, :], gn_ref[rows, :]
        root = lax.rsqrt(mean_square(value) + EPSILON)
        unit = value * root
        gain_grad = gain_grad + jnp.sum(grad * unit, axis=0, keepdims=True)
        grad = grad * gain
        grad = gres_ref[rows, :].astype(F32) + root * (
            grad - unit * jnp.mean(grad * unit, axis=-1, keepdims=True)
        )
        gh_ref[rows, :] = grad
        low = grad.astype(BF16)
        nt_ref[rows, :] = low
        ga_ref[rows, :] = mm_cols(low, w_ref[:, out_at:gate_at]).astype(BF16)

    def out_weight(tile, carry):
        cols = pl.ds(pl.multiple_of(tile * QUAD, QUAD), QUAD)
        do_ref[cols, :] = mm_rows(att_ref[:, cols], nt_ref[...]).astype(BF16)
        return carry

    lax.fori_loop(0, D // QUAD, out_weight, 0)
    return gain_grad


def backward_attention_start(dk_ref, dv_ref):
    dk_ref[...] = jnp.zeros_like(dk_ref)
    dv_ref[...] = jnp.zeros_like(dv_ref)


def backward_attention_quad(tab_ref, rank, qkv_ref, att_ref, ga_ref, lse_ref, dqkv_ref, dk_ref, dv_ref, quad):
    heads = QUAD // DH
    marks = jnp.where(iota((16, QUAD), 1) // DH == iota((16, QUAD), 0), 1.0, 0.0).astype(BF16)
    low = quad * QUAD
    cols = slice(low, low + QUAD)

    def step(tile, carry):
        first = window_start(tile)
        bias, side_bias = tile_bias(tab_ref, rank, tile, first, 0)
        bias = jnp.concatenate([bias, side_bias], axis=0)
        rows = pl.ds(pl.multiple_of(tile * QT, QT), QT)
        window = pl.ds(first, WIN)
        lse = lse_ref[tile]
        product = ga_ref[rows, cols].astype(F32) * att_ref[rows, cols].astype(F32)
        high = product.astype(BF16)
        rest = (product - high.astype(F32)).astype(BF16)
        centre = mm_cols(marks, high) + mm_cols(marks, rest)
        query = head_stack(qkv_ref[rows, cols])
        grad = head_stack(ga_ref[rows, cols])
        keys = jnp.concatenate(
            [qkv_ref[window, D + low : D + low + QUAD], qkv_ref[ROWS:, D + low : D + low + QUAD]], axis=0
        )
        values = jnp.concatenate(
            [qkv_ref[window, 2 * D + low : 2 * D + low + QUAD],
             qkv_ref[ROWS:, 2 * D + low : 2 * D + low + QUAD]], axis=0
        )
        scores = mm_cols(keys, query)
        slopes = mm_cols(values, grad)
        probs, grads = [], []
        for head in range(heads):
            part = slice(head * QT, (head + 1) * QT)
            number = quad * heads + head
            prob = jnp.exp(scores[:, part] + bias - lse[number : number + 1])
            probs.append(prob.astype(BF16))
            grads.append((prob * (slopes[:, part] - centre[head : head + 1])).astype(BF16))
        probs = jnp.concatenate(probs, axis=1)
        grads = jnp.concatenate(grads, axis=1)
        dkey = mm(grads, query)
        dvalue = mm(probs, grad)
        dk_ref[window, cols] = dk_ref[window, cols] + dkey[:WIN]
        dk_ref[ROWS:, cols] = dk_ref[ROWS:, cols] + dkey[WIN:]
        dv_ref[window, cols] = dv_ref[window, cols] + dvalue[:WIN]
        dv_ref[ROWS:, cols] = dv_ref[ROWS:, cols] + dvalue[WIN:]
        dqkv_ref[rows, cols] = head_merge(mm_rows(grads, keys)).astype(BF16)
        return carry

    lax.fori_loop(0, TILES, step, 0)
    dqkv_ref[ROWS:, cols] = jnp.zeros((SIDE_ROWS, QUAD), BF16)
    dqkv_ref[:, D + low : D + low + QUAD] = dk_ref[:, cols].astype(BF16)
    dqkv_ref[:, 2 * D + low : 2 * D + low + QUAD] = dv_ref[:, cols].astype(BF16)


def weight_grads(n_ref, dqkv_ref, refs):
    for number, ref in enumerate(refs):
        def weights(tile, carry):
            at = pl.multiple_of(tile * QUAD, QUAD)
            value = mm_rows(n_ref[...], dqkv_ref[:, pl.ds(number * D + at, QUAD)]).astype(BF16)
            if len(ref.shape) == 4:
                ref[:, :, :, pl.ds(at, QUAD)] = value.reshape(ref.shape[:3] + (QUAD,))
            else:
                ref[:, pl.ds(at, QUAD)] = value
            return carry

        lax.fori_loop(0, D // QUAD, weights, 0)


def backward_project(tab_ref, rank, x_ref, gh_ref, gains, n_ref, dqkv_ref, w_ref, gn_ref, g_ref):
    def step(tile, carry):
        cols = pl.ds(pl.multiple_of(tile * QUAD, QUAD), QUAD)
        gn_ref[:, cols] = mm_cols(dqkv_ref[...], w_ref[cols, : 3 * D])
        return carry

    lax.fori_loop(0, D // QUAD, step, 0)
    pool = pooling(tab_ref, rank)
    side = mm(pool, n_ref[:ROWS, :])
    root = lax.rsqrt(mean_square(side) + EPSILON)
    unit = side * root
    grad = gn_ref[ROWS:, :]
    side_gain = jnp.sum(grad * unit, axis=0, keepdims=True)
    grad = grad * gains[1:2]
    grad = root * (grad - unit * jnp.mean(grad * unit, axis=-1, keepdims=True))
    parts = three_way(grad)
    gain_grad = jnp.zeros((1, D), F32)
    for tile in range(TILES):
        rows = pl.ds(tile * QT, QT)
        spread = pool[:, tile * QT : (tile + 1) * QT]
        total = gn_ref[rows, :] + mm_rows(spread, parts[0]) + mm_rows(spread, parts[1])
        value = x_ref[rows, :].astype(F32)
        root = lax.rsqrt(mean_square(value) + EPSILON)
        unit = value * root
        gain_grad = gain_grad + jnp.sum(total * unit, axis=0, keepdims=True)
        total = total * gains[0:1]
        value = (
            gh_ref[rows, :] + root * (total - unit * jnp.mean(total * unit, axis=-1, keepdims=True))
        ).astype(BF16)
        if len(g_ref.shape) == 3:
            g_ref[pl.ds(tile * (QT // BLK), QT // BLK)] = value.reshape(QT // BLK, BLK, D)
        else:
            g_ref[rows, :] = value
    return gain_grad, side_gain


def first_kernel(tab_ref, x_ref, gc_ref, w_ref, n_ref, qkv_ref, att_ref, lse_ref):
    rank = lax.axis_index("rep")
    gains = gains_of(gc_ref)
    forward_norm(tab_ref, rank, x_ref, gains, n_ref)
    forward_project(n_ref, w_ref, qkv_ref)
    forward_attention(tab_ref, rank, qkv_ref, att_ref, lse_ref, 0, TILES)


def second_kernel(tab_ref, x_ref, cot_ref, att_ref, gc_ref, w_ref, wb_ref,
                  y_ref, gh_ref, ga_ref, dg_ref, du_ref, db_ref, do_ref, gain_ref, *scratch):
    rank = lax.axis_index("rep")
    gain_ref[...] = feed_forward(tab_ref, rank, x_ref, cot_ref, att_ref, gains_of(gc_ref), w_ref, wb_ref,
                                 y_ref, gh_ref, ga_ref, dg_ref, du_ref, db_ref, do_ref, *scratch)


def third_kernel(tab_ref, x_ref, gh_ref, ga_ref, att_ref, lse_ref, n_ref, qkv_ref, gain_ref, gc_ref, w_ref,
                 g_ref, dw_ref, dc_ref, dqkv_ref, dk_ref, dv_ref, gn_ref):
    rank = lax.axis_index("rep")
    gains = gains_of(gc_ref)
    backward_attention_start(dk_ref, dv_ref)
    for quad in range(D // QUAD):
        backward_attention_quad(tab_ref, rank, qkv_ref, att_ref, ga_ref, lse_ref, dqkv_ref, dk_ref, dv_ref, quad)
    weight_grads(n_ref, dqkv_ref, [dw_ref.at[:, i * D : (i + 1) * D] for i in range(3)])
    one, side = backward_project(tab_ref, rank, x_ref, gh_ref, gains, n_ref, dqkv_ref, w_ref, gn_ref, g_ref)
    grads = jnp.concatenate([one, side, gain_ref[...], jnp.zeros((5, D), F32)], axis=0)
    spread_gain_grads(grads, dc_ref)


def attend(tab, x, gc, w):
    shape = jax.ShapeDtypeStruct
    return pl.pallas_call(
        first_kernel,
        out_shape=(shape((ALL_ROWS, D), BF16), shape((ALL_ROWS, 3 * D), BF16), shape((ROWS, D), BF16),
                   shape((TILES, 16, QT), F32)),
        in_specs=[SMEM, VMEM, VMEM, pl.BlockSpec((D, 3 * D), lambda step: (0, 0))],
        grid=(1,),
        out_specs=(VMEM,) * 4,
        compiler_params=pltpu.CompilerParams(vmem_limit_bytes=VMEM_LIMIT),
        name="attend",
    )(tab, x, gc, w)


def feed(tab, x, cot, att, gc, w, wb):
    hidden = wb.shape[0]
    shape = jax.ShapeDtypeStruct
    return pl.pallas_call(
        second_kernel,
        out_shape=(shape((ROWS, D), BF16), shape((ROWS, D), F32), shape((ROWS, D), BF16),
                   shape((D, hidden), BF16), shape((D, hidden), BF16), shape((hidden, D), BF16), shape((D, D), BF16),
                   shape((1, D), F32)),
        in_specs=[SMEM] + [VMEM] * 6,
        out_specs=(VMEM,) * 8,
        scratch_shapes=[pltpu.VMEM((ROWS, D), F32), pltpu.VMEM((ROWS, D), BF16), pltpu.VMEM((D, ROWS), BF16),
                        pltpu.VMEM((ROWS, D), BF16), pltpu.VMEM((ROWS, hidden), BF16),
                        pltpu.VMEM((ROWS, hidden), BF16), pltpu.VMEM((ROWS, hidden), BF16),
                        pltpu.VMEM((ROWS, D), F32)],
        compiler_params=pltpu.CompilerParams(vmem_limit_bytes=VMEM_LIMIT),
        name="feed_forward",
    )(tab, x, cot, att, gc, w, wb)


def backward_layer(tab, x, gh, ga, att, lse, n, qkv, gain, gc, w):
    shape = jax.ShapeDtypeStruct
    return pl.pallas_call(
        third_kernel,
        out_shape=(shape((ROWS, D), BF16), shape((D, 3 * D), BF16), shape((gc.shape[0], 8, 128), F32)),
        in_specs=[SMEM] + [VMEM] * 9 + [pl.BlockSpec((D, 3 * D), lambda step: (0, 0))],
        grid=(1,),
        out_specs=(VMEM,) * 3,
        scratch_shapes=[pltpu.VMEM((ALL_ROWS, 3 * D), BF16), pltpu.VMEM((ALL_ROWS, D), F32),
                        pltpu.VMEM((ALL_ROWS, D), F32), pltpu.VMEM((ALL_ROWS, D), F32)],
        compiler_params=pltpu.CompilerParams(vmem_limit_bytes=VMEM_LIMIT),
        name="attend_back",
    )(tab, x, gh, ga, att, lse, n, qkv, gain, gc, w)


class Links:
    def __init__(self, outer, inner):
        self.outer, self.inner = outer, inner
        self.rank, self.spot = lax.axis_index("rep"), lax.axis_index("fsdp")
        self.core = self.rank % 2
        self.row, self.col = self.spot // inner, self.spot % inner
        self.mate, self.across = core_of(self.rank), across_of(self.rank)
        self.late = []

    def greet(self, everyone=False, later=False):
        barrier = pltpu.get_barrier_semaphore()
        neighbours = (
            (self.row + 1 < self.outer, {"fsdp": self.spot + self.inner}),
            (self.row > 0, {"fsdp": self.spot - self.inner}),
            (self.col + 1 < self.inner, {"fsdp": self.spot + 1}),
            (self.col > 0, {"fsdp": self.spot - 1}),
        )
        group = (self.mate, self.across) + ((across_of(self.mate),) if everyone else ())
        amount = jnp.int32(len(group))
        for there, device in neighbours:
            amount = amount + there.astype(jnp.int32)

            @pl.when(there)
            def _():
                pl.semaphore_signal(barrier, inc=1, device_id=device, device_id_type=MESH)

        for device in group:
            pl.semaphore_signal(barrier, inc=1, device_id={"rep": device}, device_id_type=MESH)
        self.met = lambda: pl.semaphore_wait(barrier, amount)
        if not later:
            self.met()

    def send(self, there, src, dst, ssem, rsem, device):
        def describe():
            return pltpu.make_async_remote_copy(
                src_ref=src, dst_ref=dst, send_sem=ssem, recv_sem=rsem,
                device_id=device, device_id_type=MESH,
            )

        if there is None:
            describe().start()
        else:
            @pl.when(there)
            def _():
                describe().start()

        self.late.append((there, lambda: describe().wait_send()))

    def arrive(self, place, rsem, spare):
        pltpu.make_async_remote_copy(
            src_ref=place, dst_ref=place, send_sem=spare, recv_sem=rsem,
            device_id={"rep": self.mate}, device_id_type=MESH,
        ).wait_recv()

    def drain(self):
        for there, finish in self.late:
            if there is None:
                finish()
            else:
                pl.when(there)(finish)


def halves(ref, which):
    half = ref.shape[-1] // 2
    cols = pl.ds(pl.multiple_of(which * half, 128), half)
    return ref.at[:, :, :, cols] if len(ref.shape) == 4 else ref.at[:, cols]


class Reduction:
    def __init__(self, links, source, total, mine, crecv, yrecv, zrecv, xrecv, stage, sems, number):
        self.links, self.source, self.total, self.mine, self.stage = links, source, total, mine, stage
        self.crecv, self.yrecv, self.zrecv, self.xrecv = crecv, yrecv, zrecv, xrecv
        self.sems, self.number = sems, number
        self.whole = total.shape[-1] % 256 != 0
        self.load = None

    def sem(self, name, *index):
        return self.sems[name].at[index + (self.number,)]

    def begin(self):
        links = self.links
        other = self.source if self.whole else halves(self.source, 1 - links.core)
        links.send(None, other, self.crecv, self.sem("c_send"), self.sem("c_recv"), {"rep": links.mate})
        if self.mine is None:
            self.mine = self.source if self.whole else halves(self.source, links.core)
        else:
            own = self.source if self.whole else halves(self.source, links.core)
            self.load = pltpu.make_async_copy(own, self.mine, self.sem("m_sem"))
            self.load.start()

    def pair(self):
        links = self.links
        if self.load is not None:
            self.load.wait()
        links.arrive(self.crecv, self.sem("c_recv"), self.sems["spare"].at[0])
        inner = links.inner

        def add(index, carry):
            row, col = index // inner, index % inner
            self.mine[row, col] = self.mine[row, col] + self.crecv[row, col]
            return carry

        lax.fori_loop(0, links.outer * inner, add, 0)
        links.send(None, self.mine.at[:, 1 - links.col], self.yrecv, self.sem("y_send"), self.sem("y_recv"),
                   {"fsdp": links.spot + 1 - 2 * links.col})

    def slot(self, way, place, dest):
        return dest - place if way == 0 else self.links.outer - place + dest

    def pass_on(self, way, dest, there, first):
        links = self.links
        step = 1 if way == 0 else -1
        mine = self.mine.at[dest, links.col]
        put = self.slot(way, links.row + step, dest)
        if not first:
            got = self.slot(way, links.row, dest)

            @pl.when(there)
            def _():
                links.arrive(self.zrecv.at[got], self.sem("z_recv", got), self.sems["spare"].at[0])
                mine[...] = mine[...] + self.zrecv[got]

        links.send(there, mine, self.zrecv.at[put], self.sem("z_send", way, dest), self.sem("z_recv", put),
                   {"fsdp": links.spot + step * links.inner})

    def column(self):
        links = self.links
        size = links.outer
        links.arrive(self.yrecv, self.sem("y_recv"), self.sems["spare"].at[0])

        def add(index, carry):
            self.mine[index, links.col] = self.mine[index, links.col] + self.yrecv[index]
            return carry

        lax.fori_loop(0, size, add, 0)
        for far in range(size - 1, 0, -1):
            self.pass_on(0, far, links.row == 0, True)
            self.pass_on(1, size - 1 - far, links.row == size - 1, True)

    def hop(self, turn):
        links = self.links
        size = links.outer
        for way in range(2):
            place = turn if way == 0 else size - 1 - turn
            here = links.row == place
            rest = range(size - 1, place, -1) if way == 0 else range(0, place)
            for dest in rest:
                self.pass_on(way, dest, here, False)
            mine = self.mine.at[place, links.col]
            got = self.slot(way, place, place)

            @pl.when(here)
            def _():
                links.arrive(self.zrecv.at[got], self.sem("z_recv", got), self.sems["spare"].at[0])
                mine[...] = mine[...] + self.zrecv[got]

    def cross(self):
        links = self.links
        mine = self.mine.at[links.row, links.col]
        links.send(None, mine, self.xrecv, self.sem("x_send"), self.sem("x_recv"), {"rep": links.across})

    def finish(self):
        links = self.links
        links.arrive(self.xrecv, self.sem("x_recv"), self.sems["spare"].at[0])
        self.stage[...] = self.mine[links.row, links.col].astype(F32) + self.xrecv[...].astype(F32)
        place = self.total if self.whole else halves(self.total, links.core)
        self.keep = pltpu.make_async_copy(self.stage, place, self.sem("m_sem"))
        self.keep.start()
        if not self.whole:
            links.send(None, self.stage, place, self.sem("f_send"), self.sem("f_recv"), {"rep": links.mate})

    def settle(self):
        self.keep.wait()
        if not self.whole:
            self.links.arrive(
                halves(self.total, 1 - self.links.core), self.sem("f_recv"), self.sems["spare"].at[0]
            )


class AcrossFirst(Reduction):
    def pair(self):
        links = self.links
        if self.load is not None:
            self.load.wait()
        links.arrive(self.crecv, self.sem("c_recv"), self.sems["spare"].at[0])
        inner = links.inner

        def add(index, carry):
            row, col = index // inner, index % inner
            self.mine[row, col] = self.mine[row, col] + self.crecv[row, col]
            return carry

        lax.fori_loop(0, links.outer * inner, add, 0)
        self.side = links.rank // 2
        links.send(None, self.rows_of(self.mine, 1 - self.side), self.xrecv, self.sem("x_send"), self.sem("x_recv"),
                   {"rep": links.across})

    def rows_of(self, ref, which):
        half = ref.shape[-2] // 2
        rows = pl.ds(pl.multiple_of(which * half, 16), half)
        return ref.at[:, :, rows, :] if len(ref.shape) == 4 else ref.at[rows, :]

    def meet(self):
        links = self.links
        links.arrive(self.xrecv, self.sem("x_recv"), self.sems["spare"].at[0])
        self.mine = self.rows_of(self.mine, self.side)
        inner = links.inner

        def add(index, carry):
            row, col = index // inner, index % inner
            self.mine[row, col] = self.mine[row, col] + self.xrecv[row, col]
            return carry

        lax.fori_loop(0, links.outer * inner, add, 0)
        links.send(None, self.mine.at[:, 1 - links.col], self.yrecv, self.sem("y_send"), self.sem("y_recv"),
                   {"fsdp": links.spot + 1 - 2 * links.col})

    def quarter(self, side, core):
        return halves(self.rows_of(self.total, side), core)

    def spread(self, stage, place, keep, ssem, rsem):
        links = self.links
        self.keeps.append(pltpu.make_async_copy(stage, place, keep))
        self.keeps[-1].start()
        links.send(None, stage, place, ssem, rsem, {"rep": links.mate})

    def cross(self):
        links = self.links
        mine = self.mine.at[links.row, links.col]
        links.send(None, mine, self.third, self.sem("h_send"), self.sem("h_recv"), {"rep": links.across})
        self.stage[...] = mine[...].astype(F32)
        self.keeps = []
        self.spread(self.stage, self.quarter(self.side, links.core), self.sem("m_sem"),
                    self.sem("f_send"), self.sem("f_recv"))

    def finish(self):
        links = self.links
        links.arrive(self.third, self.sem("h_recv"), self.sems["spare"].at[0])
        self.stage_two[...] = self.third[...].astype(F32)
        self.spread(self.stage_two, self.quarter(1 - self.side, links.core), self.sem("k_keep"),
                    self.sem("k_send"), self.sem("k_recv"))

    def settle(self):
        links = self.links
        for keep in self.keeps:
            keep.wait()
        for side, name in ((self.side, "f_recv"), (1 - self.side, "k_recv")):
            links.arrive(self.quarter(side, 1 - links.core), self.sem(name), self.sems["spare"].at[0])


SEM_NAMES = ("c_send", "c_recv", "m_sem", "y_send", "y_recv", "z_send", "z_recv", "x_send", "x_recv",
             "f_send", "f_recv", "h_send", "h_recv", "k_send", "k_recv", "k_keep", "r_send", "r_recv", "own", "spare")


class Return:
    def __init__(self, links, source, home, sems, kind):
        self.links, self.source, self.home, self.sems, self.kind = links, source, home, sems, kind

    def begin(self):
        links = self.links
        dst = self.home.at[links.rank]
        for way, device in enumerate((links.across, links.mate)):
            links.send(None, self.source, dst, self.sems["r_send"].at[self.kind, way],
                       self.sems["r_recv"].at[self.kind, way], {"rep": device})
        self.copy = pltpu.make_async_copy(self.source, dst, self.sems["own"].at[self.kind])
        self.copy.start()

    def relay(self):
        links = self.links
        place = self.home.at[links.across]
        links.arrive(place, self.sems["r_recv"].at[self.kind, 0], self.sems["spare"].at[0])
        links.send(None, place, place, self.sems["r_send"].at[self.kind, 2],
                   self.sems["r_recv"].at[self.kind, 2], {"rep": links.mate})

    def settle(self):
        links, sem = self.links, self.sems["r_recv"]
        links.arrive(self.home.at[links.mate], sem.at[self.kind, 1], self.sems["spare"].at[0])
        links.arrive(self.home.at[across_of(links.mate)], sem.at[self.kind, 2], self.sems["spare"].at[0])
        self.copy.wait()


TABLE_ROWS = 56


def packed_table(lens, tabv_ref):
    lane = iota((8, 128), 1)
    blocks = lax.div(lens + (BLK - 1), BLK)
    key = jnp.where(blocks > 0, blocks * 128 + (127 - lane), 0)
    wide = jnp.broadcast_to(key[:1], (128, 128))
    other = jnp.sum(jnp.where(iota((128, 128), 0) == iota((128, 128), 1), wide, 0), axis=1, keepdims=True)
    order = jnp.sum(jnp.where(other > wide, 1, 0), axis=0, keepdims=True)
    order = jnp.broadcast_to(order, (8, 128))
    edges, below = [], jnp.zeros((8, 1), jnp.int32)
    for size in range(MAX_SEQ_BLOCKS, 0, -1):
        below = below + jnp.sum(jnp.where(blocks == size, 1, 0), axis=1, keepdims=True)
        edges.append(jnp.broadcast_to(below, (8, 128)))

    def assign(number, carry):
        loads, slot, first = carry[:4], carry[4], carry[5]
        size = jnp.zeros((8, 128), jnp.int32)
        for step, edge in enumerate(edges):
            size = size + jnp.where(number < edge, 1, 0)
        low = jnp.minimum(jnp.minimum(loads[0], loads[1]), jnp.minimum(loads[2], loads[3]))
        best = jnp.full((8, 128), 3, jnp.int32)
        for dev in (2, 1, 0):
            best = jnp.where(loads[dev] == low, dev, best)
        mine = order == number
        slot = jnp.where(mine, best * SLOTS + low, slot)
        first = jnp.where(mine, low, first)
        loads = tuple(loads[dev] + jnp.where(best == dev, size, 0) for dev in range(4))
        return loads + (slot, first)

    zero = jnp.zeros((8, 128), jnp.int32)
    carry = lax.fori_loop(0, 32, assign, (zero,) * 6)
    slot, first = carry[4], carry[5]
    where, tokens, segment = zero - 1, zero, zero
    for step in range(MAX_SEQ_BLOCKS):
        def shifted(value):
            return value if step == 0 else pltpu.roll(value, step, 1)

        covers = shifted(blocks) > step
        where = jnp.where(covers, shifted(slot) + step, where)
        tokens = jnp.where(covers, jnp.minimum(shifted(lens) - BLK * step, BLK), tokens)
        segment = jnp.where(covers, shifted(first) + 1, segment)
    packed = jnp.where(where >= 0, (lane + 1) + 128 * tokens + 16384 * segment, 0)
    spots = jnp.broadcast_to(where[:1], (48, 128))
    values = jnp.broadcast_to(packed[:1], (48, 128))
    column = jnp.sum(jnp.where(spots == iota((48, 128), 0), values, 0), axis=1, keepdims=True)
    tabv_ref[:48] = jnp.broadcast_to(column, (48, 128))
    tabv_ref[48:] = where


ROW_FIRST = (3,)
FRONT_ORDER = (
    ("own", 1), ("own", 3), ("do", "table"), ("hop", 1, 0), ("own", 0), ("pack", 0, 1), ("own", 5), ("hop", 1, 1),
    ("pack", 0, 0), ("cross", 0), ("hop", 5, 0), ("yz", 3), ("hop", 0, 0), ("hop", 5, 1), ("hop", 1, 2), ("own", 4),
    ("hop", 0, 1), ("pack", 1, 0), ("own", 2), ("hop", 5, 2), ("hop", 0, 2), ("fr", 1), ("hop", 2, 0),
    ("pack", 1, 1), ("hop", 4, 0), ("rfin", 0), ("hop", 2, 1), ("cross", 1), ("fr", 0), ("fr", 5), ("do", "norm"),
    ("hop", 4, 1), ("hop", 3, 0), ("got", 0), ("do", "proj"), ("hop", 2, 2), ("do", "a0"), ("xin", 1), ("hop", 4, 2),
    ("do", "a1"), ("hop", 3, 1), ("fr", 2), ("do", "a2"), ("hop", 3, 2), ("fr", 4), ("rfin", 1),
)


def front_kernel(outer, inner, *refs):
    (raw_ref, rows_any, cots_any, *weights), refs = refs[:9], refs[9:]
    (wd_any, *gain_refs), refs = refs[:4], refs[4:]
    (tab_ref, gains_ref), outs_any, (ga_ref, gb_ref), refs = refs[:2], refs[2:9], refs[9:11], refs[11:]
    (stage, lens_all, tabs, psend, precv, xsend, xrecv, rows_ref, cots_ref), refs = refs[:9], refs[9:]
    (lens_ref, wd_ref, wc_ref), refs = refs[:3], refs[3:]
    held, refs = refs[:8], refs[8:]
    x_ref, cot_ref, n_ref, qkv_ref, att_ref, lse_ref, wqkv_ref, gc_ref = held
    (l_send, l_recv, t_sem, w_sem, z_send, z_recv, y_send, y_recv, c_send, c_recv, d_send, d_recv, own_sem,
     p_send, p_recv, x_send, x_recv, spare, out_sem) = refs
    links = Links(outer, inner)
    rank, spot, core, mate, across = links.rank, links.spot, links.core, links.mate, links.across
    row, col = links.row, links.col
    side = rank // 2
    count = outer * inner
    part = stage.shape[0]
    per_rank = rows_ref.shape[0]
    width = 3 * D
    tall = wd_ref.shape[0]
    hidden = weights[-1].shape[1]
    rest = stage.shape[1] - width
    cuts = [0, 7 * rest // 19, 11 * rest // 19, rest]
    spans = [(cuts[i], (cuts[i + 1] - cuts[i]) // 2) for i in range(3)]

    at = 0
    loads = []
    loads.append(pltpu.make_async_copy(wd_any, wd_ref, w_sem.at[8]))
    loads[0].start()
    row_loads = [pltpu.make_async_copy(rows_any, rows_ref, w_sem.at[6]), pltpu.make_async_copy(cots_any, cots_ref, w_sem.at[7])]
    for number, ref in enumerate(weights):
        cols = slice(at, at + ref.shape[1])
        loads.append(pltpu.make_async_copy(ref, stage.at[:, cols], w_sem.at[number]))
        loads[-1].start()
        at += ref.shape[1]
    for load in row_loads:
        load.start()

    wc_ref[...] = jnp.zeros(wc_ref.shape, wc_ref.dtype)
    for number, ref in enumerate(gain_refs):
        wc_ref[number : number + 1, :part] = ref[...].reshape(1, part)
    micro, spots = raw_ref.shape
    lens_ref[...] = jnp.zeros(lens_ref.shape, lens_ref.dtype)
    lens_ref[:micro, :spots] = raw_ref[...]
    raw = lens_ref[...]
    spread = jnp.zeros((1, 128), jnp.int32)
    for device in range(4):
        line = jnp.zeros((1, 128), jnp.int32)
        for number in range(micro):
            shift = device * micro * spots + number * spots
            moved = raw if shift == 0 else pltpu.roll(raw, shift, 1)
            line = line + moved[number : number + 1]
        spread = jnp.where(rank == device, line, spread)
    lens_ref[...] = jnp.broadcast_to(spread, (8, 128))
    links.greet(True)
    lens_all[rank] = lens_ref[...]
    for step in range(1, 4):
        links.send(None, lens_ref, lens_all.at[rank], l_send.at[step - 1], l_recv.at[step - 1],
                   {"rep": (rank + step) % 4})

    def cols_of(start, half, which):
        return pl.ds(pl.multiple_of(start + which * half, 128), half)

    down_half = D // 2

    def tall_rows(which):
        return pl.ds(pl.multiple_of(which * (tall // 2), 16), tall // 2)

    def source(number):
        if number == 0:
            return stage.at[:, cols_of(0, width // 2, core)]
        if number == 1:
            return wd_ref.at[tall_rows(side), cols_of(0, down_half, core)]
        if number == 5:
            return wc_ref
        start, half = spans[number - 2]
        return stage.at[:, cols_of(width + start, half, core)]

    def place(number, shard, which=None):
        which = core if which is None else which
        if number == 0:
            return wqkv_ref.at[pl.ds(pl.multiple_of(shard * part, 16), part), cols_of(0, width // 2, which)]
        if number in (1, 6):
            return gb_ref.at[shard, tall_rows(side if number == 1 else 1 - side), cols_of(0, down_half, which)]
        if number == 5:
            return gc_ref.at[shard]
        start, half = spans[number - 2]
        return ga_ref.at[shard, :, cols_of(start, half, which)]

    nobody = spare.at[0]

    def both(first, second):
        return second if first is None else jnp.logical_and(first, second)

    def guarded(there, action):
        if there is None:
            action()
        else:
            pl.when(there)(action)

    def share(there, number, shard):
        if number == 5:
            return
        here = place(number, shard)
        links.send(there, here, here, c_send.at[number, shard], c_recv.at[number, shard], {"rep": mate})
        if number == 1:
            links.send(there, here, here, d_send.at[shard], d_recv.at[shard], {"rep": across})

    other_column = {"fsdp": spot + 1 - 2 * col}

    def along_row(there, number, line, src):
        here = place(number, line * inner + col)
        links.send(there, here if src is None else src, here, y_send.at[line, number], y_recv.at[line, number],
                   other_column)

    def lines(step):
        return ((row - 1 - step >= 0, row - 1 - step, 0, row + 1 < outer, spot + inner),
                (row + 1 + step < outer, row + 1 + step, 1, row > 0, spot - inner))

    def along_line(number, column, src):
        here = place(number, row * inner + (col if column == 0 else 1 - col))
        src = here if src is None else src
        links.send(row + 1 < outer, src, here, z_send.at[0, 0, number, column], z_recv.at[0, 0, number, column],
                   {"fsdp": spot + inner})
        links.send(row > 0, src, here, z_send.at[1, 0, number, column], z_recv.at[1, 0, number, column],
                   {"fsdp": spot - inner})

    def own(number):
        src = source(number)
        along_line(number, 0, src)
        along_row(None, number, row, src)

    def second_column(number):
        shard = row * inner + 1 - col
        links.arrive(place(number, shard), y_recv.at[row, number], nobody)
        share(None, number, shard)
        along_line(number, 1, None)

    def hop(number, step):
        for here, line, way, onward, target in lines(step):
            for column in range(2 if number in ROW_FIRST else 1):
                shard = line * inner + (col if column == 0 else 1 - col)
                guarded(here, lambda: links.arrive(place(number, shard), z_recv.at[way, step, number, column], nobody))
                if step + 1 < outer - 1:
                    view = place(number, shard)
                    links.send(both(here, onward), view, view, z_send.at[way, step + 1, number, column],
                               z_recv.at[way, step + 1, number, column], {"fsdp": target})
                if number not in ROW_FIRST:
                    along_row(here, number, line, None)
                share(here, number, shard)

    def from_row(number):
        def one(there, line):
            shard = line * inner + 1 - col
            guarded(there, lambda: links.arrive(place(number, shard), y_recv.at[line, number], nobody))
            share(there, number, shard)

        one(None, row)
        for step in range(outer - 1):
            for here, line, *_ in lines(step):
                one(here, line)

    def gathered(*numbers):
        def wait(shard, carry):
            @pl.when(shard != spot)
            def _():
                for number in numbers:
                    links.arrive(place(number, shard, 1 - core), c_recv.at[number, shard], nobody)

            return carry

        lax.fori_loop(0, count, wait, 0)

    def from_across():
        def relay(shard, carry):
            here = place(6, shard)

            @pl.when(shard != spot)
            def _():
                links.arrive(here, d_recv.at[shard], nobody)
                pltpu.make_async_remote_copy(
                    src_ref=here, dst_ref=here, send_sem=c_send.at[6, shard], recv_sem=c_recv.at[6, shard],
                    device_id={"rep": mate}, device_id_type=MESH,
                ).start()

            return carry

        lax.fori_loop(0, count, relay, 0)

    for load in loads:
        load.wait()
    keep = [
        pltpu.make_async_copy(stage.at[:, :width], wqkv_ref.at[pl.ds(pl.multiple_of(spot * part, 16), part)], own_sem.at[0]),
        pltpu.make_async_copy(stage.at[:, width:], ga_ref.at[spot], own_sem.at[1]),
        pltpu.make_async_copy(wd_ref, gb_ref.at[spot], own_sem.at[2]),
        pltpu.make_async_copy(wc_ref, gc_ref.at[spot], own_sem.at[3]),
    ]
    for copy in keep:
        copy.start()
    leaving = []

    def leave(*numbers):
        for number in numbers:
            leaving.append(pltpu.make_async_copy(held[number], outs_any[number], out_sem.at[number]))
            leaving[-1].start()

    def make_table():
        for step in range(1, 4):
            links.arrive(lens_all.at[(rank + 4 - step) % 4], l_recv.at[step - 1], nobody)
        lens = lens_all[0] + lens_all[1] + lens_all[2] + lens_all[3]
        packed_table(jnp.broadcast_to(lens[:1], (8, 128)), tab_ref)
        to_scalar = pltpu.make_async_copy(tab_ref, tabs, t_sem.at[0])
        to_scalar.start()
        to_scalar.wait()
        for load in row_loads:
            load.wait()

    sources = (rows_ref, cots_ref)
    outs = (x_ref, cot_ref)

    def picked(kind, target, slot):
        index = block_at(tabs, target * SLOTS + slot) - rank * per_rank
        mine = jnp.logical_and(index >= 0, index < per_rank)
        return mine, sources[kind][jnp.clip(index, 0, per_rank - 1)]

    def mate_copy(kind, piece):
        return pltpu.make_async_remote_copy(
            src_ref=psend.at[kind, piece], dst_ref=precv.at[kind, piece],
            send_sem=p_send.at[kind, piece], recv_sem=p_recv.at[kind, piece],
            device_id={"rep": mate}, device_id_type=MESH,
        )

    def across_copy(kind):
        return pltpu.make_async_remote_copy(
            src_ref=xsend.at[kind], dst_ref=xrecv.at[kind],
            send_sem=x_send.at[kind], recv_sem=x_recv.at[kind],
            device_id={"rep": across}, device_id_type=MESH,
        )

    def pack_rows(kind, piece):
        target = mate if piece == 0 else across_of(mate)

        def pack(slot, carry):
            mine, value = picked(kind, target, slot)
            psend[kind, piece, slot] = jnp.where(mine, value, jnp.zeros_like(value))
            return carry

        lax.fori_loop(0, SLOTS, pack, 0)
        mate_copy(kind, piece).start()

    def cross_rows(kind):
        mate_copy(kind, 1).wait_recv()

        def merge(slot, carry):
            mine, value = picked(kind, across, slot)
            xsend[kind, slot] = jnp.where(mine, value, precv[kind, 1, slot])
            return carry

        lax.fori_loop(0, SLOTS, merge, 0)
        across_copy(kind).start()

    def finish_rows(kind):
        mate_copy(kind, 0).wait_recv()
        across_copy(kind).wait_recv()

        def finish(slot, carry):
            mine, value = picked(kind, rank, slot)
            rows = pl.ds(pl.multiple_of(slot * BLK, BLK), BLK)
            outs[kind][rows, :] = jnp.where(mine, value, precv[kind, 0, slot] + xrecv[kind, slot])
            return carry

        lax.fori_loop(0, SLOTS, finish, 0)

    def norm():
        keep[3].wait()
        gains = gains_of(gc_ref)
        gains_ref[...] = gains
        forward_norm(tabs, rank, x_ref, gains, n_ref)
        leave(2)

    def project():
        keep[0].wait()
        forward_project(n_ref, wqkv_ref, qkv_ref)
        leave(3, 6)

    def attend_tiles(begin, end):
        forward_attention(tabs, rank, qkv_ref, att_ref, lse_ref, begin, end)
        if end == TILES:
            leave(4, 5)

    work = {"table": make_table, "norm": norm, "proj": project, "a0": lambda: attend_tiles(0, 2),
            "a1": lambda: attend_tiles(2, 4), "a2": lambda: attend_tiles(4, TILES)}
    for action, which, *more in FRONT_ORDER:
        if action == "do":
            work[which]()
        elif action == "own":
            own(which)
        elif action == "hop":
            hop(which, more[0])
        elif action == "fr":
            from_row(which)
        elif action == "yz":
            second_column(which)
        elif action == "xin":
            from_across()
        elif action == "got":
            gathered(which)
        elif action == "pack":
            pack_rows(which, more[0])
        elif action == "cross":
            cross_rows(which)
        else:
            finish_rows(which)
            leave(which)
    gathered(1, 2, 3, 4, 6)

    def sent(shard, carry):
        @pl.when(shard != spot)
        def _():
            pltpu.make_async_remote_copy(
                src_ref=place(6, shard), dst_ref=place(6, shard), send_sem=c_send.at[6, shard], recv_sem=c_recv.at[6, shard],
                device_id={"rep": mate}, device_id_type=MESH,
            ).wait_send()

        return carry

    lax.fori_loop(0, count, sent, 0)
    links.drain()
    for kind in range(2):
        for piece in range(2):
            mate_copy(kind, piece).wait_send()
        across_copy(kind).wait_send()
    for copy in keep[1:3] + leaving:
        copy.wait()


def gather_and_attend(count, lens, rows, cots, weights, wd, gains):
    outer, inner = grid_of(count)
    block = rows.shape[1:]
    part = weights[0].shape[0]
    dma, shape = pltpu.SemaphoreType.DMA, jax.ShapeDtypeStruct
    total = sum(weight.shape[1] for weight in weights)
    kinds = 6
    held = (shape((ROWS, D), BF16), shape((ROWS, D), BF16), shape((ALL_ROWS, D), BF16), shape((ALL_ROWS, 3 * D), BF16),
            shape((ROWS, D), BF16), shape((TILES, 16, QT), F32), shape((D, 3 * D), BF16))
    return pl.pallas_call(
        partial(front_kernel, outer, inner),
        out_shape=(shape((TABLE_ROWS, 128), jnp.int32), shape((16, D), F32)) + held + (
            shape((count, part, total - 3 * D), BF16), shape((count,) + wd.shape, BF16),
        ),
        in_specs=[VMEM] + [ANY] * 9 + [VMEM] * 3,
        out_specs=(VMEM,) * 2 + (ANY,) * 9,
        scratch_shapes=[
            pltpu.VMEM((part, total), BF16), pltpu.VMEM((4, 8, 128), jnp.int32), pltpu.SMEM((TABLE_ROWS, 128), jnp.int32),
            pltpu.VMEM((2, 2, SLOTS) + block, BF16), pltpu.VMEM((2, 2, SLOTS) + block, BF16),
            pltpu.VMEM((2, SLOTS) + block, BF16), pltpu.VMEM((2, SLOTS) + block, BF16),
            pltpu.VMEM(rows.shape, BF16), pltpu.VMEM(cots.shape, BF16),
            pltpu.VMEM((8, 128), jnp.int32), pltpu.VMEM(wd.shape, BF16), pltpu.VMEM((16, 128), BF16),
            *(pltpu.VMEM(one.shape, one.dtype) for one in held), pltpu.VMEM((count, 16, 128), BF16),
            dma((3,)), dma((3,)), dma((1,)), dma((9,)),
            dma((2, outer - 1, kinds, 2)), dma((2, outer - 1, kinds, 2)), dma((outer, kinds)), dma((outer, kinds)),
            dma((kinds + 1, count)), dma((kinds + 1, count)), dma((count,)), dma((count,)), dma((4,)),
            dma((2, 2)), dma((2, 2)), dma((2,)), dma((2,)), dma((1,)), dma((8,)),
        ],
        compiler_params=pltpu.CompilerParams(
            collective_id=1, has_side_effects=True, vmem_limit_bytes=VMEM_LIMIT
        ),
        name="gather_and_attend",
    )(lens, rows, cots, *weights, wd, *gains)


ACROSS_FIRST = (2, 3)
REAR_ORDER = (
    ("do", "start"), ("do", "P0"), ("do", "P1a"), ("do", "gA"), ("begin", 0), ("do", "uA"), ("begin", 1),
    ("do", "P1b"), ("pair", 0), ("pair", 1), ("do", "gB"), ("begin", 2), ("do", "uB"), ("begin", 3), ("do", "d"),
    ("begin", 4), ("pair", 2), ("pair", 3), ("do", "out"), ("do", "load"), ("rows", 0), ("pair", 4), ("col", 0), ("meet", 2),
    ("do", "P4"), ("col", 1), ("do", "P5"), ("begin", 5), ("do", "q0"), ("meet", 3), ("pair", 5), ("hop", 0, 1),
    ("hop", 1, 1), ("do", "p0"), ("begin", 6), ("do", "q1"), ("pair", 6), ("col", 4), ("hop", 0, 2), ("hop", 1, 2),
    ("do", "p1"), ("begin", 7), ("do", "q2"), ("pair", 7), ("col", 2), ("col", 3), ("hop", 0, 3), ("cross", 0),
    ("hop", 1, 3), ("cross", 1), ("do", "bp"), ("rows", 1), ("relay", 0), ("col", 5), ("hop", 4, 1), ("fin", 0),
    ("fin", 1), ("do", "p2"), ("begin", 8), ("hop", 2, 1), ("do", "dc"), ("begin", 9), ("hop", 3, 1), ("pair", 8),
    ("pair", 9), ("col", 6), ("hop", 4, 2), ("hop", 5, 1), ("hop", 2, 2), ("hop", 3, 2), ("hop", 6, 1),
    ("hop", 5, 2), ("hop", 6, 2), ("hop", 4, 3), ("cross", 4), ("col", 7), ("hop", 7, 1), ("hop", 2, 3),
    ("cross", 2), ("hop", 3, 3), ("cross", 3), ("col", 8), ("col", 9), ("hop", 5, 3), ("cross", 5), ("hop", 6, 3),
    ("cross", 6), ("relay", 1), ("hop", 8, 1), ("hop", 9, 1), ("hop", 7, 2), ("hop", 8, 2), ("hop", 9, 2),
    ("fin", 4), ("fin", 2), ("fin", 3), ("hop", 7, 3), ("cross", 7), ("fin", 5), ("hop", 8, 3), ("cross", 8),
    ("hop", 9, 3), ("cross", 9), ("fin", 6), ("fin", 7), ("fin", 8), ("fin", 9),
)


def rear_kernel(outer, inner, *refs):
    (tab_ref, x_ref, att_ref, lse_ref, gc_ref), refs = refs[:5], refs[5:]
    (cot_any, n_any, qkv_any, wqkv_any, wf_any, wd_any), refs = refs[:6], refs[6:]
    kinds = 10
    (og_ref, ou_ref, od_ref, oo_ref, op_ref, oc_ref, ry_ref, rg_ref), refs = refs[:8], refs[8:]
    (y_ref, gh_ref, fa_ref, dk_ref, b0_ref, b1_ref, b2_ref, n_ref, ntt_ref, gres_ref, ga_ref), refs = refs[:11], refs[11:]
    (wf_ref, wd_ref, dg_ref, du_ref, db_ref, do_ref, dc_ref, mine_ref), refs = refs[:8], refs[8:]
    crecv, refs = list(refs[:7]), refs[7:]
    narrow = D // 2
    crecv = crecv[:6] + [crecv[i].at[:, :, :, :narrow] for i in range(3)] + crecv[6:]
    yrecv, zrecv, xrecv, stages = (refs[kinds * i : kinds * (i + 1)] for i in range(4))
    refs = refs[4 * kinds :]
    extra, refs = refs[: 2 * len(ACROSS_FIRST)], refs[2 * len(ACROSS_FIRST) :]
    sems = dict(zip(SEM_NAMES, refs))
    load_sem, free_sem = refs[len(SEM_NAMES) :]
    links = Links(outer, inner)
    rank = links.rank
    hidden = wd_ref.shape[0]
    part = wf_ref.shape[2]
    group = 4 * part

    def fetch(number, src, dst):
        copy = pltpu.make_async_copy(src, dst, load_sem.at[number])
        copy.start()
        return copy

    load_cot = fetch(0, cot_any, ga_ref)
    load_out = fetch(1, wf_any.at[:, :, :, :D], wf_ref.at[:, :, :, :D])
    load_in = fetch(2, wf_any.at[:, :, :, D:], wf_ref.at[:, :, :, D:])
    load_down = fetch(3, wd_any, wd_ref)
    links.greet(later=True)

    def weight(start, size):
        return wf_ref[:, :, :, pl.ds(start, size)].reshape(D, size)

    wide = hidden // 2
    first, second = slice(0, wide), slice(wide, hidden)
    grads = [dg_ref.at[:, :, :, first], du_ref.at[:, :, :, first], dg_ref.at[:, :, :, second], du_ref.at[:, :, :, second],
             db_ref, do_ref] + [wf_ref.at[:, :, :, i * D : (i + 1) * D] for i in range(3)] + [dc_ref]
    totals = [og_ref.at[:, first], ou_ref.at[:, first], og_ref.at[:, second], ou_ref.at[:, second],
              od_ref, oo_ref] + [op_ref.at[:, i * D : (i + 1) * D] for i in range(3)] + [oc_ref]
    tasks = [
        (AcrossFirst if i in ACROSS_FIRST else Reduction)(
            links, grads[i], totals[i], mine_ref if i == kinds - 1 else None,
            crecv[i], yrecv[i], zrecv[i], xrecv[i], stages[i], sems, i,
        )
        for i in range(kinds)
    ]
    for number, i in enumerate(ACROSS_FIRST):
        tasks[i].third, tasks[i].stage_two = extra[2 * number], extra[2 * number + 1]
    returns = (Return(links, y_ref, ry_ref, sems, 0), Return(links, gres_ref, rg_ref, sems, 1))
    gains = gc_ref[...]
    gain = gains[2:3]
    valid = valid_column(tab_ref, rank)
    h1_ref, dv_ref = fa_ref, fa_ref
    tiles = hidden // FF_TILE
    kept = {}

    def enter():
        load_cot.wait()
        load_out.wait()
        for tile in range(TILES):
            rows = pl.ds(tile * QT, QT)
            value = x_ref[rows, :].astype(F32) + mm(att_ref[rows, :], weight(0, D))
            h1_ref[rows, :] = value
            normed = (value * lax.rsqrt(mean_square(value) + EPSILON) * gain).astype(BF16)
            n_ref[rows, :] = normed
            ntt_ref[:, tile * QT : (tile + 1) * QT] = jnp.transpose(normed)
            gres_ref[rows, :] = (ga_ref[rows, :].astype(F32) * valid[tile * QT : (tile + 1) * QT]).astype(BF16)
        load_in.wait()
        load_down.wait()

    def inward(begin, end):
        def step(tile, carry):
            at = pl.multiple_of(tile * FF_TILE, FF_TILE)
            cols = pl.ds(at, FF_TILE)
            normed = n_ref[:ROWS, :]
            gate = mm(normed, weight(D + at, FF_TILE))
            up = mm(normed, weight(D + hidden + at, FF_TILE))
            back = mm_cols(gres_ref[...], wd_ref[cols, :])
            square = gate * gate
            bend = jnp.tanh(GELU_C * (gate * (1.0 + GELU_A * square)))
            half = 0.5 * (1.0 + bend)
            act = gate * half
            slope = half + (0.5 * GELU_C) * gate * (1.0 - bend * bend) * (1.0 + (3.0 * GELU_A) * square)
            b0_ref[:ROWS, cols] = (act * up).astype(BF16)
            b1_ref[:ROWS, cols] = (back * up * slope).astype(BF16)
            b2_ref[:ROWS, cols] = (back * act).astype(BF16)
            return carry

        lax.fori_loop(begin, end, step, 0)

    def outer_products(ref, right_ref, begin, end):
        def step(tile, carry):
            cols = pl.ds(pl.multiple_of(tile * FF_TILE, FF_TILE), FF_TILE)
            value = mm(ntt_ref[...], right_ref[:ROWS, cols]).astype(BF16)
            ref[:, :, :, cols] = value.reshape(outer, inner, part, FF_TILE)
            return carry

        lax.fori_loop(begin, end, step, 0)

    def down_products():
        def step(tile, carry):
            cols = pl.ds(pl.multiple_of(tile * FF_TILE, FF_TILE), FF_TILE)
            db_ref[tile // inner, tile % inner] = mm_rows(b0_ref[:ROWS, cols], gres_ref[...]).astype(BF16)
            return carry

        lax.fori_loop(0, tiles, step, 0)

    def outward():
        def step(tile, carry):
            cols = pl.ds(pl.multiple_of(tile * group, 128), group)
            value = h1_ref[:ROWS, cols] + mm(b0_ref[:ROWS, :hidden], wd_ref[:, cols])
            y_ref[:, cols] = (value * valid).astype(BF16)
            shards = pl.ds(tile * (4 // inner), 4 // inner)
            gh_ref[:, cols] = mm_cols(
                b1_ref[:ROWS, :hidden], wf_ref[shards, :, :, D : D + hidden].reshape(group, hidden)
            ) + mm_cols(b2_ref[:ROWS, :hidden], wf_ref[shards, :, :, D + hidden :].reshape(group, hidden))
            return carry

        lax.fori_loop(0, D // group, step, 0)

    def load():
        kept["qkv"] = fetch(4, qkv_any, b1_ref)
        kept["wqkv"] = fetch(5, wqkv_any, b2_ref)

    def middle():
        gain_grad = jnp.zeros((1, D), F32)
        for tile in range(TILES):
            rows = pl.ds(tile * QT, QT)
            value, grad = h1_ref[rows, :], gh_ref[rows, :]
            root = lax.rsqrt(mean_square(value) + EPSILON)
            unit = value * root
            gain_grad = gain_grad + jnp.sum(grad * unit, axis=0, keepdims=True)
            grad = grad * gain
            grad = gres_ref[rows, :].astype(F32) + root * (
                grad - unit * jnp.mean(grad * unit, axis=-1, keepdims=True)
            )
            gh_ref[rows, :] = grad
            low = grad.astype(BF16)
            n_ref[rows, :] = low
            ga_ref[rows, :] = mm_cols(low, weight(0, D)).astype(BF16)
        kept["gain"] = gain_grad

    def out_products():
        def step(tile, carry):
            cols = pl.ds(pl.multiple_of(tile * QUAD, QUAD), QUAD)
            value = mm_rows(att_ref[...], n_ref[:ROWS, cols]).astype(BF16)
            do_ref[:, :, :, cols] = value.reshape(outer, inner, part, QUAD)
            return carry

        lax.fori_loop(0, D // QUAD, step, 0)
        kept["n"] = fetch(6, n_any, n_ref)

    def attention(quad):
        if quad == 0:
            backward_attention_start(dk_ref, dv_ref)
            kept["qkv"].wait()
        backward_attention_quad(tab_ref, rank, b1_ref, att_ref, ga_ref, lse_ref, b0_ref, dk_ref, dv_ref, quad)

    def project_products(quad):
        if quad == 0:
            kept["n"].wait()
        for number in range(3):
            value = mm_rows(n_ref[...], b0_ref[:, number * D + quad * QUAD : number * D + (quad + 1) * QUAD])
            low = (quad * 3 + number) * QUAD
            wf_ref[:, :, :, low : low + QUAD] = value.astype(BF16).reshape(outer, inner, part, QUAD)

    def input_gradient():
        kept["wqkv"].wait()
        kept["one"], kept["side"] = backward_project(
            tab_ref, rank, x_ref, gh_ref, gains, n_ref, b0_ref, b2_ref, dk_ref, gres_ref
        )

    def gain_pieces():
        rows = jnp.concatenate([kept["one"], kept["side"], kept["gain"], jnp.zeros((5, D), F32)], axis=0)
        spread_gain_grads(rows, dc_ref)

    half = tiles // 2
    work = {
        "start": lambda: None, "load": load, "P0": enter, "P1a": lambda: inward(0, half), "P1b": lambda: inward(half, tiles),
        "gA": lambda: outer_products(dg_ref, b1_ref, 0, half), "gB": lambda: outer_products(dg_ref, b1_ref, half, tiles),
        "uA": lambda: outer_products(du_ref, b2_ref, 0, half), "uB": lambda: outer_products(du_ref, b2_ref, half, tiles),
        "d": down_products, "out": outward, "P4": middle, "P5": out_products,
        "q0": lambda: attention(0), "q1": lambda: attention(1), "q2": lambda: attention(2),
        "p0": lambda: project_products(0), "p1": lambda: project_products(1), "p2": lambda: project_products(2),
        "bp": input_gradient, "dc": gain_pieces,
    }
    paired, begun = set(), set()
    for action, which, *turn in REAR_ORDER:
        if action == "do":
            work[which]()
        elif action == "begin":
            if not begun:
                links.met()
            begun.add(which)
            if which == 6:
                pl.semaphore_wait(free_sem, 1)
            tasks[which].begin()
        elif action == "pair":
            tasks[which].pair()
            paired.add(which)
            if which < 3 and paired >= {0, 1, 2}:
                pl.semaphore_signal(free_sem, inc=1, device_id={"rep": links.mate}, device_id_type=MESH)
        elif action == "meet":
            tasks[which].meet()
        elif action == "col":
            tasks[which].column()
        elif action == "hop":
            tasks[which].hop(turn[0])
        elif action == "cross":
            tasks[which].cross()
        elif action == "fin":
            tasks[which].finish()
        elif action == "rows":
            returns[which].begin()
        else:
            returns[which].relay()
    for one in returns:
        one.settle()
    for task in tasks:
        task.settle()
    links.drain()


def feed_and_reduce(count, table, x, att, lse, gc, cot, n, qkv, wqkv, wf, wd):
    outer, inner = grid_of(count)
    part, tall = D // count, wd.shape[1]
    hidden = count * tall
    wf = wf.reshape((outer, inner) + wf.shape[1:])
    full = [(part, hidden), (part, hidden), (tall, D), (part, D), (part, 3 * D), (8, 128)]
    shapes = [(part, hidden // 2)] * 4 + [(tall, D)] + [(part, D)] * 4 + [(8, 128)]
    kinds = len(shapes)
    dtypes = [BF16] * (kinds - 1) + [F32]
    halved = [(a, b // 2 if b % 256 == 0 else b) for a, b in shapes]
    later = [(a // 2, b) if i in ACROSS_FIRST else (a, b) for i, (a, b) in enumerate(halved)]
    dma, vmem = pltpu.SemaphoreType.DMA, pltpu.VMEM
    scratch = [
        vmem((ROWS, D), BF16), vmem((ROWS, D), F32), vmem((ALL_ROWS, D), F32), vmem((ALL_ROWS, D), F32),
        vmem((ALL_ROWS, 3 * D), BF16), vmem((ALL_ROWS, 3 * D), BF16), vmem((D, 3 * D), BF16),
        vmem((ALL_ROWS, D), BF16), vmem((D, ROWS), BF16), vmem((ROWS, D), BF16), vmem((ROWS, D), BF16),
        vmem(wf.shape, BF16), vmem((hidden, D), BF16),
    ]
    scratch += [vmem((outer, inner) + shape, BF16) for shape in full[:4]]
    scratch += [vmem((outer, inner) + full[-1], F32)] * 2
    scratch += [vmem((outer, inner) + halved[i], dtypes[i]) for i in (0, 1, 2, 3, 4, 5, 9)]
    for lead in ((outer,), (outer + 1,), ()):
        for i in range(kinds):
            across = (outer, inner) if i in ACROSS_FIRST and lead == () else lead
            scratch.append(vmem(across + later[i], dtypes[i]))
    scratch += [vmem(shape, F32) for shape in later]
    for i in ACROSS_FIRST:
        scratch += [vmem(later[i], BF16), vmem(later[i], F32)]
    one = dma((kinds,))
    scratch += [one, one, one, one, one, dma((2, outer, kinds)), dma((outer + 1, kinds))] + [one] * 9
    scratch += [dma((2, 3)), dma((2, 3)), dma((2,)), dma((1,)), dma((7,)), pltpu.SemaphoreType.REGULAR]
    rows = jax.ShapeDtypeStruct((4, ROWS, D), BF16)
    outs = pl.pallas_call(
        partial(rear_kernel, outer, inner),
        out_shape=tuple(jax.ShapeDtypeStruct(shape, F32) for shape in full) + (rows, rows),
        in_specs=[SMEM] + [VMEM] * 4 + [ANY] * 6,
        out_specs=(ANY,) * 8,
        scratch_shapes=scratch,
        compiler_params=pltpu.CompilerParams(
            collective_id=2, has_side_effects=True, vmem_limit_bytes=67043328
        ),
        name="feed_and_reduce",
    )(table, x, att, lse, gc, cot, n, qkv, wqkv, wf, wd.reshape(hidden, D))
    return outs[:6], outs[6], outs[7]


def place_kernel(part, tab_ref, ry_ref, rg_ref, og_ref, ou_ref, od_ref, oo_ref, op_ref, oc_ref, *refs):
    (y_ref, g_ref, q_out, k_out, v_out, o_out, g_out, u_out, d_out, one_out, side_out, two_out), refs = refs[:12], refs[12:]
    (y_buf, g_buf, zero, bg, bu, bd, bo, bp, sem_in, sem_out, sem_rows, sem_home) = refs
    blocks = y_buf.shape[0]
    base = lax.axis_index("rep") * blocks
    tables = ((og_ref, bg), (ou_ref, bu), (od_ref, bd), (oo_ref, bo), (op_ref, bp))
    reads = [pltpu.make_async_copy(src, dst, sem_in.at[i]) for i, (src, dst) in enumerate(tables)]
    rows = ((ry_ref, y_buf, y_ref), (rg_ref, g_buf, g_ref))

    for read in reads:
        read.start()
    zero[...] = jnp.zeros(zero.shape, zero.dtype)

    def fetch(block, carry):
        index = tab_ref[48, base + block]
        safe = jnp.maximum(index, 0)
        for kind, (src, buf, dst) in enumerate(rows):
            @pl.when(index >= 0)
            def _():
                pltpu.make_async_copy(
                    src.at[lax.div(safe, SLOTS), lax.rem(safe, SLOTS)], buf.at[block], sem_rows.at[kind, block]
                ).start()

            @pl.when(index < 0)
            def _():
                pltpu.make_async_copy(zero, dst.at[block], sem_home.at[kind, block]).start()

        return carry

    lax.fori_loop(0, blocks, fetch, 0)
    for number, out in enumerate((one_out, side_out, two_out)):
        out[...] = oc_ref[number, :part]
    def leave(block, carry):
        @pl.when(tab_ref[48, base + block] >= 0)
        def _():
            for kind, (src, buf, dst) in enumerate(rows):
                pltpu.make_async_copy(src.at[0, 0], buf.at[block], sem_rows.at[kind, block]).wait()
                pltpu.make_async_copy(buf.at[block], dst.at[block], sem_home.at[kind, block]).start()

        return carry

    lax.fori_loop(0, blocks, leave, 0)
    writes = []
    for number, (buf, dst) in enumerate(((bg, g_out), (bu, u_out), (bd, d_out), (bo, o_out))):
        reads[number].wait()
        writes.append(pltpu.make_async_copy(buf, dst, sem_out.at[number]))
        writes[-1].start()
    reads[4].wait()
    for quad in range(D // QUAD):
        for number, dst in enumerate((q_out, k_out, v_out)):
            low = (3 * quad + number) * QUAD
            copy = pltpu.make_async_copy(
                bp.at[:, low : low + QUAD], dst.at[:, quad * QUAD : (quad + 1) * QUAD], sem_out.at[4 + 3 * quad + number]
            )
            copy.start()
            writes.append(copy)
    for write in writes:
        write.wait()

    def rest(block, carry):
        for kind, (_, buf, dst) in enumerate(rows):
            pltpu.make_async_copy(buf.at[block], dst.at[block], sem_home.at[kind, block]).wait()
        return carry

    lax.fori_loop(0, blocks, rest, 0)


def place_all(table, ry, rg, totals, blocks, part, shape):
    out = jax.ShapeDtypeStruct
    og, ou, od, oo, op, oc = totals
    block = (blocks,) + ry.shape[2:]
    dma, vmem = pltpu.SemaphoreType.DMA, pltpu.VMEM
    gain = out((part,), F32)
    y, g, q, k, v, o, gate, up, down, one, side, two = pl.pallas_call(
        partial(place_kernel, part),
        out_shape=(out(block, ry.dtype), out(block, rg.dtype), out(oo.shape, F32), out(oo.shape, F32), out(oo.shape, F32),
                   out(oo.shape, F32), out(og.shape, F32), out(ou.shape, F32), out(od.shape, F32), gain, gain, gain),
        in_specs=[SMEM] + [ANY] * 7 + [VMEM],
        out_specs=(ANY,) * 9 + (VMEM,) * 3,
        scratch_shapes=[vmem(block, ry.dtype), vmem(block, rg.dtype), vmem(block[1:], ry.dtype)] + [vmem(t.shape, F32) for t in totals[:5]]
        + [dma((5,)), dma((13,)), dma((2, blocks)), dma((2, blocks))],
        compiler_params=pltpu.CompilerParams(vmem_limit_bytes=VMEM_LIMIT),
        name="place_outputs",
    )(table, ry, rg, og, ou, od, oo, op, oc)
    return (y.reshape(shape), g.reshape(shape), one, side, q, k, v, o, two, gate, up, down)


def per_device(count, layer_input, cotangent, lengths, attn_gain, global_gain, query_weight, key_weight,
               value_weight, out_weight, ffn_gain, gate_weight, up_weight, down_weight):
    micro, span, width = layer_input.shape
    hidden = gate_weight.shape[1]
    blocks = micro * span // BLK
    part = attn_gain.shape[0]
    rows_in = layer_input.reshape(blocks, BLK, width)
    cots_in = cotangent.reshape(blocks, BLK, width)
    weights = (query_weight, key_weight, value_weight, out_weight, gate_weight, up_weight)
    gains = (attn_gain, global_gain, ffn_gain)
    if grid_of(count)[1] == 2 and part % 16 == 0:
        table, gains, x, cot, n, qkv, att, lse, wqkv, ga, gb = gather_and_attend(
            count, lengths, rows_in, cots_in, weights, down_weight, gains
        )
        totals, ry, rg = feed_and_reduce(count, table, x, att, lse, gains, cot, n, qkv, wqkv, ga, gb)
        ry, rg = (rows.reshape(4, SLOTS, BLK, width) for rows in (ry, rg))
        return place_all(table, ry, rg, totals, blocks, part, layer_input.shape)
    else:
        table = deal_table(lengths)
        wc = jnp.pad(jnp.stack(gains), ((0, 13), (0, 128 - part)))
        splits = ((0, 4 * width), (4 * width, 2 * hidden))
        ga, gb, gc, rows, cots = gather_weights(
            count, splits, table, rows_in, cots_in, jnp.concatenate(weights, axis=1), down_weight, wc
        )
        x, full = rows.reshape(ROWS, width), ga.reshape(width, -1)
        n, qkv, att, lse = attend(table, x, gc, full)
        y, gh, gatt, dg, du, db, do, gain = feed(
            table, x, cots.reshape(ROWS, width), att, gc, full, gb.reshape(-1, width)
        )
        g, dw, dc = backward_layer(table, x, gh, gatt, att, lse, n, qkv, gain, gc, full)
        grads = [grad.reshape(count, -1, grad.shape[-1]) for grad in (dg, du, db, do, dw, dc)]
        og, ou, ob, oo, ow, oc, ry, rg = reduce_grads(
            count, grads, y.reshape(SLOTS, BLK, width), g.reshape(SLOTS, BLK, width)
        )
        oq, ok, ov = ow[:, :width], ow[:, width : 2 * width], ow[:, 2 * width :]
    y_home, g_home = bring_home(table, ry, rg, blocks)
    return (
        y_home.reshape(layer_input.shape), g_home.reshape(layer_input.shape),
        oc[0, :part], oc[1, :part], oq, ok, ov, oo, oc[2, :part], og, ou, ob,
    )


def solution(mesh):
    rows = P(None, ("rep", "fsdp"), None)
    vector, matrix = P("fsdp"), P("fsdp", None)
    return jax.shard_map(
        partial(per_device, mesh.shape["fsdp"]),
        mesh=mesh,
        in_specs=(rows, rows, P(None, ("rep", "fsdp")), vector, vector, matrix, matrix, matrix, matrix,
                  vector, matrix, matrix, matrix),
        out_specs=(rows, rows, vector, vector, matrix, matrix, matrix, matrix, vector, matrix, matrix, matrix),
        check_vma=False,
    )
```

```python
from functools import partial

import jax
import jax.numpy as jnp
from jax import lax
from jax.experimental import pallas as pl
from jax.experimental.pallas import tpu as pltpu
from jax.sharding import PartitionSpec as P

H = 12
DH = 64
RADIUS = 127
GBLK = 16
BLK = 64
SLOTS = 10
MAX_SEQ_BLOCKS = 5
EPSILON = 1e-06
MASKED_SCORE = -1e30
MESH = pl.DeviceIdType.MESH
VMEM_LIMIT = 60 * 1024 * 1024
SEG_AT, LEN_AT, DEST_AT, TABLE_SIZE = 40, 80, 120, 256

ANY = pl.BlockSpec(memory_space=pl.ANY)
VMEM = pl.BlockSpec(memory_space=pltpu.VMEM)
SMEM = pl.BlockSpec(memory_space=pltpu.SMEM)


def grid_of(count):
    inner = 2 if count <= 8 else 4
    return count // inner, inner


def core_of(rank):
    return rank + 1 - 2 * (rank % 2)


def across_of(rank):
    return (rank + 2) % 4


def lens_kernel(lens_ref, all_ref, send_sem, recv_sem):
    rank = lax.axis_index("rep")
    barrier = pltpu.get_barrier_semaphore()
    for step in range(1, 4):
        pl.semaphore_signal(
            barrier, inc=1, device_id={"rep": (rank + step) % 4}, device_id_type=MESH
        )
    pl.semaphore_wait(barrier, 3)
    copies = []
    for step in range(1, 4):
        copy = pltpu.make_async_remote_copy(
            src_ref=lens_ref,
            dst_ref=all_ref.at[rank],
            send_sem=send_sem.at[step - 1],
            recv_sem=recv_sem.at[step - 1],
            device_id={"rep": (rank + step) % 4},
            device_id_type=MESH,
        )
        copy.start()
        copies.append(copy)
    all_ref[rank] = lens_ref[...]
    for copy in copies:
        copy.wait()


def table_kernel(micro, per_dev, lens_ref, tab_ref, order_ref, count_ref, load_ref):
    total = 4 * micro * per_dev

    def length_at(spot):
        return lens_ref[spot // (micro * per_dev), (spot // per_dev) % micro, spot % per_dev]

    def blocks_of(length):
        return (length + (BLK - 1)) // BLK

    def clear(spot, carry):
        tab_ref[spot] = -1
        return carry

    lax.fori_loop(0, TABLE_SIZE, clear, 0)
    for spot in range(4 * SLOTS):
        tab_ref[LEN_AT + spot] = 0
    for size in range(8):
        count_ref[size] = 0
    for dev in range(4):
        load_ref[dev] = 0

    def tally(spot, carry):
        length = length_at(spot)

        @pl.when(length > 0)
        def _():
            size = blocks_of(length)
            count_ref[size] = count_ref[size] + 1

        return carry

    lax.fori_loop(0, total, tally, 0)
    begin = 0
    for size in range(MAX_SEQ_BLOCKS, 0, -1):
        amount = count_ref[size]
        count_ref[size] = begin
        begin = begin + amount

    def place(spot, carry):
        length = length_at(spot)

        @pl.when(length > 0)
        def _():
            size = blocks_of(length)
            where = count_ref[size]
            order_ref[where] = spot
            count_ref[size] = where + 1

        return carry

    lax.fori_loop(0, total, place, 0)

    def assign(number, carry):
        spot = order_ref[number]
        length = length_at(spot)
        size = blocks_of(length)
        best = jnp.int32(0)
        low = load_ref[0]
        for dev in range(1, 4):
            here = load_ref[dev]
            best = jnp.where(here < low, dev, best)
            low = jnp.minimum(here, low)
        load_ref[best] = low + size

        def put(step, inner):
            slot = best * SLOTS + low + step
            tab_ref[slot] = spot + step
            tab_ref[SEG_AT + slot] = low
            tab_ref[LEN_AT + slot] = jnp.minimum(length - BLK * step, BLK)
            tab_ref[DEST_AT + spot + step] = slot
            return inner

        lax.fori_loop(0, size, put, 0)
        return carry

    lax.fori_loop(0, begin, assign, 0)


def deal_table(lengths):
    micro, per_dev = lengths.shape
    padded = jnp.pad(lengths, ((0, 8 - micro), (0, 128 - per_dev)))
    everyone = pl.pallas_call(
        lens_kernel,
        out_shape=jax.ShapeDtypeStruct((4, 8, 128), jnp.int32),
        in_specs=[VMEM],
        out_specs=VMEM,
        scratch_shapes=[pltpu.SemaphoreType.DMA((3,)), pltpu.SemaphoreType.DMA((3,))],
        compiler_params=pltpu.CompilerParams(collective_id=0, has_side_effects=True),
        name="lens_exchange",
    )(padded)
    return pl.pallas_call(
        partial(table_kernel, micro, per_dev),
        out_shape=jax.ShapeDtypeStruct((TABLE_SIZE,), jnp.int32),
        in_specs=[SMEM],
        out_specs=SMEM,
        scratch_shapes=[
            pltpu.SMEM((4 * micro * per_dev,), jnp.int32),
            pltpu.SMEM((8,), jnp.int32),
            pltpu.SMEM((4,), jnp.int32),
        ],
        name="deal_table",
    )(everyone)


def gather_kernel(
    outer, inner, splits, tab_ref, rows_ref, cots_ref, wa_ref, wb_ref, wc_ref,
    ga_ref, gb_ref, gc_ref, rows_out, cots_out,
    psend, precv, xsend, xrecv,
    z_send, z_recv, y_send, y_recv, c_send, c_recv, own_sem,
    p_send, p_recv, x_send, x_recv,
):
    rank = lax.axis_index("rep")
    spot = lax.axis_index("fsdp")
    core = rank % 2
    row, col = spot // inner, spot % inner
    count = outer * inner
    mate, across = core_of(rank), across_of(rank)
    pieces = [(wa_ref, ga_ref, start, width // 2) for start, width in splits]
    pieces.append((wb_ref, gb_ref, 0, wb_ref.shape[1] // 2))
    pieces.append((wc_ref, gc_ref, 0, None))
    halved = [number for number, piece in enumerate(pieces) if piece[3] is not None]

    barrier = pltpu.get_barrier_semaphore()
    neighbours = (
        (row + 1 < outer, {"fsdp": spot + inner}),
        (row > 0, {"fsdp": spot - inner}),
        (col + 1 < inner, {"fsdp": spot + 1}),
        (col > 0, {"fsdp": spot - 1}),
    )
    amount = jnp.int32(2)
    for there, device in neighbours:
        amount = amount + there.astype(jnp.int32)

        @pl.when(there)
        def _():
            pl.semaphore_signal(barrier, inc=1, device_id=device, device_id_type=MESH)

    for device in (mate, across):
        pl.semaphore_signal(barrier, inc=1, device_id={"rep": device}, device_id_type=MESH)
    pl.semaphore_wait(barrier, amount)

    def cut(ref, number):
        _, _, start, half = pieces[number]
        if half is None:
            return ref
        return ref.at[:, pl.ds(pl.multiple_of(start + core * half, 128), half)]

    def landed(number, shard):
        return cut(pieces[number][1].at[shard], number)

    late = []

    def send(there, src, dst, ssem, rsem, device):
        def describe():
            return pltpu.make_async_remote_copy(
                src_ref=src, dst_ref=dst, send_sem=ssem, recv_sem=rsem,
                device_id=device, device_id_type=MESH,
            )

        if there is None:
            describe().start()
            late.append((None, lambda: describe().wait_send()))
        else:
            @pl.when(there)
            def _():
                describe().start()

            late.append((there, lambda: describe().wait_send()))

    def arrive(number, shard, rsem):
        pltpu.make_async_remote_copy(
            src_ref=landed(number, shard), dst_ref=landed(number, shard),
            send_sem=own_sem.at[0], recv_sem=rsem,
            device_id={"rep": mate}, device_id_type=MESH,
        ).wait_recv()

    def both(first, second):
        return second if first is None else jnp.logical_and(first, second)

    def to_mate(there, number, shard):
        if number not in halved:
            return
        place = landed(number, shard)
        send(there, place, place, c_send.at[number, shard], c_recv.at[number, shard], {"rep": mate})

    def along_row(there, number, line, src):
        shard = line * inner + col
        place = landed(number, shard)
        src = place if src is None else src
        send(both(there, col + 1 < inner), src, place,
             y_send.at[0, 0, line, number], y_recv.at[0, 0, line, number], {"fsdp": spot + 1})
        send(both(there, col > 0), src, place,
             y_send.at[1, 0, line, number], y_recv.at[1, 0, line, number], {"fsdp": spot - 1})

    def from_row(there, number, line):
        for step in range(inner - 1):
            for way, source, onward, target in (
                (0, col - 1 - step, col + 1 < inner, spot + 1),
                (1, col + 1 + step, col > 0, spot - 1),
            ):
                here = jnp.logical_and(source >= 0, source < inner)
                here = both(there, here)
                shard = line * inner + source

                @pl.when(here)
                def _():
                    arrive(number, shard, y_recv.at[way, step, line, number])

                if step + 1 < inner - 1:
                    place = landed(number, shard)
                    send(both(here, onward), place, place,
                         y_send.at[way, step + 1, line, number],
                         y_recv.at[way, step + 1, line, number], {"fsdp": target})
                to_mate(here, number, shard)

    for number, piece in enumerate(pieces):
        src, place = cut(piece[0], number), landed(number, spot)
        send(row + 1 < outer, src, place, z_send.at[0, 0, number], z_recv.at[0, 0, number],
             {"fsdp": spot + inner})
        send(row > 0, src, place, z_send.at[1, 0, number], z_recv.at[1, 0, number],
             {"fsdp": spot - inner})
        along_row(None, number, row, src)
    own = [
        pltpu.make_async_copy(wa_ref, ga_ref.at[spot], own_sem.at[0]),
        pltpu.make_async_copy(wb_ref, gb_ref.at[spot], own_sem.at[1]),
        pltpu.make_async_copy(wc_ref, gc_ref.at[spot], own_sem.at[2]),
    ]
    for copy in own:
        copy.start()

    sources = (rows_ref, cots_ref)
    per_rank = rows_ref.shape[0]

    def picked(kind, target, slot):
        index = tab_ref[target * SLOTS + slot] - rank * per_rank
        mine = jnp.logical_and(index >= 0, index < per_rank)
        value = sources[kind][jnp.clip(index, 0, per_rank - 1)]
        return mine, value

    def mate_copy(kind, part):
        return pltpu.make_async_remote_copy(
            src_ref=psend.at[kind, part], dst_ref=precv.at[kind, part],
            send_sem=p_send.at[kind, part], recv_sem=p_recv.at[kind, part],
            device_id={"rep": mate}, device_id_type=MESH,
        )

    def across_copy(kind):
        return pltpu.make_async_remote_copy(
            src_ref=xsend.at[kind], dst_ref=xrecv.at[kind],
            send_sem=x_send.at[kind], recv_sem=x_recv.at[kind],
            device_id={"rep": across}, device_id_type=MESH,
        )

    for kind, part in ((0, 1), (1, 1), (0, 0), (1, 0)):
        target = mate if part == 0 else across_of(mate)

        def pack(slot, carry):
            mine, value = picked(kind, target, slot)
            psend[kind, part, slot] = jnp.where(mine, value, jnp.zeros_like(value))
            return carry

        lax.fori_loop(0, SLOTS, pack, 0)
        mate_copy(kind, part).start()
    for kind in range(2):
        mate_copy(kind, 1).wait_recv()

        def merge(slot, carry):
            mine, value = picked(kind, across, slot)
            xsend[kind, slot] = jnp.where(mine, value, precv[kind, 1, slot])
            return carry

        lax.fori_loop(0, SLOTS, merge, 0)
        across_copy(kind).start()

    def lines(step):
        return ((row - 1 - step >= 0, row - 1 - step, 0, row + 1 < outer, spot + inner),
                (row + 1 + step < outer, row + 1 + step, 1, row > 0, spot - inner))

    for step in range(outer - 1):
        for number in range(len(pieces)):
            for here, line, way, onward, target in lines(step):
                shard = line * inner + col

                @pl.when(here)
                def _():
                    arrive(number, shard, z_recv.at[way, step, number])

                if step + 1 < outer - 1:
                    place = landed(number, shard)
                    send(jnp.logical_and(here, onward), place, place,
                         z_send.at[way, step + 1, number], z_recv.at[way, step + 1, number],
                         {"fsdp": target})
                along_row(here, number, line, None)
                to_mate(here, number, shard)
        for number in range(len(pieces)):
            if step == 0:
                from_row(None, number, row)
            else:
                for here, line, *_ in lines(step - 1):
                    from_row(here, number, line)
    for number in range(len(pieces)):
        for here, line, *_ in lines(outer - 2):
            from_row(here, number, line)

    outs = (rows_out, cots_out)
    for kind in range(2):
        mate_copy(kind, 0).wait_recv()
        across_copy(kind).wait_recv()

        def finish(slot, carry):
            mine, value = picked(kind, rank, slot)
            outs[kind][slot] = jnp.where(mine, value, precv[kind, 0, slot] + xrecv[kind, slot])
            return carry

        lax.fori_loop(0, SLOTS, finish, 0)

    for shard in range(count):
        @pl.when(shard != spot)
        def _():
            for number in halved:
                other = pieces[number]
                view = other[1].at[shard].at[:, pl.ds(0, other[3])]
                pltpu.make_async_remote_copy(
                    src_ref=view, dst_ref=view, send_sem=own_sem.at[0],
                    recv_sem=c_recv.at[number, shard],
                    device_id={"rep": mate}, device_id_type=MESH,
                ).wait_recv()
    for there, finish_send in late:
        if there is None:
            finish_send()
        else:
            pl.when(there)(finish_send)
    for kind in range(2):
        for part in range(2):
            mate_copy(kind, part).wait_send()
        across_copy(kind).wait_send()
    for copy in own:
        copy.wait()


def gather_weights(count, splits, table, rows, cots, wa, wb, wc):
    outer, inner = grid_of(count)
    block = rows.shape[1:]
    kinds = len(splits) + 2
    dma = pltpu.SemaphoreType.DMA
    bf16 = jnp.bfloat16
    return pl.pallas_call(
        partial(gather_kernel, outer, inner, splits),
        out_shape=(
            jax.ShapeDtypeStruct((count,) + wa.shape, bf16),
            jax.ShapeDtypeStruct((count,) + wb.shape, bf16),
            jax.ShapeDtypeStruct((count,) + wc.shape, bf16),
            jax.ShapeDtypeStruct((SLOTS,) + block, bf16),
            jax.ShapeDtypeStruct((SLOTS,) + block, bf16),
        ),
        in_specs=[SMEM, VMEM, VMEM, VMEM, VMEM, VMEM],
        out_specs=(ANY, ANY, ANY, VMEM, VMEM),
        scratch_shapes=[
            pltpu.VMEM((2, 2, SLOTS) + block, bf16),
            pltpu.VMEM((2, 2, SLOTS) + block, bf16),
            pltpu.VMEM((2, SLOTS) + block, bf16),
            pltpu.VMEM((2, SLOTS) + block, bf16),
            dma((2, outer - 1, kinds)), dma((2, outer - 1, kinds)),
            dma((2, inner - 1, outer, kinds)), dma((2, inner - 1, outer, kinds)),
            dma((kinds, count)), dma((kinds, count)), dma((3,)),
            dma((2, 2)), dma((2, 2)), dma((2,)), dma((2,)),
        ],
        compiler_params=pltpu.CompilerParams(
            collective_id=1, has_side_effects=True, vmem_limit_bytes=VMEM_LIMIT
        ),
        name="gather_and_deal",
    )(table, rows, cots, wa, wb, wc)


def reduce_kernel(
    outer, inner, kinds, *refs
):
    grads, (y_ref, g_ref) = refs[:kinds], refs[kinds : kinds + 2]
    totals, (ry_ref, rg_ref) = refs[kinds + 2 : 2 * kinds + 2], refs[2 * kinds + 2 : 2 * kinds + 4]
    scratch = refs[2 * kinds + 4 :]
    mines, crecvs, yrecvs, zrecvs, xrecvs = (
        scratch[kinds * i : kinds * (i + 1)] for i in range(5)
    )
    (c_send, c_recv, m_sem, y_send, y_recv, z_send, z_recv, x_send, x_recv, f_send, f_recv,
     r_send, r_recv, q_sem) = scratch[5 * kinds :]
    rank = lax.axis_index("rep")
    spot = lax.axis_index("fsdp")
    core = rank % 2
    row, col = spot // inner, spot % inner
    mate, across = core_of(rank), across_of(rank)
    pieces = [(src, dst, 0, src.shape[3] // 2) for src, dst in zip(grads[:-1], totals)]
    pieces.append((grads[-1], totals[-1], 0, None))

    barrier = pltpu.get_barrier_semaphore()
    neighbours = (
        (row + 1 < outer, {"fsdp": spot + inner}),
        (row > 0, {"fsdp": spot - inner}),
        (col + 1 < inner, {"fsdp": spot + 1}),
        (col > 0, {"fsdp": spot - 1}),
    )
    amount = jnp.int32(2)
    for there, device in neighbours:
        amount = amount + there.astype(jnp.int32)

        @pl.when(there)
        def _():
            pl.semaphore_signal(barrier, inc=1, device_id=device, device_id_type=MESH)

    for device in (mate, across):
        pl.semaphore_signal(barrier, inc=1, device_id={"rep": device}, device_id_type=MESH)
    pl.semaphore_wait(barrier, amount)

    late = []

    def send(there, src, dst, ssem, rsem, device):
        def describe():
            return pltpu.make_async_remote_copy(
                src_ref=src, dst_ref=dst, send_sem=ssem, recv_sem=rsem,
                device_id=device, device_id_type=MESH,
            )

        if there is None:
            describe().start()
            late.append((None, lambda: describe().wait_send()))
        else:
            @pl.when(there)
            def _():
                describe().start()

            late.append((there, lambda: describe().wait_send()))

    def arrive(place, rsem):
        pltpu.make_async_remote_copy(
            src_ref=place, dst_ref=place, send_sem=q_sem.at[0], recv_sem=rsem,
            device_id={"rep": mate}, device_id_type=MESH,
        ).wait_recv()

    def columns(ref, number, which):
        _, _, start, half = pieces[number]
        if half is None:
            return ref
        cols = pl.ds(pl.multiple_of(start + which * half, 128), half)
        return ref.at[:, :, :, cols] if len(ref.shape) == 4 else ref.at[:, cols]

    order = list(range(kinds))
    loads = []
    for number in order:
        src = columns(pieces[number][0], number, 1 - core)
        send(None, src, crecvs[number], c_send.at[number], c_recv.at[number], {"rep": mate})
        load = pltpu.make_async_copy(
            columns(pieces[number][0], number, core), mines[number], m_sem.at[number]
        )
        load.start()
        loads.append(load)

    for kind, (src, dst) in enumerate(((y_ref, ry_ref), (g_ref, rg_ref))):
        send(None, src, dst.at[rank], r_send.at[kind, 0], r_recv.at[kind, 0], {"rep": across})
        send(None, src, dst.at[rank], r_send.at[kind, 1], r_recv.at[kind, 1], {"rep": mate})
        pltpu.make_async_copy(src, dst.at[rank], q_sem.at[kind + 1]).start()

    def slot_of(way, size, place, dest):
        if size == 2:
            return 0
        return dest - place if way == 0 else size - place + dest

    def line_sum(number, size, place, stride, buffer, view, ssem, rsem):
        for far in range(size - 1, 0, -1):
            for way in range(2):
                dest = far if way == 0 else size - 1 - far
                step = 1 if way == 0 else -1
                passes = place < dest if way == 0 else place > dest
                first = place == 0 if way == 0 else place == size - 1
                mine = view(dest)
                got = slot_of(way, size, place, dest)

                @pl.when(jnp.logical_and(passes, jnp.logical_not(first)))
                def _():
                    arrive(buffer.at[got], rsem.at[got, number])
                    mine[...] = mine[...] + buffer[got]

                put = slot_of(way, size, place + step, dest)
                send(passes, mine, buffer.at[put], ssem.at[way, dest, number], rsem.at[put, number],
                     {"fsdp": spot + step * stride})
        for way in range(2):
            has = place > 0 if way == 0 else place < size - 1
            got = slot_of(way, size, place, place)
            mine = view(place)

            @pl.when(has)
            def _():
                arrive(buffer.at[got], rsem.at[got, number])
                mine[...] = mine[...] + buffer[got]

    for number in order:
        loads[number].wait()
        arrive(crecvs[number], c_recv.at[number])
        mine, other = mines[number], crecvs[number]

        def add(index, carry):
            mine[index // inner, index % inner] = (
                mine[index // inner, index % inner] + other[index // inner, index % inner]
            )
            return carry

        lax.fori_loop(0, outer * inner, add, 0)
        if inner == 2:
            send(None, mine.at[:, 1 - col], yrecvs[number].at[0], y_send.at[0, 0, number],
                 y_recv.at[0, number], {"fsdp": spot + 1 - 2 * col})
    for kind, dst in enumerate((ry_ref, rg_ref)):
        place = dst.at[across]
        arrive(place, r_recv.at[kind, 0])
        send(None, place, place, r_send.at[kind, 2], r_recv.at[kind, 2], {"rep": mate})
    for number in order:
        mine = mines[number]
        if inner == 2:
            arrive(yrecvs[number].at[0], y_recv.at[0, number])
            buffer = yrecvs[number]

            def add(index, carry):
                mine[index, col] = mine[index, col] + buffer[0, index]
                return carry

            lax.fori_loop(0, outer, add, 0)
        else:
            line_sum(number, inner, col, 1, yrecvs[number], lambda dest: mine.at[:, dest],
                     y_send, y_recv)
        line_sum(number, outer, row, inner, zrecvs[number], lambda dest: mine.at[dest, col],
                 z_send, z_recv)
        send(None, mine.at[row, col], xrecvs[number], x_send.at[number], x_recv.at[number],
             {"rep": across})
    for number in order:
        arrive(xrecvs[number], x_recv.at[number])
        total = mines[number][row, col].astype(jnp.float32) + xrecvs[number][...].astype(jnp.float32)
        out, half = pieces[number][1], pieces[number][3]
        place = columns(out, number, core)
        place[...] = total
        if half is not None:
            send(None, place, place, f_send.at[number], f_recv.at[number], {"rep": mate})
    for number in order:
        if pieces[number][3] is not None:
            arrive(columns(pieces[number][1], number, 1 - core), f_recv.at[number])
    for kind, dst in enumerate((ry_ref, rg_ref)):
        arrive(dst.at[mate], r_recv.at[kind, 1])
        arrive(dst.at[across_of(mate)], r_recv.at[kind, 2])
        src = y_ref if kind == 0 else g_ref
        pltpu.make_async_copy(src, dst.at[rank], q_sem.at[kind + 1]).wait()
    for there, finish_send in late:
        if there is None:
            finish_send()
        else:
            pl.when(there)(finish_send)


def reduce_grads(count, grads, y_rows, g_rows):
    outer, inner = grid_of(count)
    kinds = len(grads)
    shapes = [(grad.shape[1], grad.shape[2] // 2, grad.dtype) for grad in grads[:-1]]
    shapes.append(grads[-1].shape[1:] + (grads[-1].dtype,))
    dma = pltpu.SemaphoreType.DMA
    y_slots = 1 if inner == 2 else inner + 1
    z_slots = 1 if outer == 2 else outer + 1
    scratch = []
    for lead in ((outer, inner), (outer, inner), (y_slots, outer), (z_slots,), ()):
        scratch += [pltpu.VMEM(lead + (a, b), dtype) for a, b, dtype in shapes]
    scratch += [
        dma((kinds,)), dma((kinds,)), dma((kinds,)),
        dma((2, inner, kinds)), dma((y_slots, kinds)),
        dma((2, outer, kinds)), dma((z_slots, kinds)),
        dma((kinds,)), dma((kinds,)), dma((kinds,)), dma((kinds,)),
        dma((2, 3)), dma((2, 3)), dma((3,)),
    ]
    return pl.pallas_call(
        partial(reduce_kernel, outer, inner, kinds),
        out_shape=tuple(jax.ShapeDtypeStruct(grad.shape[1:], jnp.float32) for grad in grads) + (
            jax.ShapeDtypeStruct((4,) + y_rows.shape, y_rows.dtype),
            jax.ShapeDtypeStruct((4,) + g_rows.shape, g_rows.dtype),
        ),
        in_specs=[ANY] * (kinds + 2),
        out_specs=(VMEM,) * kinds + (ANY, ANY),
        scratch_shapes=scratch,
        compiler_params=pltpu.CompilerParams(
            collective_id=2, has_side_effects=True, vmem_limit_bytes=VMEM_LIMIT
        ),
        name="reduce_and_return",
    )(*(grad.reshape((outer, inner) + grad.shape[1:]) for grad in grads), y_rows, g_rows)


def home_kernel(tab_ref, ry_ref, rg_ref, y_ref, g_ref):
    base = lax.axis_index("rep") * y_ref.shape[0]

    def fetch(block, carry):
        index = tab_ref[DEST_AT + base + block] if len(tab_ref.shape) == 1 else tab_ref[48, base + block]
        safe = jnp.maximum(index, 0)
        for src, dst in ((ry_ref, y_ref), (rg_ref, g_ref)):
            value = src[safe // SLOTS, safe % SLOTS]
            dst[block] = jnp.where(index >= 0, value, jnp.zeros_like(value))
        return carry

    lax.fori_loop(0, y_ref.shape[0], fetch, 0)


def bring_home(table, ry, rg, blocks):
    shape = jax.ShapeDtypeStruct((blocks,) + ry.shape[2:], ry.dtype)
    return pl.pallas_call(
        home_kernel,
        out_shape=(shape, shape),
        in_specs=[SMEM, VMEM, VMEM],
        out_specs=(VMEM, VMEM),
        compiler_params=pltpu.CompilerParams(vmem_limit_bytes=VMEM_LIMIT),
        name="place_rows",
    )(table, ry, rg)


D = H * DH
ROWS = SLOTS * BLK
SIDES = SLOTS * (BLK // GBLK)
SIDE_ROWS = 48
ALL_ROWS = ROWS + SIDE_ROWS
QT = 128
WIN = 384
TILES = ROWS // QT
QUAD = 256
FF_TILE = 256
GELU_C = 0.7978845608028654
GELU_A = 0.044715
F32, BF16 = jnp.float32, jnp.bfloat16


def mm(left, right):
    return lax.dot_general(left, right, (((1,), (0,)), ((), ())), preferred_element_type=F32)


def mm_cols(left, right):
    return lax.dot_general(left, right, (((1,), (1,)), ((), ())), preferred_element_type=F32)


def mm_rows(left, right):
    return lax.dot_general(left, right, (((0,), (0,)), ((), ())), preferred_element_type=F32)


def iota(shape, axis):
    return lax.broadcasted_iota(jnp.int32, shape, axis)


def pick_by(index, values, other):
    out = jnp.full(index.shape, other, jnp.int32)
    for number, value in enumerate(values):
        out = jnp.where(index == number, value, out)
    return out


def block_at(tab_ref, slot):
    return lax.rem(tab_ref[slot, 0], 128) - 1


def seg_at(tab_ref, slot):
    if len(tab_ref.shape) == 1:
        return tab_ref[SEG_AT + slot]
    return lax.div(tab_ref[slot, 0], 16384) - 1


def len_at(tab_ref, slot):
    if len(tab_ref.shape) == 1:
        return tab_ref[LEN_AT + slot]
    return lax.rem(lax.div(tab_ref[slot, 0], 128), 128)


def slot_info(tab_ref, rank):
    seg = [seg_at(tab_ref, rank * SLOTS + slot) for slot in range(SLOTS)]
    length = [len_at(tab_ref, rank * SLOTS + slot) for slot in range(SLOTS)]
    return seg, length


def valid_column(tab_ref, rank):
    _, length = slot_info(tab_ref, rank)
    row = iota((ROWS, 1), 0)
    return ((row % BLK) < pick_by(row // BLK, length, 0)).astype(F32)


def pooling(tab_ref, rank):
    _, length = slot_info(tab_ref, rank)
    row = iota((1, ROWS), 1)
    block = jnp.where((row % BLK) < pick_by(row // BLK, length, 0), row // GBLK, -1)
    return jnp.where(iota((SIDE_ROWS, ROWS), 0) == block, 1.0, 0.0).astype(BF16)


def key_segments(tab_ref, rank, first_block, index):
    blocks = WIN // BLK
    base = rank * SLOTS + first_block
    seg = [seg_at(tab_ref, base + step) for step in range(blocks)]
    length = [len_at(tab_ref, base + step) for step in range(blocks)]
    alive = (index % BLK) < pick_by(index // BLK, length, 0)
    return jnp.where(alive, pick_by(index // BLK, seg, -2), -2)


def side_segments(tab_ref, rank, index):
    seg, length = slot_info(tab_ref, rank)
    per = BLK // GBLK
    alive = (index % per) * GBLK < pick_by(index // per, length, 0)
    return jnp.where(alive, pick_by(index // per, seg, -2), -2)


def tile_bias(tab_ref, rank, tile, first_row, keys_axis):
    qs, ks, gs = ((QT, 1), (1, WIN), (1, SIDE_ROWS)) if keys_axis == 1 else ((1, QT), (WIN, 1), (SIDE_ROWS, 1))
    q_index = iota(qs, 1 - keys_axis)
    k_index = iota(ks, keys_axis)
    g_index = iota(gs, keys_axis)
    base = rank * SLOTS + tile * (QT // BLK)
    q_seg = pick_by(q_index // BLK, [seg_at(tab_ref, base + step) for step in range(QT // BLK)], -1)
    k_seg = key_segments(tab_ref, rank, first_row // BLK, k_index)
    g_seg = side_segments(tab_ref, rank, g_index)
    gap = (q_index + tile * QT) - (k_index + first_row)
    local = (jnp.abs(gap) <= RADIUS) & (q_seg == k_seg)
    return jnp.where(local, 0.0, MASKED_SCORE), jnp.where(q_seg == g_seg, 0.0, MASKED_SCORE)


def window_start(tile):
    return pl.multiple_of(jnp.clip(tile - 1, 0, TILES - WIN // QT) * QT, QT)


def head_stack(rows):
    lane = iota(rows.shape, 1) // DH
    zero = jnp.zeros_like(rows)
    return jnp.concatenate([jnp.where(lane == head, rows, zero) for head in range(QUAD // DH)], axis=0)


def head_merge(stacked):
    lane = iota((QT, QUAD), 1) // DH
    out = stacked[:QT]
    for head in range(1, QUAD // DH):
        out = jnp.where(lane == head, stacked[head * QT : (head + 1) * QT], out)
    return out


def gains_of(gc_ref):
    count = gc_ref.shape[0]
    part = D // count
    lane, column = iota((128, D), 0), iota((128, D), 1)
    total = None
    for shard in range(count):
        pick = jnp.where((column == lane + shard * part) & (lane < part), 1.0, 0.0).astype(BF16)
        term = mm(gc_ref[shard], pick)
        total = term if total is None else total + term
    return total


def three_way(value):
    high = value.astype(BF16)
    rest = value - high.astype(F32)
    middle = rest.astype(BF16)
    return high, middle, (rest - middle.astype(F32)).astype(BF16)


def spread_gain_grads(value, dc_ref):
    count = dc_ref.shape[0] if len(dc_ref.shape) == 3 else dc_ref.shape[0] * dc_ref.shape[1]
    part = D // count
    column, lane = iota((D, 128), 0), iota((D, 128), 1)
    parts = three_way(value)
    for shard in range(count):
        pick = jnp.where((column == lane + shard * part) & (lane < part), 1.0, 0.0).astype(BF16)
        place = dc_ref.at[shard] if len(dc_ref.shape) == 3 else dc_ref.at[shard // dc_ref.shape[1], shard % dc_ref.shape[1]]
        place[...] = mm(parts[0], pick) + mm(parts[1], pick) + mm(parts[2], pick)


def mean_square(value):
    return jnp.mean(value * value, axis=-1, keepdims=True)


def forward_norm(tab_ref, rank, x_ref, gains, n_ref):
    for tile in range(TILES):
        rows = pl.ds(tile * QT, QT)
        value = x_ref[rows, :].astype(F32)
        n_ref[rows, :] = (value * lax.rsqrt(mean_square(value) + EPSILON) * gains[0:1]).astype(BF16)
    side = mm(pooling(tab_ref, rank), n_ref[:ROWS, :])
    n_ref[ROWS:, :] = (side * lax.rsqrt(mean_square(side) + EPSILON) * gains[1:2]).astype(BF16)


def forward_project(n_ref, w_ref, qkv_ref):
    def step(tile, carry):
        cols = pl.ds(pl.multiple_of(tile * QUAD, QUAD), QUAD)
        qkv_ref[:, cols] = mm(n_ref[...], w_ref[:, cols]).astype(BF16)
        return carry

    lax.fori_loop(0, 3 * D // QUAD, step, 0)


def forward_attention(tab_ref, rank, qkv_ref, att_ref, lse_ref, begin, end):
    heads = QUAD // DH

    def step(tile, carry):
        first = window_start(tile)
        bias, side_bias = tile_bias(tab_ref, rank, tile, first, 1)
        rows = pl.ds(pl.multiple_of(tile * QT, QT), QT)
        window = pl.ds(first, WIN)
        lane = iota((QT, 128), 1)

        def four(quad, lse):
            low = pl.multiple_of(quad * QUAD, QUAD)
            cols, key_cols, value_cols = (pl.ds(low + number * D, QUAD) for number in range(3))
            query = head_stack(qkv_ref[rows, cols])
            scores = mm_cols(query, qkv_ref[window, key_cols])
            side_scores = mm_cols(query, qkv_ref[ROWS:, key_cols])
            local, sides, scale = [], [], []
            for head in range(heads):
                part = slice(head * QT, (head + 1) * QT)
                one = scores[part] + bias
                two = side_scores[part] + side_bias
                peak = jnp.maximum(
                    jnp.max(one, axis=-1, keepdims=True), jnp.max(two, axis=-1, keepdims=True)
                )
                one, two = jnp.exp(one - peak), jnp.exp(two - peak)
                total = jnp.sum(one, axis=-1, keepdims=True) + jnp.sum(two, axis=-1, keepdims=True)
                local.append(one.astype(BF16))
                sides.append(two.astype(BF16))
                scale.append(1.0 / total)
                lse = jnp.where(lane == quad * heads + head, peak + jnp.log(total), lse)
            mixed = mm(jnp.concatenate(local, axis=0), qkv_ref[window, value_cols])
            mixed = mixed + mm(jnp.concatenate(sides, axis=0), qkv_ref[ROWS:, value_cols])
            mixed = mixed * jnp.concatenate(scale, axis=0)
            att_ref[rows, cols] = head_merge(mixed).astype(BF16)
            return lse

        lse = lax.fori_loop(0, D // QUAD, four, jnp.zeros((QT, 128), F32))
        lse_ref[tile] = jnp.transpose(lse)[:16]
        return carry

    lax.fori_loop(begin, end, step, 0)


def feed_forward(tab_ref, rank, x_ref, cot_ref, att_ref, gains, w_ref, wb_ref,
                 y_ref, gh_ref, ga_ref, dg_ref, du_ref, db_ref, do_ref,
                 h1_ref, nt_ref, ntt_ref, gres_ref, h2_ref, gg_ref, gu_ref, gn_ref):
    hidden = wb_ref.shape[0]
    gate_at = w_ref.shape[1] - 2 * hidden
    out_at = gate_at - D
    valid = valid_column(tab_ref, rank)
    gain = gains[2:3]
    for tile in range(TILES):
        rows = pl.ds(tile * QT, QT)
        value = x_ref[rows, :].astype(F32) + mm(att_ref[rows, :], w_ref[:, out_at:gate_at])
        h1_ref[rows, :] = value
        normed = (value * lax.rsqrt(mean_square(value) + EPSILON) * gain).astype(BF16)
        nt_ref[rows, :] = normed
        ntt_ref[:, tile * QT : (tile + 1) * QT] = jnp.transpose(normed)
        gres_ref[rows, :] = (cot_ref[rows, :].astype(F32) * valid[tile * QT : (tile + 1) * QT]).astype(BF16)

    def inward(tile, carry):
        at = pl.multiple_of(tile * FF_TILE, FF_TILE)
        cols = pl.ds(at, FF_TILE)
        gate = mm(nt_ref[...], w_ref[:, pl.ds(gate_at + at, FF_TILE)])
        up = mm(nt_ref[...], w_ref[:, pl.ds(gate_at + hidden + at, FF_TILE)])
        back = mm_cols(gres_ref[...], wb_ref[cols, :])
        square = gate * gate
        bend = jnp.tanh(GELU_C * (gate * (1.0 + GELU_A * square)))
        half = 0.5 * (1.0 + bend)
        act = gate * half
        slope = half + (0.5 * GELU_C) * gate * (1.0 - bend * bend) * (1.0 + (3.0 * GELU_A) * square)
        h2_ref[:, cols] = (act * up).astype(BF16)
        gg_ref[:, cols] = (back * up * slope).astype(BF16)
        gu_ref[:, cols] = (back * act).astype(BF16)
        return carry

    lax.fori_loop(0, hidden // FF_TILE, inward, 0)

    def outward(tile, carry):
        cols = pl.ds(pl.multiple_of(tile * QUAD, QUAD), QUAD)
        value = h1_ref[:, cols] + mm(h2_ref[...], wb_ref[:, cols])
        y_ref[:, cols] = (value * valid).astype(BF16)
        gn_ref[:, cols] = mm_cols(gg_ref[...], w_ref[cols, gate_at : gate_at + hidden]) + mm_cols(
            gu_ref[...], w_ref[cols, gate_at + hidden :]
        )
        return carry

    lax.fori_loop(0, D // QUAD, outward, 0)

    def weights(tile, carry):
        at = pl.multiple_of(tile * FF_TILE, FF_TILE)
        cols = pl.ds(at, FF_TILE)
        dg_ref[:, cols] = mm(ntt_ref[...], gg_ref[:, cols]).astype(BF16)
        du_ref[:, cols] = mm(ntt_ref[...], gu_ref[:, cols]).astype(BF16)
        db_ref[cols, :] = mm_rows(h2_ref[:, cols], gres_ref[...]).astype(BF16)
        return carry

    lax.fori_loop(0, hidden // FF_TILE, weights, 0)

    gain_grad = jnp.zeros((1, D), F32)
    for tile in range(TILES):
        rows = pl.ds(tile * QT, QT)
        value, grad = h1_ref[rows, :], gn_ref[rows, :]
        root = lax.rsqrt(mean_square(value) + EPSILON)
        unit = value * root
        gain_grad = gain_grad + jnp.sum(grad * unit, axis=0, keepdims=True)
        grad = grad * gain
        grad = gres_ref[rows, :].astype(F32) + root * (
            grad - unit * jnp.mean(grad * unit, axis=-1, keepdims=True)
        )
        gh_ref[rows, :] = grad
        low = grad.astype(BF16)
        nt_ref[rows, :] = low
        ga_ref[rows, :] = mm_cols(low, w_ref[:, out_at:gate_at]).astype(BF16)

    def out_weight(tile, carry):
        cols = pl.ds(pl.multiple_of(tile * QUAD, QUAD), QUAD)
        do_ref[cols, :] = mm_rows(att_ref[:, cols], nt_ref[...]).astype(BF16)
        return carry

    lax.fori_loop(0, D // QUAD, out_weight, 0)
    return gain_grad


def backward_attention_start(dk_ref, dv_ref):
    dk_ref[...] = jnp.zeros_like(dk_ref)
    dv_ref[...] = jnp.zeros_like(dv_ref)


def backward_attention_quad(tab_ref, rank, qkv_ref, att_ref, ga_ref, lse_ref, dqkv_ref, dk_ref, dv_ref, quad):
    heads = QUAD // DH
    marks = jnp.where(iota((16, QUAD), 1) // DH == iota((16, QUAD), 0), 1.0, 0.0).astype(BF16)
    low = quad * QUAD
    cols = slice(low, low + QUAD)

    def step(tile, carry):
        first = window_start(tile)
        bias, side_bias = tile_bias(tab_ref, rank, tile, first, 0)
        bias = jnp.concatenate([bias, side_bias], axis=0)
        rows = pl.ds(pl.multiple_of(tile * QT, QT), QT)
        window = pl.ds(first, WIN)
        lse = lse_ref[tile]
        product = ga_ref[rows, cols].astype(F32) * att_ref[rows, cols].astype(F32)
        high = product.astype(BF16)
        rest = (product - high.astype(F32)).astype(BF16)
        centre = mm_cols(marks, high) + mm_cols(marks, rest)
        query = head_stack(qkv_ref[rows, cols])
        grad = head_stack(ga_ref[rows, cols])
        keys = jnp.concatenate(
            [qkv_ref[window, D + low : D + low + QUAD], qkv_ref[ROWS:, D + low : D + low + QUAD]], axis=0
        )
        values = jnp.concatenate(
            [qkv_ref[window, 2 * D + low : 2 * D + low + QUAD],
             qkv_ref[ROWS:, 2 * D + low : 2 * D + low + QUAD]], axis=0
        )
        scores = mm_cols(keys, query)
        slopes = mm_cols(values, grad)
        probs, grads = [], []
        for head in range(heads):
            part = slice(head * QT, (head + 1) * QT)
            number = quad * heads + head
            prob = jnp.exp(scores[:, part] + bias - lse[number : number + 1])
            probs.append(prob.astype(BF16))
            grads.append((prob * (slopes[:, part] - centre[head : head + 1])).astype(BF16))
        probs = jnp.concatenate(probs, axis=1)
        grads = jnp.concatenate(grads, axis=1)
        dkey = mm(grads, query)
        dvalue = mm(probs, grad)
        dk_ref[window, cols] = dk_ref[window, cols] + dkey[:WIN]
        dk_ref[ROWS:, cols] = dk_ref[ROWS:, cols] + dkey[WIN:]
        dv_ref[window, cols] = dv_ref[window, cols] + dvalue[:WIN]
        dv_ref[ROWS:, cols] = dv_ref[ROWS:, cols] + dvalue[WIN:]
        dqkv_ref[rows, cols] = head_merge(mm_rows(grads, keys)).astype(BF16)
        return carry

    lax.fori_loop(0, TILES, step, 0)
    dqkv_ref[ROWS:, cols] = jnp.zeros((SIDE_ROWS, QUAD), BF16)
    dqkv_ref[:, D + low : D + low + QUAD] = dk_ref[:, cols].astype(BF16)
    dqkv_ref[:, 2 * D + low : 2 * D + low + QUAD] = dv_ref[:, cols].astype(BF16)


def weight_grads(n_ref, dqkv_ref, refs):
    for number, ref in enumerate(refs):
        def weights(tile, carry):
            at = pl.multiple_of(tile * QUAD, QUAD)
            value = mm_rows(n_ref[...], dqkv_ref[:, pl.ds(number * D + at, QUAD)]).astype(BF16)
            if len(ref.shape) == 4:
                ref[:, :, :, pl.ds(at, QUAD)] = value.reshape(ref.shape[:3] + (QUAD,))
            else:
                ref[:, pl.ds(at, QUAD)] = value
            return carry

        lax.fori_loop(0, D // QUAD, weights, 0)


def backward_project(tab_ref, rank, x_ref, gh_ref, gains, n_ref, dqkv_ref, w_ref, gn_ref, g_ref):
    def step(tile, carry):
        cols = pl.ds(pl.multiple_of(tile * QUAD, QUAD), QUAD)
        gn_ref[:, cols] = mm_cols(dqkv_ref[...], w_ref[cols, : 3 * D])
        return carry

    lax.fori_loop(0, D // QUAD, step, 0)
    pool = pooling(tab_ref, rank)
    side = mm(pool, n_ref[:ROWS, :])
    root = lax.rsqrt(mean_square(side) + EPSILON)
    unit = side * root
    grad = gn_ref[ROWS:, :]
    side_gain = jnp.sum(grad * unit, axis=0, keepdims=True)
    grad = grad * gains[1:2]
    grad = root * (grad - unit * jnp.mean(grad * unit, axis=-1, keepdims=True))
    parts = three_way(grad)
    gain_grad = jnp.zeros((1, D), F32)
    for tile in range(TILES):
        rows = pl.ds(tile * QT, QT)
        spread = pool[:, tile * QT : (tile + 1) * QT]
        total = gn_ref[rows, :] + mm_rows(spread, parts[0]) + mm_rows(spread, parts[1])
        value = x_ref[rows, :].astype(F32)
        root = lax.rsqrt(mean_square(value) + EPSILON)
        unit = value * root
        gain_grad = gain_grad + jnp.sum(total * unit, axis=0, keepdims=True)
        total = total * gains[0:1]
        value = (
            gh_ref[rows, :] + root * (total - unit * jnp.mean(total * unit, axis=-1, keepdims=True))
        ).astype(BF16)
        if len(g_ref.shape) == 3:
            g_ref[pl.ds(tile * (QT // BLK), QT // BLK)] = value.reshape(QT // BLK, BLK, D)
        else:
            g_ref[rows, :] = value
    return gain_grad, side_gain


def gelu_both(gate):
    square = gate * gate
    bend = jnp.tanh(GELU_C * (gate * (1.0 + GELU_A * square)))
    half = 0.5 * (1.0 + bend)
    slope = half + (0.5 * GELU_C) * gate * (1.0 - bend * bend) * (1.0 + (3.0 * GELU_A) * square)
    return gate * half, slope


def first_kernel(tab_ref, x_ref, gc_ref, w_ref, n_ref, qkv_ref, att_ref, lse_ref):
    rank = lax.axis_index("rep")
    gains = gains_of(gc_ref)
    forward_norm(tab_ref, rank, x_ref, gains, n_ref)
    forward_project(n_ref, w_ref, qkv_ref)
    forward_attention(tab_ref, rank, qkv_ref, att_ref, lse_ref, 0, TILES)


def second_kernel(tab_ref, x_ref, cot_ref, att_ref, gc_ref, w_ref, wb_ref,
                  y_ref, gh_ref, ga_ref, dg_ref, du_ref, db_ref, do_ref, gain_ref, *scratch):
    rank = lax.axis_index("rep")
    gain_ref[...] = feed_forward(tab_ref, rank, x_ref, cot_ref, att_ref, gains_of(gc_ref), w_ref, wb_ref,
                                 y_ref, gh_ref, ga_ref, dg_ref, du_ref, db_ref, do_ref, *scratch)


def third_kernel(tab_ref, x_ref, gh_ref, ga_ref, att_ref, lse_ref, n_ref, qkv_ref, gain_ref, gc_ref, w_ref,
                 g_ref, dw_ref, dc_ref, dqkv_ref, dk_ref, dv_ref, gn_ref):
    rank = lax.axis_index("rep")
    gains = gains_of(gc_ref)
    backward_attention_start(dk_ref, dv_ref)
    for quad in range(D // QUAD):
        backward_attention_quad(tab_ref, rank, qkv_ref, att_ref, ga_ref, lse_ref, dqkv_ref, dk_ref, dv_ref, quad)
    weight_grads(n_ref, dqkv_ref, [dw_ref.at[:, i * D : (i + 1) * D] for i in range(3)])
    one, side = backward_project(tab_ref, rank, x_ref, gh_ref, gains, n_ref, dqkv_ref, w_ref, gn_ref, g_ref)
    grads = jnp.concatenate([one, side, gain_ref[...], jnp.zeros((5, D), F32)], axis=0)
    spread_gain_grads(grads, dc_ref)


def attend(tab, x, gc, w):
    shape = jax.ShapeDtypeStruct
    return pl.pallas_call(
        first_kernel,
        out_shape=(shape((ALL_ROWS, D), BF16), shape((ALL_ROWS, 3 * D), BF16), shape((ROWS, D), BF16),
                   shape((TILES, 16, QT), F32)),
        in_specs=[SMEM, VMEM, VMEM, pl.BlockSpec((D, 3 * D), lambda step: (0, 0))],
        grid=(1,),
        out_specs=(VMEM,) * 4,
        compiler_params=pltpu.CompilerParams(vmem_limit_bytes=VMEM_LIMIT),
        name="attend",
    )(tab, x, gc, w)


def feed(tab, x, cot, att, gc, w, wb):
    hidden = wb.shape[0]
    shape = jax.ShapeDtypeStruct
    return pl.pallas_call(
        second_kernel,
        out_shape=(shape((ROWS, D), BF16), shape((ROWS, D), F32), shape((ROWS, D), BF16),
                   shape((D, hidden), BF16), shape((D, hidden), BF16), shape((hidden, D), BF16), shape((D, D), BF16),
                   shape((1, D), F32)),
        in_specs=[SMEM] + [VMEM] * 6,
        out_specs=(VMEM,) * 8,
        scratch_shapes=[pltpu.VMEM((ROWS, D), F32), pltpu.VMEM((ROWS, D), BF16), pltpu.VMEM((D, ROWS), BF16),
                        pltpu.VMEM((ROWS, D), BF16), pltpu.VMEM((ROWS, hidden), BF16),
                        pltpu.VMEM((ROWS, hidden), BF16), pltpu.VMEM((ROWS, hidden), BF16),
                        pltpu.VMEM((ROWS, D), F32)],
        compiler_params=pltpu.CompilerParams(vmem_limit_bytes=VMEM_LIMIT),
        name="feed_forward",
    )(tab, x, cot, att, gc, w, wb)


def backward_layer(tab, x, gh, ga, att, lse, n, qkv, gain, gc, w):
    shape = jax.ShapeDtypeStruct
    return pl.pallas_call(
        third_kernel,
        out_shape=(shape((ROWS, D), BF16), shape((D, 3 * D), BF16), shape((gc.shape[0], 8, 128), F32)),
        in_specs=[SMEM] + [VMEM] * 9 + [pl.BlockSpec((D, 3 * D), lambda step: (0, 0))],
        grid=(1,),
        out_specs=(VMEM,) * 3,
        scratch_shapes=[pltpu.VMEM((ALL_ROWS, 3 * D), BF16), pltpu.VMEM((ALL_ROWS, D), F32),
                        pltpu.VMEM((ALL_ROWS, D), F32), pltpu.VMEM((ALL_ROWS, D), F32)],
        compiler_params=pltpu.CompilerParams(vmem_limit_bytes=VMEM_LIMIT),
        name="attend_back",
    )(tab, x, gh, ga, att, lse, n, qkv, gain, gc, w)


class Links:
    def __init__(self, outer, inner):
        self.outer, self.inner = outer, inner
        self.rank, self.spot = lax.axis_index("rep"), lax.axis_index("fsdp")
        self.core = self.rank % 2
        self.row, self.col = self.spot // inner, self.spot % inner
        self.mate, self.across = core_of(self.rank), across_of(self.rank)
        self.late = []

    def greet(self, everyone=False, later=False):
        barrier = pltpu.get_barrier_semaphore()
        neighbours = (
            (self.row + 1 < self.outer, {"fsdp": self.spot + self.inner}),
            (self.row > 0, {"fsdp": self.spot - self.inner}),
            (self.col + 1 < self.inner, {"fsdp": self.spot + 1}),
            (self.col > 0, {"fsdp": self.spot - 1}),
        )
        group = (self.mate, self.across) + ((across_of(self.mate),) if everyone else ())
        amount = jnp.int32(len(group))
        for there, device in neighbours:
            amount = amount + there.astype(jnp.int32)

            @pl.when(there)
            def _():
                pl.semaphore_signal(barrier, inc=1, device_id=device, device_id_type=MESH)

        for device in group:
            pl.semaphore_signal(barrier, inc=1, device_id={"rep": device}, device_id_type=MESH)
        self.met = lambda: pl.semaphore_wait(barrier, amount)
        if not later:
            self.met()

    def send(self, there, src, dst, ssem, rsem, device):
        def describe():
            return pltpu.make_async_remote_copy(
                src_ref=src, dst_ref=dst, send_sem=ssem, recv_sem=rsem,
                device_id=device, device_id_type=MESH,
            )

        if there is None:
            describe().start()
        else:
            @pl.when(there)
            def _():
                describe().start()

        self.late.append((there, lambda: describe().wait_send()))

    def arrive(self, place, rsem, spare):
        pltpu.make_async_remote_copy(
            src_ref=place, dst_ref=place, send_sem=spare, recv_sem=rsem,
            device_id={"rep": self.mate}, device_id_type=MESH,
        ).wait_recv()

    def drain(self):
        for there, finish in self.late:
            if there is None:
                finish()
            else:
                pl.when(there)(finish)


def halves(ref, which):
    half = ref.shape[-1] // 2
    cols = pl.ds(pl.multiple_of(which * half, 128), half)
    return ref.at[:, :, :, cols] if len(ref.shape) == 4 else ref.at[:, cols]


class Reduction:
    def __init__(self, links, source, total, mine, crecv, yrecv, zrecv, xrecv, stage, sems, number):
        self.links, self.source, self.total, self.mine, self.stage = links, source, total, mine, stage
        self.crecv, self.yrecv, self.zrecv, self.xrecv = crecv, yrecv, zrecv, xrecv
        self.sems, self.number = sems, number
        self.whole = total.shape[-1] % 256 != 0
        self.load = None

    def sem(self, name, *index):
        return self.sems[name].at[index + (self.number,)]

    def begin(self):
        links = self.links
        other = self.source if self.whole else halves(self.source, 1 - links.core)
        links.send(None, other, self.crecv, self.sem("c_send"), self.sem("c_recv"), {"rep": links.mate})
        if self.mine is None:
            self.mine = self.source if self.whole else halves(self.source, links.core)
        else:
            own = self.source if self.whole else halves(self.source, links.core)
            self.load = pltpu.make_async_copy(own, self.mine, self.sem("m_sem"))
            self.load.start()

    def pair(self):
        links = self.links
        if self.load is not None:
            self.load.wait()
        links.arrive(self.crecv, self.sem("c_recv"), self.sems["spare"].at[0])
        inner = links.inner

        def add(index, carry):
            row, col = index // inner, index % inner
            self.mine[row, col] = self.mine[row, col] + self.crecv[row, col]
            return carry

        lax.fori_loop(0, links.outer * inner, add, 0)
        links.send(None, self.mine.at[:, 1 - links.col], self.yrecv, self.sem("y_send"), self.sem("y_recv"),
                   {"fsdp": links.spot + 1 - 2 * links.col})

    def slot(self, way, place, dest):
        return dest - place if way == 0 else self.links.outer - place + dest

    def pass_on(self, way, dest, there, first):
        links = self.links
        step = 1 if way == 0 else -1
        mine = self.mine.at[dest, links.col]
        put = self.slot(way, links.row + step, dest)
        if not first:
            got = self.slot(way, links.row, dest)

            @pl.when(there)
            def _():
                links.arrive(self.zrecv.at[got], self.sem("z_recv", got), self.sems["spare"].at[0])
                mine[...] = mine[...] + self.zrecv[got]

        links.send(there, mine, self.zrecv.at[put], self.sem("z_send", way, dest), self.sem("z_recv", put),
                   {"fsdp": links.spot + step * links.inner})

    def column(self):
        links = self.links
        size = links.outer
        links.arrive(self.yrecv, self.sem("y_recv"), self.sems["spare"].at[0])

        def add(index, carry):
            self.mine[index, links.col] = self.mine[index, links.col] + self.yrecv[index]
            return carry

        lax.fori_loop(0, size, add, 0)
        for far in range(size - 1, 0, -1):
            self.pass_on(0, far, links.row == 0, True)
            self.pass_on(1, size - 1 - far, links.row == size - 1, True)

    def hop(self, turn):
        links = self.links
        size = links.outer
        for way in range(2):
            place = turn if way == 0 else size - 1 - turn
            here = links.row == place
            rest = range(size - 1, place, -1) if way == 0 else range(0, place)
            for dest in rest:
                self.pass_on(way, dest, here, False)
            mine = self.mine.at[place, links.col]
            got = self.slot(way, place, place)

            @pl.when(here)
            def _():
                links.arrive(self.zrecv.at[got], self.sem("z_recv", got), self.sems["spare"].at[0])
                mine[...] = mine[...] + self.zrecv[got]

    def cross(self):
        links = self.links
        mine = self.mine.at[links.row, links.col]
        links.send(None, mine, self.xrecv, self.sem("x_send"), self.sem("x_recv"), {"rep": links.across})

    def finish(self):
        links = self.links
        links.arrive(self.xrecv, self.sem("x_recv"), self.sems["spare"].at[0])
        self.stage[...] = self.mine[links.row, links.col].astype(F32) + self.xrecv[...].astype(F32)
        place = self.total if self.whole else halves(self.total, links.core)
        self.keep = pltpu.make_async_copy(self.stage, place, self.sem("m_sem"))
        self.keep.start()
        if not self.whole:
            links.send(None, self.stage, place, self.sem("f_send"), self.sem("f_recv"), {"rep": links.mate})

    def settle(self):
        self.keep.wait()
        if not self.whole:
            self.links.arrive(
                halves(self.total, 1 - self.links.core), self.sem("f_recv"), self.sems["spare"].at[0]
            )


class AcrossFirst(Reduction):
    def pair(self):
        links = self.links
        if self.load is not None:
            self.load.wait()
        links.arrive(self.crecv, self.sem("c_recv"), self.sems["spare"].at[0])
        inner = links.inner

        def add(index, carry):
            row, col = index // inner, index % inner
            self.mine[row, col] = self.mine[row, col] + self.crecv[row, col]
            return carry

        lax.fori_loop(0, links.outer * inner, add, 0)
        self.side = links.rank // 2
        links.send(None, self.rows_of(self.mine, 1 - self.side), self.xrecv, self.sem("x_send"), self.sem("x_recv"),
                   {"rep": links.across})

    def rows_of(self, ref, which):
        half = ref.shape[-2] // 2
        rows = pl.ds(pl.multiple_of(which * half, 16), half)
        return ref.at[:, :, rows, :] if len(ref.shape) == 4 else ref.at[rows, :]

    def meet(self):
        links = self.links
        links.arrive(self.xrecv, self.sem("x_recv"), self.sems["spare"].at[0])
        self.mine = self.rows_of(self.mine, self.side)
        inner = links.inner

        def add(index, carry):
            row, col = index // inner, index % inner
            self.mine[row, col] = self.mine[row, col] + self.xrecv[row, col]
            return carry

        lax.fori_loop(0, links.outer * inner, add, 0)
        links.send(None, self.mine.at[:, 1 - links.col], self.yrecv, self.sem("y_send"), self.sem("y_recv"),
                   {"fsdp": links.spot + 1 - 2 * links.col})

    def quarter(self, side, core):
        return halves(self.rows_of(self.total, side), core)

    def spread(self, stage, place, keep, ssem, rsem):
        links = self.links
        self.keeps.append(pltpu.make_async_copy(stage, place, keep))
        self.keeps[-1].start()
        links.send(None, stage, place, ssem, rsem, {"rep": links.mate})

    def cross(self):
        links = self.links
        mine = self.mine.at[links.row, links.col]
        links.send(None, mine, self.third, self.sem("h_send"), self.sem("h_recv"), {"rep": links.across})
        self.stage[...] = mine[...].astype(F32)
        self.keeps = []
        self.spread(self.stage, self.quarter(self.side, links.core), self.sem("m_sem"),
                    self.sem("f_send"), self.sem("f_recv"))

    def finish(self):
        links = self.links
        links.arrive(self.third, self.sem("h_recv"), self.sems["spare"].at[0])
        self.stage_two[...] = self.third[...].astype(F32)
        self.spread(self.stage_two, self.quarter(1 - self.side, links.core), self.sem("k_keep"),
                    self.sem("k_send"), self.sem("k_recv"))

    def settle(self):
        links = self.links
        for keep in self.keeps:
            keep.wait()
        for side, name in ((self.side, "f_recv"), (1 - self.side, "k_recv")):
            links.arrive(self.quarter(side, 1 - links.core), self.sem(name), self.sems["spare"].at[0])


SEM_NAMES = ("c_send", "c_recv", "m_sem", "y_send", "y_recv", "z_send", "z_recv", "x_send", "x_recv",
             "f_send", "f_recv", "h_send", "h_recv", "k_send", "k_recv", "k_keep", "r_send", "r_recv", "own", "spare")


class Return:
    def __init__(self, links, source, home, sems, kind):
        self.links, self.source, self.home, self.sems, self.kind = links, source, home, sems, kind

    def begin(self):
        links = self.links
        dst = self.home.at[links.rank]
        for way, device in enumerate((links.across, links.mate)):
            links.send(None, self.source, dst, self.sems["r_send"].at[self.kind, way],
                       self.sems["r_recv"].at[self.kind, way], {"rep": device})
        self.copy = pltpu.make_async_copy(self.source, dst, self.sems["own"].at[self.kind])
        self.copy.start()

    def relay(self):
        links = self.links
        place = self.home.at[links.across]
        links.arrive(place, self.sems["r_recv"].at[self.kind, 0], self.sems["spare"].at[0])
        links.send(None, place, place, self.sems["r_send"].at[self.kind, 2],
                   self.sems["r_recv"].at[self.kind, 2], {"rep": links.mate})

    def settle(self):
        links, sem = self.links, self.sems["r_recv"]
        links.arrive(self.home.at[links.mate], sem.at[self.kind, 1], self.sems["spare"].at[0])
        links.arrive(self.home.at[across_of(links.mate)], sem.at[self.kind, 2], self.sems["spare"].at[0])
        self.copy.wait()


TABLE_ROWS = 56


def packed_table(lens, tabv_ref):
    lane = iota((8, 128), 1)
    blocks = lax.div(lens + (BLK - 1), BLK)
    key = jnp.where(blocks > 0, blocks * 128 + (127 - lane), 0)
    wide = jnp.broadcast_to(key[:1], (128, 128))
    other = jnp.sum(jnp.where(iota((128, 128), 0) == iota((128, 128), 1), wide, 0), axis=1, keepdims=True)
    order = jnp.sum(jnp.where(other > wide, 1, 0), axis=0, keepdims=True)
    order = jnp.broadcast_to(order, (8, 128))
    edges, below = [], jnp.zeros((8, 1), jnp.int32)
    for size in range(MAX_SEQ_BLOCKS, 0, -1):
        below = below + jnp.sum(jnp.where(blocks == size, 1, 0), axis=1, keepdims=True)
        edges.append(jnp.broadcast_to(below, (8, 128)))

    def assign(number, carry):
        loads, slot, first = carry[:4], carry[4], carry[5]
        size = jnp.zeros((8, 128), jnp.int32)
        for step, edge in enumerate(edges):
            size = size + jnp.where(number < edge, 1, 0)
        low = jnp.minimum(jnp.minimum(loads[0], loads[1]), jnp.minimum(loads[2], loads[3]))
        best = jnp.full((8, 128), 3, jnp.int32)
        for dev in (2, 1, 0):
            best = jnp.where(loads[dev] == low, dev, best)
        mine = order == number
        slot = jnp.where(mine, best * SLOTS + low, slot)
        first = jnp.where(mine, low, first)
        loads = tuple(loads[dev] + jnp.where(best == dev, size, 0) for dev in range(4))
        return loads + (slot, first)

    zero = jnp.zeros((8, 128), jnp.int32)
    carry = lax.fori_loop(0, 32, assign, (zero,) * 6)
    slot, first = carry[4], carry[5]
    where, tokens, segment = zero - 1, zero, zero
    for step in range(MAX_SEQ_BLOCKS):
        def shifted(value):
            return value if step == 0 else pltpu.roll(value, step, 1)

        covers = shifted(blocks) > step
        where = jnp.where(covers, shifted(slot) + step, where)
        tokens = jnp.where(covers, jnp.minimum(shifted(lens) - BLK * step, BLK), tokens)
        segment = jnp.where(covers, shifted(first) + 1, segment)
    packed = jnp.where(where >= 0, (lane + 1) + 128 * tokens + 16384 * segment, 0)
    spots = jnp.broadcast_to(where[:1], (48, 128))
    values = jnp.broadcast_to(packed[:1], (48, 128))
    column = jnp.sum(jnp.where(spots == iota((48, 128), 0), values, 0), axis=1, keepdims=True)
    tabv_ref[:48] = jnp.broadcast_to(column, (48, 128))
    tabv_ref[48:] = where


ROW_FIRST = (3,)
FRONT_ORDER = (
    ("own", 1), ("own", 3), ("do", "table"), ("hop", 1, 0), ("own", 0), ("pack", 0, 1), ("hop", 1, 1), ("own", 5),
    ("cross", 0), ("own", 2), ("hop", 0, 0), ("hop", 1, 2), ("pack", 1, 1), ("pack", 0, 0), ("hop", 5, 0),
    ("hop", 5, 1), ("hop", 5, 2), ("hop", 0, 1), ("yz", 3), ("hop", 0, 2), ("own", 4), ("cross", 1), ("fr", 1),
    ("hop", 2, 0), ("pack", 1, 0), ("hop", 3, 0), ("fr", 5), ("rfin", 0), ("fr", 0), ("do", "norm"), ("hop", 2, 1),
    ("got", 0), ("hop", 4, 0), ("do", "proj"), ("do", "a0"), ("hop", 2, 2), ("hop", 4, 1), ("hop", 3, 1),
    ("do", "a1"), ("hop", 4, 2), ("fr", 2), ("do", "a2"), ("hop", 3, 2), ("got", 2), ("do", "enter"), ("rfin", 1),
    ("fr", 4), ("xin", 1), ("got", 3), ("do", "half"),
)


def front_kernel(outer, inner, *refs):
    (raw_ref, rows_any, cots_any, *weights), refs = refs[:9], refs[9:]
    (wd_any, *gain_refs), refs = refs[:4], refs[4:]
    (tab_ref, gains_ref), outs_any, (ga_ref, gb_ref), refs = refs[:2], refs[2:16], refs[16:18], refs[18:]
    (stage, lens_all, tabs, psend, precv, xsend, xrecv, rows_ref, cots_ref), refs = refs[:9], refs[9:]
    (lens_ref, wd_ref, wc_ref), refs = refs[:3], refs[3:]
    held, gc_ref, refs = refs[:14], refs[14], refs[15:]
    x_ref, cot_ref, n_ref, qkv_ref, att_ref, lse_ref, wqkv_ref, w2_ref, h1_ref, nt_ref, ntt_ref, b0_ref, b1_ref, b2_ref = held
    (l_send, l_recv, t_sem, w_sem, z_send, z_recv, y_send, y_recv, c_send, c_recv, d_send, d_recv, own_sem,
     p_send, p_recv, x_send, x_recv, spare, out_sem, piece_sem) = refs
    links = Links(outer, inner)
    rank, spot, core, mate, across = links.rank, links.spot, links.core, links.mate, links.across
    row, col = links.row, links.col
    side = rank // 2
    count = outer * inner
    part = stage.shape[0]
    per_rank = rows_ref.shape[0]
    width = 3 * D
    tall = wd_ref.shape[0]
    hidden = weights[-1].shape[1]
    rest = stage.shape[1] - width
    half = hidden // 2
    early = D + 2 * half
    spans = [(0, (D + half) // 2), (D + half, half // 2), (early, half)]

    at = 0
    loads = []
    loads.append(pltpu.make_async_copy(wd_any, wd_ref, w_sem.at[2]))
    loads[0].start()
    row_loads = [pltpu.make_async_copy(rows_any, rows_ref, w_sem.at[0]), pltpu.make_async_copy(cots_any, cots_ref, w_sem.at[1])]
    parts = [(ref, slice(0, D)) for ref in weights[:4]]
    parts += [(ref, cols) for cols in (slice(0, half), slice(half, hidden)) for ref in weights[4:]]
    for number, (ref, cols) in enumerate(parts):
        size = cols.stop - cols.start
        loads.append(pltpu.make_async_copy(ref.at[:, cols], stage.at[:, at : at + size], w_sem.at[3 + number]))
        loads[-1].start()
        at += size
    for load in row_loads:
        load.start()

    wc_ref[...] = jnp.zeros(wc_ref.shape, wc_ref.dtype)
    for number, ref in enumerate(gain_refs):
        wc_ref[number : number + 1, :part] = ref[...].reshape(1, part)
    micro, spots = raw_ref.shape
    lens_ref[...] = jnp.zeros(lens_ref.shape, lens_ref.dtype)
    lens_ref[:micro, :spots] = raw_ref[...]
    raw = lens_ref[...]
    spread = jnp.zeros((1, 128), jnp.int32)
    for device in range(4):
        line = jnp.zeros((1, 128), jnp.int32)
        for number in range(micro):
            shift = device * micro * spots + number * spots
            moved = raw if shift == 0 else pltpu.roll(raw, shift, 1)
            line = line + moved[number : number + 1]
        spread = jnp.where(rank == device, line, spread)
    lens_ref[...] = jnp.broadcast_to(spread, (8, 128))
    links.greet(True)
    lens_all[rank] = lens_ref[...]
    for step in range(1, 4):
        links.send(None, lens_ref, lens_all.at[rank], l_send.at[step - 1], l_recv.at[step - 1],
                   {"rep": (rank + step) % 4})

    def cols_of(start, half, which):
        return pl.ds(pl.multiple_of(start + which * half, 128), half)

    down_half = D // 2

    def tall_rows(which):
        return pl.ds(pl.multiple_of(which * (tall // 2), 16), tall // 2)

    def source(number):
        if number == 0:
            return stage.at[:, cols_of(0, width // 2, core)]
        if number == 1:
            return wd_ref.at[tall_rows(side), cols_of(0, down_half, core)]
        if number == 5:
            return wc_ref
        start, size = spans[number - 2]
        return stage.at[:, cols_of(width + start, size, core)]

    def place(number, shard, which=None):
        which = core if which is None else which
        if number == 0:
            return wqkv_ref.at[pl.ds(pl.multiple_of(shard * part, 16), part), cols_of(0, width // 2, which)]
        if number in (1, 6):
            return gb_ref.at[shard, tall_rows(side if number == 1 else 1 - side), cols_of(0, down_half, which)]
        if number == 5:
            return gc_ref.at[shard]
        start, size = spans[number - 2]
        if number == 4:
            return ga_ref.at[shard, :, cols_of(0, size, which)]
        return w2_ref.at[pl.ds(pl.multiple_of(shard * part, 16), part), cols_of(start, size, which)]

    nobody = spare.at[0]

    def both(first, second):
        return second if first is None else jnp.logical_and(first, second)

    def guarded(there, action):
        if there is None:
            action()
        else:
            pl.when(there)(action)

    def share(there, number, shard):
        if number == 5:
            return
        here = place(number, shard)
        links.send(there, here, here, c_send.at[number, shard], c_recv.at[number, shard], {"rep": mate})
        if number == 1:
            links.send(there, here, here, d_send.at[shard], d_recv.at[shard], {"rep": across})

    other_column = {"fsdp": spot + 1 - 2 * col}

    def along_row(there, number, line, src):
        here = place(number, line * inner + col)
        links.send(there, here if src is None else src, here, y_send.at[line, number], y_recv.at[line, number],
                   other_column)

    def lines(step):
        return ((row - 1 - step >= 0, row - 1 - step, 0, row + 1 < outer, spot + inner),
                (row + 1 + step < outer, row + 1 + step, 1, row > 0, spot - inner))

    def along_line(number, column, src):
        here = place(number, row * inner + (col if column == 0 else 1 - col))
        src = here if src is None else src
        links.send(row + 1 < outer, src, here, z_send.at[0, 0, number, column], z_recv.at[0, 0, number, column],
                   {"fsdp": spot + inner})
        links.send(row > 0, src, here, z_send.at[1, 0, number, column], z_recv.at[1, 0, number, column],
                   {"fsdp": spot - inner})

    def own(number):
        src = source(number)
        along_line(number, 0, src)
        along_row(None, number, row, src)

    def second_column(number):
        shard = row * inner + 1 - col
        links.arrive(place(number, shard), y_recv.at[row, number], nobody)
        share(None, number, shard)
        along_line(number, 1, None)

    def hop(number, step):
        for here, line, way, onward, target in lines(step):
            for column in range(2 if number in ROW_FIRST else 1):
                shard = line * inner + (col if column == 0 else 1 - col)
                guarded(here, lambda: links.arrive(place(number, shard), z_recv.at[way, step, number, column], nobody))
                if step + 1 < outer - 1:
                    view = place(number, shard)
                    links.send(both(here, onward), view, view, z_send.at[way, step + 1, number, column],
                               z_recv.at[way, step + 1, number, column], {"fsdp": target})
                if number not in ROW_FIRST:
                    along_row(here, number, line, None)
                share(here, number, shard)

    def from_row(number):
        def one(there, line):
            shard = line * inner + 1 - col
            guarded(there, lambda: links.arrive(place(number, shard), y_recv.at[line, number], nobody))
            share(there, number, shard)

        one(None, row)
        for step in range(outer - 1):
            for here, line, *_ in lines(step):
                one(here, line)

    def gathered(*numbers):
        def wait(shard, carry):
            @pl.when(shard != spot)
            def _():
                for number in numbers:
                    links.arrive(place(number, shard, 1 - core), c_recv.at[number, shard], nobody)

            return carry

        lax.fori_loop(0, count, wait, 0)

    def from_across():
        def relay(shard, carry):
            here = place(6, shard)

            @pl.when(shard != spot)
            def _():
                links.arrive(here, d_recv.at[shard], nobody)
                pltpu.make_async_remote_copy(
                    src_ref=here, dst_ref=here, send_sem=c_send.at[6, shard], recv_sem=c_recv.at[6, shard],
                    device_id={"rep": mate}, device_id_type=MESH,
                ).start()

            return carry

        lax.fori_loop(0, count, relay, 0)

    for load in loads:
        load.wait()
    keep = [
        pltpu.make_async_copy(stage.at[:, :width], wqkv_ref.at[pl.ds(pl.multiple_of(spot * part, 16), part)], own_sem.at[0]),
        pltpu.make_async_copy(stage.at[:, width + early :], ga_ref.at[spot], own_sem.at[1]),
        pltpu.make_async_copy(wd_ref, gb_ref.at[spot], own_sem.at[2]),
        pltpu.make_async_copy(wc_ref, gc_ref.at[spot], own_sem.at[3]),
        pltpu.make_async_copy(
            stage.at[:, width : width + early], w2_ref.at[pl.ds(pl.multiple_of(spot * part, 16), part)], own_sem.at[4]
        ),
    ]
    for copy in keep:
        copy.start()
    leaving = []

    def leave(*numbers):
        for number in numbers:
            leaving.append(pltpu.make_async_copy(held[number], outs_any[number], out_sem.at[number]))
            leaving[-1].start()

    def make_table():
        for step in range(1, 4):
            links.arrive(lens_all.at[(rank + 4 - step) % 4], l_recv.at[step - 1], nobody)
        lens = lens_all[0] + lens_all[1] + lens_all[2] + lens_all[3]
        packed_table(jnp.broadcast_to(lens[:1], (8, 128)), tab_ref)
        to_scalar = pltpu.make_async_copy(tab_ref, tabs, t_sem.at[0])
        to_scalar.start()
        to_scalar.wait()
        for load in row_loads:
            load.wait()

    sources = (rows_ref, cots_ref)
    outs = (x_ref, cot_ref)

    def picked(kind, target, slot):
        index = block_at(tabs, target * SLOTS + slot) - rank * per_rank
        mine = jnp.logical_and(index >= 0, index < per_rank)
        return mine, sources[kind][jnp.clip(index, 0, per_rank - 1)]

    def mate_copy(kind, piece):
        return pltpu.make_async_remote_copy(
            src_ref=psend.at[kind, piece], dst_ref=precv.at[kind, piece],
            send_sem=p_send.at[kind, piece], recv_sem=p_recv.at[kind, piece],
            device_id={"rep": mate}, device_id_type=MESH,
        )

    def across_copy(kind):
        return pltpu.make_async_remote_copy(
            src_ref=xsend.at[kind], dst_ref=xrecv.at[kind],
            send_sem=x_send.at[kind], recv_sem=x_recv.at[kind],
            device_id={"rep": across}, device_id_type=MESH,
        )

    def pack_rows(kind, piece):
        target = mate if piece == 0 else across_of(mate)

        def pack(slot, carry):
            mine, value = picked(kind, target, slot)
            psend[kind, piece, slot] = jnp.where(mine, value, jnp.zeros_like(value))
            return carry

        lax.fori_loop(0, SLOTS, pack, 0)
        mate_copy(kind, piece).start()

    def cross_rows(kind):
        mate_copy(kind, 1).wait_recv()

        def merge(slot, carry):
            mine, value = picked(kind, across, slot)
            xsend[kind, slot] = jnp.where(mine, value, precv[kind, 1, slot])
            return carry

        lax.fori_loop(0, SLOTS, merge, 0)
        across_copy(kind).start()

    def finish_rows(kind):
        mate_copy(kind, 0).wait_recv()
        across_copy(kind).wait_recv()

        def finish(slot, carry):
            mine, value = picked(kind, rank, slot)
            rows = pl.ds(pl.multiple_of(slot * BLK, BLK), BLK)
            outs[kind][rows, :] = jnp.where(mine, value, precv[kind, 0, slot] + xrecv[kind, slot])
            return carry

        lax.fori_loop(0, SLOTS, finish, 0)

    def norm():
        keep[3].wait()
        gains = gains_of(gc_ref)
        gains_ref[...] = gains
        forward_norm(tabs, rank, x_ref, gains, n_ref)
        leave(2)

    def project():
        keep[0].wait()
        forward_project(n_ref, wqkv_ref, qkv_ref)
        leave(3, 6)

    def attend_tiles(begin, end):
        forward_attention(tabs, rank, qkv_ref, att_ref, lse_ref, begin, end)
        if end == TILES:
            leave(4, 5)

    def enter():
        gain = gains_ref[2:3]
        for tile in range(TILES):
            rows = pl.ds(tile * QT, QT)
            value = x_ref[rows, :].astype(F32) + mm(att_ref[rows, :], w2_ref[:, :D])
            h1_ref[rows, :] = value
            normed = (value * lax.rsqrt(mean_square(value) + EPSILON) * gain).astype(BF16)
            nt_ref[rows, :] = normed
            ntt_ref[:, tile * QT : (tile + 1) * QT] = jnp.transpose(normed)
        leave(8, 9, 10)

    def first_half():
        def step(tile, carry):
            at = pl.multiple_of(tile * FF_TILE, FF_TILE)
            cols = pl.ds(at, FF_TILE)
            gate = mm(nt_ref[...], w2_ref[:, pl.ds(D + at, FF_TILE)])
            up = mm(nt_ref[...], w2_ref[:, pl.ds(D + half + at, FF_TILE)])
            act, slope = gelu_both(gate)
            b0_ref[:, cols] = (act * up).astype(BF16)
            b1_ref[:, cols] = (up * slope).astype(BF16)
            b2_ref[:, cols] = act.astype(BF16)
            for copy in piece_copies(tile):
                copy.start()
            return carry

        lax.fori_loop(0, half // FF_TILE, step, 0)

    def piece_copies(tile):
        cols = pl.ds(pl.multiple_of(tile * FF_TILE, FF_TILE), FF_TILE)
        return [
            pltpu.make_async_copy(held[number].at[:, cols], outs_any[number].at[:, cols], piece_sem.at[number - 11, tile])
            for number in (11, 12, 13)
        ]

    work = {"table": make_table, "enter": enter, "half": first_half, "norm": norm, "proj": project, "a0": lambda: attend_tiles(0, 2),
            "a1": lambda: attend_tiles(2, 4), "a2": lambda: attend_tiles(4, TILES)}
    for action, which, *more in FRONT_ORDER:
        if action == "do":
            work[which]()
        elif action == "own":
            own(which)
        elif action == "hop":
            hop(which, more[0])
        elif action == "fr":
            from_row(which)
        elif action == "yz":
            second_column(which)
        elif action == "xin":
            from_across()
        elif action == "got":
            gathered(which)
            if which == 2:
                keep[4].wait()
            if which == 3:
                leave(7)
        elif action == "pack":
            pack_rows(which, more[0])
        elif action == "cross":
            cross_rows(which)
        else:
            finish_rows(which)
            leave(which)
    gathered(1, 4, 6)

    def sent(shard, carry):
        @pl.when(shard != spot)
        def _():
            pltpu.make_async_remote_copy(
                src_ref=place(6, shard), dst_ref=place(6, shard), send_sem=c_send.at[6, shard], recv_sem=c_recv.at[6, shard],
                device_id={"rep": mate}, device_id_type=MESH,
            ).wait_send()

        return carry

    lax.fori_loop(0, count, sent, 0)
    links.drain()
    for kind in range(2):
        for piece in range(2):
            mate_copy(kind, piece).wait_send()
        across_copy(kind).wait_send()
    for copy in keep[1:3] + leaving:
        copy.wait()
    for tile in range(half // FF_TILE):
        for copy in piece_copies(tile):
            copy.wait()


def gather_and_attend(count, lens, rows, cots, weights, wd, gains):
    outer, inner = grid_of(count)
    block = rows.shape[1:]
    part, hidden = weights[0].shape[0], weights[-1].shape[1]
    dma, shape = pltpu.SemaphoreType.DMA, jax.ShapeDtypeStruct
    total = sum(weight.shape[1] for weight in weights)
    kinds = 6
    held = (shape((ROWS, D), BF16), shape((ROWS, D), BF16), shape((ALL_ROWS, D), BF16), shape((ALL_ROWS, 3 * D), BF16),
            shape((ROWS, D), BF16), shape((TILES, 16, QT), F32), shape((D, 3 * D), BF16), shape((D, D + hidden), BF16), shape((ROWS, D), F32),
            shape((ROWS, D), BF16), shape((D, ROWS), BF16)) + (shape((ROWS, hidden // 2), BF16),) * 3
    return pl.pallas_call(
        partial(front_kernel, outer, inner),
        out_shape=(shape((TABLE_ROWS, 128), jnp.int32), shape((16, D), F32)) + held + (
            shape((count, part, hidden), BF16), shape((count,) + wd.shape, BF16),
        ),
        in_specs=[VMEM] + [ANY] * 9 + [VMEM] * 3,
        out_specs=(VMEM,) * 2 + (ANY,) * 16,
        scratch_shapes=[
            pltpu.VMEM((part, total), BF16), pltpu.VMEM((4, 8, 128), jnp.int32), pltpu.SMEM((TABLE_ROWS, 128), jnp.int32),
            pltpu.VMEM((2, 2, SLOTS) + block, BF16), pltpu.VMEM((2, 2, SLOTS) + block, BF16),
            pltpu.VMEM((2, SLOTS) + block, BF16), pltpu.VMEM((2, SLOTS) + block, BF16),
            pltpu.VMEM(rows.shape, BF16), pltpu.VMEM(cots.shape, BF16),
            pltpu.VMEM((8, 128), jnp.int32), pltpu.VMEM(wd.shape, BF16), pltpu.VMEM((16, 128), BF16),
            *(pltpu.VMEM(one.shape, one.dtype) for one in held), pltpu.VMEM((count, 16, 128), BF16),
            dma((3,)), dma((3,)), dma((1,)), dma((11,)),
            dma((2, outer - 1, kinds, 2)), dma((2, outer - 1, kinds, 2)), dma((outer, kinds)), dma((outer, kinds)),
            dma((kinds + 1, count)), dma((kinds + 1, count)), dma((count,)), dma((count,)), dma((5,)),
            dma((2, 2)), dma((2, 2)), dma((2,)), dma((2,)), dma((1,)), dma((14,)), dma((3, hidden // 2 // FF_TILE)),
        ],
        compiler_params=pltpu.CompilerParams(
            collective_id=1, has_side_effects=True, vmem_limit_bytes=VMEM_LIMIT
        ),
        name="gather_and_attend",
    )(lens, rows, cots, *weights, wd, *gains)


ACROSS_FIRST = (1, 2)
REAR_ORDER = (
    ("do", "start"), ("do", "P0"), ("do", "P1a"), ("do", "gA"), ("begin", 0), ("do", "P1b"), ("pair", 0),
    ("do", "gB"), ("begin", 2), ("do", "uB"), ("begin", 3), ("do", "d"), ("begin", 4), ("pair", 2), ("do", "uA"),
    ("begin", 1), ("pair", 3), ("do", "out"), ("pair", 1), ("pair", 4), ("do", "load"), ("do", "P4"), ("do", "P5"),
    ("col", 0), ("col", 3), ("rows", 0), ("do", "q0"), ("do", "q1"), ("hop", 0, 1), ("meet", 2), ("do", "q2"),
    ("meet", 1), ("col", 4), ("do", "p0"), ("begin", 6), ("do", "bp"), ("rows", 1), ("pair", 6), ("do", "p1"),
    ("hop", 3, 1), ("begin", 5), ("hop", 0, 2), ("begin", 7), ("do", "dc"), ("do", "p2"), ("begin", 8), ("col", 2),
    ("pair", 7), ("hop", 4, 1), ("pair", 5), ("begin", 9), ("hop", 2, 1), ("col", 1), ("col", 6), ("hop", 0, 3),
    ("hop", 4, 2), ("col", 7), ("hop", 3, 2), ("hop", 6, 1), ("cross", 0), ("hop", 1, 1), ("pair", 8), ("hop", 4, 3),
    ("pair", 9), ("hop", 6, 2), ("col", 5), ("hop", 3, 3), ("cross", 4), ("cross", 3), ("hop", 7, 1), ("hop", 1, 2),
    ("hop", 2, 2), ("hop", 5, 1), ("col", 8), ("hop", 1, 3), ("cross", 1), ("hop", 6, 3), ("hop", 5, 2), ("col", 9),
    ("cross", 6), ("relay", 1), ("hop", 5, 3), ("cross", 5), ("hop", 2, 3), ("hop", 7, 2), ("hop", 7, 3),
    ("cross", 2), ("hop", 8, 1), ("relay", 0), ("cross", 7), ("hop", 9, 1), ("hop", 8, 2), ("hop", 9, 2),
    ("hop", 8, 3), ("cross", 8), ("fin", 2), ("fin", 4), ("hop", 9, 3), ("fin", 5), ("fin", 0), ("fin", 1),
    ("cross", 9), ("fin", 7), ("fin", 3), ("fin", 6), ("fin", 8), ("fin", 9),
)


def rear_kernel(outer, inner, *refs):
    (tab_ref, x_any, att_any, lse_ref, gc_ref), refs = refs[:5], refs[5:]
    (cot_any, n_any, qkv_any, wqkv_any, w2_any, wf_any, wd_any), refs = refs[:7], refs[7:]
    (h1_any, nt_any, ntt_any, b0_any, b1_any, b2_any), refs = refs[:6], refs[6:]
    kinds = 10
    (og_ref, ou_ref, od_ref, oo_ref, op_ref, oc_ref, ry_ref, rg_ref), refs = refs[:8], refs[8:]
    (y_ref, gh_ref, fa_ref, dk_ref, b0_ref, b1_ref, b2_ref, n_ref, ntt_ref, gres_ref, ga_ref), refs = refs[:11], refs[11:]
    (x_ref, att_ref), refs = refs[:2], refs[2:]
    (wf_ref, wd_ref, dg_ref, du_ref, db_ref, do_ref, dc_ref, mine_ref), refs = refs[:8], refs[8:]
    crecv, refs = list(refs[:7]), refs[7:]
    narrow = D // 2
    crecv = crecv[:6] + [crecv[i].at[:, :, :, :narrow] for i in range(3)] + crecv[6:]
    yrecv, zrecv, xrecv, stages = (refs[kinds * i : kinds * (i + 1)] for i in range(4))
    refs = refs[4 * kinds :]
    extra, refs = refs[: 2 * len(ACROSS_FIRST)], refs[2 * len(ACROSS_FIRST) :]
    sems = dict(zip(SEM_NAMES, refs))
    load_sem, free_sem = refs[len(SEM_NAMES) :]
    links = Links(outer, inner)
    rank = links.rank
    hidden = wd_ref.shape[0]
    part = wf_ref.shape[2]
    group = 4 * part

    def fetch(number, src, dst):
        copy = pltpu.make_async_copy(src, dst, load_sem.at[number])
        copy.start()
        return copy

    wide, early = hidden // 2, D + hidden
    load_first = [
        fetch(0, cot_any, ga_ref), fetch(1, wd_any.at[:wide], wd_ref.at[:wide]),
        fetch(7, b1_any, b1_ref.at[:ROWS, :wide]), fetch(8, b2_any, b2_ref.at[:ROWS, :wide]),
    ]
    load_products = fetch(9, ntt_any, ntt_ref)
    load_rest = [
        fetch(10, nt_any, n_ref.at[:ROWS]), fetch(2, wf_any, wf_ref.at[:, :, :, early:]),
        fetch(3, wd_any.at[wide:], wd_ref.at[wide:]), fetch(11, b0_any, b0_ref.at[:ROWS, :wide]),
        fetch(12, h1_any, fa_ref.at[:ROWS]), fetch(4, x_any, x_ref), fetch(5, att_any, att_ref), fetch(13, w2_any, wf_ref.at[:, :, :, :early]),
    ]
    links.greet(later=True)

    def weight(start, size):
        return wf_ref[:, :, :, pl.ds(start, size)].reshape(D, size)

    first, second = slice(0, wide), slice(wide, hidden)
    grads = [dg_ref.at[:, :, :, first], du_ref.at[:, :, :, first], dg_ref.at[:, :, :, second], du_ref.at[:, :, :, second],
             db_ref, do_ref] + [wf_ref.at[:, :, :, i * D : (i + 1) * D] for i in range(3)] + [dc_ref]
    totals = [og_ref.at[:, first], ou_ref.at[:, first], og_ref.at[:, second], ou_ref.at[:, second],
              od_ref, oo_ref] + [op_ref.at[:, i * D : (i + 1) * D] for i in range(3)] + [oc_ref]
    tasks = [
        (AcrossFirst if i in ACROSS_FIRST else Reduction)(
            links, grads[i], totals[i], mine_ref if i == kinds - 1 else None,
            crecv[i], yrecv[i], zrecv[i], xrecv[i], stages[i], sems, i,
        )
        for i in range(kinds)
    ]
    for number, i in enumerate(ACROSS_FIRST):
        tasks[i].third, tasks[i].stage_two = extra[2 * number], extra[2 * number + 1]
    returns = (Return(links, y_ref, ry_ref, sems, 0), Return(links, gres_ref, rg_ref, sems, 1))
    gains = gc_ref[...]
    gain = gains[2:3]
    valid = valid_column(tab_ref, rank)
    h1_ref, dv_ref = fa_ref, fa_ref
    tiles = hidden // FF_TILE
    half = tiles // 2
    kept = {}

    def enter():
        for load in load_first:
            load.wait()
        for tile in range(TILES):
            rows = pl.ds(tile * QT, QT)
            gres_ref[rows, :] = (ga_ref[rows, :].astype(F32) * valid[tile * QT : (tile + 1) * QT]).astype(BF16)

    def first_half():
        def step(tile, carry):
            cols = pl.ds(pl.multiple_of(tile * FF_TILE, FF_TILE), FF_TILE)
            back = mm_cols(gres_ref[...], wd_ref[cols, :])
            b1_ref[:ROWS, cols] = (back * b1_ref[:ROWS, cols].astype(F32)).astype(BF16)
            b2_ref[:ROWS, cols] = (back * b2_ref[:ROWS, cols].astype(F32)).astype(BF16)
            return carry

        lax.fori_loop(0, half, step, 0)
        load_products.wait()

    def second_half():
        for load in load_rest:
            load.wait()

        def step(tile, carry):
            at = pl.multiple_of(tile * FF_TILE, FF_TILE)
            cols = pl.ds(at, FF_TILE)
            normed = n_ref[:ROWS, :]
            gate = mm(normed, weight(early - wide + at, FF_TILE))
            up = mm(normed, weight(early + at, FF_TILE))
            back = mm_cols(gres_ref[...], wd_ref[cols, :])
            act, slope = gelu_both(gate)
            b0_ref[:ROWS, cols] = (act * up).astype(BF16)
            b1_ref[:ROWS, cols] = (back * up * slope).astype(BF16)
            b2_ref[:ROWS, cols] = (back * act).astype(BF16)
            return carry

        lax.fori_loop(half, tiles, step, 0)

    def outer_products(ref, right_ref, begin, end):
        def step(tile, carry):
            cols = pl.ds(pl.multiple_of(tile * FF_TILE, FF_TILE), FF_TILE)
            value = mm(ntt_ref[...], right_ref[:ROWS, cols]).astype(BF16)
            ref[:, :, :, cols] = value.reshape(outer, inner, part, FF_TILE)
            return carry

        lax.fori_loop(begin, end, step, 0)

    def down_products():
        def step(tile, carry):
            cols = pl.ds(pl.multiple_of(tile * FF_TILE, FF_TILE), FF_TILE)
            db_ref[tile // inner, tile % inner] = mm_rows(b0_ref[:ROWS, cols], gres_ref[...]).astype(BF16)
            return carry

        lax.fori_loop(0, tiles, step, 0)

    def outward():
        def step(tile, carry):
            cols = pl.ds(pl.multiple_of(tile * group, 128), group)
            value = h1_ref[:ROWS, cols] + mm(b0_ref[:ROWS, :hidden], wd_ref[:, cols])
            y_ref[:, cols] = (value * valid).astype(BF16)
            shards = pl.ds(tile * (4 // inner), 4 // inner)
            total = None
            for number, (ref, low) in enumerate(((b1_ref, 0), (b2_ref, 0), (b1_ref, wide), (b2_ref, wide))):
                at = D + number * wide
                term = mm_cols(
                    ref[:ROWS, low : low + wide], wf_ref[shards, :, :, at : at + wide].reshape(group, wide)
                )
                total = term if total is None else total + term
            gh_ref[:, cols] = total
            return carry

        lax.fori_loop(0, D // group, step, 0)

    def load():
        kept["qkv"] = fetch(14, qkv_any, b1_ref)
        kept["wqkv"] = fetch(15, wqkv_any, b2_ref)

    def middle():
        gain_grad = jnp.zeros((1, D), F32)
        for tile in range(TILES):
            rows = pl.ds(tile * QT, QT)
            value, grad = h1_ref[rows, :], gh_ref[rows, :]
            root = lax.rsqrt(mean_square(value) + EPSILON)
            unit = value * root
            gain_grad = gain_grad + jnp.sum(grad * unit, axis=0, keepdims=True)
            grad = grad * gain
            grad = gres_ref[rows, :].astype(F32) + root * (
                grad - unit * jnp.mean(grad * unit, axis=-1, keepdims=True)
            )
            gh_ref[rows, :] = grad
            low = grad.astype(BF16)
            n_ref[rows, :] = low
            ga_ref[rows, :] = mm_cols(low, weight(0, D)).astype(BF16)
        kept["gain"] = gain_grad

    def out_products():
        def step(tile, carry):
            cols = pl.ds(pl.multiple_of(tile * QUAD, QUAD), QUAD)
            value = mm_rows(att_ref[...], n_ref[:ROWS, cols]).astype(BF16)
            do_ref[:, :, :, cols] = value.reshape(outer, inner, part, QUAD)
            return carry

        lax.fori_loop(0, D // QUAD, step, 0)
        kept["n"] = fetch(6, n_any, n_ref)

    def attention(quad):
        if quad == 0:
            backward_attention_start(dk_ref, dv_ref)
            kept["qkv"].wait()
        backward_attention_quad(tab_ref, rank, b1_ref, att_ref, ga_ref, lse_ref, b0_ref, dk_ref, dv_ref, quad)

    def project_products(quad):
        if quad == 0:
            kept["n"].wait()
        for number in range(3):
            value = mm_rows(n_ref[...], b0_ref[:, number * D + quad * QUAD : number * D + (quad + 1) * QUAD])
            low = (quad * 3 + number) * QUAD
            wf_ref[:, :, :, low : low + QUAD] = value.astype(BF16).reshape(outer, inner, part, QUAD)

    def input_gradient():
        kept["wqkv"].wait()
        kept["one"], kept["side"] = backward_project(
            tab_ref, rank, x_ref, gh_ref, gains, n_ref, b0_ref, b2_ref, dk_ref, gres_ref
        )

    def gain_pieces():
        rows = jnp.concatenate([kept["one"], kept["side"], kept["gain"], jnp.zeros((5, D), F32)], axis=0)
        spread_gain_grads(rows, dc_ref)

    work = {
        "start": lambda: None, "load": load, "P0": enter, "P1a": first_half, "P1b": second_half,
        "gA": lambda: outer_products(dg_ref, b1_ref, 0, half), "gB": lambda: outer_products(dg_ref, b1_ref, half, tiles),
        "uA": lambda: outer_products(du_ref, b2_ref, 0, half), "uB": lambda: outer_products(du_ref, b2_ref, half, tiles),
        "d": down_products, "out": outward, "P4": middle, "P5": out_products,
        "q0": lambda: attention(0), "q1": lambda: attention(1), "q2": lambda: attention(2),
        "p0": lambda: project_products(0), "p1": lambda: project_products(1), "p2": lambda: project_products(2),
        "bp": input_gradient, "dc": gain_pieces,
    }
    paired, begun = set(), set()
    for action, which, *turn in REAR_ORDER:
        if action == "do":
            work[which]()
        elif action == "begin":
            if not begun:
                links.met()
            begun.add(which)
            if which == 6:
                pl.semaphore_wait(free_sem, 1)
            tasks[which].begin()
        elif action == "pair":
            tasks[which].pair()
            paired.add(which)
            if which < 3 and paired >= {0, 1, 2}:
                pl.semaphore_signal(free_sem, inc=1, device_id={"rep": links.mate}, device_id_type=MESH)
        elif action == "meet":
            tasks[which].meet()
        elif action == "col":
            tasks[which].column()
        elif action == "hop":
            tasks[which].hop(turn[0])
        elif action == "cross":
            tasks[which].cross()
        elif action == "fin":
            tasks[which].finish()
        elif action == "rows":
            returns[which].begin()
        else:
            returns[which].relay()
    for one in returns:
        one.settle()
    for task in tasks:
        task.settle()
    links.drain()


def feed_and_reduce(count, table, x, att, lse, gc, cot, n, qkv, wqkv, w2, wf, wd, *firsts):
    outer, inner = grid_of(count)
    part, tall = D // count, wd.shape[1]
    hidden = count * tall
    wf = wf.reshape((outer, inner) + wf.shape[1:])
    w2 = w2.reshape(outer, inner, part, -1)
    full = [(part, hidden), (part, hidden), (tall, D), (part, D), (part, 3 * D), (8, 128)]
    shapes = [(part, hidden // 2)] * 4 + [(tall, D)] + [(part, D)] * 4 + [(8, 128)]
    kinds = len(shapes)
    dtypes = [BF16] * (kinds - 1) + [F32]
    halved = [(a, b // 2 if b % 256 == 0 else b) for a, b in shapes]
    later = [(a // 2, b) if i in ACROSS_FIRST else (a, b) for i, (a, b) in enumerate(halved)]
    dma, vmem = pltpu.SemaphoreType.DMA, pltpu.VMEM
    scratch = [
        vmem((ROWS, D), BF16), vmem((ROWS, D), F32), vmem((ALL_ROWS, D), F32), vmem((ALL_ROWS, D), F32),
        vmem((ALL_ROWS, 3 * D), BF16), vmem((ALL_ROWS, 3 * D), BF16), vmem((D, 3 * D), BF16),
        vmem((ALL_ROWS, D), BF16), vmem((D, ROWS), BF16), vmem((ROWS, D), BF16), vmem((ROWS, D), BF16),
        vmem((ROWS, D), BF16), vmem((ROWS, D), BF16),
        vmem((outer, inner, part, D + 2 * hidden), BF16), vmem((hidden, D), BF16),
    ]
    scratch += [vmem((outer, inner) + shape, BF16) for shape in full[:4]]
    scratch += [vmem((outer, inner) + full[-1], F32)] * 2
    scratch += [vmem((outer, inner) + halved[i], dtypes[i]) for i in (0, 1, 2, 3, 4, 5, 9)]
    for lead in ((outer,), (outer + 1,), ()):
        for i in range(kinds):
            across = (outer, inner) if i in ACROSS_FIRST and lead == () else lead
            scratch.append(vmem(across + later[i], dtypes[i]))
    scratch += [vmem(shape, F32) for shape in later]
    for i in ACROSS_FIRST:
        scratch += [vmem(later[i], BF16), vmem(later[i], F32)]
    one = dma((kinds,))
    scratch += [one, one, one, one, one, dma((2, outer, kinds)), dma((outer + 1, kinds))] + [one] * 9
    scratch += [dma((2, 3)), dma((2, 3)), dma((2,)), dma((1,)), dma((16,)), pltpu.SemaphoreType.REGULAR]
    rows = jax.ShapeDtypeStruct((4, ROWS, D), BF16)
    outs = pl.pallas_call(
        partial(rear_kernel, outer, inner),
        out_shape=tuple(jax.ShapeDtypeStruct(shape, F32) for shape in full) + (rows, rows),
        in_specs=[SMEM] + [ANY] * 2 + [VMEM] * 2 + [ANY] * 13,
        out_specs=(ANY,) * 8,
        scratch_shapes=scratch,
        compiler_params=pltpu.CompilerParams(
            collective_id=2, has_side_effects=True, vmem_limit_bytes=67043328
        ),
        name="feed_and_reduce",
    )(table, x, att, lse, gc, cot, n, qkv, wqkv, w2, wf, wd.reshape(hidden, D), *firsts)
    return outs[:6], outs[6], outs[7]


def place_kernel(part, tab_ref, ry_ref, rg_ref, og_ref, ou_ref, od_ref, oo_ref, op_ref, oc_ref, *refs):
    (y_ref, g_ref, q_out, k_out, v_out, o_out, g_out, u_out, d_out, one_out, side_out, two_out), refs = refs[:12], refs[12:]
    (y_buf, g_buf, zero, bg, bu, bd, bo, bp, sem_in, sem_out, sem_rows, sem_home) = refs
    blocks = y_buf.shape[0]
    base = lax.axis_index("rep") * blocks
    tables = ((og_ref, bg), (ou_ref, bu), (od_ref, bd), (oo_ref, bo), (op_ref, bp))
    reads = [pltpu.make_async_copy(src, dst, sem_in.at[i]) for i, (src, dst) in enumerate(tables)]
    rows = ((ry_ref, y_buf, y_ref), (rg_ref, g_buf, g_ref))

    for read in reads:
        read.start()
    zero[...] = jnp.zeros(zero.shape, zero.dtype)

    def fetch(block, carry):
        index = tab_ref[48, base + block]
        safe = jnp.maximum(index, 0)
        for kind, (src, buf, dst) in enumerate(rows):
            @pl.when(index >= 0)
            def _():
                pltpu.make_async_copy(
                    src.at[lax.div(safe, SLOTS), lax.rem(safe, SLOTS)], buf.at[block], sem_rows.at[kind, block]
                ).start()

            @pl.when(index < 0)
            def _():
                pltpu.make_async_copy(zero, dst.at[block], sem_home.at[kind, block]).start()

        return carry

    lax.fori_loop(0, blocks, fetch, 0)
    for number, out in enumerate((one_out, side_out, two_out)):
        out[...] = oc_ref[number, :part]
    writes = []
    for number, (buf, dst) in enumerate(((bg, g_out), (bu, u_out), (bd, d_out), (bo, o_out))):
        reads[number].wait()
        writes.append(pltpu.make_async_copy(buf, dst, sem_out.at[number]))
        writes[-1].start()
    reads[4].wait()
    for quad in range(D // QUAD):
        for number, dst in enumerate((q_out, k_out, v_out)):
            low = (3 * quad + number) * QUAD
            copy = pltpu.make_async_copy(
                bp.at[:, low : low + QUAD], dst.at[:, quad * QUAD : (quad + 1) * QUAD], sem_out.at[4 + 3 * quad + number]
            )
            copy.start()
            writes.append(copy)
    def leave(block, carry):
        @pl.when(tab_ref[48, base + block] >= 0)
        def _():
            for kind, (src, buf, dst) in enumerate(rows):
                pltpu.make_async_copy(src.at[0, 0], buf.at[block], sem_rows.at[kind, block]).wait()
                pltpu.make_async_copy(buf.at[block], dst.at[block], sem_home.at[kind, block]).start()

        return carry

    lax.fori_loop(0, blocks, leave, 0)
    for write in writes:
        write.wait()

    def rest(block, carry):
        for kind, (_, buf, dst) in enumerate(rows):
            pltpu.make_async_copy(buf.at[block], dst.at[block], sem_home.at[kind, block]).wait()
        return carry

    lax.fori_loop(0, blocks, rest, 0)


def place_all(table, ry, rg, totals, blocks, part, shape):
    out = jax.ShapeDtypeStruct
    og, ou, od, oo, op, oc = totals
    block = (blocks,) + ry.shape[2:]
    dma, vmem = pltpu.SemaphoreType.DMA, pltpu.VMEM
    gain = out((part,), F32)
    y, g, q, k, v, o, gate, up, down, one, side, two = pl.pallas_call(
        partial(place_kernel, part),
        out_shape=(out(block, ry.dtype), out(block, rg.dtype), out(oo.shape, F32), out(oo.shape, F32), out(oo.shape, F32),
                   out(oo.shape, F32), out(og.shape, F32), out(ou.shape, F32), out(od.shape, F32), gain, gain, gain),
        in_specs=[SMEM] + [ANY] * 7 + [VMEM],
        out_specs=(ANY,) * 9 + (VMEM,) * 3,
        scratch_shapes=[vmem(block, ry.dtype), vmem(block, rg.dtype), vmem(block[1:], ry.dtype)] + [vmem(t.shape, F32) for t in totals[:5]]
        + [dma((5,)), dma((13,)), dma((2, blocks)), dma((2, blocks))],
        compiler_params=pltpu.CompilerParams(vmem_limit_bytes=VMEM_LIMIT),
        name="place_outputs",
    )(table, ry, rg, og, ou, od, oo, op, oc)
    return (y.reshape(shape), g.reshape(shape), one, side, q, k, v, o, two, gate, up, down)


def per_device(count, layer_input, cotangent, lengths, attn_gain, global_gain, query_weight, key_weight,
               value_weight, out_weight, ffn_gain, gate_weight, up_weight, down_weight):
    micro, span, width = layer_input.shape
    hidden = gate_weight.shape[1]
    blocks = micro * span // BLK
    part = attn_gain.shape[0]
    rows_in = layer_input.reshape(blocks, BLK, width)
    cots_in = cotangent.reshape(blocks, BLK, width)
    weights = (query_weight, key_weight, value_weight, out_weight, gate_weight, up_weight)
    gains = (attn_gain, global_gain, ffn_gain)
    if grid_of(count)[1] == 2 and part % 16 == 0:
        table, gains, x, cot, n, qkv, att, lse, wqkv, w2, *firsts, ga, gb = gather_and_attend(
            count, lengths, rows_in, cots_in, weights, down_weight, gains
        )
        totals, ry, rg = feed_and_reduce(count, table, x, att, lse, gains, cot, n, qkv, wqkv, w2, ga, gb, *firsts)
        ry, rg = (rows.reshape(4, SLOTS, BLK, width) for rows in (ry, rg))
        return place_all(table, ry, rg, totals, blocks, part, layer_input.shape)
    else:
        table = deal_table(lengths)
        wc = jnp.pad(jnp.stack(gains), ((0, 13), (0, 128 - part)))
        splits = ((0, 4 * width), (4 * width, 2 * hidden))
        ga, gb, gc, rows, cots = gather_weights(
            count, splits, table, rows_in, cots_in, jnp.concatenate(weights, axis=1), down_weight, wc
        )
        x, full = rows.reshape(ROWS, width), ga.reshape(width, -1)
        n, qkv, att, lse = attend(table, x, gc, full)
        y, gh, gatt, dg, du, db, do, gain = feed(
            table, x, cots.reshape(ROWS, width), att, gc, full, gb.reshape(-1, width)
        )
        g, dw, dc = backward_layer(table, x, gh, gatt, att, lse, n, qkv, gain, gc, full)
        grads = [grad.reshape(count, -1, grad.shape[-1]) for grad in (dg, du, db, do, dw, dc)]
        og, ou, ob, oo, ow, oc, ry, rg = reduce_grads(
            count, grads, y.reshape(SLOTS, BLK, width), g.reshape(SLOTS, BLK, width)
        )
        oq, ok, ov = ow[:, :width], ow[:, width : 2 * width], ow[:, 2 * width :]
    y_home, g_home = bring_home(table, ry, rg, blocks)
    return (
        y_home.reshape(layer_input.shape), g_home.reshape(layer_input.shape),
        oc[0, :part], oc[1, :part], oq, ok, ov, oo, oc[2, :part], og, ou, ob,
    )


def solution(mesh):
    rows = P(None, ("rep", "fsdp"), None)
    vector, matrix = P("fsdp"), P("fsdp", None)
    return jax.shard_map(
        partial(per_device, mesh.shape["fsdp"]),
        mesh=mesh,
        in_specs=(rows, rows, P(None, ("rep", "fsdp")), vector, vector, matrix, matrix, matrix, matrix,
                  vector, matrix, matrix, matrix),
        out_specs=(rows, rows, vector, vector, matrix, matrix, matrix, matrix, vector, matrix, matrix, matrix),
        check_vma=False,
    )
```

```python
from functools import partial

import jax
import jax.numpy as jnp
from jax import lax
from jax.experimental import pallas as pl
from jax.experimental.pallas import tpu as pltpu
from jax.sharding import PartitionSpec as P

H = 12
DH = 64
RADIUS = 127
GBLK = 16
BLK = 64
SLOTS = 10
MAX_SEQ_BLOCKS = 5
EPSILON = 1e-06
MASKED_SCORE = -1e30
MESH = pl.DeviceIdType.MESH
VMEM_LIMIT = 60 * 1024 * 1024
SEG_AT, LEN_AT, DEST_AT, TABLE_SIZE = 40, 80, 120, 256

ANY = pl.BlockSpec(memory_space=pl.ANY)
VMEM = pl.BlockSpec(memory_space=pltpu.VMEM)
SMEM = pl.BlockSpec(memory_space=pltpu.SMEM)


def grid_of(count):
    inner = 2 if count <= 8 else 4
    return count // inner, inner


def core_of(rank):
    return rank + 1 - 2 * (rank % 2)


def across_of(rank):
    return (rank + 2) % 4


def lens_kernel(lens_ref, all_ref, send_sem, recv_sem):
    rank = lax.axis_index("rep")
    barrier = pltpu.get_barrier_semaphore()
    for step in range(1, 4):
        pl.semaphore_signal(
            barrier, inc=1, device_id={"rep": (rank + step) % 4}, device_id_type=MESH
        )
    pl.semaphore_wait(barrier, 3)
    copies = []
    for step in range(1, 4):
        copy = pltpu.make_async_remote_copy(
            src_ref=lens_ref,
            dst_ref=all_ref.at[rank],
            send_sem=send_sem.at[step - 1],
            recv_sem=recv_sem.at[step - 1],
            device_id={"rep": (rank + step) % 4},
            device_id_type=MESH,
        )
        copy.start()
        copies.append(copy)
    all_ref[rank] = lens_ref[...]
    for copy in copies:
        copy.wait()


def table_kernel(micro, per_dev, lens_ref, tab_ref, order_ref, count_ref, load_ref):
    total = 4 * micro * per_dev

    def length_at(spot):
        return lens_ref[spot // (micro * per_dev), (spot // per_dev) % micro, spot % per_dev]

    def blocks_of(length):
        return (length + (BLK - 1)) // BLK

    def clear(spot, carry):
        tab_ref[spot] = -1
        return carry

    lax.fori_loop(0, TABLE_SIZE, clear, 0)
    for spot in range(4 * SLOTS):
        tab_ref[LEN_AT + spot] = 0
    for size in range(8):
        count_ref[size] = 0
    for dev in range(4):
        load_ref[dev] = 0

    def tally(spot, carry):
        length = length_at(spot)

        @pl.when(length > 0)
        def _():
            size = blocks_of(length)
            count_ref[size] = count_ref[size] + 1

        return carry

    lax.fori_loop(0, total, tally, 0)
    begin = 0
    for size in range(MAX_SEQ_BLOCKS, 0, -1):
        amount = count_ref[size]
        count_ref[size] = begin
        begin = begin + amount

    def place(spot, carry):
        length = length_at(spot)

        @pl.when(length > 0)
        def _():
            size = blocks_of(length)
            where = count_ref[size]
            order_ref[where] = spot
            count_ref[size] = where + 1

        return carry

    lax.fori_loop(0, total, place, 0)

    def assign(number, carry):
        spot = order_ref[number]
        length = length_at(spot)
        size = blocks_of(length)
        best = jnp.int32(0)
        low = load_ref[0]
        for dev in range(1, 4):
            here = load_ref[dev]
            best = jnp.where(here < low, dev, best)
            low = jnp.minimum(here, low)
        load_ref[best] = low + size

        def put(step, inner):
            slot = best * SLOTS + low + step
            tab_ref[slot] = spot + step
            tab_ref[SEG_AT + slot] = low
            tab_ref[LEN_AT + slot] = jnp.minimum(length - BLK * step, BLK)
            tab_ref[DEST_AT + spot + step] = slot
            return inner

        lax.fori_loop(0, size, put, 0)
        return carry

    lax.fori_loop(0, begin, assign, 0)


def deal_table(lengths):
    micro, per_dev = lengths.shape
    padded = jnp.pad(lengths, ((0, 8 - micro), (0, 128 - per_dev)))
    everyone = pl.pallas_call(
        lens_kernel,
        out_shape=jax.ShapeDtypeStruct((4, 8, 128), jnp.int32),
        in_specs=[VMEM],
        out_specs=VMEM,
        scratch_shapes=[pltpu.SemaphoreType.DMA((3,)), pltpu.SemaphoreType.DMA((3,))],
        compiler_params=pltpu.CompilerParams(collective_id=0, has_side_effects=True),
        name="lens_exchange",
    )(padded)
    return pl.pallas_call(
        partial(table_kernel, micro, per_dev),
        out_shape=jax.ShapeDtypeStruct((TABLE_SIZE,), jnp.int32),
        in_specs=[SMEM],
        out_specs=SMEM,
        scratch_shapes=[
            pltpu.SMEM((4 * micro * per_dev,), jnp.int32),
            pltpu.SMEM((8,), jnp.int32),
            pltpu.SMEM((4,), jnp.int32),
        ],
        name="deal_table",
    )(everyone)


def gather_kernel(
    outer, inner, splits, tab_ref, rows_ref, cots_ref, wa_ref, wb_ref, wc_ref,
    ga_ref, gb_ref, gc_ref, rows_out, cots_out,
    psend, precv, xsend, xrecv,
    z_send, z_recv, y_send, y_recv, c_send, c_recv, own_sem,
    p_send, p_recv, x_send, x_recv,
):
    rank = lax.axis_index("rep")
    spot = lax.axis_index("fsdp")
    core = rank % 2
    row, col = spot // inner, spot % inner
    count = outer * inner
    mate, across = core_of(rank), across_of(rank)
    pieces = [(wa_ref, ga_ref, start, width // 2) for start, width in splits]
    pieces.append((wb_ref, gb_ref, 0, wb_ref.shape[1] // 2))
    pieces.append((wc_ref, gc_ref, 0, None))
    halved = [number for number, piece in enumerate(pieces) if piece[3] is not None]

    barrier = pltpu.get_barrier_semaphore()
    neighbours = (
        (row + 1 < outer, {"fsdp": spot + inner}),
        (row > 0, {"fsdp": spot - inner}),
        (col + 1 < inner, {"fsdp": spot + 1}),
        (col > 0, {"fsdp": spot - 1}),
    )
    amount = jnp.int32(2)
    for there, device in neighbours:
        amount = amount + there.astype(jnp.int32)

        @pl.when(there)
        def _():
            pl.semaphore_signal(barrier, inc=1, device_id=device, device_id_type=MESH)

    for device in (mate, across):
        pl.semaphore_signal(barrier, inc=1, device_id={"rep": device}, device_id_type=MESH)
    pl.semaphore_wait(barrier, amount)

    def cut(ref, number):
        _, _, start, half = pieces[number]
        if half is None:
            return ref
        return ref.at[:, pl.ds(pl.multiple_of(start + core * half, 128), half)]

    def landed(number, shard):
        return cut(pieces[number][1].at[shard], number)

    late = []

    def send(there, src, dst, ssem, rsem, device):
        def describe():
            return pltpu.make_async_remote_copy(
                src_ref=src, dst_ref=dst, send_sem=ssem, recv_sem=rsem,
                device_id=device, device_id_type=MESH,
            )

        if there is None:
            describe().start()
            late.append((None, lambda: describe().wait_send()))
        else:
            @pl.when(there)
            def _():
                describe().start()

            late.append((there, lambda: describe().wait_send()))

    def arrive(number, shard, rsem):
        pltpu.make_async_remote_copy(
            src_ref=landed(number, shard), dst_ref=landed(number, shard),
            send_sem=own_sem.at[0], recv_sem=rsem,
            device_id={"rep": mate}, device_id_type=MESH,
        ).wait_recv()

    def both(first, second):
        return second if first is None else jnp.logical_and(first, second)

    def to_mate(there, number, shard):
        if number not in halved:
            return
        place = landed(number, shard)
        send(there, place, place, c_send.at[number, shard], c_recv.at[number, shard], {"rep": mate})

    def along_row(there, number, line, src):
        shard = line * inner + col
        place = landed(number, shard)
        src = place if src is None else src
        send(both(there, col + 1 < inner), src, place,
             y_send.at[0, 0, line, number], y_recv.at[0, 0, line, number], {"fsdp": spot + 1})
        send(both(there, col > 0), src, place,
             y_send.at[1, 0, line, number], y_recv.at[1, 0, line, number], {"fsdp": spot - 1})

    def from_row(there, number, line):
        for step in range(inner - 1):
            for way, source, onward, target in (
                (0, col - 1 - step, col + 1 < inner, spot + 1),
                (1, col + 1 + step, col > 0, spot - 1),
            ):
                here = jnp.logical_and(source >= 0, source < inner)
                here = both(there, here)
                shard = line * inner + source

                @pl.when(here)
                def _():
                    arrive(number, shard, y_recv.at[way, step, line, number])

                if step + 1 < inner - 1:
                    place = landed(number, shard)
                    send(both(here, onward), place, place,
                         y_send.at[way, step + 1, line, number],
                         y_recv.at[way, step + 1, line, number], {"fsdp": target})
                to_mate(here, number, shard)

    for number, piece in enumerate(pieces):
        src, place = cut(piece[0], number), landed(number, spot)
        send(row + 1 < outer, src, place, z_send.at[0, 0, number], z_recv.at[0, 0, number],
             {"fsdp": spot + inner})
        send(row > 0, src, place, z_send.at[1, 0, number], z_recv.at[1, 0, number],
             {"fsdp": spot - inner})
        along_row(None, number, row, src)
    own = [
        pltpu.make_async_copy(wa_ref, ga_ref.at[spot], own_sem.at[0]),
        pltpu.make_async_copy(wb_ref, gb_ref.at[spot], own_sem.at[1]),
        pltpu.make_async_copy(wc_ref, gc_ref.at[spot], own_sem.at[2]),
    ]
    for copy in own:
        copy.start()

    sources = (rows_ref, cots_ref)
    per_rank = rows_ref.shape[0]

    def picked(kind, target, slot):
        index = tab_ref[target * SLOTS + slot] - rank * per_rank
        mine = jnp.logical_and(index >= 0, index < per_rank)
        value = sources[kind][jnp.clip(index, 0, per_rank - 1)]
        return mine, value

    def mate_copy(kind, part):
        return pltpu.make_async_remote_copy(
            src_ref=psend.at[kind, part], dst_ref=precv.at[kind, part],
            send_sem=p_send.at[kind, part], recv_sem=p_recv.at[kind, part],
            device_id={"rep": mate}, device_id_type=MESH,
        )

    def across_copy(kind):
        return pltpu.make_async_remote_copy(
            src_ref=xsend.at[kind], dst_ref=xrecv.at[kind],
            send_sem=x_send.at[kind], recv_sem=x_recv.at[kind],
            device_id={"rep": across}, device_id_type=MESH,
        )

    for kind, part in ((0, 1), (1, 1), (0, 0), (1, 0)):
        target = mate if part == 0 else across_of(mate)

        def pack(slot, carry):
            mine, value = picked(kind, target, slot)
            psend[kind, part, slot] = jnp.where(mine, value, jnp.zeros_like(value))
            return carry

        lax.fori_loop(0, SLOTS, pack, 0)
        mate_copy(kind, part).start()
    for kind in range(2):
        mate_copy(kind, 1).wait_recv()

        def merge(slot, carry):
            mine, value = picked(kind, across, slot)
            xsend[kind, slot] = jnp.where(mine, value, precv[kind, 1, slot])
            return carry

        lax.fori_loop(0, SLOTS, merge, 0)
        across_copy(kind).start()

    def lines(step):
        return ((row - 1 - step >= 0, row - 1 - step, 0, row + 1 < outer, spot + inner),
                (row + 1 + step < outer, row + 1 + step, 1, row > 0, spot - inner))

    for step in range(outer - 1):
        for number in range(len(pieces)):
            for here, line, way, onward, target in lines(step):
                shard = line * inner + col

                @pl.when(here)
                def _():
                    arrive(number, shard, z_recv.at[way, step, number])

                if step + 1 < outer - 1:
                    place = landed(number, shard)
                    send(jnp.logical_and(here, onward), place, place,
                         z_send.at[way, step + 1, number], z_recv.at[way, step + 1, number],
                         {"fsdp": target})
                along_row(here, number, line, None)
                to_mate(here, number, shard)
        for number in range(len(pieces)):
            if step == 0:
                from_row(None, number, row)
            else:
                for here, line, *_ in lines(step - 1):
                    from_row(here, number, line)
    for number in range(len(pieces)):
        for here, line, *_ in lines(outer - 2):
            from_row(here, number, line)

    outs = (rows_out, cots_out)
    for kind in range(2):
        mate_copy(kind, 0).wait_recv()
        across_copy(kind).wait_recv()

        def finish(slot, carry):
            mine, value = picked(kind, rank, slot)
            outs[kind][slot] = jnp.where(mine, value, precv[kind, 0, slot] + xrecv[kind, slot])
            return carry

        lax.fori_loop(0, SLOTS, finish, 0)

    for shard in range(count):
        @pl.when(shard != spot)
        def _():
            for number in halved:
                other = pieces[number]
                view = other[1].at[shard].at[:, pl.ds(0, other[3])]
                pltpu.make_async_remote_copy(
                    src_ref=view, dst_ref=view, send_sem=own_sem.at[0],
                    recv_sem=c_recv.at[number, shard],
                    device_id={"rep": mate}, device_id_type=MESH,
                ).wait_recv()
    for there, finish_send in late:
        if there is None:
            finish_send()
        else:
            pl.when(there)(finish_send)
    for kind in range(2):
        for part in range(2):
            mate_copy(kind, part).wait_send()
        across_copy(kind).wait_send()
    for copy in own:
        copy.wait()


def gather_weights(count, splits, table, rows, cots, wa, wb, wc):
    outer, inner = grid_of(count)
    block = rows.shape[1:]
    kinds = len(splits) + 2
    dma = pltpu.SemaphoreType.DMA
    bf16 = jnp.bfloat16
    return pl.pallas_call(
        partial(gather_kernel, outer, inner, splits),
        out_shape=(
            jax.ShapeDtypeStruct((count,) + wa.shape, bf16),
            jax.ShapeDtypeStruct((count,) + wb.shape, bf16),
            jax.ShapeDtypeStruct((count,) + wc.shape, bf16),
            jax.ShapeDtypeStruct((SLOTS,) + block, bf16),
            jax.ShapeDtypeStruct((SLOTS,) + block, bf16),
        ),
        in_specs=[SMEM, VMEM, VMEM, VMEM, VMEM, VMEM],
        out_specs=(ANY, ANY, ANY, VMEM, VMEM),
        scratch_shapes=[
            pltpu.VMEM((2, 2, SLOTS) + block, bf16),
            pltpu.VMEM((2, 2, SLOTS) + block, bf16),
            pltpu.VMEM((2, SLOTS) + block, bf16),
            pltpu.VMEM((2, SLOTS) + block, bf16),
            dma((2, outer - 1, kinds)), dma((2, outer - 1, kinds)),
            dma((2, inner - 1, outer, kinds)), dma((2, inner - 1, outer, kinds)),
            dma((kinds, count)), dma((kinds, count)), dma((3,)),
            dma((2, 2)), dma((2, 2)), dma((2,)), dma((2,)),
        ],
        compiler_params=pltpu.CompilerParams(
            collective_id=1, has_side_effects=True, vmem_limit_bytes=VMEM_LIMIT
        ),
        name="gather_and_deal",
    )(table, rows, cots, wa, wb, wc)


def reduce_kernel(
    outer, inner, kinds, *refs
):
    grads, (y_ref, g_ref) = refs[:kinds], refs[kinds : kinds + 2]
    totals, (ry_ref, rg_ref) = refs[kinds + 2 : 2 * kinds + 2], refs[2 * kinds + 2 : 2 * kinds + 4]
    scratch = refs[2 * kinds + 4 :]
    mines, crecvs, yrecvs, zrecvs, xrecvs = (
        scratch[kinds * i : kinds * (i + 1)] for i in range(5)
    )
    (c_send, c_recv, m_sem, y_send, y_recv, z_send, z_recv, x_send, x_recv, f_send, f_recv,
     r_send, r_recv, q_sem) = scratch[5 * kinds :]
    rank = lax.axis_index("rep")
    spot = lax.axis_index("fsdp")
    core = rank % 2
    row, col = spot // inner, spot % inner
    mate, across = core_of(rank), across_of(rank)
    pieces = [(src, dst, 0, src.shape[3] // 2) for src, dst in zip(grads[:-1], totals)]
    pieces.append((grads[-1], totals[-1], 0, None))

    barrier = pltpu.get_barrier_semaphore()
    neighbours = (
        (row + 1 < outer, {"fsdp": spot + inner}),
        (row > 0, {"fsdp": spot - inner}),
        (col + 1 < inner, {"fsdp": spot + 1}),
        (col > 0, {"fsdp": spot - 1}),
    )
    amount = jnp.int32(2)
    for there, device in neighbours:
        amount = amount + there.astype(jnp.int32)

        @pl.when(there)
        def _():
            pl.semaphore_signal(barrier, inc=1, device_id=device, device_id_type=MESH)

    for device in (mate, across):
        pl.semaphore_signal(barrier, inc=1, device_id={"rep": device}, device_id_type=MESH)
    pl.semaphore_wait(barrier, amount)

    late = []

    def send(there, src, dst, ssem, rsem, device):
        def describe():
            return pltpu.make_async_remote_copy(
                src_ref=src, dst_ref=dst, send_sem=ssem, recv_sem=rsem,
                device_id=device, device_id_type=MESH,
            )

        if there is None:
            describe().start()
            late.append((None, lambda: describe().wait_send()))
        else:
            @pl.when(there)
            def _():
                describe().start()

            late.append((there, lambda: describe().wait_send()))

    def arrive(place, rsem):
        pltpu.make_async_remote_copy(
            src_ref=place, dst_ref=place, send_sem=q_sem.at[0], recv_sem=rsem,
            device_id={"rep": mate}, device_id_type=MESH,
        ).wait_recv()

    def columns(ref, number, which):
        _, _, start, half = pieces[number]
        if half is None:
            return ref
        cols = pl.ds(pl.multiple_of(start + which * half, 128), half)
        return ref.at[:, :, :, cols] if len(ref.shape) == 4 else ref.at[:, cols]

    order = list(range(kinds))
    loads = []
    for number in order:
        src = columns(pieces[number][0], number, 1 - core)
        send(None, src, crecvs[number], c_send.at[number], c_recv.at[number], {"rep": mate})
        load = pltpu.make_async_copy(
            columns(pieces[number][0], number, core), mines[number], m_sem.at[number]
        )
        load.start()
        loads.append(load)

    for kind, (src, dst) in enumerate(((y_ref, ry_ref), (g_ref, rg_ref))):
        send(None, src, dst.at[rank], r_send.at[kind, 0], r_recv.at[kind, 0], {"rep": across})
        send(None, src, dst.at[rank], r_send.at[kind, 1], r_recv.at[kind, 1], {"rep": mate})
        pltpu.make_async_copy(src, dst.at[rank], q_sem.at[kind + 1]).start()

    def slot_of(way, size, place, dest):
        if size == 2:
            return 0
        return dest - place if way == 0 else size - place + dest

    def line_sum(number, size, place, stride, buffer, view, ssem, rsem):
        for far in range(size - 1, 0, -1):
            for way in range(2):
                dest = far if way == 0 else size - 1 - far
                step = 1 if way == 0 else -1
                passes = place < dest if way == 0 else place > dest
                first = place == 0 if way == 0 else place == size - 1
                mine = view(dest)
                got = slot_of(way, size, place, dest)

                @pl.when(jnp.logical_and(passes, jnp.logical_not(first)))
                def _():
                    arrive(buffer.at[got], rsem.at[got, number])
                    mine[...] = mine[...] + buffer[got]

                put = slot_of(way, size, place + step, dest)
                send(passes, mine, buffer.at[put], ssem.at[way, dest, number], rsem.at[put, number],
                     {"fsdp": spot + step * stride})
        for way in range(2):
            has = place > 0 if way == 0 else place < size - 1
            got = slot_of(way, size, place, place)
            mine = view(place)

            @pl.when(has)
            def _():
                arrive(buffer.at[got], rsem.at[got, number])
                mine[...] = mine[...] + buffer[got]

    for number in order:
        loads[number].wait()
        arrive(crecvs[number], c_recv.at[number])
        mine, other = mines[number], crecvs[number]

        def add(index, carry):
            mine[index // inner, index % inner] = (
                mine[index // inner, index % inner] + other[index // inner, index % inner]
            )
            return carry

        lax.fori_loop(0, outer * inner, add, 0)
        if inner == 2:
            send(None, mine.at[:, 1 - col], yrecvs[number].at[0], y_send.at[0, 0, number],
                 y_recv.at[0, number], {"fsdp": spot + 1 - 2 * col})
    for kind, dst in enumerate((ry_ref, rg_ref)):
        place = dst.at[across]
        arrive(place, r_recv.at[kind, 0])
        send(None, place, place, r_send.at[kind, 2], r_recv.at[kind, 2], {"rep": mate})
    for number in order:
        mine = mines[number]
        if inner == 2:
            arrive(yrecvs[number].at[0], y_recv.at[0, number])
            buffer = yrecvs[number]

            def add(index, carry):
                mine[index, col] = mine[index, col] + buffer[0, index]
                return carry

            lax.fori_loop(0, outer, add, 0)
        else:
            line_sum(number, inner, col, 1, yrecvs[number], lambda dest: mine.at[:, dest],
                     y_send, y_recv)
        line_sum(number, outer, row, inner, zrecvs[number], lambda dest: mine.at[dest, col],
                 z_send, z_recv)
        send(None, mine.at[row, col], xrecvs[number], x_send.at[number], x_recv.at[number],
             {"rep": across})
    for number in order:
        arrive(xrecvs[number], x_recv.at[number])
        total = mines[number][row, col].astype(jnp.float32) + xrecvs[number][...].astype(jnp.float32)
        out, half = pieces[number][1], pieces[number][3]
        place = columns(out, number, core)
        place[...] = total
        if half is not None:
            send(None, place, place, f_send.at[number], f_recv.at[number], {"rep": mate})
    for number in order:
        if pieces[number][3] is not None:
            arrive(columns(pieces[number][1], number, 1 - core), f_recv.at[number])
    for kind, dst in enumerate((ry_ref, rg_ref)):
        arrive(dst.at[mate], r_recv.at[kind, 1])
        arrive(dst.at[across_of(mate)], r_recv.at[kind, 2])
        src = y_ref if kind == 0 else g_ref
        pltpu.make_async_copy(src, dst.at[rank], q_sem.at[kind + 1]).wait()
    for there, finish_send in late:
        if there is None:
            finish_send()
        else:
            pl.when(there)(finish_send)


def reduce_grads(count, grads, y_rows, g_rows):
    outer, inner = grid_of(count)
    kinds = len(grads)
    shapes = [(grad.shape[1], grad.shape[2] // 2, grad.dtype) for grad in grads[:-1]]
    shapes.append(grads[-1].shape[1:] + (grads[-1].dtype,))
    dma = pltpu.SemaphoreType.DMA
    y_slots = 1 if inner == 2 else inner + 1
    z_slots = 1 if outer == 2 else outer + 1
    scratch = []
    for lead in ((outer, inner), (outer, inner), (y_slots, outer), (z_slots,), ()):
        scratch += [pltpu.VMEM(lead + (a, b), dtype) for a, b, dtype in shapes]
    scratch += [
        dma((kinds,)), dma((kinds,)), dma((kinds,)),
        dma((2, inner, kinds)), dma((y_slots, kinds)),
        dma((2, outer, kinds)), dma((z_slots, kinds)),
        dma((kinds,)), dma((kinds,)), dma((kinds,)), dma((kinds,)),
        dma((2, 3)), dma((2, 3)), dma((3,)),
    ]
    return pl.pallas_call(
        partial(reduce_kernel, outer, inner, kinds),
        out_shape=tuple(jax.ShapeDtypeStruct(grad.shape[1:], jnp.float32) for grad in grads) + (
            jax.ShapeDtypeStruct((4,) + y_rows.shape, y_rows.dtype),
            jax.ShapeDtypeStruct((4,) + g_rows.shape, g_rows.dtype),
        ),
        in_specs=[ANY] * (kinds + 2),
        out_specs=(VMEM,) * kinds + (ANY, ANY),
        scratch_shapes=scratch,
        compiler_params=pltpu.CompilerParams(
            collective_id=2, has_side_effects=True, vmem_limit_bytes=VMEM_LIMIT
        ),
        name="reduce_and_return",
    )(*(grad.reshape((outer, inner) + grad.shape[1:]) for grad in grads), y_rows, g_rows)


def home_kernel(tab_ref, ry_ref, rg_ref, y_ref, g_ref):
    base = lax.axis_index("rep") * y_ref.shape[0]

    def fetch(block, carry):
        index = tab_ref[DEST_AT + base + block] if len(tab_ref.shape) == 1 else tab_ref[48, base + block]
        safe = jnp.maximum(index, 0)
        for src, dst in ((ry_ref, y_ref), (rg_ref, g_ref)):
            value = src[safe // SLOTS, safe % SLOTS]
            dst[block] = jnp.where(index >= 0, value, jnp.zeros_like(value))
        return carry

    lax.fori_loop(0, y_ref.shape[0], fetch, 0)


def bring_home(table, ry, rg, blocks):
    shape = jax.ShapeDtypeStruct((blocks,) + ry.shape[2:], ry.dtype)
    return pl.pallas_call(
        home_kernel,
        out_shape=(shape, shape),
        in_specs=[SMEM, VMEM, VMEM],
        out_specs=(VMEM, VMEM),
        compiler_params=pltpu.CompilerParams(vmem_limit_bytes=VMEM_LIMIT),
        name="place_rows",
    )(table, ry, rg)


D = H * DH
ROWS = SLOTS * BLK
SIDES = SLOTS * (BLK // GBLK)
SIDE_ROWS = 48
ALL_ROWS = ROWS + SIDE_ROWS
QT = 128
WIN = 384
TILES = ROWS // QT
QUAD = 256
FF_TILE = 256
GELU_C = 0.7978845608028654
GELU_A = 0.044715
F32, BF16 = jnp.float32, jnp.bfloat16


def mm(left, right):
    return lax.dot_general(left, right, (((1,), (0,)), ((), ())), preferred_element_type=F32)


def mm_cols(left, right):
    return lax.dot_general(left, right, (((1,), (1,)), ((), ())), preferred_element_type=F32)


def mm_rows(left, right):
    return lax.dot_general(left, right, (((0,), (0,)), ((), ())), preferred_element_type=F32)


def iota(shape, axis):
    return lax.broadcasted_iota(jnp.int32, shape, axis)


def pick_by(index, values, other):
    out = jnp.full(index.shape, other, jnp.int32)
    for number, value in enumerate(values):
        out = jnp.where(index == number, value, out)
    return out


def block_at(tab_ref, slot):
    return lax.rem(tab_ref[slot, 0], 128) - 1


def seg_at(tab_ref, slot):
    if len(tab_ref.shape) == 1:
        return tab_ref[SEG_AT + slot]
    return lax.div(tab_ref[slot, 0], 16384) - 1


def len_at(tab_ref, slot):
    if len(tab_ref.shape) == 1:
        return tab_ref[LEN_AT + slot]
    return lax.rem(lax.div(tab_ref[slot, 0], 128), 128)


def slot_info(tab_ref, rank):
    seg = [seg_at(tab_ref, rank * SLOTS + slot) for slot in range(SLOTS)]
    length = [len_at(tab_ref, rank * SLOTS + slot) for slot in range(SLOTS)]
    return seg, length


def valid_column(tab_ref, rank):
    _, length = slot_info(tab_ref, rank)
    row = iota((ROWS, 1), 0)
    return ((row % BLK) < pick_by(row // BLK, length, 0)).astype(F32)


def pooling(tab_ref, rank):
    _, length = slot_info(tab_ref, rank)
    row = iota((1, ROWS), 1)
    block = jnp.where((row % BLK) < pick_by(row // BLK, length, 0), row // GBLK, -1)
    return jnp.where(iota((SIDE_ROWS, ROWS), 0) == block, 1.0, 0.0).astype(BF16)


def key_segments(tab_ref, rank, first_block, index):
    blocks = WIN // BLK
    base = rank * SLOTS + first_block
    seg = [seg_at(tab_ref, base + step) for step in range(blocks)]
    length = [len_at(tab_ref, base + step) for step in range(blocks)]
    alive = (index % BLK) < pick_by(index // BLK, length, 0)
    return jnp.where(alive, pick_by(index // BLK, seg, -2), -2)


def side_segments(tab_ref, rank, index):
    seg, length = slot_info(tab_ref, rank)
    per = BLK // GBLK
    alive = (index % per) * GBLK < pick_by(index // per, length, 0)
    return jnp.where(alive, pick_by(index // per, seg, -2), -2)


def tile_bias(tab_ref, rank, tile, first_row, keys_axis):
    qs, ks, gs = ((QT, 1), (1, WIN), (1, SIDE_ROWS)) if keys_axis == 1 else ((1, QT), (WIN, 1), (SIDE_ROWS, 1))
    q_index = iota(qs, 1 - keys_axis)
    k_index = iota(ks, keys_axis)
    g_index = iota(gs, keys_axis)
    base = rank * SLOTS + tile * (QT // BLK)
    q_seg = pick_by(q_index // BLK, [seg_at(tab_ref, base + step) for step in range(QT // BLK)], -1)
    k_seg = key_segments(tab_ref, rank, first_row // BLK, k_index)
    g_seg = side_segments(tab_ref, rank, g_index)
    gap = (q_index + tile * QT) - (k_index + first_row)
    local = (jnp.abs(gap) <= RADIUS) & (q_seg == k_seg)
    return jnp.where(local, 0.0, MASKED_SCORE), jnp.where(q_seg == g_seg, 0.0, MASKED_SCORE)


def window_start(tile):
    return pl.multiple_of(jnp.clip(tile - 1, 0, TILES - WIN // QT) * QT, QT)


def head_stack(rows):
    lane = iota(rows.shape, 1) // DH
    zero = jnp.zeros_like(rows)
    return jnp.concatenate([jnp.where(lane == head, rows, zero) for head in range(QUAD // DH)], axis=0)


def head_merge(stacked):
    lane = iota((QT, QUAD), 1) // DH
    out = stacked[:QT]
    for head in range(1, QUAD // DH):
        out = jnp.where(lane == head, stacked[head * QT : (head + 1) * QT], out)
    return out


def gains_of(gc_ref):
    count = gc_ref.shape[0]
    part = D // count
    lane, column = iota((128, D), 0), iota((128, D), 1)
    total = None
    for shard in range(count):
        pick = jnp.where((column == lane + shard * part) & (lane < part), 1.0, 0.0).astype(BF16)
        term = mm(gc_ref[shard], pick)
        total = term if total is None else total + term
    return total


def three_way(value):
    high = value.astype(BF16)
    rest = value - high.astype(F32)
    middle = rest.astype(BF16)
    return high, middle, (rest - middle.astype(F32)).astype(BF16)


def spread_gain_grads(value, dc_ref):
    count = dc_ref.shape[0] if len(dc_ref.shape) == 3 else dc_ref.shape[0] * dc_ref.shape[1]
    part = D // count
    column, lane = iota((D, 128), 0), iota((D, 128), 1)
    parts = three_way(value)
    for shard in range(count):
        pick = jnp.where((column == lane + shard * part) & (lane < part), 1.0, 0.0).astype(BF16)
        place = dc_ref.at[shard] if len(dc_ref.shape) == 3 else dc_ref.at[shard // dc_ref.shape[1], shard % dc_ref.shape[1]]
        place[...] = mm(parts[0], pick) + mm(parts[1], pick) + mm(parts[2], pick)


def mean_square(value):
    return jnp.mean(value * value, axis=-1, keepdims=True)


def forward_norm(tab_ref, rank, x_ref, gains, n_ref):
    for tile in range(TILES):
        rows = pl.ds(tile * QT, QT)
        value = x_ref[rows, :].astype(F32)
        n_ref[rows, :] = (value * lax.rsqrt(mean_square(value) + EPSILON) * gains[0:1]).astype(BF16)
    side = mm(pooling(tab_ref, rank), n_ref[:ROWS, :])
    n_ref[ROWS:, :] = (side * lax.rsqrt(mean_square(side) + EPSILON) * gains[1:2]).astype(BF16)


def forward_project(n_ref, w_ref, qkv_ref):
    def step(tile, carry):
        cols = pl.ds(pl.multiple_of(tile * QUAD, QUAD), QUAD)
        qkv_ref[:, cols] = mm(n_ref[...], w_ref[:, cols]).astype(BF16)
        return carry

    lax.fori_loop(0, 3 * D // QUAD, step, 0)


def forward_attention(tab_ref, rank, qkv_ref, att_ref, lse_ref, begin, end):
    heads = QUAD // DH

    def step(tile, carry):
        first = window_start(tile)
        bias, side_bias = tile_bias(tab_ref, rank, tile, first, 1)
        rows = pl.ds(pl.multiple_of(tile * QT, QT), QT)
        window = pl.ds(first, WIN)
        lane = iota((QT, 128), 1)

        def four(quad, lse):
            low = pl.multiple_of(quad * QUAD, QUAD)
            cols, key_cols, value_cols = (pl.ds(low + number * D, QUAD) for number in range(3))
            query = head_stack(qkv_ref[rows, cols])
            scores = mm_cols(query, qkv_ref[window, key_cols])
            side_scores = mm_cols(query, qkv_ref[ROWS:, key_cols])
            local, sides, scale = [], [], []
            for head in range(heads):
                part = slice(head * QT, (head + 1) * QT)
                one = scores[part] + bias
                two = side_scores[part] + side_bias
                peak = jnp.maximum(
                    jnp.max(one, axis=-1, keepdims=True), jnp.max(two, axis=-1, keepdims=True)
                )
                one, two = jnp.exp(one - peak), jnp.exp(two - peak)
                total = jnp.sum(one, axis=-1, keepdims=True) + jnp.sum(two, axis=-1, keepdims=True)
                local.append(one.astype(BF16))
                sides.append(two.astype(BF16))
                scale.append(1.0 / total)
                lse = jnp.where(lane == quad * heads + head, peak + jnp.log(total), lse)
            mixed = mm(jnp.concatenate(local, axis=0), qkv_ref[window, value_cols])
            mixed = mixed + mm(jnp.concatenate(sides, axis=0), qkv_ref[ROWS:, value_cols])
            mixed = mixed * jnp.concatenate(scale, axis=0)
            att_ref[rows, cols] = head_merge(mixed).astype(BF16)
            return lse

        lse = lax.fori_loop(0, D // QUAD, four, jnp.zeros((QT, 128), F32))
        lse_ref[tile] = jnp.transpose(lse)[:16]
        return carry

    lax.fori_loop(begin, end, step, 0)


def feed_forward(tab_ref, rank, x_ref, cot_ref, att_ref, gains, w_ref, wb_ref,
                 y_ref, gh_ref, ga_ref, dg_ref, du_ref, db_ref, do_ref,
                 h1_ref, nt_ref, ntt_ref, gres_ref, h2_ref, gg_ref, gu_ref, gn_ref):
    hidden = wb_ref.shape[0]
    gate_at = w_ref.shape[1] - 2 * hidden
    out_at = gate_at - D
    valid = valid_column(tab_ref, rank)
    gain = gains[2:3]
    for tile in range(TILES):
        rows = pl.ds(tile * QT, QT)
        value = x_ref[rows, :].astype(F32) + mm(att_ref[rows, :], w_ref[:, out_at:gate_at])
        h1_ref[rows, :] = value
        normed = (value * lax.rsqrt(mean_square(value) + EPSILON) * gain).astype(BF16)
        nt_ref[rows, :] = normed
        ntt_ref[:, tile * QT : (tile + 1) * QT] = jnp.transpose(normed)
        gres_ref[rows, :] = (cot_ref[rows, :].astype(F32) * valid[tile * QT : (tile + 1) * QT]).astype(BF16)

    def inward(tile, carry):
        at = pl.multiple_of(tile * FF_TILE, FF_TILE)
        cols = pl.ds(at, FF_TILE)
        gate = mm(nt_ref[...], w_ref[:, pl.ds(gate_at + at, FF_TILE)])
        up = mm(nt_ref[...], w_ref[:, pl.ds(gate_at + hidden + at, FF_TILE)])
        back = mm_cols(gres_ref[...], wb_ref[cols, :])
        square = gate * gate
        bend = jnp.tanh(GELU_C * (gate * (1.0 + GELU_A * square)))
        half = 0.5 * (1.0 + bend)
        act = gate * half
        slope = half + (0.5 * GELU_C) * gate * (1.0 - bend * bend) * (1.0 + (3.0 * GELU_A) * square)
        h2_ref[:, cols] = (act * up).astype(BF16)
        gg_ref[:, cols] = (back * up * slope).astype(BF16)
        gu_ref[:, cols] = (back * act).astype(BF16)
        return carry

    lax.fori_loop(0, hidden // FF_TILE, inward, 0)

    def outward(tile, carry):
        cols = pl.ds(pl.multiple_of(tile * QUAD, QUAD), QUAD)
        value = h1_ref[:, cols] + mm(h2_ref[...], wb_ref[:, cols])
        y_ref[:, cols] = (value * valid).astype(BF16)
        gn_ref[:, cols] = mm_cols(gg_ref[...], w_ref[cols, gate_at : gate_at + hidden]) + mm_cols(
            gu_ref[...], w_ref[cols, gate_at + hidden :]
        )
        return carry

    lax.fori_loop(0, D // QUAD, outward, 0)

    def weights(tile, carry):
        at = pl.multiple_of(tile * FF_TILE, FF_TILE)
        cols = pl.ds(at, FF_TILE)
        dg_ref[:, cols] = mm(ntt_ref[...], gg_ref[:, cols]).astype(BF16)
        du_ref[:, cols] = mm(ntt_ref[...], gu_ref[:, cols]).astype(BF16)
        db_ref[cols, :] = mm_rows(h2_ref[:, cols], gres_ref[...]).astype(BF16)
        return carry

    lax.fori_loop(0, hidden // FF_TILE, weights, 0)

    gain_grad = jnp.zeros((1, D), F32)
    for tile in range(TILES):
        rows = pl.ds(tile * QT, QT)
        value, grad = h1_ref[rows, :], gn_ref[rows, :]
        root = lax.rsqrt(mean_square(value) + EPSILON)
        unit = value * root
        gain_grad = gain_grad + jnp.sum(grad * unit, axis=0, keepdims=True)
        grad = grad * gain
        grad = gres_ref[rows, :].astype(F32) + root * (
            grad - unit * jnp.mean(grad * unit, axis=-1, keepdims=True)
        )
        gh_ref[rows, :] = grad
        low = grad.astype(BF16)
        nt_ref[rows, :] = low
        ga_ref[rows, :] = mm_cols(low, w_ref[:, out_at:gate_at]).astype(BF16)

    def out_weight(tile, carry):
        cols = pl.ds(pl.multiple_of(tile * QUAD, QUAD), QUAD)
        do_ref[cols, :] = mm_rows(att_ref[:, cols], nt_ref[...]).astype(BF16)
        return carry

    lax.fori_loop(0, D // QUAD, out_weight, 0)
    return gain_grad


def backward_attention_start(dk_ref, dv_ref):
    dk_ref[...] = jnp.zeros_like(dk_ref)
    dv_ref[...] = jnp.zeros_like(dv_ref)


def backward_attention_quad(tab_ref, rank, qkv_ref, att_ref, ga_ref, lse_ref, dqkv_ref, dk_ref, dv_ref, quad):
    heads = QUAD // DH
    marks = jnp.where(iota((16, QUAD), 1) // DH == iota((16, QUAD), 0), 1.0, 0.0).astype(BF16)
    low = quad * QUAD
    cols = slice(low, low + QUAD)

    def step(tile, carry):
        first = window_start(tile)
        bias, side_bias = tile_bias(tab_ref, rank, tile, first, 0)
        bias = jnp.concatenate([bias, side_bias], axis=0)
        rows = pl.ds(pl.multiple_of(tile * QT, QT), QT)
        window = pl.ds(first, WIN)
        lse = lse_ref[tile]
        product = ga_ref[rows, cols].astype(F32) * att_ref[rows, cols].astype(F32)
        high = product.astype(BF16)
        rest = (product - high.astype(F32)).astype(BF16)
        centre = mm_cols(marks, high) + mm_cols(marks, rest)
        query = head_stack(qkv_ref[rows, cols])
        grad = head_stack(ga_ref[rows, cols])
        keys = jnp.concatenate(
            [qkv_ref[window, D + low : D + low + QUAD], qkv_ref[ROWS:, D + low : D + low + QUAD]], axis=0
        )
        values = jnp.concatenate(
            [qkv_ref[window, 2 * D + low : 2 * D + low + QUAD],
             qkv_ref[ROWS:, 2 * D + low : 2 * D + low + QUAD]], axis=0
        )
        scores = mm_cols(keys, query)
        slopes = mm_cols(values, grad)
        probs, grads = [], []
        for head in range(heads):
            part = slice(head * QT, (head + 1) * QT)
            number = quad * heads + head
            prob = jnp.exp(scores[:, part] + bias - lse[number : number + 1])
            probs.append(prob.astype(BF16))
            grads.append((prob * (slopes[:, part] - centre[head : head + 1])).astype(BF16))
        probs = jnp.concatenate(probs, axis=1)
        grads = jnp.concatenate(grads, axis=1)
        dkey = mm(grads, query)
        dvalue = mm(probs, grad)
        dk_ref[window, cols] = dk_ref[window, cols] + dkey[:WIN]
        dk_ref[ROWS:, cols] = dk_ref[ROWS:, cols] + dkey[WIN:]
        dv_ref[window, cols] = dv_ref[window, cols] + dvalue[:WIN]
        dv_ref[ROWS:, cols] = dv_ref[ROWS:, cols] + dvalue[WIN:]
        dqkv_ref[rows, cols] = head_merge(mm_rows(grads, keys)).astype(BF16)
        return carry

    lax.fori_loop(0, TILES, step, 0)
    dqkv_ref[ROWS:, cols] = jnp.zeros((SIDE_ROWS, QUAD), BF16)
    dqkv_ref[:, D + low : D + low + QUAD] = dk_ref[:, cols].astype(BF16)
    dqkv_ref[:, 2 * D + low : 2 * D + low + QUAD] = dv_ref[:, cols].astype(BF16)


def weight_grads(n_ref, dqkv_ref, refs):
    for number, ref in enumerate(refs):
        def weights(tile, carry):
            at = pl.multiple_of(tile * QUAD, QUAD)
            value = mm_rows(n_ref[...], dqkv_ref[:, pl.ds(number * D + at, QUAD)]).astype(BF16)
            if len(ref.shape) == 4:
                ref[:, :, :, pl.ds(at, QUAD)] = value.reshape(ref.shape[:3] + (QUAD,))
            else:
                ref[:, pl.ds(at, QUAD)] = value
            return carry

        lax.fori_loop(0, D // QUAD, weights, 0)


def backward_project(tab_ref, rank, x_ref, gh_ref, gains, n_ref, dqkv_ref, w_ref, gn_ref, g_ref):
    def step(tile, carry):
        cols = pl.ds(pl.multiple_of(tile * QUAD, QUAD), QUAD)
        gn_ref[:, cols] = mm_cols(dqkv_ref[...], w_ref[cols, : 3 * D])
        return carry

    lax.fori_loop(0, D // QUAD, step, 0)
    pool = pooling(tab_ref, rank)
    side = mm(pool, n_ref[:ROWS, :])
    root = lax.rsqrt(mean_square(side) + EPSILON)
    unit = side * root
    grad = gn_ref[ROWS:, :]
    side_gain = jnp.sum(grad * unit, axis=0, keepdims=True)
    grad = grad * gains[1:2]
    grad = root * (grad - unit * jnp.mean(grad * unit, axis=-1, keepdims=True))
    parts = three_way(grad)
    gain_grad = jnp.zeros((1, D), F32)
    for tile in range(TILES):
        rows = pl.ds(tile * QT, QT)
        spread = pool[:, tile * QT : (tile + 1) * QT]
        total = gn_ref[rows, :] + mm_rows(spread, parts[0]) + mm_rows(spread, parts[1])
        value = x_ref[rows, :].astype(F32)
        root = lax.rsqrt(mean_square(value) + EPSILON)
        unit = value * root
        gain_grad = gain_grad + jnp.sum(total * unit, axis=0, keepdims=True)
        total = total * gains[0:1]
        value = (
            gh_ref[rows, :] + root * (total - unit * jnp.mean(total * unit, axis=-1, keepdims=True))
        ).astype(BF16)
        if len(g_ref.shape) == 3:
            g_ref[pl.ds(tile * (QT // BLK), QT // BLK)] = value.reshape(QT // BLK, BLK, D)
        else:
            g_ref[rows, :] = value
    return gain_grad, side_gain


def gelu_both(gate):
    square = gate * gate
    bend = jnp.tanh(GELU_C * (gate * (1.0 + GELU_A * square)))
    half = 0.5 * (1.0 + bend)
    slope = half + (0.5 * GELU_C) * gate * (1.0 - bend * bend) * (1.0 + (3.0 * GELU_A) * square)
    return gate * half, slope


def first_kernel(tab_ref, x_ref, gc_ref, w_ref, n_ref, qkv_ref, att_ref, lse_ref):
    rank = lax.axis_index("rep")
    gains = gains_of(gc_ref)
    forward_norm(tab_ref, rank, x_ref, gains, n_ref)
    forward_project(n_ref, w_ref, qkv_ref)
    forward_attention(tab_ref, rank, qkv_ref, att_ref, lse_ref, 0, TILES)


def second_kernel(tab_ref, x_ref, cot_ref, att_ref, gc_ref, w_ref, wb_ref,
                  y_ref, gh_ref, ga_ref, dg_ref, du_ref, db_ref, do_ref, gain_ref, *scratch):
    rank = lax.axis_index("rep")
    gain_ref[...] = feed_forward(tab_ref, rank, x_ref, cot_ref, att_ref, gains_of(gc_ref), w_ref, wb_ref,
                                 y_ref, gh_ref, ga_ref, dg_ref, du_ref, db_ref, do_ref, *scratch)


def third_kernel(tab_ref, x_ref, gh_ref, ga_ref, att_ref, lse_ref, n_ref, qkv_ref, gain_ref, gc_ref, w_ref,
                 g_ref, dw_ref, dc_ref, dqkv_ref, dk_ref, dv_ref, gn_ref):
    rank = lax.axis_index("rep")
    gains = gains_of(gc_ref)
    backward_attention_start(dk_ref, dv_ref)
    for quad in range(D // QUAD):
        backward_attention_quad(tab_ref, rank, qkv_ref, att_ref, ga_ref, lse_ref, dqkv_ref, dk_ref, dv_ref, quad)
    weight_grads(n_ref, dqkv_ref, [dw_ref.at[:, i * D : (i + 1) * D] for i in range(3)])
    one, side = backward_project(tab_ref, rank, x_ref, gh_ref, gains, n_ref, dqkv_ref, w_ref, gn_ref, g_ref)
    grads = jnp.concatenate([one, side, gain_ref[...], jnp.zeros((5, D), F32)], axis=0)
    spread_gain_grads(grads, dc_ref)


def attend(tab, x, gc, w):
    shape = jax.ShapeDtypeStruct
    return pl.pallas_call(
        first_kernel,
        out_shape=(shape((ALL_ROWS, D), BF16), shape((ALL_ROWS, 3 * D), BF16), shape((ROWS, D), BF16),
                   shape((TILES, 16, QT), F32)),
        in_specs=[SMEM, VMEM, VMEM, pl.BlockSpec((D, 3 * D), lambda step: (0, 0))],
        grid=(1,),
        out_specs=(VMEM,) * 4,
        compiler_params=pltpu.CompilerParams(vmem_limit_bytes=VMEM_LIMIT),
        name="attend",
    )(tab, x, gc, w)


def feed(tab, x, cot, att, gc, w, wb):
    hidden = wb.shape[0]
    shape = jax.ShapeDtypeStruct
    return pl.pallas_call(
        second_kernel,
        out_shape=(shape((ROWS, D), BF16), shape((ROWS, D), F32), shape((ROWS, D), BF16),
                   shape((D, hidden), BF16), shape((D, hidden), BF16), shape((hidden, D), BF16), shape((D, D), BF16),
                   shape((1, D), F32)),
        in_specs=[SMEM] + [VMEM] * 6,
        out_specs=(VMEM,) * 8,
        scratch_shapes=[pltpu.VMEM((ROWS, D), F32), pltpu.VMEM((ROWS, D), BF16), pltpu.VMEM((D, ROWS), BF16),
                        pltpu.VMEM((ROWS, D), BF16), pltpu.VMEM((ROWS, hidden), BF16),
                        pltpu.VMEM((ROWS, hidden), BF16), pltpu.VMEM((ROWS, hidden), BF16),
                        pltpu.VMEM((ROWS, D), F32)],
        compiler_params=pltpu.CompilerParams(vmem_limit_bytes=VMEM_LIMIT),
        name="feed_forward",
    )(tab, x, cot, att, gc, w, wb)


def backward_layer(tab, x, gh, ga, att, lse, n, qkv, gain, gc, w):
    shape = jax.ShapeDtypeStruct
    return pl.pallas_call(
        third_kernel,
        out_shape=(shape((ROWS, D), BF16), shape((D, 3 * D), BF16), shape((gc.shape[0], 8, 128), F32)),
        in_specs=[SMEM] + [VMEM] * 9 + [pl.BlockSpec((D, 3 * D), lambda step: (0, 0))],
        grid=(1,),
        out_specs=(VMEM,) * 3,
        scratch_shapes=[pltpu.VMEM((ALL_ROWS, 3 * D), BF16), pltpu.VMEM((ALL_ROWS, D), F32),
                        pltpu.VMEM((ALL_ROWS, D), F32), pltpu.VMEM((ALL_ROWS, D), F32)],
        compiler_params=pltpu.CompilerParams(vmem_limit_bytes=VMEM_LIMIT),
        name="attend_back",
    )(tab, x, gh, ga, att, lse, n, qkv, gain, gc, w)


class Links:
    def __init__(self, outer, inner):
        self.outer, self.inner = outer, inner
        self.rank, self.spot = lax.axis_index("rep"), lax.axis_index("fsdp")
        self.core = self.rank % 2
        self.row, self.col = self.spot // inner, self.spot % inner
        self.mate, self.across = core_of(self.rank), across_of(self.rank)
        self.late = []

    def greet(self, everyone=False, later=False):
        barrier = pltpu.get_barrier_semaphore()
        neighbours = (
            (self.row + 1 < self.outer, {"fsdp": self.spot + self.inner}),
            (self.row > 0, {"fsdp": self.spot - self.inner}),
            (self.col + 1 < self.inner, {"fsdp": self.spot + 1}),
            (self.col > 0, {"fsdp": self.spot - 1}),
        )
        group = (self.mate, self.across) + ((across_of(self.mate),) if everyone else ())
        amount = jnp.int32(len(group))
        for there, device in neighbours:
            amount = amount + there.astype(jnp.int32)

            @pl.when(there)
            def _():
                pl.semaphore_signal(barrier, inc=1, device_id=device, device_id_type=MESH)

        for device in group:
            pl.semaphore_signal(barrier, inc=1, device_id={"rep": device}, device_id_type=MESH)
        self.met = lambda: pl.semaphore_wait(barrier, amount)
        if not later:
            self.met()

    def send(self, there, src, dst, ssem, rsem, device):
        def describe():
            return pltpu.make_async_remote_copy(
                src_ref=src, dst_ref=dst, send_sem=ssem, recv_sem=rsem,
                device_id=device, device_id_type=MESH,
            )

        if there is None:
            describe().start()
        else:
            @pl.when(there)
            def _():
                describe().start()

        self.late.append((there, lambda: describe().wait_send()))

    def arrive(self, place, rsem, spare):
        pltpu.make_async_remote_copy(
            src_ref=place, dst_ref=place, send_sem=spare, recv_sem=rsem,
            device_id={"rep": self.mate}, device_id_type=MESH,
        ).wait_recv()

    def drain(self):
        for there, finish in self.late:
            if there is None:
                finish()
            else:
                pl.when(there)(finish)


def halves(ref, which):
    half = ref.shape[-1] // 2
    cols = pl.ds(pl.multiple_of(which * half, 128), half)
    return ref.at[:, :, :, cols] if len(ref.shape) == 4 else ref.at[:, cols]


class Reduction:
    def __init__(self, links, source, total, mine, crecv, yrecv, zrecv, xrecv, stage, sems, number):
        self.links, self.source, self.total, self.mine, self.stage = links, source, total, mine, stage
        self.crecv, self.yrecv, self.zrecv, self.xrecv = crecv, yrecv, zrecv, xrecv
        self.sems, self.number = sems, number
        self.whole = total.shape[-1] % 256 != 0
        self.load = None

    def sem(self, name, *index):
        return self.sems[name].at[index + (self.number,)]

    def begin(self):
        links = self.links
        other = self.source if self.whole else halves(self.source, 1 - links.core)
        links.send(None, other, self.crecv, self.sem("c_send"), self.sem("c_recv"), {"rep": links.mate})
        if self.mine is None:
            self.mine = self.source if self.whole else halves(self.source, links.core)
        else:
            own = self.source if self.whole else halves(self.source, links.core)
            self.load = pltpu.make_async_copy(own, self.mine, self.sem("m_sem"))
            self.load.start()

    def pair(self):
        links = self.links
        if self.load is not None:
            self.load.wait()
        links.arrive(self.crecv, self.sem("c_recv"), self.sems["spare"].at[0])
        inner = links.inner

        def add(index, carry):
            row, col = index // inner, index % inner
            self.mine[row, col] = self.mine[row, col] + self.crecv[row, col]
            return carry

        lax.fori_loop(0, links.outer * inner, add, 0)
        links.send(None, self.mine.at[:, 1 - links.col], self.yrecv, self.sem("y_send"), self.sem("y_recv"),
                   {"fsdp": links.spot + 1 - 2 * links.col})

    def slot(self, way, place, dest):
        return dest - place if way == 0 else self.links.outer - place + dest

    def pass_on(self, way, dest, there, first):
        links = self.links
        step = 1 if way == 0 else -1
        mine = self.mine.at[dest, links.col]
        put = self.slot(way, links.row + step, dest)
        if not first:
            got = self.slot(way, links.row, dest)

            @pl.when(there)
            def _():
                links.arrive(self.zrecv.at[got], self.sem("z_recv", got), self.sems["spare"].at[0])
                mine[...] = mine[...] + self.zrecv[got]

        links.send(there, mine, self.zrecv.at[put], self.sem("z_send", way, dest), self.sem("z_recv", put),
                   {"fsdp": links.spot + step * links.inner})

    def column(self):
        links = self.links
        size = links.outer
        links.arrive(self.yrecv, self.sem("y_recv"), self.sems["spare"].at[0])

        def add(index, carry):
            self.mine[index, links.col] = self.mine[index, links.col] + self.yrecv[index]
            return carry

        lax.fori_loop(0, size, add, 0)
        for far in range(size - 1, 0, -1):
            self.pass_on(0, far, links.row == 0, True)
            self.pass_on(1, size - 1 - far, links.row == size - 1, True)

    def hop(self, turn):
        links = self.links
        size = links.outer
        for way in range(2):
            place = turn if way == 0 else size - 1 - turn
            here = links.row == place
            rest = range(size - 1, place, -1) if way == 0 else range(0, place)
            for dest in rest:
                self.pass_on(way, dest, here, False)
            mine = self.mine.at[place, links.col]
            got = self.slot(way, place, place)

            @pl.when(here)
            def _():
                links.arrive(self.zrecv.at[got], self.sem("z_recv", got), self.sems["spare"].at[0])
                mine[...] = mine[...] + self.zrecv[got]

    def cross(self):
        links = self.links
        mine = self.mine.at[links.row, links.col]
        links.send(None, mine, self.xrecv, self.sem("x_send"), self.sem("x_recv"), {"rep": links.across})

    def finish(self):
        links = self.links
        links.arrive(self.xrecv, self.sem("x_recv"), self.sems["spare"].at[0])
        self.stage[...] = self.mine[links.row, links.col].astype(F32) + self.xrecv[...].astype(F32)
        place = self.total if self.whole else halves(self.total, links.core)
        self.keep = pltpu.make_async_copy(self.stage, place, self.sem("m_sem"))
        self.keep.start()
        if not self.whole:
            links.send(None, self.stage, place, self.sem("f_send"), self.sem("f_recv"), {"rep": links.mate})

    def settle(self):
        self.keep.wait()
        if not self.whole:
            self.links.arrive(
                halves(self.total, 1 - self.links.core), self.sem("f_recv"), self.sems["spare"].at[0]
            )


class AcrossFirst(Reduction):
    def pair(self):
        links = self.links
        if self.load is not None:
            self.load.wait()
        links.arrive(self.crecv, self.sem("c_recv"), self.sems["spare"].at[0])
        inner = links.inner

        def add(index, carry):
            row, col = index // inner, index % inner
            self.mine[row, col] = self.mine[row, col] + self.crecv[row, col]
            return carry

        lax.fori_loop(0, links.outer * inner, add, 0)
        self.side = links.rank // 2
        links.send(None, self.rows_of(self.mine, 1 - self.side), self.xrecv, self.sem("x_send"), self.sem("x_recv"),
                   {"rep": links.across})

    def rows_of(self, ref, which):
        half = ref.shape[-2] // 2
        rows = pl.ds(pl.multiple_of(which * half, 16), half)
        return ref.at[:, :, rows, :] if len(ref.shape) == 4 else ref.at[rows, :]

    def meet(self):
        links = self.links
        links.arrive(self.xrecv, self.sem("x_recv"), self.sems["spare"].at[0])
        self.mine = self.rows_of(self.mine, self.side)
        inner = links.inner

        def add(index, carry):
            row, col = index // inner, index % inner
            self.mine[row, col] = self.mine[row, col] + self.xrecv[row, col]
            return carry

        lax.fori_loop(0, links.outer * inner, add, 0)
        links.send(None, self.mine.at[:, 1 - links.col], self.yrecv, self.sem("y_send"), self.sem("y_recv"),
                   {"fsdp": links.spot + 1 - 2 * links.col})

    def quarter(self, side, core):
        return halves(self.rows_of(self.total, side), core)

    def spread(self, stage, place, keep, ssem, rsem):
        links = self.links
        self.keeps.append(pltpu.make_async_copy(stage, place, keep))
        self.keeps[-1].start()
        links.send(None, stage, place, ssem, rsem, {"rep": links.mate})

    def cross(self):
        links = self.links
        mine = self.mine.at[links.row, links.col]
        links.send(None, mine, self.third, self.sem("h_send"), self.sem("h_recv"), {"rep": links.across})
        self.stage[...] = mine[...].astype(F32)
        self.keeps = []
        self.spread(self.stage, self.quarter(self.side, links.core), self.sem("m_sem"),
                    self.sem("f_send"), self.sem("f_recv"))

    def finish(self):
        links = self.links
        links.arrive(self.third, self.sem("h_recv"), self.sems["spare"].at[0])
        self.stage_two[...] = self.third[...].astype(F32)
        self.spread(self.stage_two, self.quarter(1 - self.side, links.core), self.sem("k_keep"),
                    self.sem("k_send"), self.sem("k_recv"))

    def settle(self):
        links = self.links
        for keep in self.keeps:
            keep.wait()
        for side, name in ((self.side, "f_recv"), (1 - self.side, "k_recv")):
            links.arrive(self.quarter(side, 1 - links.core), self.sem(name), self.sems["spare"].at[0])


SEM_NAMES = ("c_send", "c_recv", "m_sem", "y_send", "y_recv", "z_send", "z_recv", "x_send", "x_recv",
             "f_send", "f_recv", "h_send", "h_recv", "k_send", "k_recv", "k_keep", "r_send", "r_recv", "own", "spare")


class Return:
    def __init__(self, links, source, home, sems, kind):
        self.links, self.source, self.home, self.sems, self.kind = links, source, home, sems, kind

    def begin(self):
        links = self.links
        dst = self.home.at[links.rank]
        for way, device in enumerate((links.across, links.mate)):
            links.send(None, self.source, dst, self.sems["r_send"].at[self.kind, way],
                       self.sems["r_recv"].at[self.kind, way], {"rep": device})
        self.copy = pltpu.make_async_copy(self.source, dst, self.sems["own"].at[self.kind])
        self.copy.start()

    def relay(self):
        links = self.links
        place = self.home.at[links.across]
        links.arrive(place, self.sems["r_recv"].at[self.kind, 0], self.sems["spare"].at[0])
        links.send(None, place, place, self.sems["r_send"].at[self.kind, 2],
                   self.sems["r_recv"].at[self.kind, 2], {"rep": links.mate})

    def settle(self):
        links, sem = self.links, self.sems["r_recv"]
        links.arrive(self.home.at[links.mate], sem.at[self.kind, 1], self.sems["spare"].at[0])
        links.arrive(self.home.at[across_of(links.mate)], sem.at[self.kind, 2], self.sems["spare"].at[0])
        self.copy.wait()


TABLE_ROWS = 56


def packed_table(lens, tabv_ref):
    lane = iota((8, 128), 1)
    blocks = lax.div(lens + (BLK - 1), BLK)
    key = jnp.where(blocks > 0, blocks * 128 + (127 - lane), 0)
    wide = jnp.broadcast_to(key[:1], (128, 128))
    other = jnp.sum(jnp.where(iota((128, 128), 0) == iota((128, 128), 1), wide, 0), axis=1, keepdims=True)
    order = jnp.sum(jnp.where(other > wide, 1, 0), axis=0, keepdims=True)
    order = jnp.broadcast_to(order, (8, 128))
    edges, below = [], jnp.zeros((8, 1), jnp.int32)
    for size in range(MAX_SEQ_BLOCKS, 0, -1):
        below = below + jnp.sum(jnp.where(blocks == size, 1, 0), axis=1, keepdims=True)
        edges.append(jnp.broadcast_to(below, (8, 128)))

    def assign(number, carry):
        loads, slot, first = carry[:4], carry[4], carry[5]
        size = jnp.zeros((8, 128), jnp.int32)
        for step, edge in enumerate(edges):
            size = size + jnp.where(number < edge, 1, 0)
        low = jnp.minimum(jnp.minimum(loads[0], loads[1]), jnp.minimum(loads[2], loads[3]))
        best = jnp.full((8, 128), 3, jnp.int32)
        for dev in (2, 1, 0):
            best = jnp.where(loads[dev] == low, dev, best)
        mine = order == number
        slot = jnp.where(mine, best * SLOTS + low, slot)
        first = jnp.where(mine, low, first)
        loads = tuple(loads[dev] + jnp.where(best == dev, size, 0) for dev in range(4))
        return loads + (slot, first)

    zero = jnp.zeros((8, 128), jnp.int32)
    carry = lax.fori_loop(0, 32, assign, (zero,) * 6)
    slot, first = carry[4], carry[5]
    where, tokens, segment = zero - 1, zero, zero
    for step in range(MAX_SEQ_BLOCKS):
        def shifted(value):
            return value if step == 0 else pltpu.roll(value, step, 1)

        covers = shifted(blocks) > step
        where = jnp.where(covers, shifted(slot) + step, where)
        tokens = jnp.where(covers, jnp.minimum(shifted(lens) - BLK * step, BLK), tokens)
        segment = jnp.where(covers, shifted(first) + 1, segment)
    packed = jnp.where(where >= 0, (lane + 1) + 128 * tokens + 16384 * segment, 0)
    spots = jnp.broadcast_to(where[:1], (48, 128))
    values = jnp.broadcast_to(packed[:1], (48, 128))
    column = jnp.sum(jnp.where(spots == iota((48, 128), 0), values, 0), axis=1, keepdims=True)
    tabv_ref[:48] = jnp.broadcast_to(column, (48, 128))
    tabv_ref[48:] = where


ROW_FIRST = (3,)
FRONT_ORDER = (
    ("own", 1), ("own", 3), ("do", "table"), ("hop", 1, 0), ("own", 0), ("pack", 0, 1), ("hop", 1, 1), ("own", 5),
    ("cross", 0), ("own", 2), ("hop", 0, 0), ("hop", 1, 2), ("pack", 1, 1), ("pack", 0, 0), ("hop", 5, 0),
    ("hop", 5, 1), ("hop", 5, 2), ("hop", 0, 1), ("yz", 3), ("hop", 0, 2), ("own", 4), ("cross", 1), ("fr", 1),
    ("hop", 2, 0), ("pack", 1, 0), ("hop", 3, 0), ("fr", 5), ("rfin", 0), ("fr", 0), ("do", "norm"), ("hop", 2, 1),
    ("got", 0), ("hop", 4, 0), ("do", "proj"), ("do", "a0"), ("hop", 2, 2), ("hop", 4, 1), ("hop", 3, 1),
    ("do", "a1"), ("hop", 4, 2), ("fr", 2), ("do", "a2"), ("hop", 3, 2), ("got", 2), ("do", "enter"), ("rfin", 1),
    ("fr", 4), ("xin", 1), ("got", 3), ("do", "half"),
)


def front_kernel(outer, inner, *refs):
    (lens_ref, rows_any, cots_any, *weights), refs = refs[:9], refs[9:]
    (wd_any, wc_ref), refs = refs[:2], refs[2:]
    (tab_ref, gains_ref), outs_any, (ga_ref, gb_ref), refs = refs[:2], refs[2:16], refs[16:18], refs[18:]
    (stage, lens_all, tabs, psend, precv, xsend, xrecv, rows_ref, cots_ref), refs = refs[:9], refs[9:]
    wd_ref, refs = refs[0], refs[1:]
    held, gc_ref, refs = refs[:14], refs[14], refs[15:]
    x_ref, cot_ref, n_ref, qkv_ref, att_ref, lse_ref, wqkv_ref, w2_ref, h1_ref, nt_ref, ntt_ref, b0_ref, b1_ref, b2_ref = held
    (l_send, l_recv, t_sem, w_sem, z_send, z_recv, y_send, y_recv, c_send, c_recv, d_send, d_recv, own_sem,
     p_send, p_recv, x_send, x_recv, spare, out_sem, piece_sem) = refs
    links = Links(outer, inner)
    rank, spot, core, mate, across = links.rank, links.spot, links.core, links.mate, links.across
    row, col = links.row, links.col
    side = rank // 2
    count = outer * inner
    part = stage.shape[0]
    per_rank = rows_ref.shape[0]
    width = 3 * D
    tall = wd_ref.shape[0]
    hidden = weights[-1].shape[1]
    rest = stage.shape[1] - width
    half = hidden // 2
    early = D + 2 * half
    spans = [(0, (D + half) // 2), (D + half, half // 2), (early, half)]

    at = 0
    loads = []
    loads.append(pltpu.make_async_copy(wd_any, wd_ref, w_sem.at[2]))
    loads[0].start()
    row_loads = [pltpu.make_async_copy(rows_any, rows_ref, w_sem.at[0]), pltpu.make_async_copy(cots_any, cots_ref, w_sem.at[1])]
    parts = [(ref, slice(0, D)) for ref in weights[:4]]
    parts += [(ref, cols) for cols in (slice(0, half), slice(half, hidden)) for ref in weights[4:]]
    for number, (ref, cols) in enumerate(parts):
        size = cols.stop - cols.start
        loads.append(pltpu.make_async_copy(ref.at[:, cols], stage.at[:, at : at + size], w_sem.at[3 + number]))
        loads[-1].start()
        at += size
    for load in row_loads:
        load.start()

    links.greet(True)
    lens_all[rank] = lens_ref[...]
    for step in range(1, 4):
        links.send(None, lens_ref, lens_all.at[rank], l_send.at[step - 1], l_recv.at[step - 1],
                   {"rep": (rank + step) % 4})

    def cols_of(start, half, which):
        return pl.ds(pl.multiple_of(start + which * half, 128), half)

    down_half = D // 2

    def tall_rows(which):
        return pl.ds(pl.multiple_of(which * (tall // 2), 16), tall // 2)

    def source(number):
        if number == 0:
            return stage.at[:, cols_of(0, width // 2, core)]
        if number == 1:
            return wd_ref.at[tall_rows(side), cols_of(0, down_half, core)]
        if number == 5:
            return wc_ref
        start, size = spans[number - 2]
        return stage.at[:, cols_of(width + start, size, core)]

    def place(number, shard, which=None):
        which = core if which is None else which
        if number == 0:
            return wqkv_ref.at[pl.ds(pl.multiple_of(shard * part, 16), part), cols_of(0, width // 2, which)]
        if number in (1, 6):
            return gb_ref.at[shard, tall_rows(side if number == 1 else 1 - side), cols_of(0, down_half, which)]
        if number == 5:
            return gc_ref.at[shard]
        start, size = spans[number - 2]
        if number == 4:
            return ga_ref.at[shard, :, cols_of(0, size, which)]
        return w2_ref.at[pl.ds(pl.multiple_of(shard * part, 16), part), cols_of(start, size, which)]

    nobody = spare.at[0]

    def both(first, second):
        return second if first is None else jnp.logical_and(first, second)

    def guarded(there, action):
        if there is None:
            action()
        else:
            pl.when(there)(action)

    def share(there, number, shard):
        if number == 5:
            return
        here = place(number, shard)
        links.send(there, here, here, c_send.at[number, shard], c_recv.at[number, shard], {"rep": mate})
        if number == 1:
            links.send(there, here, here, d_send.at[shard], d_recv.at[shard], {"rep": across})

    other_column = {"fsdp": spot + 1 - 2 * col}

    def along_row(there, number, line, src):
        here = place(number, line * inner + col)
        links.send(there, here if src is None else src, here, y_send.at[line, number], y_recv.at[line, number],
                   other_column)

    def lines(step):
        return ((row - 1 - step >= 0, row - 1 - step, 0, row + 1 < outer, spot + inner),
                (row + 1 + step < outer, row + 1 + step, 1, row > 0, spot - inner))

    def along_line(number, column, src):
        here = place(number, row * inner + (col if column == 0 else 1 - col))
        src = here if src is None else src
        links.send(row + 1 < outer, src, here, z_send.at[0, 0, number, column], z_recv.at[0, 0, number, column],
                   {"fsdp": spot + inner})
        links.send(row > 0, src, here, z_send.at[1, 0, number, column], z_recv.at[1, 0, number, column],
                   {"fsdp": spot - inner})

    def own(number):
        src = source(number)
        along_line(number, 0, src)
        along_row(None, number, row, src)

    def second_column(number):
        shard = row * inner + 1 - col
        links.arrive(place(number, shard), y_recv.at[row, number], nobody)
        share(None, number, shard)
        along_line(number, 1, None)

    def hop(number, step):
        for here, line, way, onward, target in lines(step):
            for column in range(2 if number in ROW_FIRST else 1):
                shard = line * inner + (col if column == 0 else 1 - col)
                guarded(here, lambda: links.arrive(place(number, shard), z_recv.at[way, step, number, column], nobody))
                if step + 1 < outer - 1:
                    view = place(number, shard)
                    links.send(both(here, onward), view, view, z_send.at[way, step + 1, number, column],
                               z_recv.at[way, step + 1, number, column], {"fsdp": target})
                if number not in ROW_FIRST:
                    along_row(here, number, line, None)
                share(here, number, shard)

    def from_row(number):
        def one(there, line):
            shard = line * inner + 1 - col
            guarded(there, lambda: links.arrive(place(number, shard), y_recv.at[line, number], nobody))
            share(there, number, shard)

        one(None, row)
        for step in range(outer - 1):
            for here, line, *_ in lines(step):
                one(here, line)

    def gathered(*numbers):
        def wait(shard, carry):
            @pl.when(shard != spot)
            def _():
                for number in numbers:
                    links.arrive(place(number, shard, 1 - core), c_recv.at[number, shard], nobody)

            return carry

        lax.fori_loop(0, count, wait, 0)

    def from_across():
        def relay(shard, carry):
            here = place(6, shard)

            @pl.when(shard != spot)
            def _():
                links.arrive(here, d_recv.at[shard], nobody)
                pltpu.make_async_remote_copy(
                    src_ref=here, dst_ref=here, send_sem=c_send.at[6, shard], recv_sem=c_recv.at[6, shard],
                    device_id={"rep": mate}, device_id_type=MESH,
                ).start()

            return carry

        lax.fori_loop(0, count, relay, 0)

    for load in loads:
        load.wait()
    keep = [
        pltpu.make_async_copy(stage.at[:, :width], wqkv_ref.at[pl.ds(pl.multiple_of(spot * part, 16), part)], own_sem.at[0]),
        pltpu.make_async_copy(stage.at[:, width + early :], ga_ref.at[spot], own_sem.at[1]),
        pltpu.make_async_copy(wd_ref, gb_ref.at[spot], own_sem.at[2]),
        pltpu.make_async_copy(wc_ref, gc_ref.at[spot], own_sem.at[3]),
        pltpu.make_async_copy(
            stage.at[:, width : width + early], w2_ref.at[pl.ds(pl.multiple_of(spot * part, 16), part)], own_sem.at[4]
        ),
    ]
    for copy in keep:
        copy.start()
    leaving = []

    def leave(*numbers):
        for number in numbers:
            leaving.append(pltpu.make_async_copy(held[number], outs_any[number], out_sem.at[number]))
            leaving[-1].start()

    def make_table():
        for step in range(1, 4):
            links.arrive(lens_all.at[(rank + 4 - step) % 4], l_recv.at[step - 1], nobody)
        lens = lens_all[0] + lens_all[1] + lens_all[2] + lens_all[3]
        packed_table(jnp.broadcast_to(lens[:1], (8, 128)), tab_ref)
        to_scalar = pltpu.make_async_copy(tab_ref, tabs, t_sem.at[0])
        to_scalar.start()
        to_scalar.wait()
        for load in row_loads:
            load.wait()

    sources = (rows_ref, cots_ref)
    outs = (x_ref, cot_ref)

    def picked(kind, target, slot):
        index = block_at(tabs, target * SLOTS + slot) - rank * per_rank
        mine = jnp.logical_and(index >= 0, index < per_rank)
        return mine, sources[kind][jnp.clip(index, 0, per_rank - 1)]

    def mate_copy(kind, piece):
        return pltpu.make_async_remote_copy(
            src_ref=psend.at[kind, piece], dst_ref=precv.at[kind, piece],
            send_sem=p_send.at[kind, piece], recv_sem=p_recv.at[kind, piece],
            device_id={"rep": mate}, device_id_type=MESH,
        )

    def across_copy(kind):
        return pltpu.make_async_remote_copy(
            src_ref=xsend.at[kind], dst_ref=xrecv.at[kind],
            send_sem=x_send.at[kind], recv_sem=x_recv.at[kind],
            device_id={"rep": across}, device_id_type=MESH,
        )

    def pack_rows(kind, piece):
        target = mate if piece == 0 else across_of(mate)

        def pack(slot, carry):
            mine, value = picked(kind, target, slot)
            psend[kind, piece, slot] = jnp.where(mine, value, jnp.zeros_like(value))
            return carry

        lax.fori_loop(0, SLOTS, pack, 0)
        mate_copy(kind, piece).start()

    def cross_rows(kind):
        mate_copy(kind, 1).wait_recv()

        def merge(slot, carry):
            mine, value = picked(kind, across, slot)
            xsend[kind, slot] = jnp.where(mine, value, precv[kind, 1, slot])
            return carry

        lax.fori_loop(0, SLOTS, merge, 0)
        across_copy(kind).start()

    def finish_rows(kind):
        mate_copy(kind, 0).wait_recv()
        across_copy(kind).wait_recv()

        def finish(slot, carry):
            mine, value = picked(kind, rank, slot)
            rows = pl.ds(pl.multiple_of(slot * BLK, BLK), BLK)
            outs[kind][rows, :] = jnp.where(mine, value, precv[kind, 0, slot] + xrecv[kind, slot])
            return carry

        lax.fori_loop(0, SLOTS, finish, 0)

    def norm():
        keep[3].wait()
        gains = gains_of(gc_ref)
        gains_ref[...] = gains
        forward_norm(tabs, rank, x_ref, gains, n_ref)
        leave(2)

    def project():
        keep[0].wait()
        forward_project(n_ref, wqkv_ref, qkv_ref)
        leave(3, 6)

    def attend_tiles(begin, end):
        forward_attention(tabs, rank, qkv_ref, att_ref, lse_ref, begin, end)
        if end == TILES:
            leave(4, 5)

    def enter():
        gain = gains_ref[2:3]
        for tile in range(TILES):
            rows = pl.ds(tile * QT, QT)
            value = x_ref[rows, :].astype(F32) + mm(att_ref[rows, :], w2_ref[:, :D])
            h1_ref[rows, :] = value
            normed = (value * lax.rsqrt(mean_square(value) + EPSILON) * gain).astype(BF16)
            nt_ref[rows, :] = normed
            ntt_ref[:, tile * QT : (tile + 1) * QT] = jnp.transpose(normed)
        leave(8, 9, 10)

    def first_half():
        def step(tile, carry):
            at = pl.multiple_of(tile * FF_TILE, FF_TILE)
            cols = pl.ds(at, FF_TILE)
            gate = mm(nt_ref[...], w2_ref[:, pl.ds(D + at, FF_TILE)])
            up = mm(nt_ref[...], w2_ref[:, pl.ds(D + half + at, FF_TILE)])
            act, slope = gelu_both(gate)
            b0_ref[:, cols] = (act * up).astype(BF16)
            b1_ref[:, cols] = (up * slope).astype(BF16)
            b2_ref[:, cols] = act.astype(BF16)
            for copy in piece_copies(tile):
                copy.start()
            return carry

        lax.fori_loop(0, half // FF_TILE, step, 0)

    def piece_copies(tile):
        cols = pl.ds(pl.multiple_of(tile * FF_TILE, FF_TILE), FF_TILE)
        return [
            pltpu.make_async_copy(held[number].at[:, cols], outs_any[number].at[:, cols], piece_sem.at[number - 11, tile])
            for number in (11, 12, 13)
        ]

    work = {"table": make_table, "enter": enter, "half": first_half, "norm": norm, "proj": project, "a0": lambda: attend_tiles(0, 2),
            "a1": lambda: attend_tiles(2, 4), "a2": lambda: attend_tiles(4, TILES)}
    for action, which, *more in FRONT_ORDER:
        if action == "do":
            work[which]()
        elif action == "own":
            own(which)
        elif action == "hop":
            hop(which, more[0])
        elif action == "fr":
            from_row(which)
        elif action == "yz":
            second_column(which)
        elif action == "xin":
            from_across()
        elif action == "got":
            gathered(which)
            if which == 2:
                keep[4].wait()
            if which == 3:
                leave(7)
        elif action == "pack":
            pack_rows(which, more[0])
        elif action == "cross":
            cross_rows(which)
        else:
            finish_rows(which)
            leave(which)
    gathered(1, 4, 6)

    def sent(shard, carry):
        @pl.when(shard != spot)
        def _():
            pltpu.make_async_remote_copy(
                src_ref=place(6, shard), dst_ref=place(6, shard), send_sem=c_send.at[6, shard], recv_sem=c_recv.at[6, shard],
                device_id={"rep": mate}, device_id_type=MESH,
            ).wait_send()

        return carry

    lax.fori_loop(0, count, sent, 0)
    links.drain()
    for kind in range(2):
        for piece in range(2):
            mate_copy(kind, piece).wait_send()
        across_copy(kind).wait_send()
    for copy in keep[1:3] + leaving:
        copy.wait()
    for tile in range(half // FF_TILE):
        for copy in piece_copies(tile):
            copy.wait()


def gather_and_attend(count, lens, rows, cots, weights, wd, wc):
    outer, inner = grid_of(count)
    block = rows.shape[1:]
    part, hidden = weights[0].shape[0], weights[-1].shape[1]
    dma, shape = pltpu.SemaphoreType.DMA, jax.ShapeDtypeStruct
    total = sum(weight.shape[1] for weight in weights)
    kinds = 6
    held = (shape((ROWS, D), BF16), shape((ROWS, D), BF16), shape((ALL_ROWS, D), BF16), shape((ALL_ROWS, 3 * D), BF16),
            shape((ROWS, D), BF16), shape((TILES, 16, QT), F32), shape((D, 3 * D), BF16), shape((D, D + hidden), BF16), shape((ROWS, D), F32),
            shape((ROWS, D), BF16), shape((D, ROWS), BF16)) + (shape((ROWS, hidden // 2), BF16),) * 3
    return pl.pallas_call(
        partial(front_kernel, outer, inner),
        out_shape=(shape((TABLE_ROWS, 128), jnp.int32), shape((16, D), F32)) + held + (
            shape((count, part, hidden), BF16), shape((count,) + wd.shape, BF16),
        ),
        in_specs=[VMEM] + [ANY] * 9 + [VMEM],
        out_specs=(VMEM,) * 2 + (ANY,) * 16,
        scratch_shapes=[
            pltpu.VMEM((part, total), BF16), pltpu.VMEM((4, 8, 128), jnp.int32), pltpu.SMEM((TABLE_ROWS, 128), jnp.int32),
            pltpu.VMEM((2, 2, SLOTS) + block, BF16), pltpu.VMEM((2, 2, SLOTS) + block, BF16),
            pltpu.VMEM((2, SLOTS) + block, BF16), pltpu.VMEM((2, SLOTS) + block, BF16),
            pltpu.VMEM(rows.shape, BF16), pltpu.VMEM(cots.shape, BF16),
            pltpu.VMEM(wd.shape, BF16),
            *(pltpu.VMEM(one.shape, one.dtype) for one in held), pltpu.VMEM((count, 16, 128), BF16),
            dma((3,)), dma((3,)), dma((1,)), dma((11,)),
            dma((2, outer - 1, kinds, 2)), dma((2, outer - 1, kinds, 2)), dma((outer, kinds)), dma((outer, kinds)),
            dma((kinds + 1, count)), dma((kinds + 1, count)), dma((count,)), dma((count,)), dma((5,)),
            dma((2, 2)), dma((2, 2)), dma((2,)), dma((2,)), dma((1,)), dma((14,)), dma((3, hidden // 2 // FF_TILE)),
        ],
        compiler_params=pltpu.CompilerParams(
            collective_id=1, has_side_effects=True, vmem_limit_bytes=VMEM_LIMIT
        ),
        name="gather_and_attend",
    )(lens, rows, cots, *weights, wd, wc)


ACROSS_FIRST = (1, 2)
REAR_ORDER = (
    ("do", "start"), ("do", "P0"), ("do", "P1a"), ("do", "gA"), ("begin", 0), ("do", "P1b"), ("pair", 0),
    ("do", "gB"), ("begin", 2), ("do", "uB"), ("begin", 3), ("do", "d"), ("begin", 4), ("pair", 2), ("do", "uA"),
    ("begin", 1), ("pair", 3), ("do", "out"), ("pair", 1), ("pair", 4), ("do", "load"), ("do", "P4"), ("do", "P5"),
    ("col", 0), ("col", 3), ("rows", 0), ("do", "q0"), ("do", "q1"), ("hop", 0, 1), ("meet", 2), ("do", "q2"),
    ("meet", 1), ("col", 4), ("do", "p0"), ("begin", 6), ("do", "bp"), ("rows", 1), ("pair", 6), ("do", "p1"),
    ("hop", 3, 1), ("begin", 5), ("hop", 0, 2), ("begin", 7), ("do", "dc"), ("do", "p2"), ("begin", 8), ("col", 2),
    ("pair", 7), ("hop", 4, 1), ("pair", 5), ("begin", 9), ("hop", 2, 1), ("col", 1), ("col", 6), ("hop", 0, 3),
    ("hop", 4, 2), ("col", 7), ("hop", 3, 2), ("hop", 6, 1), ("cross", 0), ("hop", 1, 1), ("pair", 8), ("hop", 4, 3),
    ("pair", 9), ("hop", 6, 2), ("col", 5), ("hop", 3, 3), ("cross", 4), ("cross", 3), ("hop", 7, 1), ("hop", 1, 2),
    ("hop", 2, 2), ("hop", 5, 1), ("col", 8), ("hop", 1, 3), ("cross", 1), ("hop", 6, 3), ("hop", 5, 2), ("col", 9),
    ("cross", 6), ("relay", 1), ("hop", 5, 3), ("cross", 5), ("hop", 2, 3), ("hop", 7, 2), ("hop", 7, 3),
    ("cross", 2), ("hop", 8, 1), ("relay", 0), ("cross", 7), ("hop", 9, 1), ("hop", 8, 2), ("hop", 9, 2),
    ("hop", 8, 3), ("cross", 8), ("fin", 2), ("fin", 4), ("hop", 9, 3), ("fin", 5), ("fin", 0), ("fin", 1),
    ("cross", 9), ("fin", 7), ("fin", 3), ("fin", 6), ("fin", 8), ("fin", 9),
)


def rear_kernel(outer, inner, *refs):
    (tab_ref, x_any, att_any, lse_ref, gc_ref), refs = refs[:5], refs[5:]
    (cot_any, n_any, qkv_any, wqkv_any, w2_any, wf_any, wd_any), refs = refs[:7], refs[7:]
    (h1_any, nt_any, ntt_any, b0_any, b1_any, b2_any), refs = refs[:6], refs[6:]
    kinds = 10
    (og_ref, ou_ref, od_ref, oo_ref, op_ref, oc_ref, ry_ref, rg_ref), refs = refs[:8], refs[8:]
    (y_ref, gh_ref, fa_ref, dk_ref, b0_ref, b1_ref, b2_ref, n_ref, ntt_ref, gres_ref, ga_ref), refs = refs[:11], refs[11:]
    (x_ref, att_ref), refs = refs[:2], refs[2:]
    (wf_ref, wd_ref, dg_ref, du_ref, db_ref, do_ref, dc_ref, mine_ref), refs = refs[:8], refs[8:]
    crecv, refs = list(refs[:7]), refs[7:]
    narrow = D // 2
    crecv = crecv[:6] + [crecv[i].at[:, :, :, :narrow] for i in range(3)] + crecv[6:]
    yrecv, zrecv, xrecv, stages = (refs[kinds * i : kinds * (i + 1)] for i in range(4))
    refs = refs[4 * kinds :]
    extra, refs = refs[: 2 * len(ACROSS_FIRST)], refs[2 * len(ACROSS_FIRST) :]
    sems = dict(zip(SEM_NAMES, refs))
    load_sem, free_sem = refs[len(SEM_NAMES) :]
    links = Links(outer, inner)
    rank = links.rank
    hidden = wd_ref.shape[0]
    part = wf_ref.shape[2]
    group = 4 * part

    def fetch(number, src, dst):
        copy = pltpu.make_async_copy(src, dst, load_sem.at[number])
        copy.start()
        return copy

    wide, early = hidden // 2, D + hidden
    load_first = [
        fetch(0, cot_any, ga_ref), fetch(1, wd_any.at[:wide], wd_ref.at[:wide]),
        fetch(7, b1_any, b1_ref.at[:ROWS, :wide]), fetch(8, b2_any, b2_ref.at[:ROWS, :wide]),
    ]
    load_products = fetch(9, ntt_any, ntt_ref)
    load_rest = [
        fetch(10, nt_any, n_ref.at[:ROWS]), fetch(2, wf_any, wf_ref.at[:, :, :, early:]),
        fetch(3, wd_any.at[wide:], wd_ref.at[wide:]), fetch(11, b0_any, b0_ref.at[:ROWS, :wide]),
        fetch(12, h1_any, fa_ref.at[:ROWS]), fetch(4, x_any, x_ref), fetch(5, att_any, att_ref), fetch(13, w2_any, wf_ref.at[:, :, :, :early]),
    ]
    links.greet(later=True)

    def weight(start, size):
        return wf_ref[:, :, :, pl.ds(start, size)].reshape(D, size)

    first, second = slice(0, wide), slice(wide, hidden)
    grads = [dg_ref.at[:, :, :, first], du_ref.at[:, :, :, first], dg_ref.at[:, :, :, second], du_ref.at[:, :, :, second],
             db_ref, do_ref] + [wf_ref.at[:, :, :, i * D : (i + 1) * D] for i in range(3)] + [dc_ref]
    totals = [og_ref.at[:, first], ou_ref.at[:, first], og_ref.at[:, second], ou_ref.at[:, second],
              od_ref, oo_ref] + [op_ref.at[:, i * D : (i + 1) * D] for i in range(3)] + [oc_ref]
    tasks = [
        (AcrossFirst if i in ACROSS_FIRST else Reduction)(
            links, grads[i], totals[i], mine_ref if i == kinds - 1 else None,
            crecv[i], yrecv[i], zrecv[i], xrecv[i], stages[i], sems, i,
        )
        for i in range(kinds)
    ]
    for number, i in enumerate(ACROSS_FIRST):
        tasks[i].third, tasks[i].stage_two = extra[2 * number], extra[2 * number + 1]
    returns = (Return(links, y_ref, ry_ref, sems, 0), Return(links, gres_ref, rg_ref, sems, 1))
    gains = gc_ref[...]
    gain = gains[2:3]
    valid = valid_column(tab_ref, rank)
    h1_ref, dv_ref = fa_ref, fa_ref
    tiles = hidden // FF_TILE
    half = tiles // 2
    kept = {}

    def enter():
        for load in load_first:
            load.wait()
        for tile in range(TILES):
            rows = pl.ds(tile * QT, QT)
            gres_ref[rows, :] = (ga_ref[rows, :].astype(F32) * valid[tile * QT : (tile + 1) * QT]).astype(BF16)

    def first_half():
        def step(tile, carry):
            cols = pl.ds(pl.multiple_of(tile * FF_TILE, FF_TILE), FF_TILE)
            back = mm_cols(gres_ref[...], wd_ref[cols, :])
            b1_ref[:ROWS, cols] = (back * b1_ref[:ROWS, cols].astype(F32)).astype(BF16)
            b2_ref[:ROWS, cols] = (back * b2_ref[:ROWS, cols].astype(F32)).astype(BF16)
            return carry

        lax.fori_loop(0, half, step, 0)
        load_products.wait()

    def second_half():
        for load in load_rest:
            load.wait()

        def step(tile, carry):
            at = pl.multiple_of(tile * FF_TILE, FF_TILE)
            cols = pl.ds(at, FF_TILE)
            normed = n_ref[:ROWS, :]
            gate = mm(normed, weight(early - wide + at, FF_TILE))
            up = mm(normed, weight(early + at, FF_TILE))
            back = mm_cols(gres_ref[...], wd_ref[cols, :])
            act, slope = gelu_both(gate)
            b0_ref[:ROWS, cols] = (act * up).astype(BF16)
            b1_ref[:ROWS, cols] = (back * up * slope).astype(BF16)
            b2_ref[:ROWS, cols] = (back * act).astype(BF16)
            return carry

        lax.fori_loop(half, tiles, step, 0)

    def outer_products(ref, right_ref, begin, end):
        def step(tile, carry):
            cols = pl.ds(pl.multiple_of(tile * FF_TILE, FF_TILE), FF_TILE)
            value = mm(ntt_ref[...], right_ref[:ROWS, cols]).astype(BF16)
            ref[:, :, :, cols] = value.reshape(outer, inner, part, FF_TILE)
            return carry

        lax.fori_loop(begin, end, step, 0)

    def down_products():
        def step(tile, carry):
            cols = pl.ds(pl.multiple_of(tile * FF_TILE, FF_TILE), FF_TILE)
            db_ref[tile // inner, tile % inner] = mm_rows(b0_ref[:ROWS, cols], gres_ref[...]).astype(BF16)
            return carry

        lax.fori_loop(0, tiles, step, 0)

    def outward():
        def step(tile, carry):
            cols = pl.ds(pl.multiple_of(tile * group, 128), group)
            value = h1_ref[:ROWS, cols] + mm(b0_ref[:ROWS, :hidden], wd_ref[:, cols])
            y_ref[:, cols] = (value * valid).astype(BF16)
            shards = pl.ds(tile * (4 // inner), 4 // inner)
            total = None
            for number, (ref, low) in enumerate(((b1_ref, 0), (b2_ref, 0), (b1_ref, wide), (b2_ref, wide))):
                at = D + number * wide
                term = mm_cols(
                    ref[:ROWS, low : low + wide], wf_ref[shards, :, :, at : at + wide].reshape(group, wide)
                )
                total = term if total is None else total + term
            gh_ref[:, cols] = total
            return carry

        lax.fori_loop(0, D // group, step, 0)

    def load():
        kept["qkv"] = fetch(14, qkv_any, b1_ref)
        kept["wqkv"] = fetch(15, wqkv_any, b2_ref)

    def middle():
        gain_grad = jnp.zeros((1, D), F32)
        for tile in range(TILES):
            rows = pl.ds(tile * QT, QT)
            value, grad = h1_ref[rows, :], gh_ref[rows, :]
            root = lax.rsqrt(mean_square(value) + EPSILON)
            unit = value * root
            gain_grad = gain_grad + jnp.sum(grad * unit, axis=0, keepdims=True)
            grad = grad * gain
            grad = gres_ref[rows, :].astype(F32) + root * (
                grad - unit * jnp.mean(grad * unit, axis=-1, keepdims=True)
            )
            gh_ref[rows, :] = grad
            low = grad.astype(BF16)
            n_ref[rows, :] = low
            ga_ref[rows, :] = mm_cols(low, weight(0, D)).astype(BF16)
        kept["gain"] = gain_grad

    def out_products():
        def step(tile, carry):
            cols = pl.ds(pl.multiple_of(tile * QUAD, QUAD), QUAD)
            value = mm_rows(att_ref[...], n_ref[:ROWS, cols]).astype(BF16)
            do_ref[:, :, :, cols] = value.reshape(outer, inner, part, QUAD)
            return carry

        lax.fori_loop(0, D // QUAD, step, 0)
        kept["n"] = fetch(6, n_any, n_ref)

    def attention(quad):
        if quad == 0:
            backward_attention_start(dk_ref, dv_ref)
            kept["qkv"].wait()
        backward_attention_quad(tab_ref, rank, b1_ref, att_ref, ga_ref, lse_ref, b0_ref, dk_ref, dv_ref, quad)

    def project_products(quad):
        if quad == 0:
            kept["n"].wait()
        for number in range(3):
            value = mm_rows(n_ref[...], b0_ref[:, number * D + quad * QUAD : number * D + (quad + 1) * QUAD])
            low = (quad * 3 + number) * QUAD
            wf_ref[:, :, :, low : low + QUAD] = value.astype(BF16).reshape(outer, inner, part, QUAD)

    def input_gradient():
        kept["wqkv"].wait()
        kept["one"], kept["side"] = backward_project(
            tab_ref, rank, x_ref, gh_ref, gains, n_ref, b0_ref, b2_ref, dk_ref, gres_ref
        )

    def gain_pieces():
        rows = jnp.concatenate([kept["one"], kept["side"], kept["gain"], jnp.zeros((5, D), F32)], axis=0)
        spread_gain_grads(rows, dc_ref)

    work = {
        "start": lambda: None, "load": load, "P0": enter, "P1a": first_half, "P1b": second_half,
        "gA": lambda: outer_products(dg_ref, b1_ref, 0, half), "gB": lambda: outer_products(dg_ref, b1_ref, half, tiles),
        "uA": lambda: outer_products(du_ref, b2_ref, 0, half), "uB": lambda: outer_products(du_ref, b2_ref, half, tiles),
        "d": down_products, "out": outward, "P4": middle, "P5": out_products,
        "q0": lambda: attention(0), "q1": lambda: attention(1), "q2": lambda: attention(2),
        "p0": lambda: project_products(0), "p1": lambda: project_products(1), "p2": lambda: project_products(2),
        "bp": input_gradient, "dc": gain_pieces,
    }
    paired, begun = set(), set()
    for action, which, *turn in REAR_ORDER:
        if action == "do":
            work[which]()
        elif action == "begin":
            if not begun:
                links.met()
            begun.add(which)
            if which == 6:
                pl.semaphore_wait(free_sem, 1)
            tasks[which].begin()
        elif action == "pair":
            tasks[which].pair()
            paired.add(which)
            if which < 3 and paired >= {0, 1, 2}:
                pl.semaphore_signal(free_sem, inc=1, device_id={"rep": links.mate}, device_id_type=MESH)
        elif action == "meet":
            tasks[which].meet()
        elif action == "col":
            tasks[which].column()
        elif action == "hop":
            tasks[which].hop(turn[0])
        elif action == "cross":
            tasks[which].cross()
        elif action == "fin":
            tasks[which].finish()
        elif action == "rows":
            returns[which].begin()
        else:
            returns[which].relay()
    for one in returns:
        one.settle()
    for task in tasks:
        task.settle()
    links.drain()


def feed_and_reduce(count, table, x, att, lse, gc, cot, n, qkv, wqkv, w2, wf, wd, *firsts):
    outer, inner = grid_of(count)
    part, tall = D // count, wd.shape[1]
    hidden = count * tall
    wf = wf.reshape((outer, inner) + wf.shape[1:])
    w2 = w2.reshape(outer, inner, part, -1)
    full = [(part, hidden), (part, hidden), (tall, D), (part, D), (part, 3 * D), (8, 128)]
    shapes = [(part, hidden // 2)] * 4 + [(tall, D)] + [(part, D)] * 4 + [(8, 128)]
    kinds = len(shapes)
    dtypes = [BF16] * (kinds - 1) + [F32]
    halved = [(a, b // 2 if b % 256 == 0 else b) for a, b in shapes]
    later = [(a // 2, b) if i in ACROSS_FIRST else (a, b) for i, (a, b) in enumerate(halved)]
    dma, vmem = pltpu.SemaphoreType.DMA, pltpu.VMEM
    scratch = [
        vmem((ROWS, D), BF16), vmem((ROWS, D), F32), vmem((ALL_ROWS, D), F32), vmem((ALL_ROWS, D), F32),
        vmem((ALL_ROWS, 3 * D), BF16), vmem((ALL_ROWS, 3 * D), BF16), vmem((D, 3 * D), BF16),
        vmem((ALL_ROWS, D), BF16), vmem((D, ROWS), BF16), vmem((ROWS, D), BF16), vmem((ROWS, D), BF16),
        vmem((ROWS, D), BF16), vmem((ROWS, D), BF16),
        vmem((outer, inner, part, D + 2 * hidden), BF16), vmem((hidden, D), BF16),
    ]
    scratch += [vmem((outer, inner) + shape, BF16) for shape in full[:4]]
    scratch += [vmem((outer, inner) + full[-1], F32)] * 2
    scratch += [vmem((outer, inner) + halved[i], dtypes[i]) for i in (0, 1, 2, 3, 4, 5, 9)]
    for lead in ((outer,), (outer + 1,), ()):
        for i in range(kinds):
            across = (outer, inner) if i in ACROSS_FIRST and lead == () else lead
            scratch.append(vmem(across + later[i], dtypes[i]))
    scratch += [vmem(shape, F32) for shape in later]
    for i in ACROSS_FIRST:
        scratch += [vmem(later[i], BF16), vmem(later[i], F32)]
    one = dma((kinds,))
    scratch += [one, one, one, one, one, dma((2, outer, kinds)), dma((outer + 1, kinds))] + [one] * 9
    scratch += [dma((2, 3)), dma((2, 3)), dma((2,)), dma((1,)), dma((16,)), pltpu.SemaphoreType.REGULAR]
    rows = jax.ShapeDtypeStruct((4, ROWS, D), BF16)
    outs = pl.pallas_call(
        partial(rear_kernel, outer, inner),
        out_shape=tuple(jax.ShapeDtypeStruct(shape, F32) for shape in full) + (rows, rows),
        in_specs=[SMEM] + [ANY] * 2 + [VMEM] * 2 + [ANY] * 13,
        out_specs=(ANY,) * 8,
        scratch_shapes=scratch,
        compiler_params=pltpu.CompilerParams(
            collective_id=2, has_side_effects=True, vmem_limit_bytes=67043328
        ),
        name="feed_and_reduce",
    )(table, x, att, lse, gc, cot, n, qkv, wqkv, w2, wf, wd.reshape(hidden, D), *firsts)
    return outs[:6], outs[6], outs[7]


def place_kernel(tab_ref, ry_ref, rg_ref, og_ref, ou_ref, od_ref, oo_ref, op_ref, oc_ref, *refs):
    (y_ref, g_ref, q_out, k_out, v_out, o_out, g_out, u_out, d_out, gains_out), refs = refs[:10], refs[10:]
    (y_buf, g_buf, zero, bg, bu, bd, bo, bp, sem_in, sem_out, sem_rows, sem_home) = refs
    blocks = y_buf.shape[0]
    base = lax.axis_index("rep") * blocks
    tables = ((og_ref, bg), (ou_ref, bu), (od_ref, bd), (oo_ref, bo), (op_ref, bp))
    reads = [pltpu.make_async_copy(src, dst, sem_in.at[i]) for i, (src, dst) in enumerate(tables)]
    rows = ((ry_ref, y_buf, y_ref), (rg_ref, g_buf, g_ref))

    for read in reads:
        read.start()
    zero[...] = jnp.zeros(zero.shape, zero.dtype)

    def fetch(block, carry):
        index = tab_ref[48, base + block]
        safe = jnp.maximum(index, 0)
        for kind, (src, buf, dst) in enumerate(rows):
            @pl.when(index >= 0)
            def _():
                pltpu.make_async_copy(
                    src.at[lax.div(safe, SLOTS), lax.rem(safe, SLOTS)], buf.at[block], sem_rows.at[kind, block]
                ).start()

            @pl.when(index < 0)
            def _():
                pltpu.make_async_copy(zero, dst.at[block], sem_home.at[kind, block]).start()

        return carry

    lax.fori_loop(0, blocks, fetch, 0)
    gains_out[...] = oc_ref[...]
    writes = []
    for number, (buf, dst) in enumerate(((bg, g_out), (bu, u_out), (bd, d_out), (bo, o_out))):
        reads[number].wait()
        writes.append(pltpu.make_async_copy(buf, dst, sem_out.at[number]))
        writes[-1].start()
    reads[4].wait()
    for quad in range(D // QUAD):
        for number, dst in enumerate((q_out, k_out, v_out)):
            low = (3 * quad + number) * QUAD
            copy = pltpu.make_async_copy(
                bp.at[:, low : low + QUAD], dst.at[:, quad * QUAD : (quad + 1) * QUAD], sem_out.at[4 + 3 * quad + number]
            )
            copy.start()
            writes.append(copy)
    def leave(block, carry):
        @pl.when(tab_ref[48, base + block] >= 0)
        def _():
            for kind, (src, buf, dst) in enumerate(rows):
                pltpu.make_async_copy(src.at[0, 0], buf.at[block], sem_rows.at[kind, block]).wait()
                pltpu.make_async_copy(buf.at[block], dst.at[block], sem_home.at[kind, block]).start()

        return carry

    lax.fori_loop(0, blocks, leave, 0)
    for write in writes:
        write.wait()

    def rest(block, carry):
        for kind, (_, buf, dst) in enumerate(rows):
            pltpu.make_async_copy(buf.at[block], dst.at[block], sem_home.at[kind, block]).wait()
        return carry

    lax.fori_loop(0, blocks, rest, 0)


def place_all(table, ry, rg, totals, blocks, part, shape):
    out = jax.ShapeDtypeStruct
    og, ou, od, oo, op, oc = totals
    block = (blocks,) + ry.shape[2:]
    dma, vmem = pltpu.SemaphoreType.DMA, pltpu.VMEM
    y, g, q, k, v, o, gate, up, down, gains = pl.pallas_call(
        place_kernel,
        out_shape=(out(block, ry.dtype), out(block, rg.dtype), out(oo.shape, F32), out(oo.shape, F32), out(oo.shape, F32),
                   out(oo.shape, F32), out(og.shape, F32), out(ou.shape, F32), out(od.shape, F32), out(oc.shape, F32)),
        in_specs=[SMEM] + [ANY] * 7 + [VMEM],
        out_specs=(ANY,) * 9 + (VMEM,),
        scratch_shapes=[vmem(block, ry.dtype), vmem(block, rg.dtype), vmem(block[1:], ry.dtype)] + [vmem(t.shape, F32) for t in totals[:5]]
        + [dma((5,)), dma((13,)), dma((2, blocks)), dma((2, blocks))],
        compiler_params=pltpu.CompilerParams(vmem_limit_bytes=VMEM_LIMIT),
        name="place_outputs",
    )(table, ry, rg, og, ou, od, oo, op, oc)
    return (y.reshape(shape), g.reshape(shape), gains[0, :part], gains[1, :part], q, k, v, o, gains[2, :part], gate, up, down)


def per_device(count, layer_input, cotangent, lengths, attn_gain, global_gain, query_weight, key_weight,
               value_weight, out_weight, ffn_gain, gate_weight, up_weight, down_weight):
    micro, span, width = layer_input.shape
    hidden = gate_weight.shape[1]
    blocks = micro * span // BLK
    part = attn_gain.shape[0]
    rows_in = layer_input.reshape(blocks, BLK, width)
    cots_in = cotangent.reshape(blocks, BLK, width)
    weights = (query_weight, key_weight, value_weight, out_weight, gate_weight, up_weight)
    gains = (attn_gain, global_gain, ffn_gain)
    wc = jnp.pad(jnp.stack(gains), ((0, 13), (0, 128 - part)))
    if grid_of(count)[1] == 2 and part % 16 == 0:
        lens = lax.dynamic_update_slice(
            jnp.zeros((8, 128), jnp.int32), lengths.reshape(1, blocks), (0, lax.axis_index("rep") * blocks)
        )
        table, gains, x, cot, n, qkv, att, lse, wqkv, w2, *firsts, ga, gb = gather_and_attend(
            count, lens, rows_in, cots_in, weights, down_weight, wc
        )
        totals, ry, rg = feed_and_reduce(count, table, x, att, lse, gains, cot, n, qkv, wqkv, w2, ga, gb, *firsts)
        ry, rg = (rows.reshape(4, SLOTS, BLK, width) for rows in (ry, rg))
        return place_all(table, ry, rg, totals, blocks, part, layer_input.shape)
    else:
        table = deal_table(lengths)
        splits = ((0, 4 * width), (4 * width, 2 * hidden))
        ga, gb, gc, rows, cots = gather_weights(
            count, splits, table, rows_in, cots_in, jnp.concatenate(weights, axis=1), down_weight, wc
        )
        x, full = rows.reshape(ROWS, width), ga.reshape(width, -1)
        n, qkv, att, lse = attend(table, x, gc, full)
        y, gh, gatt, dg, du, db, do, gain = feed(
            table, x, cots.reshape(ROWS, width), att, gc, full, gb.reshape(-1, width)
        )
        g, dw, dc = backward_layer(table, x, gh, gatt, att, lse, n, qkv, gain, gc, full)
        grads = [grad.reshape(count, -1, grad.shape[-1]) for grad in (dg, du, db, do, dw, dc)]
        og, ou, ob, oo, ow, oc, ry, rg = reduce_grads(
            count, grads, y.reshape(SLOTS, BLK, width), g.reshape(SLOTS, BLK, width)
        )
        oq, ok, ov = ow[:, :width], ow[:, width : 2 * width], ow[:, 2 * width :]
    y_home, g_home = bring_home(table, ry, rg, blocks)
    return (
        y_home.reshape(layer_input.shape), g_home.reshape(layer_input.shape),
        oc[0, :part], oc[1, :part], oq, ok, ov, oo, oc[2, :part], og, ou, ob,
    )


def solution(mesh):
    rows = P(None, ("rep", "fsdp"), None)
    vector, matrix = P("fsdp"), P("fsdp", None)
    return jax.shard_map(
        partial(per_device, mesh.shape["fsdp"]),
        mesh=mesh,
        in_specs=(rows, rows, P(None, ("rep", "fsdp")), vector, vector, matrix, matrix, matrix, matrix,
                  vector, matrix, matrix, matrix),
        out_specs=(rows, rows, vector, vector, matrix, matrix, matrix, matrix, vector, matrix, matrix, matrix),
        check_vma=False,
    )
```

```python
from functools import partial

import jax
import jax.numpy as jnp
from jax import lax
from jax.experimental import pallas as pl
from jax.experimental.pallas import tpu as pltpu
from jax.sharding import PartitionSpec as P

H = 12
DH = 64
RADIUS = 127
GBLK = 16
BLK = 64
SLOTS = 10
MAX_SEQ_BLOCKS = 5
EPSILON = 1e-06
MASKED_SCORE = -1e30
MESH = pl.DeviceIdType.MESH
VMEM_LIMIT = 60 * 1024 * 1024
SEG_AT, LEN_AT, DEST_AT, TABLE_SIZE = 40, 80, 120, 256

ANY = pl.BlockSpec(memory_space=pl.ANY)
VMEM = pl.BlockSpec(memory_space=pltpu.VMEM)
SMEM = pl.BlockSpec(memory_space=pltpu.SMEM)


def grid_of(count):
    inner = 2 if count <= 8 else 4
    return count // inner, inner


def core_of(rank):
    return rank + 1 - 2 * (rank % 2)


def across_of(rank):
    return (rank + 2) % 4


def lens_kernel(lens_ref, all_ref, send_sem, recv_sem):
    rank = lax.axis_index("rep")
    barrier = pltpu.get_barrier_semaphore()
    for step in range(1, 4):
        pl.semaphore_signal(
            barrier, inc=1, device_id={"rep": (rank + step) % 4}, device_id_type=MESH
        )
    pl.semaphore_wait(barrier, 3)
    copies = []
    for step in range(1, 4):
        copy = pltpu.make_async_remote_copy(
            src_ref=lens_ref,
            dst_ref=all_ref.at[rank],
            send_sem=send_sem.at[step - 1],
            recv_sem=recv_sem.at[step - 1],
            device_id={"rep": (rank + step) % 4},
            device_id_type=MESH,
        )
        copy.start()
        copies.append(copy)
    all_ref[rank] = lens_ref[...]
    for copy in copies:
        copy.wait()


def table_kernel(micro, per_dev, lens_ref, tab_ref, order_ref, count_ref, load_ref):
    total = 4 * micro * per_dev

    def length_at(spot):
        return lens_ref[spot // (micro * per_dev), (spot // per_dev) % micro, spot % per_dev]

    def blocks_of(length):
        return (length + (BLK - 1)) // BLK

    def clear(spot, carry):
        tab_ref[spot] = -1
        return carry

    lax.fori_loop(0, TABLE_SIZE, clear, 0)
    for spot in range(4 * SLOTS):
        tab_ref[LEN_AT + spot] = 0
    for size in range(8):
        count_ref[size] = 0
    for dev in range(4):
        load_ref[dev] = 0

    def tally(spot, carry):
        length = length_at(spot)

        @pl.when(length > 0)
        def _():
            size = blocks_of(length)
            count_ref[size] = count_ref[size] + 1

        return carry

    lax.fori_loop(0, total, tally, 0)
    begin = 0
    for size in range(MAX_SEQ_BLOCKS, 0, -1):
        amount = count_ref[size]
        count_ref[size] = begin
        begin = begin + amount

    def place(spot, carry):
        length = length_at(spot)

        @pl.when(length > 0)
        def _():
            size = blocks_of(length)
            where = count_ref[size]
            order_ref[where] = spot
            count_ref[size] = where + 1

        return carry

    lax.fori_loop(0, total, place, 0)

    def assign(number, carry):
        spot = order_ref[number]
        length = length_at(spot)
        size = blocks_of(length)
        best = jnp.int32(0)
        low = load_ref[0]
        for dev in range(1, 4):
            here = load_ref[dev]
            best = jnp.where(here < low, dev, best)
            low = jnp.minimum(here, low)
        load_ref[best] = low + size

        def put(step, inner):
            slot = best * SLOTS + low + step
            tab_ref[slot] = spot + step
            tab_ref[SEG_AT + slot] = low
            tab_ref[LEN_AT + slot] = jnp.minimum(length - BLK * step, BLK)
            tab_ref[DEST_AT + spot + step] = slot
            return inner

        lax.fori_loop(0, size, put, 0)
        return carry

    lax.fori_loop(0, begin, assign, 0)


def deal_table(lengths):
    micro, per_dev = lengths.shape
    padded = jnp.pad(lengths, ((0, 8 - micro), (0, 128 - per_dev)))
    everyone = pl.pallas_call(
        lens_kernel,
        out_shape=jax.ShapeDtypeStruct((4, 8, 128), jnp.int32),
        in_specs=[VMEM],
        out_specs=VMEM,
        scratch_shapes=[pltpu.SemaphoreType.DMA((3,)), pltpu.SemaphoreType.DMA((3,))],
        compiler_params=pltpu.CompilerParams(collective_id=0, has_side_effects=True),
        name="lens_exchange",
    )(padded)
    return pl.pallas_call(
        partial(table_kernel, micro, per_dev),
        out_shape=jax.ShapeDtypeStruct((TABLE_SIZE,), jnp.int32),
        in_specs=[SMEM],
        out_specs=SMEM,
        scratch_shapes=[
            pltpu.SMEM((4 * micro * per_dev,), jnp.int32),
            pltpu.SMEM((8,), jnp.int32),
            pltpu.SMEM((4,), jnp.int32),
        ],
        name="deal_table",
    )(everyone)


def gather_kernel(
    outer, inner, splits, tab_ref, rows_ref, cots_ref, wa_ref, wb_ref, wc_ref,
    ga_ref, gb_ref, gc_ref, rows_out, cots_out,
    psend, precv, xsend, xrecv,
    z_send, z_recv, y_send, y_recv, c_send, c_recv, own_sem,
    p_send, p_recv, x_send, x_recv,
):
    rank = lax.axis_index("rep")
    spot = lax.axis_index("fsdp")
    core = rank % 2
    row, col = spot // inner, spot % inner
    count = outer * inner
    mate, across = core_of(rank), across_of(rank)
    pieces = [(wa_ref, ga_ref, start, width // 2) for start, width in splits]
    pieces.append((wb_ref, gb_ref, 0, wb_ref.shape[1] // 2))
    pieces.append((wc_ref, gc_ref, 0, None))
    halved = [number for number, piece in enumerate(pieces) if piece[3] is not None]

    barrier = pltpu.get_barrier_semaphore()
    neighbours = (
        (row + 1 < outer, {"fsdp": spot + inner}),
        (row > 0, {"fsdp": spot - inner}),
        (col + 1 < inner, {"fsdp": spot + 1}),
        (col > 0, {"fsdp": spot - 1}),
    )
    amount = jnp.int32(2)
    for there, device in neighbours:
        amount = amount + there.astype(jnp.int32)

        @pl.when(there)
        def _():
            pl.semaphore_signal(barrier, inc=1, device_id=device, device_id_type=MESH)

    for device in (mate, across):
        pl.semaphore_signal(barrier, inc=1, device_id={"rep": device}, device_id_type=MESH)
    pl.semaphore_wait(barrier, amount)

    def cut(ref, number):
        _, _, start, half = pieces[number]
        if half is None:
            return ref
        return ref.at[:, pl.ds(pl.multiple_of(start + core * half, 128), half)]

    def landed(number, shard):
        return cut(pieces[number][1].at[shard], number)

    late = []

    def send(there, src, dst, ssem, rsem, device):
        def describe():
            return pltpu.make_async_remote_copy(
                src_ref=src, dst_ref=dst, send_sem=ssem, recv_sem=rsem,
                device_id=device, device_id_type=MESH,
            )

        if there is None:
            describe().start()
            late.append((None, lambda: describe().wait_send()))
        else:
            @pl.when(there)
            def _():
                describe().start()

            late.append((there, lambda: describe().wait_send()))

    def arrive(number, shard, rsem):
        pltpu.make_async_remote_copy(
            src_ref=landed(number, shard), dst_ref=landed(number, shard),
            send_sem=own_sem.at[0], recv_sem=rsem,
            device_id={"rep": mate}, device_id_type=MESH,
        ).wait_recv()

    def both(first, second):
        return second if first is None else jnp.logical_and(first, second)

    def to_mate(there, number, shard):
        if number not in halved:
            return
        place = landed(number, shard)
        send(there, place, place, c_send.at[number, shard], c_recv.at[number, shard], {"rep": mate})

    def along_row(there, number, line, src):
        shard = line * inner + col
        place = landed(number, shard)
        src = place if src is None else src
        send(both(there, col + 1 < inner), src, place,
             y_send.at[0, 0, line, number], y_recv.at[0, 0, line, number], {"fsdp": spot + 1})
        send(both(there, col > 0), src, place,
             y_send.at[1, 0, line, number], y_recv.at[1, 0, line, number], {"fsdp": spot - 1})

    def from_row(there, number, line):
        for step in range(inner - 1):
            for way, source, onward, target in (
                (0, col - 1 - step, col + 1 < inner, spot + 1),
                (1, col + 1 + step, col > 0, spot - 1),
            ):
                here = jnp.logical_and(source >= 0, source < inner)
                here = both(there, here)
                shard = line * inner + source

                @pl.when(here)
                def _():
                    arrive(number, shard, y_recv.at[way, step, line, number])

                if step + 1 < inner - 1:
                    place = landed(number, shard)
                    send(both(here, onward), place, place,
                         y_send.at[way, step + 1, line, number],
                         y_recv.at[way, step + 1, line, number], {"fsdp": target})
                to_mate(here, number, shard)

    for number, piece in enumerate(pieces):
        src, place = cut(piece[0], number), landed(number, spot)
        send(row + 1 < outer, src, place, z_send.at[0, 0, number], z_recv.at[0, 0, number],
             {"fsdp": spot + inner})
        send(row > 0, src, place, z_send.at[1, 0, number], z_recv.at[1, 0, number],
             {"fsdp": spot - inner})
        along_row(None, number, row, src)
    own = [
        pltpu.make_async_copy(wa_ref, ga_ref.at[spot], own_sem.at[0]),
        pltpu.make_async_copy(wb_ref, gb_ref.at[spot], own_sem.at[1]),
        pltpu.make_async_copy(wc_ref, gc_ref.at[spot], own_sem.at[2]),
    ]
    for copy in own:
        copy.start()

    sources = (rows_ref, cots_ref)
    per_rank = rows_ref.shape[0]

    def picked(kind, target, slot):
        index = tab_ref[target * SLOTS + slot] - rank * per_rank
        mine = jnp.logical_and(index >= 0, index < per_rank)
        value = sources[kind][jnp.clip(index, 0, per_rank - 1)]
        return mine, value

    def mate_copy(kind, part):
        return pltpu.make_async_remote_copy(
            src_ref=psend.at[kind, part], dst_ref=precv.at[kind, part],
            send_sem=p_send.at[kind, part], recv_sem=p_recv.at[kind, part],
            device_id={"rep": mate}, device_id_type=MESH,
        )

    def across_copy(kind):
        return pltpu.make_async_remote_copy(
            src_ref=xsend.at[kind], dst_ref=xrecv.at[kind],
            send_sem=x_send.at[kind], recv_sem=x_recv.at[kind],
            device_id={"rep": across}, device_id_type=MESH,
        )

    for kind, part in ((0, 1), (1, 1), (0, 0), (1, 0)):
        target = mate if part == 0 else across_of(mate)

        def pack(slot, carry):
            mine, value = picked(kind, target, slot)
            psend[kind, part, slot] = jnp.where(mine, value, jnp.zeros_like(value))
            return carry

        lax.fori_loop(0, SLOTS, pack, 0)
        mate_copy(kind, part).start()
    for kind in range(2):
        mate_copy(kind, 1).wait_recv()

        def merge(slot, carry):
            mine, value = picked(kind, across, slot)
            xsend[kind, slot] = jnp.where(mine, value, precv[kind, 1, slot])
            return carry

        lax.fori_loop(0, SLOTS, merge, 0)
        across_copy(kind).start()

    def lines(step):
        return ((row - 1 - step >= 0, row - 1 - step, 0, row + 1 < outer, spot + inner),
                (row + 1 + step < outer, row + 1 + step, 1, row > 0, spot - inner))

    for step in range(outer - 1):
        for number in range(len(pieces)):
            for here, line, way, onward, target in lines(step):
                shard = line * inner + col

                @pl.when(here)
                def _():
                    arrive(number, shard, z_recv.at[way, step, number])

                if step + 1 < outer - 1:
                    place = landed(number, shard)
                    send(jnp.logical_and(here, onward), place, place,
                         z_send.at[way, step + 1, number], z_recv.at[way, step + 1, number],
                         {"fsdp": target})
                along_row(here, number, line, None)
                to_mate(here, number, shard)
        for number in range(len(pieces)):
            if step == 0:
                from_row(None, number, row)
            else:
                for here, line, *_ in lines(step - 1):
                    from_row(here, number, line)
    for number in range(len(pieces)):
        for here, line, *_ in lines(outer - 2):
            from_row(here, number, line)

    outs = (rows_out, cots_out)
    for kind in range(2):
        mate_copy(kind, 0).wait_recv()
        across_copy(kind).wait_recv()

        def finish(slot, carry):
            mine, value = picked(kind, rank, slot)
            outs[kind][slot] = jnp.where(mine, value, precv[kind, 0, slot] + xrecv[kind, slot])
            return carry

        lax.fori_loop(0, SLOTS, finish, 0)

    for shard in range(count):
        @pl.when(shard != spot)
        def _():
            for number in halved:
                other = pieces[number]
                view = other[1].at[shard].at[:, pl.ds(0, other[3])]
                pltpu.make_async_remote_copy(
                    src_ref=view, dst_ref=view, send_sem=own_sem.at[0],
                    recv_sem=c_recv.at[number, shard],
                    device_id={"rep": mate}, device_id_type=MESH,
                ).wait_recv()
    for there, finish_send in late:
        if there is None:
            finish_send()
        else:
            pl.when(there)(finish_send)
    for kind in range(2):
        for part in range(2):
            mate_copy(kind, part).wait_send()
        across_copy(kind).wait_send()
    for copy in own:
        copy.wait()


def gather_weights(count, splits, table, rows, cots, wa, wb, wc):
    outer, inner = grid_of(count)
    block = rows.shape[1:]
    kinds = len(splits) + 2
    dma = pltpu.SemaphoreType.DMA
    bf16 = jnp.bfloat16
    return pl.pallas_call(
        partial(gather_kernel, outer, inner, splits),
        out_shape=(
            jax.ShapeDtypeStruct((count,) + wa.shape, bf16),
            jax.ShapeDtypeStruct((count,) + wb.shape, bf16),
            jax.ShapeDtypeStruct((count,) + wc.shape, bf16),
            jax.ShapeDtypeStruct((SLOTS,) + block, bf16),
            jax.ShapeDtypeStruct((SLOTS,) + block, bf16),
        ),
        in_specs=[SMEM, VMEM, VMEM, VMEM, VMEM, VMEM],
        out_specs=(ANY, ANY, ANY, VMEM, VMEM),
        scratch_shapes=[
            pltpu.VMEM((2, 2, SLOTS) + block, bf16),
            pltpu.VMEM((2, 2, SLOTS) + block, bf16),
            pltpu.VMEM((2, SLOTS) + block, bf16),
            pltpu.VMEM((2, SLOTS) + block, bf16),
            dma((2, outer - 1, kinds)), dma((2, outer - 1, kinds)),
            dma((2, inner - 1, outer, kinds)), dma((2, inner - 1, outer, kinds)),
            dma((kinds, count)), dma((kinds, count)), dma((3,)),
            dma((2, 2)), dma((2, 2)), dma((2,)), dma((2,)),
        ],
        compiler_params=pltpu.CompilerParams(
            collective_id=1, has_side_effects=True, vmem_limit_bytes=VMEM_LIMIT
        ),
        name="gather_and_deal",
    )(table, rows, cots, wa, wb, wc)


def reduce_kernel(
    outer, inner, kinds, *refs
):
    grads, (y_ref, g_ref) = refs[:kinds], refs[kinds : kinds + 2]
    totals, (ry_ref, rg_ref) = refs[kinds + 2 : 2 * kinds + 2], refs[2 * kinds + 2 : 2 * kinds + 4]
    scratch = refs[2 * kinds + 4 :]
    mines, crecvs, yrecvs, zrecvs, xrecvs = (
        scratch[kinds * i : kinds * (i + 1)] for i in range(5)
    )
    (c_send, c_recv, m_sem, y_send, y_recv, z_send, z_recv, x_send, x_recv, f_send, f_recv,
     r_send, r_recv, q_sem) = scratch[5 * kinds :]
    rank = lax.axis_index("rep")
    spot = lax.axis_index("fsdp")
    core = rank % 2
    row, col = spot // inner, spot % inner
    mate, across = core_of(rank), across_of(rank)
    pieces = [(src, dst, 0, src.shape[3] // 2) for src, dst in zip(grads[:-1], totals)]
    pieces.append((grads[-1], totals[-1], 0, None))

    barrier = pltpu.get_barrier_semaphore()
    neighbours = (
        (row + 1 < outer, {"fsdp": spot + inner}),
        (row > 0, {"fsdp": spot - inner}),
        (col + 1 < inner, {"fsdp": spot + 1}),
        (col > 0, {"fsdp": spot - 1}),
    )
    amount = jnp.int32(2)
    for there, device in neighbours:
        amount = amount + there.astype(jnp.int32)

        @pl.when(there)
        def _():
            pl.semaphore_signal(barrier, inc=1, device_id=device, device_id_type=MESH)

    for device in (mate, across):
        pl.semaphore_signal(barrier, inc=1, device_id={"rep": device}, device_id_type=MESH)
    pl.semaphore_wait(barrier, amount)

    late = []

    def send(there, src, dst, ssem, rsem, device):
        def describe():
            return pltpu.make_async_remote_copy(
                src_ref=src, dst_ref=dst, send_sem=ssem, recv_sem=rsem,
                device_id=device, device_id_type=MESH,
            )

        if there is None:
            describe().start()
            late.append((None, lambda: describe().wait_send()))
        else:
            @pl.when(there)
            def _():
                describe().start()

            late.append((there, lambda: describe().wait_send()))

    def arrive(place, rsem):
        pltpu.make_async_remote_copy(
            src_ref=place, dst_ref=place, send_sem=q_sem.at[0], recv_sem=rsem,
            device_id={"rep": mate}, device_id_type=MESH,
        ).wait_recv()

    def columns(ref, number, which):
        _, _, start, half = pieces[number]
        if half is None:
            return ref
        cols = pl.ds(pl.multiple_of(start + which * half, 128), half)
        return ref.at[:, :, :, cols] if len(ref.shape) == 4 else ref.at[:, cols]

    order = list(range(kinds))
    loads = []
    for number in order:
        src = columns(pieces[number][0], number, 1 - core)
        send(None, src, crecvs[number], c_send.at[number], c_recv.at[number], {"rep": mate})
        load = pltpu.make_async_copy(
            columns(pieces[number][0], number, core), mines[number], m_sem.at[number]
        )
        load.start()
        loads.append(load)

    for kind, (src, dst) in enumerate(((y_ref, ry_ref), (g_ref, rg_ref))):
        send(None, src, dst.at[rank], r_send.at[kind, 0], r_recv.at[kind, 0], {"rep": across})
        send(None, src, dst.at[rank], r_send.at[kind, 1], r_recv.at[kind, 1], {"rep": mate})
        pltpu.make_async_copy(src, dst.at[rank], q_sem.at[kind + 1]).start()

    def slot_of(way, size, place, dest):
        if size == 2:
            return 0
        return dest - place if way == 0 else size - place + dest

    def line_sum(number, size, place, stride, buffer, view, ssem, rsem):
        for far in range(size - 1, 0, -1):
            for way in range(2):
                dest = far if way == 0 else size - 1 - far
                step = 1 if way == 0 else -1
                passes = place < dest if way == 0 else place > dest
                first = place == 0 if way == 0 else place == size - 1
                mine = view(dest)
                got = slot_of(way, size, place, dest)

                @pl.when(jnp.logical_and(passes, jnp.logical_not(first)))
                def _():
                    arrive(buffer.at[got], rsem.at[got, number])
                    mine[...] = mine[...] + buffer[got]

                put = slot_of(way, size, place + step, dest)
                send(passes, mine, buffer.at[put], ssem.at[way, dest, number], rsem.at[put, number],
                     {"fsdp": spot + step * stride})
        for way in range(2):
            has = place > 0 if way == 0 else place < size - 1
            got = slot_of(way, size, place, place)
            mine = view(place)

            @pl.when(has)
            def _():
                arrive(buffer.at[got], rsem.at[got, number])
                mine[...] = mine[...] + buffer[got]

    for number in order:
        loads[number].wait()
        arrive(crecvs[number], c_recv.at[number])
        mine, other = mines[number], crecvs[number]

        def add(index, carry):
            mine[index // inner, index % inner] = (
                mine[index // inner, index % inner] + other[index // inner, index % inner]
            )
            return carry

        lax.fori_loop(0, outer * inner, add, 0)
        if inner == 2:
            send(None, mine.at[:, 1 - col], yrecvs[number].at[0], y_send.at[0, 0, number],
                 y_recv.at[0, number], {"fsdp": spot + 1 - 2 * col})
    for kind, dst in enumerate((ry_ref, rg_ref)):
        place = dst.at[across]
        arrive(place, r_recv.at[kind, 0])
        send(None, place, place, r_send.at[kind, 2], r_recv.at[kind, 2], {"rep": mate})
    for number in order:
        mine = mines[number]
        if inner == 2:
            arrive(yrecvs[number].at[0], y_recv.at[0, number])
            buffer = yrecvs[number]

            def add(index, carry):
                mine[index, col] = mine[index, col] + buffer[0, index]
                return carry

            lax.fori_loop(0, outer, add, 0)
        else:
            line_sum(number, inner, col, 1, yrecvs[number], lambda dest: mine.at[:, dest],
                     y_send, y_recv)
        line_sum(number, outer, row, inner, zrecvs[number], lambda dest: mine.at[dest, col],
                 z_send, z_recv)
        send(None, mine.at[row, col], xrecvs[number], x_send.at[number], x_recv.at[number],
             {"rep": across})
    for number in order:
        arrive(xrecvs[number], x_recv.at[number])
        total = mines[number][row, col].astype(jnp.float32) + xrecvs[number][...].astype(jnp.float32)
        out, half = pieces[number][1], pieces[number][3]
        place = columns(out, number, core)
        place[...] = total
        if half is not None:
            send(None, place, place, f_send.at[number], f_recv.at[number], {"rep": mate})
    for number in order:
        if pieces[number][3] is not None:
            arrive(columns(pieces[number][1], number, 1 - core), f_recv.at[number])
    for kind, dst in enumerate((ry_ref, rg_ref)):
        arrive(dst.at[mate], r_recv.at[kind, 1])
        arrive(dst.at[across_of(mate)], r_recv.at[kind, 2])
        src = y_ref if kind == 0 else g_ref
        pltpu.make_async_copy(src, dst.at[rank], q_sem.at[kind + 1]).wait()
    for there, finish_send in late:
        if there is None:
            finish_send()
        else:
            pl.when(there)(finish_send)


def reduce_grads(count, grads, y_rows, g_rows):
    outer, inner = grid_of(count)
    kinds = len(grads)
    shapes = [(grad.shape[1], grad.shape[2] // 2, grad.dtype) for grad in grads[:-1]]
    shapes.append(grads[-1].shape[1:] + (grads[-1].dtype,))
    dma = pltpu.SemaphoreType.DMA
    y_slots = 1 if inner == 2 else inner + 1
    z_slots = 1 if outer == 2 else outer + 1
    scratch = []
    for lead in ((outer, inner), (outer, inner), (y_slots, outer), (z_slots,), ()):
        scratch += [pltpu.VMEM(lead + (a, b), dtype) for a, b, dtype in shapes]
    scratch += [
        dma((kinds,)), dma((kinds,)), dma((kinds,)),
        dma((2, inner, kinds)), dma((y_slots, kinds)),
        dma((2, outer, kinds)), dma((z_slots, kinds)),
        dma((kinds,)), dma((kinds,)), dma((kinds,)), dma((kinds,)),
        dma((2, 3)), dma((2, 3)), dma((3,)),
    ]
    return pl.pallas_call(
        partial(reduce_kernel, outer, inner, kinds),
        out_shape=tuple(jax.ShapeDtypeStruct(grad.shape[1:], jnp.float32) for grad in grads) + (
            jax.ShapeDtypeStruct((4,) + y_rows.shape, y_rows.dtype),
            jax.ShapeDtypeStruct((4,) + g_rows.shape, g_rows.dtype),
        ),
        in_specs=[ANY] * (kinds + 2),
        out_specs=(VMEM,) * kinds + (ANY, ANY),
        scratch_shapes=scratch,
        compiler_params=pltpu.CompilerParams(
            collective_id=2, has_side_effects=True, vmem_limit_bytes=VMEM_LIMIT
        ),
        name="reduce_and_return",
    )(*(grad.reshape((outer, inner) + grad.shape[1:]) for grad in grads), y_rows, g_rows)


def home_kernel(tab_ref, ry_ref, rg_ref, y_ref, g_ref):
    base = lax.axis_index("rep") * y_ref.shape[0]

    def fetch(block, carry):
        index = tab_ref[DEST_AT + base + block] if len(tab_ref.shape) == 1 else tab_ref[48, base + block]
        safe = jnp.maximum(index, 0)
        for src, dst in ((ry_ref, y_ref), (rg_ref, g_ref)):
            value = src[safe // SLOTS, safe % SLOTS]
            dst[block] = jnp.where(index >= 0, value, jnp.zeros_like(value))
        return carry

    lax.fori_loop(0, y_ref.shape[0], fetch, 0)


def bring_home(table, ry, rg, blocks):
    shape = jax.ShapeDtypeStruct((blocks,) + ry.shape[2:], ry.dtype)
    return pl.pallas_call(
        home_kernel,
        out_shape=(shape, shape),
        in_specs=[SMEM, VMEM, VMEM],
        out_specs=(VMEM, VMEM),
        compiler_params=pltpu.CompilerParams(vmem_limit_bytes=VMEM_LIMIT),
        name="place_rows",
    )(table, ry, rg)


D = H * DH
ROWS = SLOTS * BLK
SIDES = SLOTS * (BLK // GBLK)
SIDE_ROWS = 48
ALL_ROWS = ROWS + SIDE_ROWS
QT = 128
WIN = 384
TILES = ROWS // QT
QUAD = 256
FF_TILE = 256
GELU_C = 0.7978845608028654
GELU_A = 0.044715
F32, BF16 = jnp.float32, jnp.bfloat16


def mm(left, right):
    return lax.dot_general(left, right, (((1,), (0,)), ((), ())), preferred_element_type=F32)


def mm_cols(left, right):
    return lax.dot_general(left, right, (((1,), (1,)), ((), ())), preferred_element_type=F32)


def mm_rows(left, right):
    return lax.dot_general(left, right, (((0,), (0,)), ((), ())), preferred_element_type=F32)


def iota(shape, axis):
    return lax.broadcasted_iota(jnp.int32, shape, axis)


def pick_by(index, values, other):
    out = jnp.full(index.shape, other, jnp.int32)
    for number, value in enumerate(values):
        out = jnp.where(index == number, value, out)
    return out


def block_at(tab_ref, slot):
    return lax.rem(tab_ref[slot, 0], 128) - 1


def seg_at(tab_ref, slot):
    if len(tab_ref.shape) == 1:
        return tab_ref[SEG_AT + slot]
    return lax.div(tab_ref[slot, 0], 16384) - 1


def len_at(tab_ref, slot):
    if len(tab_ref.shape) == 1:
        return tab_ref[LEN_AT + slot]
    return lax.rem(lax.div(tab_ref[slot, 0], 128), 128)


def slot_info(tab_ref, rank):
    seg = [seg_at(tab_ref, rank * SLOTS + slot) for slot in range(SLOTS)]
    length = [len_at(tab_ref, rank * SLOTS + slot) for slot in range(SLOTS)]
    return seg, length


def valid_column(tab_ref, rank):
    _, length = slot_info(tab_ref, rank)
    row = iota((ROWS, 1), 0)
    return ((row % BLK) < pick_by(row // BLK, length, 0)).astype(F32)


def pooling(tab_ref, rank):
    _, length = slot_info(tab_ref, rank)
    row = iota((1, ROWS), 1)
    block = jnp.where((row % BLK) < pick_by(row // BLK, length, 0), row // GBLK, -1)
    return jnp.where(iota((SIDE_ROWS, ROWS), 0) == block, 1.0, 0.0).astype(BF16)


def key_segments(tab_ref, rank, first_block, index):
    blocks = WIN // BLK
    base = rank * SLOTS + first_block
    seg = [seg_at(tab_ref, base + step) for step in range(blocks)]
    length = [len_at(tab_ref, base + step) for step in range(blocks)]
    alive = (index % BLK) < pick_by(index // BLK, length, 0)
    return jnp.where(alive, pick_by(index // BLK, seg, -2), -2)


def side_segments(tab_ref, rank, index):
    seg, length = slot_info(tab_ref, rank)
    per = BLK // GBLK
    alive = (index % per) * GBLK < pick_by(index // per, length, 0)
    return jnp.where(alive, pick_by(index // per, seg, -2), -2)


def tile_bias(tab_ref, rank, tile, first_row, keys_axis):
    qs, ks, gs = ((QT, 1), (1, WIN), (1, SIDE_ROWS)) if keys_axis == 1 else ((1, QT), (WIN, 1), (SIDE_ROWS, 1))
    q_index = iota(qs, 1 - keys_axis)
    k_index = iota(ks, keys_axis)
    g_index = iota(gs, keys_axis)
    base = rank * SLOTS + tile * (QT // BLK)
    q_seg = pick_by(q_index // BLK, [seg_at(tab_ref, base + step) for step in range(QT // BLK)], -1)
    k_seg = key_segments(tab_ref, rank, first_row // BLK, k_index)
    g_seg = side_segments(tab_ref, rank, g_index)
    gap = (q_index + tile * QT) - (k_index + first_row)
    local = (jnp.abs(gap) <= RADIUS) & (q_seg == k_seg)
    return jnp.where(local, 0.0, MASKED_SCORE), jnp.where(q_seg == g_seg, 0.0, MASKED_SCORE)


def window_start(tile):
    return pl.multiple_of(jnp.clip(tile - 1, 0, TILES - WIN // QT) * QT, QT)


def head_stack(rows):
    lane = iota(rows.shape, 1) // DH
    zero = jnp.zeros_like(rows)
    return jnp.concatenate([jnp.where(lane == head, rows, zero) for head in range(QUAD // DH)], axis=0)


def head_merge(stacked):
    lane = iota((QT, QUAD), 1) // DH
    out = stacked[:QT]
    for head in range(1, QUAD // DH):
        out = jnp.where(lane == head, stacked[head * QT : (head + 1) * QT], out)
    return out


def gains_of(gc_ref):
    count = gc_ref.shape[0]
    part = D // count
    lane, column = iota((128, D), 0), iota((128, D), 1)
    total = None
    for shard in range(count):
        pick = jnp.where((column == lane + shard * part) & (lane < part), 1.0, 0.0).astype(BF16)
        term = mm(gc_ref[shard], pick)
        total = term if total is None else total + term
    return total


def three_way(value):
    high = value.astype(BF16)
    rest = value - high.astype(F32)
    middle = rest.astype(BF16)
    return high, middle, (rest - middle.astype(F32)).astype(BF16)


def spread_gain_grads(value, dc_ref):
    count = dc_ref.shape[0] if len(dc_ref.shape) == 3 else dc_ref.shape[0] * dc_ref.shape[1]
    part = D // count
    column, lane = iota((D, 128), 0), iota((D, 128), 1)
    parts = three_way(value)
    for shard in range(count):
        pick = jnp.where((column == lane + shard * part) & (lane < part), 1.0, 0.0).astype(BF16)
        place = dc_ref.at[shard] if len(dc_ref.shape) == 3 else dc_ref.at[shard // dc_ref.shape[1], shard % dc_ref.shape[1]]
        place[...] = mm(parts[0], pick) + mm(parts[1], pick) + mm(parts[2], pick)


def mean_square(value):
    return jnp.mean(value * value, axis=-1, keepdims=True)


def forward_norm(tab_ref, rank, x_ref, gains, n_ref):
    for tile in range(TILES):
        rows = pl.ds(tile * QT, QT)
        value = x_ref[rows, :].astype(F32)
        n_ref[rows, :] = (value * lax.rsqrt(mean_square(value) + EPSILON) * gains[0:1]).astype(BF16)
    side = mm(pooling(tab_ref, rank), n_ref[:ROWS, :])
    n_ref[ROWS:, :] = (side * lax.rsqrt(mean_square(side) + EPSILON) * gains[1:2]).astype(BF16)


def forward_project(n_ref, w_ref, qkv_ref):
    def step(tile, carry):
        cols = pl.ds(pl.multiple_of(tile * QUAD, QUAD), QUAD)
        qkv_ref[:, cols] = mm(n_ref[...], w_ref[:, cols]).astype(BF16)
        return carry

    lax.fori_loop(0, 3 * D // QUAD, step, 0)


def forward_attention(tab_ref, rank, qkv_ref, att_ref, lse_ref, begin, end):
    heads = QUAD // DH

    def step(tile, carry):
        first = window_start(tile)
        bias, side_bias = tile_bias(tab_ref, rank, tile, first, 1)
        rows = pl.ds(pl.multiple_of(tile * QT, QT), QT)
        window = pl.ds(first, WIN)
        lane = iota((QT, 128), 1)

        def four(quad, lse):
            low = pl.multiple_of(quad * QUAD, QUAD)
            cols, key_cols, value_cols = (pl.ds(low + number * D, QUAD) for number in range(3))
            query = head_stack(qkv_ref[rows, cols])
            scores = mm_cols(query, qkv_ref[window, key_cols])
            side_scores = mm_cols(query, qkv_ref[ROWS:, key_cols])
            local, sides, scale = [], [], []
            for head in range(heads):
                part = slice(head * QT, (head + 1) * QT)
                one = scores[part] + bias
                two = side_scores[part] + side_bias
                peak = jnp.maximum(
                    jnp.max(one, axis=-1, keepdims=True), jnp.max(two, axis=-1, keepdims=True)
                )
                one, two = jnp.exp(one - peak), jnp.exp(two - peak)
                total = jnp.sum(one, axis=-1, keepdims=True) + jnp.sum(two, axis=-1, keepdims=True)
                local.append(one.astype(BF16))
                sides.append(two.astype(BF16))
                scale.append(1.0 / total)
                lse = jnp.where(lane == quad * heads + head, peak + jnp.log(total), lse)
            mixed = mm(jnp.concatenate(local, axis=0), qkv_ref[window, value_cols])
            mixed = mixed + mm(jnp.concatenate(sides, axis=0), qkv_ref[ROWS:, value_cols])
            mixed = mixed * jnp.concatenate(scale, axis=0)
            att_ref[rows, cols] = head_merge(mixed).astype(BF16)
            return lse

        lse = lax.fori_loop(0, D // QUAD, four, jnp.zeros((QT, 128), F32))
        lse_ref[tile] = jnp.transpose(lse)[:16]
        return carry

    lax.fori_loop(begin, end, step, 0)


def feed_forward(tab_ref, rank, x_ref, cot_ref, att_ref, gains, w_ref, wb_ref,
                 y_ref, gh_ref, ga_ref, dg_ref, du_ref, db_ref, do_ref,
                 h1_ref, nt_ref, ntt_ref, gres_ref, h2_ref, gg_ref, gu_ref, gn_ref):
    hidden = wb_ref.shape[0]
    gate_at = w_ref.shape[1] - 2 * hidden
    out_at = gate_at - D
    valid = valid_column(tab_ref, rank)
    gain = gains[2:3]
    for tile in range(TILES):
        rows = pl.ds(tile * QT, QT)
        value = x_ref[rows, :].astype(F32) + mm(att_ref[rows, :], w_ref[:, out_at:gate_at])
        h1_ref[rows, :] = value
        normed = (value * lax.rsqrt(mean_square(value) + EPSILON) * gain).astype(BF16)
        nt_ref[rows, :] = normed
        ntt_ref[:, tile * QT : (tile + 1) * QT] = jnp.transpose(normed)
        gres_ref[rows, :] = (cot_ref[rows, :].astype(F32) * valid[tile * QT : (tile + 1) * QT]).astype(BF16)

    def inward(tile, carry):
        at = pl.multiple_of(tile * FF_TILE, FF_TILE)
        cols = pl.ds(at, FF_TILE)
        gate = mm(nt_ref[...], w_ref[:, pl.ds(gate_at + at, FF_TILE)])
        up = mm(nt_ref[...], w_ref[:, pl.ds(gate_at + hidden + at, FF_TILE)])
        back = mm_cols(gres_ref[...], wb_ref[cols, :])
        square = gate * gate
        bend = jnp.tanh(GELU_C * (gate * (1.0 + GELU_A * square)))
        half = 0.5 * (1.0 + bend)
        act = gate * half
        slope = half + (0.5 * GELU_C) * gate * (1.0 - bend * bend) * (1.0 + (3.0 * GELU_A) * square)
        h2_ref[:, cols] = (act * up).astype(BF16)
        gg_ref[:, cols] = (back * up * slope).astype(BF16)
        gu_ref[:, cols] = (back * act).astype(BF16)
        return carry

    lax.fori_loop(0, hidden // FF_TILE, inward, 0)

    def outward(tile, carry):
        cols = pl.ds(pl.multiple_of(tile * QUAD, QUAD), QUAD)
        value = h1_ref[:, cols] + mm(h2_ref[...], wb_ref[:, cols])
        y_ref[:, cols] = (value * valid).astype(BF16)
        gn_ref[:, cols] = mm_cols(gg_ref[...], w_ref[cols, gate_at : gate_at + hidden]) + mm_cols(
            gu_ref[...], w_ref[cols, gate_at + hidden :]
        )
        return carry

    lax.fori_loop(0, D // QUAD, outward, 0)

    def weights(tile, carry):
        at = pl.multiple_of(tile * FF_TILE, FF_TILE)
        cols = pl.ds(at, FF_TILE)
        dg_ref[:, cols] = mm(ntt_ref[...], gg_ref[:, cols]).astype(BF16)
        du_ref[:, cols] = mm(ntt_ref[...], gu_ref[:, cols]).astype(BF16)
        db_ref[cols, :] = mm_rows(h2_ref[:, cols], gres_ref[...]).astype(BF16)
        return carry

    lax.fori_loop(0, hidden // FF_TILE, weights, 0)

    gain_grad = jnp.zeros((1, D), F32)
    for tile in range(TILES):
        rows = pl.ds(tile * QT, QT)
        value, grad = h1_ref[rows, :], gn_ref[rows, :]
        root = lax.rsqrt(mean_square(value) + EPSILON)
        unit = value * root
        gain_grad = gain_grad + jnp.sum(grad * unit, axis=0, keepdims=True)
        grad = grad * gain
        grad = gres_ref[rows, :].astype(F32) + root * (
            grad - unit * jnp.mean(grad * unit, axis=-1, keepdims=True)
        )
        gh_ref[rows, :] = grad
        low = grad.astype(BF16)
        nt_ref[rows, :] = low
        ga_ref[rows, :] = mm_cols(low, w_ref[:, out_at:gate_at]).astype(BF16)

    def out_weight(tile, carry):
        cols = pl.ds(pl.multiple_of(tile * QUAD, QUAD), QUAD)
        do_ref[cols, :] = mm_rows(att_ref[:, cols], nt_ref[...]).astype(BF16)
        return carry

    lax.fori_loop(0, D // QUAD, out_weight, 0)
    return gain_grad


def backward_attention_start(dk_ref, dv_ref):
    dk_ref[...] = jnp.zeros_like(dk_ref)
    dv_ref[...] = jnp.zeros_like(dv_ref)


def backward_attention_quad(tab_ref, rank, qkv_ref, att_ref, ga_ref, lse_ref, dqkv_ref, dk_ref, dv_ref, quad):
    heads = QUAD // DH
    marks = jnp.where(iota((16, QUAD), 1) // DH == iota((16, QUAD), 0), 1.0, 0.0).astype(BF16)
    low = quad * QUAD
    cols = slice(low, low + QUAD)

    def step(tile, carry):
        first = window_start(tile)
        bias, side_bias = tile_bias(tab_ref, rank, tile, first, 0)
        bias = jnp.concatenate([bias, side_bias], axis=0)
        rows = pl.ds(pl.multiple_of(tile * QT, QT), QT)
        window = pl.ds(first, WIN)
        lse = lse_ref[tile]
        product = ga_ref[rows, cols].astype(F32) * att_ref[rows, cols].astype(F32)
        high = product.astype(BF16)
        rest = (product - high.astype(F32)).astype(BF16)
        centre = mm_cols(marks, high) + mm_cols(marks, rest)
        query = head_stack(qkv_ref[rows, cols])
        grad = head_stack(ga_ref[rows, cols])
        keys = jnp.concatenate(
            [qkv_ref[window, D + low : D + low + QUAD], qkv_ref[ROWS:, D + low : D + low + QUAD]], axis=0
        )
        values = jnp.concatenate(
            [qkv_ref[window, 2 * D + low : 2 * D + low + QUAD],
             qkv_ref[ROWS:, 2 * D + low : 2 * D + low + QUAD]], axis=0
        )
        scores = mm_cols(keys, query)
        slopes = mm_cols(values, grad)
        probs, grads = [], []
        for head in range(heads):
            part = slice(head * QT, (head + 1) * QT)
            number = quad * heads + head
            prob = jnp.exp(scores[:, part] + bias - lse[number : number + 1])
            probs.append(prob.astype(BF16))
            grads.append((prob * (slopes[:, part] - centre[head : head + 1])).astype(BF16))
        probs = jnp.concatenate(probs, axis=1)
        grads = jnp.concatenate(grads, axis=1)
        dkey = mm(grads, query)
        dvalue = mm(probs, grad)
        dk_ref[window, cols] = dk_ref[window, cols] + dkey[:WIN]
        dk_ref[ROWS:, cols] = dk_ref[ROWS:, cols] + dkey[WIN:]
        dv_ref[window, cols] = dv_ref[window, cols] + dvalue[:WIN]
        dv_ref[ROWS:, cols] = dv_ref[ROWS:, cols] + dvalue[WIN:]
        dqkv_ref[rows, cols] = head_merge(mm_rows(grads, keys)).astype(BF16)
        return carry

    lax.fori_loop(0, TILES, step, 0)
    dqkv_ref[ROWS:, cols] = jnp.zeros((SIDE_ROWS, QUAD), BF16)
    dqkv_ref[:, D + low : D + low + QUAD] = dk_ref[:, cols].astype(BF16)
    dqkv_ref[:, 2 * D + low : 2 * D + low + QUAD] = dv_ref[:, cols].astype(BF16)


def weight_grads(n_ref, dqkv_ref, refs):
    for number, ref in enumerate(refs):
        def weights(tile, carry):
            at = pl.multiple_of(tile * QUAD, QUAD)
            value = mm_rows(n_ref[...], dqkv_ref[:, pl.ds(number * D + at, QUAD)]).astype(BF16)
            if len(ref.shape) == 4:
                ref[:, :, :, pl.ds(at, QUAD)] = value.reshape(ref.shape[:3] + (QUAD,))
            else:
                ref[:, pl.ds(at, QUAD)] = value
            return carry

        lax.fori_loop(0, D // QUAD, weights, 0)


def backward_project(tab_ref, rank, x_ref, gh_ref, gains, n_ref, dqkv_ref, w_ref, gn_ref, g_ref):
    def step(tile, carry):
        cols = pl.ds(pl.multiple_of(tile * QUAD, QUAD), QUAD)
        gn_ref[:, cols] = mm_cols(dqkv_ref[...], w_ref[cols, : 3 * D])
        return carry

    lax.fori_loop(0, D // QUAD, step, 0)
    pool = pooling(tab_ref, rank)
    side = mm(pool, n_ref[:ROWS, :])
    root = lax.rsqrt(mean_square(side) + EPSILON)
    unit = side * root
    grad = gn_ref[ROWS:, :]
    side_gain = jnp.sum(grad * unit, axis=0, keepdims=True)
    grad = grad * gains[1:2]
    grad = root * (grad - unit * jnp.mean(grad * unit, axis=-1, keepdims=True))
    parts = three_way(grad)
    gain_grad = jnp.zeros((1, D), F32)
    for tile in range(TILES):
        rows = pl.ds(tile * QT, QT)
        spread = pool[:, tile * QT : (tile + 1) * QT]
        total = gn_ref[rows, :] + mm_rows(spread, parts[0]) + mm_rows(spread, parts[1])
        value = x_ref[rows, :].astype(F32)
        root = lax.rsqrt(mean_square(value) + EPSILON)
        unit = value * root
        gain_grad = gain_grad + jnp.sum(total * unit, axis=0, keepdims=True)
        total = total * gains[0:1]
        value = (
            gh_ref[rows, :] + root * (total - unit * jnp.mean(total * unit, axis=-1, keepdims=True))
        ).astype(BF16)
        if len(g_ref.shape) == 3:
            g_ref[pl.ds(tile * (QT // BLK), QT // BLK)] = value.reshape(QT // BLK, BLK, D)
        else:
            g_ref[rows, :] = value
    return gain_grad, side_gain


def gelu_both(gate):
    square = gate * gate
    bend = jnp.tanh(GELU_C * (gate * (1.0 + GELU_A * square)))
    half = 0.5 * (1.0 + bend)
    slope = half + (0.5 * GELU_C) * gate * (1.0 - bend * bend) * (1.0 + (3.0 * GELU_A) * square)
    return gate * half, slope


def first_kernel(tab_ref, x_ref, gc_ref, w_ref, n_ref, qkv_ref, att_ref, lse_ref):
    rank = lax.axis_index("rep")
    gains = gains_of(gc_ref)
    forward_norm(tab_ref, rank, x_ref, gains, n_ref)
    forward_project(n_ref, w_ref, qkv_ref)
    forward_attention(tab_ref, rank, qkv_ref, att_ref, lse_ref, 0, TILES)


def second_kernel(tab_ref, x_ref, cot_ref, att_ref, gc_ref, w_ref, wb_ref,
                  y_ref, gh_ref, ga_ref, dg_ref, du_ref, db_ref, do_ref, gain_ref, *scratch):
    rank = lax.axis_index("rep")
    gain_ref[...] = feed_forward(tab_ref, rank, x_ref, cot_ref, att_ref, gains_of(gc_ref), w_ref, wb_ref,
                                 y_ref, gh_ref, ga_ref, dg_ref, du_ref, db_ref, do_ref, *scratch)


def third_kernel(tab_ref, x_ref, gh_ref, ga_ref, att_ref, lse_ref, n_ref, qkv_ref, gain_ref, gc_ref, w_ref,
                 g_ref, dw_ref, dc_ref, dqkv_ref, dk_ref, dv_ref, gn_ref):
    rank = lax.axis_index("rep")
    gains = gains_of(gc_ref)
    backward_attention_start(dk_ref, dv_ref)
    for quad in range(D // QUAD):
        backward_attention_quad(tab_ref, rank, qkv_ref, att_ref, ga_ref, lse_ref, dqkv_ref, dk_ref, dv_ref, quad)
    weight_grads(n_ref, dqkv_ref, [dw_ref.at[:, i * D : (i + 1) * D] for i in range(3)])
    one, side = backward_project(tab_ref, rank, x_ref, gh_ref, gains, n_ref, dqkv_ref, w_ref, gn_ref, g_ref)
    grads = jnp.concatenate([one, side, gain_ref[...], jnp.zeros((5, D), F32)], axis=0)
    spread_gain_grads(grads, dc_ref)


def attend(tab, x, gc, w):
    shape = jax.ShapeDtypeStruct
    return pl.pallas_call(
        first_kernel,
        out_shape=(shape((ALL_ROWS, D), BF16), shape((ALL_ROWS, 3 * D), BF16), shape((ROWS, D), BF16),
                   shape((TILES, 16, QT), F32)),
        in_specs=[SMEM, VMEM, VMEM, pl.BlockSpec((D, 3 * D), lambda step: (0, 0))],
        grid=(1,),
        out_specs=(VMEM,) * 4,
        compiler_params=pltpu.CompilerParams(vmem_limit_bytes=VMEM_LIMIT),
        name="attend",
    )(tab, x, gc, w)


def feed(tab, x, cot, att, gc, w, wb):
    hidden = wb.shape[0]
    shape = jax.ShapeDtypeStruct
    return pl.pallas_call(
        second_kernel,
        out_shape=(shape((ROWS, D), BF16), shape((ROWS, D), F32), shape((ROWS, D), BF16),
                   shape((D, hidden), BF16), shape((D, hidden), BF16), shape((hidden, D), BF16), shape((D, D), BF16),
                   shape((1, D), F32)),
        in_specs=[SMEM] + [VMEM] * 6,
        out_specs=(VMEM,) * 8,
        scratch_shapes=[pltpu.VMEM((ROWS, D), F32), pltpu.VMEM((ROWS, D), BF16), pltpu.VMEM((D, ROWS), BF16),
                        pltpu.VMEM((ROWS, D), BF16), pltpu.VMEM((ROWS, hidden), BF16),
                        pltpu.VMEM((ROWS, hidden), BF16), pltpu.VMEM((ROWS, hidden), BF16),
                        pltpu.VMEM((ROWS, D), F32)],
        compiler_params=pltpu.CompilerParams(vmem_limit_bytes=VMEM_LIMIT),
        name="feed_forward",
    )(tab, x, cot, att, gc, w, wb)


def backward_layer(tab, x, gh, ga, att, lse, n, qkv, gain, gc, w):
    shape = jax.ShapeDtypeStruct
    return pl.pallas_call(
        third_kernel,
        out_shape=(shape((ROWS, D), BF16), shape((D, 3 * D), BF16), shape((gc.shape[0], 8, 128), F32)),
        in_specs=[SMEM] + [VMEM] * 9 + [pl.BlockSpec((D, 3 * D), lambda step: (0, 0))],
        grid=(1,),
        out_specs=(VMEM,) * 3,
        scratch_shapes=[pltpu.VMEM((ALL_ROWS, 3 * D), BF16), pltpu.VMEM((ALL_ROWS, D), F32),
                        pltpu.VMEM((ALL_ROWS, D), F32), pltpu.VMEM((ALL_ROWS, D), F32)],
        compiler_params=pltpu.CompilerParams(vmem_limit_bytes=VMEM_LIMIT),
        name="attend_back",
    )(tab, x, gh, ga, att, lse, n, qkv, gain, gc, w)


class Links:
    def __init__(self, outer, inner):
        self.outer, self.inner = outer, inner
        self.rank, self.spot = lax.axis_index("rep"), lax.axis_index("fsdp")
        self.core = self.rank % 2
        self.row, self.col = self.spot // inner, self.spot % inner
        self.mate, self.across = core_of(self.rank), across_of(self.rank)
        self.late = []

    def greet(self, everyone=False, later=False):
        barrier = pltpu.get_barrier_semaphore()
        neighbours = (
            (self.row + 1 < self.outer, {"fsdp": self.spot + self.inner}),
            (self.row > 0, {"fsdp": self.spot - self.inner}),
            (self.col + 1 < self.inner, {"fsdp": self.spot + 1}),
            (self.col > 0, {"fsdp": self.spot - 1}),
        )
        group = (self.mate, self.across) + ((across_of(self.mate),) if everyone else ())
        amount = jnp.int32(len(group))
        for there, device in neighbours:
            amount = amount + there.astype(jnp.int32)

            @pl.when(there)
            def _():
                pl.semaphore_signal(barrier, inc=1, device_id=device, device_id_type=MESH)

        for device in group:
            pl.semaphore_signal(barrier, inc=1, device_id={"rep": device}, device_id_type=MESH)
        self.met = lambda: pl.semaphore_wait(barrier, amount)
        if not later:
            self.met()

    def send(self, there, src, dst, ssem, rsem, device):
        def describe():
            return pltpu.make_async_remote_copy(
                src_ref=src, dst_ref=dst, send_sem=ssem, recv_sem=rsem,
                device_id=device, device_id_type=MESH,
            )

        if there is None:
            describe().start()
        else:
            @pl.when(there)
            def _():
                describe().start()

        self.late.append((there, lambda: describe().wait_send()))

    def arrive(self, place, rsem, spare):
        pltpu.make_async_remote_copy(
            src_ref=place, dst_ref=place, send_sem=spare, recv_sem=rsem,
            device_id={"rep": self.mate}, device_id_type=MESH,
        ).wait_recv()

    def drain(self):
        for there, finish in self.late:
            if there is None:
                finish()
            else:
                pl.when(there)(finish)


def halves(ref, which):
    half = ref.shape[-1] // 2
    cols = pl.ds(pl.multiple_of(which * half, 128), half)
    return ref.at[:, :, :, cols] if len(ref.shape) == 4 else ref.at[:, cols]


class Reduction:
    def __init__(self, links, source, total, mine, crecv, yrecv, zrecv, xrecv, stage, sems, number):
        self.links, self.source, self.total, self.mine, self.stage = links, source, total, mine, stage
        self.crecv, self.yrecv, self.zrecv, self.xrecv = crecv, yrecv, zrecv, xrecv
        self.sems, self.number = sems, number
        self.whole = total.shape[-1] % 256 != 0
        self.load = None

    def sem(self, name, *index):
        return self.sems[name].at[index + (self.number,)]

    def begin(self):
        links = self.links
        other = self.source if self.whole else halves(self.source, 1 - links.core)
        links.send(None, other, self.crecv, self.sem("c_send"), self.sem("c_recv"), {"rep": links.mate})
        if self.mine is None:
            self.mine = self.source if self.whole else halves(self.source, links.core)
        else:
            own = self.source if self.whole else halves(self.source, links.core)
            self.load = pltpu.make_async_copy(own, self.mine, self.sem("m_sem"))
            self.load.start()

    def pair(self):
        links = self.links
        if self.load is not None:
            self.load.wait()
        links.arrive(self.crecv, self.sem("c_recv"), self.sems["spare"].at[0])
        inner = links.inner

        def add(index, carry):
            row, col = index // inner, index % inner
            self.mine[row, col] = self.mine[row, col] + self.crecv[row, col]
            return carry

        lax.fori_loop(0, links.outer * inner, add, 0)
        links.send(None, self.mine.at[:, 1 - links.col], self.yrecv, self.sem("y_send"), self.sem("y_recv"),
                   {"fsdp": links.spot + 1 - 2 * links.col})

    def slot(self, way, place, dest):
        return dest - place if way == 0 else self.links.outer - place + dest

    def pass_on(self, way, dest, there, first):
        links = self.links
        step = 1 if way == 0 else -1
        mine = self.mine.at[dest, links.col]
        put = self.slot(way, links.row + step, dest)
        if not first:
            got = self.slot(way, links.row, dest)

            @pl.when(there)
            def _():
                links.arrive(self.zrecv.at[got], self.sem("z_recv", got), self.sems["spare"].at[0])
                mine[...] = mine[...] + self.zrecv[got]

        links.send(there, mine, self.zrecv.at[put], self.sem("z_send", way, dest), self.sem("z_recv", put),
                   {"fsdp": links.spot + step * links.inner})

    def column(self):
        links = self.links
        size = links.outer
        links.arrive(self.yrecv, self.sem("y_recv"), self.sems["spare"].at[0])

        def add(index, carry):
            self.mine[index, links.col] = self.mine[index, links.col] + self.yrecv[index]
            return carry

        lax.fori_loop(0, size, add, 0)
        for far in range(size - 1, 0, -1):
            self.pass_on(0, far, links.row == 0, True)
            self.pass_on(1, size - 1 - far, links.row == size - 1, True)

    def hop(self, turn):
        links = self.links
        size = links.outer
        for way in range(2):
            place = turn if way == 0 else size - 1 - turn
            here = links.row == place
            rest = range(size - 1, place, -1) if way == 0 else range(0, place)
            for dest in rest:
                self.pass_on(way, dest, here, False)
            mine = self.mine.at[place, links.col]
            got = self.slot(way, place, place)

            @pl.when(here)
            def _():
                links.arrive(self.zrecv.at[got], self.sem("z_recv", got), self.sems["spare"].at[0])
                mine[...] = mine[...] + self.zrecv[got]

    def cross(self):
        links = self.links
        mine = self.mine.at[links.row, links.col]
        links.send(None, mine, self.xrecv, self.sem("x_send"), self.sem("x_recv"), {"rep": links.across})

    def finish(self):
        links = self.links
        links.arrive(self.xrecv, self.sem("x_recv"), self.sems["spare"].at[0])
        self.stage[...] = self.mine[links.row, links.col].astype(F32) + self.xrecv[...].astype(F32)
        place = self.total if self.whole else halves(self.total, links.core)
        self.keep = pltpu.make_async_copy(self.stage, place, self.sem("m_sem"))
        self.keep.start()
        if not self.whole:
            links.send(None, self.stage, place, self.sem("f_send"), self.sem("f_recv"), {"rep": links.mate})

    def settle(self):
        self.keep.wait()
        if not self.whole:
            self.links.arrive(
                halves(self.total, 1 - self.links.core), self.sem("f_recv"), self.sems["spare"].at[0]
            )


class AcrossFirst(Reduction):
    def pair(self):
        links = self.links
        if self.load is not None:
            self.load.wait()
        links.arrive(self.crecv, self.sem("c_recv"), self.sems["spare"].at[0])
        inner = links.inner

        def add(index, carry):
            row, col = index // inner, index % inner
            self.mine[row, col] = self.mine[row, col] + self.crecv[row, col]
            return carry

        lax.fori_loop(0, links.outer * inner, add, 0)
        self.side = links.rank // 2
        links.send(None, self.rows_of(self.mine, 1 - self.side), self.xrecv, self.sem("x_send"), self.sem("x_recv"),
                   {"rep": links.across})

    def rows_of(self, ref, which):
        half = ref.shape[-2] // 2
        rows = pl.ds(pl.multiple_of(which * half, 16), half)
        return ref.at[:, :, rows, :] if len(ref.shape) == 4 else ref.at[rows, :]

    def meet(self):
        links = self.links
        links.arrive(self.xrecv, self.sem("x_recv"), self.sems["spare"].at[0])
        self.mine = self.rows_of(self.mine, self.side)
        inner = links.inner

        def add(index, carry):
            row, col = index // inner, index % inner
            self.mine[row, col] = self.mine[row, col] + self.xrecv[row, col]
            return carry

        lax.fori_loop(0, links.outer * inner, add, 0)
        links.send(None, self.mine.at[:, 1 - links.col], self.yrecv, self.sem("y_send"), self.sem("y_recv"),
                   {"fsdp": links.spot + 1 - 2 * links.col})

    def quarter(self, side, core):
        return halves(self.rows_of(self.total, side), core)

    def spread(self, stage, place, keep, ssem, rsem):
        links = self.links
        self.keeps.append(pltpu.make_async_copy(stage, place, keep))
        self.keeps[-1].start()
        links.send(None, stage, place, ssem, rsem, {"rep": links.mate})

    def cross(self):
        links = self.links
        mine = self.mine.at[links.row, links.col]
        links.send(None, mine, self.third, self.sem("h_send"), self.sem("h_recv"), {"rep": links.across})
        self.stage[...] = mine[...].astype(F32)
        self.keeps = []
        self.spread(self.stage, self.quarter(self.side, links.core), self.sem("m_sem"),
                    self.sem("f_send"), self.sem("f_recv"))

    def finish(self):
        links = self.links
        links.arrive(self.third, self.sem("h_recv"), self.sems["spare"].at[0])
        self.stage_two[...] = self.third[...].astype(F32)
        self.spread(self.stage_two, self.quarter(1 - self.side, links.core), self.sem("k_keep"),
                    self.sem("k_send"), self.sem("k_recv"))

    def settle(self):
        links = self.links
        for keep in self.keeps:
            keep.wait()
        for side, name in ((self.side, "f_recv"), (1 - self.side, "k_recv")):
            links.arrive(self.quarter(side, 1 - links.core), self.sem(name), self.sems["spare"].at[0])


SEM_NAMES = ("c_send", "c_recv", "m_sem", "y_send", "y_recv", "z_send", "z_recv", "x_send", "x_recv",
             "f_send", "f_recv", "h_send", "h_recv", "k_send", "k_recv", "k_keep", "r_send", "r_recv", "own", "spare")


class Return:
    def __init__(self, links, source, home, sems, kind):
        self.links, self.source, self.home, self.sems, self.kind = links, source, home, sems, kind

    def begin(self):
        links = self.links
        dst = self.home.at[links.rank]
        for way, device in enumerate((links.across, links.mate)):
            links.send(None, self.source, dst, self.sems["r_send"].at[self.kind, way],
                       self.sems["r_recv"].at[self.kind, way], {"rep": device})
        self.copy = pltpu.make_async_copy(self.source, dst, self.sems["own"].at[self.kind])
        self.copy.start()

    def relay(self):
        links = self.links
        place = self.home.at[links.across]
        links.arrive(place, self.sems["r_recv"].at[self.kind, 0], self.sems["spare"].at[0])
        links.send(None, place, place, self.sems["r_send"].at[self.kind, 2],
                   self.sems["r_recv"].at[self.kind, 2], {"rep": links.mate})

    def settle(self):
        links, sem = self.links, self.sems["r_recv"]
        links.arrive(self.home.at[links.mate], sem.at[self.kind, 1], self.sems["spare"].at[0])
        links.arrive(self.home.at[across_of(links.mate)], sem.at[self.kind, 2], self.sems["spare"].at[0])
        self.copy.wait()


TABLE_ROWS = 56


def packed_table(lens, tabv_ref):
    lane = iota((8, 128), 1)
    blocks = lax.div(lens + (BLK - 1), BLK)
    key = jnp.where(blocks > 0, blocks * 128 + (127 - lane), 0)
    wide = jnp.broadcast_to(key[:1], (128, 128))
    other = jnp.sum(jnp.where(iota((128, 128), 0) == iota((128, 128), 1), wide, 0), axis=1, keepdims=True)
    order = jnp.sum(jnp.where(other > wide, 1, 0), axis=0, keepdims=True)
    order = jnp.broadcast_to(order, (8, 128))
    edges, below = [], jnp.zeros((8, 1), jnp.int32)
    for size in range(MAX_SEQ_BLOCKS, 0, -1):
        below = below + jnp.sum(jnp.where(blocks == size, 1, 0), axis=1, keepdims=True)
        edges.append(jnp.broadcast_to(below, (8, 128)))

    def assign(number, carry):
        loads, slot, first = carry[:4], carry[4], carry[5]
        size = jnp.zeros((8, 128), jnp.int32)
        for step, edge in enumerate(edges):
            size = size + jnp.where(number < edge, 1, 0)
        low = jnp.minimum(jnp.minimum(loads[0], loads[1]), jnp.minimum(loads[2], loads[3]))
        best = jnp.full((8, 128), 3, jnp.int32)
        for dev in (2, 1, 0):
            best = jnp.where(loads[dev] == low, dev, best)
        mine = order == number
        slot = jnp.where(mine, best * SLOTS + low, slot)
        first = jnp.where(mine, low, first)
        loads = tuple(loads[dev] + jnp.where(best == dev, size, 0) for dev in range(4))
        return loads + (slot, first)

    zero = jnp.zeros((8, 128), jnp.int32)
    carry = lax.fori_loop(0, 32, assign, (zero,) * 6)
    slot, first = carry[4], carry[5]
    where, tokens, segment = zero - 1, zero, zero
    for step in range(MAX_SEQ_BLOCKS):
        def shifted(value):
            return value if step == 0 else pltpu.roll(value, step, 1)

        covers = shifted(blocks) > step
        where = jnp.where(covers, shifted(slot) + step, where)
        tokens = jnp.where(covers, jnp.minimum(shifted(lens) - BLK * step, BLK), tokens)
        segment = jnp.where(covers, shifted(first) + 1, segment)
    packed = jnp.where(where >= 0, (lane + 1) + 128 * tokens + 16384 * segment, 0)
    spots = jnp.broadcast_to(where[:1], (48, 128))
    values = jnp.broadcast_to(packed[:1], (48, 128))
    column = jnp.sum(jnp.where(spots == iota((48, 128), 0), values, 0), axis=1, keepdims=True)
    tabv_ref[:48] = jnp.broadcast_to(column, (48, 128))
    tabv_ref[48:] = where


ROW_FIRST = (3,)
FRONT_ORDER = (
    ("own", 1), ("own", 3), ("do", "table"), ("hop", 1, 0), ("own", 0), ("pack", 0, 1), ("hop", 1, 1), ("own", 5),
    ("cross", 0), ("own", 2), ("hop", 0, 0), ("hop", 1, 2), ("pack", 1, 1), ("pack", 0, 0), ("hop", 5, 0),
    ("hop", 5, 1), ("hop", 5, 2), ("hop", 0, 1), ("yz", 3), ("hop", 0, 2), ("own", 4), ("cross", 1), ("fr", 1),
    ("hop", 2, 0), ("pack", 1, 0), ("hop", 3, 0), ("fr", 5), ("rfin", 0), ("fr", 0), ("do", "norm"), ("hop", 2, 1),
    ("got", 0), ("hop", 4, 0), ("do", "proj"), ("do", "a0"), ("hop", 2, 2), ("hop", 4, 1), ("hop", 3, 1),
    ("do", "a1"), ("hop", 4, 2), ("fr", 2), ("do", "a2"), ("hop", 3, 2), ("got", 2), ("do", "enter"), ("rfin", 1),
    ("fr", 4), ("xin", 1), ("got", 3), ("do", "half"),
)


def front_kernel(outer, inner, *refs):
    (raw_ref, rows_any, cots_any, *weights), refs = refs[:9], refs[9:]
    (wd_any, *gain_refs), refs = refs[:4], refs[4:]
    (tab_ref, gains_ref), outs_any, (ga_ref, gb_ref), refs = refs[:2], refs[2:16], refs[16:18], refs[18:]
    (stage, lens_all, tabs, psend, precv, xsend, xrecv, rows_ref, cots_ref), refs = refs[:9], refs[9:]
    (lens_ref, wd_ref, wc_ref), refs = refs[:3], refs[3:]
    held, gc_ref, refs = refs[:14], refs[14], refs[15:]
    x_ref, cot_ref, n_ref, qkv_ref, att_ref, lse_ref, wqkv_ref, w2_ref, h1_ref, nt_ref, ntt_ref, b0_ref, b1_ref, b2_ref = held
    (l_send, l_recv, t_sem, w_sem, z_send, z_recv, y_send, y_recv, c_send, c_recv, d_send, d_recv, own_sem,
     p_send, p_recv, x_send, x_recv, spare, out_sem, piece_sem) = refs
    links = Links(outer, inner)
    rank, spot, core, mate, across = links.rank, links.spot, links.core, links.mate, links.across
    row, col = links.row, links.col
    side = rank // 2
    count = outer * inner
    part = stage.shape[0]
    per_rank = rows_ref.shape[0]
    width = 3 * D
    tall = wd_ref.shape[0]
    hidden = weights[-1].shape[1]
    rest = stage.shape[1] - width
    half = hidden // 2
    early = D + 2 * half
    spans = [(0, (D + half) // 2), (D + half, half // 2), (early, half)]

    at = 0
    loads = []
    loads.append(pltpu.make_async_copy(wd_any, wd_ref, w_sem.at[2]))
    loads[0].start()
    row_loads = [pltpu.make_async_copy(rows_any, rows_ref, w_sem.at[0]), pltpu.make_async_copy(cots_any, cots_ref, w_sem.at[1])]
    parts = [(ref, slice(0, D)) for ref in weights[:4]]
    parts += [(ref, cols) for cols in (slice(0, half), slice(half, hidden)) for ref in weights[4:]]
    for number, (ref, cols) in enumerate(parts):
        size = cols.stop - cols.start
        loads.append(pltpu.make_async_copy(ref.at[:, cols], stage.at[:, at : at + size], w_sem.at[3 + number]))
        loads[-1].start()
        at += size
    for load in row_loads:
        load.start()

    wc_ref[...] = jnp.zeros(wc_ref.shape, wc_ref.dtype)
    for number, ref in enumerate(gain_refs):
        wc_ref[number : number + 1, :part] = ref[...].reshape(1, part)
    micro, spots = raw_ref.shape
    lens_ref[...] = jnp.zeros(lens_ref.shape, lens_ref.dtype)
    lens_ref[:micro, :spots] = raw_ref[...]
    raw = lens_ref[...]
    spread = jnp.zeros((1, 128), jnp.int32)
    for device in range(4):
        line = jnp.zeros((1, 128), jnp.int32)
        for number in range(micro):
            shift = device * micro * spots + number * spots
            moved = raw if shift == 0 else pltpu.roll(raw, shift, 1)
            line = line + moved[number : number + 1]
        spread = jnp.where(rank == device, line, spread)
    lens_ref[...] = jnp.broadcast_to(spread, (8, 128))
    links.greet(True)
    lens_all[rank] = lens_ref[...]
    for step in range(1, 4):
        links.send(None, lens_ref, lens_all.at[rank], l_send.at[step - 1], l_recv.at[step - 1],
                   {"rep": (rank + step) % 4})

    def cols_of(start, half, which):
        return pl.ds(pl.multiple_of(start + which * half, 128), half)

    down_half = D // 2

    def tall_rows(which):
        return pl.ds(pl.multiple_of(which * (tall // 2), 16), tall // 2)

    def source(number):
        if number == 0:
            return stage.at[:, cols_of(0, width // 2, core)]
        if number == 1:
            return wd_ref.at[tall_rows(side), cols_of(0, down_half, core)]
        if number == 5:
            return wc_ref
        start, size = spans[number - 2]
        return stage.at[:, cols_of(width + start, size, core)]

    def place(number, shard, which=None):
        which = core if which is None else which
        if number == 0:
            return wqkv_ref.at[pl.ds(pl.multiple_of(shard * part, 16), part), cols_of(0, width // 2, which)]
        if number in (1, 6):
            return gb_ref.at[shard, tall_rows(side if number == 1 else 1 - side), cols_of(0, down_half, which)]
        if number == 5:
            return gc_ref.at[shard]
        start, size = spans[number - 2]
        if number == 4:
            return ga_ref.at[shard, :, cols_of(0, size, which)]
        return w2_ref.at[pl.ds(pl.multiple_of(shard * part, 16), part), cols_of(start, size, which)]

    nobody = spare.at[0]

    def both(first, second):
        return second if first is None else jnp.logical_and(first, second)

    def guarded(there, action):
        if there is None:
            action()
        else:
            pl.when(there)(action)

    def share(there, number, shard):
        if number == 5:
            return
        here = place(number, shard)
        links.send(there, here, here, c_send.at[number, shard], c_recv.at[number, shard], {"rep": mate})
        if number == 1:
            links.send(there, here, here, d_send.at[shard], d_recv.at[shard], {"rep": across})

    other_column = {"fsdp": spot + 1 - 2 * col}

    def along_row(there, number, line, src):
        here = place(number, line * inner + col)
        links.send(there, here if src is None else src, here, y_send.at[line, number], y_recv.at[line, number],
                   other_column)

    def lines(step):
        return ((row - 1 - step >= 0, row - 1 - step, 0, row + 1 < outer, spot + inner),
                (row + 1 + step < outer, row + 1 + step, 1, row > 0, spot - inner))

    def along_line(number, column, src):
        here = place(number, row * inner + (col if column == 0 else 1 - col))
        src = here if src is None else src
        links.send(row + 1 < outer, src, here, z_send.at[0, 0, number, column], z_recv.at[0, 0, number, column],
                   {"fsdp": spot + inner})
        links.send(row > 0, src, here, z_send.at[1, 0, number, column], z_recv.at[1, 0, number, column],
                   {"fsdp": spot - inner})

    def own(number):
        src = source(number)
        along_line(number, 0, src)
        along_row(None, number, row, src)

    def second_column(number):
        shard = row * inner + 1 - col
        links.arrive(place(number, shard), y_recv.at[row, number], nobody)
        share(None, number, shard)
        along_line(number, 1, None)

    def hop(number, step):
        for here, line, way, onward, target in lines(step):
            for column in range(2 if number in ROW_FIRST else 1):
                shard = line * inner + (col if column == 0 else 1 - col)
                guarded(here, lambda: links.arrive(place(number, shard), z_recv.at[way, step, number, column], nobody))
                if step + 1 < outer - 1:
                    view = place(number, shard)
                    links.send(both(here, onward), view, view, z_send.at[way, step + 1, number, column],
                               z_recv.at[way, step + 1, number, column], {"fsdp": target})
                if number not in ROW_FIRST:
                    along_row(here, number, line, None)
                share(here, number, shard)

    def from_row(number):
        def one(there, line):
            shard = line * inner + 1 - col
            guarded(there, lambda: links.arrive(place(number, shard), y_recv.at[line, number], nobody))
            share(there, number, shard)

        one(None, row)
        for step in range(outer - 1):
            for here, line, *_ in lines(step):
                one(here, line)

    def gathered(*numbers):
        def wait(shard, carry):
            @pl.when(shard != spot)
            def _():
                for number in numbers:
                    links.arrive(place(number, shard, 1 - core), c_recv.at[number, shard], nobody)

            return carry

        lax.fori_loop(0, count, wait, 0)

    def from_across():
        def relay(shard, carry):
            here = place(6, shard)

            @pl.when(shard != spot)
            def _():
                links.arrive(here, d_recv.at[shard], nobody)
                pltpu.make_async_remote_copy(
                    src_ref=here, dst_ref=here, send_sem=c_send.at[6, shard], recv_sem=c_recv.at[6, shard],
                    device_id={"rep": mate}, device_id_type=MESH,
                ).start()

            return carry

        lax.fori_loop(0, count, relay, 0)

    for load in loads:
        load.wait()
    keep = [
        pltpu.make_async_copy(stage.at[:, :width], wqkv_ref.at[pl.ds(pl.multiple_of(spot * part, 16), part)], own_sem.at[0]),
        pltpu.make_async_copy(stage.at[:, width + early :], ga_ref.at[spot], own_sem.at[1]),
        pltpu.make_async_copy(wd_ref, gb_ref.at[spot], own_sem.at[2]),
        pltpu.make_async_copy(wc_ref, gc_ref.at[spot], own_sem.at[3]),
        pltpu.make_async_copy(
            stage.at[:, width : width + early], w2_ref.at[pl.ds(pl.multiple_of(spot * part, 16), part)], own_sem.at[4]
        ),
    ]
    for copy in keep:
        copy.start()
    leaving = []

    def leave(*numbers):
        for number in numbers:
            leaving.append(pltpu.make_async_copy(held[number], outs_any[number], out_sem.at[number]))
            leaving[-1].start()

    def make_table():
        for step in range(1, 4):
            links.arrive(lens_all.at[(rank + 4 - step) % 4], l_recv.at[step - 1], nobody)
        lens = lens_all[0] + lens_all[1] + lens_all[2] + lens_all[3]
        packed_table(jnp.broadcast_to(lens[:1], (8, 128)), tab_ref)
        to_scalar = pltpu.make_async_copy(tab_ref, tabs, t_sem.at[0])
        to_scalar.start()
        to_scalar.wait()
        for load in row_loads:
            load.wait()

    sources = (rows_ref, cots_ref)
    outs = (x_ref, cot_ref)

    def picked(kind, target, slot):
        index = block_at(tabs, target * SLOTS + slot) - rank * per_rank
        mine = jnp.logical_and(index >= 0, index < per_rank)
        return mine, sources[kind][jnp.clip(index, 0, per_rank - 1)]

    def mate_copy(kind, piece):
        return pltpu.make_async_remote_copy(
            src_ref=psend.at[kind, piece], dst_ref=precv.at[kind, piece],
            send_sem=p_send.at[kind, piece], recv_sem=p_recv.at[kind, piece],
            device_id={"rep": mate}, device_id_type=MESH,
        )

    def across_copy(kind):
        return pltpu.make_async_remote_copy(
            src_ref=xsend.at[kind], dst_ref=xrecv.at[kind],
            send_sem=x_send.at[kind], recv_sem=x_recv.at[kind],
            device_id={"rep": across}, device_id_type=MESH,
        )

    def pack_rows(kind, piece):
        target = mate if piece == 0 else across_of(mate)

        def pack(slot, carry):
            mine, value = picked(kind, target, slot)
            psend[kind, piece, slot] = jnp.where(mine, value, jnp.zeros_like(value))
            return carry

        lax.fori_loop(0, SLOTS, pack, 0)
        mate_copy(kind, piece).start()

    def cross_rows(kind):
        mate_copy(kind, 1).wait_recv()

        def merge(slot, carry):
            mine, value = picked(kind, across, slot)
            xsend[kind, slot] = jnp.where(mine, value, precv[kind, 1, slot])
            return carry

        lax.fori_loop(0, SLOTS, merge, 0)
        across_copy(kind).start()

    def finish_rows(kind):
        mate_copy(kind, 0).wait_recv()
        across_copy(kind).wait_recv()

        def finish(slot, carry):
            mine, value = picked(kind, rank, slot)
            rows = pl.ds(pl.multiple_of(slot * BLK, BLK), BLK)
            outs[kind][rows, :] = jnp.where(mine, value, precv[kind, 0, slot] + xrecv[kind, slot])
            return carry

        lax.fori_loop(0, SLOTS, finish, 0)

    def norm():
        keep[3].wait()
        gains = gains_of(gc_ref)
        gains_ref[...] = gains
        forward_norm(tabs, rank, x_ref, gains, n_ref)
        leave(2)

    def project():
        keep[0].wait()
        forward_project(n_ref, wqkv_ref, qkv_ref)
        leave(3, 6)

    def attend_tiles(begin, end):
        forward_attention(tabs, rank, qkv_ref, att_ref, lse_ref, begin, end)
        if end == TILES:
            leave(4, 5)

    def enter():
        gain = gains_ref[2:3]
        for tile in range(TILES):
            rows = pl.ds(tile * QT, QT)
            value = x_ref[rows, :].astype(F32) + mm(att_ref[rows, :], w2_ref[:, :D])
            h1_ref[rows, :] = value
            normed = (value * lax.rsqrt(mean_square(value) + EPSILON) * gain).astype(BF16)
            nt_ref[rows, :] = normed
            ntt_ref[:, tile * QT : (tile + 1) * QT] = jnp.transpose(normed)
        leave(8, 9, 10)

    def first_half():
        def step(tile, carry):
            at = pl.multiple_of(tile * FF_TILE, FF_TILE)
            cols = pl.ds(at, FF_TILE)
            gate = mm(nt_ref[...], w2_ref[:, pl.ds(D + at, FF_TILE)])
            up = mm(nt_ref[...], w2_ref[:, pl.ds(D + half + at, FF_TILE)])
            act, slope = gelu_both(gate)
            b0_ref[:, cols] = (act * up).astype(BF16)
            b1_ref[:, cols] = (up * slope).astype(BF16)
            b2_ref[:, cols] = act.astype(BF16)
            for copy in piece_copies(tile):
                copy.start()
            return carry

        lax.fori_loop(0, half // FF_TILE, step, 0)

    def piece_copies(tile):
        cols = pl.ds(pl.multiple_of(tile * FF_TILE, FF_TILE), FF_TILE)
        return [
            pltpu.make_async_copy(held[number].at[:, cols], outs_any[number].at[:, cols], piece_sem.at[number - 11, tile])
            for number in (11, 12, 13)
        ]

    work = {"table": make_table, "enter": enter, "half": first_half, "norm": norm, "proj": project, "a0": lambda: attend_tiles(0, 2),
            "a1": lambda: attend_tiles(2, 4), "a2": lambda: attend_tiles(4, TILES)}
    for action, which, *more in FRONT_ORDER:
        if action == "do":
            work[which]()
        elif action == "own":
            own(which)
        elif action == "hop":
            hop(which, more[0])
        elif action == "fr":
            from_row(which)
        elif action == "yz":
            second_column(which)
        elif action == "xin":
            from_across()
        elif action == "got":
            gathered(which)
            if which == 2:
                keep[4].wait()
            if which == 3:
                leave(7)
        elif action == "pack":
            pack_rows(which, more[0])
        elif action == "cross":
            cross_rows(which)
        else:
            finish_rows(which)
            leave(which)
    gathered(1, 4, 6)

    def sent(shard, carry):
        @pl.when(shard != spot)
        def _():
            pltpu.make_async_remote_copy(
                src_ref=place(6, shard), dst_ref=place(6, shard), send_sem=c_send.at[6, shard], recv_sem=c_recv.at[6, shard],
                device_id={"rep": mate}, device_id_type=MESH,
            ).wait_send()

        return carry

    lax.fori_loop(0, count, sent, 0)
    links.drain()
    for kind in range(2):
        for piece in range(2):
            mate_copy(kind, piece).wait_send()
        across_copy(kind).wait_send()
    for copy in keep[1:3] + leaving:
        copy.wait()
    for tile in range(half // FF_TILE):
        for copy in piece_copies(tile):
            copy.wait()


def gather_and_attend(count, lens, rows, cots, weights, wd, gains):
    outer, inner = grid_of(count)
    block = rows.shape[1:]
    part, hidden = weights[0].shape[0], weights[-1].shape[1]
    dma, shape = pltpu.SemaphoreType.DMA, jax.ShapeDtypeStruct
    total = sum(weight.shape[1] for weight in weights)
    kinds = 6
    held = (shape((ROWS, D), BF16), shape((ROWS, D), BF16), shape((ALL_ROWS, D), BF16), shape((ALL_ROWS, 3 * D), BF16),
            shape((ROWS, D), BF16), shape((TILES, 16, QT), F32), shape((D, 3 * D), BF16), shape((D, D + hidden), BF16), shape((ROWS, D), F32),
            shape((ROWS, D), BF16), shape((D, ROWS), BF16)) + (shape((ROWS, hidden // 2), BF16),) * 3
    return pl.pallas_call(
        partial(front_kernel, outer, inner),
        out_shape=(shape((TABLE_ROWS, 128), jnp.int32), shape((16, D), F32)) + held + (
            shape((count, part, hidden), BF16), shape((count,) + wd.shape, BF16),
        ),
        in_specs=[VMEM] + [ANY] * 9 + [VMEM] * 3,
        out_specs=(VMEM,) * 2 + (ANY,) * 16,
        scratch_shapes=[
            pltpu.VMEM((part, total), BF16), pltpu.VMEM((4, 8, 128), jnp.int32), pltpu.SMEM((TABLE_ROWS, 128), jnp.int32),
            pltpu.VMEM((2, 2, SLOTS) + block, BF16), pltpu.VMEM((2, 2, SLOTS) + block, BF16),
            pltpu.VMEM((2, SLOTS) + block, BF16), pltpu.VMEM((2, SLOTS) + block, BF16),
            pltpu.VMEM(rows.shape, BF16), pltpu.VMEM(cots.shape, BF16),
            pltpu.VMEM((8, 128), jnp.int32), pltpu.VMEM(wd.shape, BF16), pltpu.VMEM((16, 128), BF16),
            *(pltpu.VMEM(one.shape, one.dtype) for one in held), pltpu.VMEM((count, 16, 128), BF16),
            dma((3,)), dma((3,)), dma((1,)), dma((11,)),
            dma((2, outer - 1, kinds, 2)), dma((2, outer - 1, kinds, 2)), dma((outer, kinds)), dma((outer, kinds)),
            dma((kinds + 1, count)), dma((kinds + 1, count)), dma((count,)), dma((count,)), dma((5,)),
            dma((2, 2)), dma((2, 2)), dma((2,)), dma((2,)), dma((1,)), dma((14,)), dma((3, hidden // 2 // FF_TILE)),
        ],
        compiler_params=pltpu.CompilerParams(
            collective_id=1, has_side_effects=True, vmem_limit_bytes=VMEM_LIMIT
        ),
        name="gather_and_attend",
    )(lens, rows, cots, *weights, wd, *gains)


ACROSS_FIRST = (1, 2)
REAR_ORDER = (
    ("do", "start"), ("do", "P0"), ("do", "P1a"), ("do", "gA"), ("begin", 0), ("do", "P1b"), ("pair", 0),
    ("do", "gB"), ("begin", 2), ("do", "uB"), ("begin", 3), ("do", "d"), ("begin", 4), ("pair", 2), ("do", "uA"),
    ("begin", 1), ("pair", 3), ("do", "out"), ("pair", 1), ("pair", 4), ("do", "load"), ("do", "P4"), ("do", "P5"),
    ("col", 0), ("col", 3), ("rows", 0), ("do", "q0"), ("do", "q1"), ("hop", 0, 1), ("meet", 2), ("do", "q2"),
    ("meet", 1), ("col", 4), ("do", "p0"), ("begin", 6), ("do", "bp"), ("rows", 1), ("pair", 6), ("do", "p1"),
    ("hop", 3, 1), ("begin", 5), ("hop", 0, 2), ("begin", 7), ("do", "dc"), ("do", "p2"), ("begin", 8), ("col", 2),
    ("pair", 7), ("hop", 4, 1), ("pair", 5), ("begin", 9), ("hop", 2, 1), ("col", 1), ("col", 6), ("hop", 0, 3),
    ("hop", 4, 2), ("col", 7), ("hop", 3, 2), ("hop", 6, 1), ("cross", 0), ("hop", 1, 1), ("pair", 8), ("hop", 4, 3),
    ("pair", 9), ("hop", 6, 2), ("col", 5), ("hop", 3, 3), ("cross", 4), ("cross", 3), ("hop", 7, 1), ("hop", 1, 2),
    ("hop", 2, 2), ("hop", 5, 1), ("col", 8), ("hop", 1, 3), ("cross", 1), ("hop", 6, 3), ("hop", 5, 2), ("col", 9),
    ("cross", 6), ("relay", 1), ("hop", 5, 3), ("cross", 5), ("hop", 2, 3), ("hop", 7, 2), ("hop", 7, 3),
    ("cross", 2), ("hop", 8, 1), ("relay", 0), ("cross", 7), ("hop", 9, 1), ("hop", 8, 2), ("hop", 9, 2),
    ("hop", 8, 3), ("cross", 8), ("fin", 2), ("fin", 4), ("hop", 9, 3), ("fin", 5), ("fin", 0), ("fin", 1),
    ("cross", 9), ("fin", 7), ("fin", 3), ("fin", 6), ("fin", 8), ("fin", 9),
)


def rear_kernel(outer, inner, *refs):
    (tab_ref, x_any, att_any, lse_ref, gc_ref), refs = refs[:5], refs[5:]
    (cot_any, n_any, qkv_any, wqkv_any, w2_any, wf_any, wd_any), refs = refs[:7], refs[7:]
    (h1_any, nt_any, ntt_any, b0_any, b1_any, b2_any), refs = refs[:6], refs[6:]
    kinds = 10
    (og_ref, ou_ref, od_ref, oo_ref, op_ref, oc_ref, ry_ref, rg_ref), refs = refs[:8], refs[8:]
    (y_ref, gh_ref, fa_ref, dk_ref, b0_ref, b1_ref, b2_ref, n_ref, ntt_ref, gres_ref, ga_ref), refs = refs[:11], refs[11:]
    (x_ref, att_ref), refs = refs[:2], refs[2:]
    (wf_ref, wd_ref, dg_ref, du_ref, db_ref, do_ref, dc_ref, mine_ref), refs = refs[:8], refs[8:]
    crecv, refs = list(refs[:7]), refs[7:]
    narrow = D // 2
    crecv = crecv[:6] + [crecv[i].at[:, :, :, :narrow] for i in range(3)] + crecv[6:]
    yrecv, zrecv, xrecv, stages = (refs[kinds * i : kinds * (i + 1)] for i in range(4))
    refs = refs[4 * kinds :]
    extra, refs = refs[: 2 * len(ACROSS_FIRST)], refs[2 * len(ACROSS_FIRST) :]
    sems = dict(zip(SEM_NAMES, refs))
    load_sem, free_sem = refs[len(SEM_NAMES) :]
    links = Links(outer, inner)
    rank = links.rank
    hidden = wd_ref.shape[0]
    part = wf_ref.shape[2]
    group = 4 * part

    def fetch(number, src, dst):
        copy = pltpu.make_async_copy(src, dst, load_sem.at[number])
        copy.start()
        return copy

    wide, early = hidden // 2, D + hidden
    load_first = [
        fetch(0, cot_any, ga_ref), fetch(1, wd_any.at[:wide], wd_ref.at[:wide]),
        fetch(7, b1_any, b1_ref.at[:ROWS, :wide]), fetch(8, b2_any, b2_ref.at[:ROWS, :wide]),
    ]
    load_products = fetch(9, ntt_any, ntt_ref)
    kept = {}

    def load_rest():
        kept["rest"] = [
            fetch(10, nt_any, n_ref.at[:ROWS]), fetch(2, wf_any, wf_ref.at[:, :, :, early:]),
            fetch(3, wd_any.at[wide:], wd_ref.at[wide:]), fetch(11, b0_any, b0_ref.at[:ROWS, :wide]),
        ]
        kept["late"] = [
            fetch(12, h1_any, fa_ref.at[:ROWS]), fetch(13, w2_any, wf_ref.at[:, :, :, :early]),
            fetch(4, x_any, x_ref), fetch(5, att_any, att_ref),
        ]

    links.greet(later=True)

    def weight(start, size):
        return wf_ref[:, :, :, pl.ds(start, size)].reshape(D, size)

    first, second = slice(0, wide), slice(wide, hidden)
    grads = [dg_ref.at[:, :, :, first], du_ref.at[:, :, :, first], dg_ref.at[:, :, :, second], du_ref.at[:, :, :, second],
             db_ref, do_ref] + [wf_ref.at[:, :, :, i * D : (i + 1) * D] for i in range(3)] + [dc_ref]
    totals = [og_ref.at[:, first], ou_ref.at[:, first], og_ref.at[:, second], ou_ref.at[:, second],
              od_ref, oo_ref] + [op_ref.at[:, i * D : (i + 1) * D] for i in range(3)] + [oc_ref]
    tasks = [
        (AcrossFirst if i in ACROSS_FIRST else Reduction)(
            links, grads[i], totals[i], mine_ref if i == kinds - 1 else None,
            crecv[i], yrecv[i], zrecv[i], xrecv[i], stages[i], sems, i,
        )
        for i in range(kinds)
    ]
    for number, i in enumerate(ACROSS_FIRST):
        tasks[i].third, tasks[i].stage_two = extra[2 * number], extra[2 * number + 1]
    returns = (Return(links, y_ref, ry_ref, sems, 0), Return(links, gres_ref, rg_ref, sems, 1))
    gains = gc_ref[...]
    gain = gains[2:3]
    valid = valid_column(tab_ref, rank)
    h1_ref, dv_ref = fa_ref, fa_ref
    tiles = hidden // FF_TILE
    half = tiles // 2

    def enter():
        for load in load_first:
            load.wait()
        load_products.wait()
        load_rest()
        for tile in range(TILES):
            rows = pl.ds(tile * QT, QT)
            gres_ref[rows, :] = (ga_ref[rows, :].astype(F32) * valid[tile * QT : (tile + 1) * QT]).astype(BF16)

    def first_half():
        def step(tile, carry):
            cols = pl.ds(pl.multiple_of(tile * FF_TILE, FF_TILE), FF_TILE)
            back = mm_cols(gres_ref[...], wd_ref[cols, :])
            b1_ref[:ROWS, cols] = (back * b1_ref[:ROWS, cols].astype(F32)).astype(BF16)
            b2_ref[:ROWS, cols] = (back * b2_ref[:ROWS, cols].astype(F32)).astype(BF16)
            return carry

        lax.fori_loop(0, half, step, 0)

    def second_half():
        for load in kept["rest"]:
            load.wait()

        def step(tile, carry):
            at = pl.multiple_of(tile * FF_TILE, FF_TILE)
            cols = pl.ds(at, FF_TILE)
            normed = n_ref[:ROWS, :]
            gate = mm(normed, weight(early - wide + at, FF_TILE))
            up = mm(normed, weight(early + at, FF_TILE))
            back = mm_cols(gres_ref[...], wd_ref[cols, :])
            act, slope = gelu_both(gate)
            b0_ref[:ROWS, cols] = (act * up).astype(BF16)
            b1_ref[:ROWS, cols] = (back * up * slope).astype(BF16)
            b2_ref[:ROWS, cols] = (back * act).astype(BF16)
            return carry

        lax.fori_loop(half, tiles, step, 0)

    def outer_products(ref, right_ref, begin, end):
        def step(tile, carry):
            cols = pl.ds(pl.multiple_of(tile * FF_TILE, FF_TILE), FF_TILE)
            value = mm(ntt_ref[...], right_ref[:ROWS, cols]).astype(BF16)
            ref[:, :, :, cols] = value.reshape(outer, inner, part, FF_TILE)
            return carry

        lax.fori_loop(begin, end, step, 0)

    def down_products():
        def step(tile, carry):
            cols = pl.ds(pl.multiple_of(tile * FF_TILE, FF_TILE), FF_TILE)
            db_ref[tile // inner, tile % inner] = mm_rows(b0_ref[:ROWS, cols], gres_ref[...]).astype(BF16)
            return carry

        lax.fori_loop(0, tiles, step, 0)

    def outward():
        for load in kept["late"]:
            load.wait()

        def step(tile, carry):
            cols = pl.ds(pl.multiple_of(tile * group, 128), group)
            value = h1_ref[:ROWS, cols] + mm(b0_ref[:ROWS, :hidden], wd_ref[:, cols])
            y_ref[:, cols] = (value * valid).astype(BF16)
            shards = pl.ds(tile * (4 // inner), 4 // inner)
            total = None
            for number, (ref, low) in enumerate(((b1_ref, 0), (b2_ref, 0), (b1_ref, wide), (b2_ref, wide))):
                at = D + number * wide
                term = mm_cols(
                    ref[:ROWS, low : low + wide], wf_ref[shards, :, :, at : at + wide].reshape(group, wide)
                )
                total = term if total is None else total + term
            gh_ref[:, cols] = total
            return carry

        lax.fori_loop(0, D // group, step, 0)

    def load():
        kept["qkv"] = fetch(14, qkv_any, b1_ref)
        kept["wqkv"] = fetch(15, wqkv_any, b2_ref)

    def middle():
        gain_grad = jnp.zeros((1, D), F32)
        for tile in range(TILES):
            rows = pl.ds(tile * QT, QT)
            value, grad = h1_ref[rows, :], gh_ref[rows, :]
            root = lax.rsqrt(mean_square(value) + EPSILON)
            unit = value * root
            gain_grad = gain_grad + jnp.sum(grad * unit, axis=0, keepdims=True)
            grad = grad * gain
            grad = gres_ref[rows, :].astype(F32) + root * (
                grad - unit * jnp.mean(grad * unit, axis=-1, keepdims=True)
            )
            gh_ref[rows, :] = grad
            low = grad.astype(BF16)
            n_ref[rows, :] = low
            ga_ref[rows, :] = mm_cols(low, weight(0, D)).astype(BF16)
        kept["gain"] = gain_grad

    def out_products():
        def step(tile, carry):
            cols = pl.ds(pl.multiple_of(tile * QUAD, QUAD), QUAD)
            value = mm_rows(att_ref[...], n_ref[:ROWS, cols]).astype(BF16)
            do_ref[:, :, :, cols] = value.reshape(outer, inner, part, QUAD)
            return carry

        lax.fori_loop(0, D // QUAD, step, 0)
        kept["n"] = fetch(6, n_any, n_ref)

    def attention(quad):
        if quad == 0:
            backward_attention_start(dk_ref, dv_ref)
            kept["qkv"].wait()
        backward_attention_quad(tab_ref, rank, b1_ref, att_ref, ga_ref, lse_ref, b0_ref, dk_ref, dv_ref, quad)

    def project_products(quad):
        if quad == 0:
            kept["n"].wait()
        for number in range(3):
            value = mm_rows(n_ref[...], b0_ref[:, number * D + quad * QUAD : number * D + (quad + 1) * QUAD])
            low = (quad * 3 + number) * QUAD
            wf_ref[:, :, :, low : low + QUAD] = value.astype(BF16).reshape(outer, inner, part, QUAD)

    def input_gradient():
        kept["wqkv"].wait()
        kept["one"], kept["side"] = backward_project(
            tab_ref, rank, x_ref, gh_ref, gains, n_ref, b0_ref, b2_ref, dk_ref, gres_ref
        )

    def gain_pieces():
        rows = jnp.concatenate([kept["one"], kept["side"], kept["gain"], jnp.zeros((5, D), F32)], axis=0)
        spread_gain_grads(rows, dc_ref)

    work = {
        "start": lambda: None, "load": load, "P0": enter, "P1a": first_half, "P1b": second_half,
        "gA": lambda: outer_products(dg_ref, b1_ref, 0, half), "gB": lambda: outer_products(dg_ref, b1_ref, half, tiles),
        "uA": lambda: outer_products(du_ref, b2_ref, 0, half), "uB": lambda: outer_products(du_ref, b2_ref, half, tiles),
        "d": down_products, "out": outward, "P4": middle, "P5": out_products,
        "q0": lambda: attention(0), "q1": lambda: attention(1), "q2": lambda: attention(2),
        "p0": lambda: project_products(0), "p1": lambda: project_products(1), "p2": lambda: project_products(2),
        "bp": input_gradient, "dc": gain_pieces,
    }
    paired, begun = set(), set()
    for action, which, *turn in REAR_ORDER:
        if action == "do":
            work[which]()
        elif action == "begin":
            if not begun:
                links.met()
            begun.add(which)
            if which == 6:
                pl.semaphore_wait(free_sem, 1)
            tasks[which].begin()
        elif action == "pair":
            tasks[which].pair()
            paired.add(which)
            if which < 3 and paired >= {0, 1, 2}:
                pl.semaphore_signal(free_sem, inc=1, device_id={"rep": links.mate}, device_id_type=MESH)
        elif action == "meet":
            tasks[which].meet()
        elif action == "col":
            tasks[which].column()
        elif action == "hop":
            tasks[which].hop(turn[0])
        elif action == "cross":
            tasks[which].cross()
        elif action == "fin":
            tasks[which].finish()
        elif action == "rows":
            returns[which].begin()
        else:
            returns[which].relay()
    for one in returns:
        one.settle()
    for task in tasks:
        task.settle()
    links.drain()


def feed_and_reduce(count, table, x, att, lse, gc, cot, n, qkv, wqkv, w2, wf, wd, *firsts):
    outer, inner = grid_of(count)
    part, tall = D // count, wd.shape[1]
    hidden = count * tall
    wf = wf.reshape((outer, inner) + wf.shape[1:])
    w2 = w2.reshape(outer, inner, part, -1)
    full = [(part, hidden), (part, hidden), (tall, D), (part, D), (part, 3 * D), (8, 128)]
    shapes = [(part, hidden // 2)] * 4 + [(tall, D)] + [(part, D)] * 4 + [(8, 128)]
    kinds = len(shapes)
    dtypes = [BF16] * (kinds - 1) + [F32]
    halved = [(a, b // 2 if b % 256 == 0 else b) for a, b in shapes]
    later = [(a // 2, b) if i in ACROSS_FIRST else (a, b) for i, (a, b) in enumerate(halved)]
    dma, vmem = pltpu.SemaphoreType.DMA, pltpu.VMEM
    scratch = [
        vmem((ROWS, D), BF16), vmem((ROWS, D), F32), vmem((ALL_ROWS, D), F32), vmem((ALL_ROWS, D), F32),
        vmem((ALL_ROWS, 3 * D), BF16), vmem((ALL_ROWS, 3 * D), BF16), vmem((D, 3 * D), BF16),
        vmem((ALL_ROWS, D), BF16), vmem((D, ROWS), BF16), vmem((ROWS, D), BF16), vmem((ROWS, D), BF16),
        vmem((ROWS, D), BF16), vmem((ROWS, D), BF16),
        vmem((outer, inner, part, D + 2 * hidden), BF16), vmem((hidden, D), BF16),
    ]
    scratch += [vmem((outer, inner) + shape, BF16) for shape in full[:4]]
    scratch += [vmem((outer, inner) + full[-1], F32)] * 2
    scratch += [vmem((outer, inner) + halved[i], dtypes[i]) for i in (0, 1, 2, 3, 4, 5, 9)]
    for lead in ((outer,), (outer + 1,), ()):
        for i in range(kinds):
            across = (outer, inner) if i in ACROSS_FIRST and lead == () else lead
            scratch.append(vmem(across + later[i], dtypes[i]))
    scratch += [vmem(shape, F32) for shape in later]
    for i in ACROSS_FIRST:
        scratch += [vmem(later[i], BF16), vmem(later[i], F32)]
    one = dma((kinds,))
    scratch += [one, one, one, one, one, dma((2, outer, kinds)), dma((outer + 1, kinds))] + [one] * 9
    scratch += [dma((2, 3)), dma((2, 3)), dma((2,)), dma((1,)), dma((16,)), pltpu.SemaphoreType.REGULAR]
    rows = jax.ShapeDtypeStruct((4, ROWS, D), BF16)
    outs = pl.pallas_call(
        partial(rear_kernel, outer, inner),
        out_shape=tuple(jax.ShapeDtypeStruct(shape, F32) for shape in full) + (rows, rows),
        in_specs=[SMEM] + [ANY] * 2 + [VMEM] * 2 + [ANY] * 13,
        out_specs=(ANY,) * 8,
        scratch_shapes=scratch,
        compiler_params=pltpu.CompilerParams(
            collective_id=2, has_side_effects=True, vmem_limit_bytes=67043328
        ),
        name="feed_and_reduce",
    )(table, x, att, lse, gc, cot, n, qkv, wqkv, w2, wf, wd.reshape(hidden, D), *firsts)
    return outs[:6], outs[6], outs[7]


def place_kernel(part, tab_ref, ry_ref, rg_ref, og_ref, ou_ref, od_ref, oo_ref, op_ref, oc_ref, *refs):
    (y_ref, g_ref, q_out, k_out, v_out, o_out, g_out, u_out, d_out, one_out, side_out, two_out), refs = refs[:12], refs[12:]
    (y_buf, g_buf, zero, bg, bu, bd, bo, bp, sem_in, sem_out, sem_rows, sem_home) = refs
    blocks = y_buf.shape[0]
    base = lax.axis_index("rep") * blocks
    tables = ((og_ref, bg), (ou_ref, bu), (od_ref, bd), (oo_ref, bo), (op_ref, bp))
    reads = [pltpu.make_async_copy(src, dst, sem_in.at[i]) for i, (src, dst) in enumerate(tables)]
    rows = ((ry_ref, y_buf, y_ref), (rg_ref, g_buf, g_ref))

    for read in reads:
        read.start()
    zero[...] = jnp.zeros(zero.shape, zero.dtype)

    def fetch(block, carry):
        index = tab_ref[48, base + block]
        safe = jnp.maximum(index, 0)
        for kind, (src, buf, dst) in enumerate(rows):
            @pl.when(index >= 0)
            def _():
                pltpu.make_async_copy(
                    src.at[lax.div(safe, SLOTS), lax.rem(safe, SLOTS)], buf.at[block], sem_rows.at[kind, block]
                ).start()

            @pl.when(index < 0)
            def _():
                pltpu.make_async_copy(zero, dst.at[block], sem_home.at[kind, block]).start()

        return carry

    lax.fori_loop(0, blocks, fetch, 0)
    for number, out in enumerate((one_out, side_out, two_out)):
        out[...] = oc_ref[number, :part]
    writes = []
    for number, (buf, dst) in enumerate(((bg, g_out), (bu, u_out), (bd, d_out), (bo, o_out))):
        reads[number].wait()
        writes.append(pltpu.make_async_copy(buf, dst, sem_out.at[number]))
        writes[-1].start()
    reads[4].wait()
    for quad in range(D // QUAD):
        for number, dst in enumerate((q_out, k_out, v_out)):
            low = (3 * quad + number) * QUAD
            copy = pltpu.make_async_copy(
                bp.at[:, low : low + QUAD], dst.at[:, quad * QUAD : (quad + 1) * QUAD], sem_out.at[4 + 3 * quad + number]
            )
            copy.start()
            writes.append(copy)
    def leave(block, carry):
        @pl.when(tab_ref[48, base + block] >= 0)
        def _():
            for kind, (src, buf, dst) in enumerate(rows):
                pltpu.make_async_copy(src.at[0, 0], buf.at[block], sem_rows.at[kind, block]).wait()
                pltpu.make_async_copy(buf.at[block], dst.at[block], sem_home.at[kind, block]).start()

        return carry

    lax.fori_loop(0, blocks, leave, 0)
    for write in writes:
        write.wait()

    def rest(block, carry):
        for kind, (_, buf, dst) in enumerate(rows):
            pltpu.make_async_copy(buf.at[block], dst.at[block], sem_home.at[kind, block]).wait()
        return carry

    lax.fori_loop(0, blocks, rest, 0)


def place_all(table, ry, rg, totals, blocks, part, shape):
    out = jax.ShapeDtypeStruct
    og, ou, od, oo, op, oc = totals
    block = (blocks,) + ry.shape[2:]
    dma, vmem = pltpu.SemaphoreType.DMA, pltpu.VMEM
    gain = out((part,), F32)
    y, g, q, k, v, o, gate, up, down, one, side, two = pl.pallas_call(
        partial(place_kernel, part),
        out_shape=(out(block, ry.dtype), out(block, rg.dtype), out(oo.shape, F32), out(oo.shape, F32), out(oo.shape, F32),
                   out(oo.shape, F32), out(og.shape, F32), out(ou.shape, F32), out(od.shape, F32), gain, gain, gain),
        in_specs=[SMEM] + [ANY] * 7 + [VMEM],
        out_specs=(ANY,) * 9 + (VMEM,) * 3,
        scratch_shapes=[vmem(block, ry.dtype), vmem(block, rg.dtype), vmem(block[1:], ry.dtype)] + [vmem(t.shape, F32) for t in totals[:5]]
        + [dma((5,)), dma((13,)), dma((2, blocks)), dma((2, blocks))],
        compiler_params=pltpu.CompilerParams(vmem_limit_bytes=VMEM_LIMIT),
        name="place_outputs",
    )(table, ry, rg, og, ou, od, oo, op, oc)
    return (y.reshape(shape), g.reshape(shape), one, side, q, k, v, o, two, gate, up, down)


def per_device(count, layer_input, cotangent, lengths, attn_gain, global_gain, query_weight, key_weight,
               value_weight, out_weight, ffn_gain, gate_weight, up_weight, down_weight):
    micro, span, width = layer_input.shape
    hidden = gate_weight.shape[1]
    blocks = micro * span // BLK
    part = attn_gain.shape[0]
    rows_in = layer_input.reshape(blocks, BLK, width)
    cots_in = cotangent.reshape(blocks, BLK, width)
    weights = (query_weight, key_weight, value_weight, out_weight, gate_weight, up_weight)
    gains = (attn_gain, global_gain, ffn_gain)
    if grid_of(count)[1] == 2 and part % 16 == 0:
        table, gains, x, cot, n, qkv, att, lse, wqkv, w2, *firsts, ga, gb = gather_and_attend(
            count, lengths, rows_in, cots_in, weights, down_weight, gains
        )
        totals, ry, rg = feed_and_reduce(count, table, x, att, lse, gains, cot, n, qkv, wqkv, w2, ga, gb, *firsts)
        ry, rg = (rows.reshape(4, SLOTS, BLK, width) for rows in (ry, rg))
        return place_all(table, ry, rg, totals, blocks, part, layer_input.shape)
    else:
        table = deal_table(lengths)
        wc = jnp.pad(jnp.stack(gains), ((0, 13), (0, 128 - part)))
        splits = ((0, 4 * width), (4 * width, 2 * hidden))
        ga, gb, gc, rows, cots = gather_weights(
            count, splits, table, rows_in, cots_in, jnp.concatenate(weights, axis=1), down_weight, wc
        )
        x, full = rows.reshape(ROWS, width), ga.reshape(width, -1)
        n, qkv, att, lse = attend(table, x, gc, full)
        y, gh, gatt, dg, du, db, do, gain = feed(
            table, x, cots.reshape(ROWS, width), att, gc, full, gb.reshape(-1, width)
        )
        g, dw, dc = backward_layer(table, x, gh, gatt, att, lse, n, qkv, gain, gc, full)
        grads = [grad.reshape(count, -1, grad.shape[-1]) for grad in (dg, du, db, do, dw, dc)]
        og, ou, ob, oo, ow, oc, ry, rg = reduce_grads(
            count, grads, y.reshape(SLOTS, BLK, width), g.reshape(SLOTS, BLK, width)
        )
        oq, ok, ov = ow[:, :width], ow[:, width : 2 * width], ow[:, 2 * width :]
    y_home, g_home = bring_home(table, ry, rg, blocks)
    return (
        y_home.reshape(layer_input.shape), g_home.reshape(layer_input.shape),
        oc[0, :part], oc[1, :part], oq, ok, ov, oo, oc[2, :part], og, ou, ob,
    )


def solution(mesh):
    rows = P(None, ("rep", "fsdp"), None)
    vector, matrix = P("fsdp"), P("fsdp", None)
    return jax.shard_map(
        partial(per_device, mesh.shape["fsdp"]),
        mesh=mesh,
        in_specs=(rows, rows, P(None, ("rep", "fsdp")), vector, vector, matrix, matrix, matrix, matrix,
                  vector, matrix, matrix, matrix),
        out_specs=(rows, rows, vector, vector, matrix, matrix, matrix, matrix, vector, matrix, matrix, matrix),
        check_vma=False,
    )
```
